32 devices in a mesh: dp: 16 (over z, y, core), tensor: 2 (over x).
Axes of the slice: x: 2, y: 2, z: 4, core: 2. Of those that a mesh axis runs over, the one named last changes fastest.
Arguments:
- layer_input: bfloat16 [16384, 1024], P('dp'), may hold values from -6 to 6
- w_norm1: bfloat16 [1024], P('dp'), may hold values from 0.5 to 1.5
- w_zx: bfloat16 [1024, 2, 1536], P('dp', None, 'tensor'), may hold values from -0.1875 to 0.1875
- w_bc: bfloat16 [1024, 256], P('dp'), may hold values from -0.1875 to 0.1875
- w_dt: bfloat16 [1024, 24], P('dp', 'tensor'), may hold values from -0.1875 to 0.1875
- conv_x: bfloat16 [4, 1536], P(None, 'tensor'), may hold values from -3 to 3
- conv_xb: bfloat16 [1536], P('tensor'), may hold values from -3 to 3
- conv_bc: bfloat16 [4, 256], replicated, may hold values from -3 to 3
- conv_bcb: bfloat16 [256], replicated, may hold values from -3 to 3
- dt_bias: bfloat16 [24], P('tensor'), may hold values from -6.875 to -2.296875
- a_log: bfloat16 [24], P('tensor'), may hold values from 0 to 2.765625
- d_skip: bfloat16 [24], P('tensor'), may hold values from 0.5 to 1.5
- w_mnorm: bfloat16 [1536], P('tensor'), may hold values from 0.5 to 1.5
- w_mout: bfloat16 [1536, 1024], P('tensor', 'dp'), may hold values from -0.15625 to 0.15625
- query_key_value_weight: bfloat16 [1024, 2, 384], P('dp', 'tensor'), may hold values from -4 to 4
- output_weight: bfloat16 [2, 256, 1024], P('tensor', None, 'dp'), may hold values from -1 to 1
- w_norm2: bfloat16 [1024], P('dp'), may hold values from 0.5 to 1.5
- w_gu: bfloat16 [1024, 2, 2048], P('dp', None, 'tensor'), may hold values from -0.1875 to 0.1875
- w_down: bfloat16 [2048, 1024], P('tensor', 'dp'), may hold values from -0.125 to 0.125
- grad_output: bfloat16 [16384, 1024], P('dp'), may hold values from -6 to 6
Outputs:
- layer_output: bfloat16 [16384, 1024], P('dp')
- grad_x: float32 [16384, 1024], P('dp')
- grad_norm1: float32 [1024], P('dp')
- grad_zx: float32 [1024, 2, 1536], P('dp', None, 'tensor')
- grad_bc: float32 [1024, 256], P('dp', 'tensor')
- grad_dt: float32 [1024, 24], P('dp', 'tensor')
- grad_conv_x: float32 [4, 1536], P(None, 'tensor')
- grad_conv_xb: float32 [1536], P('tensor')
- grad_conv_bc: float32 [4, 256], P(None, 'tensor')
- grad_conv_bcb: float32 [256], P('tensor')
- grad_dt_bias: float32 [24], P('tensor')
- grad_a_log: float32 [24], P('tensor')
- grad_d_skip: float32 [24], P('tensor')
- grad_mnorm: float32 [1536], P('tensor')
- grad_mout: float32 [1536, 1024], P('tensor', 'dp')
- grad_qkv: float32 [1024, 2, 384], P('dp', 'tensor')
- grad_o: float32 [2, 256, 1024], P('tensor', None, 'dp')
- grad_norm2: float32 [1024], P('dp')
- grad_gu: float32 [1024, 2, 2048], P('dp', None, 'tensor')
- grad_down: float32 [2048, 1024], P('tensor', 'dp')
The draws below stay inside these ranges and needn't reach their ends.
All inputs are finite; a program needn't handle non-finite values.
Results may differ from the reference program's by a relative error of at most 0.013.
Values may be sent and summed in bfloat16 or wider, within the bound.
A program may use at most 256 MiB of HBM per device.

```python
import math
from functools import partial
import jax
import jax.numpy as jnp
from jax import lax

MODEL_WIDTH = 1024
QUERY_HEADS = 8
KEY_VALUE_HEADS = 2
HEAD_SIZE = 64
MH = 24
MP = 64
NS = 128
FF = 2048
KCONV = 4
SPAN = 128
SEQ = 1024
QUERIES_PER_KEY = 4
TOKENS = 16384


def draw_query_key_value_weight(key, part):
    group_width = QUERY_HEADS // KEY_VALUE_HEADS
    base_value = jax.random.truncated_normal(jax.random.fold_in(key, 11), -4.0, 4.0, (MODEL_WIDTH, KEY_VALUE_HEADS, (group_width + 2) * HEAD_SIZE), jnp.float32) * MODEL_WIDTH ** (-0.5)
    return base_value.astype(jnp.bfloat16)


def block_scale(rng, extent, cuts, smallest, high):
    level = 1.0
    for dim, parts in cuts:
        steps = jax.random.uniform(jax.random.fold_in(jax.random.fold_in(rng, 6), dim), (parts,), jnp.float32, smallest / len(cuts), high / len(cuts))
        level = level * jnp.repeat(jnp.exp(steps), extent[dim] // parts).reshape((-1,) + (1,) * (len(extent) - 1 - dim))
    return level


def centred(key, extent, spread, limit, cuts=(), kind=jnp.bfloat16):
    array = jax.random.normal(key, extent, jnp.float32) * spread
    if len(cuts) > 0:
        array = block_scale(key, extent, cuts, -0.22, 0.18) * array
    return jnp.clip(array, min=-limit, max=limit).astype(kind)


def setup_inputs(seed: int = 0) -> dict:
    splits = jax.random.split(jax.random.key(seed), 21)
    layer_input = centred(splits[0], (TOKENS, MODEL_WIDTH), 1.0, 6.0, ((0, 16),))
    w_norm1 = jnp.clip(1.0 + 0.1 * jax.random.normal(splits[1], (MODEL_WIDTH,), jnp.float32), 0.5, 1.5).astype(jnp.bfloat16)
    w_zx = centred(splits[2], (MODEL_WIDTH, 2, MH * MP), MODEL_WIDTH ** -0.5, 0.1875, ((0, 16), (2, 2)))
    w_bc = centred(splits[3], (MODEL_WIDTH, 2 * NS), MODEL_WIDTH ** -0.5, 0.1875, ((0, 16),))
    w_dt = centred(splits[4], (MODEL_WIDTH, MH), MODEL_WIDTH ** -0.5, 0.1875, ((0, 16), (1, 2)))
    conv_x = centred(splits[5], (KCONV, MH * MP), KCONV ** -0.5, 3.0, ((1, 2),))
    conv_xb = centred(splits[6], (MH * MP,), 0.5, 3.0, ((0, 2),))
    conv_bc = centred(splits[7], (KCONV, 2 * NS), KCONV ** -0.5, 3.0)
    conv_bcb = centred(splits[8], (2 * NS,), 0.5, 3.0)
    dt_bias = jnp.clip(-6.875 + 4.578125 * jax.random.uniform(splits[9], (MH,), jnp.float32) ** block_scale(splits[9], (MH,), ((0, 2),), -0.2, 0.2), -6.875, -2.296875).astype(jnp.bfloat16)
    a_log = jnp.clip(2.765625 * jax.random.uniform(splits[10], (MH,), jnp.float32) ** block_scale(splits[10], (MH,), ((0, 2),), -0.2, 0.2), 0.0, 2.765625).astype(jnp.bfloat16)
    d_skip = jnp.clip(0.5 + 1.0 * jax.random.uniform(splits[11], (MH,), jnp.float32) ** block_scale(splits[11], (MH,), ((0, 2),), -0.2, 0.2), 0.5, 1.5).astype(jnp.bfloat16)
    w_mnorm = jnp.clip(1.0 + 0.1 * jax.random.normal(splits[12], (MH * MP,), jnp.float32), 0.5, 1.5).astype(jnp.bfloat16)
    w_mout = centred(splits[13], (MH * MP, MODEL_WIDTH), (MH * MP) ** -0.5, 0.15625, ((0, 2), (1, 16)))
    query_key_value_weight = draw_query_key_value_weight(jax.random.fold_in(splits[20], 71), 0)
    output_weight = centred(splits[15], (KEY_VALUE_HEADS, QUERIES_PER_KEY * HEAD_SIZE, MODEL_WIDTH), (QUERY_HEADS * HEAD_SIZE // 16) ** -0.5, 1.0, ((0, 2), (2, 16)))
    w_norm2 = jnp.clip(1.0 + 0.1 * jax.random.normal(splits[16], (MODEL_WIDTH,), jnp.float32), 0.5, 1.5).astype(jnp.bfloat16)
    w_gu = centred(splits[17], (MODEL_WIDTH, 2, FF), MODEL_WIDTH ** -0.5, 0.1875, ((0, 16), (2, 2)))
    w_down = centred(splits[18], (FF, MODEL_WIDTH), FF ** -0.5, 0.125, ((0, 2), (1, 16)))
    grad_output = centred(splits[19], (TOKENS, MODEL_WIDTH), 1.0, 6.0, ((0, 16),))
    return {"layer_input": layer_input, "w_norm1": w_norm1, "w_zx": w_zx, "w_bc": w_bc, "w_dt": w_dt, "conv_x": conv_x, "conv_xb": conv_xb, "conv_bc": conv_bc, "conv_bcb": conv_bcb, "dt_bias": dt_bias, "a_log": a_log, "d_skip": d_skip, "w_mnorm": w_mnorm, "w_mout": w_mout, "query_key_value_weight": query_key_value_weight, "output_weight": output_weight, "w_norm2": w_norm2, "w_gu": w_gu, "w_down": w_down, "grad_output": grad_output}


EPSILON = 1e-05
FULL_PRECISION = lax.Precision.HIGHEST
LOG_BASE = math.log(100000000000.0)
MASKED = -1e+30

@jax.custom_vjp
def low(v):
    return lax.optimization_barrier(v.astype(jnp.bfloat16)).astype(jnp.float32)

@jax.custom_vjp
def lowered_backward(v):
    return v

def low_keep(v):
    return (low(v), None)

def low_pass(kept, grad):
    return (grad,)

def back_keep(v):
    return (v, None)

def back_low(kept, grad):
    return (low(grad),)
low.defvjp(low_keep, low_pass)
lowered_backward.defvjp(back_keep, back_low)

def rms_norm(values, scale_gain):
    return values * lax.rsqrt(lax.optimization_barrier(jnp.mean(values * values, axis=-1, keepdims=True)) + EPSILON) * scale_gain

def rotary(values, direction):
    token_length = values.shape[0]
    half_dim = values.shape[-1] // 2
    exponent = jnp.arange(half_dim, dtype=jnp.float32) * (-2.0 * LOG_BASE / values.shape[-1])
    angles = jnp.arange(token_length, dtype=jnp.float32)[:, None] * jnp.exp(exponent)[None, :]
    target = (token_length,) + (1,) * (values.ndim - 2) + (half_dim,)
    cosine = jnp.cos(angles).reshape(target)
    sine_part = direction * jnp.sin(angles).reshape(target)
    first_half = values[..., :half_dim]
    second_half = values[..., half_dim:]
    return jnp.concatenate([first_half * cosine - second_half * sine_part, second_half * cosine + first_half * sine_part], axis=-1)

def state_scan(inputs, step_size, decay_rate, b_proj, c_proj):
    token_length, heads, head_width = inputs.shape
    blocks = token_length // SPAN
    rates = (step_size * decay_rate[None, :]).reshape(blocks, SPAN, heads)
    cumlog = jnp.cumsum(rates, axis=1)
    scaled = (inputs * step_size[:, :, None]).reshape(blocks, SPAN, heads, head_width)
    b_block = b_proj.reshape(blocks, SPAN, -1)
    c_block = c_proj.reshape(blocks, SPAN, -1)
    row_index = lax.broadcasted_iota(jnp.int32, (SPAN, SPAN), 0)
    col_index = lax.broadcasted_iota(jnp.int32, (SPAN, SPAN), 1)
    causal = (col_index <= row_index)[None, :, :, None]
    differ = cumlog[:, :, None, :] - cumlog[:, None, :, :]
    within = jnp.exp(jnp.where(causal, differ, MASKED))
    intersection_cb = jnp.einsum('cin,cjn->cij', c_block, b_block, precision=FULL_PRECISION)
    inner = jnp.einsum('cijh,cjhp->cihp', intersection_cb[:, :, :, None] * within, scaled, precision=FULL_PRECISION)
    tails = jnp.exp(cumlog[:, -1:, :] - cumlog)
    states = jnp.einsum('cjn,cjhp->chnp', b_block, scaled * tails[:, :, :, None], precision=FULL_PRECISION)
    carried = jnp.exp(cumlog[:, -1, :])

    def advance(state, item):
        factor, fresh = item
        return (factor[:, None, None] * state + fresh, state)
    start = jnp.zeros(states.shape[1:], jnp.float32)
    unused, entering = lax.scan(advance, start, (carried, states))
    outer = jnp.einsum('cin,chnp->cihp', c_block, entering, precision=FULL_PRECISION) * jnp.exp(cumlog)[:, :, :, None]
    return (inner + outer).reshape(token_length, heads, head_width)

def causal_conv(inputs, taps, bias):
    token_length = inputs.shape[0]
    padded = jnp.pad(inputs, ((KCONV - 1, 0), (0, 0)))
    conv_out = bias[None, :] + jnp.zeros_like(inputs)
    for tap_index in range(KCONV):
        conv_out = conv_out + taps[tap_index][None, :] * padded[tap_index:tap_index + token_length]
    return conv_out

def shared_proj(bc_pre, taps, bias):
    return jax.nn.silu(causal_conv(bc_pre, taps, bias))

def mamba_core(zx_rows, shared, step_raw, conv_taps, conv_bias, step_bias, log_rate, skip_gain):
    token_length = zx_rows.shape[0]
    heads = step_raw.shape[1]
    channels = heads * MP
    gate_part = zx_rows[:, :channels]
    inputs = jax.nn.silu(causal_conv(zx_rows[:, channels:], conv_taps, conv_bias)).reshape(token_length, heads, MP)
    b_proj = shared[:, :NS]
    c_proj = shared[:, NS:]
    step_size = jax.nn.softplus(step_raw + step_bias[None, :])
    decay_rate = -jnp.exp(log_rate)
    scanned = state_scan(inputs, step_size, decay_rate, b_proj, c_proj) + skip_gain[None, :, None] * inputs
    return scanned.reshape(token_length, channels) * jax.nn.silu(gate_part)

def attention_ref(query_key_value_rows):
    token_length = query_key_value_rows.shape[0]
    group_width = QUERY_HEADS // KEY_VALUE_HEADS
    query_rows = query_key_value_rows[:, :, :group_width * HEAD_SIZE].reshape(token_length, KEY_VALUE_HEADS, group_width, HEAD_SIZE)
    keys_raw = query_key_value_rows[:, :, group_width * HEAD_SIZE:(group_width + 1) * HEAD_SIZE]
    values = low(query_key_value_rows[:, :, (group_width + 1) * HEAD_SIZE:])
    query_rows = low(rotary(query_rows, 1.0))
    keys_rot = low(rotary(keys_raw, 1.0))
    raw = lowered_backward(jnp.einsum('igkd,jgd->gkij', query_rows, keys_rot, precision=FULL_PRECISION))
    scores = raw * HEAD_SIZE ** (-0.5)
    row_index = lax.broadcasted_iota(jnp.int32, (token_length, token_length), 0)
    col_index = lax.broadcasted_iota(jnp.int32, (token_length, token_length), 1)
    scores = jnp.where((col_index <= row_index)[None, None], scores, MASKED)
    totals = jax.nn.logsumexp(scores, axis=-1, keepdims=True)
    probs = low(jnp.exp(scores - totals))
    attended = jnp.einsum('gkij,jgd->igkd', probs, values, precision=FULL_PRECISION)
    return low(lowered_backward(attended.reshape(token_length, QUERY_HEADS * HEAD_SIZE)))

def layer_rows(sequence_rows, weights):
    norm_one, w_zx, w_bc, w_dt, conv_x, conv_xb, conv_bc, conv_bcb, dt_bias, a_log, d_skip, w_mnorm, w_mout, query_key_value_weight, output_weight, norm_two, w_gu, w_down = weights
    hidden_state = low(rms_norm(sequence_rows, norm_one))
    zx_rows = lowered_backward(jnp.dot(hidden_state, w_zx.reshape(MODEL_WIDTH, -1), precision=FULL_PRECISION))
    bc_pre = lowered_backward(jnp.dot(hidden_state, w_bc, precision=FULL_PRECISION))
    step_raw = lowered_backward(jnp.dot(hidden_state, w_dt, precision=FULL_PRECISION))
    shared = shared_proj(bc_pre, conv_bc, conv_bcb)
    gated = mamba_core(zx_rows, shared, step_raw, conv_x, conv_xb, dt_bias, a_log, d_skip)
    mamba_out = low(rms_norm(gated, w_mnorm))
    query_key_value_rows = lowered_backward(jnp.dot(hidden_state, query_key_value_weight.reshape(MODEL_WIDTH, -1), precision=FULL_PRECISION)).reshape(-1, KEY_VALUE_HEADS, query_key_value_weight.shape[2])
    attended = attention_ref(query_key_value_rows)
    mixed = lowered_backward(jnp.dot(mamba_out, w_mout, precision=FULL_PRECISION) + jnp.dot(attended, output_weight.reshape(-1, MODEL_WIDTH), precision=FULL_PRECISION))
    after = sequence_rows + mixed
    second = low(rms_norm(after, norm_two))
    gate_up = lowered_backward(jnp.dot(second, w_gu.reshape(MODEL_WIDTH, -1), precision=FULL_PRECISION))
    gate = gate_up[:, :FF]
    upward = gate_up[:, FF:]
    activated = low(jax.nn.silu(gate) * upward)
    ffn_out = lowered_backward(jnp.dot(activated, w_down, precision=FULL_PRECISION))
    return after + ffn_out

def forward(source, *weights):
    blocks = source.reshape(-1, SEQ, MODEL_WIDTH)
    runner = jax.checkpoint(partial(layer_rows, weights=weights))
    return lax.map(runner, blocks).reshape(-1, MODEL_WIDTH)

def reference(layer_input, w_norm1, w_zx, w_bc, w_dt, conv_x, conv_xb, conv_bc, conv_bcb, dt_bias, a_log, d_skip, w_mnorm, w_mout, query_key_value_weight, output_weight, w_norm2, w_gu, w_down, grad_output):
    weights = tuple((item.astype(jnp.float32) for item in (w_norm1, w_zx, w_bc, w_dt, conv_x, conv_xb, conv_bc, conv_bcb, dt_bias, a_log, d_skip, w_mnorm, w_mout, query_key_value_weight, output_weight, w_norm2, w_gu, w_down)))
    result, pullback = jax.vjp(forward, layer_input.astype(jnp.float32), *weights)
    grads = pullback(grad_output.astype(jnp.float32))
    return (result.astype(jnp.bfloat16), grads[0], grads[1], grads[2], grads[3], grads[4], grads[5], grads[6], grads[7], grads[8], grads[9], grads[10], grads[11], grads[12], grads[13], grads[14], grads[15], grads[16], grads[17], grads[18])
```

```python
import functools
import math

import jax
import jax.numpy as jnp
import numpy as np
from jax import lax
from jax.experimental import pallas as pl
from jax.experimental.pallas import tpu as pltpu
from jax.sharding import PartitionSpec as P

HEAD_SIZE = 64
MP = 64
NS = 128
KCONV = 4
SPAN = 128
QBLK = 256
LANES = 128
EDGE = 8

EPSILON = 1e-05
HIGHEST = lax.Precision.HIGHEST
LOG_BASE = math.log(100000000000.0)
MASKED = -1e30
MESH = pl.DeviceIdType.MESH
F32 = jnp.float32
BF16 = jnp.bfloat16

NN = ((1,), (0,))
NT = ((1,), (1,))
TN = ((0,), (0,))


def dot(left, right, dims=NN, precision=None):
    return lax.dot_general(
        left, right, (dims, ((), ())), preferred_element_type=F32, precision=precision
    )


def iota(shape, dim):
    return lax.broadcasted_iota(jnp.int32, shape, dim)


def ring_place(chip, chips):
    odd = lax.rem(chip, 2)
    half = lax.div(chip, 2)
    return (1 - odd) * half + odd * (chips - 1 - half)


def ring_chip(place, chips):
    place = lax.rem(place + 4 * chips, chips)
    back = lax.div(place, chips // 2)
    return (1 - back) * (2 * place) + back * (2 * (chips - 1 - place) + 1)


def ring_setup(chips):
    me = lax.axis_index("dp")
    group = lax.axis_index("tensor")
    chip = lax.div(me, 2)
    core = lax.rem(me, 2)
    place = ring_place(chip, chips)
    right = ring_chip(place + 1, chips) * 2 + core
    left = ring_chip(place - 1, chips) * 2 + core
    mate = chip * 2 + (1 - core)
    barrier = pltpu.get_barrier_semaphore()
    for other in (right, left, mate):
        pl.semaphore_signal(barrier, inc=1, device_id=(other, group), device_id_type=MESH)
    pl.semaphore_wait(barrier, 3)
    return me, group, core, place, right, left, mate


def gather_kernel(devices, x_ref, o_ref, fs, fr, bs, br, cs, cr, own_sem):
    rows = x_ref.shape[0]
    chips = devices // 2
    me, group, core, place, right, left, mate = ring_setup(chips)

    def slot(index):
        return o_ref.at[pl.ds(pl.multiple_of(index * rows, rows), rows), :]

    def send(source, index, ssem, rsem, target):
        copy = pltpu.make_async_remote_copy(
            src_ref=source,
            dst_ref=slot(index),
            send_sem=ssem,
            recv_sem=rsem,
            device_id=(target, group),
            device_id_type=MESH,
        )
        copy.start()
        return copy

    ahead = chips // 2
    behind = chips - 1 - ahead
    own = pltpu.make_async_copy(x_ref, slot(me), own_sem)
    fore = [send(x_ref, me, fs.at[0], fr.at[0], right)]
    back = [send(x_ref, me, bs.at[0], br.at[0], left)]
    across = [send(x_ref, me, cs.at[0], cr.at[0], mate)]
    own.start()
    for step in range(1, ahead + 1):
        fore[step - 1].wait_recv()
        index = ring_chip(place - step, chips) * 2 + core
        if step < ahead:
            fore.append(send(slot(index), index, fs.at[step], fr.at[step], right))
        across.append(send(slot(index), index, cs.at[2 * step - 1], cr.at[2 * step - 1], mate))
        if step <= behind:
            back[step - 1].wait_recv()
            index = ring_chip(place + step, chips) * 2 + core
            if step < behind:
                back.append(send(slot(index), index, bs.at[step], br.at[step], left))
            across.append(send(slot(index), index, cs.at[2 * step], cr.at[2 * step], mate))
    own.wait()
    for copy in fore + back:
        copy.wait_send()
    for copy in across:
        copy.wait()


def gather_rows(shard, devices):
    rows, cols = shard.shape
    dma = pltpu.SemaphoreType.DMA
    chips = devices // 2
    return pl.pallas_call(
        functools.partial(gather_kernel, devices),
        out_shape=jax.ShapeDtypeStruct((rows * devices, cols), shard.dtype),
        in_specs=[pl.BlockSpec(memory_space=pl.ANY)],
        out_specs=pl.BlockSpec(memory_space=pl.ANY),
        scratch_shapes=[dma((chips,))] * 6 + [dma(())],
        compiler_params=pltpu.CompilerParams(collective_id=0, has_side_effects=True),
        name="gather_rows",
    )(shard)


def scatter_kernel(devices, g_ref, o_ref, mbox, fbox, bbox, fout, bout, ms, mr, fs, fr, bs, br):
    chips = devices // 2
    rows = o_ref.shape[0]
    me, group, core, place, right, left, mate = ring_setup(chips)
    ahead = chips // 2
    behind = chips - 1 - ahead

    def block(chip, which):
        index = chip * 2 + which
        return g_ref.at[pl.ds(pl.multiple_of(index * rows, rows), rows), :]

    def copy_to(source, target_ref, ssem, rsem, target):
        copy = pltpu.make_async_remote_copy(
            src_ref=source,
            dst_ref=target_ref,
            send_sem=ssem,
            recv_sem=rsem,
            device_id=(target, group),
            device_id_type=MESH,
        )
        copy.start()
        return copy

    order = []
    for step in range(ahead):
        order.append(-(ahead - step))
        if step < behind:
            order.append(behind - step)
    order.append(0)
    mates = {}
    for slot, shift in enumerate(order):
        chip = ring_chip(place + shift, chips)
        mates[shift] = copy_to(
            block(chip, 1 - core), mbox.at[slot], ms.at[slot], mr.at[slot], mate
        )

    def own_sum(shift):
        mates[shift].wait_recv()
        chip = ring_chip(place + shift, chips)
        return block(chip, core)[...].astype(F32) + mbox[order.index(shift)].astype(F32)

    back, fore = [], []
    for step in range(ahead):
        total = own_sum(-(ahead - step))
        if step > 0:
            back[step - 1].wait_recv()
            total = total + bbox[step - 1].astype(F32)
        bout[step] = total.astype(bout.dtype)
        back.append(copy_to(bout.at[step], bbox.at[step], bs.at[step], br.at[step], left))
        if step < behind:
            total = own_sum(behind - step)
            if step > 0:
                fore[step - 1].wait_recv()
                total = total + fbox[step - 1].astype(F32)
            fout[step] = total.astype(fout.dtype)
            fore.append(copy_to(fout.at[step], fbox.at[step], fs.at[step], fr.at[step], right))
    total = own_sum(0)
    fore[behind - 1].wait_recv()
    total = total + fbox[behind - 1].astype(F32)
    back[ahead - 1].wait_recv()
    o_ref[...] = total + bbox[ahead - 1].astype(F32)
    for copy in back + fore + list(mates.values()):
        copy.wait_send()


def scatter_rows(grads, devices, collective):
    total, cols = grads.shape
    rows = total // devices
    chips = devices // 2
    ahead = chips // 2
    dma = pltpu.SemaphoreType.DMA
    vmem = pl.BlockSpec(memory_space=pltpu.VMEM)
    box = pltpu.VMEM((ahead, rows, cols), grads.dtype)
    return pl.pallas_call(
        functools.partial(scatter_kernel, devices),
        out_shape=jax.ShapeDtypeStruct((rows, cols), F32),
        in_specs=[vmem],
        out_specs=vmem,
        scratch_shapes=[pltpu.VMEM((chips, rows, cols), grads.dtype), box, box, box, box]
        + [dma((chips,))] * 6,
        compiler_params=pltpu.CompilerParams(
            collective_id=collective, has_side_effects=True, vmem_limit_bytes=60000 * 1024
        ),
        name="scatter_rows",
    )(grads)


def head_spread(channels):
    return (iota((LANES, channels), 1) // MP == iota((LANES, channels), 0)).astype(F32)


def soft_step(raw):
    return jnp.maximum(raw, 0.0) + jnp.log1p(jnp.exp(-jnp.abs(raw)))


def conv_window(buffer, taps_ref, bias_ref, span):
    total = bias_ref[...] + taps_ref[0:1, :] * buffer[EDGE - 3 : EDGE - 3 + span, :]
    for tap in range(1, KCONV):
        start = EDGE - 3 + tap
        total = total + taps_ref[tap : tap + 1, :] * buffer[start : start + span, :]
    return total


def span_rates(step_ref, bias_ref, decay_ref, spread, span):
    raw = step_ref[...] + bias_ref[...]
    step = soft_step(raw)
    lower = (iota((span, span), 1) <= iota((span, span), 0)).astype(F32)
    cum = dot(lower, step * decay_ref[...], precision=HIGHEST)
    tails = jnp.exp(cum[span - 1 : span, :] - cum)
    wide = dot(
        jnp.concatenate([step, tails, jnp.exp(cum)], axis=0), spread, precision=HIGHEST
    )
    return raw, step, cum, wide[:span], wide[span : 2 * span], wide[2 * span :]


def pair_split(values, low_lanes):
    zero = jnp.zeros_like(values)
    return jnp.concatenate(
        [jnp.where(low_lanes, values, zero), jnp.where(low_lanes, zero, values)], axis=0
    )


def pair_decay(cum, cum_rows, pair, causal):
    parts = []
    for head in (2 * pair, 2 * pair + 1):
        differ = cum[:, head : head + 1] - cum_rows[head : head + 1, :]
        parts.append(jnp.exp(jnp.where(causal, differ, MASKED)))
    return parts


def scan_forward(
    z_ref, x_ref, bc_ref, step_ref,
    tap_ref, bias_ref, tapb_ref, biasb_ref, stepb_ref, decay_ref, skip_ref,
    y_ref, gated_ref, enter_ref,
    state, xbuf, bbuf,
):
    span, channels = x_ref.shape

    @pl.when(pl.program_id(0) == 0)
    def _():
        state[...] = jnp.zeros_like(state)
        xbuf[span:, :] = jnp.zeros((EDGE, channels), F32)
        bbuf[span:, :] = jnp.zeros((EDGE, 2 * NS), F32)

    xbuf[:EDGE, :] = xbuf[span:, :]
    bbuf[:EDGE, :] = bbuf[span:, :]
    xbuf[EDGE:, :] = x_ref[...]
    bbuf[EDGE:, :] = bc_ref[...]
    inputs = jax.nn.silu(conv_window(xbuf, tap_ref, bias_ref, span))
    shared = jax.nn.silu(conv_window(bbuf, tapb_ref, biasb_ref, span))
    spread = head_spread(channels)
    raw, step, cum, step_w, tails_w, grown_w = span_rates(
        step_ref, stepb_ref, decay_ref, spread, span
    )
    cum_rows = cum.T
    b_low = shared[:, :NS].astype(BF16)
    c_low = shared[:, NS:].astype(BF16)
    scaled = inputs * step_w
    scaled_low = scaled.astype(BF16)
    enter_ref[0] = state[...]
    outer = dot(c_low, state[...].astype(BF16)) * grown_w
    fresh = dot(b_low, (scaled * tails_w).astype(BF16), TN)
    state[...] = state[...] * grown_w[span - 1 : span, :] + fresh
    cross = dot(c_low, b_low, NT)
    causal = iota((span, span), 1) <= iota((span, span), 0)
    low_lanes = iota((span, LANES), 1) < MP
    for pair in range(channels // LANES):
        lanes = slice(pair * LANES, (pair + 1) * LANES)
        first, second = pair_decay(cum, cum_rows, pair, causal)
        weights = jnp.concatenate(
            [(cross * first).astype(BF16), (cross * second).astype(BF16)], axis=1
        )
        y_ref[:, lanes] = dot(weights, pair_split(scaled_low[:, lanes], low_lanes))
    y = y_ref[...] + outer + skip_ref[...] * inputs
    y_ref[...] = y
    gated_ref[...] = y * jax.nn.silu(z_ref[...])


def scan_backward(
    z_ref, x_ref, xp_ref, bc_ref, bp_ref, step_ref, y_ref, enter_ref,
    dyg_ref, scale_ref, inner_ref, dqkv_ref,
    tap_ref, bias_ref, tapb_ref, biasb_ref, stepb_ref, decay_ref, skip_ref, gain_ref,
    grad_ref, gx_ref, gb_ref, gh_ref,
    dstate, xbuf, bbuf, dxbuf, dbbuf, du_buf, col_buf,
):
    span, channels = x_ref.shape
    turn = pl.program_id(0)
    count = pl.num_programs(0)

    @pl.when(turn == 0)
    def _():
        dstate[...] = jnp.zeros_like(dstate)
        dxbuf[...] = jnp.zeros_like(dxbuf)
        dbbuf[...] = jnp.zeros_like(dbbuf)
        col_buf[...] = jnp.zeros_like(col_buf)
        gx_ref[...] = jnp.zeros_like(gx_ref)
        gb_ref[...] = jnp.zeros_like(gb_ref)
        gh_ref[...] = jnp.zeros_like(gh_ref)

    inside = (turn < count - 1).astype(F32)
    xbuf[:EDGE, :] = xp_ref[...] * inside
    bbuf[:EDGE, :] = bp_ref[...] * inside
    xbuf[EDGE:, :] = x_ref[...]
    bbuf[EDGE:, :] = bc_ref[...]
    conv = conv_window(xbuf, tap_ref, bias_ref, span)
    sig = jax.nn.sigmoid(conv)
    inputs = conv * sig
    convb = conv_window(bbuf, tapb_ref, biasb_ref, span)
    sigb = jax.nn.sigmoid(convb)
    shared = convb * sigb
    b_low = shared[:, :NS].astype(BF16)
    c_low = shared[:, NS:].astype(BF16)
    spread = head_spread(channels)
    raw, step, cum, step_w, tails_w, grown_w = span_rates(
        step_ref, stepb_ref, decay_ref, spread, span
    )
    cum_rows = cum.T
    scaled = inputs * step_w
    scaled_low = scaled.astype(BF16)

    z = z_ref[...]
    sig_z = jax.nn.sigmoid(z)
    swish = z * sig_z
    y = y_ref[...]
    normed = y * swish * scale_ref[...]
    dyg = dyg_ref[...]
    gain_grad = jnp.sum(dyg * normed, axis=0, keepdims=True)
    dgated = scale_ref[...] * (dyg * gain_ref[...] - normed * inner_ref[...])
    dy = dgated * swish
    grad_ref[:, :channels] = (dgated * y * (sig_z * (1.0 + z * (1.0 - sig_z)))).astype(BF16)

    state_low = enter_ref[0].astype(BF16)
    dstate_low = dstate[...].astype(BF16)
    grown_low = (dy * grown_w).astype(BF16)
    dy_low = dy.astype(BF16)
    tailed = scaled * tails_w
    outer = dot(c_low, state_low) * grown_w
    from_state = dot(b_low, dstate_low)
    dc = dot(grown_low, state_low, NT)
    db = dot(tailed.astype(BF16), dstate_low, NT)
    leak = from_state * tailed
    last_w = grown_w[span - 1 : span, :]
    ends = (
        jnp.sum(leak, axis=0, keepdims=True)
        + jnp.sum(enter_ref[0] * dstate[...], axis=0, keepdims=True) * last_w
    )
    skips = jnp.sum(dy * inputs, axis=0, keepdims=True)
    dstate[...] = dstate[...] * last_w + dot(c_low, grown_low, TN)

    cross = dot(c_low, b_low, NT)
    causal = iota((span, span), 1) <= iota((span, span), 0)
    low_lanes = iota((span, LANES), 1) < MP
    lane = iota((span, LANES), 1)
    dcross = jnp.zeros((span, span), F32)
    row_part = jnp.zeros((span, LANES), F32)
    for pair in range(channels // LANES):
        lanes = slice(pair * LANES, (pair + 1) * LANES)
        decays = pair_decay(cum, cum_rows, pair, causal)
        dy_pair = pair_split(dy_low[:, lanes], low_lanes)
        dweights = dot(dy_pair, scaled_low[:, lanes], NT)
        both = []
        for part in range(2):
            head = 2 * pair + part
            dterm = dweights[part * span : (part + 1) * span] * decays[part]
            dcross = dcross + dterm
            flow = dterm * cross
            row_part = row_part + jnp.where(
                lane == head, jnp.sum(flow, axis=1, keepdims=True), 0.0
            )
            col_buf[head : head + 1, :] = jnp.sum(flow, axis=0, keepdims=True)
            both.append((cross * decays[part]).astype(BF16))
        du_buf[:, lanes] = dot(jnp.concatenate(both, axis=0), dy_pair, TN)
    du = du_buf[...] + from_state * tails_w
    dcross_low = dcross.astype(BF16)
    dc = dc + dot(dcross_low, b_low)
    db = db + dot(dcross_low, c_low, TN)

    sums = dot(
        jnp.concatenate(
            [dy * outer - leak, du * inputs, ends, skips, jnp.zeros((EDGE - 2, channels), F32)],
            axis=0,
        ),
        spread,
        NT,
        HIGHEST,
    )
    at_end = sums[2 * span : 2 * span + 1, :]
    dcum = sums[:span] + row_part - col_buf[...].T
    upper = (iota((span, span), 1) >= iota((span, span), 0)).astype(F32)
    drate = dot(upper, dcum, precision=HIGHEST) + at_end
    dstep = drate * decay_ref[...] + sums[span : 2 * span]
    draw = dstep * jax.nn.sigmoid(raw)
    gh_ref[0:1, :] += jnp.sum(draw, axis=0, keepdims=True)
    gh_ref[1:2, :] += jnp.sum(drate * step, axis=0, keepdims=True) * decay_ref[...]
    gh_ref[2:3, :] += sums[2 * span + 1 : 2 * span + 2, :]

    dinputs = du * step_w + skip_ref[...] * dy
    dxbuf[span:, :] = dxbuf[:EDGE, :]
    dbbuf[span:, :] = dbbuf[:EDGE, :]
    dconv = dinputs * (sig * (1.0 + conv * (1.0 - sig)))
    dconvb = jnp.concatenate([db, dc], axis=1) * (sigb * (1.0 + convb * (1.0 - sigb)))
    dxbuf[:span, :] = dconv
    dbbuf[:span, :] = dconvb
    dx = jnp.zeros_like(dconv)
    dbc = jnp.zeros_like(dconvb)
    for tap in range(KCONV):
        back = KCONV - 1 - tap
        start = EDGE - 3 + tap
        dx = dx + tap_ref[tap : tap + 1, :] * dxbuf[back : back + span, :]
        dbc = dbc + tapb_ref[tap : tap + 1, :] * dbbuf[back : back + span, :]
        gx_ref[tap : tap + 1, :] += jnp.sum(
            dconv * xbuf[start : start + span, :], axis=0, keepdims=True
        )
        gb_ref[tap : tap + 1, :] += jnp.sum(
            dconvb * bbuf[start : start + span, :], axis=0, keepdims=True
        )
    gx_ref[KCONV : KCONV + 1, :] += jnp.sum(dconv, axis=0, keepdims=True)
    gb_ref[KCONV : KCONV + 1, :] += jnp.sum(dconvb, axis=0, keepdims=True)
    gx_ref[KCONV + 1 : KCONV + 2, :] += gain_grad
    width = 2 * channels + 2 * NS
    grad_ref[:, channels : 2 * channels] = dx.astype(BF16)
    grad_ref[:, 2 * channels : width] = dbc.astype(BF16)
    grad_ref[:, width : width + dqkv_ref.shape[1]] = dqkv_ref[...]
    grad_ref[:, width + dqkv_ref.shape[1] :] = draw.astype(BF16)


def scan_params(conv_x, conv_xb, conv_bc, conv_bcb, dt_bias, a_log, d_skip):
    heads = dt_bias.shape[0]

    def wide(row):
        return jnp.pad(row, (0, LANES - heads))[None, :]

    f32 = lambda value: value.astype(F32)
    return (
        f32(conv_x),
        f32(conv_xb)[None, :],
        f32(conv_bc),
        f32(conv_bcb)[None, :],
        wide(f32(dt_bias)),
        wide(-jnp.exp(f32(a_log))),
        jnp.repeat(f32(d_skip), MP)[None, :],
    )


def whole_spec(array):
    return pl.BlockSpec(array.shape, lambda turn: (0,) * array.ndim)


def run_scan_forward(proj, qkv_width, params):
    tokens = proj.shape[0]
    channels = params[1].shape[1]
    step_at = (2 * channels + 2 * NS + qkv_width) // LANES
    spans = tokens // SPAN
    bc_at = 2 * channels // (2 * NS)
    rows = lambda width, at: pl.BlockSpec((SPAN, width), lambda turn: (turn, at))
    return pl.pallas_call(
        scan_forward,
        grid=(spans,),
        out_shape=(
            jax.ShapeDtypeStruct((tokens, channels), F32),
            jax.ShapeDtypeStruct((tokens, channels), F32),
            jax.ShapeDtypeStruct((spans, NS, channels), F32),
        ),
        in_specs=[rows(channels, 0), rows(channels, 1), rows(2 * NS, bc_at), rows(LANES, step_at)]
        + [whole_spec(item) for item in params],
        out_specs=(
            rows(channels, 0),
            rows(channels, 0),
            pl.BlockSpec((1, NS, channels), lambda turn: (turn, 0, 0)),
        ),
        scratch_shapes=[
            pltpu.VMEM((NS, channels), F32),
            pltpu.VMEM((SPAN + EDGE, channels), F32),
            pltpu.VMEM((SPAN + EDGE, 2 * NS), F32),
        ],
        name="scan_forward",
    )(proj, proj, proj, proj, *params)


def run_scan_backward(proj, y, entering, dyg, scale, inner, dqkv, params, gain):
    tokens, width = proj.shape
    channels = params[1].shape[1]
    qkv_width = dqkv.shape[1]
    step_at = (2 * channels + 2 * NS + qkv_width) // LANES
    spans = tokens // SPAN
    bc_at = 2 * channels // (2 * NS)
    edges = SPAN // EDGE
    rows = lambda size, at: pl.BlockSpec((SPAN, size), lambda turn: (spans - 1 - turn, at))
    edge = lambda size, at: pl.BlockSpec(
        (EDGE, size), lambda turn: (jnp.maximum((spans - 1 - turn) * edges - 1, 0), at)
    )
    keep = lambda shape: pl.BlockSpec(shape, lambda turn: (0, 0))
    return pl.pallas_call(
        scan_backward,
        grid=(spans,),
        out_shape=(
            jax.ShapeDtypeStruct((tokens, width), BF16),
            jax.ShapeDtypeStruct((EDGE, channels), F32),
            jax.ShapeDtypeStruct((EDGE, 2 * NS), F32),
            jax.ShapeDtypeStruct((EDGE, LANES), F32),
        ),
        in_specs=[
            rows(channels, 0),
            rows(channels, 1),
            edge(channels, 1),
            rows(2 * NS, bc_at),
            edge(2 * NS, bc_at),
            rows(LANES, step_at),
            rows(channels, 0),
            pl.BlockSpec((1, NS, channels), lambda turn: (spans - 1 - turn, 0, 0)),
            rows(channels, 0),
            rows(1, 0),
            rows(1, 0),
            rows(qkv_width, 0),
        ]
        + [whole_spec(item) for item in params]
        + [whole_spec(gain)],
        out_specs=(
            rows(width, 0),
            keep((EDGE, channels)),
            keep((EDGE, 2 * NS)),
            keep((EDGE, LANES)),
        ),
        scratch_shapes=[
            pltpu.VMEM((NS, channels), F32),
            pltpu.VMEM((SPAN + EDGE, channels), F32),
            pltpu.VMEM((SPAN + EDGE, 2 * NS), F32),
            pltpu.VMEM((SPAN + EDGE, channels), F32),
            pltpu.VMEM((SPAN + EDGE, 2 * NS), F32),
            pltpu.VMEM((SPAN, channels), F32),
            pltpu.VMEM((LANES, SPAN), F32),
        ],
        name="scan_backward",
    )(
        proj, proj, proj, proj, proj, proj, y, entering, dyg, scale, inner, dqkv, *params, gain
    )


def rotary_tables(tokens):
    half = HEAD_SIZE // 2
    exponent = np.arange(half, dtype=np.float32) * np.float32(-2.0 * LOG_BASE / HEAD_SIZE)
    angles = np.arange(tokens, dtype=np.float32)[:, None] * np.exp(exponent)[None, :]
    cosine = np.cos(angles).astype(np.float32)
    sine = np.sin(angles).astype(np.float32)
    return (
        np.concatenate([cosine] * 4, axis=1),
        np.concatenate([-sine, sine, -sine, sine], axis=1),
    )


def rotate(values, cosine, sine):
    half = HEAD_SIZE // 2
    low = iota(values.shape, 1) % HEAD_SIZE < half
    turned = jnp.where(
        low, pltpu.roll(values, LANES - half, 1), pltpu.roll(values, half, 1)
    )
    return values * cosine + turned * sine


def attend_forward(q_ref, kv_ref, cos_ref, sin_ref, qkv_ref, lse_ref, o_ref, heads_q, heads_o, vt):
    tokens, query_width = q_ref.shape
    heads = query_width // HEAD_SIZE
    cosine, sine = cos_ref[...], sin_ref[...]
    for pair in range(heads // 2):
        lanes = slice(pair * LANES, (pair + 1) * LANES)
        turned = (rotate(q_ref[:, lanes], cosine, sine) * HEAD_SIZE**-0.5).astype(BF16)
        qkv_ref[:, lanes] = turned
        heads_q[2 * pair] = turned[:, :HEAD_SIZE]
        heads_q[2 * pair + 1] = turned[:, HEAD_SIZE:]
    kv = kv_ref[...]
    first = iota(kv.shape, 1) < HEAD_SIZE
    qkv_ref[:, query_width:] = jnp.where(first, rotate(kv, cosine, sine), kv).astype(BF16)
    vt[...] = kv[:, HEAD_SIZE:].T.astype(BF16)
    visible = iota((QBLK, QBLK), 0) <= iota((QBLK, QBLK), 1)
    for start in range(0, tokens, QBLK):
        limit = start + QBLK

        def one(head, carry):
            keys = qkv_ref[:limit, query_width : query_width + HEAD_SIZE]
            scores = dot(keys, heads_q[head, start:limit, :], NT)
            edge = jnp.where(visible, scores[start:], MASKED)
            top = jnp.max(edge, axis=0, keepdims=True)
            if start:
                top = jnp.maximum(top, jnp.max(scores[:start], axis=0, keepdims=True))
            probs = jnp.exp(edge - top)
            if start:
                probs = jnp.concatenate([jnp.exp(scores[:start] - top), probs], axis=0)
            total = jnp.sum(probs, axis=0, keepdims=True)
            out = dot(vt[:, :limit], probs.astype(BF16)) / total
            heads_o[head, start:limit, :] = out.T.astype(BF16)
            lse_ref[pl.ds(head, 1), start:limit] = top + jnp.log(total)
            return carry

        lax.fori_loop(0, heads, one, 0)
    for pair in range(heads // 2):
        o_ref[:, pair * LANES : (pair + 1) * LANES] = jnp.concatenate(
            [heads_o[2 * pair], heads_o[2 * pair + 1]], axis=1
        )


def attend_backward(
    qkv_ref, lse_ref, o_ref, do_ref, cos_ref, sin_ref, dqkv_ref,
    heads_q, heads_do, heads_dq, heads_sum, kt, dk, dv,
):
    tokens, query_width = o_ref.shape
    heads = query_width // HEAD_SIZE
    ones = jnp.ones((EDGE, HEAD_SIZE), F32)
    for head in range(heads):
        lanes = slice(head * HEAD_SIZE, (head + 1) * HEAD_SIZE)
        grad = do_ref[:, lanes]
        heads_q[head] = qkv_ref[:, lanes]
        heads_do[head] = grad
        both = grad.astype(F32) * o_ref[:, lanes].astype(F32)
        heads_sum[head : head + 1, :] = dot(ones, both, NT, HIGHEST)[:1]
    kt[...] = qkv_ref[:, query_width : query_width + HEAD_SIZE].astype(F32).T.astype(BF16)
    dk[...] = jnp.zeros_like(dk)
    dv[...] = jnp.zeros_like(dv)
    visible = iota((QBLK, QBLK), 0) <= iota((QBLK, QBLK), 1)
    for start in range(0, tokens, QBLK):
        limit = start + QBLK

        def one(head, carry):
            keys = qkv_ref[:limit, query_width : query_width + HEAD_SIZE]
            values = qkv_ref[:limit, query_width + HEAD_SIZE :]
            query = heads_q[head, start:limit, :]
            grad = heads_do[head, start:limit, :]
            scores = dot(keys, query, NT) - lse_ref[pl.ds(head, 1), start:limit]
            probs = jnp.exp(jnp.where(visible, scores[start:], MASKED))
            if start:
                probs = jnp.concatenate([jnp.exp(scores[:start]), probs], axis=0)
            dprobs = dot(values, grad, NT)
            dscores = (probs * (dprobs - heads_sum[pl.ds(head, 1), start:limit])).astype(BF16)
            dv[:limit, :] += dot(probs.astype(BF16), grad)
            dk[:limit, :] += dot(dscores, query)
            heads_dq[head, start:limit, :] = dot(kt[:, :limit], dscores).T
            return carry

        lax.fori_loop(0, heads, one, 0)
    cosine, sine = cos_ref[...], -sin_ref[...]
    for pair in range(heads // 2):
        joined = jnp.concatenate([heads_dq[2 * pair], heads_dq[2 * pair + 1]], axis=1)
        dqkv_ref[:, pair * LANES : (pair + 1) * LANES] = (
            rotate(joined, cosine, sine) * HEAD_SIZE**-0.5
        ).astype(BF16)
    joined = jnp.concatenate([dk[...], dv[...]], axis=1)
    first = iota(joined.shape, 1) < HEAD_SIZE
    dqkv_ref[:, query_width:] = jnp.where(
        first, rotate(joined, cosine, sine), joined
    ).astype(BF16)


def run_attend_forward(queries, keys_values, tables):
    tokens, query_width = queries.shape
    heads = query_width // HEAD_SIZE
    vmem = pl.BlockSpec(memory_space=pltpu.VMEM)
    return pl.pallas_call(
        attend_forward,
        out_shape=(
            jax.ShapeDtypeStruct((tokens, query_width + 2 * HEAD_SIZE), BF16),
            jax.ShapeDtypeStruct((EDGE, tokens), F32),
            jax.ShapeDtypeStruct((tokens, query_width), BF16),
        ),
        in_specs=[vmem] * 4,
        out_specs=(vmem,) * 3,
        scratch_shapes=[
            pltpu.VMEM((heads, tokens, HEAD_SIZE), BF16),
            pltpu.VMEM((heads, tokens, HEAD_SIZE), BF16),
            pltpu.VMEM((HEAD_SIZE, tokens), BF16),
        ],
        name="attend_forward",
    )(queries, keys_values, *tables)


def run_attend_backward(qkv, lse, attended, grad, tables):
    tokens, query_width = attended.shape
    heads = query_width // HEAD_SIZE
    vmem = pl.BlockSpec(memory_space=pltpu.VMEM)
    return pl.pallas_call(
        attend_backward,
        out_shape=jax.ShapeDtypeStruct((tokens, query_width + 2 * HEAD_SIZE), BF16),
        in_specs=[vmem] * 6,
        out_specs=vmem,
        scratch_shapes=[
            pltpu.VMEM((heads, tokens, HEAD_SIZE), BF16),
            pltpu.VMEM((heads, tokens, HEAD_SIZE), BF16),
            pltpu.VMEM((heads, tokens, HEAD_SIZE), F32),
            pltpu.VMEM((EDGE, tokens), F32),
            pltpu.VMEM((HEAD_SIZE, tokens), BF16),
            pltpu.VMEM((tokens, HEAD_SIZE), F32),
            pltpu.VMEM((tokens, HEAD_SIZE), F32),
        ],
        name="attend_backward",
    )(qkv, lse, attended, grad, *tables)


def tensor_sum(partial):
    pairs = [(0, 1), (1, 0)]
    other = lax.ppermute(partial, "tensor", pairs)
    return partial.astype(F32) + other.astype(F32)


def norm_back(normed, scale, gain, grad):
    weighted = grad * gain
    grad_input = scale * (weighted - normed * jnp.mean(weighted * normed, axis=-1, keepdims=True))
    return (grad_input, jnp.sum(grad * normed, axis=0))


def local(
    layer_input, w_norm1, w_zx, w_bc, w_dt, conv_x, conv_xb, conv_bc, conv_bcb, dt_bias, a_log,
    d_skip, w_mnorm, w_mout, query_key_value_weight, output_weight, w_norm2, w_gu, w_down,
    grad_output,
):
    devices = lax.axis_size("dp")
    tokens, width = layer_input.shape
    shard = w_zx.shape[0]
    channels = conv_xb.shape[0]
    heads = dt_bias.shape[0]
    qkv_width = query_key_value_weight.shape[2]
    units = w_down.shape[0]
    attn_width = output_weight.shape[1]
    tail = jnp.concatenate(
        [w_dt, w_norm1[:, None], w_norm2[:, None], jnp.zeros((shard, LANES - heads - 2), BF16)],
        axis=1,
    )
    mixer_in = jnp.concatenate(
        [w_zx.reshape(shard, -1), w_bc, query_key_value_weight.reshape(shard, -1), tail], axis=1
    )
    rest = jnp.concatenate(
        [w_mout.T, output_weight.reshape(attn_width, -1).T, w_gu.reshape(shard, -1), w_down.T],
        axis=1,
    )
    in_width = mixer_in.shape[1]
    gathered = gather_rows(jnp.concatenate([mixer_in, rest], axis=1), devices)
    w_in = gathered[:, :in_width]
    norm1 = w_in[:, in_width - LANES + heads].astype(F32)
    norm2 = w_in[:, in_width - LANES + heads + 1].astype(F32)
    out_at = in_width
    gu_at = out_at + channels + attn_width
    down_at = gu_at + 2 * units
    w_out = gathered[:, out_at:gu_at]
    w_gate_up = gathered[:, gu_at:down_at]
    w_down_t = gathered[:, down_at:]

    source = layer_input.astype(F32)
    scale_one = lax.rsqrt(jnp.mean(source * source, axis=-1, keepdims=True) + EPSILON)
    normed_one = source * scale_one
    hidden_one = (normed_one * norm1).astype(BF16)
    proj = dot(hidden_one, w_in)
    params = scan_params(conv_x, conv_xb, conv_bc, conv_bcb, dt_bias, a_log, d_skip)
    y, gated, entering = run_scan_forward(proj, qkv_width, params)
    channels_all = channels * lax.axis_size("tensor")
    square_sum = tensor_sum(jnp.sum(gated * gated, axis=-1))
    scale_m = lax.rsqrt(square_sum / channels_all + EPSILON)[:, None]
    tables = rotary_tables(tokens)
    qkv_at = 2 * channels + 2 * NS
    qkv, lse, attended = run_attend_forward(
        proj[:, qkv_at : qkv_at + attn_width],
        proj[:, qkv_at + attn_width : qkv_at + qkv_width],
        tables,
    )
    gain_m = w_mnorm.astype(F32)
    mamba_low = (gated * scale_m * gain_m).astype(BF16)
    mixer_out = jnp.concatenate([mamba_low, attended], axis=1)
    mixed = tensor_sum(dot(mixer_out, w_out, NT).astype(BF16))
    after = source + mixed
    scale_two = lax.rsqrt(jnp.mean(after * after, axis=-1, keepdims=True) + EPSILON)
    normed_two = after * scale_two
    hidden_two = (normed_two * norm2).astype(BF16)
    gate_up = dot(hidden_two, w_gate_up)
    gate = gate_up[:, :units]
    upward = gate_up[:, units:]
    sigma = jax.nn.sigmoid(gate)
    swish = gate * sigma
    activated = (swish * upward).astype(BF16)
    grad_act = dot(grad_output, w_down_t)
    grad_gate = grad_act * upward * sigma * (1.0 + gate * (1.0 - sigma))
    grad_up = grad_act * swish
    grad_gu_low = jnp.concatenate([grad_gate, grad_up], axis=1).astype(BF16)
    grad_hidden_two = tensor_sum(dot(grad_gu_low, w_gate_up, NT).astype(BF16))
    ffn_out = tensor_sum(dot(activated, w_down_t, NT).astype(BF16))
    result = (after + ffn_out).astype(BF16)
    grad_norm_in, grad_norm2 = norm_back(normed_two, scale_two, norm2, grad_hidden_two)
    grad_after = grad_output.astype(F32) + grad_norm_in
    grad_mix_low = grad_after.astype(BF16)
    grad_mixer = dot(grad_mix_low, w_out)
    grad_mamba = grad_mixer[:, :channels]
    normed_m = gated * scale_m
    inner_m = tensor_sum(jnp.sum(grad_mamba * gain_m * normed_m, axis=-1))[:, None] / channels_all
    dqkv = run_attend_backward(
        qkv, lse, attended, grad_mixer[:, channels:].astype(BF16), tables
    )
    grad_proj, small_x, small_b, small_h = run_scan_backward(
        proj, y, entering, grad_mamba, scale_m, inner_m, dqkv, params, gain_m[None, :]
    )
    partial_one = dot(grad_proj, w_in, NT).astype(BF16)
    grad_hidden_one = tensor_sum(partial_one)
    grad_in = dot(hidden_one, grad_proj, TN)
    grad_out = dot(grad_mix_low, mixer_out, TN)
    grad_gu = dot(hidden_two, grad_gu_low, TN)
    grad_down = dot(grad_output, activated, TN)
    packed = jnp.concatenate(
        [item.astype(BF16) for item in (grad_in, grad_out, grad_gu, grad_down)], axis=1
    )
    mine = scatter_rows(packed, devices, 1)
    grad_norm_x, grad_norm1 = norm_back(normed_one, scale_one, norm1, grad_hidden_one)
    grad_source = grad_after + grad_norm_x

    shared_at = 2 * channels
    shared_cols = mine[:, shared_at:qkv_at]
    half = NS * 2 // lax.axis_size("tensor")
    shared_cols = tensor_sum(shared_cols)
    begin = lax.axis_index("tensor") * half
    grad_bc = lax.dynamic_slice_in_dim(shared_cols, begin, half, 1)
    small = jnp.concatenate(
        [
            small_x[: KCONV + 2].reshape(-1),
            small_h[:3].reshape(-1),
            small_b[: KCONV + 1].reshape(-1),
            grad_norm1,
            grad_norm2,
        ]
    )
    small = lax.psum(small, "dp")
    x_size = (KCONV + 2) * channels
    h_size = 3 * LANES
    b_size = (KCONV + 1) * 2 * NS
    total_x = small[:x_size].reshape(KCONV + 2, channels)
    total_h = small[x_size : x_size + h_size].reshape(3, LANES)
    total_b = small[x_size + h_size : x_size + h_size + b_size]
    total_b = tensor_sum(total_b).reshape(KCONV + 1, 2 * NS)
    total_b = lax.dynamic_slice_in_dim(total_b, begin, half, 1)
    norms = small[x_size + h_size + b_size :].reshape(2, width)
    norms = lax.dynamic_slice_in_dim(norms, lax.axis_index("dp") * shard, shard, 1)
    step_at = qkv_at + qkv_width
    return (
        result,
        grad_source,
        norms[0],
        mine[:, :shared_at].reshape(w_zx.shape),
        grad_bc,
        mine[:, step_at : step_at + heads],
        total_x[:KCONV],
        total_x[KCONV],
        total_b[:KCONV],
        total_b[KCONV],
        total_h[0, :heads],
        total_h[1, :heads],
        total_h[2, :heads],
        total_x[KCONV + 1],
        mine[:, out_at : out_at + channels].T,
        mine[:, qkv_at:step_at].reshape(query_key_value_weight.shape),
        mine[:, out_at + channels : gu_at].T.reshape(output_weight.shape),
        norms[1],
        mine[:, gu_at:down_at].reshape(w_gu.shape),
        mine[:, down_at:].T,
    )


def solution(mesh):
    return jax.shard_map(
        local,
        mesh=mesh,
        in_specs=(
            P("dp", None),
            P("dp"),
            P("dp", None, "tensor"),
            P("dp", None),
            P("dp", "tensor"),
            P(None, "tensor"),
            P("tensor"),
            P(),
            P(),
            P("tensor"),
            P("tensor"),
            P("tensor"),
            P("tensor"),
            P("tensor", "dp"),
            P("dp", "tensor", None),
            P("tensor", None, "dp"),
            P("dp"),
            P("dp", None, "tensor"),
            P("tensor", "dp"),
            P("dp", None),
        ),
        out_specs=(
            P("dp", None),
            P("dp", None),
            P("dp"),
            P("dp", None, "tensor"),
            P("dp", "tensor"),
            P("dp", "tensor"),
            P(None, "tensor"),
            P("tensor"),
            P(None, "tensor"),
            P("tensor"),
            P("tensor"),
            P("tensor"),
            P("tensor"),
            P("tensor"),
            P("tensor", "dp"),
            P("dp", "tensor", None),
            P("tensor", None, "dp"),
            P("dp"),
            P("dp", None, "tensor"),
            P("tensor", "dp"),
        ),
        check_vma=False,
    )
```

```python
import functools
import math

import jax
import jax.numpy as jnp
import numpy as np
from jax import lax
from jax.experimental import pallas as pl
from jax.experimental.pallas import tpu as pltpu
from jax.sharding import PartitionSpec as P

HEAD_SIZE = 64
MP = 64
NS = 128
KCONV = 4
SPAN = 128
QBLK = 256
LANES = 128
EDGE = 8

EPSILON = 1e-05
HIGHEST = lax.Precision.HIGHEST
LOG_BASE = math.log(100000000000.0)
MASKED = -1e30
MESH = pl.DeviceIdType.MESH
F32 = jnp.float32
BF16 = jnp.bfloat16

NN = ((1,), (0,))
NT = ((1,), (1,))
TN = ((0,), (0,))


def dot(left, right, dims=NN, precision=None):
    return lax.dot_general(
        left, right, (dims, ((), ())), preferred_element_type=F32, precision=precision
    )


def iota(shape, dim):
    return lax.broadcasted_iota(jnp.int32, shape, dim)


def ring_place(chip, chips):
    odd = lax.rem(chip, 2)
    half = lax.div(chip, 2)
    return (1 - odd) * half + odd * (chips - 1 - half)


def ring_chip(place, chips):
    place = lax.rem(place + 4 * chips, chips)
    back = lax.div(place, chips // 2)
    return (1 - back) * (2 * place) + back * (2 * (chips - 1 - place) + 1)


def ring_setup(chips):
    me = lax.axis_index("dp")
    group = lax.axis_index("tensor")
    chip = lax.div(me, 2)
    core = lax.rem(me, 2)
    place = ring_place(chip, chips)
    right = ring_chip(place + 1, chips) * 2 + core
    left = ring_chip(place - 1, chips) * 2 + core
    mate = chip * 2 + (1 - core)
    barrier = pltpu.get_barrier_semaphore()
    for other in (right, left, mate):
        pl.semaphore_signal(barrier, inc=1, device_id=(other, group), device_id_type=MESH)
    pl.semaphore_wait(barrier, 3)
    return me, group, core, place, right, left, mate


class RingGather:
    def __init__(self, devices, x_ref, o_ref, sems):
        self.chips = devices // 2
        self.ahead = self.chips // 2
        self.behind = self.chips - 1 - self.ahead
        self.x_ref, self.o_ref, self.rows = x_ref, o_ref, x_ref.shape[0]
        self.fs, self.fr, self.bs, self.br, self.cs, self.cr, self.own_sem = sems

    def locate(self):
        me = lax.axis_index("dp")
        self.group = lax.axis_index("tensor")
        self.core = lax.rem(me, 2)
        chip = lax.div(me, 2)
        self.place = ring_place(chip, self.chips)
        self.right = ring_chip(self.place + 1, self.chips) * 2 + self.core
        self.left = ring_chip(self.place - 1, self.chips) * 2 + self.core
        self.mate = chip * 2 + (1 - self.core)
        self.me = me

    def slot(self, index):
        return self.o_ref.at[pl.ds(pl.multiple_of(index * self.rows, self.rows), self.rows), :]

    def copy(self, shift, ssem, rsem, target):
        if shift == 0:
            index, source = self.me, self.x_ref
        else:
            index = ring_chip(self.place + shift, self.chips) * 2 + self.core
            source = self.slot(index)
        return pltpu.make_async_remote_copy(
            src_ref=source,
            dst_ref=self.slot(index),
            send_sem=ssem,
            recv_sem=rsem,
            device_id=(target, self.group),
            device_id_type=MESH,
        )

    def fore(self, step):
        return self.copy(-step, self.fs.at[step], self.fr.at[step], self.right)

    def back(self, step):
        return self.copy(step, self.bs.at[step], self.br.at[step], self.left)

    def across(self, shift):
        number = 0 if shift == 0 else 2 * abs(shift) - (1 if shift < 0 else 0)
        return self.copy(shift, self.cs.at[number], self.cr.at[number], self.mate)

    def own(self):
        return pltpu.make_async_copy(self.x_ref, self.slot(self.me), self.own_sem)

    def begin(self):
        self.locate()
        barrier = pltpu.get_barrier_semaphore()
        for other in (self.right, self.left, self.mate):
            pl.semaphore_signal(
                barrier, inc=1, device_id=(other, self.group), device_id_type=MESH
            )
        pl.semaphore_wait(barrier, 3)
        self.fore(0).start()
        self.back(0).start()
        self.across(0).start()
        self.own().start()

    def hop(self, step):
        self.locate()
        self.fore(step - 1).wait_recv()
        if step < self.ahead:
            self.fore(step).start()
        self.across(-step).start()
        if step <= self.behind:
            self.back(step - 1).wait_recv()
            if step < self.behind:
                self.back(step).start()
            self.across(step).start()

    def finish(self):
        self.locate()
        self.own().wait()
        for step in range(self.ahead):
            self.fore(step).wait_send()
        for step in range(self.behind):
            self.back(step).wait_send()
        for shift in range(-self.ahead, self.behind + 1):
            self.across(shift).wait()

    def run(self):
        self.begin()
        for step in range(1, self.ahead + 1):
            self.hop(step)
        self.finish()


def gather_sems(devices):
    dma = pltpu.SemaphoreType.DMA
    return [dma((devices // 2,))] * 6 + [dma(())]


def gather_shape(shard, devices):
    return jax.ShapeDtypeStruct((shard.shape[0] * devices, shard.shape[1]), shard.dtype)


def gather_kernel(devices, x_ref, o_ref, *sems):
    RingGather(devices, x_ref, o_ref, sems).run()


def gather_rows(shard, devices):
    return pl.pallas_call(
        functools.partial(gather_kernel, devices),
        out_shape=gather_shape(shard, devices),
        in_specs=[pl.BlockSpec(memory_space=pl.ANY)],
        out_specs=pl.BlockSpec(memory_space=pl.ANY),
        scratch_shapes=gather_sems(devices),
        compiler_params=pltpu.CompilerParams(collective_id=0, has_side_effects=True),
        name="gather_rows",
    )(shard)


def scatter_order(chips):
    ahead = chips // 2
    behind = chips - 1 - ahead
    order = []
    for step in range(ahead):
        order.append(-(ahead - step))
        if step < behind:
            order.append(behind - step)
    order.append(0)
    return order


def scatter_kernel(devices, count, *refs):
    grads, refs = refs[:count], refs[count:]
    o_ref, refs = refs[0], refs[1:]
    boxes, refs = refs[:count], refs[count:]
    fbox, bbox, fout, bout, ms, mr, fs, fr, bs, br = refs
    chips = devices // 2
    rows = o_ref.shape[0]
    me, group, core, place, right, left, mate = ring_setup(chips)
    ahead = chips // 2
    behind = chips - 1 - ahead
    starts = [sum(g.shape[1] for g in grads[:i]) for i in range(count)]

    def block(ref, chip, which):
        index = chip * 2 + which
        return ref.at[pl.ds(pl.multiple_of(index * rows, rows), rows), :]

    def copy_to(source, target_ref, ssem, rsem, target):
        copy = pltpu.make_async_remote_copy(
            src_ref=source,
            dst_ref=target_ref,
            send_sem=ssem,
            recv_sem=rsem,
            device_id=(target, group),
            device_id_type=MESH,
        )
        copy.start()
        return copy

    order = scatter_order(chips)
    mates = {}
    for slot, shift in enumerate(order):
        chip = ring_chip(place + shift, chips)
        mates[shift] = [
            copy_to(
                block(grads[i], chip, 1 - core),
                boxes[i].at[slot],
                ms.at[i, slot],
                mr.at[i, slot],
                mate,
            )
            for i in range(count)
        ]

    def put(target, shift, *others):
        slot = order.index(shift)
        chip = ring_chip(place + shift, chips)
        for i in range(count):
            cols = slice(starts[i], starts[i] + grads[i].shape[1])
            mates[shift][i].wait_recv()
            total = block(grads[i], chip, core)[...].astype(F32) + boxes[i][slot].astype(F32)
            for ref in others:
                total = total + ref[:, cols].astype(F32)
            target[:, cols] = total.astype(target.dtype)

    back, fore = [], []
    for step in range(ahead):
        if step > 0:
            back[step - 1].wait_recv()
        put(bout.at[step], -(ahead - step), *([bbox.at[step - 1]] if step else []))
        back.append(copy_to(bout.at[step], bbox.at[step], bs.at[step], br.at[step], left))
        if step < behind:
            if step > 0:
                fore[step - 1].wait_recv()
            put(fout.at[step], behind - step, *([fbox.at[step - 1]] if step else []))
            fore.append(copy_to(fout.at[step], fbox.at[step], fs.at[step], fr.at[step], right))
    fore[behind - 1].wait_recv()
    back[ahead - 1].wait_recv()
    put(o_ref, 0, fbox.at[behind - 1], bbox.at[ahead - 1])
    for copy in back + fore + sum(mates.values(), []):
        copy.wait_send()


def scatter_rows(grads, devices, collective):
    rows = grads[0].shape[0] // devices
    cols = sum(item.shape[1] for item in grads)
    count = len(grads)
    chips = devices // 2
    dma = pltpu.SemaphoreType.DMA
    vmem = pl.BlockSpec(memory_space=pltpu.VMEM)
    box = pltpu.VMEM((chips // 2, rows, cols), BF16)
    return pl.pallas_call(
        functools.partial(scatter_kernel, devices, count),
        out_shape=jax.ShapeDtypeStruct((rows, cols), F32),
        in_specs=[vmem] * count,
        out_specs=vmem,
        scratch_shapes=[pltpu.VMEM((chips, rows, item.shape[1]), BF16) for item in grads]
        + [box] * 4
        + [dma((count, chips))] * 2
        + [dma((chips,))] * 4,
        compiler_params=pltpu.CompilerParams(
            collective_id=collective, has_side_effects=True, vmem_limit_bytes=60000 * 1024
        ),
        name="scatter_rows",
    )(*grads)


def total_kernel(devices, x_ref, o_ref, mate_box, joined, boxes, ms, mr, ss, sr):
    chips = devices // 2
    me = lax.axis_index("dp")
    group = lax.axis_index("tensor")
    chip = lax.div(me, 2)
    core = lax.rem(me, 2)
    mate = chip * 2 + (1 - core)
    peers = [lax.rem(chip + shift, chips) * 2 + core for shift in range(chips)]
    barrier = pltpu.get_barrier_semaphore()
    for other in [mate] + peers[1:]:
        pl.semaphore_signal(barrier, inc=1, device_id=(other, group), device_id_type=MESH)
    pl.semaphore_wait(barrier, chips)

    def copy_to(source, target_ref, ssem, rsem, target):
        copy = pltpu.make_async_remote_copy(
            src_ref=source,
            dst_ref=target_ref,
            send_sem=ssem,
            recv_sem=rsem,
            device_id=(target, group),
            device_id_type=MESH,
        )
        copy.start()
        return copy

    across = copy_to(x_ref, mate_box, ms, mr, mate)
    across.wait_recv()
    total = x_ref[...] + mate_box[...]
    joined[...] = total
    copies = [
        copy_to(joined, boxes.at[chip], ss.at[shift], sr.at[shift], peers[shift])
        for shift in range(1, chips)
    ]
    boxes[chip] = total
    for copy in copies:
        copy.wait_recv()
    result = boxes[0]
    for other in range(1, chips):
        result = result + boxes[other]
    o_ref[...] = result
    across.wait_send()
    for copy in copies:
        copy.wait_send()


def total_rows(values, devices, collective):
    dma = pltpu.SemaphoreType.DMA
    vmem = pl.BlockSpec(memory_space=pltpu.VMEM)
    chips = devices // 2
    return pl.pallas_call(
        functools.partial(total_kernel, devices),
        out_shape=jax.ShapeDtypeStruct(values.shape, F32),
        in_specs=[vmem],
        out_specs=vmem,
        scratch_shapes=[
            pltpu.VMEM(values.shape, F32),
            pltpu.VMEM(values.shape, F32),
            pltpu.VMEM((chips,) + values.shape, F32),
            dma(()),
            dma(()),
            dma((chips,)),
            dma((chips,)),
        ],
        compiler_params=pltpu.CompilerParams(collective_id=collective, has_side_effects=True),
        name="total_rows",
    )(values)


def head_spread(channels):
    return (iota((LANES, channels), 1) // MP == iota((LANES, channels), 0)).astype(F32)


def soft_step(raw):
    return jnp.maximum(raw, 0.0) + jnp.log1p(jnp.exp(-jnp.abs(raw)))


def conv_window(buffer, taps_ref, bias_ref, span):
    total = bias_ref[...] + taps_ref[0:1, :] * buffer[EDGE - 3 : EDGE - 3 + span, :]
    for tap in range(1, KCONV):
        start = EDGE - 3 + tap
        total = total + taps_ref[tap : tap + 1, :] * buffer[start : start + span, :]
    return total


def span_rates(step_ref, bias_ref, decay_ref, spread, span):
    raw = step_ref[...] + bias_ref[...]
    step = soft_step(raw)
    lower = (iota((span, span), 1) <= iota((span, span), 0)).astype(F32)
    cum = dot(lower, step * decay_ref[...], precision=HIGHEST)
    tails = jnp.exp(cum[span - 1 : span, :] - cum)
    wide = dot(
        jnp.concatenate([step, tails, jnp.exp(cum)], axis=0), spread, precision=HIGHEST
    )
    return raw, step, cum, wide[:span], wide[span : 2 * span], wide[2 * span :]


def pair_split(values, low_lanes):
    zero = jnp.zeros_like(values)
    return jnp.concatenate(
        [jnp.where(low_lanes, values, zero), jnp.where(low_lanes, zero, values)], axis=0
    )


def pair_decay(cum, cum_rows, pair, causal):
    parts = []
    for head in (2 * pair, 2 * pair + 1):
        differ = cum[:, head : head + 1] - cum_rows[head : head + 1, :]
        parts.append(jnp.exp(jnp.where(causal, differ, MASKED)))
    return parts


def scan_forward(
    devices, spans,
    z_ref, x_ref, bc_ref, step_ref,
    tap_ref, bias_ref, tapb_ref, biasb_ref, stepb_ref, decay_ref, skip_ref, shard_ref,
    y_ref, gated_ref, enter_ref, all_ref,
    state, xbuf, bbuf, *sems,
):
    span, channels = x_ref.shape
    ring = RingGather(devices, shard_ref, all_ref, sems)
    turn = pl.program_id(0)
    pl.when(turn == 0)(ring.begin)

    @pl.when(pl.program_id(0) == 0)
    def _():
        state[...] = jnp.zeros_like(state)
        xbuf[span:, :] = jnp.zeros((EDGE, channels), F32)
        bbuf[span:, :] = jnp.zeros((EDGE, 2 * NS), F32)

    xbuf[:EDGE, :] = xbuf[span:, :]
    bbuf[:EDGE, :] = bbuf[span:, :]
    xbuf[EDGE:, :] = x_ref[...]
    bbuf[EDGE:, :] = bc_ref[...]
    inputs = jax.nn.silu(conv_window(xbuf, tap_ref, bias_ref, span))
    shared = jax.nn.silu(conv_window(bbuf, tapb_ref, biasb_ref, span))
    spread = head_spread(channels)
    raw, step, cum, step_w, tails_w, grown_w = span_rates(
        step_ref, stepb_ref, decay_ref, spread, span
    )
    cum_rows = cum.T
    b_low = shared[:, :NS].astype(BF16)
    c_low = shared[:, NS:].astype(BF16)
    scaled = inputs * step_w
    scaled_low = scaled.astype(BF16)
    enter_ref[0] = state[...]
    outer = dot(c_low, state[...].astype(BF16)) * grown_w
    fresh = dot(b_low, (scaled * tails_w).astype(BF16), TN)
    state[...] = state[...] * grown_w[span - 1 : span, :] + fresh
    cross = dot(c_low, b_low, NT)
    causal = iota((span, span), 1) <= iota((span, span), 0)
    low_lanes = iota((span, LANES), 1) < MP
    for pair in range(channels // LANES):
        lanes = slice(pair * LANES, (pair + 1) * LANES)
        first, second = pair_decay(cum, cum_rows, pair, causal)
        weights = jnp.concatenate(
            [(cross * first).astype(BF16), (cross * second).astype(BF16)], axis=1
        )
        y_ref[:, lanes] = dot(weights, pair_split(scaled_low[:, lanes], low_lanes))
    y = y_ref[...] + outer + skip_ref[...] * inputs
    y_ref[...] = y
    gated_ref[...] = y * jax.nn.silu(z_ref[...])

    count = spans
    for step in range(1, ring.ahead + 1):
        pl.when(turn == min(count - 1, count * step // ring.ahead))(
            functools.partial(ring.hop, step)
        )
    pl.when(turn == count - 1)(ring.finish)


def scan_backward(
    z_ref, x_ref, xp_ref, bc_ref, bp_ref, step_ref, y_ref, enter_ref,
    dyg_ref, scale_ref, inner_ref, dqkv_ref,
    tap_ref, bias_ref, tapb_ref, biasb_ref, stepb_ref, decay_ref, skip_ref, gain_ref,
    grad_ref, gx_ref, gb_ref, gh_ref,
    dstate, xbuf, bbuf, dxbuf, dbbuf, du_buf, col_buf,
):
    span, channels = x_ref.shape
    turn = pl.program_id(0)
    count = pl.num_programs(0)

    @pl.when(turn == 0)
    def _():
        dstate[...] = jnp.zeros_like(dstate)
        dxbuf[...] = jnp.zeros_like(dxbuf)
        dbbuf[...] = jnp.zeros_like(dbbuf)
        col_buf[...] = jnp.zeros_like(col_buf)
        gx_ref[...] = jnp.zeros_like(gx_ref)
        gb_ref[...] = jnp.zeros_like(gb_ref)
        gh_ref[...] = jnp.zeros_like(gh_ref)

    inside = (turn < count - 1).astype(F32)
    xbuf[:EDGE, :] = xp_ref[...] * inside
    bbuf[:EDGE, :] = bp_ref[...] * inside
    xbuf[EDGE:, :] = x_ref[...]
    bbuf[EDGE:, :] = bc_ref[...]
    conv = conv_window(xbuf, tap_ref, bias_ref, span)
    sig = jax.nn.sigmoid(conv)
    inputs = conv * sig
    convb = conv_window(bbuf, tapb_ref, biasb_ref, span)
    sigb = jax.nn.sigmoid(convb)
    shared = convb * sigb
    b_low = shared[:, :NS].astype(BF16)
    c_low = shared[:, NS:].astype(BF16)
    spread = head_spread(channels)
    raw, step, cum, step_w, tails_w, grown_w = span_rates(
        step_ref, stepb_ref, decay_ref, spread, span
    )
    cum_rows = cum.T
    scaled = inputs * step_w
    scaled_low = scaled.astype(BF16)

    z = z_ref[...]
    sig_z = jax.nn.sigmoid(z)
    swish = z * sig_z
    y = y_ref[...]
    normed = y * swish * scale_ref[...]
    dyg = dyg_ref[...]
    gain_grad = jnp.sum(dyg * normed, axis=0, keepdims=True)
    dgated = scale_ref[...] * (dyg * gain_ref[...] - normed * inner_ref[...])
    dy = dgated * swish
    grad_ref[:, :channels] = (dgated * y * (sig_z * (1.0 + z * (1.0 - sig_z)))).astype(BF16)

    state_low = enter_ref[0].astype(BF16)
    dstate_low = dstate[...].astype(BF16)
    grown_low = (dy * grown_w).astype(BF16)
    dy_low = dy.astype(BF16)
    tailed = scaled * tails_w
    outer = dot(c_low, state_low) * grown_w
    from_state = dot(b_low, dstate_low)
    dc = dot(grown_low, state_low, NT)
    db = dot(tailed.astype(BF16), dstate_low, NT)
    leak = from_state * tailed
    last_w = grown_w[span - 1 : span, :]
    ends = (
        jnp.sum(leak, axis=0, keepdims=True)
        + jnp.sum(enter_ref[0] * dstate[...], axis=0, keepdims=True) * last_w
    )
    skips = jnp.sum(dy * inputs, axis=0, keepdims=True)
    dstate[...] = dstate[...] * last_w + dot(c_low, grown_low, TN)

    cross = dot(c_low, b_low, NT)
    causal = iota((span, span), 1) <= iota((span, span), 0)
    low_lanes = iota((span, LANES), 1) < MP
    lane = iota((span, LANES), 1)
    dcross = jnp.zeros((span, span), F32)
    row_part = jnp.zeros((span, LANES), F32)
    for pair in range(channels // LANES):
        lanes = slice(pair * LANES, (pair + 1) * LANES)
        decays = pair_decay(cum, cum_rows, pair, causal)
        dy_pair = pair_split(dy_low[:, lanes], low_lanes)
        dweights = dot(dy_pair, scaled_low[:, lanes], NT)
        both = []
        for part in range(2):
            head = 2 * pair + part
            dterm = dweights[part * span : (part + 1) * span] * decays[part]
            dcross = dcross + dterm
            flow = dterm * cross
            row_part = row_part + jnp.where(
                lane == head, jnp.sum(flow, axis=1, keepdims=True), 0.0
            )
            col_buf[head : head + 1, :] = jnp.sum(flow, axis=0, keepdims=True)
            both.append((cross * decays[part]).astype(BF16))
        du_buf[:, lanes] = dot(jnp.concatenate(both, axis=0), dy_pair, TN)
    du = du_buf[...] + from_state * tails_w
    dcross_low = dcross.astype(BF16)
    dc = dc + dot(dcross_low, b_low)
    db = db + dot(dcross_low, c_low, TN)

    sums = dot(
        jnp.concatenate(
            [dy * outer - leak, du * inputs, ends, skips, jnp.zeros((EDGE - 2, channels), F32)],
            axis=0,
        ),
        spread,
        NT,
        HIGHEST,
    )
    at_end = sums[2 * span : 2 * span + 1, :]
    dcum = sums[:span] + row_part - col_buf[...].T
    upper = (iota((span, span), 1) >= iota((span, span), 0)).astype(F32)
    drate = dot(upper, dcum, precision=HIGHEST) + at_end
    dstep = drate * decay_ref[...] + sums[span : 2 * span]
    draw = dstep * jax.nn.sigmoid(raw)
    gh_ref[0:1, :] += jnp.sum(draw, axis=0, keepdims=True)
    gh_ref[1:2, :] += jnp.sum(drate * step, axis=0, keepdims=True) * decay_ref[...]
    gh_ref[2:3, :] += sums[2 * span + 1 : 2 * span + 2, :]

    dinputs = du * step_w + skip_ref[...] * dy
    dxbuf[span:, :] = dxbuf[:EDGE, :]
    dbbuf[span:, :] = dbbuf[:EDGE, :]
    dconv = dinputs * (sig * (1.0 + conv * (1.0 - sig)))
    dconvb = jnp.concatenate([db, dc], axis=1) * (sigb * (1.0 + convb * (1.0 - sigb)))
    dxbuf[:span, :] = dconv
    dbbuf[:span, :] = dconvb
    dx = jnp.zeros_like(dconv)
    dbc = jnp.zeros_like(dconvb)
    for tap in range(KCONV):
        back = KCONV - 1 - tap
        start = EDGE - 3 + tap
        dx = dx + tap_ref[tap : tap + 1, :] * dxbuf[back : back + span, :]
        dbc = dbc + tapb_ref[tap : tap + 1, :] * dbbuf[back : back + span, :]
        gx_ref[tap : tap + 1, :] += jnp.sum(
            dconv * xbuf[start : start + span, :], axis=0, keepdims=True
        )
        gb_ref[tap : tap + 1, :] += jnp.sum(
            dconvb * bbuf[start : start + span, :], axis=0, keepdims=True
        )
    gx_ref[KCONV : KCONV + 1, :] += jnp.sum(dconv, axis=0, keepdims=True)
    gb_ref[KCONV : KCONV + 1, :] += jnp.sum(dconvb, axis=0, keepdims=True)
    gx_ref[KCONV + 1 : KCONV + 2, :] += gain_grad
    width = 2 * channels + 2 * NS
    grad_ref[:, channels : 2 * channels] = dx.astype(BF16)
    grad_ref[:, 2 * channels : width] = dbc.astype(BF16)
    grad_ref[:, width : width + dqkv_ref.shape[1]] = dqkv_ref[...]
    grad_ref[:, width + dqkv_ref.shape[1] :] = draw.astype(BF16)


def scan_params(conv_x, conv_xb, conv_bc, conv_bcb, dt_bias, a_log, d_skip):
    heads = dt_bias.shape[0]

    def wide(row):
        return jnp.pad(row, (0, LANES - heads))[None, :]

    f32 = lambda value: value.astype(F32)
    return (
        f32(conv_x),
        f32(conv_xb)[None, :],
        f32(conv_bc),
        f32(conv_bcb)[None, :],
        wide(f32(dt_bias)),
        wide(-jnp.exp(f32(a_log))),
        jnp.repeat(f32(d_skip), MP)[None, :],
    )


def whole_spec(array):
    return pl.BlockSpec(array.shape, lambda turn: (0,) * array.ndim)


def run_scan_forward(proj, qkv_width, params, shard, devices):
    tokens = proj.shape[0]
    channels = params[1].shape[1]
    step_at = (2 * channels + 2 * NS + qkv_width) // LANES
    spans = tokens // SPAN
    bc_at = 2 * channels // (2 * NS)
    rows = lambda width, at: pl.BlockSpec((SPAN, width), lambda turn: (turn, at))
    anywhere = pl.BlockSpec(memory_space=pl.ANY)
    return pl.pallas_call(
        functools.partial(scan_forward, devices, spans),
        grid=(spans,),
        out_shape=(
            jax.ShapeDtypeStruct((tokens, channels), F32),
            jax.ShapeDtypeStruct((tokens, channels), F32),
            jax.ShapeDtypeStruct((spans, NS, channels), F32),
            gather_shape(shard, devices),
        ),
        in_specs=[rows(channels, 0), rows(channels, 1), rows(2 * NS, bc_at), rows(LANES, step_at)]
        + [whole_spec(item) for item in params]
        + [anywhere],
        out_specs=(
            rows(channels, 0),
            rows(channels, 0),
            pl.BlockSpec((1, NS, channels), lambda turn: (turn, 0, 0)),
            anywhere,
        ),
        scratch_shapes=[
            pltpu.VMEM((NS, channels), F32),
            pltpu.VMEM((SPAN + EDGE, channels), F32),
            pltpu.VMEM((SPAN + EDGE, 2 * NS), F32),
        ]
        + gather_sems(devices),
        compiler_params=pltpu.CompilerParams(collective_id=2, has_side_effects=True),
        name="scan_forward",
    )(proj, proj, proj, proj, *params, shard)


def run_scan_backward(proj, y, entering, dyg, scale, inner, dqkv, params, gain):
    tokens, width = proj.shape
    channels = params[1].shape[1]
    qkv_width = dqkv.shape[1]
    step_at = (2 * channels + 2 * NS + qkv_width) // LANES
    spans = tokens // SPAN
    bc_at = 2 * channels // (2 * NS)
    edges = SPAN // EDGE
    rows = lambda size, at: pl.BlockSpec((SPAN, size), lambda turn: (spans - 1 - turn, at))
    edge = lambda size, at: pl.BlockSpec(
        (EDGE, size), lambda turn: (jnp.maximum((spans - 1 - turn) * edges - 1, 0), at)
    )
    keep = lambda shape: pl.BlockSpec(shape, lambda turn: (0, 0))
    return pl.pallas_call(
        scan_backward,
        grid=(spans,),
        out_shape=(
            jax.ShapeDtypeStruct((tokens, width), BF16),
            jax.ShapeDtypeStruct((EDGE, channels), F32),
            jax.ShapeDtypeStruct((EDGE, 2 * NS), F32),
            jax.ShapeDtypeStruct((EDGE, LANES), F32),
        ),
        in_specs=[
            rows(channels, 0),
            rows(channels, 1),
            edge(channels, 1),
            rows(2 * NS, bc_at),
            edge(2 * NS, bc_at),
            rows(LANES, step_at),
            rows(channels, 0),
            pl.BlockSpec((1, NS, channels), lambda turn: (spans - 1 - turn, 0, 0)),
            rows(channels, 0),
            rows(1, 0),
            rows(1, 0),
            rows(qkv_width, 0),
        ]
        + [whole_spec(item) for item in params]
        + [whole_spec(gain)],
        out_specs=(
            rows(width, 0),
            keep((EDGE, channels)),
            keep((EDGE, 2 * NS)),
            keep((EDGE, LANES)),
        ),
        scratch_shapes=[
            pltpu.VMEM((NS, channels), F32),
            pltpu.VMEM((SPAN + EDGE, channels), F32),
            pltpu.VMEM((SPAN + EDGE, 2 * NS), F32),
            pltpu.VMEM((SPAN + EDGE, channels), F32),
            pltpu.VMEM((SPAN + EDGE, 2 * NS), F32),
            pltpu.VMEM((SPAN, channels), F32),
            pltpu.VMEM((LANES, SPAN), F32),
        ],
        name="scan_backward",
    )(
        proj, proj, proj, proj, proj, proj, y, entering, dyg, scale, inner, dqkv, *params, gain
    )


def rotary_tables(tokens):
    half = HEAD_SIZE // 2
    exponent = np.arange(half, dtype=np.float32) * np.float32(-2.0 * LOG_BASE / HEAD_SIZE)
    angles = np.arange(tokens, dtype=np.float32)[:, None] * np.exp(exponent)[None, :]
    cosine = np.cos(angles).astype(np.float32)
    sine = np.sin(angles).astype(np.float32)
    return (
        np.concatenate([cosine] * 4, axis=1),
        np.concatenate([-sine, sine, -sine, sine], axis=1),
    )


def rotate(values, cosine, sine):
    half = HEAD_SIZE // 2
    low = iota(values.shape, 1) % HEAD_SIZE < half
    turned = jnp.where(
        low, pltpu.roll(values, LANES - half, 1), pltpu.roll(values, half, 1)
    )
    return values * cosine + turned * sine


def attend_forward(
    devices,
    q_ref, kv_ref, cos_ref, sin_ref, shard_ref,
    qkv_ref, lse_ref, o_ref, all_ref,
    heads_q, heads_o, vt, *sems,
):
    ring = RingGather(devices, shard_ref, all_ref, sems)
    ring.begin()
    tokens, query_width = q_ref.shape
    heads = query_width // HEAD_SIZE
    cosine, sine = cos_ref[...], sin_ref[...]
    for pair in range(heads // 2):
        lanes = slice(pair * LANES, (pair + 1) * LANES)
        turned = (rotate(q_ref[:, lanes], cosine, sine) * HEAD_SIZE**-0.5).astype(BF16)
        qkv_ref[:, lanes] = turned
        heads_q[2 * pair] = turned[:, :HEAD_SIZE]
        heads_q[2 * pair + 1] = turned[:, HEAD_SIZE:]
    kv = kv_ref[...]
    first = iota(kv.shape, 1) < HEAD_SIZE
    qkv_ref[:, query_width:] = jnp.where(first, rotate(kv, cosine, sine), kv).astype(BF16)
    vt[...] = kv[:, HEAD_SIZE:].T.astype(BF16)
    visible = iota((QBLK, QBLK), 0) <= iota((QBLK, QBLK), 1)
    for start in range(0, tokens, QBLK):
        limit = start + QBLK

        def one(head, carry):
            keys = qkv_ref[:limit, query_width : query_width + HEAD_SIZE]
            scores = dot(keys, heads_q[head, start:limit, :], NT)
            edge = jnp.where(visible, scores[start:], MASKED)
            top = jnp.max(edge, axis=0, keepdims=True)
            if start:
                top = jnp.maximum(top, jnp.max(scores[:start], axis=0, keepdims=True))
            probs = jnp.exp(edge - top)
            if start:
                probs = jnp.concatenate([jnp.exp(scores[:start] - top), probs], axis=0)
            total = jnp.sum(probs, axis=0, keepdims=True)
            out = dot(vt[:, :limit], probs.astype(BF16)) / total
            heads_o[head, start:limit, :] = out.T.astype(BF16)
            lse_ref[pl.ds(head, 1), start:limit] = top + jnp.log(total)
            return carry

        lax.fori_loop(0, heads, one, 0)
        for step in range(1, ring.ahead):
            if min(tokens, QBLK * max(1, tokens * step // (ring.ahead * QBLK))) == limit:
                ring.hop(step)
    for pair in range(heads // 2):
        o_ref[:, pair * LANES : (pair + 1) * LANES] = jnp.concatenate(
            [heads_o[2 * pair], heads_o[2 * pair + 1]], axis=1
        )
    ring.hop(ring.ahead)
    ring.finish()


def attend_backward(
    qkv_ref, lse_ref, o_ref, do_ref, cos_ref, sin_ref, dqkv_ref,
    heads_q, heads_do, heads_dq, heads_sum, kt, dk, dv,
):
    tokens, query_width = o_ref.shape
    heads = query_width // HEAD_SIZE
    ones = jnp.ones((EDGE, HEAD_SIZE), F32)
    for head in range(heads):
        lanes = slice(head * HEAD_SIZE, (head + 1) * HEAD_SIZE)
        grad = do_ref[:, lanes]
        heads_q[head] = qkv_ref[:, lanes]
        heads_do[head] = grad
        both = grad.astype(F32) * o_ref[:, lanes].astype(F32)
        heads_sum[head : head + 1, :] = dot(ones, both, NT, HIGHEST)[:1]
    kt[...] = qkv_ref[:, query_width : query_width + HEAD_SIZE].astype(F32).T.astype(BF16)
    dk[...] = jnp.zeros_like(dk)
    dv[...] = jnp.zeros_like(dv)
    visible = iota((QBLK, QBLK), 0) <= iota((QBLK, QBLK), 1)
    for start in range(0, tokens, QBLK):
        limit = start + QBLK

        def one(head, carry):
            keys = qkv_ref[:limit, query_width : query_width + HEAD_SIZE]
            values = qkv_ref[:limit, query_width + HEAD_SIZE :]
            query = heads_q[head, start:limit, :]
            grad = heads_do[head, start:limit, :]
            scores = dot(keys, query, NT) - lse_ref[pl.ds(head, 1), start:limit]
            probs = jnp.exp(jnp.where(visible, scores[start:], MASKED))
            if start:
                probs = jnp.concatenate([jnp.exp(scores[:start]), probs], axis=0)
            dprobs = dot(values, grad, NT)
            dscores = (probs * (dprobs - heads_sum[pl.ds(head, 1), start:limit])).astype(BF16)
            dv[:limit, :] += dot(probs.astype(BF16), grad)
            dk[:limit, :] += dot(dscores, query)
            heads_dq[head, start:limit, :] = dot(kt[:, :limit], dscores).T
            return carry

        lax.fori_loop(0, heads, one, 0)
    cosine, sine = cos_ref[...], -sin_ref[...]
    for pair in range(heads // 2):
        joined = jnp.concatenate([heads_dq[2 * pair], heads_dq[2 * pair + 1]], axis=1)
        dqkv_ref[:, pair * LANES : (pair + 1) * LANES] = (
            rotate(joined, cosine, sine) * HEAD_SIZE**-0.5
        ).astype(BF16)
    joined = jnp.concatenate([dk[...], dv[...]], axis=1)
    first = iota(joined.shape, 1) < HEAD_SIZE
    dqkv_ref[:, query_width:] = jnp.where(
        first, rotate(joined, cosine, sine), joined
    ).astype(BF16)


def run_attend_forward(queries, keys_values, tables, shard, devices):
    tokens, query_width = queries.shape
    heads = query_width // HEAD_SIZE
    vmem = pl.BlockSpec(memory_space=pltpu.VMEM)
    anywhere = pl.BlockSpec(memory_space=pl.ANY)
    return pl.pallas_call(
        functools.partial(attend_forward, devices),
        out_shape=(
            jax.ShapeDtypeStruct((tokens, query_width + 2 * HEAD_SIZE), BF16),
            jax.ShapeDtypeStruct((EDGE, tokens), F32),
            jax.ShapeDtypeStruct((tokens, query_width), BF16),
            gather_shape(shard, devices),
        ),
        in_specs=[vmem] * 4 + [anywhere],
        out_specs=(vmem,) * 3 + (anywhere,),
        scratch_shapes=[
            pltpu.VMEM((heads, tokens, HEAD_SIZE), BF16),
            pltpu.VMEM((heads, tokens, HEAD_SIZE), BF16),
            pltpu.VMEM((HEAD_SIZE, tokens), BF16),
        ]
        + gather_sems(devices),
        compiler_params=pltpu.CompilerParams(collective_id=3, has_side_effects=True),
        name="attend_forward",
    )(queries, keys_values, *tables, shard)


def run_attend_backward(qkv, lse, attended, grad, tables):
    tokens, query_width = attended.shape
    heads = query_width // HEAD_SIZE
    vmem = pl.BlockSpec(memory_space=pltpu.VMEM)
    return pl.pallas_call(
        attend_backward,
        out_shape=jax.ShapeDtypeStruct((tokens, query_width + 2 * HEAD_SIZE), BF16),
        in_specs=[vmem] * 6,
        out_specs=vmem,
        scratch_shapes=[
            pltpu.VMEM((heads, tokens, HEAD_SIZE), BF16),
            pltpu.VMEM((heads, tokens, HEAD_SIZE), BF16),
            pltpu.VMEM((heads, tokens, HEAD_SIZE), F32),
            pltpu.VMEM((EDGE, tokens), F32),
            pltpu.VMEM((HEAD_SIZE, tokens), BF16),
            pltpu.VMEM((tokens, HEAD_SIZE), F32),
            pltpu.VMEM((tokens, HEAD_SIZE), F32),
        ],
        name="attend_backward",
    )(qkv, lse, attended, grad, *tables)


def tensor_sum(partial):
    pairs = [(0, 1), (1, 0)]
    other = lax.ppermute(partial, "tensor", pairs)
    return partial.astype(F32) + other.astype(F32)


def norm_back(normed, scale, gain, grad):
    weighted = grad * gain
    grad_input = scale * (weighted - normed * jnp.mean(weighted * normed, axis=-1, keepdims=True))
    return (grad_input, jnp.sum(grad * normed, axis=0))


def local(
    layer_input, w_norm1, w_zx, w_bc, w_dt, conv_x, conv_xb, conv_bc, conv_bcb, dt_bias, a_log,
    d_skip, w_mnorm, w_mout, query_key_value_weight, output_weight, w_norm2, w_gu, w_down,
    grad_output,
):
    devices = lax.axis_size("dp")
    tokens, width = layer_input.shape
    shard = w_zx.shape[0]
    channels = conv_xb.shape[0]
    heads = dt_bias.shape[0]
    qkv_width = query_key_value_weight.shape[2]
    units = w_down.shape[0]
    attn_width = output_weight.shape[1]
    tail = jnp.concatenate(
        [w_dt, w_norm1[:, None], w_norm2[:, None], jnp.zeros((shard, LANES - heads - 2), BF16)],
        axis=1,
    )
    mixer_in = jnp.concatenate(
        [w_zx.reshape(shard, -1), w_bc, query_key_value_weight.reshape(shard, -1), tail], axis=1
    )
    in_width = mixer_in.shape[1]
    mixer_all = jnp.concatenate(
        [mixer_in, w_mout.T, output_weight.reshape(attn_width, -1).T], axis=1
    )
    gathered = gather_rows(mixer_all, devices)
    w_in = gathered[:, :in_width]
    norm1 = w_in[:, in_width - LANES + heads].astype(F32)
    norm2 = w_in[:, in_width - LANES + heads + 1].astype(F32)
    out_at = in_width
    gu_at = out_at + channels + attn_width
    down_at = gu_at + 2 * units
    w_out = gathered[:, out_at:gu_at]

    source = layer_input.astype(F32)
    scale_one = lax.rsqrt(jnp.mean(source * source, axis=-1, keepdims=True) + EPSILON)
    normed_one = source * scale_one
    hidden_one = (normed_one * norm1).astype(BF16)
    proj = dot(hidden_one, w_in)
    params = scan_params(conv_x, conv_xb, conv_bc, conv_bcb, dt_bias, a_log, d_skip)
    y, gated, entering, w_gate_up = run_scan_forward(
        proj, qkv_width, params, w_gu.reshape(shard, -1), devices
    )
    channels_all = channels * lax.axis_size("tensor")
    square_sum = tensor_sum(jnp.sum(gated * gated, axis=-1))
    scale_m = lax.rsqrt(square_sum / channels_all + EPSILON)[:, None]
    tables = rotary_tables(tokens)
    qkv_at = 2 * channels + 2 * NS
    qkv, lse, attended, w_down_t = run_attend_forward(
        proj[:, qkv_at : qkv_at + attn_width],
        proj[:, qkv_at + attn_width : qkv_at + qkv_width],
        tables,
        w_down.T,
        devices,
    )
    gain_m = w_mnorm.astype(F32)
    mamba_low = (gated * scale_m * gain_m).astype(BF16)
    mixer_out = jnp.concatenate([mamba_low, attended], axis=1)
    mixed = tensor_sum(dot(mixer_out, w_out, NT).astype(BF16))
    after = source + mixed
    scale_two = lax.rsqrt(jnp.mean(after * after, axis=-1, keepdims=True) + EPSILON)
    normed_two = after * scale_two
    hidden_two = (normed_two * norm2).astype(BF16)
    gate_up = dot(hidden_two, w_gate_up)
    gate = gate_up[:, :units]
    upward = gate_up[:, units:]
    sigma = jax.nn.sigmoid(gate)
    swish = gate * sigma
    activated = (swish * upward).astype(BF16)
    grad_act = dot(grad_output, w_down_t)
    grad_gate = grad_act * upward * sigma * (1.0 + gate * (1.0 - sigma))
    grad_up = grad_act * swish
    grad_gu_low = jnp.concatenate([grad_gate, grad_up], axis=1).astype(BF16)
    grad_hidden_two = tensor_sum(dot(grad_gu_low, w_gate_up, NT).astype(BF16))
    ffn_part, grad_hidden_two = lax.optimization_barrier(
        (dot(activated, w_down_t, NT).astype(BF16), grad_hidden_two)
    )
    ffn_out = tensor_sum(ffn_part)
    result = (after + ffn_out).astype(BF16)
    grad_norm_in, grad_norm2 = norm_back(normed_two, scale_two, norm2, grad_hidden_two)
    grad_after = grad_output.astype(F32) + grad_norm_in
    grad_mix_low = grad_after.astype(BF16)
    grad_mixer = dot(grad_mix_low, w_out)
    grad_mamba = grad_mixer[:, :channels]
    normed_m = gated * scale_m
    inner_m = tensor_sum(jnp.sum(grad_mamba * gain_m * normed_m, axis=-1))[:, None] / channels_all
    dqkv = run_attend_backward(
        qkv, lse, attended, grad_mixer[:, channels:].astype(BF16), tables
    )
    grad_proj, small_x, small_b, small_h = run_scan_backward(
        proj, y, entering, grad_mamba, scale_m, inner_m, dqkv, params, gain_m[None, :]
    )
    partial_one = dot(grad_proj, w_in, NT).astype(BF16)
    grad_hidden_one = tensor_sum(partial_one)
    grad_in = dot(hidden_one, grad_proj, TN)
    grad_out = dot(grad_mix_low, mixer_out, TN)
    grad_gu = dot(hidden_two, grad_gu_low, TN)
    grad_down = dot(grad_output, activated, TN)
    mine = scatter_rows(
        [item.astype(BF16) for item in (grad_in, grad_out, grad_gu, grad_down)], devices, 1
    )
    grad_norm_x, grad_norm1 = norm_back(normed_one, scale_one, norm1, grad_hidden_one)
    grad_source = grad_after + grad_norm_x

    shared_at = 2 * channels
    shared_cols = mine[:, shared_at:qkv_at]
    half = NS * 2 // lax.axis_size("tensor")
    shared_cols = tensor_sum(shared_cols)
    begin = lax.axis_index("tensor") * half
    grad_bc = lax.dynamic_slice_in_dim(shared_cols, begin, half, 1)
    small = jnp.concatenate(
        [
            small_x[: KCONV + 2].reshape(-1, LANES),
            small_h[:3],
            tensor_sum(small_b[: KCONV + 1].reshape(-1)).reshape(-1, LANES),
            grad_norm1.reshape(-1, LANES),
            grad_norm2.reshape(-1, LANES),
        ],
        axis=0,
    )
    small_rows = small.shape[0]
    small = jnp.pad(small, ((0, -small_rows % EDGE), (0, 0)))
    small = total_rows(small, devices, 4)[:small_rows].reshape(-1)
    x_size = (KCONV + 2) * channels
    h_size = 3 * LANES
    b_size = (KCONV + 1) * 2 * NS
    total_x = small[:x_size].reshape(KCONV + 2, channels)
    total_h = small[x_size : x_size + h_size].reshape(3, LANES)
    total_b = small[x_size + h_size : x_size + h_size + b_size].reshape(KCONV + 1, 2 * NS)
    total_b = lax.dynamic_slice_in_dim(total_b, begin, half, 1)
    norms = small[x_size + h_size + b_size :].reshape(2, width)
    norms = lax.dynamic_slice_in_dim(norms, lax.axis_index("dp") * shard, shard, 1)
    step_at = qkv_at + qkv_width
    return (
        result,
        grad_source,
        norms[0],
        mine[:, :shared_at].reshape(w_zx.shape),
        grad_bc,
        mine[:, step_at : step_at + heads],
        total_x[:KCONV],
        total_x[KCONV],
        total_b[:KCONV],
        total_b[KCONV],
        total_h[0, :heads],
        total_h[1, :heads],
        total_h[2, :heads],
        total_x[KCONV + 1],
        mine[:, out_at : out_at + channels].T,
        mine[:, qkv_at:step_at].reshape(query_key_value_weight.shape),
        mine[:, out_at + channels : gu_at].T.reshape(output_weight.shape),
        norms[1],
        mine[:, gu_at:down_at].reshape(w_gu.shape),
        mine[:, down_at:].T,
    )


def solution(mesh):
    return jax.shard_map(
        local,
        mesh=mesh,
        in_specs=(
            P("dp", None),
            P("dp"),
            P("dp", None, "tensor"),
            P("dp", None),
            P("dp", "tensor"),
            P(None, "tensor"),
            P("tensor"),
            P(),
            P(),
            P("tensor"),
            P("tensor"),
            P("tensor"),
            P("tensor"),
            P("tensor", "dp"),
            P("dp", "tensor", None),
            P("tensor", None, "dp"),
            P("dp"),
            P("dp", None, "tensor"),
            P("tensor", "dp"),
            P("dp", None),
        ),
        out_specs=(
            P("dp", None),
            P("dp", None),
            P("dp"),
            P("dp", None, "tensor"),
            P("dp", "tensor"),
            P("dp", "tensor"),
            P(None, "tensor"),
            P("tensor"),
            P(None, "tensor"),
            P("tensor"),
            P("tensor"),
            P("tensor"),
            P("tensor"),
            P("tensor"),
            P("tensor", "dp"),
            P("dp", "tensor", None),
            P("tensor", None, "dp"),
            P("dp"),
            P("dp", None, "tensor"),
            P("tensor", "dp"),
        ),
        check_vma=False,
    )
```

```python
import functools
import math

import jax
import jax.numpy as jnp
import numpy as np
from jax import lax
from jax.experimental import pallas as pl
from jax.experimental.pallas import tpu as pltpu
from jax.sharding import PartitionSpec as P

HEAD_SIZE = 64
MP = 64
NS = 128
KCONV = 4
SPAN = 128
QBLK = 256
LANES = 128
EDGE = 8

EPSILON = 1e-05
HIGHEST = lax.Precision.HIGHEST
LOG_BASE = math.log(100000000000.0)
MASKED = -1e30
MESH = pl.DeviceIdType.MESH
F32 = jnp.float32
BF16 = jnp.bfloat16

NN = ((1,), (0,))
NT = ((1,), (1,))
TN = ((0,), (0,))


def dot(left, right, dims=NN, precision=None):
    return lax.dot_general(
        left, right, (dims, ((), ())), preferred_element_type=F32, precision=precision
    )


def iota(shape, dim):
    return lax.broadcasted_iota(jnp.int32, shape, dim)


def ring_place(chip, chips):
    odd = lax.rem(chip, 2)
    half = lax.div(chip, 2)
    return (1 - odd) * half + odd * (chips - 1 - half)


def ring_chip(place, chips):
    place = lax.rem(place + 4 * chips, chips)
    back = lax.div(place, chips // 2)
    return (1 - back) * (2 * place) + back * (2 * (chips - 1 - place) + 1)


def ring_setup(chips):
    me = lax.axis_index("dp")
    group = lax.axis_index("tensor")
    chip = lax.div(me, 2)
    core = lax.rem(me, 2)
    place = ring_place(chip, chips)
    right = ring_chip(place + 1, chips) * 2 + core
    left = ring_chip(place - 1, chips) * 2 + core
    mate = chip * 2 + (1 - core)
    barrier = pltpu.get_barrier_semaphore()
    for other in (right, left, mate):
        pl.semaphore_signal(barrier, inc=1, device_id=(other, group), device_id_type=MESH)
    pl.semaphore_wait(barrier, 3)
    return me, group, core, place, right, left, mate


class RingGather:
    def __init__(self, devices, x_ref, o_ref, sems):
        self.chips = devices // 2
        self.ahead = self.chips // 2
        self.behind = self.chips - 1 - self.ahead
        self.x_ref, self.o_ref, self.rows = x_ref, o_ref, x_ref.shape[0]
        self.fs, self.fr, self.bs, self.br, self.cs, self.cr, self.own_sem = sems

    def locate(self):
        me = lax.axis_index("dp")
        self.group = lax.axis_index("tensor")
        self.core = lax.rem(me, 2)
        chip = lax.div(me, 2)
        self.place = ring_place(chip, self.chips)
        self.right = ring_chip(self.place + 1, self.chips) * 2 + self.core
        self.left = ring_chip(self.place - 1, self.chips) * 2 + self.core
        self.mate = chip * 2 + (1 - self.core)
        self.me = me

    def slot(self, index):
        return self.o_ref.at[pl.ds(pl.multiple_of(index * self.rows, self.rows), self.rows), :]

    def copy(self, shift, ssem, rsem, target):
        if shift == 0:
            index, source = self.me, self.x_ref
        else:
            index = ring_chip(self.place + shift, self.chips) * 2 + self.core
            source = self.slot(index)
        return pltpu.make_async_remote_copy(
            src_ref=source,
            dst_ref=self.slot(index),
            send_sem=ssem,
            recv_sem=rsem,
            device_id=(target, self.group),
            device_id_type=MESH,
        )

    def fore(self, step):
        return self.copy(-step, self.fs.at[step], self.fr.at[step], self.right)

    def back(self, step):
        return self.copy(step, self.bs.at[step], self.br.at[step], self.left)

    def across(self, shift):
        number = 0 if shift == 0 else 2 * abs(shift) - (1 if shift < 0 else 0)
        return self.copy(shift, self.cs.at[number], self.cr.at[number], self.mate)

    def own(self):
        return pltpu.make_async_copy(self.x_ref, self.slot(self.me), self.own_sem)

    def greet(self):
        self.locate()
        barrier = pltpu.get_barrier_semaphore()
        for other in (self.right, self.left, self.mate):
            pl.semaphore_signal(
                barrier, inc=1, device_id=(other, self.group), device_id_type=MESH
            )
        pl.semaphore_wait(barrier, 3)

    def begin(self):
        self.locate()
        self.fore(0).start()
        self.back(0).start()
        self.across(0).start()
        self.own().start()

    def hop(self, step):
        self.locate()
        self.fore(step - 1).wait_recv()
        if step < self.ahead:
            self.fore(step).start()
        self.across(-step).start()
        if step <= self.behind:
            self.back(step - 1).wait_recv()
            if step < self.behind:
                self.back(step).start()
            self.across(step).start()

    def finish(self):
        self.locate()
        self.own().wait()
        for step in range(self.ahead):
            self.fore(step).wait_send()
        for step in range(self.behind):
            self.back(step).wait_send()
        for shift in range(-self.ahead, self.behind + 1):
            self.across(shift).wait()


def gather_sems(devices):
    dma = pltpu.SemaphoreType.DMA
    return [dma((devices // 2,))] * 6 + [dma(())]


def gather_shape(shard, devices):
    return jax.ShapeDtypeStruct((shard.shape[0] * devices, shard.shape[1]), shard.dtype)


def gather_kernel(devices, count, *refs):
    shards, outs, sems = refs[:count], refs[count : 2 * count], refs[2 * count :]
    each = len(sems) // count
    rings = [
        RingGather(devices, shards[i], outs[i], sems[i * each : (i + 1) * each])
        for i in range(count)
    ]
    rings[0].greet()
    for ring in rings:
        ring.begin()
    for step in range(1, rings[0].ahead + 1):
        for ring in rings:
            ring.hop(step)
    for ring in rings:
        ring.finish()


def cost(micros):
    return pl.CostEstimate(flops=int(micros * 1e9), bytes_accessed=0, transcendentals=0)


def gather_rows(shards, devices, collective):
    count = len(shards)
    anywhere = pl.BlockSpec(memory_space=pl.ANY)
    return pl.pallas_call(
        functools.partial(gather_kernel, devices, count),
        out_shape=tuple(gather_shape(shard, devices) for shard in shards),
        in_specs=[anywhere] * count,
        out_specs=(anywhere,) * count,
        scratch_shapes=gather_sems(devices) * count,
        compiler_params=pltpu.CompilerParams(collective_id=collective, has_side_effects=True),
        cost_estimate=cost(3),
        name="gather_rows",
    )(*shards)


def scatter_order(chips):
    ahead = chips // 2
    behind = chips - 1 - ahead
    order = []
    for step in range(ahead):
        order.append(-(ahead - step))
        if step < behind:
            order.append(behind - step)
    order.append(0)
    return order


class RingScatter:
    def __init__(self, devices, pieces, grads, outs, scratch):
        self.chips = devices // 2
        self.ahead = self.chips // 2
        self.behind = self.chips - 1 - self.ahead
        self.order = scatter_order(self.chips)
        self.pieces, self.grads, self.outs = pieces, grads, outs
        count = len(grads)
        self.mine, self.boxes, rest = scratch[:count], scratch[count : 2 * count], scratch[2 * count :]
        self.fbox, self.bbox, self.fout, self.bout = rest[:4]
        self.os, self.ms, self.mr, self.fs, self.fr, self.bs, self.br = rest[4:]
        self.rows = self.mine[0].shape[1]
        widths = [item.shape[2] for item in self.mine]
        self.cols = [slice(sum(widths[:i]), sum(widths[: i + 1])) for i in range(count)]

    def locate(self):
        me = lax.axis_index("dp")
        self.group = lax.axis_index("tensor")
        self.core = lax.rem(me, 2)
        chip = lax.div(me, 2)
        self.place = ring_place(chip, self.chips)
        self.right = ring_chip(self.place + 1, self.chips) * 2 + self.core
        self.left = ring_chip(self.place - 1, self.chips) * 2 + self.core
        self.mate = chip * 2 + (1 - self.core)

    def greet(self):
        self.locate()
        barrier = pltpu.get_barrier_semaphore()
        for other in (self.right, self.left, self.mate):
            pl.semaphore_signal(
                barrier, inc=1, device_id=(other, self.group), device_id_type=MESH
            )
        pl.semaphore_wait(barrier, 3)

    def block(self, i, shift, which):
        index = ring_chip(self.place + shift, self.chips) * 2 + which
        return self.grads[i].at[pl.ds(pl.multiple_of(index * self.rows, self.rows), self.rows), :]

    def remote(self, source, target_ref, ssem, rsem, target):
        return pltpu.make_async_remote_copy(
            src_ref=source,
            dst_ref=target_ref,
            send_sem=ssem,
            recv_sem=rsem,
            device_id=(target, self.group),
            device_id_type=MESH,
        )

    def across(self, i, slot):
        return self.remote(
            self.block(i, self.order[slot], 1 - self.core),
            self.boxes[i].at[slot],
            self.ms.at[i, slot],
            self.mr.at[i, slot],
            self.mate,
        )

    def own(self, i, slot):
        return pltpu.make_async_copy(
            self.block(i, self.order[slot], self.core), self.mine[i].at[slot], self.os.at[i, slot]
        )

    def fore(self, step):
        return self.remote(
            self.fout.at[step], self.fbox.at[step], self.fs.at[step], self.fr.at[step], self.right
        )

    def back(self, step):
        return self.remote(
            self.bout.at[step], self.bbox.at[step], self.bs.at[step], self.br.at[step], self.left
        )

    def begin(self):
        self.locate()
        for slot in range(self.chips):
            for i in range(len(self.grads)):
                self.across(i, slot).start()
                self.own(i, slot).start()

    def local_sum(self, i, slot, cols, others):
        total = self.mine[i][slot, :, cols].astype(F32) + self.boxes[i][slot, :, cols].astype(F32)
        whole = slice(self.cols[i].start + cols.start, self.cols[i].start + cols.stop)
        for ref in others:
            total = total + ref[:, whole].astype(F32)
        return total

    def arrive(self, slot):
        for i in range(len(self.grads)):
            self.own(i, slot).wait()
            self.across(i, slot).wait_recv()

    def put(self, target, shift, others):
        slot = self.order.index(shift)
        self.arrive(slot)
        for i, cols in enumerate(self.cols):
            total = self.local_sum(i, slot, slice(0, cols.stop - cols.start), others)
            target[:, cols] = total.astype(BF16)

    def hop(self, step):
        self.locate()
        if step > 0:
            self.back(step - 1).wait_recv()
        self.put(
            self.bout.at[step], -(self.ahead - step), [self.bbox.at[step - 1]] if step else []
        )
        self.back(step).start()
        if step < self.behind:
            if step > 0:
                self.fore(step - 1).wait_recv()
            self.put(
                self.fout.at[step], self.behind - step, [self.fbox.at[step - 1]] if step else []
            )
            self.fore(step).start()

    def finish(self):
        self.locate()
        slot = self.order.index(0)
        self.arrive(slot)
        self.fore(self.behind - 1).wait_recv()
        self.back(self.ahead - 1).wait_recv()
        others = [self.fbox.at[self.behind - 1], self.bbox.at[self.ahead - 1]]
        for out, (i, first, last) in zip(self.outs, self.pieces):
            out[...] = self.local_sum(i, slot, slice(first, last), others)
        for step in range(self.ahead):
            self.back(step).wait_send()
        for step in range(self.behind):
            self.fore(step).wait_send()
        for slot in range(self.chips):
            for i in range(len(self.grads)):
                self.across(i, slot).wait_send()


def scatter_scratch(grads, devices):
    chips = devices // 2
    rows = grads[0].shape[0] // devices
    count = len(grads)
    dma = pltpu.SemaphoreType.DMA
    boxes = [pltpu.VMEM((chips, rows, item.shape[1]), BF16) for item in grads]
    box = pltpu.VMEM((chips // 2, rows, sum(item.shape[1] for item in grads)), BF16)
    return boxes * 2 + [box] * 4 + [dma((count, chips))] * 3 + [dma((chips,))] * 4


def scatter_shapes(grads, pieces, devices):
    rows = grads[0].shape[0] // devices
    return tuple(jax.ShapeDtypeStruct((rows, last - first), F32) for i, first, last in pieces)


def scatter_kernel(devices, count, pieces, *refs):
    outs = len(pieces)
    ring = RingScatter(
        devices, pieces, refs[:count], refs[count : count + outs], refs[count + outs :]
    )
    ring.greet()
    ring.begin()
    for step in range(ring.ahead):
        ring.hop(step)
    ring.finish()


def scatter_rows(grads, pieces, devices, collective):
    count = len(grads)
    return pl.pallas_call(
        functools.partial(scatter_kernel, devices, count, pieces),
        out_shape=scatter_shapes(grads, pieces, devices),
        in_specs=[pl.BlockSpec(memory_space=pl.ANY)] * count,
        out_specs=(pl.BlockSpec(memory_space=pltpu.VMEM),) * len(pieces),
        scratch_shapes=scatter_scratch(grads, devices),
        compiler_params=pltpu.CompilerParams(collective_id=collective, has_side_effects=True),
        cost_estimate=cost(3),
        name="scatter_rows",
    )(*grads)


def total_kernel(devices, x_ref, o_ref, mate_box, joined, boxes, ms, mr, ss, sr):
    chips = devices // 2
    me = lax.axis_index("dp")
    group = lax.axis_index("tensor")
    chip = lax.div(me, 2)
    core = lax.rem(me, 2)
    mate = chip * 2 + (1 - core)
    peers = [lax.rem(chip + shift, chips) * 2 + core for shift in range(chips)]
    barrier = pltpu.get_barrier_semaphore()
    for other in [mate] + peers[1:]:
        pl.semaphore_signal(barrier, inc=1, device_id=(other, group), device_id_type=MESH)
    pl.semaphore_wait(barrier, chips)

    def copy_to(source, target_ref, ssem, rsem, target):
        copy = pltpu.make_async_remote_copy(
            src_ref=source,
            dst_ref=target_ref,
            send_sem=ssem,
            recv_sem=rsem,
            device_id=(target, group),
            device_id_type=MESH,
        )
        copy.start()
        return copy

    across = copy_to(x_ref, mate_box, ms, mr, mate)
    across.wait_recv()
    total = x_ref[...] + mate_box[...]
    joined[...] = total
    copies = [
        copy_to(joined, boxes.at[chip], ss.at[shift], sr.at[shift], peers[shift])
        for shift in range(1, chips)
    ]
    boxes[chip] = total
    for copy in copies:
        copy.wait_recv()
    result = boxes[0]
    for other in range(1, chips):
        result = result + boxes[other]
    o_ref[...] = result
    across.wait_send()
    for copy in copies:
        copy.wait_send()


def total_rows(values, devices, collective):
    dma = pltpu.SemaphoreType.DMA
    vmem = pl.BlockSpec(memory_space=pltpu.VMEM)
    chips = devices // 2
    return pl.pallas_call(
        functools.partial(total_kernel, devices),
        out_shape=jax.ShapeDtypeStruct(values.shape, F32),
        in_specs=[vmem],
        out_specs=vmem,
        scratch_shapes=[
            pltpu.VMEM(values.shape, F32),
            pltpu.VMEM(values.shape, F32),
            pltpu.VMEM((chips,) + values.shape, F32),
            dma(()),
            dma(()),
            dma((chips,)),
            dma((chips,)),
        ],
        compiler_params=pltpu.CompilerParams(collective_id=collective, has_side_effects=True),
        name="total_rows",
    )(values)


def head_spread(channels):
    return (iota((LANES, channels), 1) // MP == iota((LANES, channels), 0)).astype(F32)


def soft_step(raw):
    return jnp.maximum(raw, 0.0) + jnp.log1p(jnp.exp(-jnp.abs(raw)))


def conv_window(buffer, taps_ref, bias_ref, span):
    total = bias_ref[...] + taps_ref[0:1, :] * buffer[EDGE - 3 : EDGE - 3 + span, :]
    for tap in range(1, KCONV):
        start = EDGE - 3 + tap
        total = total + taps_ref[tap : tap + 1, :] * buffer[start : start + span, :]
    return total


def span_rates(step_ref, bias_ref, decay_ref, spread, span):
    raw = step_ref[...] + bias_ref[...]
    step = soft_step(raw)
    lower = (iota((span, span), 1) <= iota((span, span), 0)).astype(F32)
    cum = dot(lower, step * decay_ref[...], precision=HIGHEST)
    tails = jnp.exp(cum[span - 1 : span, :] - cum)
    wide = dot(
        jnp.concatenate([step, tails, jnp.exp(cum)], axis=0), spread, precision=HIGHEST
    )
    return raw, step, cum, wide[:span], wide[span : 2 * span], wide[2 * span :]


def pair_split(values, low_lanes):
    zero = jnp.zeros_like(values)
    return jnp.concatenate(
        [jnp.where(low_lanes, values, zero), jnp.where(low_lanes, zero, values)], axis=0
    )


def pair_decay(cum, cum_rows, pair, causal):
    parts = []
    for head in (2 * pair, 2 * pair + 1):
        differ = cum[:, head : head + 1] - cum_rows[head : head + 1, :]
        parts.append(jnp.exp(jnp.where(causal, differ, MASKED)))
    return parts


def scan_forward(
    devices, spans,
    z_ref, x_ref, bc_ref, step_ref,
    tap_ref, bias_ref, tapb_ref, biasb_ref, stepb_ref, decay_ref, skip_ref, shard_ref,
    y_ref, gated_ref, enter_ref, all_ref,
    state, xbuf, bbuf, *sems,
):
    span, channels = x_ref.shape
    ring = RingGather(devices, shard_ref, all_ref, sems)
    turn = pl.program_id(0)

    @pl.when(turn == 0)
    def _():
        ring.greet()
        ring.begin()


    @pl.when(pl.program_id(0) == 0)
    def _():
        state[...] = jnp.zeros_like(state)
        xbuf[span:, :] = jnp.zeros((EDGE, channels), F32)
        bbuf[span:, :] = jnp.zeros((EDGE, 2 * NS), F32)

    xbuf[:EDGE, :] = xbuf[span:, :]
    bbuf[:EDGE, :] = bbuf[span:, :]
    xbuf[EDGE:, :] = x_ref[...]
    bbuf[EDGE:, :] = bc_ref[...]
    inputs = jax.nn.silu(conv_window(xbuf, tap_ref, bias_ref, span))
    shared = jax.nn.silu(conv_window(bbuf, tapb_ref, biasb_ref, span))
    spread = head_spread(channels)
    raw, step, cum, step_w, tails_w, grown_w = span_rates(
        step_ref, stepb_ref, decay_ref, spread, span
    )
    cum_rows = cum.T
    b_low = shared[:, :NS].astype(BF16)
    c_low = shared[:, NS:].astype(BF16)
    scaled = inputs * step_w
    scaled_low = scaled.astype(BF16)
    enter_ref[0] = state[...]
    outer = dot(c_low, state[...].astype(BF16)) * grown_w
    fresh = dot(b_low, (scaled * tails_w).astype(BF16), TN)
    state[...] = state[...] * grown_w[span - 1 : span, :] + fresh
    cross = dot(c_low, b_low, NT)
    causal = iota((span, span), 1) <= iota((span, span), 0)
    low_lanes = iota((span, LANES), 1) < MP
    for pair in range(channels // LANES):
        lanes = slice(pair * LANES, (pair + 1) * LANES)
        first, second = pair_decay(cum, cum_rows, pair, causal)
        weights = jnp.concatenate(
            [(cross * first).astype(BF16), (cross * second).astype(BF16)], axis=1
        )
        y_ref[:, lanes] = dot(weights, pair_split(scaled_low[:, lanes], low_lanes))
    y = y_ref[...] + outer + skip_ref[...] * inputs
    y_ref[...] = y
    gated_ref[...] = y * jax.nn.silu(z_ref[...])

    count = spans
    for step in range(1, ring.ahead + 1):
        pl.when(turn == min(count - 1, count * step // ring.ahead))(
            functools.partial(ring.hop, step)
        )
    pl.when(turn == count - 1)(ring.finish)


def scan_backward(
    devices, spans, pieces, count,
    z_ref, x_ref, xp_ref, bc_ref, bp_ref, step_ref, y_ref, enter_ref,
    dyg_ref, scale_ref, inner_ref, dqkv_ref,
    tap_ref, bias_ref, tapb_ref, biasb_ref, stepb_ref, decay_ref, skip_ref, gain_ref,
    *refs,
):
    sent, refs = refs[:count], refs[count:]
    (grad_ref, gx_ref, gb_ref, gh_ref), refs = refs[:4], refs[4:]
    outs, refs = refs[: len(pieces)], refs[len(pieces) :]
    (dstate, xbuf, bbuf, dxbuf, dbbuf, du_buf, col_buf), scratch = refs[:7], refs[7:]
    ring = RingScatter(devices, pieces, sent, outs, scratch)
    span, channels = x_ref.shape
    turn = pl.program_id(0)

    @pl.when(turn == 0)
    def _():
        ring.greet()
        ring.begin()
        dstate[...] = jnp.zeros_like(dstate)
        dxbuf[...] = jnp.zeros_like(dxbuf)
        dbbuf[...] = jnp.zeros_like(dbbuf)
        col_buf[...] = jnp.zeros_like(col_buf)
        gx_ref[...] = jnp.zeros_like(gx_ref)
        gb_ref[...] = jnp.zeros_like(gb_ref)
        gh_ref[...] = jnp.zeros_like(gh_ref)

    inside = (turn < spans - 1).astype(F32)
    xbuf[:EDGE, :] = xp_ref[...] * inside
    bbuf[:EDGE, :] = bp_ref[...] * inside
    xbuf[EDGE:, :] = x_ref[...]
    bbuf[EDGE:, :] = bc_ref[...]
    conv = conv_window(xbuf, tap_ref, bias_ref, span)
    sig = jax.nn.sigmoid(conv)
    inputs = conv * sig
    convb = conv_window(bbuf, tapb_ref, biasb_ref, span)
    sigb = jax.nn.sigmoid(convb)
    shared = convb * sigb
    b_low = shared[:, :NS].astype(BF16)
    c_low = shared[:, NS:].astype(BF16)
    spread = head_spread(channels)
    raw, step, cum, step_w, tails_w, grown_w = span_rates(
        step_ref, stepb_ref, decay_ref, spread, span
    )
    cum_rows = cum.T
    scaled = inputs * step_w
    scaled_low = scaled.astype(BF16)

    z = z_ref[...]
    sig_z = jax.nn.sigmoid(z)
    swish = z * sig_z
    y = y_ref[...]
    normed = y * swish * scale_ref[...]
    dyg = dyg_ref[...]
    gain_grad = jnp.sum(dyg * normed, axis=0, keepdims=True)
    dgated = scale_ref[...] * (dyg * gain_ref[...] - normed * inner_ref[...])
    dy = dgated * swish
    grad_ref[:, :channels] = (dgated * y * (sig_z * (1.0 + z * (1.0 - sig_z)))).astype(BF16)

    state_low = enter_ref[0].astype(BF16)
    dstate_low = dstate[...].astype(BF16)
    grown_low = (dy * grown_w).astype(BF16)
    dy_low = dy.astype(BF16)
    tailed = scaled * tails_w
    outer = dot(c_low, state_low) * grown_w
    from_state = dot(b_low, dstate_low)
    dc = dot(grown_low, state_low, NT)
    db = dot(tailed.astype(BF16), dstate_low, NT)
    leak = from_state * tailed
    last_w = grown_w[span - 1 : span, :]
    ends = (
        jnp.sum(leak, axis=0, keepdims=True)
        + jnp.sum(enter_ref[0] * dstate[...], axis=0, keepdims=True) * last_w
    )
    skips = jnp.sum(dy * inputs, axis=0, keepdims=True)
    dstate[...] = dstate[...] * last_w + dot(c_low, grown_low, TN)

    cross = dot(c_low, b_low, NT)
    causal = iota((span, span), 1) <= iota((span, span), 0)
    low_lanes = iota((span, LANES), 1) < MP
    lane = iota((span, LANES), 1)
    dcross = jnp.zeros((span, span), F32)
    row_part = jnp.zeros((span, LANES), F32)
    for pair in range(channels // LANES):
        lanes = slice(pair * LANES, (pair + 1) * LANES)
        decays = pair_decay(cum, cum_rows, pair, causal)
        dy_pair = pair_split(dy_low[:, lanes], low_lanes)
        dweights = dot(dy_pair, scaled_low[:, lanes], NT)
        both = []
        for part in range(2):
            head = 2 * pair + part
            dterm = dweights[part * span : (part + 1) * span] * decays[part]
            dcross = dcross + dterm
            flow = dterm * cross
            row_part = row_part + jnp.where(
                lane == head, jnp.sum(flow, axis=1, keepdims=True), 0.0
            )
            col_buf[head : head + 1, :] = jnp.sum(flow, axis=0, keepdims=True)
            both.append((cross * decays[part]).astype(BF16))
        du_buf[:, lanes] = dot(jnp.concatenate(both, axis=0), dy_pair, TN)
    du = du_buf[...] + from_state * tails_w
    dcross_low = dcross.astype(BF16)
    dc = dc + dot(dcross_low, b_low)
    db = db + dot(dcross_low, c_low, TN)

    sums = dot(
        jnp.concatenate(
            [dy * outer - leak, du * inputs, ends, skips, jnp.zeros((EDGE - 2, channels), F32)],
            axis=0,
        ),
        spread,
        NT,
        HIGHEST,
    )
    at_end = sums[2 * span : 2 * span + 1, :]
    dcum = sums[:span] + row_part - col_buf[...].T
    upper = (iota((span, span), 1) >= iota((span, span), 0)).astype(F32)
    drate = dot(upper, dcum, precision=HIGHEST) + at_end
    dstep = drate * decay_ref[...] + sums[span : 2 * span]
    draw = dstep * jax.nn.sigmoid(raw)
    gh_ref[0:1, :] += jnp.sum(draw, axis=0, keepdims=True)
    gh_ref[1:2, :] += jnp.sum(drate * step, axis=0, keepdims=True) * decay_ref[...]
    gh_ref[2:3, :] += sums[2 * span + 1 : 2 * span + 2, :]

    dinputs = du * step_w + skip_ref[...] * dy
    dxbuf[span:, :] = dxbuf[:EDGE, :]
    dbbuf[span:, :] = dbbuf[:EDGE, :]
    dconv = dinputs * (sig * (1.0 + conv * (1.0 - sig)))
    dconvb = jnp.concatenate([db, dc], axis=1) * (sigb * (1.0 + convb * (1.0 - sigb)))
    dxbuf[:span, :] = dconv
    dbbuf[:span, :] = dconvb
    dx = jnp.zeros_like(dconv)
    dbc = jnp.zeros_like(dconvb)
    for tap in range(KCONV):
        back = KCONV - 1 - tap
        start = EDGE - 3 + tap
        dx = dx + tap_ref[tap : tap + 1, :] * dxbuf[back : back + span, :]
        dbc = dbc + tapb_ref[tap : tap + 1, :] * dbbuf[back : back + span, :]
        gx_ref[tap : tap + 1, :] += jnp.sum(
            dconv * xbuf[start : start + span, :], axis=0, keepdims=True
        )
        gb_ref[tap : tap + 1, :] += jnp.sum(
            dconvb * bbuf[start : start + span, :], axis=0, keepdims=True
        )
    gx_ref[KCONV : KCONV + 1, :] += jnp.sum(dconv, axis=0, keepdims=True)
    gb_ref[KCONV : KCONV + 1, :] += jnp.sum(dconvb, axis=0, keepdims=True)
    gx_ref[KCONV + 1 : KCONV + 2, :] += gain_grad
    width = 2 * channels + 2 * NS
    grad_ref[:, channels : 2 * channels] = dx.astype(BF16)
    grad_ref[:, 2 * channels : width] = dbc.astype(BF16)
    grad_ref[:, width : width + dqkv_ref.shape[1]] = dqkv_ref[...]
    grad_ref[:, width + dqkv_ref.shape[1] :] = draw.astype(BF16)
    for step in range(ring.ahead):
        pl.when(turn == spans * step // ring.ahead)(functools.partial(ring.hop, step))
    pl.when(turn == spans - 1)(ring.finish)


def scan_params(conv_x, conv_xb, conv_bc, conv_bcb, dt_bias, a_log, d_skip):
    heads = dt_bias.shape[0]

    def wide(row):
        return jnp.pad(row, (0, LANES - heads))[None, :]

    f32 = lambda value: value.astype(F32)
    return (
        f32(conv_x),
        f32(conv_xb)[None, :],
        f32(conv_bc),
        f32(conv_bcb)[None, :],
        wide(f32(dt_bias)),
        wide(-jnp.exp(f32(a_log))),
        jnp.repeat(f32(d_skip), MP)[None, :],
    )


def whole_spec(array):
    return pl.BlockSpec(array.shape, lambda turn: (0,) * array.ndim)


def run_scan_forward(proj, qkv_width, params, shard, devices):
    tokens = proj.shape[0]
    channels = params[1].shape[1]
    step_at = (2 * channels + 2 * NS + qkv_width) // LANES
    spans = tokens // SPAN
    bc_at = 2 * channels // (2 * NS)
    rows = lambda width, at: pl.BlockSpec((SPAN, width), lambda turn: (turn, at))
    anywhere = pl.BlockSpec(memory_space=pl.ANY)
    return pl.pallas_call(
        functools.partial(scan_forward, devices, spans),
        grid=(spans,),
        out_shape=(
            jax.ShapeDtypeStruct((tokens, channels), F32),
            jax.ShapeDtypeStruct((tokens, channels), F32),
            jax.ShapeDtypeStruct((spans, NS, channels), F32),
            gather_shape(shard, devices),
        ),
        in_specs=[rows(channels, 0), rows(channels, 1), rows(2 * NS, bc_at), rows(LANES, step_at)]
        + [whole_spec(item) for item in params]
        + [anywhere],
        out_specs=(
            rows(channels, 0),
            rows(channels, 0),
            pl.BlockSpec((1, NS, channels), lambda turn: (turn, 0, 0)),
            anywhere,
        ),
        scratch_shapes=[
            pltpu.VMEM((NS, channels), F32),
            pltpu.VMEM((SPAN + EDGE, channels), F32),
            pltpu.VMEM((SPAN + EDGE, 2 * NS), F32),
        ]
        + gather_sems(devices),
        compiler_params=pltpu.CompilerParams(collective_id=2, has_side_effects=True),
        cost_estimate=cost(20),
        name="scan_forward",
    )(proj, proj, proj, proj, *params, shard)


def run_scan_backward(
    proj, y, entering, dyg, scale, inner, dqkv, params, gain, sent, pieces, devices
):
    tokens, width = proj.shape
    channels = params[1].shape[1]
    qkv_width = dqkv.shape[1]
    step_at = (2 * channels + 2 * NS + qkv_width) // LANES
    spans = tokens // SPAN
    bc_at = 2 * channels // (2 * NS)
    edges = SPAN // EDGE
    rows = lambda size, at: pl.BlockSpec((SPAN, size), lambda turn: (spans - 1 - turn, at))
    edge = lambda size, at: pl.BlockSpec(
        (EDGE, size), lambda turn: (jnp.maximum((spans - 1 - turn) * edges - 1, 0), at)
    )
    keep = lambda shape: pl.BlockSpec(shape, lambda turn: (0, 0))
    shapes = scatter_shapes(sent, pieces, devices)
    return pl.pallas_call(
        functools.partial(scan_backward, devices, spans, pieces, len(sent)),
        grid=(spans,),
        out_shape=(
            jax.ShapeDtypeStruct((tokens, width), BF16),
            jax.ShapeDtypeStruct((EDGE, channels), F32),
            jax.ShapeDtypeStruct((EDGE, 2 * NS), F32),
            jax.ShapeDtypeStruct((EDGE, LANES), F32),
        )
        + shapes,
        in_specs=[
            rows(channels, 0),
            rows(channels, 1),
            edge(channels, 1),
            rows(2 * NS, bc_at),
            edge(2 * NS, bc_at),
            rows(LANES, step_at),
            rows(channels, 0),
            pl.BlockSpec((1, NS, channels), lambda turn: (spans - 1 - turn, 0, 0)),
            rows(channels, 0),
            rows(1, 0),
            rows(1, 0),
            rows(qkv_width, 0),
        ]
        + [whole_spec(item) for item in params]
        + [whole_spec(gain)]
        + [pl.BlockSpec(memory_space=pl.ANY)] * len(sent),
        out_specs=(
            rows(width, 0),
            keep((EDGE, channels)),
            keep((EDGE, 2 * NS)),
            keep((EDGE, LANES)),
        )
        + tuple(keep(item.shape) for item in shapes),
        scratch_shapes=[
            pltpu.VMEM((NS, channels), F32),
            pltpu.VMEM((SPAN + EDGE, channels), F32),
            pltpu.VMEM((SPAN + EDGE, 2 * NS), F32),
            pltpu.VMEM((SPAN + EDGE, channels), F32),
            pltpu.VMEM((SPAN + EDGE, 2 * NS), F32),
            pltpu.VMEM((SPAN, channels), F32),
            pltpu.VMEM((LANES, SPAN), F32),
        ]
        + scatter_scratch(sent, devices),
        compiler_params=pltpu.CompilerParams(collective_id=6, has_side_effects=True),
        cost_estimate=cost(47),
        name="scan_backward",
    )(
        proj, proj, proj, proj, proj, proj, y, entering, dyg, scale, inner, dqkv, *params, gain,
        *sent,
    )


def rotary_tables(tokens):
    half = HEAD_SIZE // 2
    exponent = np.arange(half, dtype=np.float32) * np.float32(-2.0 * LOG_BASE / HEAD_SIZE)
    angles = np.arange(tokens, dtype=np.float32)[:, None] * np.exp(exponent)[None, :]
    cosine = np.cos(angles).astype(np.float32)
    sine = np.sin(angles).astype(np.float32)
    return (
        np.concatenate([cosine] * 4, axis=1),
        np.concatenate([-sine, sine, -sine, sine], axis=1),
    )


def rotate(values, cosine, sine):
    half = HEAD_SIZE // 2
    low = iota(values.shape, 1) % HEAD_SIZE < half
    turned = jnp.where(
        low, pltpu.roll(values, LANES - half, 1), pltpu.roll(values, half, 1)
    )
    return values * cosine + turned * sine


def attend_forward(
    q_ref, kv_ref, cos_ref, sin_ref, qkv_ref, lse_ref, o_ref, heads_q, heads_o, vt
):
    tokens, query_width = q_ref.shape
    heads = query_width // HEAD_SIZE
    cosine, sine = cos_ref[...], sin_ref[...]
    for pair in range(heads // 2):
        lanes = slice(pair * LANES, (pair + 1) * LANES)
        turned = (rotate(q_ref[:, lanes], cosine, sine) * HEAD_SIZE**-0.5).astype(BF16)
        qkv_ref[:, lanes] = turned
        heads_q[2 * pair] = turned[:, :HEAD_SIZE]
        heads_q[2 * pair + 1] = turned[:, HEAD_SIZE:]
    kv = kv_ref[...]
    first = iota(kv.shape, 1) < HEAD_SIZE
    qkv_ref[:, query_width:] = jnp.where(first, rotate(kv, cosine, sine), kv).astype(BF16)
    vt[...] = kv[:, HEAD_SIZE:].T.astype(BF16)
    visible = iota((QBLK, QBLK), 0) <= iota((QBLK, QBLK), 1)
    for start in range(0, tokens, QBLK):
        limit = start + QBLK

        def one(head, carry):
            keys = qkv_ref[:limit, query_width : query_width + HEAD_SIZE]
            scores = dot(keys, heads_q[head, start:limit, :], NT)
            edge = jnp.where(visible, scores[start:], MASKED)
            top = jnp.max(edge, axis=0, keepdims=True)
            if start:
                top = jnp.maximum(top, jnp.max(scores[:start], axis=0, keepdims=True))
            probs = jnp.exp(edge - top)
            if start:
                probs = jnp.concatenate([jnp.exp(scores[:start] - top), probs], axis=0)
            total = jnp.sum(probs, axis=0, keepdims=True)
            out = dot(vt[:, :limit], probs.astype(BF16)) / total
            heads_o[head, start:limit, :] = out.T.astype(BF16)
            lse_ref[pl.ds(head, 1), start:limit] = top + jnp.log(total)
            return carry

        lax.fori_loop(0, heads, one, 0)
    for pair in range(heads // 2):
        o_ref[:, pair * LANES : (pair + 1) * LANES] = jnp.concatenate(
            [heads_o[2 * pair], heads_o[2 * pair + 1]], axis=1
        )


def attend_backward(
    qkv_ref, lse_ref, o_ref, do_ref, cos_ref, sin_ref, dqkv_ref,
    heads_q, heads_do, heads_dq, heads_sum, kt, dk, dv,
):
    tokens, query_width = o_ref.shape
    heads = query_width // HEAD_SIZE
    ones = jnp.ones((EDGE, HEAD_SIZE), F32)
    for head in range(heads):
        lanes = slice(head * HEAD_SIZE, (head + 1) * HEAD_SIZE)
        grad = do_ref[:, lanes]
        heads_q[head] = qkv_ref[:, lanes]
        heads_do[head] = grad
        both = grad.astype(F32) * o_ref[:, lanes].astype(F32)
        heads_sum[head : head + 1, :] = dot(ones, both, NT, HIGHEST)[:1]
    kt[...] = qkv_ref[:, query_width : query_width + HEAD_SIZE].astype(F32).T.astype(BF16)
    dk[...] = jnp.zeros_like(dk)
    dv[...] = jnp.zeros_like(dv)
    visible = iota((QBLK, QBLK), 0) <= iota((QBLK, QBLK), 1)
    for start in range(0, tokens, QBLK):
        limit = start + QBLK

        def one(head, carry):
            keys = qkv_ref[:limit, query_width : query_width + HEAD_SIZE]
            values = qkv_ref[:limit, query_width + HEAD_SIZE :]
            query = heads_q[head, start:limit, :]
            grad = heads_do[head, start:limit, :]
            scores = dot(keys, query, NT) - lse_ref[pl.ds(head, 1), start:limit]
            probs = jnp.exp(jnp.where(visible, scores[start:], MASKED))
            if start:
                probs = jnp.concatenate([jnp.exp(scores[:start]), probs], axis=0)
            dprobs = dot(values, grad, NT)
            dscores = (probs * (dprobs - heads_sum[pl.ds(head, 1), start:limit])).astype(BF16)
            dv[:limit, :] += dot(probs.astype(BF16), grad)
            dk[:limit, :] += dot(dscores, query)
            heads_dq[head, start:limit, :] = dot(kt[:, :limit], dscores).T
            return carry

        lax.fori_loop(0, heads, one, 0)
    cosine, sine = cos_ref[...], -sin_ref[...]
    for pair in range(heads // 2):
        joined = jnp.concatenate([heads_dq[2 * pair], heads_dq[2 * pair + 1]], axis=1)
        dqkv_ref[:, pair * LANES : (pair + 1) * LANES] = (
            rotate(joined, cosine, sine) * HEAD_SIZE**-0.5
        ).astype(BF16)
    joined = jnp.concatenate([dk[...], dv[...]], axis=1)
    first = iota(joined.shape, 1) < HEAD_SIZE
    dqkv_ref[:, query_width:] = jnp.where(
        first, rotate(joined, cosine, sine), joined
    ).astype(BF16)


def run_attend_forward(proj, query_at, query_width, tables):
    tokens = proj.shape[0]
    heads = query_width // HEAD_SIZE
    cols = lambda size, at: pl.BlockSpec((tokens, size), lambda turn: (0, at // size))
    return pl.pallas_call(
        attend_forward,
        grid=(1,),
        out_shape=(
            jax.ShapeDtypeStruct((tokens, query_width + 2 * HEAD_SIZE), BF16),
            jax.ShapeDtypeStruct((EDGE, tokens), F32),
            jax.ShapeDtypeStruct((tokens, query_width), BF16),
        ),
        in_specs=[
            cols(query_width, query_at),
            cols(2 * HEAD_SIZE, query_at + query_width),
            cols(LANES, 0),
            cols(LANES, 0),
        ],
        out_specs=(
            cols(query_width + 2 * HEAD_SIZE, 0),
            pl.BlockSpec((EDGE, tokens), lambda turn: (0, 0)),
            cols(query_width, 0),
        ),
        scratch_shapes=[
            pltpu.VMEM((heads, tokens, HEAD_SIZE), BF16),
            pltpu.VMEM((heads, tokens, HEAD_SIZE), BF16),
            pltpu.VMEM((HEAD_SIZE, tokens), BF16),
        ],
        cost_estimate=cost(15),
        name="attend_forward",
    )(proj, proj, *tables)


def run_attend_backward(qkv, lse, attended, grad, tables):
    tokens, query_width = attended.shape
    heads = query_width // HEAD_SIZE
    vmem = pl.BlockSpec(memory_space=pltpu.VMEM)
    return pl.pallas_call(
        attend_backward,
        out_shape=jax.ShapeDtypeStruct((tokens, query_width + 2 * HEAD_SIZE), BF16),
        in_specs=[vmem] * 6,
        out_specs=vmem,
        scratch_shapes=[
            pltpu.VMEM((heads, tokens, HEAD_SIZE), BF16),
            pltpu.VMEM((heads, tokens, HEAD_SIZE), BF16),
            pltpu.VMEM((heads, tokens, HEAD_SIZE), F32),
            pltpu.VMEM((EDGE, tokens), F32),
            pltpu.VMEM((HEAD_SIZE, tokens), BF16),
            pltpu.VMEM((tokens, HEAD_SIZE), F32),
            pltpu.VMEM((tokens, HEAD_SIZE), F32),
        ],
        cost_estimate=cost(16),
        name="attend_backward",
    )(qkv, lse, attended, grad, *tables)


def swap(partial):
    return lax.ppermute(partial, "tensor", [(0, 1), (1, 0)])


def join(mine, other):
    return mine.astype(F32) + other.astype(F32)


def tensor_sum(partial):
    return join(partial, swap(partial))


def norm_back(normed, scale, gain, grad):
    weighted = grad * gain
    grad_input = scale * (weighted - normed * jnp.mean(weighted * normed, axis=-1, keepdims=True))
    return (grad_input, jnp.sum(grad * normed, axis=0))


def local(
    layer_input, w_norm1, w_zx, w_bc, w_dt, conv_x, conv_xb, conv_bc, conv_bcb, dt_bias, a_log,
    d_skip, w_mnorm, w_mout, query_key_value_weight, output_weight, w_norm2, w_gu, w_down,
    grad_output,
):
    devices = lax.axis_size("dp")
    tokens, width = layer_input.shape
    shard = w_zx.shape[0]
    channels = conv_xb.shape[0]
    heads = dt_bias.shape[0]
    qkv_width = query_key_value_weight.shape[2]
    units = w_down.shape[0]
    attn_width = output_weight.shape[1]
    tail = jnp.concatenate(
        [w_dt, w_norm1[:, None], w_norm2[:, None], jnp.zeros((shard, LANES - heads - 2), BF16)],
        axis=1,
    )
    mixer_in = jnp.concatenate(
        [w_zx.reshape(shard, -1), w_bc, query_key_value_weight.reshape(shard, -1), tail], axis=1
    )
    in_width = mixer_in.shape[1]
    (w_in,) = gather_rows([mixer_in], devices, 0)
    norm1 = w_in[:, in_width - LANES + heads].astype(F32)
    norm2 = w_in[:, in_width - LANES + heads + 1].astype(F32)

    source = layer_input.astype(F32)
    scale_one = lax.rsqrt(jnp.mean(source * source, axis=-1, keepdims=True) + EPSILON)
    normed_one = source * scale_one
    hidden_one = (normed_one * norm1).astype(BF16)
    proj = dot(hidden_one, w_in)
    params = scan_params(conv_x, conv_xb, conv_bc, conv_bcb, dt_bias, a_log, d_skip)
    out_shard = jnp.concatenate([w_mout.T, output_weight.reshape(attn_width, -1).T], axis=1)
    y, gated, entering, w_out = run_scan_forward(proj, qkv_width, params, out_shard, devices)
    channels_all = channels * lax.axis_size("tensor")
    square_sum = tensor_sum(jnp.sum(gated * gated, axis=-1))
    scale_m = lax.rsqrt(square_sum / channels_all + EPSILON)[:, None]
    tables = rotary_tables(tokens)
    qkv_at = 2 * channels + 2 * NS
    qkv, lse, attended = run_attend_forward(proj, qkv_at, attn_width, tables)
    gain_m = w_mnorm.astype(F32)
    mamba_low = (gated * scale_m * gain_m).astype(BF16)
    mixer_out = jnp.concatenate([mamba_low, attended], axis=1)
    mixed, gate_up_shard, down_shard = lax.optimization_barrier(
        (dot(mixer_out, w_out, NT).astype(BF16), w_gu.reshape(shard, -1), w_down.T)
    )
    other = swap(mixed)
    w_gate_up, w_down_t = gather_rows([gate_up_shard, down_shard], devices, 3)
    other, w_gate_up, w_down_t = lax.optimization_barrier((other, w_gate_up, w_down_t))
    after = source + join(mixed, other)
    scale_two = lax.rsqrt(jnp.mean(after * after, axis=-1, keepdims=True) + EPSILON)
    normed_two = after * scale_two
    hidden_two = (normed_two * norm2).astype(BF16)
    gate_up = dot(hidden_two, w_gate_up)
    gate = gate_up[:, :units]
    upward = gate_up[:, units:]
    sigma = jax.nn.sigmoid(gate)
    swish = gate * sigma
    activated = (swish * upward).astype(BF16)
    grad_act = dot(grad_output, w_down_t)
    grad_gate = grad_act * upward * sigma * (1.0 + gate * (1.0 - sigma))
    grad_up = grad_act * swish
    grad_gu_low = jnp.concatenate([grad_gate, grad_up], axis=1).astype(BF16)
    partial_two, grad_gu_low = lax.optimization_barrier(
        (dot(grad_gu_low, w_gate_up, NT).astype(BF16), grad_gu_low)
    )
    other = swap(partial_two)
    grad_gu = dot(hidden_two, grad_gu_low, TN).astype(BF16)
    grad_down = dot(grad_output, activated, TN).astype(BF16)
    (mine_gu,) = scatter_rows([grad_gu], [(0, 0, 2 * units)], devices, 1)
    ffn_part = dot(activated, w_down_t, NT).astype(BF16)
    other, mine_gu, grad_down, ffn_part = lax.optimization_barrier(
        (other, mine_gu, grad_down, ffn_part)
    )
    grad_hidden_two = join(partial_two, other)
    ffn_other = swap(ffn_part)
    grad_norm_in, grad_norm2 = norm_back(normed_two, scale_two, norm2, grad_hidden_two)
    grad_after = grad_output.astype(F32) + grad_norm_in
    grad_mix_low = grad_after.astype(BF16)
    grad_mixer = dot(grad_mix_low, w_out)
    grad_mamba = grad_mixer[:, :channels]
    normed_m = gated * scale_m
    inner_m = tensor_sum(jnp.sum(grad_mamba * gain_m * normed_m, axis=-1))[:, None] / channels_all
    dqkv = run_attend_backward(
        qkv, lse, attended, grad_mixer[:, channels:].astype(BF16), tables
    )
    grad_out = dot(grad_mix_low, mixer_out, TN).astype(BF16)
    pieces = [
        (0, 0, channels),
        (0, channels, channels + attn_width),
        (1, 0, units),
    ]
    grad_proj, small_x, small_b, small_h, mine_mout, mine_o, mine_down = run_scan_backward(
        proj, y, entering, grad_mamba, scale_m, inner_m, dqkv, params, gain_m[None, :],
        [grad_out, grad_down], pieces, devices,
    )
    ffn_other, grad_proj = lax.optimization_barrier((ffn_other, grad_proj))
    result = (after + join(ffn_part, ffn_other)).astype(BF16)
    partial_one, grad_proj = lax.optimization_barrier(
        (dot(grad_proj, w_in, NT).astype(BF16), grad_proj)
    )
    other = swap(partial_one)
    grad_in = dot(hidden_one, grad_proj, TN).astype(BF16)
    shared_at = 2 * channels
    step_at = qkv_at + qkv_width
    mine_zx, mine_bc, mine_qkv, mine_step = scatter_rows(
        [grad_in],
        [
            (0, 0, shared_at),
            (0, shared_at, qkv_at),
            (0, qkv_at, step_at),
            (0, step_at, in_width),
        ],
        devices,
        5,
    )
    other, mine_bc = lax.optimization_barrier((other, mine_bc))
    grad_hidden_one = join(partial_one, other)
    grad_norm_x, grad_norm1 = norm_back(normed_one, scale_one, norm1, grad_hidden_one)
    grad_source = grad_after + grad_norm_x

    half = NS * 2 // lax.axis_size("tensor")
    shared_cols = tensor_sum(mine_bc)
    begin = lax.axis_index("tensor") * half
    grad_bc = lax.dynamic_slice_in_dim(shared_cols, begin, half, 1)
    small = jnp.concatenate(
        [
            small_x[: KCONV + 2].reshape(-1, LANES),
            small_h[:3],
            tensor_sum(small_b[: KCONV + 1].reshape(-1)).reshape(-1, LANES),
            grad_norm1.reshape(-1, LANES),
            grad_norm2.reshape(-1, LANES),
        ],
        axis=0,
    )
    small_rows = small.shape[0]
    small = jnp.pad(small, ((0, -small_rows % EDGE), (0, 0)))
    small = total_rows(small, devices, 4)[:small_rows].reshape(-1)
    x_size = (KCONV + 2) * channels
    h_size = 3 * LANES
    b_size = (KCONV + 1) * 2 * NS
    total_x = small[:x_size].reshape(KCONV + 2, channels)
    total_h = small[x_size : x_size + h_size].reshape(3, LANES)
    total_b = small[x_size + h_size : x_size + h_size + b_size].reshape(KCONV + 1, 2 * NS)
    total_b = lax.dynamic_slice_in_dim(total_b, begin, half, 1)
    norms = small[x_size + h_size + b_size :].reshape(2, width)
    norms = lax.dynamic_slice_in_dim(norms, lax.axis_index("dp") * shard, shard, 1)
    return (
        result,
        grad_source,
        norms[0],
        mine_zx.reshape(w_zx.shape),
        grad_bc,
        mine_step[:, :heads],
        total_x[:KCONV],
        total_x[KCONV],
        total_b[:KCONV],
        total_b[KCONV],
        total_h[0, :heads],
        total_h[1, :heads],
        total_h[2, :heads],
        total_x[KCONV + 1],
        mine_mout.T,
        mine_qkv.reshape(query_key_value_weight.shape),
        mine_o.T.reshape(output_weight.shape),
        norms[1],
        mine_gu.reshape(w_gu.shape),
        mine_down.T,
    )


def solution(mesh):
    return jax.shard_map(
        local,
        mesh=mesh,
        in_specs=(
            P("dp", None),
            P("dp"),
            P("dp", None, "tensor"),
            P("dp", None),
            P("dp", "tensor"),
            P(None, "tensor"),
            P("tensor"),
            P(),
            P(),
            P("tensor"),
            P("tensor"),
            P("tensor"),
            P("tensor"),
            P("tensor", "dp"),
            P("dp", "tensor", None),
            P("tensor", None, "dp"),
            P("dp"),
            P("dp", None, "tensor"),
            P("tensor", "dp"),
            P("dp", None),
        ),
        out_specs=(
            P("dp", None),
            P("dp", None),
            P("dp"),
            P("dp", None, "tensor"),
            P("dp", "tensor"),
            P("dp", "tensor"),
            P(None, "tensor"),
            P("tensor"),
            P(None, "tensor"),
            P("tensor"),
            P("tensor"),
            P("tensor"),
            P("tensor"),
            P("tensor"),
            P("tensor", "dp"),
            P("dp", "tensor", None),
            P("tensor", None, "dp"),
            P("dp"),
            P("dp", None, "tensor"),
            P("tensor", "dp"),
        ),
        check_vma=False,
    )
```

```python
import functools
import math

import jax
import jax.numpy as jnp
import numpy as np
from jax import lax
from jax.experimental import pallas as pl
from jax.experimental.pallas import tpu as pltpu
from jax.sharding import PartitionSpec as P

HEAD_SIZE = 64
MP = 64
NS = 128
KCONV = 4
SPAN = 128
QBLK = 256
FINE = 32
LANES = 128
EDGE = 8

EPSILON = 1e-05
HIGHEST = lax.Precision.HIGHEST
LOG_BASE = math.log(100000000000.0)
MASKED = -1e30
MESH = pl.DeviceIdType.MESH
F32 = jnp.float32
BF16 = jnp.bfloat16

NN = ((1,), (0,))
NT = ((1,), (1,))
TN = ((0,), (0,))


def dot(left, right, dims=NN, precision=None):
    return lax.dot_general(
        left, right, (dims, ((), ())), preferred_element_type=F32, precision=precision
    )


def iota(shape, dim):
    return lax.broadcasted_iota(jnp.int32, shape, dim)


def ring_place(chip, chips):
    odd = lax.rem(chip, 2)
    half = lax.div(chip, 2)
    return (1 - odd) * half + odd * (chips - 1 - half)


def ring_chip(place, chips):
    place = lax.rem(place + 4 * chips, chips)
    back = lax.div(place, chips // 2)
    return (1 - back) * (2 * place) + back * (2 * (chips - 1 - place) + 1)


def ring_setup(chips):
    me = lax.axis_index("dp")
    group = lax.axis_index("tensor")
    chip = lax.div(me, 2)
    core = lax.rem(me, 2)
    place = ring_place(chip, chips)
    right = ring_chip(place + 1, chips) * 2 + core
    left = ring_chip(place - 1, chips) * 2 + core
    mate = chip * 2 + (1 - core)
    barrier = pltpu.get_barrier_semaphore()
    for other in (right, left, mate):
        pl.semaphore_signal(barrier, inc=1, device_id=(other, group), device_id_type=MESH)
    pl.semaphore_wait(barrier, 3)
    return me, group, core, place, right, left, mate


class RingGather:
    def __init__(self, devices, x_ref, o_ref, sems):
        self.chips = devices // 2
        self.ahead = self.chips // 2
        self.behind = self.chips - 1 - self.ahead
        self.x_ref, self.o_ref, self.rows = x_ref, o_ref, x_ref.shape[0]
        self.fs, self.fr, self.bs, self.br, self.cs, self.cr, self.own_sem = sems

    def locate(self):
        me = lax.axis_index("dp")
        self.group = lax.axis_index("tensor")
        self.core = lax.rem(me, 2)
        chip = lax.div(me, 2)
        self.place = ring_place(chip, self.chips)
        self.right = ring_chip(self.place + 1, self.chips) * 2 + self.core
        self.left = ring_chip(self.place - 1, self.chips) * 2 + self.core
        self.mate = chip * 2 + (1 - self.core)
        self.me = me

    def slot(self, index):
        return self.o_ref.at[pl.ds(pl.multiple_of(index * self.rows, self.rows), self.rows), :]

    def copy(self, shift, ssem, rsem, target):
        if shift == 0:
            index, source = self.me, self.x_ref
        else:
            index = ring_chip(self.place + shift, self.chips) * 2 + self.core
            source = self.slot(index)
        return pltpu.make_async_remote_copy(
            src_ref=source,
            dst_ref=self.slot(index),
            send_sem=ssem,
            recv_sem=rsem,
            device_id=(target, self.group),
            device_id_type=MESH,
        )

    def fore(self, step):
        return self.copy(-step, self.fs.at[step], self.fr.at[step], self.right)

    def back(self, step):
        return self.copy(step, self.bs.at[step], self.br.at[step], self.left)

    def across(self, shift):
        number = 0 if shift == 0 else 2 * abs(shift) - (1 if shift < 0 else 0)
        return self.copy(shift, self.cs.at[number], self.cr.at[number], self.mate)

    def own(self):
        return pltpu.make_async_copy(self.x_ref, self.slot(self.me), self.own_sem)

    def greet(self):
        self.locate()
        barrier = pltpu.get_barrier_semaphore()
        for other in (self.right, self.left, self.mate):
            pl.semaphore_signal(
                barrier, inc=1, device_id=(other, self.group), device_id_type=MESH
            )
        pl.semaphore_wait(barrier, 3)

    def begin(self):
        self.locate()
        self.fore(0).start()
        self.back(0).start()
        self.across(0).start()
        self.own().start()

    def hop(self, step):
        self.locate()
        self.fore(step - 1).wait_recv()
        if step < self.ahead:
            self.fore(step).start()
        self.across(-step).start()
        if step <= self.behind:
            self.back(step - 1).wait_recv()
            if step < self.behind:
                self.back(step).start()
            self.across(step).start()

    def finish(self):
        self.locate()
        self.own().wait()
        for step in range(self.ahead):
            self.fore(step).wait_send()
        for step in range(self.behind):
            self.back(step).wait_send()
        for shift in range(-self.ahead, self.behind + 1):
            self.across(shift).wait()


def gather_sems(devices):
    dma = pltpu.SemaphoreType.DMA
    return [dma((devices // 2,))] * 6 + [dma(())]


def gather_shape(shard, devices):
    return jax.ShapeDtypeStruct((shard.shape[0] * devices, shard.shape[1]), shard.dtype)


def gather_kernel(devices, count, *refs):
    shards, outs, sems = refs[:count], refs[count : 2 * count], refs[2 * count :]
    each = len(sems) // count
    rings = [
        RingGather(devices, shards[i], outs[i], sems[i * each : (i + 1) * each])
        for i in range(count)
    ]
    rings[0].greet()
    for ring in rings:
        ring.begin()
    for step in range(1, rings[0].ahead + 1):
        for ring in rings:
            ring.hop(step)
    for ring in rings:
        ring.finish()


def cost(micros):
    return pl.CostEstimate(flops=int(micros * 1e9), bytes_accessed=0, transcendentals=0)


def gather_rows(shards, devices, collective):
    count = len(shards)
    anywhere = pl.BlockSpec(memory_space=pl.ANY)
    return pl.pallas_call(
        functools.partial(gather_kernel, devices, count),
        out_shape=tuple(gather_shape(shard, devices) for shard in shards),
        in_specs=[anywhere] * count,
        out_specs=(anywhere,) * count,
        scratch_shapes=gather_sems(devices) * count,
        compiler_params=pltpu.CompilerParams(collective_id=collective, has_side_effects=True),
        cost_estimate=cost(3),
        name="gather_rows",
    )(*shards)


def scatter_order(chips):
    ahead = chips // 2
    behind = chips - 1 - ahead
    order = []
    for step in range(ahead):
        order.append(-(ahead - step))
        if step < behind:
            order.append(behind - step)
    order.append(0)
    return order


class RingScatter:
    def __init__(self, devices, pieces, grads, outs, scratch):
        self.chips = devices // 2
        self.ahead = self.chips // 2
        self.behind = self.chips - 1 - self.ahead
        self.order = scatter_order(self.chips)
        self.pieces, self.grads, self.outs = pieces, grads, outs
        count = len(grads)
        self.mine, self.boxes, rest = scratch[:count], scratch[count : 2 * count], scratch[2 * count :]
        self.fbox, self.bbox, self.fout, self.bout = rest[:4]
        self.os, self.ms, self.mr, self.fs, self.fr, self.bs, self.br = rest[4:]
        self.rows = self.mine[0].shape[1]
        widths = [item.shape[2] for item in self.mine]
        self.cols = [slice(sum(widths[:i]), sum(widths[: i + 1])) for i in range(count)]

    def locate(self):
        me = lax.axis_index("dp")
        self.group = lax.axis_index("tensor")
        self.core = lax.rem(me, 2)
        chip = lax.div(me, 2)
        self.place = ring_place(chip, self.chips)
        self.right = ring_chip(self.place + 1, self.chips) * 2 + self.core
        self.left = ring_chip(self.place - 1, self.chips) * 2 + self.core
        self.mate = chip * 2 + (1 - self.core)

    def greet(self):
        self.locate()
        barrier = pltpu.get_barrier_semaphore()
        for other in (self.right, self.left, self.mate):
            pl.semaphore_signal(
                barrier, inc=1, device_id=(other, self.group), device_id_type=MESH
            )
        pl.semaphore_wait(barrier, 3)

    def block(self, i, shift, which):
        index = ring_chip(self.place + shift, self.chips) * 2 + which
        return self.grads[i].at[pl.ds(pl.multiple_of(index * self.rows, self.rows), self.rows), :]

    def remote(self, source, target_ref, ssem, rsem, target):
        return pltpu.make_async_remote_copy(
            src_ref=source,
            dst_ref=target_ref,
            send_sem=ssem,
            recv_sem=rsem,
            device_id=(target, self.group),
            device_id_type=MESH,
        )

    def across(self, i, slot):
        return self.remote(
            self.block(i, self.order[slot], 1 - self.core),
            self.boxes[i].at[slot],
            self.ms.at[i, slot],
            self.mr.at[i, slot],
            self.mate,
        )

    def own(self, i, slot):
        return pltpu.make_async_copy(
            self.block(i, self.order[slot], self.core), self.mine[i].at[slot], self.os.at[i, slot]
        )

    def fore(self, step):
        return self.remote(
            self.fout.at[step], self.fbox.at[step], self.fs.at[step], self.fr.at[step], self.right
        )

    def back(self, step):
        return self.remote(
            self.bout.at[step], self.bbox.at[step], self.bs.at[step], self.br.at[step], self.left
        )

    def begin(self):
        self.locate()
        for slot in range(self.chips):
            for i in range(len(self.grads)):
                self.across(i, slot).start()
                self.own(i, slot).start()

    def local_sum(self, i, slot, cols, others):
        total = self.mine[i][slot, :, cols].astype(F32) + self.boxes[i][slot, :, cols].astype(F32)
        whole = slice(self.cols[i].start + cols.start, self.cols[i].start + cols.stop)
        for ref in others:
            total = total + ref[:, whole].astype(F32)
        return total

    def arrive(self, slot):
        for i in range(len(self.grads)):
            self.own(i, slot).wait()
            self.across(i, slot).wait_recv()

    def put(self, target, shift, others):
        slot = self.order.index(shift)
        self.arrive(slot)
        for i, cols in enumerate(self.cols):
            total = self.local_sum(i, slot, slice(0, cols.stop - cols.start), others)
            target[:, cols] = total.astype(BF16)

    def hop(self, step):
        self.locate()
        if step > 0:
            self.back(step - 1).wait_recv()
        self.put(
            self.bout.at[step], -(self.ahead - step), [self.bbox.at[step - 1]] if step else []
        )
        self.back(step).start()
        if step < self.behind:
            if step > 0:
                self.fore(step - 1).wait_recv()
            self.put(
                self.fout.at[step], self.behind - step, [self.fbox.at[step - 1]] if step else []
            )
            self.fore(step).start()

    def finish(self):
        self.locate()
        slot = self.order.index(0)
        self.arrive(slot)
        self.fore(self.behind - 1).wait_recv()
        self.back(self.ahead - 1).wait_recv()
        others = [self.fbox.at[self.behind - 1], self.bbox.at[self.ahead - 1]]
        for out, (i, first, last) in zip(self.outs, self.pieces):
            out[...] = self.local_sum(i, slot, slice(first, last), others)
        for step in range(self.ahead):
            self.back(step).wait_send()
        for step in range(self.behind):
            self.fore(step).wait_send()
        for slot in range(self.chips):
            for i in range(len(self.grads)):
                self.across(i, slot).wait_send()


def scatter_scratch(grads, devices):
    chips = devices // 2
    rows = grads[0].shape[0] // devices
    count = len(grads)
    dma = pltpu.SemaphoreType.DMA
    boxes = [pltpu.VMEM((chips, rows, item.shape[1]), BF16) for item in grads]
    box = pltpu.VMEM((chips // 2, rows, sum(item.shape[1] for item in grads)), BF16)
    return boxes * 2 + [box] * 4 + [dma((count, chips))] * 3 + [dma((chips,))] * 4


def scatter_shapes(grads, pieces, devices):
    rows = grads[0].shape[0] // devices
    return tuple(jax.ShapeDtypeStruct((rows, last - first), F32) for i, first, last in pieces)


class Total:
    def __init__(self, devices, x_ref, o_ref, scratch):
        self.chips = devices // 2
        self.x_ref, self.o_ref = x_ref, o_ref
        self.mate_box, self.joined, self.boxes, self.ms, self.mr, self.ss, self.sr = scratch
        me = lax.axis_index("dp")
        self.group = lax.axis_index("tensor")
        self.chip = lax.div(me, 2)
        core = lax.rem(me, 2)
        self.mate = self.chip * 2 + (1 - core)
        self.peers = [
            lax.rem(self.chip + shift, self.chips) * 2 + core for shift in range(self.chips)
        ]

    def greet(self):
        barrier = pltpu.get_barrier_semaphore()
        for other in [self.mate] + self.peers[1:]:
            pl.semaphore_signal(
                barrier, inc=1, device_id=(other, self.group), device_id_type=MESH
            )
        pl.semaphore_wait(barrier, self.chips)

    def remote(self, source, target_ref, ssem, rsem, target):
        return pltpu.make_async_remote_copy(
            src_ref=source,
            dst_ref=target_ref,
            send_sem=ssem,
            recv_sem=rsem,
            device_id=(target, self.group),
            device_id_type=MESH,
        )

    def begin(self):
        self.across = self.remote(self.x_ref, self.mate_box, self.ms, self.mr, self.mate)
        self.across.start()

    def spread(self):
        self.across.wait_recv()
        self.joined[...] = self.x_ref[...] + self.mate_box[...]
        self.copies = [
            self.remote(
                self.joined,
                self.boxes.at[self.chip],
                self.ss.at[shift],
                self.sr.at[shift],
                self.peers[shift],
            )
            for shift in range(1, self.chips)
        ]
        for copy in self.copies:
            copy.start()
        self.boxes[self.chip] = self.joined[...]

    def finish(self):
        for copy in self.copies:
            copy.wait_recv()
        result = self.boxes[0]
        for other in range(1, self.chips):
            result = result + self.boxes[other]
        self.o_ref[...] = result
        self.across.wait_send()
        for copy in self.copies:
            copy.wait_send()


def total_scratch(values, devices):
    chips = devices // 2
    dma = pltpu.SemaphoreType.DMA
    return [
        pltpu.VMEM(values.shape, F32),
        pltpu.VMEM(values.shape, F32),
        pltpu.VMEM((chips,) + values.shape, F32),
        dma(()),
        dma(()),
        dma((chips,)),
        dma((chips,)),
    ]


def scatter_kernel(devices, count, pieces, *refs):
    outs = len(pieces)
    ring = RingScatter(
        devices, pieces, refs[:count], refs[count : count + outs], refs[count + outs :]
    )
    ring.greet()
    ring.begin()
    for step in range(ring.ahead):
        ring.hop(step)
    ring.finish()


def scatter_rows(grads, pieces, devices, collective):
    count = len(grads)
    return pl.pallas_call(
        functools.partial(scatter_kernel, devices, count, pieces),
        out_shape=scatter_shapes(grads, pieces, devices),
        in_specs=[pl.BlockSpec(memory_space=pl.ANY)] * count,
        out_specs=(pl.BlockSpec(memory_space=pltpu.VMEM),) * len(pieces),
        scratch_shapes=scatter_scratch(grads, devices),
        compiler_params=pltpu.CompilerParams(collective_id=collective, has_side_effects=True),
        cost_estimate=cost(3),
        name="scatter_rows",
    )(*grads)


def last_kernel(devices, count, pieces, *refs):
    outs = len(pieces)
    grads, values, refs = refs[:count], refs[count], refs[count + 1 :]
    pieces_out, total_out, scratch = refs[:outs], refs[outs], refs[outs + 1 :]
    ring = RingScatter(devices, pieces, grads, pieces_out, scratch[:-7])
    total = Total(devices, values, total_out, scratch[-7:])
    total.greet()
    ring.begin()
    total.begin()
    for step in range(ring.ahead):
        ring.hop(step)
        if step == 0:
            total.spread()
    ring.finish()
    total.finish()


def scatter_last(grads, values, pieces, devices, collective):
    count = len(grads)
    vmem = pl.BlockSpec(memory_space=pltpu.VMEM)
    return pl.pallas_call(
        functools.partial(last_kernel, devices, count, pieces),
        out_shape=scatter_shapes(grads, pieces, devices)
        + (jax.ShapeDtypeStruct(values.shape, F32),),
        in_specs=[pl.BlockSpec(memory_space=pl.ANY)] * count + [vmem],
        out_specs=(vmem,) * (len(pieces) + 1),
        scratch_shapes=scatter_scratch(grads, devices) + total_scratch(values, devices),
        compiler_params=pltpu.CompilerParams(collective_id=collective, has_side_effects=True),
        cost_estimate=cost(3),
        name="scatter_last",
    )(*grads, values)


def head_spread(channels):
    return (iota((LANES, channels), 1) // MP == iota((LANES, channels), 0)).astype(BF16)


def parts(values, count):
    terms = []
    for _ in range(count):
        term = values.astype(BF16)
        terms.append(term)
        values = values - term.astype(F32)
    return terms


def pick(values, mask, count=2):
    return dot(jnp.concatenate(parts(values, count), axis=1), jnp.concatenate([mask] * count, axis=0))


def pick_left(mask, values, count):
    return dot(jnp.concatenate([mask] * count, axis=1), jnp.concatenate(parts(values, count), axis=0))


def gather_heads(values, spread):
    high, low = parts(values, 2)
    return dot(high, spread, NT) + dot(low, spread, NT)


def soft_step(raw):
    return jnp.maximum(raw, 0.0) + jnp.log1p(jnp.exp(-jnp.abs(raw)))


def conv_window(buffer, taps_ref, bias_ref, span):
    total = bias_ref[...] + taps_ref[0:1, :] * buffer[EDGE - 3 : EDGE - 3 + span, :]
    for tap in range(1, KCONV):
        start = EDGE - 3 + tap
        total = total + taps_ref[tap : tap + 1, :] * buffer[start : start + span, :]
    return total


def span_rates(step_ref, bias_ref, decay_ref, spread, span):
    raw = step_ref[...] + bias_ref[...]
    step = soft_step(raw)
    lower = (iota((span, span), 1) <= iota((span, span), 0)).astype(BF16)
    cum = pick_left(lower, step * decay_ref[...], 3)
    tails = jnp.exp(cum[span - 1 : span, :] - cum)
    wide = pick(jnp.concatenate([step, tails, jnp.exp(cum)], axis=0), spread)
    return raw, step, cum, wide[:span], wide[span : 2 * span], wide[2 * span :]


def pair_split(values, low_lanes):
    zero = jnp.zeros_like(values)
    return jnp.concatenate(
        [jnp.where(low_lanes, values, zero), jnp.where(low_lanes, zero, values)], axis=0
    )


def pair_decay(cum, cum_rows, pair, causal):
    parts = []
    for head in (2 * pair, 2 * pair + 1):
        differ = cum[:, head : head + 1] - cum_rows[head : head + 1, :]
        parts.append(jnp.exp(jnp.where(causal, differ, MASKED)))
    return parts


def scan_forward(
    devices, spans,
    z_ref, x_ref, bc_ref, step_ref,
    tap_ref, bias_ref, tapb_ref, biasb_ref, stepb_ref, decay_ref, skip_ref, shard_ref,
    y_ref, gated_ref, enter_ref, all_ref,
    state, xbuf, bbuf, *sems,
):
    span, channels = x_ref.shape
    ring = RingGather(devices, shard_ref, all_ref, sems)
    turn = pl.program_id(0)

    @pl.when(turn == 0)
    def _():
        ring.greet()
        ring.begin()


    @pl.when(pl.program_id(0) == 0)
    def _():
        state[...] = jnp.zeros_like(state)
        xbuf[span:, :] = jnp.zeros((EDGE, channels), F32)
        bbuf[span:, :] = jnp.zeros((EDGE, 2 * NS), F32)

    xbuf[:EDGE, :] = xbuf[span:, :]
    bbuf[:EDGE, :] = bbuf[span:, :]
    xbuf[EDGE:, :] = x_ref[...]
    bbuf[EDGE:, :] = bc_ref[...]
    inputs = jax.nn.silu(conv_window(xbuf, tap_ref, bias_ref, span))
    shared = jax.nn.silu(conv_window(bbuf, tapb_ref, biasb_ref, span))
    spread = head_spread(channels)
    raw, step, cum, step_w, tails_w, grown_w = span_rates(
        step_ref, stepb_ref, decay_ref, spread, span
    )
    cum_rows = cum.T
    b_low = shared[:, :NS].astype(BF16)
    c_low = shared[:, NS:].astype(BF16)
    scaled = inputs * step_w
    scaled_low = scaled.astype(BF16)
    enter_ref[0] = state[...]
    outer = dot(c_low, state[...].astype(BF16)) * grown_w
    fresh = dot(b_low, (scaled * tails_w).astype(BF16), TN)
    state[...] = state[...] * grown_w[span - 1 : span, :] + fresh
    cross = dot(c_low, b_low, NT)
    causal = iota((span, span), 1) <= iota((span, span), 0)
    low_lanes = iota((span, LANES), 1) < MP
    for pair in range(channels // LANES):
        lanes = slice(pair * LANES, (pair + 1) * LANES)
        first, second = pair_decay(cum, cum_rows, pair, causal)
        weights = jnp.concatenate(
            [(cross * first).astype(BF16), (cross * second).astype(BF16)], axis=1
        )
        y_ref[:, lanes] = dot(weights, pair_split(scaled_low[:, lanes], low_lanes))
    y = y_ref[...] + outer + skip_ref[...] * inputs
    y_ref[...] = y
    gated_ref[...] = y * jax.nn.silu(z_ref[...])

    count = spans
    for step in range(1, ring.ahead + 1):
        pl.when(turn == min(count - 1, count * step // ring.ahead))(
            functools.partial(ring.hop, step)
        )
    pl.when(turn == count - 1)(ring.finish)


def scan_backward(
    devices, spans, pieces, count,
    z_ref, x_ref, xp_ref, bc_ref, bp_ref, step_ref, y_ref, enter_ref,
    dyg_ref, scale_ref, inner_ref, dqkv_ref,
    tap_ref, bias_ref, tapb_ref, biasb_ref, stepb_ref, decay_ref, skip_ref, gain_ref,
    *refs,
):
    sent, refs = refs[:count], refs[count:]
    (grad_ref, gx_ref, gb_ref, gh_ref), refs = refs[:4], refs[4:]
    outs, refs = refs[: len(pieces)], refs[len(pieces) :]
    (dstate, xbuf, bbuf, dxbuf, dbbuf, du_buf, col_buf), scratch = refs[:7], refs[7:]
    ring = RingScatter(devices, pieces, sent, outs, scratch)
    span, channels = x_ref.shape
    turn = pl.program_id(0)

    @pl.when(turn == 0)
    def _():
        ring.greet()
        ring.begin()
        dstate[...] = jnp.zeros_like(dstate)
        dxbuf[...] = jnp.zeros_like(dxbuf)
        dbbuf[...] = jnp.zeros_like(dbbuf)
        col_buf[...] = jnp.zeros_like(col_buf)
        gx_ref[...] = jnp.zeros_like(gx_ref)
        gb_ref[...] = jnp.zeros_like(gb_ref)
        gh_ref[...] = jnp.zeros_like(gh_ref)

    inside = (turn < spans - 1).astype(F32)
    xbuf[:EDGE, :] = xp_ref[...] * inside
    bbuf[:EDGE, :] = bp_ref[...] * inside
    xbuf[EDGE:, :] = x_ref[...]
    bbuf[EDGE:, :] = bc_ref[...]
    conv = conv_window(xbuf, tap_ref, bias_ref, span)
    sig = jax.nn.sigmoid(conv)
    inputs = conv * sig
    convb = conv_window(bbuf, tapb_ref, biasb_ref, span)
    sigb = jax.nn.sigmoid(convb)
    shared = convb * sigb
    b_low = shared[:, :NS].astype(BF16)
    c_low = shared[:, NS:].astype(BF16)
    spread = head_spread(channels)
    raw, step, cum, step_w, tails_w, grown_w = span_rates(
        step_ref, stepb_ref, decay_ref, spread, span
    )
    cum_rows = cum.T
    scaled = inputs * step_w
    scaled_low = scaled.astype(BF16)

    z = z_ref[...]
    sig_z = jax.nn.sigmoid(z)
    swish = z * sig_z
    y = y_ref[...]
    normed = y * swish * scale_ref[...]
    dyg = dyg_ref[...]
    gain_grad = jnp.sum(dyg * normed, axis=0, keepdims=True)
    dgated = scale_ref[...] * (dyg * gain_ref[...] - normed * inner_ref[...])
    dy = dgated * swish
    grad_ref[:, :channels] = (dgated * y * (sig_z * (1.0 + z * (1.0 - sig_z)))).astype(BF16)

    state_low = enter_ref[0].astype(BF16)
    dstate_low = dstate[...].astype(BF16)
    grown_low = (dy * grown_w).astype(BF16)
    dy_low = dy.astype(BF16)
    tailed = scaled * tails_w
    outer = dot(c_low, state_low) * grown_w
    from_state = dot(b_low, dstate_low)
    dc = dot(grown_low, state_low, NT)
    db = dot(tailed.astype(BF16), dstate_low, NT)
    leak = from_state * tailed
    last_w = grown_w[span - 1 : span, :]
    ends = (
        jnp.sum(leak, axis=0, keepdims=True)
        + jnp.sum(enter_ref[0] * dstate[...], axis=0, keepdims=True) * last_w
    )
    skips = jnp.sum(dy * inputs, axis=0, keepdims=True)
    dstate[...] = dstate[...] * last_w + dot(c_low, grown_low, TN)

    cross = dot(c_low, b_low, NT)
    causal = iota((span, span), 1) <= iota((span, span), 0)
    low_lanes = iota((span, LANES), 1) < MP
    lane = iota((span, LANES), 1)
    dcross = jnp.zeros((span, span), F32)
    row_part = jnp.zeros((span, LANES), F32)
    for pair in range(channels // LANES):
        lanes = slice(pair * LANES, (pair + 1) * LANES)
        decays = pair_decay(cum, cum_rows, pair, causal)
        dy_pair = pair_split(dy_low[:, lanes], low_lanes)
        dweights = dot(dy_pair, scaled_low[:, lanes], NT)
        both = []
        for part in range(2):
            head = 2 * pair + part
            dterm = dweights[part * span : (part + 1) * span] * decays[part]
            dcross = dcross + dterm
            flow = dterm * cross
            row_part = row_part + jnp.where(
                lane == head, jnp.sum(flow, axis=1, keepdims=True), 0.0
            )
            col_buf[head : head + 1, :] = jnp.sum(flow, axis=0, keepdims=True)
            both.append((cross * decays[part]).astype(BF16))
        du_buf[:, lanes] = dot(jnp.concatenate(both, axis=0), dy_pair, TN)
    du = du_buf[...] + from_state * tails_w
    dcross_low = dcross.astype(BF16)
    dc = dc + dot(dcross_low, b_low)
    db = db + dot(dcross_low, c_low, TN)

    sums = gather_heads(
        jnp.concatenate(
            [dy * outer - leak, du * inputs, ends, skips, jnp.zeros((EDGE - 2, channels), F32)],
            axis=0,
        ),
        spread,
    )
    at_end = sums[2 * span : 2 * span + 1, :]
    dcum = sums[:span] + row_part - col_buf[...].T
    upper = (iota((span, span), 1) >= iota((span, span), 0)).astype(BF16)
    drate = pick_left(upper, dcum, 3) + at_end
    dstep = drate * decay_ref[...] + sums[span : 2 * span]
    draw = dstep * jax.nn.sigmoid(raw)
    gh_ref[0:1, :] += jnp.sum(draw, axis=0, keepdims=True)
    gh_ref[1:2, :] += jnp.sum(drate * step, axis=0, keepdims=True) * decay_ref[...]
    gh_ref[2:3, :] += sums[2 * span + 1 : 2 * span + 2, :]

    dinputs = du * step_w + skip_ref[...] * dy
    dxbuf[span:, :] = dxbuf[:EDGE, :]
    dbbuf[span:, :] = dbbuf[:EDGE, :]
    dconv = dinputs * (sig * (1.0 + conv * (1.0 - sig)))
    dconvb = jnp.concatenate([db, dc], axis=1) * (sigb * (1.0 + convb * (1.0 - sigb)))
    dxbuf[:span, :] = dconv
    dbbuf[:span, :] = dconvb
    dx = jnp.zeros_like(dconv)
    dbc = jnp.zeros_like(dconvb)
    for tap in range(KCONV):
        back = KCONV - 1 - tap
        start = EDGE - 3 + tap
        dx = dx + tap_ref[tap : tap + 1, :] * dxbuf[back : back + span, :]
        dbc = dbc + tapb_ref[tap : tap + 1, :] * dbbuf[back : back + span, :]
        gx_ref[tap : tap + 1, :] += jnp.sum(
            dconv * xbuf[start : start + span, :], axis=0, keepdims=True
        )
        gb_ref[tap : tap + 1, :] += jnp.sum(
            dconvb * bbuf[start : start + span, :], axis=0, keepdims=True
        )
    gx_ref[KCONV : KCONV + 1, :] += jnp.sum(dconv, axis=0, keepdims=True)
    gb_ref[KCONV : KCONV + 1, :] += jnp.sum(dconvb, axis=0, keepdims=True)
    gx_ref[KCONV + 1 : KCONV + 2, :] += gain_grad
    width = 2 * channels + 2 * NS
    grad_ref[:, channels : 2 * channels] = dx.astype(BF16)
    grad_ref[:, 2 * channels : width] = dbc.astype(BF16)
    grad_ref[:, width : width + dqkv_ref.shape[1]] = dqkv_ref[...]
    grad_ref[:, width + dqkv_ref.shape[1] :] = draw.astype(BF16)
    for step in range(ring.ahead):
        pl.when(turn == spans * step // ring.ahead)(functools.partial(ring.hop, step))
    pl.when(turn == spans - 1)(ring.finish)


def scan_params(conv_x, conv_xb, conv_bc, conv_bcb, dt_bias, a_log, d_skip):
    heads = dt_bias.shape[0]

    def wide(row):
        return jnp.pad(row, (0, LANES - heads))[None, :]

    f32 = lambda value: value.astype(F32)
    return (
        f32(conv_x),
        f32(conv_xb)[None, :],
        f32(conv_bc),
        f32(conv_bcb)[None, :],
        wide(f32(dt_bias)),
        wide(-jnp.exp(f32(a_log))),
        jnp.repeat(f32(d_skip), MP)[None, :],
    )


def whole_spec(array):
    return pl.BlockSpec(array.shape, lambda turn: (0,) * array.ndim)


def run_scan_forward(proj, qkv_width, params, shard, devices):
    tokens = proj.shape[0]
    channels = params[1].shape[1]
    step_at = (2 * channels + 2 * NS + qkv_width) // LANES
    spans = tokens // SPAN
    bc_at = 2 * channels // (2 * NS)
    rows = lambda width, at: pl.BlockSpec((SPAN, width), lambda turn: (turn, at))
    anywhere = pl.BlockSpec(memory_space=pl.ANY)
    return pl.pallas_call(
        functools.partial(scan_forward, devices, spans),
        grid=(spans,),
        out_shape=(
            jax.ShapeDtypeStruct((tokens, channels), F32),
            jax.ShapeDtypeStruct((tokens, channels), F32),
            jax.ShapeDtypeStruct((spans, NS, channels), F32),
            gather_shape(shard, devices),
        ),
        in_specs=[rows(channels, 0), rows(channels, 1), rows(2 * NS, bc_at), rows(LANES, step_at)]
        + [whole_spec(item) for item in params]
        + [anywhere],
        out_specs=(
            rows(channels, 0),
            rows(channels, 0),
            pl.BlockSpec((1, NS, channels), lambda turn: (turn, 0, 0)),
            anywhere,
        ),
        scratch_shapes=[
            pltpu.VMEM((NS, channels), F32),
            pltpu.VMEM((SPAN + EDGE, channels), F32),
            pltpu.VMEM((SPAN + EDGE, 2 * NS), F32),
        ]
        + gather_sems(devices),
        compiler_params=pltpu.CompilerParams(collective_id=2, has_side_effects=True),
        cost_estimate=cost(20),
        name="scan_forward",
    )(proj, proj, proj, proj, *params, shard)


def run_scan_backward(
    proj, y, entering, dyg, scale, inner, dqkv, params, gain, sent, pieces, devices
):
    tokens, width = proj.shape
    channels = params[1].shape[1]
    qkv_width = dqkv.shape[1]
    step_at = (2 * channels + 2 * NS + qkv_width) // LANES
    spans = tokens // SPAN
    bc_at = 2 * channels // (2 * NS)
    edges = SPAN // EDGE
    rows = lambda size, at: pl.BlockSpec((SPAN, size), lambda turn: (spans - 1 - turn, at))
    edge = lambda size, at: pl.BlockSpec(
        (EDGE, size), lambda turn: (jnp.maximum((spans - 1 - turn) * edges - 1, 0), at)
    )
    keep = lambda shape: pl.BlockSpec(shape, lambda turn: (0, 0))
    shapes = scatter_shapes(sent, pieces, devices)
    return pl.pallas_call(
        functools.partial(scan_backward, devices, spans, pieces, len(sent)),
        grid=(spans,),
        out_shape=(
            jax.ShapeDtypeStruct((tokens, width), BF16),
            jax.ShapeDtypeStruct((EDGE, channels), F32),
            jax.ShapeDtypeStruct((EDGE, 2 * NS), F32),
            jax.ShapeDtypeStruct((EDGE, LANES), F32),
        )
        + shapes,
        in_specs=[
            rows(channels, 0),
            rows(channels, 1),
            edge(channels, 1),
            rows(2 * NS, bc_at),
            edge(2 * NS, bc_at),
            rows(LANES, step_at),
            rows(channels, 0),
            pl.BlockSpec((1, NS, channels), lambda turn: (spans - 1 - turn, 0, 0)),
            rows(channels, 0),
            rows(1, 0),
            rows(1, 0),
            rows(qkv_width, 0),
        ]
        + [whole_spec(item) for item in params]
        + [whole_spec(gain)]
        + [pl.BlockSpec(memory_space=pl.ANY)] * len(sent),
        out_specs=(
            rows(width, 0),
            keep((EDGE, channels)),
            keep((EDGE, 2 * NS)),
            keep((EDGE, LANES)),
        )
        + tuple(keep(item.shape) for item in shapes),
        scratch_shapes=[
            pltpu.VMEM((NS, channels), F32),
            pltpu.VMEM((SPAN + EDGE, channels), F32),
            pltpu.VMEM((SPAN + EDGE, 2 * NS), F32),
            pltpu.VMEM((SPAN + EDGE, channels), F32),
            pltpu.VMEM((SPAN + EDGE, 2 * NS), F32),
            pltpu.VMEM((SPAN, channels), F32),
            pltpu.VMEM((LANES, SPAN), F32),
        ]
        + scatter_scratch(sent, devices),
        compiler_params=pltpu.CompilerParams(collective_id=6, has_side_effects=True),
        cost_estimate=cost(47),
        name="scan_backward",
    )(
        proj, proj, proj, proj, proj, proj, y, entering, dyg, scale, inner, dqkv, *params, gain,
        *sent,
    )


def rotary_tables(tokens):
    half = HEAD_SIZE // 2
    exponent = np.arange(half, dtype=np.float64) * (-2.0 * LOG_BASE / HEAD_SIZE)
    rates = np.tile(np.exp(exponent.astype(np.float32)).astype(np.float64), LANES // half)
    tables = []
    for places in (np.arange(FINE), np.arange(0, tokens, FINE)):
        angles = places[:, None] * rates[None, :]
        tables += [np.cos(angles).astype(np.float32), np.sin(angles).astype(np.float32)]
    return tables


def fill_rotary(fine_cos, fine_sin, coarse_cos, coarse_sin, cosine, sine, direction):
    half = HEAD_SIZE // 2
    sign = jnp.where(iota((FINE, LANES), 1) % HEAD_SIZE < half, -direction, direction)
    small_cos, small_sin = fine_cos[...], fine_sin[...]
    for turn in range(coarse_cos.shape[0]):
        big_cos, big_sin = coarse_cos[turn : turn + 1, :], coarse_sin[turn : turn + 1, :]
        rows = slice(turn * FINE, (turn + 1) * FINE)
        cosine[rows, :] = small_cos * big_cos - small_sin * big_sin
        sine[rows, :] = (small_sin * big_cos + small_cos * big_sin) * sign


def rotate(values, cosine, sine):
    half = HEAD_SIZE // 2
    low = iota(values.shape, 1) % HEAD_SIZE < half
    turned = jnp.where(
        low, pltpu.roll(values, LANES - half, 1), pltpu.roll(values, half, 1)
    )
    return values * cosine + turned * sine


def attend_forward(
    q_ref, kv_ref, fine_cos, fine_sin, coarse_cos, coarse_sin,
    qkv_ref, lse_ref, o_ref, heads_q, heads_o, vt, cos_ref, sin_ref,
):
    fill_rotary(fine_cos, fine_sin, coarse_cos, coarse_sin, cos_ref, sin_ref, 1.0)
    tokens, query_width = q_ref.shape
    heads = query_width // HEAD_SIZE
    cosine, sine = cos_ref[...], sin_ref[...]
    for pair in range(heads // 2):
        lanes = slice(pair * LANES, (pair + 1) * LANES)
        turned = (rotate(q_ref[:, lanes], cosine, sine) * HEAD_SIZE**-0.5).astype(BF16)
        qkv_ref[:, lanes] = turned
        heads_q[2 * pair] = turned[:, :HEAD_SIZE]
        heads_q[2 * pair + 1] = turned[:, HEAD_SIZE:]
    kv = kv_ref[...]
    first = iota(kv.shape, 1) < HEAD_SIZE
    qkv_ref[:, query_width:] = jnp.where(first, rotate(kv, cosine, sine), kv).astype(BF16)
    vt[...] = kv[:, HEAD_SIZE:].T.astype(BF16)
    visible = iota((QBLK, QBLK), 0) <= iota((QBLK, QBLK), 1)
    for start in range(0, tokens, QBLK):
        limit = start + QBLK

        def one(head, carry):
            keys = qkv_ref[:limit, query_width : query_width + HEAD_SIZE]
            scores = dot(keys, heads_q[head, start:limit, :], NT)
            edge = jnp.where(visible, scores[start:], MASKED)
            top = jnp.max(edge, axis=0, keepdims=True)
            if start:
                top = jnp.maximum(top, jnp.max(scores[:start], axis=0, keepdims=True))
            probs = jnp.exp(edge - top)
            if start:
                probs = jnp.concatenate([jnp.exp(scores[:start] - top), probs], axis=0)
            total = jnp.sum(probs, axis=0, keepdims=True)
            out = dot(vt[:, :limit], probs.astype(BF16)) / total
            heads_o[head, start:limit, :] = out.T.astype(BF16)
            lse_ref[pl.ds(head, 1), start:limit] = top + jnp.log(total)
            return carry

        lax.fori_loop(0, heads, one, 0)
    for pair in range(heads // 2):
        o_ref[:, pair * LANES : (pair + 1) * LANES] = jnp.concatenate(
            [heads_o[2 * pair], heads_o[2 * pair + 1]], axis=1
        )


def attend_backward(
    qkv_ref, lse_ref, o_ref, do_ref, fine_cos, fine_sin, coarse_cos, coarse_sin, dqkv_ref,
    heads_q, heads_do, heads_dq, heads_sum, kt, dk, dv, cos_ref, sin_ref,
):
    fill_rotary(fine_cos, fine_sin, coarse_cos, coarse_sin, cos_ref, sin_ref, -1.0)
    tokens, query_width = o_ref.shape
    heads = query_width // HEAD_SIZE
    ones = jnp.ones((EDGE, HEAD_SIZE), F32)
    for head in range(heads):
        lanes = slice(head * HEAD_SIZE, (head + 1) * HEAD_SIZE)
        grad = do_ref[:, lanes]
        heads_q[head] = qkv_ref[:, lanes]
        heads_do[head] = grad
        both = grad.astype(F32) * o_ref[:, lanes].astype(F32)
        heads_sum[head : head + 1, :] = dot(ones, both, NT, HIGHEST)[:1]
    kt[...] = qkv_ref[:, query_width : query_width + HEAD_SIZE].astype(F32).T.astype(BF16)
    dk[...] = jnp.zeros_like(dk)
    dv[...] = jnp.zeros_like(dv)
    visible = iota((QBLK, QBLK), 0) <= iota((QBLK, QBLK), 1)
    for start in range(0, tokens, QBLK):
        limit = start + QBLK

        def one(head, carry):
            keys = qkv_ref[:limit, query_width : query_width + HEAD_SIZE]
            values = qkv_ref[:limit, query_width + HEAD_SIZE :]
            query = heads_q[head, start:limit, :]
            grad = heads_do[head, start:limit, :]
            scores = dot(keys, query, NT) - lse_ref[pl.ds(head, 1), start:limit]
            probs = jnp.exp(jnp.where(visible, scores[start:], MASKED))
            if start:
                probs = jnp.concatenate([jnp.exp(scores[:start]), probs], axis=0)
            dprobs = dot(values, grad, NT)
            dscores = (probs * (dprobs - heads_sum[pl.ds(head, 1), start:limit])).astype(BF16)
            dv[:limit, :] += dot(probs.astype(BF16), grad)
            dk[:limit, :] += dot(dscores, query)
            heads_dq[head, start:limit, :] = dot(kt[:, :limit], dscores).T
            return carry

        lax.fori_loop(0, heads, one, 0)
    cosine, sine = cos_ref[...], sin_ref[...]
    for pair in range(heads // 2):
        joined = jnp.concatenate([heads_dq[2 * pair], heads_dq[2 * pair + 1]], axis=1)
        dqkv_ref[:, pair * LANES : (pair + 1) * LANES] = (
            rotate(joined, cosine, sine) * HEAD_SIZE**-0.5
        ).astype(BF16)
    joined = jnp.concatenate([dk[...], dv[...]], axis=1)
    first = iota(joined.shape, 1) < HEAD_SIZE
    dqkv_ref[:, query_width:] = jnp.where(
        first, rotate(joined, cosine, sine), joined
    ).astype(BF16)


def run_attend_forward(proj, query_at, query_width, tables):
    tokens = proj.shape[0]
    heads = query_width // HEAD_SIZE
    cols = lambda size, at: pl.BlockSpec((tokens, size), lambda turn: (0, at // size))
    return pl.pallas_call(
        attend_forward,
        grid=(1,),
        out_shape=(
            jax.ShapeDtypeStruct((tokens, query_width + 2 * HEAD_SIZE), BF16),
            jax.ShapeDtypeStruct((EDGE, tokens), F32),
            jax.ShapeDtypeStruct((tokens, query_width), BF16),
        ),
        in_specs=[
            cols(query_width, query_at),
            cols(2 * HEAD_SIZE, query_at + query_width),
        ]
        + [whole_spec(table) for table in tables],
        out_specs=(
            cols(query_width + 2 * HEAD_SIZE, 0),
            pl.BlockSpec((EDGE, tokens), lambda turn: (0, 0)),
            cols(query_width, 0),
        ),
        scratch_shapes=[
            pltpu.VMEM((heads, tokens, HEAD_SIZE), BF16),
            pltpu.VMEM((heads, tokens, HEAD_SIZE), BF16),
            pltpu.VMEM((HEAD_SIZE, tokens), BF16),
            pltpu.VMEM((tokens, LANES), F32),
            pltpu.VMEM((tokens, LANES), F32),
        ],
        cost_estimate=cost(15),
        name="attend_forward",
    )(proj, proj, *tables)


def run_attend_backward(qkv, lse, attended, grad, tables):
    tokens, query_width = attended.shape
    heads = query_width // HEAD_SIZE
    vmem = pl.BlockSpec(memory_space=pltpu.VMEM)
    return pl.pallas_call(
        attend_backward,
        out_shape=jax.ShapeDtypeStruct((tokens, query_width + 2 * HEAD_SIZE), BF16),
        in_specs=[vmem] * 8,
        out_specs=vmem,
        scratch_shapes=[
            pltpu.VMEM((heads, tokens, HEAD_SIZE), BF16),
            pltpu.VMEM((heads, tokens, HEAD_SIZE), BF16),
            pltpu.VMEM((heads, tokens, HEAD_SIZE), F32),
            pltpu.VMEM((EDGE, tokens), F32),
            pltpu.VMEM((HEAD_SIZE, tokens), BF16),
            pltpu.VMEM((tokens, HEAD_SIZE), F32),
            pltpu.VMEM((tokens, HEAD_SIZE), F32),
            pltpu.VMEM((tokens, LANES), F32),
            pltpu.VMEM((tokens, LANES), F32),
        ],
        cost_estimate=cost(16),
        name="attend_backward",
    )(qkv, lse, attended, grad, *tables)


def swap(partial):
    return lax.ppermute(partial, "tensor", [(0, 1), (1, 0)])


def join(mine, other):
    return mine.astype(F32) + other.astype(F32)


def tensor_sum(partial):
    return join(partial, swap(partial))


def norm_back(normed, scale, gain, grad):
    weighted = grad * gain
    grad_input = scale * (weighted - normed * jnp.mean(weighted * normed, axis=-1, keepdims=True))
    return (grad_input, jnp.sum(grad * normed, axis=0))


def local(
    layer_input, w_norm1, w_zx, w_bc, w_dt, conv_x, conv_xb, conv_bc, conv_bcb, dt_bias, a_log,
    d_skip, w_mnorm, w_mout, query_key_value_weight, output_weight, w_norm2, w_gu, w_down,
    grad_output,
):
    devices = lax.axis_size("dp")
    tokens, width = layer_input.shape
    shard = w_zx.shape[0]
    channels = conv_xb.shape[0]
    heads = dt_bias.shape[0]
    qkv_width = query_key_value_weight.shape[2]
    units = w_down.shape[0]
    attn_width = output_weight.shape[1]
    tail = jnp.concatenate(
        [w_dt, w_norm1[:, None], w_norm2[:, None], jnp.zeros((shard, LANES - heads - 2), BF16)],
        axis=1,
    )
    mixer_in = jnp.concatenate(
        [w_zx.reshape(shard, -1), w_bc, query_key_value_weight.reshape(shard, -1), tail], axis=1
    )
    in_width = mixer_in.shape[1]
    (w_in,) = gather_rows([mixer_in], devices, 0)
    norm1 = w_in[:, in_width - LANES + heads].astype(F32)
    norm2 = w_in[:, in_width - LANES + heads + 1].astype(F32)

    source = layer_input.astype(F32)
    scale_one = lax.rsqrt(jnp.mean(source * source, axis=-1, keepdims=True) + EPSILON)
    normed_one = source * scale_one
    hidden_one = (normed_one * norm1).astype(BF16)
    proj = dot(hidden_one, w_in)
    params = scan_params(conv_x, conv_xb, conv_bc, conv_bcb, dt_bias, a_log, d_skip)
    out_shard = jnp.concatenate([w_mout.T, output_weight.reshape(attn_width, -1).T], axis=1)
    y, gated, entering, w_out = run_scan_forward(proj, qkv_width, params, out_shard, devices)
    channels_all = channels * lax.axis_size("tensor")
    square_sum = tensor_sum(jnp.sum(gated * gated, axis=-1))
    scale_m = lax.rsqrt(square_sum / channels_all + EPSILON)[:, None]
    tables = rotary_tables(tokens)
    qkv_at = 2 * channels + 2 * NS
    qkv, lse, attended = run_attend_forward(proj, qkv_at, attn_width, tables)
    gain_m = w_mnorm.astype(F32)
    mamba_low = (gated * scale_m * gain_m).astype(BF16)
    mixer_out = jnp.concatenate([mamba_low, attended], axis=1)
    mixed, gate_up_shard, down_shard = lax.optimization_barrier(
        (dot(mixer_out, w_out, NT).astype(BF16), w_gu.reshape(shard, -1), w_down.T)
    )
    other = swap(mixed)
    w_gate_up, w_down_t = gather_rows([gate_up_shard, down_shard], devices, 3)
    other, w_gate_up, w_down_t = lax.optimization_barrier((other, w_gate_up, w_down_t))
    after = source + join(mixed, other)
    scale_two = lax.rsqrt(jnp.mean(after * after, axis=-1, keepdims=True) + EPSILON)
    normed_two = after * scale_two
    hidden_two = (normed_two * norm2).astype(BF16)
    gate_up = dot(hidden_two, w_gate_up)
    gate = gate_up[:, :units]
    upward = gate_up[:, units:]
    sigma = jax.nn.sigmoid(gate)
    swish = gate * sigma
    activated = (swish * upward).astype(BF16)
    grad_act = dot(grad_output, w_down_t)
    grad_gate = grad_act * upward * sigma * (1.0 + gate * (1.0 - sigma))
    grad_up = grad_act * swish
    grad_gu_low = jnp.concatenate([grad_gate, grad_up], axis=1).astype(BF16)
    partial_two, grad_gu_low = lax.optimization_barrier(
        (dot(grad_gu_low, w_gate_up, NT).astype(BF16), grad_gu_low)
    )
    other = swap(partial_two)
    grad_gu = dot(hidden_two, grad_gu_low, TN).astype(BF16)
    grad_down = dot(grad_output, activated, TN).astype(BF16)
    (mine_gu,) = scatter_rows([grad_gu], [(0, 0, 2 * units)], devices, 1)
    ffn_part = dot(activated, w_down_t, NT).astype(BF16)
    other, mine_gu, grad_down, ffn_part = lax.optimization_barrier(
        (other, mine_gu, grad_down, ffn_part)
    )
    grad_hidden_two = join(partial_two, other)
    ffn_other = swap(ffn_part)
    grad_norm_in, grad_norm2 = norm_back(normed_two, scale_two, norm2, grad_hidden_two)
    grad_after = grad_output.astype(F32) + grad_norm_in
    grad_mix_low = grad_after.astype(BF16)
    grad_mixer = dot(grad_mix_low, w_out)
    grad_mamba = grad_mixer[:, :channels]
    normed_m = gated * scale_m
    inner_m = tensor_sum(jnp.sum(grad_mamba * gain_m * normed_m, axis=-1))[:, None] / channels_all
    dqkv = run_attend_backward(
        qkv, lse, attended, grad_mixer[:, channels:].astype(BF16), tables
    )
    grad_out = dot(grad_mix_low, mixer_out, TN).astype(BF16)
    pieces = [
        (0, 0, channels),
        (0, channels, channels + attn_width),
        (1, 0, units),
    ]
    grad_proj, small_x, small_b, small_h, mine_mout, mine_o, mine_down = run_scan_backward(
        proj, y, entering, grad_mamba, scale_m, inner_m, dqkv, params, gain_m[None, :],
        [grad_out, grad_down], pieces, devices,
    )
    ffn_other, grad_proj = lax.optimization_barrier((ffn_other, grad_proj))
    result = (after + join(ffn_part, ffn_other)).astype(BF16)
    partial_one, grad_proj = lax.optimization_barrier(
        (dot(grad_proj, w_in, NT).astype(BF16), grad_proj)
    )
    crossing = jnp.concatenate(
        [
            small_b[: KCONV + 1].reshape(-1, LANES),
            jnp.sum(partial_one.astype(F32) * normed_one, axis=0).reshape(-1, LANES),
        ],
        axis=0,
    )
    crossing = tensor_sum(crossing)
    partial_one, crossing = lax.optimization_barrier((partial_one, crossing))
    other = swap(partial_one)
    grad_in = dot(hidden_one, grad_proj, TN).astype(BF16)
    small = jnp.concatenate(
        [
            small_x[: KCONV + 2].reshape(-1, LANES),
            small_h[:3],
            crossing,
            grad_norm2.reshape(-1, LANES),
        ],
        axis=0,
    )
    small_rows = small.shape[0]
    small = jnp.pad(small, ((0, -small_rows % EDGE), (0, 0)))
    shared_at = 2 * channels
    step_at = qkv_at + qkv_width
    mine_zx, mine_bc, mine_qkv, mine_step, small = scatter_last(
        [grad_in],
        small,
        [
            (0, 0, shared_at),
            (0, shared_at, qkv_at),
            (0, qkv_at, step_at),
            (0, step_at, in_width),
        ],
        devices,
        5,
    )
    other, mine_bc = lax.optimization_barrier((other, mine_bc))
    grad_hidden_one = join(partial_one, other)
    weighted = grad_hidden_one * norm1
    grad_source = grad_after + scale_one * (
        weighted - normed_one * jnp.mean(weighted * normed_one, axis=-1, keepdims=True)
    )

    half = NS * 2 // lax.axis_size("tensor")
    shared_cols = tensor_sum(mine_bc)
    begin = lax.axis_index("tensor") * half
    grad_bc = lax.dynamic_slice_in_dim(shared_cols, begin, half, 1)
    small = small[:small_rows].reshape(-1)
    x_size = (KCONV + 2) * channels
    h_size = 3 * LANES
    b_size = (KCONV + 1) * 2 * NS
    total_x = small[:x_size].reshape(KCONV + 2, channels)
    total_h = small[x_size : x_size + h_size].reshape(3, LANES)
    total_b = small[x_size + h_size : x_size + h_size + b_size].reshape(KCONV + 1, 2 * NS)
    total_b = lax.dynamic_slice_in_dim(total_b, begin, half, 1)
    norms = small[x_size + h_size + b_size :].reshape(2, width)
    norms = lax.dynamic_slice_in_dim(norms, lax.axis_index("dp") * shard, shard, 1)
    return (
        result,
        grad_source,
        norms[0],
        mine_zx.reshape(w_zx.shape),
        grad_bc,
        mine_step[:, :heads],
        total_x[:KCONV],
        total_x[KCONV],
        total_b[:KCONV],
        total_b[KCONV],
        total_h[0, :heads],
        total_h[1, :heads],
        total_h[2, :heads],
        total_x[KCONV + 1],
        mine_mout.T,
        mine_qkv.reshape(query_key_value_weight.shape),
        mine_o.T.reshape(output_weight.shape),
        norms[1],
        mine_gu.reshape(w_gu.shape),
        mine_down.T,
    )


def solution(mesh):
    return jax.shard_map(
        local,
        mesh=mesh,
        in_specs=(
            P("dp", None),
            P("dp"),
            P("dp", None, "tensor"),
            P("dp", None),
            P("dp", "tensor"),
            P(None, "tensor"),
            P("tensor"),
            P(),
            P(),
            P("tensor"),
            P("tensor"),
            P("tensor"),
            P("tensor"),
            P("tensor", "dp"),
            P("dp", "tensor", None),
            P("tensor", None, "dp"),
            P("dp"),
            P("dp", None, "tensor"),
            P("tensor", "dp"),
            P("dp", None),
        ),
        out_specs=(
            P("dp", None),
            P("dp", None),
            P("dp"),
            P("dp", None, "tensor"),
            P("dp", "tensor"),
            P("dp", "tensor"),
            P(None, "tensor"),
            P("tensor"),
            P(None, "tensor"),
            P("tensor"),
            P("tensor"),
            P("tensor"),
            P("tensor"),
            P("tensor"),
            P("tensor", "dp"),
            P("dp", "tensor", None),
            P("tensor", None, "dp"),
            P("dp"),
            P("dp", None, "tensor"),
            P("tensor", "dp"),
        ),
        check_vma=False,
    )
```

```python
import functools
import math

import jax
import jax.numpy as jnp
import numpy as np
from jax import lax
from jax.experimental import pallas as pl
from jax.experimental.pallas import tpu as pltpu
from jax.sharding import PartitionSpec as P

HEAD_SIZE = 64
MP = 64
NS = 128
KCONV = 4
SPAN = 128
QBLK = 256
FINE = 32
TBLK = 256
UBLK = 256
LANES = 128
EDGE = 8

EPSILON = 1e-05
HIGHEST = lax.Precision.HIGHEST
LOG_BASE = math.log(100000000000.0)
MASKED = -1e30
MESH = pl.DeviceIdType.MESH
F32 = jnp.float32
BF16 = jnp.bfloat16

NN = ((1,), (0,))
NT = ((1,), (1,))
TN = ((0,), (0,))


def dot(left, right, dims=NN, precision=None):
    return lax.dot_general(
        left, right, (dims, ((), ())), preferred_element_type=F32, precision=precision
    )


def iota(shape, dim):
    return lax.broadcasted_iota(jnp.int32, shape, dim)


def ring_place(chip, chips):
    odd = lax.rem(chip, 2)
    half = lax.div(chip, 2)
    return (1 - odd) * half + odd * (chips - 1 - half)


def ring_chip(place, chips):
    place = lax.rem(place + 4 * chips, chips)
    back = lax.div(place, chips // 2)
    return (1 - back) * (2 * place) + back * (2 * (chips - 1 - place) + 1)


def ring_setup(chips):
    me = lax.axis_index("dp")
    group = lax.axis_index("tensor")
    chip = lax.div(me, 2)
    core = lax.rem(me, 2)
    place = ring_place(chip, chips)
    right = ring_chip(place + 1, chips) * 2 + core
    left = ring_chip(place - 1, chips) * 2 + core
    mate = chip * 2 + (1 - core)
    barrier = pltpu.get_barrier_semaphore()
    for other in (right, left, mate):
        pl.semaphore_signal(barrier, inc=1, device_id=(other, group), device_id_type=MESH)
    pl.semaphore_wait(barrier, 3)
    return me, group, core, place, right, left, mate


class RingGather:
    def __init__(self, devices, x_ref, o_ref, sems):
        self.chips = devices // 2
        self.ahead = self.chips // 2
        self.behind = self.chips - 1 - self.ahead
        self.x_ref, self.o_ref, self.rows = x_ref, o_ref, x_ref.shape[0]
        self.fs, self.fr, self.bs, self.br, self.cs, self.cr, self.own_sem = sems

    def locate(self):
        me = lax.axis_index("dp")
        self.group = lax.axis_index("tensor")
        self.core = lax.rem(me, 2)
        chip = lax.div(me, 2)
        self.place = ring_place(chip, self.chips)
        self.right = ring_chip(self.place + 1, self.chips) * 2 + self.core
        self.left = ring_chip(self.place - 1, self.chips) * 2 + self.core
        self.mate = chip * 2 + (1 - self.core)
        self.me = me

    def slot(self, index):
        return self.o_ref.at[pl.ds(pl.multiple_of(index * self.rows, self.rows), self.rows), :]

    def copy(self, shift, ssem, rsem, target):
        if shift == 0:
            index, source = self.me, self.x_ref
        else:
            index = ring_chip(self.place + shift, self.chips) * 2 + self.core
            source = self.slot(index)
        return pltpu.make_async_remote_copy(
            src_ref=source,
            dst_ref=self.slot(index),
            send_sem=ssem,
            recv_sem=rsem,
            device_id=(target, self.group),
            device_id_type=MESH,
        )

    def fore(self, step):
        return self.copy(-step, self.fs.at[step], self.fr.at[step], self.right)

    def back(self, step):
        return self.copy(step, self.bs.at[step], self.br.at[step], self.left)

    def across(self, shift):
        number = 0 if shift == 0 else 2 * abs(shift) - (1 if shift < 0 else 0)
        return self.copy(shift, self.cs.at[number], self.cr.at[number], self.mate)

    def own(self):
        return pltpu.make_async_copy(self.x_ref, self.slot(self.me), self.own_sem)

    def greet(self):
        self.locate()
        barrier = pltpu.get_barrier_semaphore()
        for other in (self.right, self.left, self.mate):
            pl.semaphore_signal(
                barrier, inc=1, device_id=(other, self.group), device_id_type=MESH
            )
        pl.semaphore_wait(barrier, 3)

    def begin(self):
        self.locate()
        self.fore(0).start()
        self.back(0).start()
        self.across(0).start()
        self.own().start()

    def hop(self, step):
        self.locate()
        self.fore(step - 1).wait_recv()
        if step < self.ahead:
            self.fore(step).start()
        self.across(-step).start()
        if step <= self.behind:
            self.back(step - 1).wait_recv()
            if step < self.behind:
                self.back(step).start()
            self.across(step).start()

    def finish(self):
        self.locate()
        self.own().wait()
        for step in range(self.ahead):
            self.fore(step).wait_send()
        for step in range(self.behind):
            self.back(step).wait_send()
        for shift in range(-self.ahead, self.behind + 1):
            self.across(shift).wait()


def gather_sems(devices):
    dma = pltpu.SemaphoreType.DMA
    return [dma((devices // 2,))] * 6 + [dma(())]


def gather_shape(shard, devices):
    return jax.ShapeDtypeStruct((shard.shape[0] * devices, shard.shape[1]), shard.dtype)


def gather_kernel(devices, count, *refs):
    shards, outs, sems = refs[:count], refs[count : 2 * count], refs[2 * count :]
    each = len(sems) // count
    rings = [
        RingGather(devices, shards[i], outs[i], sems[i * each : (i + 1) * each])
        for i in range(count)
    ]
    rings[0].greet()
    for ring in rings:
        ring.begin()
    for step in range(1, rings[0].ahead + 1):
        for ring in rings:
            ring.hop(step)
    for ring in rings:
        ring.finish()


def cost(micros):
    return pl.CostEstimate(flops=int(micros * 1e9), bytes_accessed=0, transcendentals=0)


def gather_rows(shards, devices, collective):
    count = len(shards)
    anywhere = pl.BlockSpec(memory_space=pl.ANY)
    return pl.pallas_call(
        functools.partial(gather_kernel, devices, count),
        out_shape=tuple(gather_shape(shard, devices) for shard in shards),
        in_specs=[anywhere] * count,
        out_specs=(anywhere,) * count,
        scratch_shapes=gather_sems(devices) * count,
        compiler_params=pltpu.CompilerParams(collective_id=collective, has_side_effects=True),
        cost_estimate=cost(3),
        name="gather_rows",
    )(*shards)


def scatter_order(chips):
    ahead = chips // 2
    behind = chips - 1 - ahead
    order = []
    for step in range(ahead):
        order.append(-(ahead - step))
        if step < behind:
            order.append(behind - step)
    order.append(0)
    return order


class RingScatter:
    def __init__(self, devices, pieces, grads, outs, scratch):
        self.chips = devices // 2
        self.ahead = self.chips // 2
        self.behind = self.chips - 1 - self.ahead
        self.order = scatter_order(self.chips)
        self.pieces, self.grads, self.outs = pieces, grads, outs
        count = len(grads)
        self.mine, self.boxes, rest = scratch[:count], scratch[count : 2 * count], scratch[2 * count :]
        self.fbox, self.bbox, self.fout, self.bout = rest[:4]
        self.os, self.ms, self.mr, self.fs, self.fr, self.bs, self.br = rest[4:]
        self.rows = self.mine[0].shape[1]
        widths = [item.shape[2] for item in self.mine]
        self.cols = [slice(sum(widths[:i]), sum(widths[: i + 1])) for i in range(count)]

    def locate(self):
        me = lax.axis_index("dp")
        self.group = lax.axis_index("tensor")
        self.core = lax.rem(me, 2)
        chip = lax.div(me, 2)
        self.place = ring_place(chip, self.chips)
        self.right = ring_chip(self.place + 1, self.chips) * 2 + self.core
        self.left = ring_chip(self.place - 1, self.chips) * 2 + self.core
        self.mate = chip * 2 + (1 - self.core)

    def greet(self):
        self.locate()
        barrier = pltpu.get_barrier_semaphore()
        for other in (self.right, self.left, self.mate):
            pl.semaphore_signal(
                barrier, inc=1, device_id=(other, self.group), device_id_type=MESH
            )
        pl.semaphore_wait(barrier, 3)

    def block(self, i, shift, which):
        index = ring_chip(self.place + shift, self.chips) * 2 + which
        return self.grads[i].at[pl.ds(pl.multiple_of(index * self.rows, self.rows), self.rows), :]

    def remote(self, source, target_ref, ssem, rsem, target):
        return pltpu.make_async_remote_copy(
            src_ref=source,
            dst_ref=target_ref,
            send_sem=ssem,
            recv_sem=rsem,
            device_id=(target, self.group),
            device_id_type=MESH,
        )

    def across(self, i, slot):
        return self.remote(
            self.block(i, self.order[slot], 1 - self.core),
            self.boxes[i].at[slot],
            self.ms.at[i, slot],
            self.mr.at[i, slot],
            self.mate,
        )

    def own(self, i, slot):
        return pltpu.make_async_copy(
            self.block(i, self.order[slot], self.core), self.mine[i].at[slot], self.os.at[i, slot]
        )

    def fore(self, step):
        return self.remote(
            self.fout.at[step], self.fbox.at[step], self.fs.at[step], self.fr.at[step], self.right
        )

    def back(self, step):
        return self.remote(
            self.bout.at[step], self.bbox.at[step], self.bs.at[step], self.br.at[step], self.left
        )

    def begin(self):
        self.locate()
        for slot in range(self.chips):
            for i in range(len(self.grads)):
                self.across(i, slot).start()
                self.own(i, slot).start()

    def local_sum(self, i, slot, cols, others):
        total = self.mine[i][slot, :, cols].astype(F32) + self.boxes[i][slot, :, cols].astype(F32)
        whole = slice(self.cols[i].start + cols.start, self.cols[i].start + cols.stop)
        for ref in others:
            total = total + ref[:, whole].astype(F32)
        return total

    def arrive(self, slot):
        for i in range(len(self.grads)):
            self.own(i, slot).wait()
            self.across(i, slot).wait_recv()

    def put(self, target, shift, others):
        slot = self.order.index(shift)
        self.arrive(slot)
        for i, cols in enumerate(self.cols):
            total = self.local_sum(i, slot, slice(0, cols.stop - cols.start), others)
            target[:, cols] = total.astype(BF16)

    def hop(self, step):
        self.locate()
        if step > 0:
            self.back(step - 1).wait_recv()
        self.put(
            self.bout.at[step], -(self.ahead - step), [self.bbox.at[step - 1]] if step else []
        )
        self.back(step).start()
        if step < self.behind:
            if step > 0:
                self.fore(step - 1).wait_recv()
            self.put(
                self.fout.at[step], self.behind - step, [self.fbox.at[step - 1]] if step else []
            )
            self.fore(step).start()

    def finish(self):
        self.locate()
        slot = self.order.index(0)
        self.arrive(slot)
        self.fore(self.behind - 1).wait_recv()
        self.back(self.ahead - 1).wait_recv()
        others = [self.fbox.at[self.behind - 1], self.bbox.at[self.ahead - 1]]
        for out, (i, first, last) in zip(self.outs, self.pieces):
            out[...] = self.local_sum(i, slot, slice(first, last), others)
        for step in range(self.ahead):
            self.back(step).wait_send()
        for step in range(self.behind):
            self.fore(step).wait_send()
        for slot in range(self.chips):
            for i in range(len(self.grads)):
                self.across(i, slot).wait_send()


def scatter_scratch(grads, devices):
    chips = devices // 2
    rows = grads[0].shape[0] // devices
    count = len(grads)
    dma = pltpu.SemaphoreType.DMA
    boxes = [pltpu.VMEM((chips, rows, item.shape[1]), BF16) for item in grads]
    box = pltpu.VMEM((chips // 2, rows, sum(item.shape[1] for item in grads)), BF16)
    return boxes * 2 + [box] * 4 + [dma((count, chips))] * 3 + [dma((chips,))] * 4


def scatter_shapes(grads, pieces, devices):
    rows = grads[0].shape[0] // devices
    return tuple(jax.ShapeDtypeStruct((rows, last - first), F32) for i, first, last in pieces)


class Total:
    def __init__(self, devices, x_ref, o_ref, scratch):
        self.chips = devices // 2
        self.x_ref, self.o_ref = x_ref, o_ref
        self.mate_box, self.joined, self.boxes, self.ms, self.mr, self.ss, self.sr = scratch
        me = lax.axis_index("dp")
        self.group = lax.axis_index("tensor")
        self.chip = lax.div(me, 2)
        core = lax.rem(me, 2)
        self.mate = self.chip * 2 + (1 - core)
        self.peers = [
            lax.rem(self.chip + shift, self.chips) * 2 + core for shift in range(self.chips)
        ]

    def greet(self):
        barrier = pltpu.get_barrier_semaphore()
        for other in [self.mate] + self.peers[1:]:
            pl.semaphore_signal(
                barrier, inc=1, device_id=(other, self.group), device_id_type=MESH
            )
        pl.semaphore_wait(barrier, self.chips)

    def remote(self, source, target_ref, ssem, rsem, target):
        return pltpu.make_async_remote_copy(
            src_ref=source,
            dst_ref=target_ref,
            send_sem=ssem,
            recv_sem=rsem,
            device_id=(target, self.group),
            device_id_type=MESH,
        )

    def begin(self):
        self.across = self.remote(self.x_ref, self.mate_box, self.ms, self.mr, self.mate)
        self.across.start()

    def spread(self):
        self.across.wait_recv()
        self.joined[...] = self.x_ref[...] + self.mate_box[...]
        self.copies = [
            self.remote(
                self.joined,
                self.boxes.at[self.chip],
                self.ss.at[shift],
                self.sr.at[shift],
                self.peers[shift],
            )
            for shift in range(1, self.chips)
        ]
        for copy in self.copies:
            copy.start()
        self.boxes[self.chip] = self.joined[...]

    def finish(self):
        for copy in self.copies:
            copy.wait_recv()
        result = self.boxes[0]
        for other in range(1, self.chips):
            result = result + self.boxes[other]
        self.o_ref[...] = result
        self.across.wait_send()
        for copy in self.copies:
            copy.wait_send()


def total_scratch(values, devices):
    chips = devices // 2
    dma = pltpu.SemaphoreType.DMA
    return [
        pltpu.VMEM(values.shape, F32),
        pltpu.VMEM(values.shape, F32),
        pltpu.VMEM((chips,) + values.shape, F32),
        dma(()),
        dma(()),
        dma((chips,)),
        dma((chips,)),
    ]


def scatter_kernel(devices, count, pieces, *refs):
    outs = len(pieces)
    ring = RingScatter(
        devices, pieces, refs[:count], refs[count : count + outs], refs[count + outs :]
    )
    ring.greet()
    ring.begin()
    for step in range(ring.ahead):
        ring.hop(step)
    ring.finish()


def scatter_rows(grads, pieces, devices, collective):
    count = len(grads)
    return pl.pallas_call(
        functools.partial(scatter_kernel, devices, count, pieces),
        out_shape=scatter_shapes(grads, pieces, devices),
        in_specs=[pl.BlockSpec(memory_space=pl.ANY)] * count,
        out_specs=(pl.BlockSpec(memory_space=pltpu.VMEM),) * len(pieces),
        scratch_shapes=scatter_scratch(grads, devices),
        compiler_params=pltpu.CompilerParams(collective_id=collective, has_side_effects=True),
        cost_estimate=cost(3),
        name="scatter_rows",
    )(*grads)


def last_kernel(devices, count, pieces, *refs):
    outs = len(pieces)
    grads, values, refs = refs[:count], refs[count], refs[count + 1 :]
    pieces_out, total_out, scratch = refs[:outs], refs[outs], refs[outs + 1 :]
    ring = RingScatter(devices, pieces, grads, pieces_out, scratch[:-7])
    total = Total(devices, values, total_out, scratch[-7:])
    total.greet()
    ring.begin()
    total.begin()
    for step in range(ring.ahead):
        ring.hop(step)
        if step == 0:
            total.spread()
    ring.finish()
    total.finish()


def scatter_last(grads, values, pieces, devices, collective):
    count = len(grads)
    vmem = pl.BlockSpec(memory_space=pltpu.VMEM)
    return pl.pallas_call(
        functools.partial(last_kernel, devices, count, pieces),
        out_shape=scatter_shapes(grads, pieces, devices)
        + (jax.ShapeDtypeStruct(values.shape, F32),),
        in_specs=[pl.BlockSpec(memory_space=pl.ANY)] * count + [vmem],
        out_specs=(vmem,) * (len(pieces) + 1),
        scratch_shapes=scatter_scratch(grads, devices) + total_scratch(values, devices),
        compiler_params=pltpu.CompilerParams(collective_id=collective, has_side_effects=True),
        cost_estimate=cost(3),
        name="scatter_last",
    )(*grads, values)


def head_spread(channels):
    return (iota((LANES, channels), 1) // MP == iota((LANES, channels), 0)).astype(BF16)


def parts(values, count):
    terms = []
    for _ in range(count):
        term = values.astype(BF16)
        terms.append(term)
        values = values - term.astype(F32)
    return terms


def pick(values, mask, count=2):
    return dot(jnp.concatenate(parts(values, count), axis=1), jnp.concatenate([mask] * count, axis=0))


def pick_left(mask, values, count):
    return dot(jnp.concatenate([mask] * count, axis=1), jnp.concatenate(parts(values, count), axis=0))


def gather_heads(values, spread):
    high, low = parts(values, 2)
    return dot(high, spread, NT) + dot(low, spread, NT)


def soft_step(raw):
    return jnp.maximum(raw, 0.0) + jnp.log1p(jnp.exp(-jnp.abs(raw)))


def conv_window(buffer, taps_ref, bias_ref, span):
    total = bias_ref[...] + taps_ref[0:1, :] * buffer[EDGE - 3 : EDGE - 3 + span, :]
    for tap in range(1, KCONV):
        start = EDGE - 3 + tap
        total = total + taps_ref[tap : tap + 1, :] * buffer[start : start + span, :]
    return total


def span_rates(step_ref, bias_ref, decay_ref, spread, span):
    raw = step_ref[...] + bias_ref[...]
    step = soft_step(raw)
    lower = (iota((span, span), 1) <= iota((span, span), 0)).astype(BF16)
    cum = pick_left(lower, step * decay_ref[...], 3)
    tails = jnp.exp(cum[span - 1 : span, :] - cum)
    wide = pick(jnp.concatenate([step, tails, jnp.exp(cum)], axis=0), spread)
    return raw, step, cum, wide[:span], wide[span : 2 * span], wide[2 * span :]


def pair_split(values, low_lanes):
    zero = jnp.zeros_like(values)
    return jnp.concatenate(
        [jnp.where(low_lanes, values, zero), jnp.where(low_lanes, zero, values)], axis=0
    )


def pair_decay(cum, cum_rows, pair, causal):
    parts = []
    for head in (2 * pair, 2 * pair + 1):
        differ = cum[:, head : head + 1] - cum_rows[head : head + 1, :]
        parts.append(jnp.exp(jnp.where(causal, differ, MASKED)))
    return parts


def scan_forward(
    devices, spans,
    z_ref, x_ref, bc_ref, step_ref,
    tap_ref, bias_ref, tapb_ref, biasb_ref, stepb_ref, decay_ref, skip_ref, shard_ref,
    y_ref, gated_ref, enter_ref, all_ref,
    state, xbuf, bbuf, *sems,
):
    span, channels = x_ref.shape
    ring = RingGather(devices, shard_ref, all_ref, sems)
    turn = pl.program_id(0)

    @pl.when(turn == 0)
    def _():
        ring.greet()
        ring.begin()


    @pl.when(pl.program_id(0) == 0)
    def _():
        state[...] = jnp.zeros_like(state)
        xbuf[span:, :] = jnp.zeros((EDGE, channels), F32)
        bbuf[span:, :] = jnp.zeros((EDGE, 2 * NS), F32)

    xbuf[:EDGE, :] = xbuf[span:, :]
    bbuf[:EDGE, :] = bbuf[span:, :]
    xbuf[EDGE:, :] = x_ref[...]
    bbuf[EDGE:, :] = bc_ref[...]
    inputs = jax.nn.silu(conv_window(xbuf, tap_ref, bias_ref, span))
    shared = jax.nn.silu(conv_window(bbuf, tapb_ref, biasb_ref, span))
    spread = head_spread(channels)
    raw, step, cum, step_w, tails_w, grown_w = span_rates(
        step_ref, stepb_ref, decay_ref, spread, span
    )
    cum_rows = cum.T
    b_low = shared[:, :NS].astype(BF16)
    c_low = shared[:, NS:].astype(BF16)
    scaled = inputs * step_w
    scaled_low = scaled.astype(BF16)
    enter_ref[0] = state[...]
    outer = dot(c_low, state[...].astype(BF16)) * grown_w
    fresh = dot(b_low, (scaled * tails_w).astype(BF16), TN)
    state[...] = state[...] * grown_w[span - 1 : span, :] + fresh
    cross = dot(c_low, b_low, NT)
    causal = iota((span, span), 1) <= iota((span, span), 0)
    low_lanes = iota((span, LANES), 1) < MP
    for pair in range(channels // LANES):
        lanes = slice(pair * LANES, (pair + 1) * LANES)
        first, second = pair_decay(cum, cum_rows, pair, causal)
        weights = jnp.concatenate(
            [(cross * first).astype(BF16), (cross * second).astype(BF16)], axis=1
        )
        y_ref[:, lanes] = dot(weights, pair_split(scaled_low[:, lanes], low_lanes))
    y = y_ref[...] + outer + skip_ref[...] * inputs
    y_ref[...] = y
    gated_ref[...] = y * jax.nn.silu(z_ref[...])

    count = spans
    for step in range(1, ring.ahead + 1):
        pl.when(turn == min(count - 1, count * step // ring.ahead))(
            functools.partial(ring.hop, step)
        )
    pl.when(turn == count - 1)(ring.finish)


def scan_backward(
    devices, spans, pieces, count,
    z_ref, x_ref, xp_ref, bc_ref, bp_ref, step_ref, y_ref, enter_ref,
    dyg_ref, scale_ref, inner_ref, dqkv_ref,
    tap_ref, bias_ref, tapb_ref, biasb_ref, stepb_ref, decay_ref, skip_ref, gain_ref,
    *refs,
):
    sent, refs = refs[:count], refs[count:]
    (grad_ref, gx_ref, gb_ref, gh_ref), refs = refs[:4], refs[4:]
    outs, refs = refs[: len(pieces)], refs[len(pieces) :]
    (dstate, xbuf, bbuf, dxbuf, dbbuf, du_buf, col_buf), scratch = refs[:7], refs[7:]
    ring = RingScatter(devices, pieces, sent, outs, scratch)
    span, channels = x_ref.shape
    turn = pl.program_id(0)

    @pl.when(turn == 0)
    def _():
        ring.greet()
        ring.begin()
        dstate[...] = jnp.zeros_like(dstate)
        dxbuf[...] = jnp.zeros_like(dxbuf)
        dbbuf[...] = jnp.zeros_like(dbbuf)
        col_buf[...] = jnp.zeros_like(col_buf)
        gx_ref[...] = jnp.zeros_like(gx_ref)
        gb_ref[...] = jnp.zeros_like(gb_ref)
        gh_ref[...] = jnp.zeros_like(gh_ref)

    inside = (turn < spans - 1).astype(F32)
    xbuf[:EDGE, :] = xp_ref[...] * inside
    bbuf[:EDGE, :] = bp_ref[...] * inside
    xbuf[EDGE:, :] = x_ref[...]
    bbuf[EDGE:, :] = bc_ref[...]
    conv = conv_window(xbuf, tap_ref, bias_ref, span)
    sig = jax.nn.sigmoid(conv)
    inputs = conv * sig
    convb = conv_window(bbuf, tapb_ref, biasb_ref, span)
    sigb = jax.nn.sigmoid(convb)
    shared = convb * sigb
    b_low = shared[:, :NS].astype(BF16)
    c_low = shared[:, NS:].astype(BF16)
    spread = head_spread(channels)
    raw, step, cum, step_w, tails_w, grown_w = span_rates(
        step_ref, stepb_ref, decay_ref, spread, span
    )
    cum_rows = cum.T
    scaled = inputs * step_w
    scaled_low = scaled.astype(BF16)

    z = z_ref[...]
    sig_z = jax.nn.sigmoid(z)
    swish = z * sig_z
    y = y_ref[...]
    normed = y * swish * scale_ref[...]
    dyg = dyg_ref[...]
    gain_grad = jnp.sum(dyg * normed, axis=0, keepdims=True)
    dgated = scale_ref[...] * (dyg * gain_ref[...] - normed * inner_ref[...])
    dy = dgated * swish
    grad_ref[:, :channels] = (dgated * y * (sig_z * (1.0 + z * (1.0 - sig_z)))).astype(BF16)

    state_low = enter_ref[0].astype(BF16)
    dstate_low = dstate[...].astype(BF16)
    grown_low = (dy * grown_w).astype(BF16)
    dy_low = dy.astype(BF16)
    tailed = scaled * tails_w
    outer = dot(c_low, state_low) * grown_w
    from_state = dot(b_low, dstate_low)
    dc = dot(grown_low, state_low, NT)
    db = dot(tailed.astype(BF16), dstate_low, NT)
    leak = from_state * tailed
    last_w = grown_w[span - 1 : span, :]
    ends = (
        jnp.sum(leak, axis=0, keepdims=True)
        + jnp.sum(enter_ref[0] * dstate[...], axis=0, keepdims=True) * last_w
    )
    skips = jnp.sum(dy * inputs, axis=0, keepdims=True)
    dstate[...] = dstate[...] * last_w + dot(c_low, grown_low, TN)

    cross = dot(c_low, b_low, NT)
    causal = iota((span, span), 1) <= iota((span, span), 0)
    low_lanes = iota((span, LANES), 1) < MP
    lane = iota((span, LANES), 1)
    dcross = jnp.zeros((span, span), F32)
    row_part = jnp.zeros((span, LANES), F32)
    for pair in range(channels // LANES):
        lanes = slice(pair * LANES, (pair + 1) * LANES)
        decays = pair_decay(cum, cum_rows, pair, causal)
        dy_pair = pair_split(dy_low[:, lanes], low_lanes)
        dweights = dot(dy_pair, scaled_low[:, lanes], NT)
        both = []
        for part in range(2):
            head = 2 * pair + part
            dterm = dweights[part * span : (part + 1) * span] * decays[part]
            dcross = dcross + dterm
            flow = dterm * cross
            row_part = row_part + jnp.where(
                lane == head, jnp.sum(flow, axis=1, keepdims=True), 0.0
            )
            col_buf[head : head + 1, :] = jnp.sum(flow, axis=0, keepdims=True)
            both.append((cross * decays[part]).astype(BF16))
        du_buf[:, lanes] = dot(jnp.concatenate(both, axis=0), dy_pair, TN)
    du = du_buf[...] + from_state * tails_w
    dcross_low = dcross.astype(BF16)
    dc = dc + dot(dcross_low, b_low)
    db = db + dot(dcross_low, c_low, TN)

    sums = gather_heads(
        jnp.concatenate(
            [dy * outer - leak, du * inputs, ends, skips, jnp.zeros((EDGE - 2, channels), F32)],
            axis=0,
        ),
        spread,
    )
    at_end = sums[2 * span : 2 * span + 1, :]
    dcum = sums[:span] + row_part - col_buf[...].T
    upper = (iota((span, span), 1) >= iota((span, span), 0)).astype(BF16)
    drate = pick_left(upper, dcum, 3) + at_end
    dstep = drate * decay_ref[...] + sums[span : 2 * span]
    draw = dstep * jax.nn.sigmoid(raw)
    gh_ref[0:1, :] += jnp.sum(draw, axis=0, keepdims=True)
    gh_ref[1:2, :] += jnp.sum(drate * step, axis=0, keepdims=True) * decay_ref[...]
    gh_ref[2:3, :] += sums[2 * span + 1 : 2 * span + 2, :]

    dinputs = du * step_w + skip_ref[...] * dy
    dxbuf[span:, :] = dxbuf[:EDGE, :]
    dbbuf[span:, :] = dbbuf[:EDGE, :]
    dconv = dinputs * (sig * (1.0 + conv * (1.0 - sig)))
    dconvb = jnp.concatenate([db, dc], axis=1) * (sigb * (1.0 + convb * (1.0 - sigb)))
    dxbuf[:span, :] = dconv
    dbbuf[:span, :] = dconvb
    dx = jnp.zeros_like(dconv)
    dbc = jnp.zeros_like(dconvb)
    for tap in range(KCONV):
        back = KCONV - 1 - tap
        start = EDGE - 3 + tap
        dx = dx + tap_ref[tap : tap + 1, :] * dxbuf[back : back + span, :]
        dbc = dbc + tapb_ref[tap : tap + 1, :] * dbbuf[back : back + span, :]
        gx_ref[tap : tap + 1, :] += jnp.sum(
            dconv * xbuf[start : start + span, :], axis=0, keepdims=True
        )
        gb_ref[tap : tap + 1, :] += jnp.sum(
            dconvb * bbuf[start : start + span, :], axis=0, keepdims=True
        )
    gx_ref[KCONV : KCONV + 1, :] += jnp.sum(dconv, axis=0, keepdims=True)
    gb_ref[KCONV : KCONV + 1, :] += jnp.sum(dconvb, axis=0, keepdims=True)
    gx_ref[KCONV + 1 : KCONV + 2, :] += gain_grad
    width = 2 * channels + 2 * NS
    grad_ref[:, channels : 2 * channels] = dx.astype(BF16)
    grad_ref[:, 2 * channels : width] = dbc.astype(BF16)
    grad_ref[:, width : width + dqkv_ref.shape[1]] = dqkv_ref[...]
    grad_ref[:, width + dqkv_ref.shape[1] :] = draw.astype(BF16)
    for step in range(ring.ahead):
        pl.when(turn == spans * step // ring.ahead)(functools.partial(ring.hop, step))
    pl.when(turn == spans - 1)(ring.finish)


def scan_params(conv_x, conv_xb, conv_bc, conv_bcb, dt_bias, a_log, d_skip):
    heads = dt_bias.shape[0]

    def wide(row):
        return jnp.pad(row, (0, LANES - heads))[None, :]

    f32 = lambda value: value.astype(F32)
    return (
        f32(conv_x),
        f32(conv_xb)[None, :],
        f32(conv_bc),
        f32(conv_bcb)[None, :],
        wide(f32(dt_bias)),
        wide(-jnp.exp(f32(a_log))),
        jnp.repeat(f32(d_skip), MP)[None, :],
    )


def whole_spec(array):
    return pl.BlockSpec(array.shape, lambda turn: (0,) * array.ndim)


def run_scan_forward(proj, qkv_width, params, shard, devices):
    tokens = proj.shape[0]
    channels = params[1].shape[1]
    step_at = (2 * channels + 2 * NS + qkv_width) // LANES
    spans = tokens // SPAN
    bc_at = 2 * channels // (2 * NS)
    rows = lambda width, at: pl.BlockSpec((SPAN, width), lambda turn: (turn, at))
    anywhere = pl.BlockSpec(memory_space=pl.ANY)
    return pl.pallas_call(
        functools.partial(scan_forward, devices, spans),
        grid=(spans,),
        out_shape=(
            jax.ShapeDtypeStruct((tokens, channels), F32),
            jax.ShapeDtypeStruct((tokens, channels), F32),
            jax.ShapeDtypeStruct((spans, NS, channels), F32),
            gather_shape(shard, devices),
        ),
        in_specs=[rows(channels, 0), rows(channels, 1), rows(2 * NS, bc_at), rows(LANES, step_at)]
        + [whole_spec(item) for item in params]
        + [anywhere],
        out_specs=(
            rows(channels, 0),
            rows(channels, 0),
            pl.BlockSpec((1, NS, channels), lambda turn: (turn, 0, 0)),
            anywhere,
        ),
        scratch_shapes=[
            pltpu.VMEM((NS, channels), F32),
            pltpu.VMEM((SPAN + EDGE, channels), F32),
            pltpu.VMEM((SPAN + EDGE, 2 * NS), F32),
        ]
        + gather_sems(devices),
        compiler_params=pltpu.CompilerParams(collective_id=2, has_side_effects=True),
        cost_estimate=cost(20),
        name="scan_forward",
    )(proj, proj, proj, proj, *params, shard)


def run_scan_backward(
    proj, y, entering, dyg, scale, inner, dqkv, params, gain, sent, pieces, devices
):
    tokens, width = proj.shape
    channels = params[1].shape[1]
    qkv_width = dqkv.shape[1]
    step_at = (2 * channels + 2 * NS + qkv_width) // LANES
    spans = tokens // SPAN
    bc_at = 2 * channels // (2 * NS)
    edges = SPAN // EDGE
    rows = lambda size, at: pl.BlockSpec((SPAN, size), lambda turn: (spans - 1 - turn, at))
    edge = lambda size, at: pl.BlockSpec(
        (EDGE, size), lambda turn: (jnp.maximum((spans - 1 - turn) * edges - 1, 0), at)
    )
    keep = lambda shape: pl.BlockSpec(shape, lambda turn: (0, 0))
    shapes = scatter_shapes(sent, pieces, devices)
    return pl.pallas_call(
        functools.partial(scan_backward, devices, spans, pieces, len(sent)),
        grid=(spans,),
        out_shape=(
            jax.ShapeDtypeStruct((tokens, width), BF16),
            jax.ShapeDtypeStruct((EDGE, channels), F32),
            jax.ShapeDtypeStruct((EDGE, 2 * NS), F32),
            jax.ShapeDtypeStruct((EDGE, LANES), F32),
        )
        + shapes,
        in_specs=[
            rows(channels, 0),
            rows(channels, 1),
            edge(channels, 1),
            rows(2 * NS, bc_at),
            edge(2 * NS, bc_at),
            rows(LANES, step_at),
            rows(channels, 0),
            pl.BlockSpec((1, NS, channels), lambda turn: (spans - 1 - turn, 0, 0)),
            rows(channels, 0),
            rows(1, 0),
            rows(1, 0),
            rows(qkv_width, 0),
        ]
        + [whole_spec(item) for item in params]
        + [whole_spec(gain)]
        + [pl.BlockSpec(memory_space=pl.ANY)] * len(sent),
        out_specs=(
            rows(width, 0),
            keep((EDGE, channels)),
            keep((EDGE, 2 * NS)),
            keep((EDGE, LANES)),
        )
        + tuple(keep(item.shape) for item in shapes),
        scratch_shapes=[
            pltpu.VMEM((NS, channels), F32),
            pltpu.VMEM((SPAN + EDGE, channels), F32),
            pltpu.VMEM((SPAN + EDGE, 2 * NS), F32),
            pltpu.VMEM((SPAN + EDGE, channels), F32),
            pltpu.VMEM((SPAN + EDGE, 2 * NS), F32),
            pltpu.VMEM((SPAN, channels), F32),
            pltpu.VMEM((LANES, SPAN), F32),
        ]
        + scatter_scratch(sent, devices),
        compiler_params=pltpu.CompilerParams(collective_id=6, has_side_effects=True),
        cost_estimate=cost(47),
        name="scan_backward",
    )(
        proj, proj, proj, proj, proj, proj, y, entering, dyg, scale, inner, dqkv, *params, gain,
        *sent,
    )


def rotary_tables(tokens):
    half = HEAD_SIZE // 2
    exponent = np.arange(half, dtype=np.float64) * (-2.0 * LOG_BASE / HEAD_SIZE)
    rates = np.tile(np.exp(exponent.astype(np.float32)).astype(np.float64), LANES // half)
    tables = []
    for places in (np.arange(FINE), np.arange(0, tokens, FINE)):
        angles = places[:, None] * rates[None, :]
        tables += [np.cos(angles).astype(np.float32), np.sin(angles).astype(np.float32)]
    return tables


def fill_rotary(fine_cos, fine_sin, coarse_cos, coarse_sin, cosine, sine):
    small_cos, small_sin = fine_cos[...], fine_sin[...]
    for turn in range(coarse_cos.shape[0]):
        big_cos, big_sin = coarse_cos[turn : turn + 1, :], coarse_sin[turn : turn + 1, :]
        rows = slice(turn * FINE, (turn + 1) * FINE)
        cosine[rows, :] = small_cos * big_cos - small_sin * big_sin
        sine[rows, :] = small_sin * big_cos + small_cos * big_sin


def head_masks():
    half = HEAD_SIZE // 2
    row, col = iota((LANES, LANES), 0), iota((LANES, LANES), 1)
    place = col % HEAD_SIZE
    ahead = jnp.where(place < half, -1.0, 0.0)
    behind = jnp.where(place < half, 0.0, 1.0)

    def turn(start):
        return jnp.where(row == start + half, ahead, jnp.where(row == start - half, behind, 0.0))

    first = row < HEAD_SIZE
    left = col < HEAD_SIZE
    low = lambda mask: mask.astype(BF16)
    within = low(turn(col))
    copy = low(jnp.where(row == place, 1.0, 0.0))
    copy_turn = low(jnp.where(first, turn(place), 0.0))
    value = low(jnp.where(row == place + HEAD_SIZE, 1.0, 0.0))
    fold = low(jnp.where(left & (row % HEAD_SIZE == place), 1.0, 0.0))
    other = row % HEAD_SIZE
    fold_turn = low(
        jnp.where(
            left,
            jnp.where(other == place + half, ahead, jnp.where(other == place - half, behind, 0.0)),
            0.0,
        )
    )
    fold_value = low(jnp.where(left, 0.0, jnp.where(other == place, 1.0, 0.0)))
    return within, copy, copy_turn, value, fold, fold_turn, fold_value


def attend_forward(
    q_ref, kv_ref, fine_cos, fine_sin, coarse_cos, coarse_sin,
    qkv_ref, lse_ref, o_ref, vt, cos_ref, sin_ref,
):
    fill_rotary(fine_cos, fine_sin, coarse_cos, coarse_sin, cos_ref, sin_ref)
    tokens, query_width = q_ref.shape
    pairs = query_width // LANES
    within, copy, copy_turn, value = head_masks()[:4]
    for start in range(0, tokens, QBLK):
        rows = slice(start, start + QBLK)
        cosine, sine = cos_ref[rows, :], sin_ref[rows, :]
        for pair in range(pairs):
            lanes = slice(pair * LANES, (pair + 1) * LANES)
            query = q_ref[rows, lanes]
            turned = query * cosine + pick(query, within) * sine
            qkv_ref[rows, lanes] = (turned * HEAD_SIZE**-0.5).astype(BF16)
        kv = kv_ref[rows, :]
        keys = pick(kv, copy) * cosine + pick(kv, copy_turn) * sine
        qkv_ref[rows, query_width : query_width + LANES] = keys.astype(BF16)
        qkv_ref[rows, query_width + LANES :] = dot(kv.astype(BF16), value).astype(BF16)
        vt[:, rows] = kv.T[HEAD_SIZE:, :].astype(BF16)
    low_lanes = iota((QBLK, LANES), 1) < HEAD_SIZE
    wide = (QBLK, 2 * QBLK)
    visible = iota(wide, 0) <= iota(wide, 1) % QBLK

    def block(i, carry):
        here = pl.ds(pl.multiple_of(i * QBLK, QBLK), QBLK)
        queries = [
            pair_split(qkv_ref[here, pair * LANES : (pair + 1) * LANES], low_lanes)
            for pair in range(pairs)
        ]

        def tile(there, state, edge):
            keys = qkv_ref[there, query_width : query_width + LANES]
            result = []
            for pair in range(pairs):
                top, total, out = state[3 * pair : 3 * pair + 3]
                scores = dot(keys, queries[pair], NT)
                if edge:
                    scores = jnp.where(visible, scores, MASKED)
                higher = jnp.maximum(top, jnp.max(scores, axis=0, keepdims=True))
                probs = jnp.exp(scores - higher)
                fade = jnp.exp(top - higher)
                total = total * fade + jnp.sum(probs, axis=0, keepdims=True)
                out = out * fade + dot(vt[:, there], probs.astype(BF16))
                result += [higher, total, out]
            return tuple(result)

        state = (
            jnp.full((1, 2 * QBLK), MASKED, F32),
            jnp.zeros((1, 2 * QBLK), F32),
            jnp.zeros((HEAD_SIZE, 2 * QBLK), F32),
        ) * pairs
        state = lax.fori_loop(
            0,
            i,
            lambda j, state: tile(pl.ds(pl.multiple_of(j * QBLK, QBLK), QBLK), state, False),
            state,
        )
        state = tile(here, state, True)
        for pair in range(pairs):
            top, total, out = state[3 * pair : 3 * pair + 3]
            out = out / total
            lse = top + jnp.log(total)
            lse_ref[2 * pair : 2 * pair + 1, here] = lse[:, :QBLK]
            lse_ref[2 * pair + 1 : 2 * pair + 2, here] = lse[:, QBLK:]
            both = jnp.concatenate([out[:, :QBLK], out[:, QBLK:]], axis=0)
            o_ref[here, pair * LANES : (pair + 1) * LANES] = both.T.astype(BF16)
        return carry

    lax.fori_loop(0, tokens // QBLK, block, 0)


def attend_backward(
    qkv_ref, lse_ref, o_ref, do_ref, fine_cos, fine_sin, coarse_cos, coarse_sin,
    dqkv_ref,
    dq, kt, dk, dv, cos_ref, sin_ref,
):
    fill_rotary(fine_cos, fine_sin, coarse_cos, coarse_sin, cos_ref, sin_ref)
    tokens, query_width = o_ref.shape
    pairs = query_width // LANES
    key_lanes = slice(query_width, query_width + LANES)
    value_lanes = slice(query_width + LANES, query_width + 2 * LANES)
    for start in range(0, tokens, QBLK):
        rows = slice(start, start + QBLK)
        kt[:, rows] = qkv_ref[rows, key_lanes].astype(F32).T[:HEAD_SIZE, :].astype(BF16)
    dk[...] = jnp.zeros_like(dk)
    dv[...] = jnp.zeros_like(dv)
    low_lanes = iota((QBLK, LANES), 1) < HEAD_SIZE
    wide = (QBLK, 2 * QBLK)
    visible = iota(wide, 0) <= iota(wide, 1) % QBLK
    ones = jnp.ones((EDGE, LANES), BF16)

    def block(i, carry):
        here = pl.ds(pl.multiple_of(i * QBLK, QBLK), QBLK)
        queries, grads, inners, lses = [], [], [], []
        for pair in range(pairs):
            lanes = slice(pair * LANES, (pair + 1) * LANES)
            queries.append(pair_split(qkv_ref[here, lanes], low_lanes))
            grad = do_ref[here, lanes]
            grads.append(pair_split(grad, low_lanes))
            both = pair_split(grad.astype(F32) * o_ref[here, lanes].astype(F32), low_lanes)
            high, low = parts(both, 2)
            inners.append((dot(ones, high, NT) + dot(ones, low, NT))[:1])
            lses.append(
                jnp.concatenate(
                    [
                        lse_ref[2 * pair : 2 * pair + 1, here],
                        lse_ref[2 * pair + 1 : 2 * pair + 2, here],
                    ],
                    axis=1,
                )
            )
        query_all = jnp.concatenate(queries, axis=0)
        grad_all = jnp.concatenate(grads, axis=0)

        def tile(there, state, edge):
            keys = qkv_ref[there, key_lanes]
            values = qkv_ref[there, value_lanes]
            all_probs, all_dscores, result = [], [], []
            for pair in range(pairs):
                probs = dot(keys, queries[pair], NT) - lses[pair]
                if edge:
                    probs = jnp.where(visible, probs, MASKED)
                probs = jnp.exp(probs)
                dprobs = dot(values, grads[pair], NT)
                dscores = (probs * (dprobs - inners[pair])).astype(BF16)
                all_probs.append(probs.astype(BF16))
                all_dscores.append(dscores)
                result.append(state[pair] + dot(kt[:, there], dscores))
            dv[there, :] += dot(jnp.concatenate(all_probs, axis=1), grad_all)
            dk[there, :] += dot(jnp.concatenate(all_dscores, axis=1), query_all)
            return tuple(result)

        state = (jnp.zeros((HEAD_SIZE, 2 * QBLK), F32),) * pairs
        state = lax.fori_loop(
            0,
            i,
            lambda j, state: tile(pl.ds(pl.multiple_of(j * QBLK, QBLK), QBLK), state, False),
            state,
        )
        state = tile(here, state, True)
        for pair in range(pairs):
            both = jnp.concatenate([state[pair][:, :QBLK], state[pair][:, QBLK:]], axis=0)
            dq[here, pair * LANES : (pair + 1) * LANES] = both.T
        return carry

    lax.fori_loop(0, tokens // QBLK, block, 0)
    masks = head_masks()
    within, (fold, fold_turn, fold_value) = masks[0], masks[4:]
    for start in range(0, tokens, QBLK):
        rows = slice(start, start + QBLK)
        cosine, sine = cos_ref[rows, :], sin_ref[rows, :]
        for pair in range(pairs):
            lanes = slice(pair * LANES, (pair + 1) * LANES)
            grad = dq[rows, lanes]
            grad = grad * cosine - pick(grad, within) * sine
            dqkv_ref[rows, lanes] = (grad * HEAD_SIZE**-0.5).astype(BF16)
        grad = dk[rows, :]
        grad = pick(grad, fold) * cosine - pick(grad, fold_turn) * sine
        grad = grad + pick(dv[rows, :], fold_value)
        dqkv_ref[rows, query_width:] = grad.astype(BF16)


def run_attend_forward(proj, query_at, query_width, tables):
    tokens = proj.shape[0]
    cols = lambda size, at: pl.BlockSpec((tokens, size), lambda turn: (0, at // size))
    return pl.pallas_call(
        attend_forward,
        grid=(1,),
        out_shape=(
            jax.ShapeDtypeStruct((tokens, query_width + 2 * LANES), BF16),
            jax.ShapeDtypeStruct((EDGE, tokens), F32),
            jax.ShapeDtypeStruct((tokens, query_width), BF16),
        ),
        in_specs=[
            cols(query_width, query_at),
            cols(2 * HEAD_SIZE, query_at + query_width),
        ]
        + [whole_spec(table) for table in tables],
        out_specs=(
            cols(query_width + 2 * LANES, 0),
            pl.BlockSpec((EDGE, tokens), lambda turn: (0, 0)),
            cols(query_width, 0),
        ),
        scratch_shapes=[
            pltpu.VMEM((HEAD_SIZE, tokens), BF16),
            pltpu.VMEM((tokens, LANES), F32),
            pltpu.VMEM((tokens, LANES), F32),
        ],
        cost_estimate=cost(15),
        name="attend_forward",
    )(proj, proj, *tables)


def run_attend_backward(qkv, lse, attended, grads, grad_at, tables):
    tokens, query_width = attended.shape
    vmem = pl.BlockSpec(memory_space=pltpu.VMEM)
    cols = lambda size, at: pl.BlockSpec((tokens, size), lambda turn: (0, at // size))
    return pl.pallas_call(
        attend_backward,
        grid=(1,),
        out_shape=jax.ShapeDtypeStruct((tokens, query_width + 2 * HEAD_SIZE), BF16),
        in_specs=[
            whole_spec(qkv),
            whole_spec(lse),
            whole_spec(attended),
            cols(query_width, grad_at),
        ]
        + [whole_spec(table) for table in tables],
        out_specs=cols(query_width + 2 * HEAD_SIZE, 0),
        scratch_shapes=[
            pltpu.VMEM((tokens, query_width), F32),
            pltpu.VMEM((HEAD_SIZE, tokens), BF16),
            pltpu.VMEM((tokens, LANES), F32),
            pltpu.VMEM((tokens, LANES), F32),
            pltpu.VMEM((tokens, LANES), F32),
            pltpu.VMEM((tokens, LANES), F32),
        ],
        cost_estimate=cost(16),
        name="attend_backward",
    )(qkv, lse, attended, grads, *tables)


def feed_forward(
    x_ref, mixed_ref, other_ref, top_ref, gain_ref, gu_ref, down_ref,
    after_ref, scale_ref, hidden_ref, act_ref, dgu_ref, part_ref, back_ref,
):
    units = down_ref.shape[1]
    after = x_ref[...].astype(F32) + (mixed_ref[...].astype(F32) + other_ref[...].astype(F32))
    after_ref[...] = after
    scale = lax.rsqrt(jnp.mean(after * after, axis=-1, keepdims=True) + EPSILON)
    scale_ref[...] = scale
    hidden = (after * scale * gain_ref[...]).astype(BF16)
    hidden_ref[...] = hidden
    top = top_ref[...]
    for start in range(0, units, UBLK):
        cols = slice(start, start + UBLK)
        up_cols = slice(units + start, units + start + UBLK)
        gate = dot(hidden, gu_ref[:, cols])
        upward = dot(hidden, gu_ref[:, up_cols])
        grad = dot(top, down_ref[:, cols])
        sigma = jax.nn.sigmoid(gate)
        swish = gate * sigma
        act_ref[:, cols] = (swish * upward).astype(BF16)
        slope = sigma * (1.0 + gate * (1.0 - sigma))
        dgu_ref[:, cols] = (grad * upward * slope).astype(BF16)
        dgu_ref[:, up_cols] = (grad * swish).astype(BF16)
    back_ref[...] = dot(dgu_ref[...], gu_ref[...], NT).astype(BF16)
    part_ref[...] = dot(act_ref[...], down_ref[...], NT).astype(BF16)


def run_feed_forward(x, mixed, other, top, gain, w_gate_up, w_down_t):
    tokens, width = x.shape
    units = w_down_t.shape[1]
    rows = lambda size: pl.BlockSpec((TBLK, size), lambda turn: (turn, 0))
    once = lambda item: pl.BlockSpec(
        item.shape, lambda turn: (0, 0), pipeline_mode=pl.Buffered(1)
    )
    shape = jax.ShapeDtypeStruct
    return pl.pallas_call(
        feed_forward,
        grid=(tokens // TBLK,),
        out_shape=(
            shape((tokens, width), F32),
            shape((tokens, 1), F32),
            shape((tokens, width), BF16),
            shape((tokens, units), BF16),
            shape((tokens, 2 * units), BF16),
            shape((tokens, width), BF16),
            shape((tokens, width), BF16),
        ),
        in_specs=[rows(width)] * 4 + [once(gain), once(w_gate_up), once(w_down_t)],
        out_specs=(
            rows(width), rows(1), rows(width), rows(units), rows(2 * units), rows(width),
            rows(width),
        ),
        cost_estimate=cost(20),
        name="feed_forward",
    )(x, mixed, other, top, gain, w_gate_up, w_down_t)


def swap(partial):
    return lax.ppermute(partial, "tensor", [(0, 1), (1, 0)])


def join(mine, other):
    return mine.astype(F32) + other.astype(F32)


def tensor_sum(partial):
    return join(partial, swap(partial))


def norm_back(normed, scale, gain, grad):
    weighted = grad * gain
    grad_input = scale * (weighted - normed * jnp.mean(weighted * normed, axis=-1, keepdims=True))
    return (grad_input, jnp.sum(grad * normed, axis=0))


def local(
    layer_input, w_norm1, w_zx, w_bc, w_dt, conv_x, conv_xb, conv_bc, conv_bcb, dt_bias, a_log,
    d_skip, w_mnorm, w_mout, query_key_value_weight, output_weight, w_norm2, w_gu, w_down,
    grad_output,
):
    devices = lax.axis_size("dp")
    tokens, width = layer_input.shape
    shard = w_zx.shape[0]
    channels = conv_xb.shape[0]
    heads = dt_bias.shape[0]
    qkv_width = query_key_value_weight.shape[2]
    units = w_down.shape[0]
    attn_width = output_weight.shape[1]
    tail = jnp.concatenate(
        [w_dt, w_norm1[:, None], w_norm2[:, None], jnp.zeros((shard, LANES - heads - 2), BF16)],
        axis=1,
    )
    mixer_in = jnp.concatenate(
        [w_zx.reshape(shard, -1), w_bc, query_key_value_weight.reshape(shard, -1), tail], axis=1
    )
    in_width = mixer_in.shape[1]
    (w_in,) = gather_rows([mixer_in], devices, 0)
    norm1 = w_in[:, in_width - LANES + heads].astype(F32)
    norm2 = w_in[:, in_width - LANES + heads + 1].astype(F32)

    source = layer_input.astype(F32)
    scale_one = lax.rsqrt(jnp.mean(source * source, axis=-1, keepdims=True) + EPSILON)
    normed_one = source * scale_one
    hidden_one = (normed_one * norm1).astype(BF16)
    proj = dot(hidden_one, w_in)
    params = scan_params(conv_x, conv_xb, conv_bc, conv_bcb, dt_bias, a_log, d_skip)
    out_shard = jnp.concatenate([w_mout.T, output_weight.reshape(attn_width, -1).T], axis=1)
    y, gated, entering, w_out = run_scan_forward(proj, qkv_width, params, out_shard, devices)
    channels_all = channels * lax.axis_size("tensor")
    square_sum = tensor_sum(jnp.sum(gated * gated, axis=-1))
    scale_m = lax.rsqrt(square_sum / channels_all + EPSILON)[:, None]
    tables = rotary_tables(tokens)
    qkv_at = 2 * channels + 2 * NS
    qkv, lse, attended = run_attend_forward(proj, qkv_at, attn_width, tables)
    gain_m = w_mnorm.astype(F32)
    mamba_low = (gated * scale_m * gain_m).astype(BF16)
    mixer_out = jnp.concatenate([mamba_low, attended], axis=1)
    mixed, gate_up_shard, down_shard = lax.optimization_barrier(
        (dot(mixer_out, w_out, NT).astype(BF16), w_gu.reshape(shard, -1), w_down.T)
    )
    other = swap(mixed)
    w_gate_up, w_down_t = gather_rows([gate_up_shard, down_shard], devices, 3)
    other, w_gate_up, w_down_t = lax.optimization_barrier((other, w_gate_up, w_down_t))
    after, scale_two, hidden_two, activated, grad_gu_low, ffn_part, partial_two = run_feed_forward(
        layer_input, mixed, other, grad_output, norm2[None, :], w_gate_up, w_down_t
    )
    other = swap(partial_two)
    grad_gu = dot(hidden_two, grad_gu_low, TN).astype(BF16)
    grad_down = dot(grad_output, activated, TN).astype(BF16)
    (mine_gu,) = scatter_rows([grad_gu], [(0, 0, 2 * units)], devices, 1)
    other, mine_gu, grad_down, ffn_part = lax.optimization_barrier(
        (other, mine_gu, grad_down, ffn_part)
    )
    normed_two = after * scale_two
    grad_hidden_two = join(partial_two, other)
    ffn_other = swap(ffn_part)
    grad_norm_in, grad_norm2 = norm_back(normed_two, scale_two, norm2, grad_hidden_two)
    grad_after = grad_output.astype(F32) + grad_norm_in
    grad_mix_low = grad_after.astype(BF16)
    grad_mixer = dot(grad_mix_low, w_out)
    grad_mamba = grad_mixer[:, :channels]
    normed_m = gated * scale_m
    inner_m = tensor_sum(jnp.sum(grad_mamba * gain_m * normed_m, axis=-1))[:, None] / channels_all
    dqkv = run_attend_backward(
        qkv, lse, attended, grad_mixer[:, channels:].astype(BF16), 0, tables
    )
    grad_out = dot(grad_mix_low, mixer_out, TN).astype(BF16)
    pieces = [
        (0, 0, channels),
        (0, channels, channels + attn_width),
        (1, 0, units),
    ]
    grad_proj, small_x, small_b, small_h, mine_mout, mine_o, mine_down = run_scan_backward(
        proj, y, entering, grad_mamba, scale_m, inner_m, dqkv, params, gain_m[None, :],
        [grad_out, grad_down], pieces, devices,
    )
    ffn_other, grad_proj = lax.optimization_barrier((ffn_other, grad_proj))
    result = (after + join(ffn_part, ffn_other)).astype(BF16)
    partial_one, grad_proj = lax.optimization_barrier(
        (dot(grad_proj, w_in, NT).astype(BF16), grad_proj)
    )
    crossing = jnp.concatenate(
        [
            small_b[: KCONV + 1].reshape(-1, LANES),
            jnp.sum(partial_one.astype(F32) * normed_one, axis=0).reshape(-1, LANES),
        ],
        axis=0,
    )
    crossing = tensor_sum(crossing)
    partial_one, crossing = lax.optimization_barrier((partial_one, crossing))
    other = swap(partial_one)
    grad_in = dot(hidden_one, grad_proj, TN).astype(BF16)
    small = jnp.concatenate(
        [
            small_x[: KCONV + 2].reshape(-1, LANES),
            small_h[:3],
            crossing,
            grad_norm2.reshape(-1, LANES),
        ],
        axis=0,
    )
    small_rows = small.shape[0]
    small = jnp.pad(small, ((0, -small_rows % EDGE), (0, 0)))
    shared_at = 2 * channels
    step_at = qkv_at + qkv_width
    mine_zx, mine_bc, mine_qkv, mine_step, small = scatter_last(
        [grad_in],
        small,
        [
            (0, 0, shared_at),
            (0, shared_at, qkv_at),
            (0, qkv_at, step_at),
            (0, step_at, in_width),
        ],
        devices,
        5,
    )
    other, mine_bc = lax.optimization_barrier((other, mine_bc))
    grad_hidden_one = join(partial_one, other)
    weighted = grad_hidden_one * norm1
    grad_source = grad_after + scale_one * (
        weighted - normed_one * jnp.mean(weighted * normed_one, axis=-1, keepdims=True)
    )

    half = NS * 2 // lax.axis_size("tensor")
    shared_cols = tensor_sum(mine_bc)
    begin = lax.axis_index("tensor") * half
    grad_bc = lax.dynamic_slice_in_dim(shared_cols, begin, half, 1)
    small = small[:small_rows].reshape(-1)
    x_size = (KCONV + 2) * channels
    h_size = 3 * LANES
    b_size = (KCONV + 1) * 2 * NS
    total_x = small[:x_size].reshape(KCONV + 2, channels)
    total_h = small[x_size : x_size + h_size].reshape(3, LANES)
    total_b = small[x_size + h_size : x_size + h_size + b_size].reshape(KCONV + 1, 2 * NS)
    total_b = lax.dynamic_slice_in_dim(total_b, begin, half, 1)
    norms = small[x_size + h_size + b_size :].reshape(2, width)
    norms = lax.dynamic_slice_in_dim(norms, lax.axis_index("dp") * shard, shard, 1)
    return (
        result,
        grad_source,
        norms[0],
        mine_zx.reshape(w_zx.shape),
        grad_bc,
        mine_step[:, :heads],
        total_x[:KCONV],
        total_x[KCONV],
        total_b[:KCONV],
        total_b[KCONV],
        total_h[0, :heads],
        total_h[1, :heads],
        total_h[2, :heads],
        total_x[KCONV + 1],
        mine_mout.T,
        mine_qkv.reshape(query_key_value_weight.shape),
        mine_o.T.reshape(output_weight.shape),
        norms[1],
        mine_gu.reshape(w_gu.shape),
        mine_down.T,
    )


def solution(mesh):
    return jax.shard_map(
        local,
        mesh=mesh,
        in_specs=(
            P("dp", None),
            P("dp"),
            P("dp", None, "tensor"),
            P("dp", None),
            P("dp", "tensor"),
            P(None, "tensor"),
            P("tensor"),
            P(),
            P(),
            P("tensor"),
            P("tensor"),
            P("tensor"),
            P("tensor"),
            P("tensor", "dp"),
            P("dp", "tensor", None),
            P("tensor", None, "dp"),
            P("dp"),
            P("dp", None, "tensor"),
            P("tensor", "dp"),
            P("dp", None),
        ),
        out_specs=(
            P("dp", None),
            P("dp", None),
            P("dp"),
            P("dp", None, "tensor"),
            P("dp", "tensor"),
            P("dp", "tensor"),
            P(None, "tensor"),
            P("tensor"),
            P(None, "tensor"),
            P("tensor"),
            P("tensor"),
            P("tensor"),
            P("tensor"),
            P("tensor"),
            P("tensor", "dp"),
            P("dp", "tensor", None),
            P("tensor", None, "dp"),
            P("dp"),
            P("dp", None, "tensor"),
            P("tensor", "dp"),
        ),
        check_vma=False,
    )
```

```python
import functools
import math

import jax
import jax.numpy as jnp
import numpy as np
from jax import lax
from jax.experimental import pallas as pl
from jax.experimental.pallas import tpu as pltpu
from jax.sharding import PartitionSpec as P


HEAD_SIZE = 64
MP = 64
NS = 128
KCONV = 4
SPAN = 128
QBLK = 256
FINE = 32
TBLK = 256
UBLK = 256
LANES = 128
EDGE = 8

EPSILON = 1e-05
LOG_BASE = math.log(100000000000.0)
MASKED = -1e30
MESH = pl.DeviceIdType.MESH
F32 = jnp.float32
BF16 = jnp.bfloat16

NN = ((1,), (0,))
NT = ((1,), (1,))
TN = ((0,), (0,))


def dot(left, right, dims=NN, precision=None):
    return lax.dot_general(
        left, right, (dims, ((), ())), preferred_element_type=F32, precision=precision
    )


def iota(shape, dim):
    return lax.broadcasted_iota(jnp.int32, shape, dim)


def ring_place(chip, chips):
    odd = lax.rem(chip, 2)
    half = lax.div(chip, 2)
    return (1 - odd) * half + odd * (chips - 1 - half)


def ring_chip(place, chips):
    place = lax.rem(place + 4 * chips, chips)
    back = lax.div(place, chips // 2)
    return (1 - back) * (2 * place) + back * (2 * (chips - 1 - place) + 1)


class RingGather:
    def __init__(self, devices, x_ref, o_ref, sems):
        self.chips = devices // 2
        self.ahead = self.chips // 2
        self.behind = self.chips - 1 - self.ahead
        self.x_ref, self.o_ref, self.rows = x_ref, o_ref, x_ref.shape[0]
        self.fs, self.fr, self.bs, self.br, self.cs, self.cr, self.own_sem = sems

    def locate(self):
        me = lax.axis_index("dp")
        self.group = lax.axis_index("tensor")
        self.core = lax.rem(me, 2)
        chip = lax.div(me, 2)
        self.place = ring_place(chip, self.chips)
        self.right = ring_chip(self.place + 1, self.chips) * 2 + self.core
        self.left = ring_chip(self.place - 1, self.chips) * 2 + self.core
        self.mate = chip * 2 + (1 - self.core)
        self.me = me

    def slot(self, index):
        return self.o_ref.at[pl.ds(pl.multiple_of(index * self.rows, self.rows), self.rows), :]

    def copy(self, shift, ssem, rsem, target):
        if shift == 0:
            index, source = self.me, self.x_ref
        else:
            index = ring_chip(self.place + shift, self.chips) * 2 + self.core
            source = self.slot(index)
        return pltpu.make_async_remote_copy(
            src_ref=source,
            dst_ref=self.slot(index),
            send_sem=ssem,
            recv_sem=rsem,
            device_id=(target, self.group),
            device_id_type=MESH,
        )

    def fore(self, step):
        return self.copy(-step, self.fs.at[step], self.fr.at[step], self.right)

    def back(self, step):
        return self.copy(step, self.bs.at[step], self.br.at[step], self.left)

    def across(self, shift):
        number = 0 if shift == 0 else 2 * abs(shift) - (1 if shift < 0 else 0)
        return self.copy(shift, self.cs.at[number], self.cr.at[number], self.mate)

    def own(self):
        return pltpu.make_async_copy(self.x_ref, self.slot(self.me), self.own_sem)

    def greet(self):
        self.locate()
        barrier = pltpu.get_barrier_semaphore()
        for other in (self.right, self.left, self.mate):
            pl.semaphore_signal(
                barrier, inc=1, device_id=(other, self.group), device_id_type=MESH
            )
        pl.semaphore_wait(barrier, 3)

    def begin(self):
        self.locate()
        self.fore(0).start()
        self.back(0).start()
        self.across(0).start()
        self.own().start()

    def hop(self, step):
        self.locate()
        self.fore(step - 1).wait_recv()
        if step < self.ahead:
            self.fore(step).start()
        self.across(-step).start()
        if step <= self.behind:
            self.back(step - 1).wait_recv()
            if step < self.behind:
                self.back(step).start()
            self.across(step).start()

    def finish(self):
        self.locate()
        self.own().wait()
        for step in range(self.ahead):
            self.fore(step).wait_send()
        for step in range(self.behind):
            self.back(step).wait_send()
        for shift in range(-self.ahead, self.behind + 1):
            self.across(shift).wait()


def gather_sems(devices):
    dma = pltpu.SemaphoreType.DMA
    return [dma((devices // 2,))] * 6 + [dma(())]


def gather_shape(shard, devices):
    return jax.ShapeDtypeStruct((shard.shape[0] * devices, shard.shape[1]), shard.dtype)


def gather_kernel(devices, count, *refs):
    shards, outs, sems = refs[:count], refs[count : 2 * count], refs[2 * count :]
    each = len(sems) // count
    rings = [
        RingGather(devices, shards[i], outs[i], sems[i * each : (i + 1) * each])
        for i in range(count)
    ]
    rings[0].greet()
    for ring in rings:
        ring.begin()
    for step in range(1, rings[0].ahead + 1):
        for ring in rings:
            ring.hop(step)
    for ring in rings:
        ring.finish()


def cost(micros):
    return pl.CostEstimate(flops=int(micros * 1e9), bytes_accessed=0, transcendentals=0)


def gather_rows(shards, devices, collective):
    count = len(shards)
    anywhere = pl.BlockSpec(memory_space=pl.ANY)
    return pl.pallas_call(
        functools.partial(gather_kernel, devices, count),
        out_shape=tuple(gather_shape(shard, devices) for shard in shards),
        in_specs=[anywhere] * count,
        out_specs=(anywhere,) * count,
        scratch_shapes=gather_sems(devices) * count,
        compiler_params=pltpu.CompilerParams(collective_id=collective, has_side_effects=True),
        cost_estimate=cost(3),
        name="gather_rows",
    )(*shards)


def scatter_order(chips):
    ahead = chips // 2
    behind = chips - 1 - ahead
    order = []
    for step in range(ahead):
        order.append(-(ahead - step))
        if step < behind:
            order.append(behind - step)
    order.append(0)
    return order


class RingScatter:
    def __init__(self, devices, windows, pieces, grads, outs, scratch):
        self.windows = windows
        self.chips = devices // 2
        self.ahead = self.chips // 2
        self.behind = self.chips - 1 - self.ahead
        self.order = scatter_order(self.chips)
        self.pieces, self.grads, self.outs = pieces, grads, outs
        count = len(windows)
        self.mine, self.boxes, rest = scratch[:count], scratch[count : 2 * count], scratch[2 * count :]
        self.fbox, self.bbox, self.fout, self.bout = rest[:4]
        self.os, self.ms, self.mr, self.fs, self.fr, self.bs, self.br = rest[4:]
        self.rows = self.mine[0].shape[1]
        widths = [item.shape[2] for item in self.mine]
        self.cols = [slice(sum(widths[:i]), sum(widths[: i + 1])) for i in range(count)]

    def locate(self):
        me = lax.axis_index("dp")
        self.group = lax.axis_index("tensor")
        self.core = lax.rem(me, 2)
        chip = lax.div(me, 2)
        self.place = ring_place(chip, self.chips)
        self.right = ring_chip(self.place + 1, self.chips) * 2 + self.core
        self.left = ring_chip(self.place - 1, self.chips) * 2 + self.core
        self.mate = chip * 2 + (1 - self.core)

    def greet(self):
        self.locate()
        barrier = pltpu.get_barrier_semaphore()
        for other in (self.right, self.left, self.mate):
            pl.semaphore_signal(
                barrier, inc=1, device_id=(other, self.group), device_id_type=MESH
            )
        pl.semaphore_wait(barrier, 3)

    def block(self, i, shift, which):
        index = ring_chip(self.place + shift, self.chips) * 2 + which
        which, first, last = self.windows[i]
        rows = pl.ds(pl.multiple_of(index * self.rows, self.rows), self.rows)
        return self.grads[which].at[rows, first:last]

    def remote(self, source, target_ref, ssem, rsem, target):
        return pltpu.make_async_remote_copy(
            src_ref=source,
            dst_ref=target_ref,
            send_sem=ssem,
            recv_sem=rsem,
            device_id=(target, self.group),
            device_id_type=MESH,
        )

    def across(self, i, slot):
        return self.remote(
            self.block(i, self.order[slot], 1 - self.core),
            self.boxes[i].at[slot],
            self.ms.at[i, slot],
            self.mr.at[i, slot],
            self.mate,
        )

    def own(self, i, slot):
        return pltpu.make_async_copy(
            self.block(i, self.order[slot], self.core), self.mine[i].at[slot], self.os.at[i, slot]
        )

    def fore(self, step):
        return self.remote(
            self.fout.at[step], self.fbox.at[step], self.fs.at[step], self.fr.at[step], self.right
        )

    def back(self, step):
        return self.remote(
            self.bout.at[step], self.bbox.at[step], self.bs.at[step], self.br.at[step], self.left
        )

    def begin(self):
        self.locate()
        for slot in range(self.chips):
            for i in range(len(self.windows)):
                self.across(i, slot).start()
                self.own(i, slot).start()

    def local_sum(self, i, slot, cols, others):
        total = self.mine[i][slot, :, cols].astype(F32) + self.boxes[i][slot, :, cols].astype(F32)
        whole = slice(self.cols[i].start + cols.start, self.cols[i].start + cols.stop)
        for ref in others:
            total = total + ref[:, whole].astype(F32)
        return total

    def arrive(self, slot):
        for i in range(len(self.windows)):
            self.own(i, slot).wait()
            self.across(i, slot).wait_recv()

    def put(self, target, shift, others):
        slot = self.order.index(shift)
        self.arrive(slot)
        for i, cols in enumerate(self.cols):
            total = self.local_sum(i, slot, slice(0, cols.stop - cols.start), others)
            target[:, cols] = total.astype(BF16)

    def hop(self, step):
        self.locate()
        if step > 0:
            self.back(step - 1).wait_recv()
        self.put(
            self.bout.at[step], -(self.ahead - step), [self.bbox.at[step - 1]] if step else []
        )
        self.back(step).start()
        if step < self.behind:
            if step > 0:
                self.fore(step - 1).wait_recv()
            self.put(
                self.fout.at[step], self.behind - step, [self.fbox.at[step - 1]] if step else []
            )
            self.fore(step).start()

    def finish(self):
        self.locate()
        slot = self.order.index(0)
        self.arrive(slot)
        self.fore(self.behind - 1).wait_recv()
        self.back(self.ahead - 1).wait_recv()
        others = [self.fbox.at[self.behind - 1], self.bbox.at[self.ahead - 1]]
        for out, (i, first, last) in zip(self.outs, self.pieces):
            out[...] = self.local_sum(i, slot, slice(first, last), others)
        for step in range(self.ahead):
            self.back(step).wait_send()
        for step in range(self.behind):
            self.fore(step).wait_send()
        for slot in range(self.chips):
            for i in range(len(self.windows)):
                self.across(i, slot).wait_send()


def scatter_scratch(grads, windows, devices):
    chips = devices // 2
    rows = grads[0].shape[0] // devices
    count = len(windows)
    dma = pltpu.SemaphoreType.DMA
    widths = [last - first for which, first, last in windows]
    boxes = [pltpu.VMEM((chips, rows, width), BF16) for width in widths]
    box = pltpu.VMEM((chips // 2, rows, sum(widths)), BF16)
    return boxes * 2 + [box] * 4 + [dma((count, chips))] * 3 + [dma((chips,))] * 4


def scatter_shapes(grads, pieces, devices):
    rows = grads[0].shape[0] // devices
    return tuple(jax.ShapeDtypeStruct((rows, last - first), F32) for i, first, last in pieces)


class Total:
    def __init__(self, devices, x_ref, o_ref, scratch):
        self.chips = devices // 2
        self.x_ref, self.o_ref = x_ref, o_ref
        self.mate_box, self.joined, self.boxes, self.ms, self.mr, self.ss, self.sr = scratch
        me = lax.axis_index("dp")
        self.group = lax.axis_index("tensor")
        self.chip = lax.div(me, 2)
        core = lax.rem(me, 2)
        self.mate = self.chip * 2 + (1 - core)
        self.peers = [
            lax.rem(self.chip + shift, self.chips) * 2 + core for shift in range(self.chips)
        ]

    def greet(self):
        barrier = pltpu.get_barrier_semaphore()
        for other in [self.mate] + self.peers[1:]:
            pl.semaphore_signal(
                barrier, inc=1, device_id=(other, self.group), device_id_type=MESH
            )
        pl.semaphore_wait(barrier, self.chips)

    def remote(self, source, target_ref, ssem, rsem, target):
        return pltpu.make_async_remote_copy(
            src_ref=source,
            dst_ref=target_ref,
            send_sem=ssem,
            recv_sem=rsem,
            device_id=(target, self.group),
            device_id_type=MESH,
        )

    def begin(self):
        self.across = self.remote(self.x_ref, self.mate_box, self.ms, self.mr, self.mate)
        self.across.start()

    def spread(self):
        self.across.wait_recv()
        self.joined[...] = self.x_ref[...] + self.mate_box[...]
        self.copies = [
            self.remote(
                self.joined,
                self.boxes.at[self.chip],
                self.ss.at[shift],
                self.sr.at[shift],
                self.peers[shift],
            )
            for shift in range(1, self.chips)
        ]
        for copy in self.copies:
            copy.start()
        self.boxes[self.chip] = self.joined[...]

    def finish(self):
        for copy in self.copies:
            copy.wait_recv()
        result = self.boxes[0]
        for other in range(1, self.chips):
            result = result + self.boxes[other]
        self.o_ref[...] = result
        self.across.wait_send()
        for copy in self.copies:
            copy.wait_send()


def total_scratch(values, devices):
    chips = devices // 2
    dma = pltpu.SemaphoreType.DMA
    return [
        pltpu.VMEM(values.shape, F32),
        pltpu.VMEM(values.shape, F32),
        pltpu.VMEM((chips,) + values.shape, F32),
        dma(()),
        dma(()),
        dma((chips,)),
        dma((chips,)),
    ]


def scatter_kernel(devices, count, windows, pieces, *refs):
    outs = len(pieces)
    ring = RingScatter(
        devices, windows, pieces, refs[:count], refs[count : count + outs], refs[count + outs :]
    )
    ring.greet()
    ring.begin()
    for step in range(ring.ahead):
        ring.hop(step)
    ring.finish()


def scatter_rows(grads, windows, pieces, devices, collective):
    count = len(grads)
    return pl.pallas_call(
        functools.partial(scatter_kernel, devices, count, windows, pieces),
        out_shape=scatter_shapes(grads, pieces, devices),
        in_specs=[pl.BlockSpec(memory_space=pl.ANY)] * count,
        out_specs=(pl.BlockSpec(memory_space=pltpu.VMEM),) * len(pieces),
        scratch_shapes=scatter_scratch(grads, windows, devices),
        compiler_params=pltpu.CompilerParams(collective_id=collective, has_side_effects=True),
        cost_estimate=cost(3),
        name="scatter_rows",
    )(*grads)


def last_kernel(devices, count, windows, pieces, *refs):
    outs = len(pieces)
    grads, values, refs = refs[:count], refs[count], refs[count + 1 :]
    pieces_out, total_out, scratch = refs[:outs], refs[outs], refs[outs + 1 :]
    ring = RingScatter(devices, windows, pieces, grads, pieces_out, scratch[:-7])
    total = Total(devices, values, total_out, scratch[-7:])
    total.greet()
    ring.begin()
    total.begin()
    for step in range(ring.ahead):
        ring.hop(step)
        if step == 0:
            total.spread()
    ring.finish()
    total.finish()


def scatter_last(grads, values, windows, pieces, devices, collective):
    count = len(grads)
    vmem = pl.BlockSpec(memory_space=pltpu.VMEM)
    return pl.pallas_call(
        functools.partial(last_kernel, devices, count, windows, pieces),
        out_shape=scatter_shapes(grads, pieces, devices)
        + (jax.ShapeDtypeStruct(values.shape, F32),),
        in_specs=[pl.BlockSpec(memory_space=pl.ANY)] * count + [vmem],
        out_specs=(vmem,) * (len(pieces) + 1),
        scratch_shapes=scatter_scratch(grads, windows, devices) + total_scratch(values, devices),
        compiler_params=pltpu.CompilerParams(collective_id=collective, has_side_effects=True),
        cost_estimate=cost(3),
        name="scatter_last",
    )(*grads, values)


def head_spread(channels):
    return (iota((LANES, channels), 1) // MP == iota((LANES, channels), 0)).astype(BF16)


def parts(values, count):
    terms = []
    for _ in range(count):
        term = values.astype(BF16)
        terms.append(term)
        values = values - term.astype(F32)
    return terms


def pick(values, mask, count=2):
    return dot(jnp.concatenate(parts(values, count), axis=1), jnp.concatenate([mask] * count, axis=0))


def pick_left(mask, values, count):
    return dot(jnp.concatenate([mask] * count, axis=1), jnp.concatenate(parts(values, count), axis=0))


def gather_heads(values, spread):
    high, low = parts(values, 2)
    return dot(high, spread, NT) + dot(low, spread, NT)


def row_sums(values):
    high, low = parts(values, 2)
    ones = jnp.ones((EDGE, values.shape[1]), BF16)
    return dot(ones, high, NT) + dot(ones, low, NT)


def soft_step(raw):
    return jnp.maximum(raw, 0.0) + jnp.log1p(jnp.exp(-jnp.abs(raw)))


def conv_window(buffer, taps_ref, bias_ref, span):
    total = bias_ref[...] + taps_ref[0:1, :] * buffer[EDGE - 3 : EDGE - 3 + span, :]
    for tap in range(1, KCONV):
        start = EDGE - 3 + tap
        total = total + taps_ref[tap : tap + 1, :] * buffer[start : start + span, :]
    return total


def span_rates(step_ref, bias_ref, decay_ref, spread, span):
    raw = step_ref[...] + bias_ref[...]
    step = soft_step(raw)
    lower = (iota((span, span), 1) <= iota((span, span), 0)).astype(BF16)
    cum = pick_left(lower, step * decay_ref[...], 3)
    tails = jnp.exp(cum[span - 1 : span, :] - cum)
    wide = pick(jnp.concatenate([step, tails, jnp.exp(cum)], axis=0), spread)
    return raw, step, cum, wide[:span], wide[span : 2 * span], wide[2 * span :]


def pair_split(values, low_lanes):
    zero = jnp.zeros_like(values)
    return jnp.concatenate(
        [jnp.where(low_lanes, values, zero), jnp.where(low_lanes, zero, values)], axis=0
    )


def pair_decay(cum, cum_rows, pair, causal):
    parts = []
    for head in (2 * pair, 2 * pair + 1):
        differ = cum[:, head : head + 1] - cum_rows[head : head + 1, :]
        parts.append(jnp.exp(jnp.where(causal, differ, MASKED)))
    return parts


def scan_forward(
    devices, spans,
    z_ref, x_ref, bc_ref, step_ref,
    tap_ref, bias_ref, tapb_ref, biasb_ref, stepb_ref, decay_ref, skip_ref, shard_ref,
    y_ref, gated_ref, square_ref, enter_ref, all_ref,
    state, xbuf, bbuf, *sems,
):
    span, channels = x_ref.shape
    ring = RingGather(devices, shard_ref, all_ref, sems)
    turn = pl.program_id(0)

    @pl.when(turn == 0)
    def _():
        ring.greet()
        ring.begin()


    @pl.when(pl.program_id(0) == 0)
    def _():
        state[...] = jnp.zeros_like(state)
        xbuf[span:, :] = jnp.zeros((EDGE, channels), F32)
        bbuf[span:, :] = jnp.zeros((EDGE, 2 * NS), F32)

    xbuf[:EDGE, :] = xbuf[span:, :]
    bbuf[:EDGE, :] = bbuf[span:, :]
    xbuf[EDGE:, :] = x_ref[...]
    bbuf[EDGE:, :] = bc_ref[...]
    inputs = jax.nn.silu(conv_window(xbuf, tap_ref, bias_ref, span))
    shared = jax.nn.silu(conv_window(bbuf, tapb_ref, biasb_ref, span))
    spread = head_spread(channels)
    _, step, cum, step_w, tails_w, grown_w = span_rates(
        step_ref, stepb_ref, decay_ref, spread, span
    )
    cum_rows = cum.T
    b_low = shared[:, :NS].astype(BF16)
    c_low = shared[:, NS:].astype(BF16)
    scaled = inputs * step_w
    scaled_low = scaled.astype(BF16)
    enter_ref[0] = state[...]
    outer = dot(c_low, state[...].astype(BF16)) * grown_w
    fresh = dot(b_low, (scaled * tails_w).astype(BF16), TN)
    state[...] = state[...] * grown_w[span - 1 : span, :] + fresh
    cross = dot(c_low, b_low, NT)
    causal = iota((span, span), 1) <= iota((span, span), 0)
    low_lanes = iota((span, LANES), 1) < MP
    for pair in range(channels // LANES):
        lanes = slice(pair * LANES, (pair + 1) * LANES)
        first, second = pair_decay(cum, cum_rows, pair, causal)
        weights = jnp.concatenate(
            [(cross * first).astype(BF16), (cross * second).astype(BF16)], axis=1
        )
        y_ref[:, lanes] = dot(weights, pair_split(scaled_low[:, lanes], low_lanes))
    y = y_ref[...] + outer + skip_ref[...] * inputs
    y_ref[...] = y
    gated = y * jax.nn.silu(z_ref[...])
    gated_ref[...] = gated
    square_ref[...] = row_sums(gated * gated)

    count = spans
    for step in range(1, ring.ahead + 1):
        pl.when(turn == min(count - 1, count * step // ring.ahead))(
            functools.partial(ring.hop, step)
        )
    pl.when(turn == count - 1)(ring.finish)


def scan_backward(
    devices, spans, windows, pieces, count,
    z_ref, x_ref, xp_ref, bc_ref, bp_ref, step_ref, y_ref, enter_ref,
    dyg_ref, scale_ref, inner_ref, dqkv_ref,
    tap_ref, bias_ref, tapb_ref, biasb_ref, stepb_ref, decay_ref, skip_ref, gain_ref,
    *refs,
):
    sent, refs = refs[:count], refs[count:]
    (grad_ref, gx_ref, gb_ref, gh_ref), refs = refs[:4], refs[4:]
    outs, refs = refs[: len(pieces)], refs[len(pieces) :]
    (dstate, xbuf, bbuf, dxbuf, dbbuf, du_buf, col_buf), scratch = refs[:7], refs[7:]
    ring = RingScatter(devices, windows, pieces, sent, outs, scratch)
    span, channels = x_ref.shape
    turn = pl.program_id(0)

    @pl.when(turn == 0)
    def _():
        ring.greet()
        ring.begin()
        dstate[...] = jnp.zeros_like(dstate)
        dxbuf[...] = jnp.zeros_like(dxbuf)
        dbbuf[...] = jnp.zeros_like(dbbuf)
        col_buf[...] = jnp.zeros_like(col_buf)
        gx_ref[...] = jnp.zeros_like(gx_ref)
        gb_ref[...] = jnp.zeros_like(gb_ref)
        gh_ref[...] = jnp.zeros_like(gh_ref)

    inside = (turn < spans - 1).astype(F32)
    xbuf[:EDGE, :] = xp_ref[...] * inside
    bbuf[:EDGE, :] = bp_ref[...] * inside
    xbuf[EDGE:, :] = x_ref[...]
    bbuf[EDGE:, :] = bc_ref[...]
    conv = conv_window(xbuf, tap_ref, bias_ref, span)
    sig = jax.nn.sigmoid(conv)
    inputs = conv * sig
    convb = conv_window(bbuf, tapb_ref, biasb_ref, span)
    sigb = jax.nn.sigmoid(convb)
    shared = convb * sigb
    b_low = shared[:, :NS].astype(BF16)
    c_low = shared[:, NS:].astype(BF16)
    spread = head_spread(channels)
    raw, step, cum, step_w, tails_w, grown_w = span_rates(
        step_ref, stepb_ref, decay_ref, spread, span
    )
    cum_rows = cum.T
    scaled = inputs * step_w
    scaled_low = scaled.astype(BF16)

    z = z_ref[...]
    sig_z = jax.nn.sigmoid(z)
    swish = z * sig_z
    y = y_ref[...]
    scale = scale_ref[...].T[:, :1]
    normed = y * swish * scale
    dyg = dyg_ref[...]
    gain_grad = jnp.sum(dyg * normed, axis=0, keepdims=True)
    dgated = scale * (dyg * gain_ref[...] - normed * inner_ref[...].T[:, :1])
    dy = dgated * swish
    grad_ref[:, :channels] = (dgated * y * (sig_z * (1.0 + z * (1.0 - sig_z)))).astype(BF16)

    state_low = enter_ref[0].astype(BF16)
    dstate_low = dstate[...].astype(BF16)
    grown_low = (dy * grown_w).astype(BF16)
    dy_low = dy.astype(BF16)
    tailed = scaled * tails_w
    outer = dot(c_low, state_low) * grown_w
    from_state = dot(b_low, dstate_low)
    dc = dot(grown_low, state_low, NT)
    db = dot(tailed.astype(BF16), dstate_low, NT)
    leak = from_state * tailed
    last_w = grown_w[span - 1 : span, :]
    ends = (
        jnp.sum(leak, axis=0, keepdims=True)
        + jnp.sum(enter_ref[0] * dstate[...], axis=0, keepdims=True) * last_w
    )
    skips = jnp.sum(dy * inputs, axis=0, keepdims=True)
    dstate[...] = dstate[...] * last_w + dot(c_low, grown_low, TN)

    cross = dot(c_low, b_low, NT)
    causal = iota((span, span), 1) <= iota((span, span), 0)
    low_lanes = iota((span, LANES), 1) < MP
    lane = iota((span, LANES), 1)
    dcross = jnp.zeros((span, span), F32)
    row_part = jnp.zeros((span, LANES), F32)
    for pair in range(channels // LANES):
        lanes = slice(pair * LANES, (pair + 1) * LANES)
        decays = pair_decay(cum, cum_rows, pair, causal)
        dy_pair = pair_split(dy_low[:, lanes], low_lanes)
        dweights = dot(dy_pair, scaled_low[:, lanes], NT)
        both = []
        for part in range(2):
            head = 2 * pair + part
            dterm = dweights[part * span : (part + 1) * span] * decays[part]
            dcross = dcross + dterm
            flow = dterm * cross
            row_part = row_part + jnp.where(
                lane == head, jnp.sum(flow, axis=1, keepdims=True), 0.0
            )
            col_buf[head : head + 1, :] = jnp.sum(flow, axis=0, keepdims=True)
            both.append((cross * decays[part]).astype(BF16))
        du_buf[:, lanes] = dot(jnp.concatenate(both, axis=0), dy_pair, TN)
    du = du_buf[...] + from_state * tails_w
    dcross_low = dcross.astype(BF16)
    dc = dc + dot(dcross_low, b_low)
    db = db + dot(dcross_low, c_low, TN)

    sums = gather_heads(
        jnp.concatenate(
            [dy * outer - leak, du * inputs, ends, skips, jnp.zeros((EDGE - 2, channels), F32)],
            axis=0,
        ),
        spread,
    )
    at_end = sums[2 * span : 2 * span + 1, :]
    dcum = sums[:span] + row_part - col_buf[...].T
    upper = (iota((span, span), 1) >= iota((span, span), 0)).astype(BF16)
    drate = pick_left(upper, dcum, 3) + at_end
    dstep = drate * decay_ref[...] + sums[span : 2 * span]
    draw = dstep * jax.nn.sigmoid(raw)
    gh_ref[0:1, :] += jnp.sum(draw, axis=0, keepdims=True)
    gh_ref[1:2, :] += jnp.sum(drate * step, axis=0, keepdims=True) * decay_ref[...]
    gh_ref[2:3, :] += sums[2 * span + 1 : 2 * span + 2, :]

    dinputs = du * step_w + skip_ref[...] * dy
    dxbuf[span:, :] = dxbuf[:EDGE, :]
    dbbuf[span:, :] = dbbuf[:EDGE, :]
    dconv = dinputs * (sig * (1.0 + conv * (1.0 - sig)))
    dconvb = jnp.concatenate([db, dc], axis=1) * (sigb * (1.0 + convb * (1.0 - sigb)))
    dxbuf[:span, :] = dconv
    dbbuf[:span, :] = dconvb
    dx = jnp.zeros_like(dconv)
    dbc = jnp.zeros_like(dconvb)
    for tap in range(KCONV):
        back = KCONV - 1 - tap
        start = EDGE - 3 + tap
        dx = dx + tap_ref[tap : tap + 1, :] * dxbuf[back : back + span, :]
        dbc = dbc + tapb_ref[tap : tap + 1, :] * dbbuf[back : back + span, :]
        gx_ref[tap : tap + 1, :] += jnp.sum(
            dconv * xbuf[start : start + span, :], axis=0, keepdims=True
        )
        gb_ref[tap : tap + 1, :] += jnp.sum(
            dconvb * bbuf[start : start + span, :], axis=0, keepdims=True
        )
    gx_ref[KCONV : KCONV + 1, :] += jnp.sum(dconv, axis=0, keepdims=True)
    gb_ref[KCONV : KCONV + 1, :] += jnp.sum(dconvb, axis=0, keepdims=True)
    gx_ref[KCONV + 1 : KCONV + 2, :] += gain_grad
    width = 2 * channels + 2 * NS
    grad_ref[:, channels : 2 * channels] = dx.astype(BF16)
    grad_ref[:, 2 * channels : width] = dbc.astype(BF16)
    grad_ref[:, width : width + dqkv_ref.shape[1]] = dqkv_ref[...]
    grad_ref[:, width + dqkv_ref.shape[1] :] = draw.astype(BF16)
    for step in range(ring.ahead):
        pl.when(turn == spans * step // ring.ahead)(functools.partial(ring.hop, step))
    pl.when(turn == spans - 1)(ring.finish)


def scan_params(conv_x, conv_xb, conv_bc, conv_bcb, dt_bias, a_log, d_skip):
    heads = dt_bias.shape[0]

    def wide(row):
        return jnp.pad(row, (0, LANES - heads))[None, :]

    f32 = lambda value: value.astype(F32)
    return (
        f32(conv_x),
        f32(conv_xb)[None, :],
        f32(conv_bc),
        f32(conv_bcb)[None, :],
        wide(f32(dt_bias)),
        wide(-jnp.exp(f32(a_log))),
        jnp.repeat(f32(d_skip), MP)[None, :],
    )


def whole_spec(array):
    return pl.BlockSpec(array.shape, lambda turn: (0,) * array.ndim)


def run_scan_forward(proj, qkv_width, params, shard, devices):
    tokens = proj.shape[0]
    channels = params[1].shape[1]
    step_at = (2 * channels + 2 * NS + qkv_width) // LANES
    spans = tokens // SPAN
    bc_at = 2 * channels // (2 * NS)
    rows = lambda width, at: pl.BlockSpec((SPAN, width), lambda turn: (turn, at))
    anywhere = pl.BlockSpec(memory_space=pl.ANY)
    return pl.pallas_call(
        functools.partial(scan_forward, devices, spans),
        grid=(spans,),
        out_shape=(
            jax.ShapeDtypeStruct((tokens, channels), F32),
            jax.ShapeDtypeStruct((tokens, channels), F32),
            jax.ShapeDtypeStruct((EDGE, tokens), F32),
            jax.ShapeDtypeStruct((spans, NS, channels), F32),
            gather_shape(shard, devices),
        ),
        in_specs=[rows(channels, 0), rows(channels, 1), rows(2 * NS, bc_at), rows(LANES, step_at)]
        + [whole_spec(item) for item in params]
        + [anywhere],
        out_specs=(
            rows(channels, 0),
            rows(channels, 0),
            pl.BlockSpec((EDGE, SPAN), lambda turn: (0, turn)),
            pl.BlockSpec((1, NS, channels), lambda turn: (turn, 0, 0)),
            anywhere,
        ),
        scratch_shapes=[
            pltpu.VMEM((NS, channels), F32),
            pltpu.VMEM((SPAN + EDGE, channels), F32),
            pltpu.VMEM((SPAN + EDGE, 2 * NS), F32),
        ]
        + gather_sems(devices),
        compiler_params=pltpu.CompilerParams(collective_id=2, has_side_effects=True),
        cost_estimate=cost(20),
        name="scan_forward",
    )(proj, proj, proj, proj, *params, shard)


def run_scan_backward(
    proj, y, entering, dyg, scale, inner, dqkv, params, gain, sent, windows, pieces,
    devices,
):
    tokens, width = proj.shape
    channels = params[1].shape[1]
    qkv_width = dqkv.shape[1]
    step_at = (2 * channels + 2 * NS + qkv_width) // LANES
    spans = tokens // SPAN
    bc_at = 2 * channels // (2 * NS)
    edges = SPAN // EDGE
    rows = lambda size, at: pl.BlockSpec((SPAN, size), lambda turn: (spans - 1 - turn, at))
    edge = lambda size, at: pl.BlockSpec(
        (EDGE, size), lambda turn: (jnp.maximum((spans - 1 - turn) * edges - 1, 0), at)
    )
    keep = lambda shape: pl.BlockSpec(shape, lambda turn: (0, 0))
    shapes = scatter_shapes(sent, pieces, devices)
    return pl.pallas_call(
        functools.partial(scan_backward, devices, spans, windows, pieces, len(sent)),
        grid=(spans,),
        out_shape=(
            jax.ShapeDtypeStruct((tokens, width), BF16),
            jax.ShapeDtypeStruct((EDGE, channels), F32),
            jax.ShapeDtypeStruct((EDGE, 2 * NS), F32),
            jax.ShapeDtypeStruct((EDGE, LANES), F32),
        )
        + shapes,
        in_specs=[
            rows(channels, 0),
            rows(channels, 1),
            edge(channels, 1),
            rows(2 * NS, bc_at),
            edge(2 * NS, bc_at),
            rows(LANES, step_at),
            rows(channels, 0),
            pl.BlockSpec((1, NS, channels), lambda turn: (spans - 1 - turn, 0, 0)),
            rows(channels, 0),
            pl.BlockSpec((EDGE, SPAN), lambda turn: (0, spans - 1 - turn)),
            pl.BlockSpec((EDGE, SPAN), lambda turn: (0, spans - 1 - turn)),
            rows(qkv_width, 0),
        ]
        + [whole_spec(item) for item in params]
        + [whole_spec(gain)]
        + [pl.BlockSpec(memory_space=pl.ANY)] * len(sent),
        out_specs=(
            rows(width, 0),
            keep((EDGE, channels)),
            keep((EDGE, 2 * NS)),
            keep((EDGE, LANES)),
        )
        + tuple(keep(item.shape) for item in shapes),
        scratch_shapes=[
            pltpu.VMEM((NS, channels), F32),
            pltpu.VMEM((SPAN + EDGE, channels), F32),
            pltpu.VMEM((SPAN + EDGE, 2 * NS), F32),
            pltpu.VMEM((SPAN + EDGE, channels), F32),
            pltpu.VMEM((SPAN + EDGE, 2 * NS), F32),
            pltpu.VMEM((SPAN, channels), F32),
            pltpu.VMEM((LANES, SPAN), F32),
        ]
        + scatter_scratch(sent, windows, devices),
        compiler_params=pltpu.CompilerParams(collective_id=6, has_side_effects=True),
        cost_estimate=cost(47),
        name="scan_backward",
    )(
        proj, proj, proj, proj, proj, proj, y, entering, dyg, scale, inner, dqkv, *params, gain,
        *sent,
    )


def rotary_tables(tokens):
    half = HEAD_SIZE // 2
    exponent = np.arange(half, dtype=np.float64) * (-2.0 * LOG_BASE / HEAD_SIZE)
    rates = np.tile(np.exp(exponent.astype(np.float32)).astype(np.float64), LANES // half)
    tables = []
    for places in (np.arange(FINE), np.arange(0, tokens, FINE)):
        angles = places[:, None] * rates[None, :]
        tables += [np.cos(angles).astype(np.float32), np.sin(angles).astype(np.float32)]
    return tables


def fill_rotary(fine_cos, fine_sin, coarse_cos, coarse_sin, cosine, sine):
    small_cos, small_sin = fine_cos[...], fine_sin[...]
    for turn in range(coarse_cos.shape[0]):
        big_cos, big_sin = coarse_cos[turn : turn + 1, :], coarse_sin[turn : turn + 1, :]
        rows = slice(turn * FINE, (turn + 1) * FINE)
        cosine[rows, :] = small_cos * big_cos - small_sin * big_sin
        sine[rows, :] = small_sin * big_cos + small_cos * big_sin


def head_masks():
    half = HEAD_SIZE // 2
    row, col = iota((LANES, LANES), 0), iota((LANES, LANES), 1)
    place = col % HEAD_SIZE
    ahead = jnp.where(place < half, -1.0, 0.0)
    behind = jnp.where(place < half, 0.0, 1.0)

    def turn(start):
        return jnp.where(row == start + half, ahead, jnp.where(row == start - half, behind, 0.0))

    first = row < HEAD_SIZE
    left = col < HEAD_SIZE
    low = lambda mask: mask.astype(BF16)
    within = low(turn(col))
    copy = low(jnp.where(row == place, 1.0, 0.0))
    copy_turn = low(jnp.where(first, turn(place), 0.0))
    value = low(jnp.where(row == place + HEAD_SIZE, 1.0, 0.0))
    fold = low(jnp.where(left & (row % HEAD_SIZE == place), 1.0, 0.0))
    other = row % HEAD_SIZE
    fold_turn = low(
        jnp.where(
            left,
            jnp.where(other == place + half, ahead, jnp.where(other == place - half, behind, 0.0)),
            0.0,
        )
    )
    fold_value = low(jnp.where(left, 0.0, jnp.where(other == place, 1.0, 0.0)))
    return within, copy, copy_turn, value, fold, fold_turn, fold_value


def attend_forward(
    q_ref, kv_ref, fine_cos, fine_sin, coarse_cos, coarse_sin,
    qkv_ref, lse_ref, o_ref, vt, cos_ref, sin_ref,
):
    fill_rotary(fine_cos, fine_sin, coarse_cos, coarse_sin, cos_ref, sin_ref)
    tokens, query_width = q_ref.shape
    pairs = query_width // LANES
    within, copy, copy_turn, value = head_masks()[:4]
    for start in range(0, tokens, QBLK):
        rows = slice(start, start + QBLK)
        cosine, sine = cos_ref[rows, :], sin_ref[rows, :]
        for pair in range(pairs):
            lanes = slice(pair * LANES, (pair + 1) * LANES)
            query = q_ref[rows, lanes]
            turned = query * cosine + pick(query, within) * sine
            qkv_ref[rows, lanes] = (turned * HEAD_SIZE**-0.5).astype(BF16)
        kv = kv_ref[rows, :]
        keys = pick(kv, copy) * cosine + pick(kv, copy_turn) * sine
        qkv_ref[rows, query_width : query_width + LANES] = keys.astype(BF16)
        qkv_ref[rows, query_width + LANES :] = dot(kv.astype(BF16), value).astype(BF16)
        vt[:, rows] = kv.T[HEAD_SIZE:, :].astype(BF16)
    low_lanes = iota((QBLK, LANES), 1) < HEAD_SIZE
    wide = (QBLK, 2 * QBLK)
    visible = iota(wide, 0) <= iota(wide, 1) % QBLK

    def block(i, carry):
        here = pl.ds(pl.multiple_of(i * QBLK, QBLK), QBLK)
        queries = [
            pair_split(qkv_ref[here, pair * LANES : (pair + 1) * LANES], low_lanes)
            for pair in range(pairs)
        ]

        def tile(there, state, edge):
            keys = qkv_ref[there, query_width : query_width + LANES]
            result = []
            for pair in range(pairs):
                top, total, out = state[3 * pair : 3 * pair + 3]
                scores = dot(keys, queries[pair], NT)
                if edge:
                    scores = jnp.where(visible, scores, MASKED)
                higher = jnp.maximum(top, jnp.max(scores, axis=0, keepdims=True))
                probs = jnp.exp(scores - higher)
                fade = jnp.exp(top - higher)
                total = total * fade + jnp.sum(probs, axis=0, keepdims=True)
                out = out * fade + dot(vt[:, there], probs.astype(BF16))
                result += [higher, total, out]
            return tuple(result)

        state = (
            jnp.full((1, 2 * QBLK), MASKED, F32),
            jnp.zeros((1, 2 * QBLK), F32),
            jnp.zeros((HEAD_SIZE, 2 * QBLK), F32),
        ) * pairs
        state = lax.fori_loop(
            0,
            i,
            lambda j, state: tile(pl.ds(pl.multiple_of(j * QBLK, QBLK), QBLK), state, False),
            state,
        )
        state = tile(here, state, True)
        for pair in range(pairs):
            top, total, out = state[3 * pair : 3 * pair + 3]
            out = out / total
            lse = top + jnp.log(total)
            lse_ref[2 * pair : 2 * pair + 1, here] = lse[:, :QBLK]
            lse_ref[2 * pair + 1 : 2 * pair + 2, here] = lse[:, QBLK:]
            both = jnp.concatenate([out[:, :QBLK], out[:, QBLK:]], axis=0)
            o_ref[here, pair * LANES : (pair + 1) * LANES] = both.T.astype(BF16)
        return carry

    lax.fori_loop(0, tokens // QBLK, block, 0)


def attend_backward(
    qkv_ref, lse_ref, o_ref, do_ref, fine_cos, fine_sin, coarse_cos, coarse_sin,
    dqkv_ref,
    dq, kt, dk, dv, cos_ref, sin_ref,
):
    fill_rotary(fine_cos, fine_sin, coarse_cos, coarse_sin, cos_ref, sin_ref)
    tokens, query_width = o_ref.shape
    pairs = query_width // LANES
    key_lanes = slice(query_width, query_width + LANES)
    value_lanes = slice(query_width + LANES, query_width + 2 * LANES)
    for start in range(0, tokens, QBLK):
        rows = slice(start, start + QBLK)
        kt[:, rows] = qkv_ref[rows, key_lanes].astype(F32).T[:HEAD_SIZE, :].astype(BF16)
    dk[...] = jnp.zeros_like(dk)
    dv[...] = jnp.zeros_like(dv)
    low_lanes = iota((QBLK, LANES), 1) < HEAD_SIZE
    wide = (QBLK, 2 * QBLK)
    visible = iota(wide, 0) <= iota(wide, 1) % QBLK
    ones = jnp.ones((EDGE, LANES), BF16)

    def block(i, carry):
        here = pl.ds(pl.multiple_of(i * QBLK, QBLK), QBLK)
        queries, grads, inners, lses = [], [], [], []
        for pair in range(pairs):
            lanes = slice(pair * LANES, (pair + 1) * LANES)
            queries.append(pair_split(qkv_ref[here, lanes], low_lanes))
            grad = do_ref[here, lanes]
            grads.append(pair_split(grad, low_lanes))
            both = pair_split(grad.astype(F32) * o_ref[here, lanes].astype(F32), low_lanes)
            high, low = parts(both, 2)
            inners.append((dot(ones, high, NT) + dot(ones, low, NT))[:1])
            lses.append(
                jnp.concatenate(
                    [
                        lse_ref[2 * pair : 2 * pair + 1, here],
                        lse_ref[2 * pair + 1 : 2 * pair + 2, here],
                    ],
                    axis=1,
                )
            )
        query_all = jnp.concatenate(queries, axis=0)
        grad_all = jnp.concatenate(grads, axis=0)

        def tile(there, state, edge):
            keys = qkv_ref[there, key_lanes]
            values = qkv_ref[there, value_lanes]
            all_probs, all_dscores, result = [], [], []
            for pair in range(pairs):
                probs = dot(keys, queries[pair], NT) - lses[pair]
                if edge:
                    probs = jnp.where(visible, probs, MASKED)
                probs = jnp.exp(probs)
                dprobs = dot(values, grads[pair], NT)
                dscores = (probs * (dprobs - inners[pair])).astype(BF16)
                all_probs.append(probs.astype(BF16))
                all_dscores.append(dscores)
                result.append(state[pair] + dot(kt[:, there], dscores))
            dv[there, :] += dot(jnp.concatenate(all_probs, axis=1), grad_all)
            dk[there, :] += dot(jnp.concatenate(all_dscores, axis=1), query_all)
            return tuple(result)

        state = (jnp.zeros((HEAD_SIZE, 2 * QBLK), F32),) * pairs
        state = lax.fori_loop(
            0,
            i,
            lambda j, state: tile(pl.ds(pl.multiple_of(j * QBLK, QBLK), QBLK), state, False),
            state,
        )
        state = tile(here, state, True)
        for pair in range(pairs):
            both = jnp.concatenate([state[pair][:, :QBLK], state[pair][:, QBLK:]], axis=0)
            dq[here, pair * LANES : (pair + 1) * LANES] = both.T
        return carry

    lax.fori_loop(0, tokens // QBLK, block, 0)
    masks = head_masks()
    within, (fold, fold_turn, fold_value) = masks[0], masks[4:]
    for start in range(0, tokens, QBLK):
        rows = slice(start, start + QBLK)
        cosine, sine = cos_ref[rows, :], sin_ref[rows, :]
        for pair in range(pairs):
            lanes = slice(pair * LANES, (pair + 1) * LANES)
            grad = dq[rows, lanes]
            grad = grad * cosine - pick(grad, within) * sine
            dqkv_ref[rows, lanes] = (grad * HEAD_SIZE**-0.5).astype(BF16)
        grad = dk[rows, :]
        grad = pick(grad, fold) * cosine - pick(grad, fold_turn) * sine
        grad = grad + pick(dv[rows, :], fold_value)
        dqkv_ref[rows, query_width:] = grad.astype(BF16)


def run_attend_forward(proj, query_at, query_width, tables):
    tokens = proj.shape[0]
    cols = lambda size, at: pl.BlockSpec((tokens, size), lambda turn: (0, at // size))
    return pl.pallas_call(
        attend_forward,
        grid=(1,),
        out_shape=(
            jax.ShapeDtypeStruct((tokens, query_width + 2 * LANES), BF16),
            jax.ShapeDtypeStruct((EDGE, tokens), F32),
            jax.ShapeDtypeStruct((tokens, query_width), BF16),
        ),
        in_specs=[
            cols(query_width, query_at),
            cols(2 * HEAD_SIZE, query_at + query_width),
        ]
        + [whole_spec(table) for table in tables],
        out_specs=(
            cols(query_width + 2 * LANES, 0),
            pl.BlockSpec((EDGE, tokens), lambda turn: (0, 0)),
            cols(query_width, 0),
        ),
        scratch_shapes=[
            pltpu.VMEM((HEAD_SIZE, tokens), BF16),
            pltpu.VMEM((tokens, LANES), F32),
            pltpu.VMEM((tokens, LANES), F32),
        ],
        cost_estimate=cost(15),
        name="attend_forward",
    )(proj, proj, *tables)


def run_attend_backward(qkv, lse, attended, grads, grad_at, tables):
    tokens, query_width = attended.shape
    vmem = pl.BlockSpec(memory_space=pltpu.VMEM)
    cols = lambda size, at: pl.BlockSpec((tokens, size), lambda turn: (0, at // size))
    return pl.pallas_call(
        attend_backward,
        grid=(1,),
        out_shape=jax.ShapeDtypeStruct((tokens, query_width + 2 * HEAD_SIZE), BF16),
        in_specs=[
            whole_spec(qkv),
            whole_spec(lse),
            whole_spec(attended),
            cols(query_width, grad_at),
        ]
        + [whole_spec(table) for table in tables],
        out_specs=cols(query_width + 2 * HEAD_SIZE, 0),
        scratch_shapes=[
            pltpu.VMEM((tokens, query_width), F32),
            pltpu.VMEM((HEAD_SIZE, tokens), BF16),
            pltpu.VMEM((tokens, LANES), F32),
            pltpu.VMEM((tokens, LANES), F32),
            pltpu.VMEM((tokens, LANES), F32),
            pltpu.VMEM((tokens, LANES), F32),
        ],
        cost_estimate=cost(16),
        name="attend_backward",
    )(qkv, lse, attended, grads, *tables)


def feed_forward(
    x_ref, mixed_ref, other_ref, top_ref, gain_ref, gu_ref, down_ref, *refs,
):
    back_ref, after_ref, scale_ref, hidden_ref, act_ref, dgu_ref, part_ref = refs[-7:]
    units = down_ref.shape[1]
    after = x_ref[...].astype(F32) + (mixed_ref[...].astype(F32) + other_ref[...].astype(F32))
    after_ref[...] = after
    scale = lax.rsqrt(jnp.mean(after * after, axis=-1, keepdims=True) + EPSILON)
    scale_ref[...] = scale
    hidden = (after * scale * gain_ref[...]).astype(BF16)
    hidden_ref[...] = hidden
    top = top_ref[...]
    for start in range(0, units, UBLK):
        cols = slice(start, start + UBLK)
        up_cols = slice(units + start, units + start + UBLK)
        gate = dot(hidden, gu_ref[:, cols])
        upward = dot(hidden, gu_ref[:, up_cols])
        grad = dot(top, down_ref[:, cols])
        sigma = jax.nn.sigmoid(gate)
        swish = gate * sigma
        act_ref[:, cols] = (swish * upward).astype(BF16)
        slope = sigma * (1.0 + gate * (1.0 - sigma))
        dgu_ref[:, cols] = (grad * upward * slope).astype(BF16)
        dgu_ref[:, up_cols] = (grad * swish).astype(BF16)
    back_ref[...] = dot(dgu_ref[...], gu_ref[...], NT).astype(BF16)
    part_ref[...] = dot(act_ref[...], down_ref[...], NT).astype(BF16)


def once(item):
    return pl.BlockSpec(item.shape, lambda turn: (0, 0), pipeline_mode=pl.Buffered(1))


def run_feed_forward(half, x, mixed, other, top, gain, w_gate_up, w_down_t, before=()):
    tokens, width = x.shape
    units = w_down_t.shape[1]
    turns = tokens // TBLK // 2
    rows = lambda size: pl.BlockSpec((TBLK, size), lambda turn: (turn + half * turns, 0))
    shape = jax.ShapeDtypeStruct
    return pl.pallas_call(
        feed_forward,
        grid=(turns,),
        out_shape=(
            shape((tokens // 2, width), BF16),
            shape((tokens, width), F32),
            shape((tokens, 1), F32),
            shape((tokens, width), BF16),
            shape((tokens, units), BF16),
            shape((tokens, 2 * units), BF16),
            shape((tokens, width), BF16),
        ),
        in_specs=[rows(width)] * 4
        + [once(gain), once(w_gate_up), once(w_down_t)]
        + [pl.BlockSpec(memory_space=pl.ANY)] * len(before),
        out_specs=(
            pl.BlockSpec((TBLK, width), lambda turn: (turn, 0)),
            rows(width), rows(1), rows(width), rows(units), rows(2 * units), rows(width),
        ),
        input_output_aliases={7 + i: 1 + i for i in range(len(before))},
        cost_estimate=cost(10),
        name="feed_forward",
    )(x, mixed, other, top, gain, w_gate_up, w_down_t, *before)


def mixer_forward(gated_ref, scale_ref, gain_ref, attended_ref, w_ref, low_ref, mixed_ref):
    channels = gated_ref.shape[1]
    scale = scale_ref[...].T[:, :1]
    low_ref[:, :channels] = (gated_ref[...] * scale * gain_ref[...]).astype(BF16)
    low_ref[:, channels:] = attended_ref[...]
    mixed_ref[...] = dot(low_ref[...], w_ref[...], NT).astype(BF16)


def run_mixer_forward(gated, scale, gain, attended, w_out):
    tokens, channels = gated.shape
    width, inner = w_out.shape
    rows = lambda size: pl.BlockSpec((TBLK, size), lambda turn: (turn, 0))
    return pl.pallas_call(
        mixer_forward,
        grid=(tokens // TBLK,),
        out_shape=(
            jax.ShapeDtypeStruct((tokens, inner), BF16),
            jax.ShapeDtypeStruct((tokens, width), BF16),
        ),
        in_specs=[
            rows(channels),
            pl.BlockSpec((EDGE, TBLK), lambda turn: (0, turn)),
            once(gain),
            rows(attended.shape[1]),
            once(w_out),
        ],
        out_specs=(rows(inner), rows(width)),
        cost_estimate=cost(5),
        name="mixer_forward",
    )(gated, scale, gain, attended, w_out)


def mixer_backward(
    pa_ref, oa_ref, pb_ref, ob_ref, after_ref, scale_ref, top_ref, gain_ref,
    w_ref, gated_ref, scale_m_ref, gain_m_ref,
    grad_ref, low_ref, mamba_ref, attended_ref, inner_ref, gain_grad_ref,
):
    turn = pl.program_id(0)
    channels = gated_ref.shape[1]

    @pl.when(turn == 0)
    def _():
        gain_grad_ref[...] = jnp.zeros_like(gain_grad_ref)

    first = turn < pl.num_programs(0) // 2
    grad = jnp.where(
        first,
        pa_ref[...].astype(F32) + oa_ref[...].astype(F32),
        pb_ref[...].astype(F32) + ob_ref[...].astype(F32),
    )
    scale = scale_ref[...]
    normed = after_ref[...] * scale
    gain_grad_ref[:1, :] += jnp.sum(grad * normed, axis=0, keepdims=True)
    weighted = grad * gain_ref[...]
    mean = jnp.mean(weighted * normed, axis=-1, keepdims=True)
    total = top_ref[...].astype(F32) + scale * (weighted - normed * mean)
    grad_ref[...] = total
    low_ref[...] = total.astype(BF16)
    back = dot(low_ref[...], w_ref[...])
    mamba = back[:, :channels]
    mamba_ref[...] = mamba
    attended_ref[...] = back[:, channels:].astype(BF16)
    inner_ref[...] = row_sums(mamba * gain_m_ref[...] * gated_ref[...]) * scale_m_ref[...]


def run_mixer_backward(halves, after, scale, top, gain, w_out, gated, scale_m, gain_m):
    tokens, width = after.shape
    channels = gated.shape[1]
    inner = w_out.shape[1]
    turns = tokens // TBLK
    shape = jax.ShapeDtypeStruct
    rows = lambda size: pl.BlockSpec((TBLK, size), lambda turn: (turn, 0))
    lanes = pl.BlockSpec((EDGE, TBLK), lambda turn: (0, turn))
    low_half = pl.BlockSpec((TBLK, width), lambda turn: (jnp.minimum(turn, turns // 2 - 1), 0))
    high_half = pl.BlockSpec((TBLK, width), lambda turn: (jnp.maximum(turn - turns // 2, 0), 0))
    return pl.pallas_call(
        mixer_backward,
        grid=(turns,),
        out_shape=(
            shape((tokens, width), F32),
            shape((tokens, width), BF16),
            shape((tokens, channels), F32),
            shape((tokens, inner - channels), BF16),
            shape((EDGE, tokens), F32),
            shape((EDGE, width), F32),
        ),
        in_specs=[low_half] * 2
        + [high_half] * 2
        + [rows(width), rows(1), rows(width), once(gain), once(w_out), rows(channels), lanes]
        + [once(gain_m)],
        out_specs=(
            rows(width), rows(width), rows(channels), rows(inner - channels), lanes,
            pl.BlockSpec((EDGE, width), lambda turn: (0, 0)),
        ),
        cost_estimate=cost(8),
        name="mixer_backward",
    )(*halves, after, scale, top, gain, w_out, gated, scale_m, gain_m)


def swap(partial):
    return lax.ppermute(partial, "tensor", [(0, 1), (1, 0)])


def join(mine, other):
    return mine.astype(F32) + other.astype(F32)


def tensor_sum(partial):
    return join(partial, swap(partial))


def local(
    layer_input, w_norm1, w_zx, w_bc, w_dt, conv_x, conv_xb, conv_bc, conv_bcb, dt_bias, a_log,
    d_skip, w_mnorm, w_mout, query_key_value_weight, output_weight, w_norm2, w_gu, w_down,
    grad_output,
):
    devices = lax.axis_size("dp")
    tokens, width = layer_input.shape
    shard = w_zx.shape[0]
    channels = conv_xb.shape[0]
    heads = dt_bias.shape[0]
    qkv_width = query_key_value_weight.shape[2]
    units = w_down.shape[0]
    attn_width = output_weight.shape[1]
    tail = jnp.concatenate(
        [w_dt, w_norm1[:, None], w_norm2[:, None], jnp.zeros((shard, LANES - heads - 2), BF16)],
        axis=1,
    )
    mixer_in = jnp.concatenate(
        [w_zx.reshape(shard, -1), w_bc, query_key_value_weight.reshape(shard, -1), tail], axis=1
    )
    in_width = mixer_in.shape[1]
    (w_in,) = gather_rows([mixer_in], devices, 0)
    norm1 = w_in[:, in_width - LANES + heads].astype(F32)
    norm2 = w_in[:, in_width - LANES + heads + 1].astype(F32)

    source = layer_input.astype(F32)
    scale_one = lax.rsqrt(jnp.mean(source * source, axis=-1, keepdims=True) + EPSILON)
    normed_one = source * scale_one
    hidden_one = (normed_one * norm1).astype(BF16)
    proj = dot(hidden_one, w_in)
    params = scan_params(conv_x, conv_xb, conv_bc, conv_bcb, dt_bias, a_log, d_skip)
    out_shard = jnp.concatenate([w_mout.T, output_weight.reshape(attn_width, -1).T], axis=1)
    y, gated, square_sum, entering, w_out = run_scan_forward(
        proj, qkv_width, params, out_shard, devices
    )
    channels_all = channels * lax.axis_size("tensor")
    scale_m = lax.rsqrt(tensor_sum(square_sum) / channels_all + EPSILON)
    tables = rotary_tables(tokens)
    qkv_at = 2 * channels + 2 * NS
    qkv, lse, attended = run_attend_forward(proj, qkv_at, attn_width, tables)
    gain_m = w_mnorm.astype(F32)[None, :]
    mixer_out, mixed = run_mixer_forward(gated, scale_m, gain_m, attended, w_out)
    mixed, gate_up_shard, down_shard = lax.optimization_barrier(
        (mixed, w_gu.reshape(shard, -1), w_down.T)
    )
    other = swap(mixed)
    w_gate_up, w_down_t = gather_rows([gate_up_shard, down_shard], devices, 3)
    other, w_gate_up, w_down_t = lax.optimization_barrier((other, w_gate_up, w_down_t))
    ffn_args = (layer_input, mixed, other, grad_output, norm2[None, :], w_gate_up, w_down_t)
    part_a, *filled = run_feed_forward(0, *ffn_args)
    other_a = swap(part_a)
    part_b, *filled = run_feed_forward(1, *ffn_args, before=tuple(filled))
    after, scale_two, hidden_two, activated, grad_gu_low, ffn_part = filled
    part_b, hidden_two, grad_gu_low = lax.optimization_barrier((part_b, hidden_two, grad_gu_low))
    other_b = swap(part_b)
    grad_gu = dot(hidden_two, grad_gu_low, TN).astype(BF16)
    grad_down = dot(grad_output, activated, TN).astype(BF16)
    (mine_gate,) = scatter_rows([grad_gu], [(0, 0, units)], [(0, 0, units)], devices, 1)
    other_a, other_b, mine_gate, grad_down, ffn_part = lax.optimization_barrier(
        (other_a, other_b, mine_gate, grad_down, ffn_part)
    )
    ffn_other = swap(ffn_part)
    grad_after, grad_mix_low, grad_mamba, grad_attended, inner_m, grad_norm2 = run_mixer_backward(
        (part_a, other_a, part_b, other_b), after, scale_two, grad_output, norm2[None, :], w_out,
        gated, scale_m, gain_m,
    )
    inner_m = tensor_sum(inner_m) / channels_all
    dqkv = run_attend_backward(qkv, lse, attended, grad_attended, 0, tables)
    grad_out = dot(grad_mix_low, mixer_out, TN).astype(BF16)
    windows = [(0, 0, channels + attn_width), (1, 0, units), (2, units, 2 * units)]
    pieces = [
        (0, 0, channels),
        (0, channels, channels + attn_width),
        (1, 0, units),
        (2, 0, units),
    ]
    grad_proj, small_x, small_b, small_h, mine_mout, mine_o, mine_down, mine_up = run_scan_backward(
        proj, y, entering, grad_mamba, scale_m, inner_m, dqkv, params, gain_m,
        [grad_out, grad_down, grad_gu], windows, pieces, devices,
    )
    ffn_other, grad_proj = lax.optimization_barrier((ffn_other, grad_proj))
    result = (after + join(ffn_part, ffn_other)).astype(BF16)
    partial_one, grad_proj = lax.optimization_barrier(
        (dot(grad_proj, w_in, NT).astype(BF16), grad_proj)
    )
    crossing = jnp.concatenate(
        [
            small_b[: KCONV + 1].reshape(-1, LANES),
            jnp.sum(partial_one.astype(F32) * normed_one, axis=0).reshape(-1, LANES),
        ],
        axis=0,
    )
    crossing = tensor_sum(crossing)
    partial_one, crossing = lax.optimization_barrier((partial_one, crossing))
    other = swap(partial_one)
    grad_in = dot(hidden_one, grad_proj, TN).astype(BF16)
    small = jnp.concatenate(
        [
            small_x[: KCONV + 2].reshape(-1, LANES),
            small_h[:3],
            crossing,
            grad_norm2[0].reshape(-1, LANES),
        ],
        axis=0,
    )
    small_rows = small.shape[0]
    small = jnp.pad(small, ((0, -small_rows % EDGE), (0, 0)))
    shared_at = 2 * channels
    step_at = qkv_at + qkv_width
    mine_zx, mine_bc, mine_qkv, mine_step, small = scatter_last(
        [grad_in],
        small,
        [(0, 0, in_width)],
        [
            (0, 0, shared_at),
            (0, shared_at, qkv_at),
            (0, qkv_at, step_at),
            (0, step_at, in_width),
        ],
        devices,
        5,
    )
    other, mine_bc = lax.optimization_barrier((other, mine_bc))
    grad_hidden_one = join(partial_one, other)
    weighted = grad_hidden_one * norm1
    grad_source = grad_after + scale_one * (
        weighted - normed_one * jnp.mean(weighted * normed_one, axis=-1, keepdims=True)
    )

    half = NS * 2 // lax.axis_size("tensor")
    shared_cols = tensor_sum(mine_bc)
    begin = lax.axis_index("tensor") * half
    grad_bc = lax.dynamic_slice_in_dim(shared_cols, begin, half, 1)
    small = small[:small_rows].reshape(-1)
    x_size = (KCONV + 2) * channels
    h_size = 3 * LANES
    b_size = (KCONV + 1) * 2 * NS
    total_x = small[:x_size].reshape(KCONV + 2, channels)
    total_h = small[x_size : x_size + h_size].reshape(3, LANES)
    total_b = small[x_size + h_size : x_size + h_size + b_size].reshape(KCONV + 1, 2 * NS)
    total_b = lax.dynamic_slice_in_dim(total_b, begin, half, 1)
    norms = small[x_size + h_size + b_size :].reshape(2, width)
    norms = lax.dynamic_slice_in_dim(norms, lax.axis_index("dp") * shard, shard, 1)
    return (
        result,
        grad_source,
        norms[0],
        mine_zx.reshape(w_zx.shape),
        grad_bc,
        mine_step[:, :heads],
        total_x[:KCONV],
        total_x[KCONV],
        total_b[:KCONV],
        total_b[KCONV],
        total_h[0, :heads],
        total_h[1, :heads],
        total_h[2, :heads],
        total_x[KCONV + 1],
        mine_mout.T,
        mine_qkv.reshape(query_key_value_weight.shape),
        mine_o.T.reshape(output_weight.shape),
        norms[1],
        jnp.stack([mine_gate, mine_up], axis=1),
        mine_down.T,
    )


def solution(mesh):
    return jax.shard_map(
        local,
        mesh=mesh,
        in_specs=(
            P("dp", None),
            P("dp"),
            P("dp", None, "tensor"),
            P("dp", None),
            P("dp", "tensor"),
            P(None, "tensor"),
            P("tensor"),
            P(),
            P(),
            P("tensor"),
            P("tensor"),
            P("tensor"),
            P("tensor"),
            P("tensor", "dp"),
            P("dp", "tensor", None),
            P("tensor", None, "dp"),
            P("dp"),
            P("dp", None, "tensor"),
            P("tensor", "dp"),
            P("dp", None),
        ),
        out_specs=(
            P("dp", None),
            P("dp", None),
            P("dp"),
            P("dp", None, "tensor"),
            P("dp", "tensor"),
            P("dp", "tensor"),
            P(None, "tensor"),
            P("tensor"),
            P(None, "tensor"),
            P("tensor"),
            P("tensor"),
            P("tensor"),
            P("tensor"),
            P("tensor"),
            P("tensor", "dp"),
            P("dp", "tensor", None),
            P("tensor", None, "dp"),
            P("dp"),
            P("dp", None, "tensor"),
            P("tensor", "dp"),
        ),
        check_vma=False,
    )
```

```python
import functools
import math

import jax
import jax.numpy as jnp
import numpy as np
from jax import lax
from jax.experimental import pallas as pl
from jax.experimental.pallas import tpu as pltpu
from jax.sharding import PartitionSpec as P

HEAD_SIZE = 64
MP = 64
NS = 128
KCONV = 4
SPAN = 128
QBLK = 256
FINE = 32
TBLK = 256
UBLK = 256
LANES = 128
EDGE = 8

EPSILON = 1e-05
HIGHEST = lax.Precision.HIGHEST
LOG_BASE = math.log(100000000000.0)
MASKED = -1e30
MESH = pl.DeviceIdType.MESH
F32 = jnp.float32
BF16 = jnp.bfloat16

NN = ((1,), (0,))
NT = ((1,), (1,))
TN = ((0,), (0,))


def dot(left, right, dims=NN, precision=None):
    return lax.dot_general(
        left, right, (dims, ((), ())), preferred_element_type=F32, precision=precision
    )


def iota(shape, dim):
    return lax.broadcasted_iota(jnp.int32, shape, dim)


def ring_place(chip, chips):
    odd = lax.rem(chip, 2)
    half = lax.div(chip, 2)
    return (1 - odd) * half + odd * (chips - 1 - half)


def ring_chip(place, chips):
    place = lax.rem(place + 4 * chips, chips)
    back = lax.div(place, chips // 2)
    return (1 - back) * (2 * place) + back * (2 * (chips - 1 - place) + 1)


def ring_setup(chips):
    me = lax.axis_index("dp")
    group = lax.axis_index("tensor")
    chip = lax.div(me, 2)
    core = lax.rem(me, 2)
    place = ring_place(chip, chips)
    right = ring_chip(place + 1, chips) * 2 + core
    left = ring_chip(place - 1, chips) * 2 + core
    mate = chip * 2 + (1 - core)
    barrier = pltpu.get_barrier_semaphore()
    for other in (right, left, mate):
        pl.semaphore_signal(barrier, inc=1, device_id=(other, group), device_id_type=MESH)
    pl.semaphore_wait(barrier, 3)
    return me, group, core, place, right, left, mate


class RingGather:
    def __init__(self, devices, x_ref, o_ref, sems):
        self.chips = devices // 2
        self.ahead = self.chips // 2
        self.behind = self.chips - 1 - self.ahead
        self.x_ref, self.o_ref, self.rows = x_ref, o_ref, x_ref.shape[0]
        self.fs, self.fr, self.bs, self.br, self.cs, self.cr, self.own_sem = sems

    def locate(self):
        me = lax.axis_index("dp")
        self.group = lax.axis_index("tensor")
        self.core = lax.rem(me, 2)
        chip = lax.div(me, 2)
        self.place = ring_place(chip, self.chips)
        self.right = ring_chip(self.place + 1, self.chips) * 2 + self.core
        self.left = ring_chip(self.place - 1, self.chips) * 2 + self.core
        self.mate = chip * 2 + (1 - self.core)
        self.me = me

    def slot(self, index):
        return self.o_ref.at[pl.ds(pl.multiple_of(index * self.rows, self.rows), self.rows), :]

    def copy(self, shift, ssem, rsem, target):
        if shift == 0:
            index, source = self.me, self.x_ref
        else:
            index = ring_chip(self.place + shift, self.chips) * 2 + self.core
            source = self.slot(index)
        return pltpu.make_async_remote_copy(
            src_ref=source,
            dst_ref=self.slot(index),
            send_sem=ssem,
            recv_sem=rsem,
            device_id=(target, self.group),
            device_id_type=MESH,
        )

    def fore(self, step):
        return self.copy(-step, self.fs.at[step], self.fr.at[step], self.right)

    def back(self, step):
        return self.copy(step, self.bs.at[step], self.br.at[step], self.left)

    def across(self, shift):
        number = 0 if shift == 0 else 2 * abs(shift) - (1 if shift < 0 else 0)
        return self.copy(shift, self.cs.at[number], self.cr.at[number], self.mate)

    def own(self):
        return pltpu.make_async_copy(self.x_ref, self.slot(self.me), self.own_sem)

    def greet(self):
        self.locate()
        barrier = pltpu.get_barrier_semaphore()
        for other in (self.right, self.left, self.mate):
            pl.semaphore_signal(
                barrier, inc=1, device_id=(other, self.group), device_id_type=MESH
            )
        pl.semaphore_wait(barrier, 3)

    def begin(self):
        self.locate()
        self.fore(0).start()
        self.back(0).start()
        self.across(0).start()
        self.own().start()

    def hop(self, step):
        self.locate()
        self.fore(step - 1).wait_recv()
        if step < self.ahead:
            self.fore(step).start()
        self.across(-step).start()
        if step <= self.behind:
            self.back(step - 1).wait_recv()
            if step < self.behind:
                self.back(step).start()
            self.across(step).start()

    def finish(self):
        self.locate()
        self.own().wait()
        for step in range(self.ahead):
            self.fore(step).wait_send()
        for step in range(self.behind):
            self.back(step).wait_send()
        for shift in range(-self.ahead, self.behind + 1):
            self.across(shift).wait()


def gather_sems(devices):
    dma = pltpu.SemaphoreType.DMA
    return [dma((devices // 2,))] * 6 + [dma(())]


def gather_shape(shard, devices):
    return jax.ShapeDtypeStruct((shard.shape[0] * devices, shard.shape[1]), shard.dtype)


def gather_kernel(devices, count, *refs):
    shards, outs, sems = refs[:count], refs[count : 2 * count], refs[2 * count :]
    each = len(sems) // count
    rings = [
        RingGather(devices, shards[i], outs[i], sems[i * each : (i + 1) * each])
        for i in range(count)
    ]
    rings[0].greet()
    for ring in rings:
        ring.begin()
    for step in range(1, rings[0].ahead + 1):
        for ring in rings:
            ring.hop(step)
    for ring in rings:
        ring.finish()


def cost(micros):
    return pl.CostEstimate(flops=int(micros * 1e9), bytes_accessed=0, transcendentals=0)


def gather_rows(shards, devices, collective):
    count = len(shards)
    anywhere = pl.BlockSpec(memory_space=pl.ANY)
    return pl.pallas_call(
        functools.partial(gather_kernel, devices, count),
        out_shape=tuple(gather_shape(shard, devices) for shard in shards),
        in_specs=[anywhere] * count,
        out_specs=(anywhere,) * count,
        scratch_shapes=gather_sems(devices) * count,
        compiler_params=pltpu.CompilerParams(collective_id=collective, has_side_effects=True),
        cost_estimate=cost(3),
        name="gather_rows",
    )(*shards)


def scatter_order(chips):
    ahead = chips // 2
    behind = chips - 1 - ahead
    order = []
    for step in range(ahead):
        order.append(-(ahead - step))
        if step < behind:
            order.append(behind - step)
    order.append(0)
    return order


class RingScatter:
    def __init__(self, devices, windows, pieces, operands, outs, scratch):
        self.chips = devices // 2
        self.ahead = self.chips // 2
        self.behind = self.chips - 1 - self.ahead
        self.windows, self.pieces, self.operands, self.outs = windows, pieces, operands, outs
        count = len(windows)
        self.mine, self.boxes, rest = scratch[:count], scratch[count : 2 * count], scratch[2 * count :]
        self.fbox, self.bbox, self.fout, self.bout = rest[:4]
        self.os, self.ms, self.mr, self.fs, self.fr, self.bs, self.br = rest[4:]
        self.rows = self.fbox.shape[1]
        widths = [item.shape[2] for item in self.mine]
        self.cols = [slice(sum(widths[:i]), sum(widths[: i + 1])) for i in range(count)]

    def locate(self):
        me = lax.axis_index("dp")
        self.group = lax.axis_index("tensor")
        self.core = lax.rem(me, 2)
        chip = lax.div(me, 2)
        self.place = ring_place(chip, self.chips)
        self.right = ring_chip(self.place + 1, self.chips) * 2 + self.core
        self.left = ring_chip(self.place - 1, self.chips) * 2 + self.core
        self.mate = chip * 2 + (1 - self.core)

    def greet(self):
        self.locate()
        barrier = pltpu.get_barrier_semaphore()
        for other in (self.right, self.left, self.mate):
            pl.semaphore_signal(
                barrier, inc=1, device_id=(other, self.group), device_id_type=MESH
            )
        pl.semaphore_wait(barrier, 3)

    def product(self, i):
        return self.windows[i][1] is not None

    def shift_of(self, slot):
        step = slot // 2
        odd = slot % 2
        return (1 - odd) * (step - self.ahead) + odd * (self.behind - step)

    def half(self, which):
        return pl.ds(pl.multiple_of(which * self.rows, self.rows), self.rows)

    def block(self, i, slot, which):
        index = ring_chip(self.place + self.shift_of(slot), self.chips) * 2 + which
        left, right, first, last = self.windows[i]
        return self.operands[left].at[self.half(index), first:last]

    def remote(self, source, target_ref, ssem, rsem, target):
        return pltpu.make_async_remote_copy(
            src_ref=source,
            dst_ref=target_ref,
            send_sem=ssem,
            recv_sem=rsem,
            device_id=(target, self.group),
            device_id_type=MESH,
        )

    def across(self, i, slot):
        if self.product(i):
            source = self.mine[i].at[slot, self.half(1 - self.core)]
        else:
            source = self.block(i, slot, 1 - self.core)
        return self.remote(
            source, self.boxes[i].at[slot], self.ms.at[i, slot], self.mr.at[i, slot], self.mate
        )

    def own(self, i, slot):
        return pltpu.make_async_copy(
            self.block(i, slot, self.core), self.mine[i].at[slot], self.os.at[i, slot]
        )

    def fore(self, step):
        return self.remote(
            self.fout.at[step], self.fbox.at[step], self.fs.at[step], self.fr.at[step], self.right
        )

    def back(self, step):
        return self.remote(
            self.bout.at[step], self.bbox.at[step], self.bs.at[step], self.br.at[step], self.left
        )

    def begin(self):
        self.locate()
        for i in range(len(self.windows)):
            if not self.product(i):
                for slot in range(self.chips):
                    self.across(i, slot).start()
                    self.own(i, slot).start()

    def produce(self, slot):
        chip = ring_chip(self.place + self.shift_of(slot), self.chips)
        size = 2 * self.rows
        for i, (left, right, first, last) in enumerate(self.windows):
            if right is None:
                continue
            at = pl.multiple_of(chip * size, size)
            terms = dot(self.operands[left][pl.ds(at, size), :], self.operands[right][:, first:last])
            self.mine[i][slot] = terms.astype(BF16)
            self.across(i, slot).start()

    def local_sum(self, i, slot, cols, others):
        rows = self.half(self.core) if self.product(i) else slice(None)
        total = self.mine[i][slot, rows, cols].astype(F32) + self.boxes[i][slot, :, cols].astype(F32)
        whole = slice(self.cols[i].start + cols.start, self.cols[i].start + cols.stop)
        for ref in others:
            total = total + ref[:, whole].astype(F32)
        return total

    def arrive(self, slot):
        for i in range(len(self.windows)):
            if not self.product(i):
                self.own(i, slot).wait()
            self.across(i, slot).wait_recv()

    def put(self, target, slot, others):
        self.arrive(slot)
        for i, cols in enumerate(self.cols):
            total = self.local_sum(i, slot, slice(0, cols.stop - cols.start), others)
            target[:, cols] = total.astype(BF16)

    def hop_back(self, step, later):
        if later:
            self.back(step - 1).wait_recv()
        self.put(self.bout.at[step], 2 * step, [self.bbox.at[step - 1]] if later else [])
        self.back(step).start()

    def hop_fore(self, step, later):
        if later:
            self.fore(step - 1).wait_recv()
        self.put(self.fout.at[step], 2 * step + 1, [self.fbox.at[step - 1]] if later else [])
        self.fore(step).start()

    def hop(self, step):
        self.locate()
        self.hop_back(step, step > 0)
        if step < self.behind:
            self.hop_fore(step, step > 0)

    def run(self, after_first=None):
        def turn(step, carry):
            lax.fori_loop(0, 2, lambda part, kept: (self.produce(2 * step + part), kept)[1], 0)

            @pl.when(step == 0)
            def _():
                self.hop_back(0, False)
                self.hop_fore(0, False)
                if after_first is not None:
                    after_first()

            pl.when(step > 0)(lambda: self.hop_back(step, True))
            pl.when((step > 0) & (step < self.behind))(lambda: self.hop_fore(step, True))
            return carry

        lax.fori_loop(0, self.ahead, turn, 0)

    def finish(self):
        self.locate()
        slot = self.chips - 1
        self.arrive(slot)
        self.fore(self.behind - 1).wait_recv()
        self.back(self.ahead - 1).wait_recv()
        others = [self.fbox.at[self.behind - 1], self.bbox.at[self.ahead - 1]]
        for i, first, last, out, form in self.pieces:
            total = self.local_sum(i, slot, slice(first, last), others)
            if form == "turned":
                self.outs[out][...] = total.T[: self.outs[out].shape[0]]
            elif form is None:
                self.outs[out][...] = total
            else:
                self.outs[out][:, form, :] = total
        for step in range(self.ahead):
            self.back(step).wait_send()
        for step in range(self.behind):
            self.fore(step).wait_send()
        for slot in range(self.chips):
            for i in range(len(self.windows)):
                self.across(i, slot).wait_send()


def scatter_scratch(windows, rows, devices):
    chips = devices // 2
    count = len(windows)
    dma = pltpu.SemaphoreType.DMA
    widths = [last - first for left, right, first, last in windows]
    mine = [
        pltpu.VMEM((chips, rows if right is None else 2 * rows, last - first), BF16)
        for left, right, first, last in windows
    ]
    boxes = [pltpu.VMEM((chips, rows, width), BF16) for width in widths]
    box = pltpu.VMEM((chips // 2, rows, sum(widths)), BF16)
    return mine + boxes + [box] * 4 + [dma((count, chips))] * 3 + [dma((chips,))] * 4


class Total:
    def __init__(self, devices, x_ref, o_ref, scratch):
        self.chips = devices // 2
        self.x_ref, self.o_ref = x_ref, o_ref
        self.mate_box, self.joined, self.boxes, self.ms, self.mr, self.ss, self.sr = scratch
        me = lax.axis_index("dp")
        self.group = lax.axis_index("tensor")
        self.chip = lax.div(me, 2)
        core = lax.rem(me, 2)
        self.mate = self.chip * 2 + (1 - core)
        self.peers = [
            lax.rem(self.chip + shift, self.chips) * 2 + core for shift in range(self.chips)
        ]

    def greet(self):
        barrier = pltpu.get_barrier_semaphore()
        for other in [self.mate] + self.peers[1:]:
            pl.semaphore_signal(
                barrier, inc=1, device_id=(other, self.group), device_id_type=MESH
            )
        pl.semaphore_wait(barrier, self.chips)

    def remote(self, source, target_ref, ssem, rsem, target):
        return pltpu.make_async_remote_copy(
            src_ref=source,
            dst_ref=target_ref,
            send_sem=ssem,
            recv_sem=rsem,
            device_id=(target, self.group),
            device_id_type=MESH,
        )

    def across(self):
        return self.remote(self.x_ref, self.mate_box, self.ms, self.mr, self.mate)

    def copies(self):
        return [
            self.remote(
                self.joined,
                self.boxes.at[self.chip],
                self.ss.at[shift],
                self.sr.at[shift],
                self.peers[shift],
            )
            for shift in range(1, self.chips)
        ]

    def begin(self):
        self.across().start()

    def spread(self):
        self.across().wait_recv()
        self.joined[...] = self.x_ref[...] + self.mate_box[...]
        for copy in self.copies():
            copy.start()
        self.boxes[self.chip] = self.joined[...]

    def finish(self):
        for copy in self.copies():
            copy.wait_recv()
        result = self.boxes[0]
        for other in range(1, self.chips):
            result = result + self.boxes[other]
        self.o_ref[...] = result
        self.across().wait_send()
        for copy in self.copies():
            copy.wait_send()


def total_scratch(values, devices):
    chips = devices // 2
    dma = pltpu.SemaphoreType.DMA
    return [
        pltpu.VMEM(values.shape, F32),
        pltpu.VMEM(values.shape, F32),
        pltpu.VMEM((chips,) + values.shape, F32),
        dma(()),
        dma(()),
        dma((chips,)),
        dma((chips,)),
    ]


def turned_copy(source, target):
    for start in range(0, source.shape[1], LANES):
        target[start : start + LANES, :] = source[:, start : start + LANES].T


def product_kernel(devices, windows, pieces, outs, summed, left_ref, right_ref, *refs):
    values = refs[:summed]
    refs = refs[summed:]
    pieces_out, refs = refs[:outs], refs[outs:]
    totals_out, refs = refs[:summed], refs[summed:]
    turned, scratch = refs[0], refs[1:]
    total = None
    if summed:
        scratch, rest = scratch[:-7], scratch[-7:]
        total = Total(devices, values[0], totals_out[0], rest)
    ring = RingScatter(devices, windows, pieces, (turned, right_ref), pieces_out, scratch)
    if total is None:
        ring.greet()
    else:
        ring.locate()
        total.greet()
        total.begin()
    turned_copy(left_ref, turned)
    ring.run(total.spread if total is not None else None)
    ring.finish()
    if total is not None:
        total.finish()


def scatter_product(left, right, windows, pieces, shapes, devices, collective, values=()):
    vmem = pl.BlockSpec(memory_space=pltpu.VMEM)
    rows = left.shape[1] // devices
    scratch = [pltpu.VMEM(left.shape[::-1], BF16)] + scatter_scratch(windows, rows, devices)
    for item in values:
        scratch += total_scratch(item, devices)
    return pl.pallas_call(
        functools.partial(
            product_kernel, devices, windows, pieces, len(shapes), len(values)
        ),
        out_shape=tuple(jax.ShapeDtypeStruct(shape, F32) for shape in shapes)
        + tuple(jax.ShapeDtypeStruct(item.shape, F32) for item in values),
        in_specs=[vmem] * (2 + len(values)),
        out_specs=(vmem,) * (len(shapes) + len(values)),
        scratch_shapes=scratch,
        compiler_params=pltpu.CompilerParams(collective_id=collective, has_side_effects=True),
        cost_estimate=cost(3),
        name="scatter_product",
    )(left, right, *values)


def head_spread(channels):
    return (iota((LANES, channels), 1) // MP == iota((LANES, channels), 0)).astype(BF16)


def parts(values, count):
    terms = []
    for _ in range(count):
        term = values.astype(BF16)
        terms.append(term)
        values = values - term.astype(F32)
    return terms


def pick(values, mask, count=2):
    return dot(jnp.concatenate(parts(values, count), axis=1), jnp.concatenate([mask] * count, axis=0))


def pick_left(mask, values, count):
    return dot(jnp.concatenate([mask] * count, axis=1), jnp.concatenate(parts(values, count), axis=0))


def gather_heads(values, spread):
    high, low = parts(values, 2)
    return dot(high, spread, NT) + dot(low, spread, NT)


def soft_step(raw):
    return jnp.maximum(raw, 0.0) + jnp.log1p(jnp.exp(-jnp.abs(raw)))


def conv_window(buffer, taps_ref, bias_ref, span):
    total = bias_ref[...] + taps_ref[0:1, :] * buffer[EDGE - 3 : EDGE - 3 + span, :]
    for tap in range(1, KCONV):
        start = EDGE - 3 + tap
        total = total + taps_ref[tap : tap + 1, :] * buffer[start : start + span, :]
    return total


def span_rates(step_ref, bias_ref, decay_ref, spread, span):
    raw = step_ref[...] + bias_ref[...]
    step = soft_step(raw)
    lower = (iota((span, span), 1) <= iota((span, span), 0)).astype(BF16)
    cum = pick_left(lower, step * decay_ref[...], 3)
    tails = jnp.exp(cum[span - 1 : span, :] - cum)
    wide = pick(jnp.concatenate([step, tails, jnp.exp(cum)], axis=0), spread)
    return raw, step, cum, wide[:span], wide[span : 2 * span], wide[2 * span :]


def pair_split(values, low_lanes):
    zero = jnp.zeros_like(values)
    return jnp.concatenate(
        [jnp.where(low_lanes, values, zero), jnp.where(low_lanes, zero, values)], axis=0
    )


def pair_decay(cum, cum_rows, pair, causal):
    parts = []
    for head in (2 * pair, 2 * pair + 1):
        differ = cum[:, head : head + 1] - cum_rows[head : head + 1, :]
        parts.append(jnp.exp(jnp.where(causal, differ, MASKED)))
    return parts


def scan_forward(
    devices, spans,
    z_ref, x_ref, bc_ref, step_ref,
    tap_ref, bias_ref, tapb_ref, biasb_ref, stepb_ref, decay_ref, skip_ref, shard_ref,
    y_ref, gated_ref, enter_ref, all_ref,
    state, xbuf, bbuf, *sems,
):
    span, channels = x_ref.shape
    ring = RingGather(devices, shard_ref, all_ref, sems)
    turn = pl.program_id(0)

    @pl.when(turn == 0)
    def _():
        ring.greet()
        ring.begin()


    @pl.when(pl.program_id(0) == 0)
    def _():
        state[...] = jnp.zeros_like(state)
        xbuf[span:, :] = jnp.zeros((EDGE, channels), F32)
        bbuf[span:, :] = jnp.zeros((EDGE, 2 * NS), F32)

    xbuf[:EDGE, :] = xbuf[span:, :]
    bbuf[:EDGE, :] = bbuf[span:, :]
    xbuf[EDGE:, :] = x_ref[...]
    bbuf[EDGE:, :] = bc_ref[...]
    inputs = jax.nn.silu(conv_window(xbuf, tap_ref, bias_ref, span))
    shared = jax.nn.silu(conv_window(bbuf, tapb_ref, biasb_ref, span))
    spread = head_spread(channels)
    raw, step, cum, step_w, tails_w, grown_w = span_rates(
        step_ref, stepb_ref, decay_ref, spread, span
    )
    cum_rows = cum.T
    b_low = shared[:, :NS].astype(BF16)
    c_low = shared[:, NS:].astype(BF16)
    scaled = inputs * step_w
    scaled_low = scaled.astype(BF16)
    enter_ref[0] = state[...]
    outer = dot(c_low, state[...].astype(BF16)) * grown_w
    fresh = dot(b_low, (scaled * tails_w).astype(BF16), TN)
    state[...] = state[...] * grown_w[span - 1 : span, :] + fresh
    cross = dot(c_low, b_low, NT)
    causal = iota((span, span), 1) <= iota((span, span), 0)
    low_lanes = iota((span, LANES), 1) < MP
    for pair in range(channels // LANES):
        lanes = slice(pair * LANES, (pair + 1) * LANES)
        first, second = pair_decay(cum, cum_rows, pair, causal)
        weights = jnp.concatenate(
            [(cross * first).astype(BF16), (cross * second).astype(BF16)], axis=1
        )
        y_ref[:, lanes] = dot(weights, pair_split(scaled_low[:, lanes], low_lanes))
    y = y_ref[...] + outer + skip_ref[...] * inputs
    y_ref[...] = y
    gated_ref[...] = y * jax.nn.silu(z_ref[...])

    count = spans
    for step in range(1, ring.ahead + 1):
        pl.when(turn == min(count - 1, count * step // ring.ahead))(
            functools.partial(ring.hop, step)
        )
    pl.when(turn == count - 1)(ring.finish)


def scan_backward(
    devices, spans, windows, pieces, outs_count, count,
    z_ref, x_ref, xp_ref, bc_ref, bp_ref, step_ref, y_ref, enter_ref,
    dyg_ref, scale_ref, inner_ref, dqkv_ref,
    tap_ref, bias_ref, tapb_ref, biasb_ref, stepb_ref, decay_ref, skip_ref, gain_ref,
    *refs,
):
    sent, refs = refs[:count], refs[count:]
    (grad_ref, gx_ref, gb_ref, gh_ref), refs = refs[:4], refs[4:]
    outs, refs = refs[:outs_count], refs[outs_count:]
    (dstate, xbuf, bbuf, dxbuf, dbbuf, du_buf, col_buf), scratch = refs[:7], refs[7:]
    ring = RingScatter(devices, windows, pieces, sent, outs, scratch)
    span, channels = x_ref.shape
    turn = pl.program_id(0)

    @pl.when(turn == 0)
    def _():
        ring.greet()
        ring.begin()
        dstate[...] = jnp.zeros_like(dstate)
        dxbuf[...] = jnp.zeros_like(dxbuf)
        dbbuf[...] = jnp.zeros_like(dbbuf)
        col_buf[...] = jnp.zeros_like(col_buf)
        gx_ref[...] = jnp.zeros_like(gx_ref)
        gb_ref[...] = jnp.zeros_like(gb_ref)
        gh_ref[...] = jnp.zeros_like(gh_ref)

    inside = (turn < spans - 1).astype(F32)
    xbuf[:EDGE, :] = xp_ref[...] * inside
    bbuf[:EDGE, :] = bp_ref[...] * inside
    xbuf[EDGE:, :] = x_ref[...]
    bbuf[EDGE:, :] = bc_ref[...]
    conv = conv_window(xbuf, tap_ref, bias_ref, span)
    sig = jax.nn.sigmoid(conv)
    inputs = conv * sig
    convb = conv_window(bbuf, tapb_ref, biasb_ref, span)
    sigb = jax.nn.sigmoid(convb)
    shared = convb * sigb
    b_low = shared[:, :NS].astype(BF16)
    c_low = shared[:, NS:].astype(BF16)
    spread = head_spread(channels)
    raw, step, cum, step_w, tails_w, grown_w = span_rates(
        step_ref, stepb_ref, decay_ref, spread, span
    )
    cum_rows = cum.T
    scaled = inputs * step_w
    scaled_low = scaled.astype(BF16)

    z = z_ref[...]
    sig_z = jax.nn.sigmoid(z)
    swish = z * sig_z
    y = y_ref[...]
    normed = y * swish * scale_ref[...]
    dyg = dyg_ref[...]
    gain_grad = jnp.sum(dyg * normed, axis=0, keepdims=True)
    dgated = scale_ref[...] * (dyg * gain_ref[...] - normed * inner_ref[...])
    dy = dgated * swish
    grad_ref[:, :channels] = (dgated * y * (sig_z * (1.0 + z * (1.0 - sig_z)))).astype(BF16)

    state_low = enter_ref[0].astype(BF16)
    dstate_low = dstate[...].astype(BF16)
    grown_low = (dy * grown_w).astype(BF16)
    dy_low = dy.astype(BF16)
    tailed = scaled * tails_w
    outer = dot(c_low, state_low) * grown_w
    from_state = dot(b_low, dstate_low)
    dc = dot(grown_low, state_low, NT)
    db = dot(tailed.astype(BF16), dstate_low, NT)
    leak = from_state * tailed
    last_w = grown_w[span - 1 : span, :]
    ends = (
        jnp.sum(leak, axis=0, keepdims=True)
        + jnp.sum(enter_ref[0] * dstate[...], axis=0, keepdims=True) * last_w
    )
    skips = jnp.sum(dy * inputs, axis=0, keepdims=True)
    dstate[...] = dstate[...] * last_w + dot(c_low, grown_low, TN)

    cross = dot(c_low, b_low, NT)
    causal = iota((span, span), 1) <= iota((span, span), 0)
    low_lanes = iota((span, LANES), 1) < MP
    lane = iota((span, LANES), 1)
    dcross = jnp.zeros((span, span), F32)
    row_part = jnp.zeros((span, LANES), F32)
    for pair in range(channels // LANES):
        lanes = slice(pair * LANES, (pair + 1) * LANES)
        decays = pair_decay(cum, cum_rows, pair, causal)
        dy_pair = pair_split(dy_low[:, lanes], low_lanes)
        dweights = dot(dy_pair, scaled_low[:, lanes], NT)
        both = []
        for part in range(2):
            head = 2 * pair + part
            dterm = dweights[part * span : (part + 1) * span] * decays[part]
            dcross = dcross + dterm
            flow = dterm * cross
            row_part = row_part + jnp.where(
                lane == head, jnp.sum(flow, axis=1, keepdims=True), 0.0
            )
            col_buf[head : head + 1, :] = jnp.sum(flow, axis=0, keepdims=True)
            both.append((cross * decays[part]).astype(BF16))
        du_buf[:, lanes] = dot(jnp.concatenate(both, axis=0), dy_pair, TN)
    du = du_buf[...] + from_state * tails_w
    dcross_low = dcross.astype(BF16)
    dc = dc + dot(dcross_low, b_low)
    db = db + dot(dcross_low, c_low, TN)

    sums = gather_heads(
        jnp.concatenate(
            [dy * outer - leak, du * inputs, ends, skips, jnp.zeros((EDGE - 2, channels), F32)],
            axis=0,
        ),
        spread,
    )
    at_end = sums[2 * span : 2 * span + 1, :]
    dcum = sums[:span] + row_part - col_buf[...].T
    upper = (iota((span, span), 1) >= iota((span, span), 0)).astype(BF16)
    drate = pick_left(upper, dcum, 3) + at_end
    dstep = drate * decay_ref[...] + sums[span : 2 * span]
    draw = dstep * jax.nn.sigmoid(raw)
    gh_ref[0:1, :] += jnp.sum(draw, axis=0, keepdims=True)
    gh_ref[1:2, :] += jnp.sum(drate * step, axis=0, keepdims=True) * decay_ref[...]
    gh_ref[2:3, :] += sums[2 * span + 1 : 2 * span + 2, :]

    dinputs = du * step_w + skip_ref[...] * dy
    dxbuf[span:, :] = dxbuf[:EDGE, :]
    dbbuf[span:, :] = dbbuf[:EDGE, :]
    dconv = dinputs * (sig * (1.0 + conv * (1.0 - sig)))
    dconvb = jnp.concatenate([db, dc], axis=1) * (sigb * (1.0 + convb * (1.0 - sigb)))
    dxbuf[:span, :] = dconv
    dbbuf[:span, :] = dconvb
    dx = jnp.zeros_like(dconv)
    dbc = jnp.zeros_like(dconvb)
    for tap in range(KCONV):
        back = KCONV - 1 - tap
        start = EDGE - 3 + tap
        dx = dx + tap_ref[tap : tap + 1, :] * dxbuf[back : back + span, :]
        dbc = dbc + tapb_ref[tap : tap + 1, :] * dbbuf[back : back + span, :]
        gx_ref[tap : tap + 1, :] += jnp.sum(
            dconv * xbuf[start : start + span, :], axis=0, keepdims=True
        )
        gb_ref[tap : tap + 1, :] += jnp.sum(
            dconvb * bbuf[start : start + span, :], axis=0, keepdims=True
        )
    gx_ref[KCONV : KCONV + 1, :] += jnp.sum(dconv, axis=0, keepdims=True)
    gb_ref[KCONV : KCONV + 1, :] += jnp.sum(dconvb, axis=0, keepdims=True)
    gx_ref[KCONV + 1 : KCONV + 2, :] += gain_grad
    width = 2 * channels + 2 * NS
    grad_ref[:, channels : 2 * channels] = dx.astype(BF16)
    grad_ref[:, 2 * channels : width] = dbc.astype(BF16)
    grad_ref[:, width : width + dqkv_ref.shape[1]] = dqkv_ref[...]
    grad_ref[:, width + dqkv_ref.shape[1] :] = draw.astype(BF16)
    for step in range(ring.ahead):
        pl.when(turn == spans * step // ring.ahead)(functools.partial(ring.hop, step))
    pl.when(turn == spans - 1)(ring.finish)


def scan_params(conv_x, conv_xb, conv_bc, conv_bcb, dt_bias, a_log, d_skip):
    heads = dt_bias.shape[0]

    def wide(row):
        return jnp.pad(row, (0, LANES - heads))[None, :]

    f32 = lambda value: value.astype(F32)
    return (
        f32(conv_x),
        f32(conv_xb)[None, :],
        f32(conv_bc),
        f32(conv_bcb)[None, :],
        wide(f32(dt_bias)),
        wide(-jnp.exp(f32(a_log))),
        jnp.repeat(f32(d_skip), MP)[None, :],
    )


def whole_spec(array):
    return pl.BlockSpec(array.shape, lambda turn: (0,) * array.ndim)


def run_scan_forward(proj, qkv_width, params, shard, devices):
    tokens = proj.shape[0]
    channels = params[1].shape[1]
    step_at = (2 * channels + 2 * NS + qkv_width) // LANES
    spans = tokens // SPAN
    bc_at = 2 * channels // (2 * NS)
    rows = lambda width, at: pl.BlockSpec((SPAN, width), lambda turn: (turn, at))
    anywhere = pl.BlockSpec(memory_space=pl.ANY)
    return pl.pallas_call(
        functools.partial(scan_forward, devices, spans),
        grid=(spans,),
        out_shape=(
            jax.ShapeDtypeStruct((tokens, channels), F32),
            jax.ShapeDtypeStruct((tokens, channels), F32),
            jax.ShapeDtypeStruct((spans, NS, channels), F32),
            gather_shape(shard, devices),
        ),
        in_specs=[rows(channels, 0), rows(channels, 1), rows(2 * NS, bc_at), rows(LANES, step_at)]
        + [whole_spec(item) for item in params]
        + [anywhere],
        out_specs=(
            rows(channels, 0),
            rows(channels, 0),
            pl.BlockSpec((1, NS, channels), lambda turn: (turn, 0, 0)),
            anywhere,
        ),
        scratch_shapes=[
            pltpu.VMEM((NS, channels), F32),
            pltpu.VMEM((SPAN + EDGE, channels), F32),
            pltpu.VMEM((SPAN + EDGE, 2 * NS), F32),
        ]
        + gather_sems(devices),
        compiler_params=pltpu.CompilerParams(collective_id=2, has_side_effects=True),
        cost_estimate=cost(20),
        name="scan_forward",
    )(proj, proj, proj, proj, *params, shard)


def run_scan_backward(
    proj, y, entering, dyg, scale, inner, dqkv, params, gain, sent, windows, pieces,
    shapes, devices,
):
    tokens, width = proj.shape
    channels = params[1].shape[1]
    qkv_width = dqkv.shape[1]
    step_at = (2 * channels + 2 * NS + qkv_width) // LANES
    spans = tokens // SPAN
    bc_at = 2 * channels // (2 * NS)
    edges = SPAN // EDGE
    rows = lambda size, at: pl.BlockSpec((SPAN, size), lambda turn: (spans - 1 - turn, at))
    edge = lambda size, at: pl.BlockSpec(
        (EDGE, size), lambda turn: (jnp.maximum((spans - 1 - turn) * edges - 1, 0), at)
    )
    keep = lambda shape: pl.BlockSpec(shape, lambda turn: (0, 0))
    shapes = tuple(jax.ShapeDtypeStruct(shape, F32) for shape in shapes)
    return pl.pallas_call(
        functools.partial(
            scan_backward, devices, spans, windows, pieces, len(shapes), len(sent)
        ),
        grid=(spans,),
        out_shape=(
            jax.ShapeDtypeStruct((tokens, width), BF16),
            jax.ShapeDtypeStruct((EDGE, channels), F32),
            jax.ShapeDtypeStruct((EDGE, 2 * NS), F32),
            jax.ShapeDtypeStruct((EDGE, LANES), F32),
        )
        + shapes,
        in_specs=[
            rows(channels, 0),
            rows(channels, 1),
            edge(channels, 1),
            rows(2 * NS, bc_at),
            edge(2 * NS, bc_at),
            rows(LANES, step_at),
            rows(channels, 0),
            pl.BlockSpec((1, NS, channels), lambda turn: (spans - 1 - turn, 0, 0)),
            rows(channels, 0),
            rows(1, 0),
            rows(1, 0),
            rows(qkv_width, 0),
        ]
        + [whole_spec(item) for item in params]
        + [whole_spec(gain)]
        + [pl.BlockSpec(memory_space=pl.ANY)] * len(sent),
        out_specs=(
            rows(width, 0),
            keep((EDGE, channels)),
            keep((EDGE, 2 * NS)),
            keep((EDGE, LANES)),
        )
        + tuple(keep(item.shape) for item in shapes),
        scratch_shapes=[
            pltpu.VMEM((NS, channels), F32),
            pltpu.VMEM((SPAN + EDGE, channels), F32),
            pltpu.VMEM((SPAN + EDGE, 2 * NS), F32),
            pltpu.VMEM((SPAN + EDGE, channels), F32),
            pltpu.VMEM((SPAN + EDGE, 2 * NS), F32),
            pltpu.VMEM((SPAN, channels), F32),
            pltpu.VMEM((LANES, SPAN), F32),
        ]
        + scatter_scratch(windows, sent[0].shape[0] // devices, devices),
        compiler_params=pltpu.CompilerParams(collective_id=6, has_side_effects=True),
        cost_estimate=cost(47),
        name="scan_backward",
    )(
        proj, proj, proj, proj, proj, proj, y, entering, dyg, scale, inner, dqkv, *params, gain,
        *sent,
    )


def rotary_tables(tokens):
    half = HEAD_SIZE // 2
    exponent = np.arange(half, dtype=np.float64) * (-2.0 * LOG_BASE / HEAD_SIZE)
    rates = np.tile(np.exp(exponent.astype(np.float32)).astype(np.float64), LANES // half)
    tables = []
    for places in (np.arange(FINE), np.arange(0, tokens, FINE)):
        angles = places[:, None] * rates[None, :]
        tables += [np.cos(angles).astype(np.float32), np.sin(angles).astype(np.float32)]
    return tables


def fill_rotary(fine_cos, fine_sin, coarse_cos, coarse_sin, cosine, sine):
    small_cos, small_sin = fine_cos[...], fine_sin[...]
    for turn in range(coarse_cos.shape[0]):
        big_cos, big_sin = coarse_cos[turn : turn + 1, :], coarse_sin[turn : turn + 1, :]
        rows = slice(turn * FINE, (turn + 1) * FINE)
        cosine[rows, :] = small_cos * big_cos - small_sin * big_sin
        sine[rows, :] = small_sin * big_cos + small_cos * big_sin


def head_masks():
    half = HEAD_SIZE // 2
    row, col = iota((LANES, LANES), 0), iota((LANES, LANES), 1)
    place = col % HEAD_SIZE
    ahead = jnp.where(place < half, -1.0, 0.0)
    behind = jnp.where(place < half, 0.0, 1.0)

    def turn(start):
        return jnp.where(row == start + half, ahead, jnp.where(row == start - half, behind, 0.0))

    first = row < HEAD_SIZE
    left = col < HEAD_SIZE
    low = lambda mask: mask.astype(BF16)
    within = low(turn(col))
    copy = low(jnp.where(row == place, 1.0, 0.0))
    copy_turn = low(jnp.where(first, turn(place), 0.0))
    value = low(jnp.where(row == place + HEAD_SIZE, 1.0, 0.0))
    fold = low(jnp.where(left & (row % HEAD_SIZE == place), 1.0, 0.0))
    other = row % HEAD_SIZE
    fold_turn = low(
        jnp.where(
            left,
            jnp.where(other == place + half, ahead, jnp.where(other == place - half, behind, 0.0)),
            0.0,
        )
    )
    fold_value = low(jnp.where(left, 0.0, jnp.where(other == place, 1.0, 0.0)))
    return within, copy, copy_turn, value, fold, fold_turn, fold_value


def attend_forward(
    q_ref, kv_ref, fine_cos, fine_sin, coarse_cos, coarse_sin,
    qkv_ref, lse_ref, o_ref, vt, cos_ref, sin_ref,
):
    fill_rotary(fine_cos, fine_sin, coarse_cos, coarse_sin, cos_ref, sin_ref)
    tokens, query_width = q_ref.shape
    pairs = query_width // LANES
    within, copy, copy_turn, value = head_masks()[:4]
    for start in range(0, tokens, QBLK):
        rows = slice(start, start + QBLK)
        cosine, sine = cos_ref[rows, :], sin_ref[rows, :]
        for pair in range(pairs):
            lanes = slice(pair * LANES, (pair + 1) * LANES)
            query = q_ref[rows, lanes]
            turned = query * cosine + pick(query, within) * sine
            qkv_ref[rows, lanes] = (turned * HEAD_SIZE**-0.5).astype(BF16)
        kv = kv_ref[rows, :]
        keys = pick(kv, copy) * cosine + pick(kv, copy_turn) * sine
        qkv_ref[rows, query_width : query_width + LANES] = keys.astype(BF16)
        qkv_ref[rows, query_width + LANES :] = dot(kv.astype(BF16), value).astype(BF16)
        vt[:, rows] = kv.T[HEAD_SIZE:, :].astype(BF16)
    low_lanes = iota((QBLK, LANES), 1) < HEAD_SIZE
    wide = (QBLK, 2 * QBLK)
    visible = iota(wide, 0) <= iota(wide, 1) % QBLK

    def block(i, carry):
        here = pl.ds(pl.multiple_of(i * QBLK, QBLK), QBLK)
        queries = [
            pair_split(qkv_ref[here, pair * LANES : (pair + 1) * LANES], low_lanes)
            for pair in range(pairs)
        ]

        def tile(there, state, edge):
            keys = qkv_ref[there, query_width : query_width + LANES]
            result = []
            for pair in range(pairs):
                top, total, out = state[3 * pair : 3 * pair + 3]
                scores = dot(keys, queries[pair], NT)
                if edge:
                    scores = jnp.where(visible, scores, MASKED)
                higher = jnp.maximum(top, jnp.max(scores, axis=0, keepdims=True))
                probs = jnp.exp(scores - higher)
                fade = jnp.exp(top - higher)
                total = total * fade + jnp.sum(probs, axis=0, keepdims=True)
                out = out * fade + dot(vt[:, there], probs.astype(BF16))
                result += [higher, total, out]
            return tuple(result)

        state = (
            jnp.full((1, 2 * QBLK), MASKED, F32),
            jnp.zeros((1, 2 * QBLK), F32),
            jnp.zeros((HEAD_SIZE, 2 * QBLK), F32),
        ) * pairs
        state = lax.fori_loop(
            0,
            i,
            lambda j, state: tile(pl.ds(pl.multiple_of(j * QBLK, QBLK), QBLK), state, False),
            state,
        )
        state = tile(here, state, True)
        for pair in range(pairs):
            top, total, out = state[3 * pair : 3 * pair + 3]
            out = out / total
            lse = top + jnp.log(total)
            lse_ref[2 * pair : 2 * pair + 1, here] = lse[:, :QBLK]
            lse_ref[2 * pair + 1 : 2 * pair + 2, here] = lse[:, QBLK:]
            both = jnp.concatenate([out[:, :QBLK], out[:, QBLK:]], axis=0)
            o_ref[here, pair * LANES : (pair + 1) * LANES] = both.T.astype(BF16)
        return carry

    lax.fori_loop(0, tokens // QBLK, block, 0)


def attend_backward(
    qkv_ref, lse_ref, o_ref, do_ref, fine_cos, fine_sin, coarse_cos, coarse_sin,
    dqkv_ref,
    dq, kt, dk, dv, cos_ref, sin_ref,
):
    fill_rotary(fine_cos, fine_sin, coarse_cos, coarse_sin, cos_ref, sin_ref)
    tokens, query_width = o_ref.shape
    pairs = query_width // LANES
    key_lanes = slice(query_width, query_width + LANES)
    value_lanes = slice(query_width + LANES, query_width + 2 * LANES)
    for start in range(0, tokens, QBLK):
        rows = slice(start, start + QBLK)
        kt[:, rows] = qkv_ref[rows, key_lanes].astype(F32).T[:HEAD_SIZE, :].astype(BF16)
    dk[...] = jnp.zeros_like(dk)
    dv[...] = jnp.zeros_like(dv)
    low_lanes = iota((QBLK, LANES), 1) < HEAD_SIZE
    wide = (QBLK, 2 * QBLK)
    visible = iota(wide, 0) <= iota(wide, 1) % QBLK
    ones = jnp.ones((EDGE, LANES), BF16)

    def block(i, carry):
        here = pl.ds(pl.multiple_of(i * QBLK, QBLK), QBLK)
        queries, grads, inners, lses = [], [], [], []
        for pair in range(pairs):
            lanes = slice(pair * LANES, (pair + 1) * LANES)
            queries.append(pair_split(qkv_ref[here, lanes], low_lanes))
            grad = do_ref[here, lanes]
            grads.append(pair_split(grad, low_lanes))
            both = pair_split(grad.astype(F32) * o_ref[here, lanes].astype(F32), low_lanes)
            high, low = parts(both, 2)
            inners.append((dot(ones, high, NT) + dot(ones, low, NT))[:1])
            lses.append(
                jnp.concatenate(
                    [
                        lse_ref[2 * pair : 2 * pair + 1, here],
                        lse_ref[2 * pair + 1 : 2 * pair + 2, here],
                    ],
                    axis=1,
                )
            )
        query_all = jnp.concatenate(queries, axis=0)
        grad_all = jnp.concatenate(grads, axis=0)

        def tile(there, state, edge):
            keys = qkv_ref[there, key_lanes]
            values = qkv_ref[there, value_lanes]
            all_probs, all_dscores, result = [], [], []
            for pair in range(pairs):
                probs = dot(keys, queries[pair], NT) - lses[pair]
                if edge:
                    probs = jnp.where(visible, probs, MASKED)
                probs = jnp.exp(probs)
                dprobs = dot(values, grads[pair], NT)
                dscores = (probs * (dprobs - inners[pair])).astype(BF16)
                all_probs.append(probs.astype(BF16))
                all_dscores.append(dscores)
                result.append(state[pair] + dot(kt[:, there], dscores))
            dv[there, :] += dot(jnp.concatenate(all_probs, axis=1), grad_all)
            dk[there, :] += dot(jnp.concatenate(all_dscores, axis=1), query_all)
            return tuple(result)

        state = (jnp.zeros((HEAD_SIZE, 2 * QBLK), F32),) * pairs
        state = lax.fori_loop(
            0,
            i,
            lambda j, state: tile(pl.ds(pl.multiple_of(j * QBLK, QBLK), QBLK), state, False),
            state,
        )
        state = tile(here, state, True)
        for pair in range(pairs):
            both = jnp.concatenate([state[pair][:, :QBLK], state[pair][:, QBLK:]], axis=0)
            dq[here, pair * LANES : (pair + 1) * LANES] = both.T
        return carry

    lax.fori_loop(0, tokens // QBLK, block, 0)
    masks = head_masks()
    within, (fold, fold_turn, fold_value) = masks[0], masks[4:]
    for start in range(0, tokens, QBLK):
        rows = slice(start, start + QBLK)
        cosine, sine = cos_ref[rows, :], sin_ref[rows, :]
        for pair in range(pairs):
            lanes = slice(pair * LANES, (pair + 1) * LANES)
            grad = dq[rows, lanes]
            grad = grad * cosine - pick(grad, within) * sine
            dqkv_ref[rows, lanes] = (grad * HEAD_SIZE**-0.5).astype(BF16)
        grad = dk[rows, :]
        grad = pick(grad, fold) * cosine - pick(grad, fold_turn) * sine
        grad = grad + pick(dv[rows, :], fold_value)
        dqkv_ref[rows, query_width:] = grad.astype(BF16)


def run_attend_forward(proj, query_at, query_width, tables):
    tokens = proj.shape[0]
    cols = lambda size, at: pl.BlockSpec((tokens, size), lambda turn: (0, at // size))
    return pl.pallas_call(
        attend_forward,
        grid=(1,),
        out_shape=(
            jax.ShapeDtypeStruct((tokens, query_width + 2 * LANES), BF16),
            jax.ShapeDtypeStruct((EDGE, tokens), F32),
            jax.ShapeDtypeStruct((tokens, query_width), BF16),
        ),
        in_specs=[
            cols(query_width, query_at),
            cols(2 * HEAD_SIZE, query_at + query_width),
        ]
        + [whole_spec(table) for table in tables],
        out_specs=(
            cols(query_width + 2 * LANES, 0),
            pl.BlockSpec((EDGE, tokens), lambda turn: (0, 0)),
            cols(query_width, 0),
        ),
        scratch_shapes=[
            pltpu.VMEM((HEAD_SIZE, tokens), BF16),
            pltpu.VMEM((tokens, LANES), F32),
            pltpu.VMEM((tokens, LANES), F32),
        ],
        cost_estimate=cost(15),
        name="attend_forward",
    )(proj, proj, *tables)


def run_attend_backward(qkv, lse, attended, grads, grad_at, tables):
    tokens, query_width = attended.shape
    vmem = pl.BlockSpec(memory_space=pltpu.VMEM)
    cols = lambda size, at: pl.BlockSpec((tokens, size), lambda turn: (0, at // size))
    return pl.pallas_call(
        attend_backward,
        grid=(1,),
        out_shape=jax.ShapeDtypeStruct((tokens, query_width + 2 * HEAD_SIZE), BF16),
        in_specs=[
            whole_spec(qkv),
            whole_spec(lse),
            whole_spec(attended),
            cols(query_width, grad_at),
        ]
        + [whole_spec(table) for table in tables],
        out_specs=cols(query_width + 2 * HEAD_SIZE, 0),
        scratch_shapes=[
            pltpu.VMEM((tokens, query_width), F32),
            pltpu.VMEM((HEAD_SIZE, tokens), BF16),
            pltpu.VMEM((tokens, LANES), F32),
            pltpu.VMEM((tokens, LANES), F32),
            pltpu.VMEM((tokens, LANES), F32),
            pltpu.VMEM((tokens, LANES), F32),
        ],
        cost_estimate=cost(16),
        name="attend_backward",
    )(qkv, lse, attended, grads, *tables)


def feed_forward(
    x_ref, mixed_ref, other_ref, top_ref, gain_ref, gu_ref, down_ref,
    after_ref, scale_ref, hidden_ref, act_ref, dgu_ref, part_ref, back_ref,
):
    units = down_ref.shape[1]
    after = x_ref[...].astype(F32) + (mixed_ref[...].astype(F32) + other_ref[...].astype(F32))
    after_ref[...] = after
    scale = lax.rsqrt(jnp.mean(after * after, axis=-1, keepdims=True) + EPSILON)
    scale_ref[...] = scale
    hidden = (after * scale * gain_ref[...]).astype(BF16)
    hidden_ref[...] = hidden
    top = top_ref[...]

    def block(turn, carry):
        cols = pl.ds(pl.multiple_of(turn * UBLK, UBLK), UBLK)
        up_cols = pl.ds(pl.multiple_of(units + turn * UBLK, UBLK), UBLK)
        gate = dot(hidden, gu_ref[:, cols])
        upward = dot(hidden, gu_ref[:, up_cols])
        grad = dot(top, down_ref[:, cols])
        sigma = jax.nn.sigmoid(gate)
        swish = gate * sigma
        act_ref[:, cols] = (swish * upward).astype(BF16)
        slope = sigma * (1.0 + gate * (1.0 - sigma))
        dgu_ref[:, cols] = (grad * upward * slope).astype(BF16)
        dgu_ref[:, up_cols] = (grad * swish).astype(BF16)
        return carry

    lax.fori_loop(0, units // UBLK, block, 0)
    back_ref[...] = dot(dgu_ref[...], gu_ref[...], NT).astype(BF16)
    part_ref[...] = dot(act_ref[...], down_ref[...], NT).astype(BF16)


def run_feed_forward(x, mixed, other, top, gain, w_gate_up, w_down_t):
    tokens, width = x.shape
    units = w_down_t.shape[1]
    rows = lambda size: pl.BlockSpec((TBLK, size), lambda turn: (turn, 0))
    once = lambda item: pl.BlockSpec(
        item.shape, lambda turn: (0, 0), pipeline_mode=pl.Buffered(1)
    )
    shape = jax.ShapeDtypeStruct
    return pl.pallas_call(
        feed_forward,
        grid=(tokens // TBLK,),
        out_shape=(
            shape((tokens, width), F32),
            shape((tokens, 1), F32),
            shape((tokens, width), BF16),
            shape((tokens, units), BF16),
            shape((tokens, 2 * units), BF16),
            shape((tokens, width), BF16),
            shape((tokens, width), BF16),
        ),
        in_specs=[rows(width)] * 4 + [once(gain), once(w_gate_up), once(w_down_t)],
        out_specs=(
            rows(width), rows(1), rows(width), rows(units), rows(2 * units), rows(width),
            rows(width),
        ),
        cost_estimate=cost(20),
        name="feed_forward",
    )(x, mixed, other, top, gain, w_gate_up, w_down_t)


def swap(partial):
    return lax.ppermute(partial, "tensor", [(0, 1), (1, 0)])


def join(mine, other):
    return mine.astype(F32) + other.astype(F32)


def tensor_sum(partial):
    return join(partial, swap(partial))


def norm_back(normed, scale, gain, grad):
    weighted = grad * gain
    grad_input = scale * (weighted - normed * jnp.mean(weighted * normed, axis=-1, keepdims=True))
    return (grad_input, jnp.sum(grad * normed, axis=0))


def local(
    layer_input, w_norm1, w_zx, w_bc, w_dt, conv_x, conv_xb, conv_bc, conv_bcb, dt_bias, a_log,
    d_skip, w_mnorm, w_mout, query_key_value_weight, output_weight, w_norm2, w_gu, w_down,
    grad_output,
):
    devices = lax.axis_size("dp")
    tokens, width = layer_input.shape
    shard = w_zx.shape[0]
    channels = conv_xb.shape[0]
    heads = dt_bias.shape[0]
    qkv_width = query_key_value_weight.shape[2]
    units = w_down.shape[0]
    attn_width = output_weight.shape[1]
    tail = jnp.concatenate(
        [w_dt, w_norm1[:, None], w_norm2[:, None], jnp.zeros((shard, LANES - heads - 2), BF16)],
        axis=1,
    )
    mixer_in = jnp.concatenate(
        [w_zx.reshape(shard, -1), w_bc, query_key_value_weight.reshape(shard, -1), tail], axis=1
    )
    in_width = mixer_in.shape[1]
    (w_in,) = gather_rows([mixer_in], devices, 0)
    norm1 = w_in[:, in_width - LANES + heads].astype(F32)
    norm2 = w_in[:, in_width - LANES + heads + 1].astype(F32)

    source = layer_input.astype(F32)
    scale_one = lax.rsqrt(jnp.mean(source * source, axis=-1, keepdims=True) + EPSILON)
    normed_one = source * scale_one
    hidden_one = lax.optimization_barrier((normed_one * norm1).astype(BF16))
    proj = dot(hidden_one, w_in)
    params = scan_params(conv_x, conv_xb, conv_bc, conv_bcb, dt_bias, a_log, d_skip)
    out_shard = jnp.concatenate([w_mout.T, output_weight.reshape(attn_width, -1).T], axis=1)
    y, gated, entering, w_out = run_scan_forward(proj, qkv_width, params, out_shard, devices)
    channels_all = channels * lax.axis_size("tensor")
    square_sum = tensor_sum(jnp.sum(gated * gated, axis=-1))
    scale_m = lax.rsqrt(square_sum / channels_all + EPSILON)[:, None]
    tables = rotary_tables(tokens)
    qkv_at = 2 * channels + 2 * NS
    qkv, lse, attended = run_attend_forward(proj, qkv_at, attn_width, tables)
    gain_m = w_mnorm.astype(F32)
    mamba_low = (gated * scale_m * gain_m).astype(BF16)
    mixer_out = jnp.concatenate([mamba_low, attended], axis=1)
    mixed, gate_up_shard, down_shard = lax.optimization_barrier(
        (dot(mixer_out, w_out, NT).astype(BF16), w_gu.reshape(shard, -1), w_down.T)
    )
    other = swap(mixed)
    w_gate_up, w_down_t = gather_rows([gate_up_shard, down_shard], devices, 3)
    other, w_gate_up, w_down_t = lax.optimization_barrier((other, w_gate_up, w_down_t))
    after, scale_two, hidden_two, activated, grad_gu_low, ffn_part, partial_two = run_feed_forward(
        layer_input, mixed, other, grad_output, norm2[None, :], w_gate_up, w_down_t
    )
    other = swap(partial_two)
    grad_down = dot(grad_output, activated, TN).astype(BF16)
    (mine_gu,) = scatter_product(
        hidden_two,
        grad_gu_low,
        [(0, 1, 0, 2 * units)],
        [(0, 0, units, 0, 0), (0, units, 2 * units, 0, 1)],
        [(shard, 2, units)],
        devices,
        1,
    )
    other, mine_gu, grad_down, ffn_part = lax.optimization_barrier(
        (other, mine_gu, grad_down, ffn_part)
    )
    normed_two = after * scale_two
    grad_hidden_two = join(partial_two, other)
    ffn_other = swap(ffn_part)
    grad_norm_in, grad_norm2 = norm_back(normed_two, scale_two, norm2, grad_hidden_two)
    grad_after = grad_output.astype(F32) + grad_norm_in
    grad_mix_low = grad_after.astype(BF16)
    grad_mixer = dot(grad_mix_low, w_out)
    grad_mamba = grad_mixer[:, :channels]
    normed_m = gated * scale_m
    inner_m = tensor_sum(jnp.sum(grad_mamba * gain_m * normed_m, axis=-1))[:, None] / channels_all
    dqkv = run_attend_backward(
        qkv, lse, attended, grad_mixer[:, channels:].astype(BF16), 0, tables
    )
    grad_out = dot(grad_mix_low, mixer_out, TN).astype(BF16)
    windows = [(0, None, 0, channels + attn_width), (1, None, 0, units)]
    pieces = [
        (0, 0, channels, 0, None),
        (0, channels, channels + attn_width, 1, None),
        (1, 0, units, 2, None),
    ]
    shapes = [(shard, channels), (shard, attn_width), (shard, units)]
    grad_proj, small_x, small_b, small_h, mine_mout, mine_o, mine_down = run_scan_backward(
        proj, y, entering, grad_mamba, scale_m, inner_m, dqkv, params, gain_m[None, :],
        [grad_out, grad_down], windows, pieces, shapes, devices,
    )
    ffn_other, grad_proj = lax.optimization_barrier((ffn_other, grad_proj))
    result = (after + join(ffn_part, ffn_other)).astype(BF16)
    partial_one, grad_proj = lax.optimization_barrier(
        (dot(grad_proj, w_in, NT).astype(BF16), grad_proj)
    )
    crossing = jnp.concatenate(
        [
            small_b[: KCONV + 1].reshape(-1, LANES),
            jnp.sum(partial_one.astype(F32) * normed_one, axis=0).reshape(-1, LANES),
        ],
        axis=0,
    )
    crossing = tensor_sum(crossing)
    partial_one, crossing = lax.optimization_barrier((partial_one, crossing))
    other = swap(partial_one)
    small = jnp.concatenate(
        [
            small_x[: KCONV + 2].reshape(-1, LANES),
            small_h[:3],
            crossing,
            grad_norm2.reshape(-1, LANES),
        ],
        axis=0,
    )
    small_rows = small.shape[0]
    small = jnp.pad(small, ((0, -small_rows % EDGE), (0, 0)))
    shared_at = 2 * channels
    step_at = qkv_at + qkv_width
    mine_zx, mine_bc, mine_qkv, mine_step, small = scatter_product(
        hidden_one,
        grad_proj,
        [(0, 1, 0, in_width)],
        [
            (0, 0, channels, 0, 0),
            (0, channels, shared_at, 0, 1),
            (0, shared_at, qkv_at, 1, None),
            (0, qkv_at, step_at, 2, 0),
            (0, step_at, in_width, 3, "turned"),
        ],
        [
            (shard, 2, channels),
            (shard, 2 * NS),
            (shard, 1, qkv_width),
            (heads, shard),
        ],
        devices,
        5,
        (small,),
    )
    other, mine_bc = lax.optimization_barrier((other, mine_bc))
    grad_hidden_one = join(partial_one, other)
    weighted = grad_hidden_one * norm1
    grad_source = grad_after + scale_one * (
        weighted - normed_one * jnp.mean(weighted * normed_one, axis=-1, keepdims=True)
    )

    half = NS * 2 // lax.axis_size("tensor")
    shared_cols = tensor_sum(mine_bc)
    begin = lax.axis_index("tensor") * half
    grad_bc = lax.dynamic_slice_in_dim(shared_cols, begin, half, 1)
    small = small[:small_rows].reshape(-1)
    x_size = (KCONV + 2) * channels
    h_size = 3 * LANES
    b_size = (KCONV + 1) * 2 * NS
    total_x = small[:x_size].reshape(KCONV + 2, channels)
    total_h = small[x_size : x_size + h_size].reshape(3, LANES)
    total_b = small[x_size + h_size : x_size + h_size + b_size].reshape(KCONV + 1, 2 * NS)
    total_b = lax.dynamic_slice_in_dim(total_b, begin, half, 1)
    norms = small[x_size + h_size + b_size :].reshape(2, width)
    norms = lax.dynamic_slice_in_dim(norms, lax.axis_index("dp") * shard, shard, 1)
    return (
        result,
        grad_source,
        norms[0],
        mine_zx,
        grad_bc,
        mine_step.T,
        total_x[:KCONV],
        total_x[KCONV],
        total_b[:KCONV],
        total_b[KCONV],
        total_h[0, :heads],
        total_h[1, :heads],
        total_h[2, :heads],
        total_x[KCONV + 1],
        mine_mout.T,
        mine_qkv,
        mine_o.T.reshape(output_weight.shape),
        norms[1],
        mine_gu,
        mine_down.T,
    )


def solution(mesh):
    return jax.shard_map(
        local,
        mesh=mesh,
        in_specs=(
            P("dp", None),
            P("dp"),
            P("dp", None, "tensor"),
            P("dp", None),
            P("dp", "tensor"),
            P(None, "tensor"),
            P("tensor"),
            P(),
            P(),
            P("tensor"),
            P("tensor"),
            P("tensor"),
            P("tensor"),
            P("tensor", "dp"),
            P("dp", "tensor", None),
            P("tensor", None, "dp"),
            P("dp"),
            P("dp", None, "tensor"),
            P("tensor", "dp"),
            P("dp", None),
        ),
        out_specs=(
            P("dp", None),
            P("dp", None),
            P("dp"),
            P("dp", None, "tensor"),
            P("dp", "tensor"),
            P("dp", "tensor"),
            P(None, "tensor"),
            P("tensor"),
            P(None, "tensor"),
            P("tensor"),
            P("tensor"),
            P("tensor"),
            P("tensor"),
            P("tensor"),
            P("tensor", "dp"),
            P("dp", "tensor", None),
            P("tensor", None, "dp"),
            P("dp"),
            P("dp", None, "tensor"),
            P("tensor", "dp"),
        ),
        check_vma=False,
    )
```

```python
import functools
import math

import jax
import jax.numpy as jnp
import numpy as np
from jax import lax
from jax.experimental import pallas as pl
from jax.experimental.pallas import tpu as pltpu
from jax.sharding import PartitionSpec as P

HEAD_SIZE = 64
MP = 64
NS = 128
KCONV = 4
SPAN = 128
QBLK = 256
FINE = 32
TBLK = 256
NBLK = 128
UBLK = 256
LANES = 128
EDGE = 8

EPSILON = 1e-05
HIGHEST = lax.Precision.HIGHEST
LOG_BASE = math.log(100000000000.0)
MASKED = -1e30
MESH = pl.DeviceIdType.MESH
F32 = jnp.float32
BF16 = jnp.bfloat16

NN = ((1,), (0,))
NT = ((1,), (1,))
TN = ((0,), (0,))


def dot(left, right, dims=NN, precision=None):
    return lax.dot_general(
        left, right, (dims, ((), ())), preferred_element_type=F32, precision=precision
    )


def iota(shape, dim):
    return lax.broadcasted_iota(jnp.int32, shape, dim)


def ring_place(chip, chips):
    odd = lax.rem(chip, 2)
    half = lax.div(chip, 2)
    return (1 - odd) * half + odd * (chips - 1 - half)


def ring_chip(place, chips):
    place = lax.rem(place + 4 * chips, chips)
    back = lax.div(place, chips // 2)
    return (1 - back) * (2 * place) + back * (2 * (chips - 1 - place) + 1)


def ring_setup(chips):
    me = lax.axis_index("dp")
    group = lax.axis_index("tensor")
    chip = lax.div(me, 2)
    core = lax.rem(me, 2)
    place = ring_place(chip, chips)
    right = ring_chip(place + 1, chips) * 2 + core
    left = ring_chip(place - 1, chips) * 2 + core
    mate = chip * 2 + (1 - core)
    barrier = pltpu.get_barrier_semaphore()
    for other in (right, left, mate):
        pl.semaphore_signal(barrier, inc=1, device_id=(other, group), device_id_type=MESH)
    pl.semaphore_wait(barrier, 3)
    return me, group, core, place, right, left, mate


class RingGather:
    def __init__(self, devices, x_ref, o_ref, sems):
        self.chips = devices // 2
        self.ahead = self.chips // 2
        self.behind = self.chips - 1 - self.ahead
        self.x_ref, self.o_ref, self.rows = x_ref, o_ref, x_ref.shape[0]
        self.fs, self.fr, self.bs, self.br, self.cs, self.cr, self.own_sem = sems

    def locate(self):
        me = lax.axis_index("dp")
        self.group = lax.axis_index("tensor")
        self.core = lax.rem(me, 2)
        chip = lax.div(me, 2)
        self.place = ring_place(chip, self.chips)
        self.right = ring_chip(self.place + 1, self.chips) * 2 + self.core
        self.left = ring_chip(self.place - 1, self.chips) * 2 + self.core
        self.mate = chip * 2 + (1 - self.core)
        self.me = me

    def slot(self, index):
        return self.o_ref.at[pl.ds(pl.multiple_of(index * self.rows, self.rows), self.rows), :]

    def copy(self, shift, ssem, rsem, target):
        if shift == 0:
            index, source = self.me, self.x_ref
        else:
            index = ring_chip(self.place + shift, self.chips) * 2 + self.core
            source = self.slot(index)
        return pltpu.make_async_remote_copy(
            src_ref=source,
            dst_ref=self.slot(index),
            send_sem=ssem,
            recv_sem=rsem,
            device_id=(target, self.group),
            device_id_type=MESH,
        )

    def fore(self, step):
        return self.copy(-step, self.fs.at[step], self.fr.at[step], self.right)

    def back(self, step):
        return self.copy(step, self.bs.at[step], self.br.at[step], self.left)

    def across(self, shift):
        number = 0 if shift == 0 else 2 * abs(shift) - (1 if shift < 0 else 0)
        return self.copy(shift, self.cs.at[number], self.cr.at[number], self.mate)

    def own(self):
        return pltpu.make_async_copy(self.x_ref, self.slot(self.me), self.own_sem)

    def greet(self):
        self.locate()
        barrier = pltpu.get_barrier_semaphore()
        for other in (self.right, self.left, self.mate):
            pl.semaphore_signal(
                barrier, inc=1, device_id=(other, self.group), device_id_type=MESH
            )
        pl.semaphore_wait(barrier, 3)

    def begin(self):
        self.locate()
        self.fore(0).start()
        self.back(0).start()
        self.across(0).start()
        self.own().start()

    def hop(self, step):
        self.locate()
        self.fore(step - 1).wait_recv()
        if step < self.ahead:
            self.fore(step).start()
        self.across(-step).start()
        if step <= self.behind:
            self.back(step - 1).wait_recv()
            if step < self.behind:
                self.back(step).start()
            self.across(step).start()

    def finish(self):
        self.locate()
        self.own().wait()
        for step in range(self.ahead):
            self.fore(step).wait_send()
        for step in range(self.behind):
            self.back(step).wait_send()
        for shift in range(-self.ahead, self.behind + 1):
            self.across(shift).wait()


def gather_sems(devices):
    dma = pltpu.SemaphoreType.DMA
    return [dma((devices // 2,))] * 6 + [dma(())]


def gather_shape(shard, devices):
    return jax.ShapeDtypeStruct((shard.shape[0] * devices, shard.shape[1]), shard.dtype)


def gather_kernel(devices, count, *refs):
    shards, outs, sems = refs[:count], refs[count : 2 * count], refs[2 * count :]
    each = len(sems) // count
    rings = [
        RingGather(devices, shards[i], outs[i], sems[i * each : (i + 1) * each])
        for i in range(count)
    ]
    rings[0].greet()
    for ring in rings:
        ring.begin()
    for step in range(1, rings[0].ahead + 1):
        for ring in rings:
            ring.hop(step)
    for ring in rings:
        ring.finish()


def cost(micros):
    return pl.CostEstimate(flops=int(micros * 1e9), bytes_accessed=0, transcendentals=0)


def gather_rows(shards, devices, collective):
    count = len(shards)
    anywhere = pl.BlockSpec(memory_space=pl.ANY)
    return pl.pallas_call(
        functools.partial(gather_kernel, devices, count),
        out_shape=tuple(gather_shape(shard, devices) for shard in shards),
        in_specs=[anywhere] * count,
        out_specs=(anywhere,) * count,
        scratch_shapes=gather_sems(devices) * count,
        compiler_params=pltpu.CompilerParams(collective_id=collective, has_side_effects=True),
        cost_estimate=cost(3),
        name="gather_rows",
    )(*shards)


def scatter_order(chips):
    ahead = chips // 2
    behind = chips - 1 - ahead
    order = []
    for step in range(ahead):
        order.append(-(ahead - step))
        if step < behind:
            order.append(behind - step)
    order.append(0)
    return order


class RingScatter:
    def __init__(self, devices, windows, pieces, operands, outs, scratch):
        self.chips = devices // 2
        self.ahead = self.chips // 2
        self.behind = self.chips - 1 - self.ahead
        self.windows, self.pieces, self.operands, self.outs = windows, pieces, operands, outs
        count = len(windows)
        self.mine, self.boxes, rest = scratch[:count], scratch[count : 2 * count], scratch[2 * count :]
        self.fbox, self.bbox, self.fout, self.bout = rest[:4]
        self.os, self.ms, self.mr, self.fs, self.fr, self.bs, self.br = rest[4:]
        self.rows = self.fbox.shape[1]
        widths = [item.shape[2] for item in self.mine]
        self.cols = [slice(sum(widths[:i]), sum(widths[: i + 1])) for i in range(count)]

    def locate(self):
        me = lax.axis_index("dp")
        self.group = lax.axis_index("tensor")
        self.core = lax.rem(me, 2)
        chip = lax.div(me, 2)
        self.place = ring_place(chip, self.chips)
        self.right = ring_chip(self.place + 1, self.chips) * 2 + self.core
        self.left = ring_chip(self.place - 1, self.chips) * 2 + self.core
        self.mate = chip * 2 + (1 - self.core)

    def greet(self):
        self.locate()
        barrier = pltpu.get_barrier_semaphore()
        for other in (self.right, self.left, self.mate):
            pl.semaphore_signal(
                barrier, inc=1, device_id=(other, self.group), device_id_type=MESH
            )
        pl.semaphore_wait(barrier, 3)

    def product(self, i):
        return self.windows[i][1] is not None

    def shift_of(self, slot):
        step = slot // 2
        odd = slot % 2
        return (1 - odd) * (step - self.ahead) + odd * (self.behind - step)

    def half(self, which):
        return pl.ds(pl.multiple_of(which * self.rows, self.rows), self.rows)

    def block(self, i, slot, which):
        index = ring_chip(self.place + self.shift_of(slot), self.chips) * 2 + which
        left, right, first, last = self.windows[i]
        return self.operands[left].at[self.half(index), first:last]

    def remote(self, source, target_ref, ssem, rsem, target):
        return pltpu.make_async_remote_copy(
            src_ref=source,
            dst_ref=target_ref,
            send_sem=ssem,
            recv_sem=rsem,
            device_id=(target, self.group),
            device_id_type=MESH,
        )

    def across(self, i, slot):
        if self.product(i):
            source = self.mine[i].at[slot, self.half(1 - self.core)]
        else:
            source = self.block(i, slot, 1 - self.core)
        return self.remote(
            source, self.boxes[i].at[slot], self.ms.at[i, slot], self.mr.at[i, slot], self.mate
        )

    def own(self, i, slot):
        return pltpu.make_async_copy(
            self.block(i, slot, self.core), self.mine[i].at[slot], self.os.at[i, slot]
        )

    def fore(self, step):
        return self.remote(
            self.fout.at[step], self.fbox.at[step], self.fs.at[step], self.fr.at[step], self.right
        )

    def back(self, step):
        return self.remote(
            self.bout.at[step], self.bbox.at[step], self.bs.at[step], self.br.at[step], self.left
        )

    def begin(self):
        self.locate()
        for i in range(len(self.windows)):
            if not self.product(i):
                for slot in range(self.chips):
                    self.across(i, slot).start()
                    self.own(i, slot).start()

    def produce(self, slot):
        chip = ring_chip(self.place + self.shift_of(slot), self.chips)
        size = 2 * self.rows
        for i, (left, right, first, last) in enumerate(self.windows):
            if right is None:
                continue
            at = pl.multiple_of(chip * size, size)
            terms = dot(self.operands[left][pl.ds(at, size), :], self.operands[right][:, first:last])
            self.mine[i][slot] = terms.astype(BF16)
            self.across(i, slot).start()

    def local_sum(self, i, slot, cols, others):
        rows = self.half(self.core) if self.product(i) else slice(None)
        total = self.mine[i][slot, rows, cols].astype(F32) + self.boxes[i][slot, :, cols].astype(F32)
        whole = slice(self.cols[i].start + cols.start, self.cols[i].start + cols.stop)
        for ref in others:
            total = total + ref[:, whole].astype(F32)
        return total

    def arrive(self, slot):
        for i in range(len(self.windows)):
            if not self.product(i):
                self.own(i, slot).wait()
            self.across(i, slot).wait_recv()

    def put(self, target, slot, others):
        self.arrive(slot)
        for i, cols in enumerate(self.cols):
            total = self.local_sum(i, slot, slice(0, cols.stop - cols.start), others)
            target[:, cols] = total.astype(BF16)

    def hop_back(self, step, later):
        if later:
            self.back(step - 1).wait_recv()
        self.put(self.bout.at[step], 2 * step, [self.bbox.at[step - 1]] if later else [])
        self.back(step).start()

    def hop_fore(self, step, later):
        if later:
            self.fore(step - 1).wait_recv()
        self.put(self.fout.at[step], 2 * step + 1, [self.fbox.at[step - 1]] if later else [])
        self.fore(step).start()

    def hop(self, step):
        self.locate()
        self.hop_back(step, step > 0)
        if step < self.behind:
            self.hop_fore(step, step > 0)

    def run(self, after_first=None):
        def turn(step, carry):
            lax.fori_loop(0, 2, lambda part, kept: (self.produce(2 * step + part), kept)[1], 0)

            @pl.when(step == 0)
            def _():
                self.hop_back(0, False)
                self.hop_fore(0, False)
                if after_first is not None:
                    after_first()

            pl.when(step > 0)(lambda: self.hop_back(step, True))
            pl.when((step > 0) & (step < self.behind))(lambda: self.hop_fore(step, True))
            return carry

        lax.fori_loop(0, self.ahead, turn, 0)

    def finish(self):
        self.locate()
        slot = self.chips - 1
        self.arrive(slot)
        self.fore(self.behind - 1).wait_recv()
        self.back(self.ahead - 1).wait_recv()
        others = [self.fbox.at[self.behind - 1], self.bbox.at[self.ahead - 1]]
        for i, first, last, out, form in self.pieces:
            total = self.local_sum(i, slot, slice(first, last), others)
            if form == "turned":
                self.outs[out][...] = total.T[: self.outs[out].shape[0]]
            elif form is None:
                self.outs[out][...] = total
            else:
                self.outs[out][:, form, :] = total
        for step in range(self.ahead):
            self.back(step).wait_send()
        for step in range(self.behind):
            self.fore(step).wait_send()
        for slot in range(self.chips):
            for i in range(len(self.windows)):
                self.across(i, slot).wait_send()


def scatter_scratch(windows, rows, devices):
    chips = devices // 2
    count = len(windows)
    dma = pltpu.SemaphoreType.DMA
    widths = [last - first for left, right, first, last in windows]
    mine = [
        pltpu.VMEM((chips, rows if right is None else 2 * rows, last - first), BF16)
        for left, right, first, last in windows
    ]
    boxes = [pltpu.VMEM((chips, rows, width), BF16) for width in widths]
    box = pltpu.VMEM((chips // 2, rows, sum(widths)), BF16)
    return mine + boxes + [box] * 4 + [dma((count, chips))] * 3 + [dma((chips,))] * 4


class Total:
    def __init__(self, devices, x_ref, o_ref, scratch):
        self.chips = devices // 2
        self.x_ref, self.o_ref = x_ref, o_ref
        self.mate_box, self.joined, self.boxes, self.ms, self.mr, self.ss, self.sr = scratch
        me = lax.axis_index("dp")
        self.group = lax.axis_index("tensor")
        self.chip = lax.div(me, 2)
        core = lax.rem(me, 2)
        self.mate = self.chip * 2 + (1 - core)
        self.peers = [
            lax.rem(self.chip + shift, self.chips) * 2 + core for shift in range(self.chips)
        ]

    def greet(self):
        barrier = pltpu.get_barrier_semaphore()
        for other in [self.mate] + self.peers[1:]:
            pl.semaphore_signal(
                barrier, inc=1, device_id=(other, self.group), device_id_type=MESH
            )
        pl.semaphore_wait(barrier, self.chips)

    def remote(self, source, target_ref, ssem, rsem, target):
        return pltpu.make_async_remote_copy(
            src_ref=source,
            dst_ref=target_ref,
            send_sem=ssem,
            recv_sem=rsem,
            device_id=(target, self.group),
            device_id_type=MESH,
        )

    def across(self):
        return self.remote(self.x_ref, self.mate_box, self.ms, self.mr, self.mate)

    def copies(self):
        return [
            self.remote(
                self.joined,
                self.boxes.at[self.chip],
                self.ss.at[shift],
                self.sr.at[shift],
                self.peers[shift],
            )
            for shift in range(1, self.chips)
        ]

    def begin(self):
        self.across().start()

    def spread(self):
        self.across().wait_recv()
        self.joined[...] = self.x_ref[...] + self.mate_box[...]
        for copy in self.copies():
            copy.start()
        self.boxes[self.chip] = self.joined[...]

    def finish(self):
        for copy in self.copies():
            copy.wait_recv()
        result = self.boxes[0]
        for other in range(1, self.chips):
            result = result + self.boxes[other]
        self.o_ref[...] = result
        self.across().wait_send()
        for copy in self.copies():
            copy.wait_send()


def total_scratch(values, devices):
    chips = devices // 2
    dma = pltpu.SemaphoreType.DMA
    return [
        pltpu.VMEM(values.shape, F32),
        pltpu.VMEM(values.shape, F32),
        pltpu.VMEM((chips,) + values.shape, F32),
        dma(()),
        dma(()),
        dma((chips,)),
        dma((chips,)),
    ]


def turned_copy(source, target):
    for start in range(0, source.shape[1], LANES):
        target[start : start + LANES, :] = source[:, start : start + LANES].T


def product_kernel(devices, windows, pieces, outs, summed, left_ref, right_ref, *refs):
    values = refs[:summed]
    refs = refs[summed:]
    pieces_out, refs = refs[:outs], refs[outs:]
    totals_out, refs = refs[:summed], refs[summed:]
    turned, scratch = refs[0], refs[1:]
    total = None
    if summed:
        scratch, rest = scratch[:-7], scratch[-7:]
        total = Total(devices, values[0], totals_out[0], rest)
    ring = RingScatter(devices, windows, pieces, (turned, right_ref), pieces_out, scratch)
    if total is None:
        ring.greet()
    else:
        ring.locate()
        total.greet()
        total.begin()
    turned_copy(left_ref, turned)
    ring.run(total.spread if total is not None else None)
    ring.finish()
    if total is not None:
        total.finish()


def scatter_product(left, right, windows, pieces, shapes, devices, collective, values=()):
    vmem = pl.BlockSpec(memory_space=pltpu.VMEM)
    rows = left.shape[1] // devices
    scratch = [pltpu.VMEM(left.shape[::-1], BF16)] + scatter_scratch(windows, rows, devices)
    for item in values:
        scratch += total_scratch(item, devices)
    return pl.pallas_call(
        functools.partial(
            product_kernel, devices, windows, pieces, len(shapes), len(values)
        ),
        out_shape=tuple(jax.ShapeDtypeStruct(shape, F32) for shape in shapes)
        + tuple(jax.ShapeDtypeStruct(item.shape, F32) for item in values),
        in_specs=[vmem] * (2 + len(values)),
        out_specs=(vmem,) * (len(shapes) + len(values)),
        scratch_shapes=scratch,
        compiler_params=pltpu.CompilerParams(collective_id=collective, has_side_effects=True),
        cost_estimate=cost(3),
        name="scatter_product",
    )(left, right, *values)


def head_spread(channels):
    return (iota((LANES, channels), 1) // MP == iota((LANES, channels), 0)).astype(BF16)


def parts(values, count):
    terms = []
    for _ in range(count):
        term = values.astype(BF16)
        terms.append(term)
        values = values - term.astype(F32)
    return terms


def pick(values, mask, count=2):
    return dot(jnp.concatenate(parts(values, count), axis=1), jnp.concatenate([mask] * count, axis=0))


def pick_left(mask, values, count):
    return dot(jnp.concatenate([mask] * count, axis=1), jnp.concatenate(parts(values, count), axis=0))


def gather_heads(values, spread):
    high, low = parts(values, 2)
    return dot(high, spread, NT) + dot(low, spread, NT)


def row_sums(values):
    high, low = parts(values, 2)
    ones = jnp.ones((EDGE, values.shape[1]), BF16)
    return dot(ones, high, NT) + dot(ones, low, NT)


def soft_step(raw):
    return jnp.maximum(raw, 0.0) + jnp.log1p(jnp.exp(-jnp.abs(raw)))


def conv_window(buffer, taps_ref, bias_ref, span):
    total = bias_ref[...] + taps_ref[0:1, :] * buffer[EDGE - 3 : EDGE - 3 + span, :]
    for tap in range(1, KCONV):
        start = EDGE - 3 + tap
        total = total + taps_ref[tap : tap + 1, :] * buffer[start : start + span, :]
    return total


def span_rates(step_ref, bias_ref, decay_ref, spread, span):
    raw = step_ref[...] + bias_ref[...]
    step = soft_step(raw)
    lower = (iota((span, span), 1) <= iota((span, span), 0)).astype(BF16)
    cum = pick_left(lower, step * decay_ref[...], 3)
    tails = jnp.exp(cum[span - 1 : span, :] - cum)
    wide = pick(jnp.concatenate([step, tails, jnp.exp(cum)], axis=0), spread)
    return raw, step, cum, wide[:span], wide[span : 2 * span], wide[2 * span :]


def pair_split(values, low_lanes):
    zero = jnp.zeros_like(values)
    return jnp.concatenate(
        [jnp.where(low_lanes, values, zero), jnp.where(low_lanes, zero, values)], axis=0
    )


def pair_decay(cum, cum_rows, pair, causal):
    parts = []
    for head in (2 * pair, 2 * pair + 1):
        differ = cum[:, head : head + 1] - cum_rows[head : head + 1, :]
        parts.append(jnp.exp(jnp.where(causal, differ, MASKED)))
    return parts


def scan_forward(
    devices, spans,
    z_ref, x_ref, bc_ref, step_ref,
    tap_ref, bias_ref, tapb_ref, biasb_ref, stepb_ref, decay_ref, skip_ref, shard_ref,
    y_ref, gated_ref, square_ref, enter_ref, all_ref,
    state, xbuf, bbuf, *sems,
):
    span, channels = x_ref.shape
    ring = RingGather(devices, shard_ref, all_ref, sems)
    turn = pl.program_id(0)

    @pl.when(turn == 0)
    def _():
        ring.greet()
        ring.begin()


    @pl.when(pl.program_id(0) == 0)
    def _():
        state[...] = jnp.zeros_like(state)
        xbuf[span:, :] = jnp.zeros((EDGE, channels), F32)
        bbuf[span:, :] = jnp.zeros((EDGE, 2 * NS), F32)

    xbuf[:EDGE, :] = xbuf[span:, :]
    bbuf[:EDGE, :] = bbuf[span:, :]
    xbuf[EDGE:, :] = x_ref[...]
    bbuf[EDGE:, :] = bc_ref[...]
    inputs = jax.nn.silu(conv_window(xbuf, tap_ref, bias_ref, span))
    shared = jax.nn.silu(conv_window(bbuf, tapb_ref, biasb_ref, span))
    spread = head_spread(channels)
    raw, step, cum, step_w, tails_w, grown_w = span_rates(
        step_ref, stepb_ref, decay_ref, spread, span
    )
    cum_rows = cum.T
    b_low = shared[:, :NS].astype(BF16)
    c_low = shared[:, NS:].astype(BF16)
    scaled = inputs * step_w
    scaled_low = scaled.astype(BF16)
    enter_ref[0] = state[...]
    outer = dot(c_low, state[...].astype(BF16)) * grown_w
    fresh = dot(b_low, (scaled * tails_w).astype(BF16), TN)
    state[...] = state[...] * grown_w[span - 1 : span, :] + fresh
    cross = dot(c_low, b_low, NT)
    causal = iota((span, span), 1) <= iota((span, span), 0)
    low_lanes = iota((span, LANES), 1) < MP
    for pair in range(channels // LANES):
        lanes = slice(pair * LANES, (pair + 1) * LANES)
        first, second = pair_decay(cum, cum_rows, pair, causal)
        weights = jnp.concatenate(
            [(cross * first).astype(BF16), (cross * second).astype(BF16)], axis=1
        )
        y_ref[:, lanes] = dot(weights, pair_split(scaled_low[:, lanes], low_lanes))
    y = y_ref[...] + outer + skip_ref[...] * inputs
    y_ref[...] = y
    gated = y * jax.nn.silu(z_ref[...])
    gated_ref[...] = gated
    square_ref[...] = row_sums(gated * gated)

    count = spans
    for step in range(1, ring.ahead + 1):
        pl.when(turn == min(count - 1, count * step // ring.ahead))(
            functools.partial(ring.hop, step)
        )
    pl.when(turn == count - 1)(ring.finish)


def scan_backward(
    devices, spans, windows, pieces, outs_count, count,
    z_ref, x_ref, xp_ref, bc_ref, bp_ref, step_ref, y_ref, enter_ref,
    dyg_ref, scale_ref, inner_ref, dqkv_ref,
    tap_ref, bias_ref, tapb_ref, biasb_ref, stepb_ref, decay_ref, skip_ref, gain_ref,
    *refs,
):
    sent, refs = refs[:count], refs[count:]
    (grad_ref, gx_ref, gb_ref, gh_ref), refs = refs[:4], refs[4:]
    outs, refs = refs[:outs_count], refs[outs_count:]
    (dstate, xbuf, bbuf, dxbuf, dbbuf, du_buf, col_buf), scratch = refs[:7], refs[7:]
    ring = RingScatter(devices, windows, pieces, sent, outs, scratch)
    span, channels = x_ref.shape
    turn = pl.program_id(0)

    @pl.when(turn == 0)
    def _():
        ring.greet()
        ring.begin()
        dstate[...] = jnp.zeros_like(dstate)
        dxbuf[...] = jnp.zeros_like(dxbuf)
        dbbuf[...] = jnp.zeros_like(dbbuf)
        col_buf[...] = jnp.zeros_like(col_buf)
        gx_ref[...] = jnp.zeros_like(gx_ref)
        gb_ref[...] = jnp.zeros_like(gb_ref)
        gh_ref[...] = jnp.zeros_like(gh_ref)

    inside = (turn < spans - 1).astype(F32)
    xbuf[:EDGE, :] = xp_ref[...] * inside
    bbuf[:EDGE, :] = bp_ref[...] * inside
    xbuf[EDGE:, :] = x_ref[...]
    bbuf[EDGE:, :] = bc_ref[...]
    conv = conv_window(xbuf, tap_ref, bias_ref, span)
    sig = jax.nn.sigmoid(conv)
    inputs = conv * sig
    convb = conv_window(bbuf, tapb_ref, biasb_ref, span)
    sigb = jax.nn.sigmoid(convb)
    shared = convb * sigb
    b_low = shared[:, :NS].astype(BF16)
    c_low = shared[:, NS:].astype(BF16)
    spread = head_spread(channels)
    raw, step, cum, step_w, tails_w, grown_w = span_rates(
        step_ref, stepb_ref, decay_ref, spread, span
    )
    cum_rows = cum.T
    scaled = inputs * step_w
    scaled_low = scaled.astype(BF16)

    z = z_ref[...]
    sig_z = jax.nn.sigmoid(z)
    swish = z * sig_z
    y = y_ref[...]
    scale = scale_ref[...].T[:, :1]
    normed = y * swish * scale
    dyg = dyg_ref[...]
    gain_grad = jnp.sum(dyg * normed, axis=0, keepdims=True)
    dgated = scale * (dyg * gain_ref[...] - normed * inner_ref[...].T[:, :1])
    dy = dgated * swish
    grad_ref[:, :channels] = (dgated * y * (sig_z * (1.0 + z * (1.0 - sig_z)))).astype(BF16)

    state_low = enter_ref[0].astype(BF16)
    dstate_low = dstate[...].astype(BF16)
    grown_low = (dy * grown_w).astype(BF16)
    dy_low = dy.astype(BF16)
    tailed = scaled * tails_w
    outer = dot(c_low, state_low) * grown_w
    from_state = dot(b_low, dstate_low)
    dc = dot(grown_low, state_low, NT)
    db = dot(tailed.astype(BF16), dstate_low, NT)
    leak = from_state * tailed
    last_w = grown_w[span - 1 : span, :]
    ends = (
        jnp.sum(leak, axis=0, keepdims=True)
        + jnp.sum(enter_ref[0] * dstate[...], axis=0, keepdims=True) * last_w
    )
    skips = jnp.sum(dy * inputs, axis=0, keepdims=True)
    dstate[...] = dstate[...] * last_w + dot(c_low, grown_low, TN)

    cross = dot(c_low, b_low, NT)
    causal = iota((span, span), 1) <= iota((span, span), 0)
    low_lanes = iota((span, LANES), 1) < MP
    lane = iota((span, LANES), 1)
    dcross = jnp.zeros((span, span), F32)
    row_part = jnp.zeros((span, LANES), F32)
    for pair in range(channels // LANES):
        lanes = slice(pair * LANES, (pair + 1) * LANES)
        decays = pair_decay(cum, cum_rows, pair, causal)
        dy_pair = pair_split(dy_low[:, lanes], low_lanes)
        dweights = dot(dy_pair, scaled_low[:, lanes], NT)
        both = []
        for part in range(2):
            head = 2 * pair + part
            dterm = dweights[part * span : (part + 1) * span] * decays[part]
            dcross = dcross + dterm
            flow = dterm * cross
            row_part = row_part + jnp.where(
                lane == head, jnp.sum(flow, axis=1, keepdims=True), 0.0
            )
            col_buf[head : head + 1, :] = jnp.sum(flow, axis=0, keepdims=True)
            both.append((cross * decays[part]).astype(BF16))
        du_buf[:, lanes] = dot(jnp.concatenate(both, axis=0), dy_pair, TN)
    du = du_buf[...] + from_state * tails_w
    dcross_low = dcross.astype(BF16)
    dc = dc + dot(dcross_low, b_low)
    db = db + dot(dcross_low, c_low, TN)

    sums = gather_heads(
        jnp.concatenate(
            [dy * outer - leak, du * inputs, ends, skips, jnp.zeros((EDGE - 2, channels), F32)],
            axis=0,
        ),
        spread,
    )
    at_end = sums[2 * span : 2 * span + 1, :]
    dcum = sums[:span] + row_part - col_buf[...].T
    upper = (iota((span, span), 1) >= iota((span, span), 0)).astype(BF16)
    drate = pick_left(upper, dcum, 3) + at_end
    dstep = drate * decay_ref[...] + sums[span : 2 * span]
    draw = dstep * jax.nn.sigmoid(raw)
    gh_ref[0:1, :] += jnp.sum(draw, axis=0, keepdims=True)
    gh_ref[1:2, :] += jnp.sum(drate * step, axis=0, keepdims=True) * decay_ref[...]
    gh_ref[2:3, :] += sums[2 * span + 1 : 2 * span + 2, :]

    dinputs = du * step_w + skip_ref[...] * dy
    dxbuf[span:, :] = dxbuf[:EDGE, :]
    dbbuf[span:, :] = dbbuf[:EDGE, :]
    dconv = dinputs * (sig * (1.0 + conv * (1.0 - sig)))
    dconvb = jnp.concatenate([db, dc], axis=1) * (sigb * (1.0 + convb * (1.0 - sigb)))
    dxbuf[:span, :] = dconv
    dbbuf[:span, :] = dconvb
    dx = jnp.zeros_like(dconv)
    dbc = jnp.zeros_like(dconvb)
    for tap in range(KCONV):
        back = KCONV - 1 - tap
        start = EDGE - 3 + tap
        dx = dx + tap_ref[tap : tap + 1, :] * dxbuf[back : back + span, :]
        dbc = dbc + tapb_ref[tap : tap + 1, :] * dbbuf[back : back + span, :]
        gx_ref[tap : tap + 1, :] += jnp.sum(
            dconv * xbuf[start : start + span, :], axis=0, keepdims=True
        )
        gb_ref[tap : tap + 1, :] += jnp.sum(
            dconvb * bbuf[start : start + span, :], axis=0, keepdims=True
        )
    gx_ref[KCONV : KCONV + 1, :] += jnp.sum(dconv, axis=0, keepdims=True)
    gb_ref[KCONV : KCONV + 1, :] += jnp.sum(dconvb, axis=0, keepdims=True)
    gx_ref[KCONV + 1 : KCONV + 2, :] += gain_grad
    width = 2 * channels + 2 * NS
    grad_ref[:, channels : 2 * channels] = dx.astype(BF16)
    grad_ref[:, 2 * channels : width] = dbc.astype(BF16)
    grad_ref[:, width : width + dqkv_ref.shape[1]] = dqkv_ref[...]
    grad_ref[:, width + dqkv_ref.shape[1] :] = draw.astype(BF16)
    for step in range(ring.ahead):
        pl.when(turn == spans * step // ring.ahead)(functools.partial(ring.hop, step))
    pl.when(turn == spans - 1)(ring.finish)


def scan_params(conv_x, conv_xb, conv_bc, conv_bcb, dt_bias, a_log, d_skip):
    heads = dt_bias.shape[0]

    def wide(row):
        return jnp.pad(row, (0, LANES - heads))[None, :]

    f32 = lambda value: value.astype(F32)
    return (
        f32(conv_x),
        f32(conv_xb)[None, :],
        f32(conv_bc),
        f32(conv_bcb)[None, :],
        wide(f32(dt_bias)),
        wide(-jnp.exp(f32(a_log))),
        jnp.repeat(f32(d_skip), MP)[None, :],
    )


def whole_spec(array):
    return pl.BlockSpec(array.shape, lambda turn: (0,) * array.ndim)


def run_scan_forward(proj, qkv_width, params, shard, devices):
    tokens = proj.shape[0]
    channels = params[1].shape[1]
    step_at = (2 * channels + 2 * NS + qkv_width) // LANES
    spans = tokens // SPAN
    bc_at = 2 * channels // (2 * NS)
    rows = lambda width, at: pl.BlockSpec((SPAN, width), lambda turn: (turn, at))
    anywhere = pl.BlockSpec(memory_space=pl.ANY)
    return pl.pallas_call(
        functools.partial(scan_forward, devices, spans),
        grid=(spans,),
        out_shape=(
            jax.ShapeDtypeStruct((tokens, channels), F32),
            jax.ShapeDtypeStruct((tokens, channels), F32),
            jax.ShapeDtypeStruct((EDGE, tokens), F32),
            jax.ShapeDtypeStruct((spans, NS, channels), F32),
            gather_shape(shard, devices),
        ),
        in_specs=[rows(channels, 0), rows(channels, 1), rows(2 * NS, bc_at), rows(LANES, step_at)]
        + [whole_spec(item) for item in params]
        + [anywhere],
        out_specs=(
            rows(channels, 0),
            rows(channels, 0),
            pl.BlockSpec((EDGE, SPAN), lambda turn: (0, turn)),
            pl.BlockSpec((1, NS, channels), lambda turn: (turn, 0, 0)),
            anywhere,
        ),
        scratch_shapes=[
            pltpu.VMEM((NS, channels), F32),
            pltpu.VMEM((SPAN + EDGE, channels), F32),
            pltpu.VMEM((SPAN + EDGE, 2 * NS), F32),
        ]
        + gather_sems(devices),
        compiler_params=pltpu.CompilerParams(collective_id=2, has_side_effects=True),
        cost_estimate=cost(20),
        name="scan_forward",
    )(proj, proj, proj, proj, *params, shard)


def run_scan_backward(
    proj, y, entering, dyg, scale, inner, dqkv, params, gain, sent, windows, pieces,
    shapes, devices,
):
    tokens, width = proj.shape
    channels = params[1].shape[1]
    qkv_width = dqkv.shape[1]
    step_at = (2 * channels + 2 * NS + qkv_width) // LANES
    spans = tokens // SPAN
    bc_at = 2 * channels // (2 * NS)
    edges = SPAN // EDGE
    rows = lambda size, at: pl.BlockSpec((SPAN, size), lambda turn: (spans - 1 - turn, at))
    edge = lambda size, at: pl.BlockSpec(
        (EDGE, size), lambda turn: (jnp.maximum((spans - 1 - turn) * edges - 1, 0), at)
    )
    keep = lambda shape: pl.BlockSpec(shape, lambda turn: (0, 0))
    shapes = tuple(jax.ShapeDtypeStruct(shape, F32) for shape in shapes)
    return pl.pallas_call(
        functools.partial(
            scan_backward, devices, spans, windows, pieces, len(shapes), len(sent)
        ),
        grid=(spans,),
        out_shape=(
            jax.ShapeDtypeStruct((tokens, width), BF16),
            jax.ShapeDtypeStruct((EDGE, channels), F32),
            jax.ShapeDtypeStruct((EDGE, 2 * NS), F32),
            jax.ShapeDtypeStruct((EDGE, LANES), F32),
        )
        + shapes,
        in_specs=[
            rows(channels, 0),
            rows(channels, 1),
            edge(channels, 1),
            rows(2 * NS, bc_at),
            edge(2 * NS, bc_at),
            rows(LANES, step_at),
            rows(channels, 0),
            pl.BlockSpec((1, NS, channels), lambda turn: (spans - 1 - turn, 0, 0)),
            rows(channels, 0),
            pl.BlockSpec((EDGE, SPAN), lambda turn: (0, spans - 1 - turn)),
            pl.BlockSpec((EDGE, SPAN), lambda turn: (0, spans - 1 - turn)),
            rows(qkv_width, 0),
        ]
        + [whole_spec(item) for item in params]
        + [whole_spec(gain)]
        + [pl.BlockSpec(memory_space=pl.ANY)] * len(sent),
        out_specs=(
            rows(width, 0),
            keep((EDGE, channels)),
            keep((EDGE, 2 * NS)),
            keep((EDGE, LANES)),
        )
        + tuple(keep(item.shape) for item in shapes),
        scratch_shapes=[
            pltpu.VMEM((NS, channels), F32),
            pltpu.VMEM((SPAN + EDGE, channels), F32),
            pltpu.VMEM((SPAN + EDGE, 2 * NS), F32),
            pltpu.VMEM((SPAN + EDGE, channels), F32),
            pltpu.VMEM((SPAN + EDGE, 2 * NS), F32),
            pltpu.VMEM((SPAN, channels), F32),
            pltpu.VMEM((LANES, SPAN), F32),
        ]
        + scatter_scratch(windows, sent[0].shape[0] // devices, devices),
        compiler_params=pltpu.CompilerParams(collective_id=6, has_side_effects=True),
        cost_estimate=cost(47),
        name="scan_backward",
    )(
        proj, proj, proj, proj, proj, proj, y, entering, dyg, scale, inner, dqkv, *params, gain,
        *sent,
    )


def rotary_tables(tokens):
    half = HEAD_SIZE // 2
    exponent = np.arange(half, dtype=np.float64) * (-2.0 * LOG_BASE / HEAD_SIZE)
    rates = np.tile(np.exp(exponent.astype(np.float32)).astype(np.float64), LANES // half)
    tables = []
    for places in (np.arange(FINE), np.arange(0, tokens, FINE)):
        angles = places[:, None] * rates[None, :]
        tables += [np.cos(angles).astype(np.float32), np.sin(angles).astype(np.float32)]
    return tables


def fill_rotary(fine_cos, fine_sin, coarse_cos, coarse_sin, cosine, sine):
    small_cos, small_sin = fine_cos[...], fine_sin[...]
    for turn in range(coarse_cos.shape[0]):
        big_cos, big_sin = coarse_cos[turn : turn + 1, :], coarse_sin[turn : turn + 1, :]
        rows = slice(turn * FINE, (turn + 1) * FINE)
        cosine[rows, :] = small_cos * big_cos - small_sin * big_sin
        sine[rows, :] = small_sin * big_cos + small_cos * big_sin


def head_masks():
    half = HEAD_SIZE // 2
    row, col = iota((LANES, LANES), 0), iota((LANES, LANES), 1)
    place = col % HEAD_SIZE
    ahead = jnp.where(place < half, -1.0, 0.0)
    behind = jnp.where(place < half, 0.0, 1.0)

    def turn(start):
        return jnp.where(row == start + half, ahead, jnp.where(row == start - half, behind, 0.0))

    first = row < HEAD_SIZE
    left = col < HEAD_SIZE
    low = lambda mask: mask.astype(BF16)
    within = low(turn(col))
    copy = low(jnp.where(row == place, 1.0, 0.0))
    copy_turn = low(jnp.where(first, turn(place), 0.0))
    value = low(jnp.where(row == place + HEAD_SIZE, 1.0, 0.0))
    fold = low(jnp.where(left & (row % HEAD_SIZE == place), 1.0, 0.0))
    other = row % HEAD_SIZE
    fold_turn = low(
        jnp.where(
            left,
            jnp.where(other == place + half, ahead, jnp.where(other == place - half, behind, 0.0)),
            0.0,
        )
    )
    fold_value = low(jnp.where(left, 0.0, jnp.where(other == place, 1.0, 0.0)))
    return within, copy, copy_turn, value, fold, fold_turn, fold_value


def attend_forward(
    q_ref, kv_ref, fine_cos, fine_sin, coarse_cos, coarse_sin,
    qkv_ref, lse_ref, o_ref, vt, cos_ref, sin_ref,
):
    fill_rotary(fine_cos, fine_sin, coarse_cos, coarse_sin, cos_ref, sin_ref)
    tokens, query_width = q_ref.shape
    pairs = query_width // LANES
    within, copy, copy_turn, value = head_masks()[:4]

    def turn_rows(i, carry):
        rows = pl.ds(pl.multiple_of(i * QBLK, QBLK), QBLK)
        cosine, sine = cos_ref[rows, :], sin_ref[rows, :]
        for pair in range(pairs):
            lanes = slice(pair * LANES, (pair + 1) * LANES)
            query = q_ref[rows, lanes]
            turned = query * cosine + pick(query, within) * sine
            qkv_ref[rows, lanes] = (turned * HEAD_SIZE**-0.5).astype(BF16)
        kv = kv_ref[rows, :]
        keys = pick(kv, copy) * cosine + pick(kv, copy_turn) * sine
        qkv_ref[rows, query_width : query_width + LANES] = keys.astype(BF16)
        qkv_ref[rows, query_width + LANES :] = dot(kv.astype(BF16), value).astype(BF16)
        vt[:, rows] = kv.T[HEAD_SIZE:, :].astype(BF16)
        return carry

    lax.fori_loop(0, tokens // QBLK, turn_rows, 0)
    low_lanes = iota((QBLK, LANES), 1) < HEAD_SIZE
    wide = (QBLK, 2 * QBLK)
    visible = iota(wide, 0) <= iota(wide, 1) % QBLK

    def block(i, carry):
        here = pl.ds(pl.multiple_of(i * QBLK, QBLK), QBLK)
        queries = [
            pair_split(qkv_ref[here, pair * LANES : (pair + 1) * LANES], low_lanes)
            for pair in range(pairs)
        ]

        def tile(there, state, edge):
            keys = qkv_ref[there, query_width : query_width + LANES]
            result = []
            for pair in range(pairs):
                top, total, out = state[3 * pair : 3 * pair + 3]
                scores = dot(keys, queries[pair], NT)
                if edge:
                    scores = jnp.where(visible, scores, MASKED)
                higher = jnp.maximum(top, jnp.max(scores, axis=0, keepdims=True))
                probs = jnp.exp(scores - higher)
                fade = jnp.exp(top - higher)
                total = total * fade + jnp.sum(probs, axis=0, keepdims=True)
                out = out * fade + dot(vt[:, there], probs.astype(BF16))
                result += [higher, total, out]
            return tuple(result)

        state = (
            jnp.full((1, 2 * QBLK), MASKED, F32),
            jnp.zeros((1, 2 * QBLK), F32),
            jnp.zeros((HEAD_SIZE, 2 * QBLK), F32),
        ) * pairs
        state = lax.fori_loop(
            0,
            i,
            lambda j, state: tile(pl.ds(pl.multiple_of(j * QBLK, QBLK), QBLK), state, False),
            state,
        )
        state = tile(here, state, True)
        for pair in range(pairs):
            top, total, out = state[3 * pair : 3 * pair + 3]
            out = out / total
            lse = top + jnp.log(total)
            lse_ref[2 * pair : 2 * pair + 1, here] = lse[:, :QBLK]
            lse_ref[2 * pair + 1 : 2 * pair + 2, here] = lse[:, QBLK:]
            both = jnp.concatenate([out[:, :QBLK], out[:, QBLK:]], axis=0)
            o_ref[here, pair * LANES : (pair + 1) * LANES] = both.T.astype(BF16)
        return carry

    lax.fori_loop(0, tokens // QBLK, block, 0)


def attend_backward(
    qkv_ref, lse_ref, o_ref, do_ref, fine_cos, fine_sin, coarse_cos, coarse_sin,
    dqkv_ref,
    dq, kt, dk, dv, cos_ref, sin_ref,
):
    fill_rotary(fine_cos, fine_sin, coarse_cos, coarse_sin, cos_ref, sin_ref)
    tokens, query_width = o_ref.shape
    pairs = query_width // LANES
    key_lanes = slice(query_width, query_width + LANES)
    value_lanes = slice(query_width + LANES, query_width + 2 * LANES)

    def turn_keys(i, carry):
        rows = pl.ds(pl.multiple_of(i * QBLK, QBLK), QBLK)
        kt[:, rows] = qkv_ref[rows, key_lanes].astype(F32).T[:HEAD_SIZE, :].astype(BF16)
        return carry

    lax.fori_loop(0, tokens // QBLK, turn_keys, 0)
    dk[...] = jnp.zeros_like(dk)
    dv[...] = jnp.zeros_like(dv)
    low_lanes = iota((QBLK, LANES), 1) < HEAD_SIZE
    wide = (QBLK, 2 * QBLK)
    visible = iota(wide, 0) <= iota(wide, 1) % QBLK
    ones = jnp.ones((EDGE, LANES), BF16)

    def block(i, carry):
        here = pl.ds(pl.multiple_of(i * QBLK, QBLK), QBLK)
        queries, grads, inners, lses = [], [], [], []
        for pair in range(pairs):
            lanes = slice(pair * LANES, (pair + 1) * LANES)
            queries.append(pair_split(qkv_ref[here, lanes], low_lanes))
            grad = do_ref[here, lanes]
            grads.append(pair_split(grad, low_lanes))
            both = pair_split(grad.astype(F32) * o_ref[here, lanes].astype(F32), low_lanes)
            high, low = parts(both, 2)
            inners.append((dot(ones, high, NT) + dot(ones, low, NT))[:1])
            lses.append(
                jnp.concatenate(
                    [
                        lse_ref[2 * pair : 2 * pair + 1, here],
                        lse_ref[2 * pair + 1 : 2 * pair + 2, here],
                    ],
                    axis=1,
                )
            )
        query_all = jnp.concatenate(queries, axis=0)
        grad_all = jnp.concatenate(grads, axis=0)

        def tile(there, state, edge):
            keys = qkv_ref[there, key_lanes]
            values = qkv_ref[there, value_lanes]
            all_probs, all_dscores, result = [], [], []
            for pair in range(pairs):
                probs = dot(keys, queries[pair], NT) - lses[pair]
                if edge:
                    probs = jnp.where(visible, probs, MASKED)
                probs = jnp.exp(probs)
                dprobs = dot(values, grads[pair], NT)
                dscores = (probs * (dprobs - inners[pair])).astype(BF16)
                all_probs.append(probs.astype(BF16))
                all_dscores.append(dscores)
                result.append(state[pair] + dot(kt[:, there], dscores))
            dv[there, :] += dot(jnp.concatenate(all_probs, axis=1), grad_all)
            dk[there, :] += dot(jnp.concatenate(all_dscores, axis=1), query_all)
            return tuple(result)

        state = (jnp.zeros((HEAD_SIZE, 2 * QBLK), F32),) * pairs
        state = lax.fori_loop(
            0,
            i,
            lambda j, state: tile(pl.ds(pl.multiple_of(j * QBLK, QBLK), QBLK), state, False),
            state,
        )
        state = tile(here, state, True)
        for pair in range(pairs):
            both = jnp.concatenate([state[pair][:, :QBLK], state[pair][:, QBLK:]], axis=0)
            dq[here, pair * LANES : (pair + 1) * LANES] = both.T
        return carry

    lax.fori_loop(0, tokens // QBLK, block, 0)
    masks = head_masks()
    within, (fold, fold_turn, fold_value) = masks[0], masks[4:]

    def turn_back(i, carry):
        rows = pl.ds(pl.multiple_of(i * QBLK, QBLK), QBLK)
        cosine, sine = cos_ref[rows, :], sin_ref[rows, :]
        for pair in range(pairs):
            lanes = slice(pair * LANES, (pair + 1) * LANES)
            grad = dq[rows, lanes]
            grad = grad * cosine - pick(grad, within) * sine
            dqkv_ref[rows, lanes] = (grad * HEAD_SIZE**-0.5).astype(BF16)
        grad = dk[rows, :]
        grad = pick(grad, fold) * cosine - pick(grad, fold_turn) * sine
        grad = grad + pick(dv[rows, :], fold_value)
        dqkv_ref[rows, query_width:] = grad.astype(BF16)
        return carry

    lax.fori_loop(0, tokens // QBLK, turn_back, 0)


def run_attend_forward(proj, query_at, query_width, tables):
    tokens = proj.shape[0]
    cols = lambda size, at: pl.BlockSpec((tokens, size), lambda turn: (0, at // size))
    return pl.pallas_call(
        attend_forward,
        grid=(1,),
        out_shape=(
            jax.ShapeDtypeStruct((tokens, query_width + 2 * LANES), BF16),
            jax.ShapeDtypeStruct((EDGE, tokens), F32),
            jax.ShapeDtypeStruct((tokens, query_width), BF16),
        ),
        in_specs=[
            cols(query_width, query_at),
            cols(2 * HEAD_SIZE, query_at + query_width),
        ]
        + [whole_spec(table) for table in tables],
        out_specs=(
            cols(query_width + 2 * LANES, 0),
            pl.BlockSpec((EDGE, tokens), lambda turn: (0, 0)),
            cols(query_width, 0),
        ),
        scratch_shapes=[
            pltpu.VMEM((HEAD_SIZE, tokens), BF16),
            pltpu.VMEM((tokens, LANES), F32),
            pltpu.VMEM((tokens, LANES), F32),
        ],
        cost_estimate=cost(15),
        name="attend_forward",
    )(proj, proj, *tables)


def run_attend_backward(qkv, lse, attended, grads, grad_at, tables):
    tokens, query_width = attended.shape
    vmem = pl.BlockSpec(memory_space=pltpu.VMEM)
    cols = lambda size, at: pl.BlockSpec((tokens, size), lambda turn: (0, at // size))
    return pl.pallas_call(
        attend_backward,
        grid=(1,),
        out_shape=jax.ShapeDtypeStruct((tokens, query_width + 2 * HEAD_SIZE), BF16),
        in_specs=[
            whole_spec(qkv),
            whole_spec(lse),
            whole_spec(attended),
            cols(query_width, grad_at),
        ]
        + [whole_spec(table) for table in tables],
        out_specs=cols(query_width + 2 * HEAD_SIZE, 0),
        scratch_shapes=[
            pltpu.VMEM((tokens, query_width), F32),
            pltpu.VMEM((HEAD_SIZE, tokens), BF16),
            pltpu.VMEM((tokens, LANES), F32),
            pltpu.VMEM((tokens, LANES), F32),
            pltpu.VMEM((tokens, LANES), F32),
            pltpu.VMEM((tokens, LANES), F32),
        ],
        cost_estimate=cost(16),
        name="attend_backward",
    )(qkv, lse, attended, grads, *tables)


def feed_forward(
    x_ref, mixed_ref, other_ref, top_ref, gain_ref, gu_ref, down_ref,
    after_ref, scale_ref, hidden_ref, act_ref, dgu_ref, part_ref, back_ref,
):
    units = down_ref.shape[1]
    after = x_ref[...].astype(F32) + (mixed_ref[...].astype(F32) + other_ref[...].astype(F32))
    after_ref[...] = after
    scale = lax.rsqrt(jnp.mean(after * after, axis=-1, keepdims=True) + EPSILON)
    scale_ref[...] = scale
    hidden = (after * scale * gain_ref[...]).astype(BF16)
    hidden_ref[...] = hidden
    top = top_ref[...]
    for start in range(0, units, UBLK):
        cols = slice(start, start + UBLK)
        up_cols = slice(units + start, units + start + UBLK)
        gate = dot(hidden, gu_ref[:, cols])
        upward = dot(hidden, gu_ref[:, up_cols])
        grad = dot(top, down_ref[:, cols])
        sigma = jax.nn.sigmoid(gate)
        swish = gate * sigma
        act_ref[:, cols] = (swish * upward).astype(BF16)
        slope = sigma * (1.0 + gate * (1.0 - sigma))
        dgu_ref[:, cols] = (grad * upward * slope).astype(BF16)
        dgu_ref[:, up_cols] = (grad * swish).astype(BF16)
    back_ref[...] = dot(dgu_ref[...], gu_ref[...], NT).astype(BF16)
    part_ref[...] = dot(act_ref[...], down_ref[...], NT).astype(BF16)


def once(item):
    return pl.BlockSpec(item.shape, lambda turn: (0,) * item.ndim, pipeline_mode=pl.Buffered(1))


def run_feed_forward(x, mixed, other, top, gain, w_gate_up, w_down_t):
    tokens, width = x.shape
    units = w_down_t.shape[1]
    rows = lambda size: pl.BlockSpec((TBLK, size), lambda turn: (turn, 0))
    shape = jax.ShapeDtypeStruct
    return pl.pallas_call(
        feed_forward,
        grid=(tokens // TBLK,),
        out_shape=(
            shape((tokens, width), F32),
            shape((tokens, 1), F32),
            shape((tokens, width), BF16),
            shape((tokens, units), BF16),
            shape((tokens, 2 * units), BF16),
            shape((tokens, width), BF16),
            shape((tokens, width), BF16),
        ),
        in_specs=[rows(width)] * 4 + [once(gain), once(w_gate_up), once(w_down_t)],
        out_specs=(
            rows(width), rows(1), rows(width), rows(units), rows(2 * units), rows(width),
            rows(width),
        ),
        cost_estimate=cost(20),
        name="feed_forward",
    )(x, mixed, other, top, gain, w_gate_up, w_down_t)


def mixer_forward(gated_ref, scale_ref, gain_ref, attended_ref, w_ref, low_ref, mixed_ref):
    channels = gated_ref.shape[1]
    scale = scale_ref[...].T[:, :1]
    low_ref[:, :channels] = (gated_ref[...] * scale * gain_ref[...]).astype(BF16)
    low_ref[:, channels:] = attended_ref[...]
    mixed_ref[...] = dot(low_ref[...], w_ref[...], NT).astype(BF16)


def run_mixer_forward(gated, scale, gain, attended, w_out):
    tokens, channels = gated.shape
    width, inner = w_out.shape
    rows = lambda size: pl.BlockSpec((TBLK, size), lambda turn: (turn, 0))
    return pl.pallas_call(
        mixer_forward,
        grid=(tokens // TBLK,),
        out_shape=(
            jax.ShapeDtypeStruct((tokens, inner), BF16),
            jax.ShapeDtypeStruct((tokens, width), BF16),
        ),
        in_specs=[
            rows(channels),
            pl.BlockSpec((EDGE, TBLK), lambda turn: (0, turn)),
            once(gain),
            rows(attended.shape[1]),
            once(w_out),
        ],
        out_specs=(rows(inner), rows(width)),
        cost_estimate=cost(5),
        name="mixer_forward",
    )(gated, scale, gain, attended, w_out)


def mixer_backward(
    part_ref, other_ref, after_ref, scale_ref, top_ref, gain_ref,
    w_ref, gated_ref, scale_m_ref, gain_m_ref,
    grad_ref, low_ref, mamba_ref, attended_ref, inner_ref, gain_grad_ref,
):
    channels = gated_ref.shape[1]

    @pl.when(pl.program_id(0) == 0)
    def _():
        gain_grad_ref[...] = jnp.zeros_like(gain_grad_ref)

    grad = part_ref[...].astype(F32) + other_ref[...].astype(F32)
    scale = scale_ref[...]
    normed = after_ref[...] * scale
    gain_grad_ref[:1, :] += jnp.sum(grad * normed, axis=0, keepdims=True)
    weighted = grad * gain_ref[...]
    mean = jnp.mean(weighted * normed, axis=-1, keepdims=True)
    total = top_ref[...].astype(F32) + scale * (weighted - normed * mean)
    grad_ref[...] = total
    low_ref[...] = total.astype(BF16)
    back = dot(low_ref[...], w_ref[...])
    mamba = back[:, :channels]
    mamba_ref[...] = mamba
    attended_ref[...] = back[:, channels:].astype(BF16)
    inner_ref[...] = row_sums(mamba * gain_m_ref[...] * gated_ref[...]) * scale_m_ref[...]


def run_mixer_backward(part, other, after, scale, top, gain, w_out, gated, scale_m, gain_m):
    tokens, width = after.shape
    channels = gated.shape[1]
    inner = w_out.shape[1]
    shape = jax.ShapeDtypeStruct
    rows = lambda size: pl.BlockSpec((NBLK, size), lambda turn: (turn, 0))
    lanes = pl.BlockSpec((EDGE, NBLK), lambda turn: (0, turn))
    return pl.pallas_call(
        mixer_backward,
        grid=(tokens // NBLK,),
        out_shape=(
            shape((tokens, width), F32),
            shape((tokens, width), BF16),
            shape((tokens, channels), F32),
            shape((tokens, inner - channels), BF16),
            shape((EDGE, tokens), F32),
            shape((EDGE, width), F32),
        ),
        in_specs=[rows(width)] * 3
        + [rows(1), rows(width), once(gain), once(w_out), rows(channels), lanes, once(gain_m)],
        out_specs=(
            rows(width), rows(width), rows(channels), rows(inner - channels), lanes,
            pl.BlockSpec((EDGE, width), lambda turn: (0, 0)),
        ),
        cost_estimate=cost(8),
        name="mixer_backward",
    )(part, other, after, scale, top, gain, w_out, gated, scale_m, gain_m)


def weight_grad(left_ref, right_ref, out_ref):
    out_ref[...] = dot(left_ref[...], right_ref[...], TN).astype(BF16)


def run_weight_grad(left, right):
    tokens, rows = left.shape
    cols = right.shape[1]
    return pl.pallas_call(
        weight_grad,
        grid=(rows // LANES,),
        out_shape=jax.ShapeDtypeStruct((rows, cols), BF16),
        in_specs=[pl.BlockSpec((tokens, LANES), lambda turn: (0, turn)), once(right)],
        out_specs=pl.BlockSpec((LANES, cols), lambda turn: (turn, 0)),
        cost_estimate=cost(5),
        name="weight_grad",
    )(left, right)


def finish_layer(
    x_ref, gain_ref, part_ref, other_ref, grad_ref, after_ref, ffn_ref, ffn_other_ref,
    out_ref, result_ref,
):
    x = x_ref[...].astype(F32)
    scale = lax.rsqrt(jnp.mean(x * x, axis=-1, keepdims=True) + EPSILON)
    normed = x * scale
    weighted = (part_ref[...].astype(F32) + other_ref[...].astype(F32)) * gain_ref[...]
    mean = jnp.mean(weighted * normed, axis=-1, keepdims=True)
    out_ref[...] = grad_ref[...] + scale * (weighted - normed * mean)
    ffn = ffn_ref[...].astype(F32) + ffn_other_ref[...].astype(F32)
    result_ref[...] = (after_ref[...] + ffn).astype(BF16)


def run_finish(x, gain, part, other, grad, after, ffn, ffn_other):
    tokens, width = x.shape
    rows = pl.BlockSpec((NBLK, width), lambda turn: (turn, 0))
    return pl.pallas_call(
        finish_layer,
        grid=(tokens // NBLK,),
        out_shape=(
            jax.ShapeDtypeStruct((tokens, width), F32),
            jax.ShapeDtypeStruct((tokens, width), BF16),
        ),
        in_specs=[rows, once(gain)] + [rows] * 6,
        out_specs=(rows, rows),
        cost_estimate=cost(8),
        name="finish_layer",
    )(x, gain, part, other, grad, after, ffn, ffn_other)


def swap(partial):
    return lax.ppermute(partial, "tensor", [(0, 1), (1, 0)])


def join(mine, other):
    return mine.astype(F32) + other.astype(F32)


def tensor_sum(partial):
    return join(partial, swap(partial))


def local(
    layer_input, w_norm1, w_zx, w_bc, w_dt, conv_x, conv_xb, conv_bc, conv_bcb, dt_bias, a_log,
    d_skip, w_mnorm, w_mout, query_key_value_weight, output_weight, w_norm2, w_gu, w_down,
    grad_output,
):
    devices = lax.axis_size("dp")
    tokens, width = layer_input.shape
    shard = w_zx.shape[0]
    channels = conv_xb.shape[0]
    heads = dt_bias.shape[0]
    qkv_width = query_key_value_weight.shape[2]
    units = w_down.shape[0]
    attn_width = output_weight.shape[1]
    tail = jnp.concatenate(
        [w_dt, w_norm1[:, None], w_norm2[:, None], jnp.zeros((shard, LANES - heads - 2), BF16)],
        axis=1,
    )
    mixer_in = jnp.concatenate(
        [w_zx.reshape(shard, -1), w_bc, query_key_value_weight.reshape(shard, -1), tail], axis=1
    )
    in_width = mixer_in.shape[1]
    (w_in,) = gather_rows([mixer_in], devices, 0)
    norm1 = w_in[:, in_width - LANES + heads].astype(F32)
    norm2 = w_in[:, in_width - LANES + heads + 1].astype(F32)

    source = layer_input.astype(F32)
    scale_one = lax.rsqrt(jnp.mean(source * source, axis=-1, keepdims=True) + EPSILON)
    normed_one = source * scale_one
    hidden_one = lax.optimization_barrier((normed_one * norm1).astype(BF16))
    proj = dot(hidden_one, w_in)
    params = scan_params(conv_x, conv_xb, conv_bc, conv_bcb, dt_bias, a_log, d_skip)
    out_shard = jnp.concatenate([w_mout.T, output_weight.reshape(attn_width, -1).T], axis=1)
    y, gated, square_sum, entering, w_out = run_scan_forward(
        proj, qkv_width, params, out_shard, devices
    )
    channels_all = channels * lax.axis_size("tensor")
    scale_m = lax.rsqrt(tensor_sum(square_sum) / channels_all + EPSILON)
    tables = rotary_tables(tokens)
    qkv_at = 2 * channels + 2 * NS
    qkv, lse, attended = run_attend_forward(proj, qkv_at, attn_width, tables)
    gain_m = w_mnorm.astype(F32)[None, :]
    mixer_out, mixed = run_mixer_forward(gated, scale_m, gain_m, attended, w_out)
    mixed, gate_up_shard, down_shard = lax.optimization_barrier(
        (mixed, w_gu.reshape(shard, -1), w_down.T)
    )
    other = swap(mixed)
    w_gate_up, w_down_t = gather_rows([gate_up_shard, down_shard], devices, 3)
    other, w_gate_up, w_down_t = lax.optimization_barrier((other, w_gate_up, w_down_t))
    after, scale_two, hidden_two, activated, grad_gu_low, ffn_part, partial_two = run_feed_forward(
        layer_input, mixed, other, grad_output, norm2[None, :], w_gate_up, w_down_t
    )
    other = swap(partial_two)
    grad_down = run_weight_grad(grad_output, activated)
    (mine_gu,) = scatter_product(
        hidden_two,
        grad_gu_low,
        [(0, 1, 0, 2 * units)],
        [(0, 0, units, 0, 0), (0, units, 2 * units, 0, 1)],
        [(shard, 2, units)],
        devices,
        1,
    )
    other, mine_gu, grad_down, ffn_part = lax.optimization_barrier(
        (other, mine_gu, grad_down, ffn_part)
    )
    ffn_other = swap(ffn_part)
    grad_after, grad_mix_low, grad_mamba, grad_attended, inner_m, grad_norm2 = run_mixer_backward(
        partial_two, other, after, scale_two, grad_output, norm2[None, :], w_out, gated, scale_m,
        gain_m,
    )
    inner_m = tensor_sum(inner_m) / channels_all
    dqkv = run_attend_backward(qkv, lse, attended, grad_attended, 0, tables)
    grad_out = run_weight_grad(grad_mix_low, mixer_out)
    windows = [(0, None, 0, channels + attn_width), (1, None, 0, units)]
    pieces = [
        (0, 0, channels, 0, None),
        (0, channels, channels + attn_width, 1, None),
        (1, 0, units, 2, None),
    ]
    shapes = [(shard, channels), (shard, attn_width), (shard, units)]
    grad_proj, small_x, small_b, small_h, mine_mout, mine_o, mine_down = run_scan_backward(
        proj, y, entering, grad_mamba, scale_m, inner_m, dqkv, params, gain_m,
        [grad_out, grad_down], windows, pieces, shapes, devices,
    )
    ffn_other, grad_proj = lax.optimization_barrier((ffn_other, grad_proj))
    partial_one, grad_proj = lax.optimization_barrier(
        (dot(grad_proj, w_in, NT).astype(BF16), grad_proj)
    )
    crossing = jnp.concatenate(
        [
            small_b[: KCONV + 1].reshape(-1, LANES),
            jnp.sum(partial_one.astype(F32) * normed_one, axis=0).reshape(-1, LANES),
        ],
        axis=0,
    )
    crossing = tensor_sum(crossing)
    partial_one, crossing = lax.optimization_barrier((partial_one, crossing))
    other = swap(partial_one)
    small = jnp.concatenate(
        [
            small_x[: KCONV + 2].reshape(-1, LANES),
            small_h[:3],
            crossing,
            grad_norm2[0].reshape(-1, LANES),
        ],
        axis=0,
    )
    small_rows = small.shape[0]
    small = jnp.pad(small, ((0, -small_rows % EDGE), (0, 0)))
    shared_at = 2 * channels
    step_at = qkv_at + qkv_width
    mine_zx, mine_bc, mine_qkv, mine_step, small = scatter_product(
        hidden_one,
        grad_proj,
        [(0, 1, 0, in_width)],
        [
            (0, 0, channels, 0, 0),
            (0, channels, shared_at, 0, 1),
            (0, shared_at, qkv_at, 1, None),
            (0, qkv_at, step_at, 2, 0),
            (0, step_at, in_width, 3, "turned"),
        ],
        [
            (shard, 2, channels),
            (shard, 2 * NS),
            (shard, 1, qkv_width),
            (heads, shard),
        ],
        devices,
        5,
        (small,),
    )
    other, mine_bc = lax.optimization_barrier((other, mine_bc))
    grad_source, result = run_finish(
        layer_input, norm1[None, :], partial_one, other, grad_after, after, ffn_part, ffn_other
    )

    half = NS * 2 // lax.axis_size("tensor")
    shared_cols = tensor_sum(mine_bc)
    begin = lax.axis_index("tensor") * half
    grad_bc = lax.dynamic_slice_in_dim(shared_cols, begin, half, 1)
    small = small[:small_rows].reshape(-1)
    x_size = (KCONV + 2) * channels
    h_size = 3 * LANES
    b_size = (KCONV + 1) * 2 * NS
    total_x = small[:x_size].reshape(KCONV + 2, channels)
    total_h = small[x_size : x_size + h_size].reshape(3, LANES)
    total_b = small[x_size + h_size : x_size + h_size + b_size].reshape(KCONV + 1, 2 * NS)
    total_b = lax.dynamic_slice_in_dim(total_b, begin, half, 1)
    norms = small[x_size + h_size + b_size :].reshape(2, width)
    norms = lax.dynamic_slice_in_dim(norms, lax.axis_index("dp") * shard, shard, 1)
    return (
        result,
        grad_source,
        norms[0],
        mine_zx,
        grad_bc,
        mine_step.T,
        total_x[:KCONV],
        total_x[KCONV],
        total_b[:KCONV],
        total_b[KCONV],
        total_h[0, :heads],
        total_h[1, :heads],
        total_h[2, :heads],
        total_x[KCONV + 1],
        mine_mout.T,
        mine_qkv,
        mine_o.T.reshape(output_weight.shape),
        norms[1],
        mine_gu,
        mine_down.T,
    )


def solution(mesh):
    return jax.shard_map(
        local,
        mesh=mesh,
        in_specs=(
            P("dp", None),
            P("dp"),
            P("dp", None, "tensor"),
            P("dp", None),
            P("dp", "tensor"),
            P(None, "tensor"),
            P("tensor"),
            P(),
            P(),
            P("tensor"),
            P("tensor"),
            P("tensor"),
            P("tensor"),
            P("tensor", "dp"),
            P("dp", "tensor", None),
            P("tensor", None, "dp"),
            P("dp"),
            P("dp", None, "tensor"),
            P("tensor", "dp"),
            P("dp", None),
        ),
        out_specs=(
            P("dp", None),
            P("dp", None),
            P("dp"),
            P("dp", None, "tensor"),
            P("dp", "tensor"),
            P("dp", "tensor"),
            P(None, "tensor"),
            P("tensor"),
            P(None, "tensor"),
            P("tensor"),
            P("tensor"),
            P("tensor"),
            P("tensor"),
            P("tensor"),
            P("tensor", "dp"),
            P("dp", "tensor", None),
            P("tensor", None, "dp"),
            P("dp"),
            P("dp", None, "tensor"),
            P("tensor", "dp"),
        ),
        check_vma=False,
    )
```

```python
import functools
import math

import jax
import jax.numpy as jnp
import numpy as np
from jax import lax
from jax.experimental import pallas as pl
from jax.experimental.pallas import tpu as pltpu
from jax.sharding import PartitionSpec as P

HEAD_SIZE = 64
MP = 64
NS = 128
KCONV = 4
SPAN = 128
QBLK = 256
FINE = 32
TBLK = 256
NBLK = 128
UBLK = 256
LANES = 128
EDGE = 8

EPSILON = 1e-05
HIGHEST = lax.Precision.HIGHEST
LOG_BASE = math.log(100000000000.0)
MASKED = -1e30
MESH = pl.DeviceIdType.MESH
F32 = jnp.float32
BF16 = jnp.bfloat16

NN = ((1,), (0,))
NT = ((1,), (1,))
TN = ((0,), (0,))


def dot(left, right, dims=NN, precision=None):
    return lax.dot_general(
        left, right, (dims, ((), ())), preferred_element_type=F32, precision=precision
    )


def iota(shape, dim):
    return lax.broadcasted_iota(jnp.int32, shape, dim)


def ring_place(chip, chips):
    odd = lax.rem(chip, 2)
    half = lax.div(chip, 2)
    return (1 - odd) * half + odd * (chips - 1 - half)


def ring_chip(place, chips):
    place = lax.rem(place + 4 * chips, chips)
    back = lax.div(place, chips // 2)
    return (1 - back) * (2 * place) + back * (2 * (chips - 1 - place) + 1)


def ring_setup(chips):
    me = lax.axis_index("dp")
    group = lax.axis_index("tensor")
    chip = lax.div(me, 2)
    core = lax.rem(me, 2)
    place = ring_place(chip, chips)
    right = ring_chip(place + 1, chips) * 2 + core
    left = ring_chip(place - 1, chips) * 2 + core
    mate = chip * 2 + (1 - core)
    barrier = pltpu.get_barrier_semaphore()
    for other in (right, left, mate):
        pl.semaphore_signal(barrier, inc=1, device_id=(other, group), device_id_type=MESH)
    pl.semaphore_wait(barrier, 3)
    return me, group, core, place, right, left, mate


class RingGather:
    def __init__(self, devices, x_ref, o_ref, sems):
        self.chips = devices // 2
        self.ahead = self.chips // 2
        self.behind = self.chips - 1 - self.ahead
        self.x_ref, self.o_ref, self.rows = x_ref, o_ref, x_ref.shape[0]
        self.fs, self.fr, self.bs, self.br, self.cs, self.cr, self.own_sem = sems

    def locate(self):
        me = lax.axis_index("dp")
        self.group = lax.axis_index("tensor")
        self.core = lax.rem(me, 2)
        chip = lax.div(me, 2)
        self.place = ring_place(chip, self.chips)
        self.right = ring_chip(self.place + 1, self.chips) * 2 + self.core
        self.left = ring_chip(self.place - 1, self.chips) * 2 + self.core
        self.mate = chip * 2 + (1 - self.core)
        self.me = me

    def slot(self, index):
        return self.o_ref.at[pl.ds(pl.multiple_of(index * self.rows, self.rows), self.rows), :]

    def copy(self, shift, ssem, rsem, target):
        if shift == 0:
            index, source = self.me, self.x_ref
        else:
            index = ring_chip(self.place + shift, self.chips) * 2 + self.core
            source = self.slot(index)
        return pltpu.make_async_remote_copy(
            src_ref=source,
            dst_ref=self.slot(index),
            send_sem=ssem,
            recv_sem=rsem,
            device_id=(target, self.group),
            device_id_type=MESH,
        )

    def fore(self, step):
        return self.copy(-step, self.fs.at[step], self.fr.at[step], self.right)

    def back(self, step):
        return self.copy(step, self.bs.at[step], self.br.at[step], self.left)

    def across(self, shift):
        number = 0 if shift == 0 else 2 * abs(shift) - (1 if shift < 0 else 0)
        return self.copy(shift, self.cs.at[number], self.cr.at[number], self.mate)

    def own(self):
        return pltpu.make_async_copy(self.x_ref, self.slot(self.me), self.own_sem)

    def greet(self):
        self.locate()
        barrier = pltpu.get_barrier_semaphore()
        for other in (self.right, self.left, self.mate):
            pl.semaphore_signal(
                barrier, inc=1, device_id=(other, self.group), device_id_type=MESH
            )
        pl.semaphore_wait(barrier, 3)

    def begin(self):
        self.locate()
        self.fore(0).start()
        self.back(0).start()
        self.across(0).start()
        self.own().start()

    def hop(self, step):
        self.locate()
        self.fore(step - 1).wait_recv()
        if step < self.ahead:
            self.fore(step).start()
        self.across(-step).start()
        if step <= self.behind:
            self.back(step - 1).wait_recv()
            if step < self.behind:
                self.back(step).start()
            self.across(step).start()

    def finish(self):
        self.locate()
        self.own().wait()
        for step in range(self.ahead):
            self.fore(step).wait_send()
        for step in range(self.behind):
            self.back(step).wait_send()
        for shift in range(-self.ahead, self.behind + 1):
            self.across(shift).wait()


def gather_sems(devices):
    dma = pltpu.SemaphoreType.DMA
    return [dma((devices // 2,))] * 6 + [dma(())]


def gather_shape(shard, devices):
    return jax.ShapeDtypeStruct((shard.shape[0] * devices, shard.shape[1]), shard.dtype)


def gather_kernel(devices, count, *refs):
    shards, outs, sems = refs[:count], refs[count : 2 * count], refs[2 * count :]
    each = len(sems) // count
    rings = [
        RingGather(devices, shards[i], outs[i], sems[i * each : (i + 1) * each])
        for i in range(count)
    ]
    rings[0].greet()
    for ring in rings:
        ring.begin()
    for step in range(1, rings[0].ahead + 1):
        for ring in rings:
            ring.hop(step)
    for ring in rings:
        ring.finish()


def cost(micros):
    return pl.CostEstimate(flops=int(micros * 1e9), bytes_accessed=0, transcendentals=0)


def gather_rows(shards, devices, collective):
    count = len(shards)
    anywhere = pl.BlockSpec(memory_space=pl.ANY)
    return pl.pallas_call(
        functools.partial(gather_kernel, devices, count),
        out_shape=tuple(gather_shape(shard, devices) for shard in shards),
        in_specs=[anywhere] * count,
        out_specs=(anywhere,) * count,
        scratch_shapes=gather_sems(devices) * count,
        compiler_params=pltpu.CompilerParams(collective_id=collective, has_side_effects=True),
        cost_estimate=cost(3),
        name="gather_rows",
    )(*shards)


def scatter_order(chips):
    ahead = chips // 2
    behind = chips - 1 - ahead
    order = []
    for step in range(ahead):
        order.append(-(ahead - step))
        if step < behind:
            order.append(behind - step)
    order.append(0)
    return order


class RingScatter:
    def __init__(self, devices, windows, pieces, operands, outs, scratch):
        self.chips = devices // 2
        self.ahead = self.chips // 2
        self.behind = self.chips - 1 - self.ahead
        self.windows, self.pieces, self.operands, self.outs = windows, pieces, operands, outs
        count = len(windows)
        self.mine, self.boxes, rest = scratch[:count], scratch[count : 2 * count], scratch[2 * count :]
        self.fbox, self.bbox, self.fout, self.bout = rest[:4]
        self.os, self.ms, self.mr, self.fs, self.fr, self.bs, self.br = rest[4:]
        self.rows = self.fbox.shape[1]
        widths = [item.shape[2] for item in self.mine]
        self.cols = [slice(sum(widths[:i]), sum(widths[: i + 1])) for i in range(count)]

    def locate(self):
        me = lax.axis_index("dp")
        self.group = lax.axis_index("tensor")
        self.core = lax.rem(me, 2)
        chip = lax.div(me, 2)
        self.place = ring_place(chip, self.chips)
        self.right = ring_chip(self.place + 1, self.chips) * 2 + self.core
        self.left = ring_chip(self.place - 1, self.chips) * 2 + self.core
        self.mate = chip * 2 + (1 - self.core)

    def greet(self):
        self.locate()
        barrier = pltpu.get_barrier_semaphore()
        for other in (self.right, self.left, self.mate):
            pl.semaphore_signal(
                barrier, inc=1, device_id=(other, self.group), device_id_type=MESH
            )
        pl.semaphore_wait(barrier, 3)

    def product(self, i):
        return self.windows[i][1] is not None

    def shift_of(self, slot):
        step = slot // 2
        odd = slot % 2
        return (1 - odd) * (step - self.ahead) + odd * (self.behind - step)

    def half(self, which):
        return pl.ds(pl.multiple_of(which * self.rows, self.rows), self.rows)

    def block(self, i, slot, which):
        index = ring_chip(self.place + self.shift_of(slot), self.chips) * 2 + which
        left, right, first, last = self.windows[i]
        return self.operands[left].at[self.half(index), first:last]

    def remote(self, source, target_ref, ssem, rsem, target):
        return pltpu.make_async_remote_copy(
            src_ref=source,
            dst_ref=target_ref,
            send_sem=ssem,
            recv_sem=rsem,
            device_id=(target, self.group),
            device_id_type=MESH,
        )

    def across(self, i, slot):
        if self.product(i):
            source = self.mine[i].at[slot, self.half(1 - self.core)]
        else:
            source = self.block(i, slot, 1 - self.core)
        return self.remote(
            source, self.boxes[i].at[slot], self.ms.at[i, slot], self.mr.at[i, slot], self.mate
        )

    def own(self, i, slot):
        return pltpu.make_async_copy(
            self.block(i, slot, self.core), self.mine[i].at[slot], self.os.at[i, slot]
        )

    def fore(self, step):
        return self.remote(
            self.fout.at[step], self.fbox.at[step], self.fs.at[step], self.fr.at[step], self.right
        )

    def back(self, step):
        return self.remote(
            self.bout.at[step], self.bbox.at[step], self.bs.at[step], self.br.at[step], self.left
        )

    def begin(self):
        self.locate()
        for i in range(len(self.windows)):
            if not self.product(i):
                for slot in range(self.chips):
                    self.across(i, slot).start()
                    self.own(i, slot).start()

    def produce(self, slot):
        chip = ring_chip(self.place + self.shift_of(slot), self.chips)
        size = 2 * self.rows
        for i, (left, right, first, last) in enumerate(self.windows):
            if right is None:
                continue
            at = pl.multiple_of(chip * size, size)
            terms = dot(self.operands[left][pl.ds(at, size), :], self.operands[right][:, first:last])
            self.mine[i][slot] = terms.astype(BF16)
            self.across(i, slot).start()

    def local_sum(self, i, slot, cols, others):
        rows = self.half(self.core) if self.product(i) else slice(None)
        total = self.mine[i][slot, rows, cols].astype(F32) + self.boxes[i][slot, :, cols].astype(F32)
        whole = slice(self.cols[i].start + cols.start, self.cols[i].start + cols.stop)
        for ref in others:
            total = total + ref[:, whole].astype(F32)
        return total

    def arrive(self, slot):
        for i in range(len(self.windows)):
            if not self.product(i):
                self.own(i, slot).wait()
            self.across(i, slot).wait_recv()

    def put(self, target, slot, others):
        self.arrive(slot)
        for i, cols in enumerate(self.cols):
            total = self.local_sum(i, slot, slice(0, cols.stop - cols.start), others)
            target[:, cols] = total.astype(BF16)

    def hop_back(self, step, later):
        if later:
            self.back(step - 1).wait_recv()
        self.put(self.bout.at[step], 2 * step, [self.bbox.at[step - 1]] if later else [])
        self.back(step).start()

    def hop_fore(self, step, later):
        if later:
            self.fore(step - 1).wait_recv()
        self.put(self.fout.at[step], 2 * step + 1, [self.fbox.at[step - 1]] if later else [])
        self.fore(step).start()

    def hop(self, step):
        self.locate()
        self.hop_back(step, step > 0)
        if step < self.behind:
            self.hop_fore(step, step > 0)

    def run(self, after_first=None):
        def turn(step, carry):
            lax.fori_loop(0, 2, lambda part, kept: (self.produce(2 * step + part), kept)[1], 0)

            @pl.when(step == 0)
            def _():
                self.hop_back(0, False)
                self.hop_fore(0, False)
                if after_first is not None:
                    after_first()

            pl.when(step > 0)(lambda: self.hop_back(step, True))
            pl.when((step > 0) & (step < self.behind))(lambda: self.hop_fore(step, True))
            return carry

        lax.fori_loop(0, self.ahead, turn, 0)

    def finish(self):
        self.locate()
        slot = self.chips - 1
        self.arrive(slot)
        self.fore(self.behind - 1).wait_recv()
        self.back(self.ahead - 1).wait_recv()
        others = [self.fbox.at[self.behind - 1], self.bbox.at[self.ahead - 1]]
        for i, first, last, out, form in self.pieces:
            total = self.local_sum(i, slot, slice(first, last), others)
            if form == "turned":
                self.outs[out][...] = total.T[: self.outs[out].shape[0]]
            elif form is None:
                self.outs[out][...] = total
            else:
                self.outs[out][:, form, :] = total
        for step in range(self.ahead):
            self.back(step).wait_send()
        for step in range(self.behind):
            self.fore(step).wait_send()
        for slot in range(self.chips):
            for i in range(len(self.windows)):
                self.across(i, slot).wait_send()


def scatter_scratch(windows, rows, devices):
    chips = devices // 2
    count = len(windows)
    dma = pltpu.SemaphoreType.DMA
    widths = [last - first for left, right, first, last in windows]
    mine = [
        pltpu.VMEM((chips, rows if right is None else 2 * rows, last - first), BF16)
        for left, right, first, last in windows
    ]
    boxes = [pltpu.VMEM((chips, rows, width), BF16) for width in widths]
    box = pltpu.VMEM((chips // 2, rows, sum(widths)), BF16)
    return mine + boxes + [box] * 4 + [dma((count, chips))] * 3 + [dma((chips,))] * 4


class Total:
    def __init__(self, devices, x_ref, o_ref, scratch):
        self.chips = devices // 2
        self.x_ref, self.o_ref = x_ref, o_ref
        self.mate_box, self.joined, self.boxes, self.ms, self.mr, self.ss, self.sr = scratch
        me = lax.axis_index("dp")
        self.group = lax.axis_index("tensor")
        self.chip = lax.div(me, 2)
        core = lax.rem(me, 2)
        self.mate = self.chip * 2 + (1 - core)
        self.peers = [
            lax.rem(self.chip + shift, self.chips) * 2 + core for shift in range(self.chips)
        ]

    def greet(self):
        barrier = pltpu.get_barrier_semaphore()
        for other in [self.mate] + self.peers[1:]:
            pl.semaphore_signal(
                barrier, inc=1, device_id=(other, self.group), device_id_type=MESH
            )
        pl.semaphore_wait(barrier, self.chips)

    def remote(self, source, target_ref, ssem, rsem, target):
        return pltpu.make_async_remote_copy(
            src_ref=source,
            dst_ref=target_ref,
            send_sem=ssem,
            recv_sem=rsem,
            device_id=(target, self.group),
            device_id_type=MESH,
        )

    def across(self):
        return self.remote(self.x_ref, self.mate_box, self.ms, self.mr, self.mate)

    def copies(self):
        return [
            self.remote(
                self.joined,
                self.boxes.at[self.chip],
                self.ss.at[shift],
                self.sr.at[shift],
                self.peers[shift],
            )
            for shift in range(1, self.chips)
        ]

    def begin(self):
        self.across().start()

    def spread(self):
        self.across().wait_recv()
        self.joined[...] = self.x_ref[...] + self.mate_box[...]
        for copy in self.copies():
            copy.start()
        self.boxes[self.chip] = self.joined[...]

    def finish(self):
        for copy in self.copies():
            copy.wait_recv()
        result = self.boxes[0]
        for other in range(1, self.chips):
            result = result + self.boxes[other]
        self.o_ref[...] = result
        self.across().wait_send()
        for copy in self.copies():
            copy.wait_send()


def total_scratch(values, devices):
    chips = devices // 2
    dma = pltpu.SemaphoreType.DMA
    return [
        pltpu.VMEM(values.shape, F32),
        pltpu.VMEM(values.shape, F32),
        pltpu.VMEM((chips,) + values.shape, F32),
        dma(()),
        dma(()),
        dma((chips,)),
        dma((chips,)),
    ]


def turned_copy(source, target):
    for start in range(0, source.shape[1], LANES):
        target[start : start + LANES, :] = source[:, start : start + LANES].T


def product_kernel(devices, windows, pieces, outs, summed, left_ref, right_ref, *refs):
    values = refs[:summed]
    refs = refs[summed:]
    pieces_out, refs = refs[:outs], refs[outs:]
    totals_out, refs = refs[:summed], refs[summed:]
    turned, scratch = refs[0], refs[1:]
    total = None
    if summed:
        scratch, rest = scratch[:-7], scratch[-7:]
        total = Total(devices, values[0], totals_out[0], rest)
    ring = RingScatter(devices, windows, pieces, (turned, right_ref), pieces_out, scratch)
    if total is None:
        ring.greet()
    else:
        ring.locate()
        total.greet()
        total.begin()
    turned_copy(left_ref, turned)
    ring.run(total.spread if total is not None else None)
    ring.finish()
    if total is not None:
        total.finish()


def scatter_product(left, right, windows, pieces, shapes, devices, collective, values=()):
    vmem = pl.BlockSpec(memory_space=pltpu.VMEM)
    rows = left.shape[1] // devices
    scratch = [pltpu.VMEM(left.shape[::-1], BF16)] + scatter_scratch(windows, rows, devices)
    for item in values:
        scratch += total_scratch(item, devices)
    return pl.pallas_call(
        functools.partial(
            product_kernel, devices, windows, pieces, len(shapes), len(values)
        ),
        out_shape=tuple(jax.ShapeDtypeStruct(shape, F32) for shape in shapes)
        + tuple(jax.ShapeDtypeStruct(item.shape, F32) for item in values),
        in_specs=[vmem] * (2 + len(values)),
        out_specs=(vmem,) * (len(shapes) + len(values)),
        scratch_shapes=scratch,
        compiler_params=pltpu.CompilerParams(collective_id=collective, has_side_effects=True),
        cost_estimate=cost(3),
        name="scatter_product",
    )(left, right, *values)


def head_spread(channels):
    return (iota((LANES, channels), 1) // MP == iota((LANES, channels), 0)).astype(BF16)


def parts(values, count):
    terms = []
    for _ in range(count):
        term = values.astype(BF16)
        terms.append(term)
        values = values - term.astype(F32)
    return terms


def pick(values, mask, count=2):
    return dot(jnp.concatenate(parts(values, count), axis=1), jnp.concatenate([mask] * count, axis=0))


def pick_left(mask, values, count):
    return dot(jnp.concatenate([mask] * count, axis=1), jnp.concatenate(parts(values, count), axis=0))


def gather_heads(values, spread):
    high, low = parts(values, 2)
    return dot(high, spread, NT) + dot(low, spread, NT)


def row_sums(values):
    high, low = parts(values, 2)
    ones = jnp.ones((EDGE, values.shape[1]), BF16)
    return dot(ones, high, NT) + dot(ones, low, NT)


def soft_step(raw):
    return jnp.maximum(raw, 0.0) + jnp.log1p(jnp.exp(-jnp.abs(raw)))


def conv_window(buffer, taps_ref, bias, span):
    total = bias + taps_ref[0:1, :] * buffer[EDGE - 3 : EDGE - 3 + span, :]
    for tap in range(1, KCONV):
        start = EDGE - 3 + tap
        total = total + taps_ref[tap : tap + 1, :] * buffer[start : start + span, :]
    return total


def span_rates(step_ref, bias, decay, spread, span):
    raw = step_ref[...] + bias
    step = soft_step(raw)
    lower = (iota((span, span), 1) <= iota((span, span), 0)).astype(BF16)
    cum = pick_left(lower, step * decay, 3)
    tails = jnp.exp(cum[span - 1 : span, :] - cum)
    wide = pick(jnp.concatenate([step, tails, jnp.exp(cum)], axis=0), spread)
    return raw, step, cum, wide[:span], wide[span : 2 * span], wide[2 * span :]


def pair_split(values, low_lanes):
    zero = jnp.zeros_like(values)
    return jnp.concatenate(
        [jnp.where(low_lanes, values, zero), jnp.where(low_lanes, zero, values)], axis=0
    )


def pair_decay(cum, cum_rows, pair, causal):
    parts = []
    for head in (2 * pair, 2 * pair + 1):
        differ = cum[:, head : head + 1] - cum_rows[head : head + 1, :]
        parts.append(jnp.exp(jnp.where(causal, differ, MASKED)))
    return parts


def scan_forward(
    devices, spans,
    z_ref, x_ref, bc_ref, step_ref,
    tap_ref, tapb_ref, row_ref, shard_ref,
    y_ref, gated_ref, square_ref, enter_ref, all_ref,
    state, xbuf, bbuf, *sems,
):
    span, channels = x_ref.shape
    ring = RingGather(devices, shard_ref, all_ref, sems)
    turn = pl.program_id(0)

    @pl.when(turn == 0)
    def _():
        ring.greet()
        ring.begin()


    @pl.when(pl.program_id(0) == 0)
    def _():
        state[...] = jnp.zeros_like(state)
        xbuf[span:, :] = jnp.zeros((EDGE, channels), F32)
        bbuf[span:, :] = jnp.zeros((EDGE, 2 * NS), F32)

    xbuf[:EDGE, :] = xbuf[span:, :]
    bbuf[:EDGE, :] = bbuf[span:, :]
    xbuf[EDGE:, :] = x_ref[...]
    bbuf[EDGE:, :] = bc_ref[...]
    spread = head_spread(channels)
    bias, gain, biasb, stepb, decay, skip = unpack_rows(row_ref, spread)
    inputs = jax.nn.silu(conv_window(xbuf, tap_ref, bias, span))
    shared = jax.nn.silu(conv_window(bbuf, tapb_ref, biasb, span))
    raw, step, cum, step_w, tails_w, grown_w = span_rates(step_ref, stepb, decay, spread, span)
    cum_rows = cum.T
    b_low = shared[:, :NS].astype(BF16)
    c_low = shared[:, NS:].astype(BF16)
    scaled = inputs * step_w
    scaled_low = scaled.astype(BF16)
    enter_ref[0] = state[...]
    outer = dot(c_low, state[...].astype(BF16)) * grown_w
    fresh = dot(b_low, (scaled * tails_w).astype(BF16), TN)
    state[...] = state[...] * grown_w[span - 1 : span, :] + fresh
    cross = dot(c_low, b_low, NT)
    causal = iota((span, span), 1) <= iota((span, span), 0)
    low_lanes = iota((span, LANES), 1) < MP
    for pair in range(channels // LANES):
        lanes = slice(pair * LANES, (pair + 1) * LANES)
        first, second = pair_decay(cum, cum_rows, pair, causal)
        weights = jnp.concatenate(
            [(cross * first).astype(BF16), (cross * second).astype(BF16)], axis=1
        )
        y_ref[:, lanes] = dot(weights, pair_split(scaled_low[:, lanes], low_lanes))
    y = y_ref[...] + outer + skip * inputs
    y_ref[...] = y
    gated = y * jax.nn.silu(z_ref[...])
    gated_ref[...] = gated
    square_ref[...] = row_sums(gated * gated)

    count = spans
    for step in range(1, ring.ahead + 1):
        pl.when(turn == min(count - 1, count * step // ring.ahead))(
            functools.partial(ring.hop, step)
        )
    pl.when(turn == count - 1)(ring.finish)


def scan_backward(
    devices, spans, windows, pieces, outs_count, count,
    z_ref, x_ref, xp_ref, bc_ref, bp_ref, step_ref, y_ref, enter_ref,
    dyg_ref, scale_ref, inner_ref, dqkv_ref,
    tap_ref, tapb_ref, row_ref,
    *refs,
):
    sent, refs = refs[:count], refs[count:]
    (grad_ref, gx_ref, gb_ref, gh_ref), refs = refs[:4], refs[4:]
    outs, refs = refs[:outs_count], refs[outs_count:]
    (dstate, xbuf, bbuf, dxbuf, dbbuf, du_buf, col_buf), scratch = refs[:7], refs[7:]
    ring = RingScatter(devices, windows, pieces, sent, outs, scratch)
    span, channels = x_ref.shape
    turn = pl.program_id(0)

    @pl.when(turn == 0)
    def _():
        ring.greet()
        ring.begin()
        dstate[...] = jnp.zeros_like(dstate)
        dxbuf[...] = jnp.zeros_like(dxbuf)
        dbbuf[...] = jnp.zeros_like(dbbuf)
        col_buf[...] = jnp.zeros_like(col_buf)
        gx_ref[...] = jnp.zeros_like(gx_ref)
        gb_ref[...] = jnp.zeros_like(gb_ref)
        gh_ref[...] = jnp.zeros_like(gh_ref)

    inside = (turn < spans - 1).astype(F32)
    xbuf[:EDGE, :] = xp_ref[...] * inside
    bbuf[:EDGE, :] = bp_ref[...] * inside
    xbuf[EDGE:, :] = x_ref[...]
    bbuf[EDGE:, :] = bc_ref[...]
    spread = head_spread(channels)
    bias, gain, biasb, stepb, decay, skip = unpack_rows(row_ref, spread)
    conv = conv_window(xbuf, tap_ref, bias, span)
    sig = jax.nn.sigmoid(conv)
    inputs = conv * sig
    convb = conv_window(bbuf, tapb_ref, biasb, span)
    sigb = jax.nn.sigmoid(convb)
    shared = convb * sigb
    b_low = shared[:, :NS].astype(BF16)
    c_low = shared[:, NS:].astype(BF16)
    raw, step, cum, step_w, tails_w, grown_w = span_rates(step_ref, stepb, decay, spread, span)
    cum_rows = cum.T
    scaled = inputs * step_w
    scaled_low = scaled.astype(BF16)

    z = z_ref[...]
    sig_z = jax.nn.sigmoid(z)
    swish = z * sig_z
    y = y_ref[...]
    scale = scale_ref[...].T[:, :1]
    normed = y * swish * scale
    dyg = dyg_ref[...]
    gain_grad = jnp.sum(dyg * normed, axis=0, keepdims=True)
    dgated = scale * (dyg * gain - normed * inner_ref[...].T[:, :1])
    dy = dgated * swish
    grad_ref[:, :channels] = (dgated * y * (sig_z * (1.0 + z * (1.0 - sig_z)))).astype(BF16)

    state_low = enter_ref[0].astype(BF16)
    dstate_low = dstate[...].astype(BF16)
    grown_low = (dy * grown_w).astype(BF16)
    dy_low = dy.astype(BF16)
    tailed = scaled * tails_w
    outer = dot(c_low, state_low) * grown_w
    from_state = dot(b_low, dstate_low)
    dc = dot(grown_low, state_low, NT)
    db = dot(tailed.astype(BF16), dstate_low, NT)
    leak = from_state * tailed
    last_w = grown_w[span - 1 : span, :]
    ends = (
        jnp.sum(leak, axis=0, keepdims=True)
        + jnp.sum(enter_ref[0] * dstate[...], axis=0, keepdims=True) * last_w
    )
    skips = jnp.sum(dy * inputs, axis=0, keepdims=True)
    dstate[...] = dstate[...] * last_w + dot(c_low, grown_low, TN)

    cross = dot(c_low, b_low, NT)
    causal = iota((span, span), 1) <= iota((span, span), 0)
    low_lanes = iota((span, LANES), 1) < MP
    lane = iota((span, LANES), 1)
    dcross = jnp.zeros((span, span), F32)
    row_part = jnp.zeros((span, LANES), F32)
    for pair in range(channels // LANES):
        lanes = slice(pair * LANES, (pair + 1) * LANES)
        decays = pair_decay(cum, cum_rows, pair, causal)
        dy_pair = pair_split(dy_low[:, lanes], low_lanes)
        dweights = dot(dy_pair, scaled_low[:, lanes], NT)
        both = []
        for part in range(2):
            head = 2 * pair + part
            dterm = dweights[part * span : (part + 1) * span] * decays[part]
            dcross = dcross + dterm
            flow = dterm * cross
            row_part = row_part + jnp.where(
                lane == head, jnp.sum(flow, axis=1, keepdims=True), 0.0
            )
            col_buf[head : head + 1, :] = jnp.sum(flow, axis=0, keepdims=True)
            both.append((cross * decays[part]).astype(BF16))
        du_buf[:, lanes] = dot(jnp.concatenate(both, axis=0), dy_pair, TN)
    du = du_buf[...] + from_state * tails_w
    dcross_low = dcross.astype(BF16)
    dc = dc + dot(dcross_low, b_low)
    db = db + dot(dcross_low, c_low, TN)

    sums = gather_heads(
        jnp.concatenate(
            [dy * outer - leak, du * inputs, ends, skips, jnp.zeros((EDGE - 2, channels), F32)],
            axis=0,
        ),
        spread,
    )
    at_end = sums[2 * span : 2 * span + 1, :]
    dcum = sums[:span] + row_part - col_buf[...].T
    upper = (iota((span, span), 1) >= iota((span, span), 0)).astype(BF16)
    drate = pick_left(upper, dcum, 3) + at_end
    dstep = drate * decay + sums[span : 2 * span]
    draw = dstep * jax.nn.sigmoid(raw)
    gh_ref[0:1, :] += jnp.sum(draw, axis=0, keepdims=True)
    gh_ref[1:2, :] += jnp.sum(drate * step, axis=0, keepdims=True) * decay
    gh_ref[2:3, :] += sums[2 * span + 1 : 2 * span + 2, :]

    dinputs = du * step_w + skip * dy
    dxbuf[span:, :] = dxbuf[:EDGE, :]
    dbbuf[span:, :] = dbbuf[:EDGE, :]
    dconv = dinputs * (sig * (1.0 + conv * (1.0 - sig)))
    dconvb = jnp.concatenate([db, dc], axis=1) * (sigb * (1.0 + convb * (1.0 - sigb)))
    dxbuf[:span, :] = dconv
    dbbuf[:span, :] = dconvb
    dx = jnp.zeros_like(dconv)
    dbc = jnp.zeros_like(dconvb)
    for tap in range(KCONV):
        back = KCONV - 1 - tap
        start = EDGE - 3 + tap
        dx = dx + tap_ref[tap : tap + 1, :] * dxbuf[back : back + span, :]
        dbc = dbc + tapb_ref[tap : tap + 1, :] * dbbuf[back : back + span, :]
        gx_ref[tap : tap + 1, :] += jnp.sum(
            dconv * xbuf[start : start + span, :], axis=0, keepdims=True
        )
        gb_ref[tap : tap + 1, :] += jnp.sum(
            dconvb * bbuf[start : start + span, :], axis=0, keepdims=True
        )
    gx_ref[KCONV : KCONV + 1, :] += jnp.sum(dconv, axis=0, keepdims=True)
    gb_ref[KCONV : KCONV + 1, :] += jnp.sum(dconvb, axis=0, keepdims=True)
    gx_ref[KCONV + 1 : KCONV + 2, :] += gain_grad
    width = 2 * channels + 2 * NS
    grad_ref[:, channels : 2 * channels] = dx.astype(BF16)
    grad_ref[:, 2 * channels : width] = dbc.astype(BF16)
    grad_ref[:, width : width + dqkv_ref.shape[1]] = dqkv_ref[...]
    grad_ref[:, width + dqkv_ref.shape[1] :] = draw.astype(BF16)
    for step in range(ring.ahead):
        pl.when(turn == spans * step // ring.ahead)(functools.partial(ring.hop, step))
    pl.when(turn == spans - 1)(ring.finish)


def scan_params(conv_x, conv_xb, conv_bc, conv_bcb, dt_bias, a_log, d_skip, w_mnorm):
    heads = dt_bias.shape[0]
    fill = jnp.zeros((LANES - heads,), BF16)
    flat = [conv_xb, w_mnorm, conv_bcb, dt_bias, fill, a_log, fill, d_skip, fill]
    size = sum(item.shape[0] for item in flat) // LANES
    flat.append(jnp.zeros((-size % EDGE * LANES,), BF16))
    rows = jnp.concatenate(flat).astype(F32).reshape(-1, LANES)
    return (conv_x.astype(F32), conv_bc.astype(F32), rows)


def unpack_rows(row_ref, spread):
    channels = spread.shape[1]
    count = channels // LANES
    at = 2 * count + 2 * NS // LANES

    def join_rows(first, number):
        return jnp.concatenate(
            [row_ref[i : i + 1, :] for i in range(first, first + number)], axis=1
        )

    skip = jnp.broadcast_to(row_ref[at + 2 : at + 3, :], (EDGE, LANES)).astype(BF16)
    return (
        join_rows(0, count),
        join_rows(count, count),
        join_rows(2 * count, 2 * NS // LANES),
        row_ref[at : at + 1, :],
        -jnp.exp(row_ref[at + 1 : at + 2, :]),
        dot(skip, spread)[:1],
    )


def whole_spec(array):
    return pl.BlockSpec(array.shape, lambda turn: (0,) * array.ndim)


def run_scan_forward(proj, qkv_width, params, shard, devices):
    tokens = proj.shape[0]
    channels = params[0].shape[1]
    step_at = (2 * channels + 2 * NS + qkv_width) // LANES
    spans = tokens // SPAN
    bc_at = 2 * channels // (2 * NS)
    rows = lambda width, at: pl.BlockSpec((SPAN, width), lambda turn: (turn, at))
    anywhere = pl.BlockSpec(memory_space=pl.ANY)
    return pl.pallas_call(
        functools.partial(scan_forward, devices, spans),
        grid=(spans,),
        out_shape=(
            jax.ShapeDtypeStruct((tokens, channels), F32),
            jax.ShapeDtypeStruct((tokens, channels), F32),
            jax.ShapeDtypeStruct((EDGE, tokens), F32),
            jax.ShapeDtypeStruct((spans, NS, channels), F32),
            gather_shape(shard, devices),
        ),
        in_specs=[rows(channels, 0), rows(channels, 1), rows(2 * NS, bc_at), rows(LANES, step_at)]
        + [whole_spec(item) for item in params]
        + [anywhere],
        out_specs=(
            rows(channels, 0),
            rows(channels, 0),
            pl.BlockSpec((EDGE, SPAN), lambda turn: (0, turn)),
            pl.BlockSpec((1, NS, channels), lambda turn: (turn, 0, 0)),
            anywhere,
        ),
        scratch_shapes=[
            pltpu.VMEM((NS, channels), F32),
            pltpu.VMEM((SPAN + EDGE, channels), F32),
            pltpu.VMEM((SPAN + EDGE, 2 * NS), F32),
        ]
        + gather_sems(devices),
        compiler_params=pltpu.CompilerParams(collective_id=2, has_side_effects=True),
        cost_estimate=cost(20),
        name="scan_forward",
    )(proj, proj, proj, proj, *params, shard)


def run_scan_backward(
    proj, y, entering, dyg, scale, inner, dqkv, params, sent, windows, pieces, shapes,
    devices,
):
    tokens, width = proj.shape
    channels = params[0].shape[1]
    qkv_width = dqkv.shape[1]
    step_at = (2 * channels + 2 * NS + qkv_width) // LANES
    spans = tokens // SPAN
    bc_at = 2 * channels // (2 * NS)
    edges = SPAN // EDGE
    rows = lambda size, at: pl.BlockSpec((SPAN, size), lambda turn: (spans - 1 - turn, at))
    edge = lambda size, at: pl.BlockSpec(
        (EDGE, size), lambda turn: (jnp.maximum((spans - 1 - turn) * edges - 1, 0), at)
    )
    keep = lambda shape: pl.BlockSpec(shape, lambda turn: (0, 0))
    shapes = tuple(jax.ShapeDtypeStruct(shape, F32) for shape in shapes)
    return pl.pallas_call(
        functools.partial(
            scan_backward, devices, spans, windows, pieces, len(shapes), len(sent)
        ),
        grid=(spans,),
        out_shape=(
            jax.ShapeDtypeStruct((tokens, width), BF16),
            jax.ShapeDtypeStruct((EDGE, channels), F32),
            jax.ShapeDtypeStruct((EDGE, 2 * NS), F32),
            jax.ShapeDtypeStruct((EDGE, LANES), F32),
        )
        + shapes,
        in_specs=[
            rows(channels, 0),
            rows(channels, 1),
            edge(channels, 1),
            rows(2 * NS, bc_at),
            edge(2 * NS, bc_at),
            rows(LANES, step_at),
            rows(channels, 0),
            pl.BlockSpec((1, NS, channels), lambda turn: (spans - 1 - turn, 0, 0)),
            rows(channels, 0),
            pl.BlockSpec((EDGE, SPAN), lambda turn: (0, spans - 1 - turn)),
            pl.BlockSpec((EDGE, SPAN), lambda turn: (0, spans - 1 - turn)),
            rows(qkv_width, 0),
        ]
        + [whole_spec(item) for item in params]
        + [pl.BlockSpec(memory_space=pl.ANY)] * len(sent),
        out_specs=(
            rows(width, 0),
            keep((EDGE, channels)),
            keep((EDGE, 2 * NS)),
            keep((EDGE, LANES)),
        )
        + tuple(keep(item.shape) for item in shapes),
        scratch_shapes=[
            pltpu.VMEM((NS, channels), F32),
            pltpu.VMEM((SPAN + EDGE, channels), F32),
            pltpu.VMEM((SPAN + EDGE, 2 * NS), F32),
            pltpu.VMEM((SPAN + EDGE, channels), F32),
            pltpu.VMEM((SPAN + EDGE, 2 * NS), F32),
            pltpu.VMEM((SPAN, channels), F32),
            pltpu.VMEM((LANES, SPAN), F32),
        ]
        + scatter_scratch(windows, sent[0].shape[0] // devices, devices),
        compiler_params=pltpu.CompilerParams(collective_id=6, has_side_effects=True),
        cost_estimate=cost(47),
        name="scan_backward",
    )(
        proj, proj, proj, proj, proj, proj, y, entering, dyg, scale, inner, dqkv, *params, *sent,
    )


def rotary_tables(tokens):
    half = HEAD_SIZE // 2
    exponent = np.arange(half, dtype=np.float64) * (-2.0 * LOG_BASE / HEAD_SIZE)
    rates = np.tile(np.exp(exponent.astype(np.float32)).astype(np.float64), LANES // half)
    tables = []
    for places in (np.arange(FINE), np.arange(0, tokens, FINE)):
        angles = places[:, None] * rates[None, :]
        tables += [np.cos(angles).astype(np.float32), np.sin(angles).astype(np.float32)]
    return tables


def fill_rotary(fine_cos, fine_sin, coarse_cos, coarse_sin, cosine, sine):
    small_cos, small_sin = fine_cos[...], fine_sin[...]
    for turn in range(coarse_cos.shape[0]):
        big_cos, big_sin = coarse_cos[turn : turn + 1, :], coarse_sin[turn : turn + 1, :]
        rows = slice(turn * FINE, (turn + 1) * FINE)
        cosine[rows, :] = small_cos * big_cos - small_sin * big_sin
        sine[rows, :] = small_sin * big_cos + small_cos * big_sin


def head_masks():
    half = HEAD_SIZE // 2
    row, col = iota((LANES, LANES), 0), iota((LANES, LANES), 1)
    place = col % HEAD_SIZE
    ahead = jnp.where(place < half, -1.0, 0.0)
    behind = jnp.where(place < half, 0.0, 1.0)

    def turn(start):
        return jnp.where(row == start + half, ahead, jnp.where(row == start - half, behind, 0.0))

    first = row < HEAD_SIZE
    left = col < HEAD_SIZE
    low = lambda mask: mask.astype(BF16)
    within = low(turn(col))
    copy = low(jnp.where(row == place, 1.0, 0.0))
    copy_turn = low(jnp.where(first, turn(place), 0.0))
    value = low(jnp.where(row == place + HEAD_SIZE, 1.0, 0.0))
    fold = low(jnp.where(left & (row % HEAD_SIZE == place), 1.0, 0.0))
    other = row % HEAD_SIZE
    fold_turn = low(
        jnp.where(
            left,
            jnp.where(other == place + half, ahead, jnp.where(other == place - half, behind, 0.0)),
            0.0,
        )
    )
    fold_value = low(jnp.where(left, 0.0, jnp.where(other == place, 1.0, 0.0)))
    return within, copy, copy_turn, value, fold, fold_turn, fold_value


def attend_forward(
    q_ref, kv_ref, fine_cos, fine_sin, coarse_cos, coarse_sin,
    qkv_ref, lse_ref, o_ref, vt, cos_ref, sin_ref,
):
    fill_rotary(fine_cos, fine_sin, coarse_cos, coarse_sin, cos_ref, sin_ref)
    tokens, query_width = q_ref.shape
    pairs = query_width // LANES
    within, copy, copy_turn, value = head_masks()[:4]

    def turn_rows(i, carry):
        rows = pl.ds(pl.multiple_of(i * QBLK, QBLK), QBLK)
        cosine, sine = cos_ref[rows, :], sin_ref[rows, :]
        for pair in range(pairs):
            lanes = slice(pair * LANES, (pair + 1) * LANES)
            query = q_ref[rows, lanes]
            turned = query * cosine + pick(query, within) * sine
            qkv_ref[rows, lanes] = (turned * HEAD_SIZE**-0.5).astype(BF16)
        kv = kv_ref[rows, :]
        keys = pick(kv, copy) * cosine + pick(kv, copy_turn) * sine
        qkv_ref[rows, query_width : query_width + LANES] = keys.astype(BF16)
        qkv_ref[rows, query_width + LANES :] = dot(kv.astype(BF16), value).astype(BF16)
        vt[:, rows] = kv.T[HEAD_SIZE:, :].astype(BF16)
        return carry

    lax.fori_loop(0, tokens // QBLK, turn_rows, 0)
    low_lanes = iota((QBLK, LANES), 1) < HEAD_SIZE
    wide = (QBLK, 2 * QBLK)
    visible = iota(wide, 0) <= iota(wide, 1) % QBLK

    def block(i, carry):
        here = pl.ds(pl.multiple_of(i * QBLK, QBLK), QBLK)
        queries = [
            pair_split(qkv_ref[here, pair * LANES : (pair + 1) * LANES], low_lanes)
            for pair in range(pairs)
        ]

        def tile(there, state, edge):
            keys = qkv_ref[there, query_width : query_width + LANES]
            result = []
            for pair in range(pairs):
                top, total, out = state[3 * pair : 3 * pair + 3]
                scores = dot(keys, queries[pair], NT)
                if edge:
                    scores = jnp.where(visible, scores, MASKED)
                higher = jnp.maximum(top, jnp.max(scores, axis=0, keepdims=True))
                probs = jnp.exp(scores - higher)
                fade = jnp.exp(top - higher)
                total = total * fade + jnp.sum(probs, axis=0, keepdims=True)
                out = out * fade + dot(vt[:, there], probs.astype(BF16))
                result += [higher, total, out]
            return tuple(result)

        state = (
            jnp.full((1, 2 * QBLK), MASKED, F32),
            jnp.zeros((1, 2 * QBLK), F32),
            jnp.zeros((HEAD_SIZE, 2 * QBLK), F32),
        ) * pairs
        state = lax.fori_loop(
            0,
            i,
            lambda j, state: tile(pl.ds(pl.multiple_of(j * QBLK, QBLK), QBLK), state, False),
            state,
        )
        state = tile(here, state, True)
        for pair in range(pairs):
            top, total, out = state[3 * pair : 3 * pair + 3]
            out = out / total
            lse = top + jnp.log(total)
            lse_ref[2 * pair : 2 * pair + 1, here] = lse[:, :QBLK]
            lse_ref[2 * pair + 1 : 2 * pair + 2, here] = lse[:, QBLK:]
            both = jnp.concatenate([out[:, :QBLK], out[:, QBLK:]], axis=0)
            o_ref[here, pair * LANES : (pair + 1) * LANES] = both.T.astype(BF16)
        return carry

    lax.fori_loop(0, tokens // QBLK, block, 0)


def attend_backward(
    qkv_ref, lse_ref, o_ref, do_ref, fine_cos, fine_sin, coarse_cos, coarse_sin,
    dqkv_ref,
    dq, kt, dk, dv, cos_ref, sin_ref,
):
    fill_rotary(fine_cos, fine_sin, coarse_cos, coarse_sin, cos_ref, sin_ref)
    tokens, query_width = o_ref.shape
    pairs = query_width // LANES
    key_lanes = slice(query_width, query_width + LANES)
    value_lanes = slice(query_width + LANES, query_width + 2 * LANES)

    def turn_keys(i, carry):
        rows = pl.ds(pl.multiple_of(i * QBLK, QBLK), QBLK)
        kt[:, rows] = qkv_ref[rows, key_lanes].astype(F32).T[:HEAD_SIZE, :].astype(BF16)
        return carry

    lax.fori_loop(0, tokens // QBLK, turn_keys, 0)
    dk[...] = jnp.zeros_like(dk)
    dv[...] = jnp.zeros_like(dv)
    low_lanes = iota((QBLK, LANES), 1) < HEAD_SIZE
    wide = (QBLK, 2 * QBLK)
    visible = iota(wide, 0) <= iota(wide, 1) % QBLK
    ones = jnp.ones((EDGE, LANES), BF16)

    def block(i, carry):
        here = pl.ds(pl.multiple_of(i * QBLK, QBLK), QBLK)
        queries, grads, inners, lses = [], [], [], []
        for pair in range(pairs):
            lanes = slice(pair * LANES, (pair + 1) * LANES)
            queries.append(pair_split(qkv_ref[here, lanes], low_lanes))
            grad = do_ref[here, lanes]
            grads.append(pair_split(grad, low_lanes))
            both = pair_split(grad.astype(F32) * o_ref[here, lanes].astype(F32), low_lanes)
            high, low = parts(both, 2)
            inners.append((dot(ones, high, NT) + dot(ones, low, NT))[:1])
            lses.append(
                jnp.concatenate(
                    [
                        lse_ref[2 * pair : 2 * pair + 1, here],
                        lse_ref[2 * pair + 1 : 2 * pair + 2, here],
                    ],
                    axis=1,
                )
            )
        query_all = jnp.concatenate(queries, axis=0)
        grad_all = jnp.concatenate(grads, axis=0)

        def tile(there, state, edge):
            keys = qkv_ref[there, key_lanes]
            values = qkv_ref[there, value_lanes]
            all_probs, all_dscores, result = [], [], []
            for pair in range(pairs):
                probs = dot(keys, queries[pair], NT) - lses[pair]
                if edge:
                    probs = jnp.where(visible, probs, MASKED)
                probs = jnp.exp(probs)
                dprobs = dot(values, grads[pair], NT)
                dscores = (probs * (dprobs - inners[pair])).astype(BF16)
                all_probs.append(probs.astype(BF16))
                all_dscores.append(dscores)
                result.append(state[pair] + dot(kt[:, there], dscores))
            dv[there, :] += dot(jnp.concatenate(all_probs, axis=1), grad_all)
            dk[there, :] += dot(jnp.concatenate(all_dscores, axis=1), query_all)
            return tuple(result)

        state = (jnp.zeros((HEAD_SIZE, 2 * QBLK), F32),) * pairs
        state = lax.fori_loop(
            0,
            i,
            lambda j, state: tile(pl.ds(pl.multiple_of(j * QBLK, QBLK), QBLK), state, False),
            state,
        )
        state = tile(here, state, True)
        for pair in range(pairs):
            both = jnp.concatenate([state[pair][:, :QBLK], state[pair][:, QBLK:]], axis=0)
            dq[here, pair * LANES : (pair + 1) * LANES] = both.T
        return carry

    lax.fori_loop(0, tokens // QBLK, block, 0)
    masks = head_masks()
    within, (fold, fold_turn, fold_value) = masks[0], masks[4:]

    def turn_back(i, carry):
        rows = pl.ds(pl.multiple_of(i * QBLK, QBLK), QBLK)
        cosine, sine = cos_ref[rows, :], sin_ref[rows, :]
        for pair in range(pairs):
            lanes = slice(pair * LANES, (pair + 1) * LANES)
            grad = dq[rows, lanes]
            grad = grad * cosine - pick(grad, within) * sine
            dqkv_ref[rows, lanes] = (grad * HEAD_SIZE**-0.5).astype(BF16)
        grad = dk[rows, :]
        grad = pick(grad, fold) * cosine - pick(grad, fold_turn) * sine
        grad = grad + pick(dv[rows, :], fold_value)
        dqkv_ref[rows, query_width:] = grad.astype(BF16)
        return carry

    lax.fori_loop(0, tokens // QBLK, turn_back, 0)


def run_attend_forward(proj, query_at, query_width, tables):
    tokens = proj.shape[0]
    cols = lambda size, at: pl.BlockSpec((tokens, size), lambda turn: (0, at // size))
    return pl.pallas_call(
        attend_forward,
        grid=(1,),
        out_shape=(
            jax.ShapeDtypeStruct((tokens, query_width + 2 * LANES), BF16),
            jax.ShapeDtypeStruct((EDGE, tokens), F32),
            jax.ShapeDtypeStruct((tokens, query_width), BF16),
        ),
        in_specs=[
            cols(query_width, query_at),
            cols(2 * HEAD_SIZE, query_at + query_width),
        ]
        + [whole_spec(table) for table in tables],
        out_specs=(
            cols(query_width + 2 * LANES, 0),
            pl.BlockSpec((EDGE, tokens), lambda turn: (0, 0)),
            cols(query_width, 0),
        ),
        scratch_shapes=[
            pltpu.VMEM((HEAD_SIZE, tokens), BF16),
            pltpu.VMEM((tokens, LANES), F32),
            pltpu.VMEM((tokens, LANES), F32),
        ],
        cost_estimate=cost(15),
        name="attend_forward",
    )(proj, proj, *tables)


def run_attend_backward(qkv, lse, attended, grads, grad_at, tables):
    tokens, query_width = attended.shape
    vmem = pl.BlockSpec(memory_space=pltpu.VMEM)
    cols = lambda size, at: pl.BlockSpec((tokens, size), lambda turn: (0, at // size))
    return pl.pallas_call(
        attend_backward,
        grid=(1,),
        out_shape=jax.ShapeDtypeStruct((tokens, query_width + 2 * HEAD_SIZE), BF16),
        in_specs=[
            whole_spec(qkv),
            whole_spec(lse),
            whole_spec(attended),
            cols(query_width, grad_at),
        ]
        + [whole_spec(table) for table in tables],
        out_specs=cols(query_width + 2 * HEAD_SIZE, 0),
        scratch_shapes=[
            pltpu.VMEM((tokens, query_width), F32),
            pltpu.VMEM((HEAD_SIZE, tokens), BF16),
            pltpu.VMEM((tokens, LANES), F32),
            pltpu.VMEM((tokens, LANES), F32),
            pltpu.VMEM((tokens, LANES), F32),
            pltpu.VMEM((tokens, LANES), F32),
        ],
        cost_estimate=cost(16),
        name="attend_backward",
    )(qkv, lse, attended, grads, *tables)


def feed_forward(
    x_ref, mixed_ref, other_ref, top_ref, gain_ref, gu_ref, down_ref,
    after_ref, scale_ref, hidden_ref, act_ref, dgu_ref, part_ref, back_ref,
):
    units = down_ref.shape[1]
    after = x_ref[...].astype(F32) + (mixed_ref[...].astype(F32) + other_ref[...].astype(F32))
    after_ref[...] = after
    scale = lax.rsqrt(jnp.mean(after * after, axis=-1, keepdims=True) + EPSILON)
    scale_ref[...] = scale
    hidden = (after * scale * gain_ref[...]).astype(BF16)
    hidden_ref[...] = hidden
    top = top_ref[...]
    for start in range(0, units, UBLK):
        cols = slice(start, start + UBLK)
        up_cols = slice(units + start, units + start + UBLK)
        gate = dot(hidden, gu_ref[:, cols])
        upward = dot(hidden, gu_ref[:, up_cols])
        grad = dot(top, down_ref[:, cols])
        sigma = jax.nn.sigmoid(gate)
        swish = gate * sigma
        act_ref[:, cols] = (swish * upward).astype(BF16)
        slope = sigma * (1.0 + gate * (1.0 - sigma))
        dgu_ref[:, cols] = (grad * upward * slope).astype(BF16)
        dgu_ref[:, up_cols] = (grad * swish).astype(BF16)
    back_ref[...] = dot(dgu_ref[...], gu_ref[...], NT).astype(BF16)
    part_ref[...] = dot(act_ref[...], down_ref[...], NT).astype(BF16)


def once(item):
    return pl.BlockSpec(item.shape, lambda turn: (0,) * item.ndim, pipeline_mode=pl.Buffered(1))


def run_feed_forward(x, mixed, other, top, gain, w_gate_up, w_down_t):
    tokens, width = x.shape
    units = w_down_t.shape[1]
    rows = lambda size: pl.BlockSpec((TBLK, size), lambda turn: (turn, 0))
    shape = jax.ShapeDtypeStruct
    return pl.pallas_call(
        feed_forward,
        grid=(tokens // TBLK,),
        out_shape=(
            shape((tokens, width), F32),
            shape((tokens, 1), F32),
            shape((tokens, width), BF16),
            shape((tokens, units), BF16),
            shape((tokens, 2 * units), BF16),
            shape((tokens, width), BF16),
            shape((tokens, width), BF16),
        ),
        in_specs=[rows(width)] * 4 + [once(gain), once(w_gate_up), once(w_down_t)],
        out_specs=(
            rows(width), rows(1), rows(width), rows(units), rows(2 * units), rows(width),
            rows(width),
        ),
        cost_estimate=cost(20),
        name="feed_forward",
    )(x, mixed, other, top, gain, w_gate_up, w_down_t)


def mixer_forward(gated_ref, scale_ref, gain_ref, attended_ref, w_ref, low_ref, mixed_ref):
    channels = gated_ref.shape[1]
    scale = scale_ref[...].T[:, :1]
    low_ref[:, :channels] = (gated_ref[...] * scale * gain_ref[...]).astype(BF16)
    low_ref[:, channels:] = attended_ref[...]
    mixed_ref[...] = dot(low_ref[...], w_ref[...], NT).astype(BF16)


def run_mixer_forward(gated, scale, gain, attended, w_out):
    tokens, channels = gated.shape
    width, inner = w_out.shape
    rows = lambda size: pl.BlockSpec((TBLK, size), lambda turn: (turn, 0))
    return pl.pallas_call(
        mixer_forward,
        grid=(tokens // TBLK,),
        out_shape=(
            jax.ShapeDtypeStruct((tokens, inner), BF16),
            jax.ShapeDtypeStruct((tokens, width), BF16),
        ),
        in_specs=[
            rows(channels),
            pl.BlockSpec((EDGE, TBLK), lambda turn: (0, turn)),
            once(gain),
            rows(attended.shape[1]),
            once(w_out),
        ],
        out_specs=(rows(inner), rows(width)),
        cost_estimate=cost(5),
        name="mixer_forward",
    )(gated, scale, gain, attended, w_out)


def mixer_backward(
    part_ref, other_ref, after_ref, scale_ref, top_ref, gain_ref,
    w_ref, gated_ref, scale_m_ref, gain_m_ref,
    grad_ref, low_ref, mamba_ref, attended_ref, inner_ref, gain_grad_ref,
):
    channels = gated_ref.shape[1]

    @pl.when(pl.program_id(0) == 0)
    def _():
        gain_grad_ref[...] = jnp.zeros_like(gain_grad_ref)

    grad = part_ref[...].astype(F32) + other_ref[...].astype(F32)
    scale = scale_ref[...]
    normed = after_ref[...] * scale
    gain_grad_ref[:1, :] += jnp.sum(grad * normed, axis=0, keepdims=True)
    weighted = grad * gain_ref[...]
    mean = jnp.mean(weighted * normed, axis=-1, keepdims=True)
    total = top_ref[...].astype(F32) + scale * (weighted - normed * mean)
    grad_ref[...] = total
    low_ref[...] = total.astype(BF16)
    back = dot(low_ref[...], w_ref[...])
    mamba = back[:, :channels]
    mamba_ref[...] = mamba
    attended_ref[...] = back[:, channels:].astype(BF16)
    inner_ref[...] = row_sums(mamba * gain_m_ref[...] * gated_ref[...]) * scale_m_ref[...]


def run_mixer_backward(part, other, after, scale, top, gain, w_out, gated, scale_m, gain_m):
    tokens, width = after.shape
    channels = gated.shape[1]
    inner = w_out.shape[1]
    shape = jax.ShapeDtypeStruct
    rows = lambda size: pl.BlockSpec((NBLK, size), lambda turn: (turn, 0))
    lanes = pl.BlockSpec((EDGE, NBLK), lambda turn: (0, turn))
    return pl.pallas_call(
        mixer_backward,
        grid=(tokens // NBLK,),
        out_shape=(
            shape((tokens, width), F32),
            shape((tokens, width), BF16),
            shape((tokens, channels), F32),
            shape((tokens, inner - channels), BF16),
            shape((EDGE, tokens), F32),
            shape((EDGE, width), F32),
        ),
        in_specs=[rows(width)] * 3
        + [rows(1), rows(width), once(gain), once(w_out), rows(channels), lanes, once(gain_m)],
        out_specs=(
            rows(width), rows(width), rows(channels), rows(inner - channels), lanes,
            pl.BlockSpec((EDGE, width), lambda turn: (0, 0)),
        ),
        cost_estimate=cost(8),
        name="mixer_backward",
    )(part, other, after, scale, top, gain, w_out, gated, scale_m, gain_m)


def finish_layer(
    x_ref, gain_ref, part_ref, other_ref, grad_ref, after_ref, ffn_ref, ffn_other_ref, *refs,
):
    count = len(refs) // 2 - 1
    passed, out_ref, result_ref, handed = refs[:count], refs[count], refs[count + 1], refs[count + 2 :]

    @pl.when(pl.program_id(0) == 0)
    def _():
        for source, target in zip(passed, handed):
            target[...] = source[...]

    x = x_ref[...].astype(F32)
    scale = lax.rsqrt(jnp.mean(x * x, axis=-1, keepdims=True) + EPSILON)
    normed = x * scale
    weighted = (part_ref[...].astype(F32) + other_ref[...].astype(F32)) * gain_ref[...]
    mean = jnp.mean(weighted * normed, axis=-1, keepdims=True)
    out_ref[...] = grad_ref[...] + scale * (weighted - normed * mean)
    ffn = ffn_ref[...].astype(F32) + ffn_other_ref[...].astype(F32)
    result_ref[...] = (after_ref[...] + ffn).astype(BF16)


def run_finish(x, gain, part, other, grad, after, ffn, ffn_other, passed):
    tokens, width = x.shape
    rows = pl.BlockSpec((TBLK, width), lambda turn: (turn, 0))
    return pl.pallas_call(
        finish_layer,
        grid=(tokens // TBLK,),
        out_shape=(
            jax.ShapeDtypeStruct((tokens, width), F32),
            jax.ShapeDtypeStruct((tokens, width), BF16),
        )
        + tuple(jax.ShapeDtypeStruct(item.shape, F32) for item in passed),
        in_specs=[rows, once(gain)] + [rows] * 6 + [once(item) for item in passed],
        out_specs=(rows, rows) + tuple(once(item) for item in passed),
        cost_estimate=cost(8),
        name="finish_layer",
    )(x, gain, part, other, grad, after, ffn, ffn_other, *passed)


def swap(partial):
    return lax.ppermute(partial, "tensor", [(0, 1), (1, 0)])


def join(mine, other):
    return mine.astype(F32) + other.astype(F32)


def tensor_sum(partial):
    return join(partial, swap(partial))


def local(
    layer_input, w_norm1, w_zx, w_bc, w_dt, conv_x, conv_xb, conv_bc, conv_bcb, dt_bias, a_log,
    d_skip, w_mnorm, w_mout, query_key_value_weight, output_weight, w_norm2, w_gu, w_down,
    grad_output,
):
    devices = lax.axis_size("dp")
    tokens, width = layer_input.shape
    shard = w_zx.shape[0]
    channels = conv_xb.shape[0]
    heads = dt_bias.shape[0]
    qkv_width = query_key_value_weight.shape[2]
    units = w_down.shape[0]
    attn_width = output_weight.shape[1]
    tail = jnp.concatenate(
        [w_dt, w_norm1[:, None], w_norm2[:, None], jnp.zeros((shard, LANES - heads - 2), BF16)],
        axis=1,
    )
    mixer_in = jnp.concatenate(
        [w_zx.reshape(shard, -1), w_bc, query_key_value_weight.reshape(shard, -1), tail], axis=1
    )
    in_width = mixer_in.shape[1]
    (w_in,) = gather_rows([mixer_in], devices, 0)
    norm1 = w_in[:, in_width - LANES + heads].astype(F32)
    norm2 = w_in[:, in_width - LANES + heads + 1].astype(F32)

    source = layer_input.astype(F32)
    scale_one = lax.rsqrt(jnp.mean(source * source, axis=-1, keepdims=True) + EPSILON)
    normed_one = source * scale_one
    hidden_one = lax.optimization_barrier((normed_one * norm1).astype(BF16))
    proj = dot(hidden_one, w_in)
    params = scan_params(
        conv_x, conv_xb, conv_bc, conv_bcb, dt_bias, a_log, d_skip, w_mnorm
    )
    out_shard = jnp.concatenate([w_mout.T, output_weight.reshape(attn_width, -1).T], axis=1)
    y, gated, square_sum, entering, w_out = run_scan_forward(
        proj, qkv_width, params, out_shard, devices
    )
    channels_all = channels * lax.axis_size("tensor")
    scale_m = lax.rsqrt(tensor_sum(square_sum) / channels_all + EPSILON)
    tables = rotary_tables(tokens)
    qkv_at = 2 * channels + 2 * NS
    qkv, lse, attended = run_attend_forward(proj, qkv_at, attn_width, tables)
    gain_m = w_mnorm.astype(F32)[None, :]
    mixer_out, mixed = run_mixer_forward(gated, scale_m, gain_m, attended, w_out)
    mixed, gate_up_shard, down_shard = lax.optimization_barrier(
        (mixed, w_gu.reshape(shard, -1), w_down.T)
    )
    other = swap(mixed)
    w_gate_up, w_down_t = gather_rows([gate_up_shard, down_shard], devices, 3)
    other, w_gate_up, w_down_t = lax.optimization_barrier((other, w_gate_up, w_down_t))
    after, scale_two, hidden_two, activated, grad_gu_low, ffn_part, partial_two = run_feed_forward(
        layer_input, mixed, other, grad_output, norm2[None, :], w_gate_up, w_down_t
    )
    other = swap(partial_two)
    grad_down = dot(grad_output, activated, TN).astype(BF16)
    (mine_gu,) = scatter_product(
        hidden_two,
        grad_gu_low,
        [(0, 1, 0, 2 * units)],
        [(0, 0, units, 0, 0), (0, units, 2 * units, 0, 1)],
        [(shard, 2, units)],
        devices,
        1,
    )
    other, mine_gu, grad_down, ffn_part = lax.optimization_barrier(
        (other, mine_gu, grad_down, ffn_part)
    )
    ffn_other = swap(ffn_part)
    grad_after, grad_mix_low, grad_mamba, grad_attended, inner_m, grad_norm2 = run_mixer_backward(
        partial_two, other, after, scale_two, grad_output, norm2[None, :], w_out, gated, scale_m,
        gain_m,
    )
    inner_m = tensor_sum(inner_m) / channels_all
    dqkv = run_attend_backward(qkv, lse, attended, grad_attended, 0, tables)
    grad_out = dot(grad_mix_low, mixer_out, TN).astype(BF16)
    windows = [(0, None, 0, channels + attn_width), (1, None, 0, units)]
    pieces = [
        (0, 0, channels, 0, None),
        (0, channels, channels + attn_width, 1, None),
        (1, 0, units, 2, None),
    ]
    shapes = [(shard, channels), (shard, attn_width), (shard, units)]
    grad_proj, small_x, small_b, small_h, mine_mout, mine_o, mine_down = run_scan_backward(
        proj, y, entering, grad_mamba, scale_m, inner_m, dqkv, params,
        [grad_out, grad_down], windows, pieces, shapes, devices,
    )
    ffn_other, grad_proj = lax.optimization_barrier((ffn_other, grad_proj))
    partial_one, grad_proj = lax.optimization_barrier(
        (dot(grad_proj, w_in, NT).astype(BF16), grad_proj)
    )
    other = swap(partial_one)
    grad_norm1 = jnp.sum(partial_one.astype(F32) * normed_one, axis=0)
    small = jnp.concatenate(
        [
            small_x[: KCONV + 2].reshape(-1, LANES),
            small_h[:3],
            grad_norm2[0].reshape(-1, LANES),
            small_b[: KCONV + 1].reshape(-1, LANES),
            grad_norm1.reshape(-1, LANES),
        ],
        axis=0,
    )
    small_rows = small.shape[0]
    cross_rows = (KCONV + 1) * 2 * NS // LANES + width // LANES
    cross_at = small_rows - cross_rows
    small = jnp.pad(small, ((0, -small_rows % EDGE), (0, 0)))
    shared_at = 2 * channels
    step_at = qkv_at + qkv_width
    mine_zx, mine_bc, mine_qkv, mine_step, small = scatter_product(
        hidden_one,
        grad_proj,
        [(0, 1, 0, in_width)],
        [
            (0, 0, channels, 0, 0),
            (0, channels, shared_at, 0, 1),
            (0, shared_at, qkv_at, 1, None),
            (0, qkv_at, step_at, 2, 0),
            (0, step_at, in_width, 3, "turned"),
        ],
        [
            (shard, 2, channels),
            (shard, 2 * NS),
            (shard, 1, qkv_width),
            (heads, shard),
        ],
        devices,
        5,
        (small,),
    )
    other, mine_bc = lax.optimization_barrier((other, mine_bc))
    crossing = tensor_sum(small[cross_at : cross_at + cross_rows])
    shared_cols = tensor_sum(mine_bc)
    passed = (mine_zx, mine_qkv, mine_step, mine_mout, mine_o, mine_gu, mine_down)
    grad_source, result, *passed = run_finish(
        layer_input, norm1[None, :], partial_one, other, grad_after, after, ffn_part, ffn_other,
        passed,
    )
    mine_zx, mine_qkv, mine_step, mine_mout, mine_o, mine_gu, mine_down = passed

    half = NS * 2 // lax.axis_size("tensor")
    begin = lax.axis_index("tensor") * half
    grad_bc = lax.dynamic_slice_in_dim(shared_cols, begin, half, 1)
    x_rows = (KCONV + 2) * channels // LANES
    norm_rows = width // LANES
    total_x = small[:x_rows].reshape(KCONV + 2, channels)
    total_h = small[x_rows : x_rows + 3]
    norm2_total = small[x_rows + 3 : cross_at].reshape(width)
    total_b = crossing[: cross_rows - norm_rows].reshape(KCONV + 1, 2 * NS)
    total_b = lax.dynamic_slice_in_dim(total_b, begin, half, 1)
    norm1_total = crossing[cross_rows - norm_rows :].reshape(width)
    norms = [
        lax.dynamic_slice_in_dim(item, lax.axis_index("dp") * shard, shard, 0)
        for item in (norm1_total, norm2_total)
    ]
    return (
        result,
        grad_source,
        norms[0],
        mine_zx,
        grad_bc,
        mine_step.T,
        total_x[:KCONV],
        total_x[KCONV],
        total_b[:KCONV],
        total_b[KCONV],
        total_h[0, :heads],
        total_h[1, :heads],
        total_h[2, :heads],
        total_x[KCONV + 1],
        mine_mout.T,
        mine_qkv,
        mine_o.T.reshape(output_weight.shape),
        norms[1],
        mine_gu,
        mine_down.T,
    )


def solution(mesh):
    return jax.shard_map(
        local,
        mesh=mesh,
        in_specs=(
            P("dp", None),
            P("dp"),
            P("dp", None, "tensor"),
            P("dp", None),
            P("dp", "tensor"),
            P(None, "tensor"),
            P("tensor"),
            P(),
            P(),
            P("tensor"),
            P("tensor"),
            P("tensor"),
            P("tensor"),
            P("tensor", "dp"),
            P("dp", "tensor", None),
            P("tensor", None, "dp"),
            P("dp"),
            P("dp", None, "tensor"),
            P("tensor", "dp"),
            P("dp", None),
        ),
        out_specs=(
            P("dp", None),
            P("dp", None),
            P("dp"),
            P("dp", None, "tensor"),
            P("dp", "tensor"),
            P("dp", "tensor"),
            P(None, "tensor"),
            P("tensor"),
            P(None, "tensor"),
            P("tensor"),
            P("tensor"),
            P("tensor"),
            P("tensor"),
            P("tensor"),
            P("tensor", "dp"),
            P("dp", "tensor", None),
            P("tensor", None, "dp"),
            P("dp"),
            P("dp", None, "tensor"),
            P("tensor", "dp"),
        ),
        check_vma=False,
    )
```

```python
import functools
import math

import jax
import jax.numpy as jnp
import numpy as np
from jax import lax
from jax.experimental import pallas as pl
from jax.experimental.pallas import tpu as pltpu
from jax.sharding import PartitionSpec as P

HEAD_SIZE = 64
MP = 64
NS = 128
KCONV = 4
SPAN = 128
QBLK = 256
FINE = 32
TBLK = 256
NBLK = 128
UBLK = 256
LANES = 128
EDGE = 8

EPSILON = 1e-05
HIGHEST = lax.Precision.HIGHEST
LOG_BASE = math.log(100000000000.0)
MASKED = -1e30
MESH = pl.DeviceIdType.MESH
F32 = jnp.float32
BF16 = jnp.bfloat16

NN = ((1,), (0,))
NT = ((1,), (1,))
TN = ((0,), (0,))


def dot(left, right, dims=NN, precision=None):
    return lax.dot_general(
        left, right, (dims, ((), ())), preferred_element_type=F32, precision=precision
    )


def iota(shape, dim):
    return lax.broadcasted_iota(jnp.int32, shape, dim)


def ring_place(chip, chips):
    odd = lax.rem(chip, 2)
    half = lax.div(chip, 2)
    return (1 - odd) * half + odd * (chips - 1 - half)


def ring_chip(place, chips):
    place = lax.rem(place + 4 * chips, chips)
    back = lax.div(place, chips // 2)
    return (1 - back) * (2 * place) + back * (2 * (chips - 1 - place) + 1)


def ring_setup(chips):
    me = lax.axis_index("dp")
    group = lax.axis_index("tensor")
    chip = lax.div(me, 2)
    core = lax.rem(me, 2)
    place = ring_place(chip, chips)
    right = ring_chip(place + 1, chips) * 2 + core
    left = ring_chip(place - 1, chips) * 2 + core
    mate = chip * 2 + (1 - core)
    barrier = pltpu.get_barrier_semaphore()
    for other in (right, left, mate):
        pl.semaphore_signal(barrier, inc=1, device_id=(other, group), device_id_type=MESH)
    pl.semaphore_wait(barrier, 3)
    return me, group, core, place, right, left, mate


class RingGather:
    def __init__(self, devices, x_ref, o_ref, sems, cols=slice(None)):
        self.cols = cols
        self.chips = devices // 2
        self.ahead = self.chips // 2
        self.behind = self.chips - 1 - self.ahead
        self.x_ref, self.o_ref, self.rows = x_ref, o_ref, x_ref.shape[0]
        self.fs, self.fr, self.bs, self.br, self.cs, self.cr, self.own_sem = sems

    def locate(self):
        me = lax.axis_index("dp")
        self.group = lax.axis_index("tensor")
        self.core = lax.rem(me, 2)
        chip = lax.div(me, 2)
        self.place = ring_place(chip, self.chips)
        self.right = ring_chip(self.place + 1, self.chips) * 2 + self.core
        self.left = ring_chip(self.place - 1, self.chips) * 2 + self.core
        self.mate = chip * 2 + (1 - self.core)
        self.me = me

    def slot(self, index):
        rows = pl.ds(pl.multiple_of(index * self.rows, self.rows), self.rows)
        return self.o_ref.at[rows, self.cols]

    def copy(self, shift, ssem, rsem, target):
        if shift == 0:
            index, source = self.me, self.x_ref.at[:, self.cols]
        else:
            index = ring_chip(self.place + shift, self.chips) * 2 + self.core
            source = self.slot(index)
        return pltpu.make_async_remote_copy(
            src_ref=source,
            dst_ref=self.slot(index),
            send_sem=ssem,
            recv_sem=rsem,
            device_id=(target, self.group),
            device_id_type=MESH,
        )

    def fore(self, step):
        return self.copy(-step, self.fs.at[step], self.fr.at[step], self.right)

    def back(self, step):
        return self.copy(step, self.bs.at[step], self.br.at[step], self.left)

    def across(self, shift):
        number = 0 if shift == 0 else 2 * abs(shift) - (1 if shift < 0 else 0)
        return self.copy(shift, self.cs.at[number], self.cr.at[number], self.mate)

    def own(self):
        return pltpu.make_async_copy(
            self.x_ref.at[:, self.cols], self.slot(self.me), self.own_sem
        )

    def greet(self):
        self.locate()
        barrier = pltpu.get_barrier_semaphore()
        for other in (self.right, self.left, self.mate):
            pl.semaphore_signal(
                barrier, inc=1, device_id=(other, self.group), device_id_type=MESH
            )
        pl.semaphore_wait(barrier, 3)

    def begin(self):
        self.locate()
        self.fore(0).start()
        self.back(0).start()
        self.across(0).start()
        self.own().start()

    def hop(self, step):
        self.locate()
        self.fore(step - 1).wait_recv()
        if step < self.ahead:
            self.fore(step).start()
        self.across(-step).start()
        if step <= self.behind:
            self.back(step - 1).wait_recv()
            if step < self.behind:
                self.back(step).start()
            self.across(step).start()

    def finish(self):
        self.locate()
        self.own().wait()
        for step in range(self.ahead):
            self.fore(step).wait_send()
        for step in range(self.behind):
            self.back(step).wait_send()
        for shift in range(-self.ahead, self.behind + 1):
            self.across(shift).wait()


def gather_sems(devices):
    dma = pltpu.SemaphoreType.DMA
    return [dma((devices // 2,))] * 6 + [dma(())]


def gather_shape(shard, devices):
    return jax.ShapeDtypeStruct((shard.shape[0] * devices, shard.shape[1]), shard.dtype)


def gather_kernel(devices, count, windows, *refs):
    shards, outs, sems = refs[:count], refs[count : 2 * count], refs[2 * count :]
    each = len(sems) // len(windows)
    rings = [
        RingGather(
            devices, shards[i], outs[i], sems[place * each : (place + 1) * each], slice(first, last)
        )
        for place, (i, first, last) in enumerate(windows)
    ]
    rings[0].greet()
    for ring in rings:
        ring.begin()
    for step in range(1, rings[0].ahead + 1):
        for ring in rings:
            ring.hop(step)
    for ring in rings:
        ring.finish()


def cost(micros):
    return pl.CostEstimate(flops=int(micros * 1e9), bytes_accessed=0, transcendentals=0)


def gather_rows(shards, devices, collective, windows):
    count = len(shards)
    anywhere = pl.BlockSpec(memory_space=pl.ANY)
    return pl.pallas_call(
        functools.partial(gather_kernel, devices, count, windows),
        out_shape=tuple(gather_shape(shard, devices) for shard in shards),
        in_specs=[anywhere] * count,
        out_specs=(anywhere,) * count,
        scratch_shapes=gather_sems(devices) * len(windows),
        compiler_params=pltpu.CompilerParams(collective_id=collective, has_side_effects=True),
        cost_estimate=cost(3),
        name="gather_rows",
    )(*shards)


def scatter_order(chips):
    ahead = chips // 2
    behind = chips - 1 - ahead
    order = []
    for step in range(ahead):
        order.append(-(ahead - step))
        if step < behind:
            order.append(behind - step)
    order.append(0)
    return order


class RingScatter:
    def __init__(self, devices, windows, pieces, operands, outs, scratch):
        self.chips = devices // 2
        self.ahead = self.chips // 2
        self.behind = self.chips - 1 - self.ahead
        self.windows, self.pieces, self.operands, self.outs = windows, pieces, operands, outs
        count = len(windows)
        self.mine, self.boxes, rest = scratch[:count], scratch[count : 2 * count], scratch[2 * count :]
        self.fbox, self.bbox, self.fout, self.bout = rest[:4]
        self.os, self.ms, self.mr, self.fs, self.fr, self.bs, self.br = rest[4:]
        self.rows = self.fbox.shape[1]
        widths = [item.shape[2] for item in self.mine]
        self.cols = [slice(sum(widths[:i]), sum(widths[: i + 1])) for i in range(count)]

    def locate(self):
        me = lax.axis_index("dp")
        self.group = lax.axis_index("tensor")
        self.core = lax.rem(me, 2)
        chip = lax.div(me, 2)
        self.place = ring_place(chip, self.chips)
        self.right = ring_chip(self.place + 1, self.chips) * 2 + self.core
        self.left = ring_chip(self.place - 1, self.chips) * 2 + self.core
        self.mate = chip * 2 + (1 - self.core)

    def greet(self):
        self.locate()
        barrier = pltpu.get_barrier_semaphore()
        for other in (self.right, self.left, self.mate):
            pl.semaphore_signal(
                barrier, inc=1, device_id=(other, self.group), device_id_type=MESH
            )
        pl.semaphore_wait(barrier, 3)

    def product(self, i):
        return self.windows[i][1] is not None

    def shift_of(self, slot):
        step = slot // 2
        odd = slot % 2
        return (1 - odd) * (step - self.ahead) + odd * (self.behind - step)

    def half(self, which):
        return pl.ds(pl.multiple_of(which * self.rows, self.rows), self.rows)

    def block(self, i, slot, which):
        index = ring_chip(self.place + self.shift_of(slot), self.chips) * 2 + which
        left, right, first, last = self.windows[i]
        return self.operands[left].at[self.half(index), first:last]

    def remote(self, source, target_ref, ssem, rsem, target):
        return pltpu.make_async_remote_copy(
            src_ref=source,
            dst_ref=target_ref,
            send_sem=ssem,
            recv_sem=rsem,
            device_id=(target, self.group),
            device_id_type=MESH,
        )

    def across(self, i, slot):
        if self.product(i):
            source = self.mine[i].at[slot, self.half(1 - self.core)]
        else:
            source = self.block(i, slot, 1 - self.core)
        return self.remote(
            source, self.boxes[i].at[slot], self.ms.at[i, slot], self.mr.at[i, slot], self.mate
        )

    def own(self, i, slot):
        return pltpu.make_async_copy(
            self.block(i, slot, self.core), self.mine[i].at[slot], self.os.at[i, slot]
        )

    def fore(self, step):
        return self.remote(
            self.fout.at[step], self.fbox.at[step], self.fs.at[step], self.fr.at[step], self.right
        )

    def back(self, step):
        return self.remote(
            self.bout.at[step], self.bbox.at[step], self.bs.at[step], self.br.at[step], self.left
        )

    def begin(self):
        self.locate()
        for i in range(len(self.windows)):
            if not self.product(i):
                for slot in range(self.chips):
                    self.across(i, slot).start()
                    self.own(i, slot).start()

    def produce(self, slot):
        chip = ring_chip(self.place + self.shift_of(slot), self.chips)
        size = 2 * self.rows
        for i, (left, right, first, last) in enumerate(self.windows):
            if right is None:
                continue
            at = pl.multiple_of(chip * size, size)
            terms = dot(self.operands[left][pl.ds(at, size), :], self.operands[right][:, first:last])
            self.mine[i][slot] = terms.astype(BF16)
            self.across(i, slot).start()

    def local_sum(self, i, slot, cols, others):
        rows = self.half(self.core) if self.product(i) else slice(None)
        total = self.mine[i][slot, rows, cols].astype(F32) + self.boxes[i][slot, :, cols].astype(F32)
        whole = slice(self.cols[i].start + cols.start, self.cols[i].start + cols.stop)
        for ref in others:
            total = total + ref[:, whole].astype(F32)
        return total

    def arrive(self, slot):
        for i in range(len(self.windows)):
            if not self.product(i):
                self.own(i, slot).wait()
            self.across(i, slot).wait_recv()

    def put(self, target, slot, others):
        self.arrive(slot)
        for i, cols in enumerate(self.cols):
            total = self.local_sum(i, slot, slice(0, cols.stop - cols.start), others)
            target[:, cols] = total.astype(BF16)

    def hop_back(self, step, later):
        if later:
            self.back(step - 1).wait_recv()
        self.put(self.bout.at[step], 2 * step, [self.bbox.at[step - 1]] if later else [])
        self.back(step).start()

    def hop_fore(self, step, later):
        if later:
            self.fore(step - 1).wait_recv()
        self.put(self.fout.at[step], 2 * step + 1, [self.fbox.at[step - 1]] if later else [])
        self.fore(step).start()

    def hop(self, step):
        self.locate()
        self.hop_back(step, step > 0)
        if step < self.behind:
            self.hop_fore(step, step > 0)

    def finish(self):
        self.locate()
        slot = self.chips - 1
        self.arrive(slot)
        self.fore(self.behind - 1).wait_recv()
        self.back(self.ahead - 1).wait_recv()
        others = [self.fbox.at[self.behind - 1], self.bbox.at[self.ahead - 1]]
        for i, first, last, out, form in self.pieces:
            total = self.local_sum(i, slot, slice(first, last), others)
            if form == "turned":
                self.outs[out][...] = total.T[: self.outs[out].shape[0]]
            elif form is None:
                self.outs[out][...] = total
            else:
                self.outs[out][:, form, :] = total
        for step in range(self.ahead):
            self.back(step).wait_send()
        for step in range(self.behind):
            self.fore(step).wait_send()
        for slot in range(self.chips):
            for i in range(len(self.windows)):
                self.across(i, slot).wait_send()


def run_rings(rings, after_first=None):
    ahead, behind = rings[0].ahead, rings[0].behind

    def turn(step, carry):
        def part(odd, kept):
            for ring in rings:
                ring.produce(2 * step + odd)
            return kept

        lax.fori_loop(0, 2, part, 0)

        @pl.when(step == 0)
        def _():
            for ring in rings:
                ring.hop_back(0, False)
                ring.hop_fore(0, False)
            if after_first is not None:
                after_first()

        @pl.when(step > 0)
        def _():
            for ring in rings:
                ring.hop_back(step, True)
                pl.when(step < behind)(functools.partial(ring.hop_fore, step, True))

        return carry

    lax.fori_loop(0, ahead, turn, 0)


def scatter_scratch(windows, rows, devices):
    chips = devices // 2
    count = len(windows)
    dma = pltpu.SemaphoreType.DMA
    widths = [last - first for left, right, first, last in windows]
    mine = [
        pltpu.VMEM((chips, rows if right is None else 2 * rows, last - first), BF16)
        for left, right, first, last in windows
    ]
    boxes = [pltpu.VMEM((chips, rows, width), BF16) for width in widths]
    box = pltpu.VMEM((chips // 2, rows, sum(widths)), BF16)
    return mine + boxes + [box] * 4 + [dma((count, chips))] * 3 + [dma((chips,))] * 4


class Total:
    def __init__(self, devices, x_ref, o_ref, scratch):
        self.chips = devices // 2
        self.x_ref, self.o_ref = x_ref, o_ref
        self.mate_box, self.joined, self.boxes, self.ms, self.mr, self.ss, self.sr = scratch
        me = lax.axis_index("dp")
        self.group = lax.axis_index("tensor")
        self.chip = lax.div(me, 2)
        core = lax.rem(me, 2)
        self.mate = self.chip * 2 + (1 - core)
        self.peers = [
            lax.rem(self.chip + shift, self.chips) * 2 + core for shift in range(self.chips)
        ]

    def greet(self):
        barrier = pltpu.get_barrier_semaphore()
        for other in [self.mate] + self.peers[1:]:
            pl.semaphore_signal(
                barrier, inc=1, device_id=(other, self.group), device_id_type=MESH
            )
        pl.semaphore_wait(barrier, self.chips)

    def remote(self, source, target_ref, ssem, rsem, target):
        return pltpu.make_async_remote_copy(
            src_ref=source,
            dst_ref=target_ref,
            send_sem=ssem,
            recv_sem=rsem,
            device_id=(target, self.group),
            device_id_type=MESH,
        )

    def across(self):
        return self.remote(self.x_ref, self.mate_box, self.ms, self.mr, self.mate)

    def copies(self):
        return [
            self.remote(
                self.joined,
                self.boxes.at[self.chip],
                self.ss.at[shift],
                self.sr.at[shift],
                self.peers[shift],
            )
            for shift in range(1, self.chips)
        ]

    def begin(self):
        self.across().start()

    def spread(self):
        self.across().wait_recv()
        self.joined[...] = self.x_ref[...] + self.mate_box[...]
        for copy in self.copies():
            copy.start()
        self.boxes[self.chip] = self.joined[...]

    def finish(self):
        for copy in self.copies():
            copy.wait_recv()
        result = self.boxes[0]
        for other in range(1, self.chips):
            result = result + self.boxes[other]
        self.o_ref[...] = result
        self.across().wait_send()
        for copy in self.copies():
            copy.wait_send()


def total_scratch(values, devices):
    chips = devices // 2
    dma = pltpu.SemaphoreType.DMA
    return [
        pltpu.VMEM(values.shape, F32),
        pltpu.VMEM(values.shape, F32),
        pltpu.VMEM((chips,) + values.shape, F32),
        dma(()),
        dma(()),
        dma((chips,)),
        dma((chips,)),
    ]


def turned_copy(source, target):
    for start in range(0, source.shape[1], LANES):
        target[start : start + LANES, :] = source[:, start : start + LANES].T


def product_kernel(devices, groups, outs, summed, left_ref, right_ref, *refs):
    values = refs[:summed]
    refs = refs[summed:]
    pieces_out, refs = refs[:outs], refs[outs:]
    totals_out, refs = refs[:summed], refs[summed:]
    turned, scratch = refs[0], refs[1:]
    total = None
    if summed:
        scratch, rest = scratch[:-7], scratch[-7:]
        total = Total(devices, values[0], totals_out[0], rest)
    each = len(scratch) // len(groups)
    rings = [
        RingScatter(
            devices, windows, pieces, (turned, right_ref), pieces_out,
            scratch[place * each : (place + 1) * each],
        )
        for place, (windows, pieces) in enumerate(groups)
    ]
    if total is None:
        rings[0].greet()
    else:
        total.greet()
        total.begin()
    for ring in rings:
        ring.locate()
    turned_copy(left_ref, turned)
    run_rings(rings, total.spread if total is not None else None)
    for ring in rings:
        ring.finish()
    if total is not None:
        total.finish()


def scatter_product(left, right, groups, shapes, devices, collective, values=()):
    vmem = pl.BlockSpec(memory_space=pltpu.VMEM)
    rows = left.shape[1] // devices
    scratch = [pltpu.VMEM(left.shape[::-1], BF16)]
    for windows, pieces in groups:
        scratch += scatter_scratch(windows, rows, devices)
    for item in values:
        scratch += total_scratch(item, devices)
    return pl.pallas_call(
        functools.partial(
            product_kernel, devices, groups, len(shapes), len(values)
        ),
        out_shape=tuple(jax.ShapeDtypeStruct(shape, F32) for shape in shapes)
        + tuple(jax.ShapeDtypeStruct(item.shape, F32) for item in values),
        in_specs=[vmem] * (2 + len(values)),
        out_specs=(vmem,) * (len(shapes) + len(values)),
        scratch_shapes=scratch,
        compiler_params=pltpu.CompilerParams(collective_id=collective, has_side_effects=True),
        cost_estimate=cost(3),
        name="scatter_product",
    )(left, right, *values)


def head_spread(channels):
    return (iota((LANES, channels), 1) // MP == iota((LANES, channels), 0)).astype(BF16)


def parts(values, count):
    terms = []
    for _ in range(count):
        term = values.astype(BF16)
        terms.append(term)
        values = values - term.astype(F32)
    return terms


def pick(values, mask, count=2):
    return dot(jnp.concatenate(parts(values, count), axis=1), jnp.concatenate([mask] * count, axis=0))


def pick_left(mask, values, count):
    return dot(jnp.concatenate([mask] * count, axis=1), jnp.concatenate(parts(values, count), axis=0))


def gather_heads(values, spread):
    high, low = parts(values, 2)
    return dot(high, spread, NT) + dot(low, spread, NT)


def row_sums(values):
    high, low = parts(values, 2)
    ones = jnp.ones((EDGE, values.shape[1]), BF16)
    return dot(ones, high, NT) + dot(ones, low, NT)


def soft_step(raw):
    return jnp.maximum(raw, 0.0) + jnp.log1p(jnp.exp(-jnp.abs(raw)))


def conv_window(buffer, taps_ref, bias, span):
    total = bias + taps_ref[0:1, :] * buffer[EDGE - 3 : EDGE - 3 + span, :]
    for tap in range(1, KCONV):
        start = EDGE - 3 + tap
        total = total + taps_ref[tap : tap + 1, :] * buffer[start : start + span, :]
    return total


def span_rates(step_ref, bias, decay, spread, span):
    raw = step_ref[...] + bias
    step = soft_step(raw)
    lower = (iota((span, span), 1) <= iota((span, span), 0)).astype(BF16)
    cum = pick_left(lower, step * decay, 3)
    tails = jnp.exp(cum[span - 1 : span, :] - cum)
    wide = pick(jnp.concatenate([step, tails, jnp.exp(cum)], axis=0), spread)
    return raw, step, cum, wide[:span], wide[span : 2 * span], wide[2 * span :]


def pair_split(values, low_lanes):
    zero = jnp.zeros_like(values)
    return jnp.concatenate(
        [jnp.where(low_lanes, values, zero), jnp.where(low_lanes, zero, values)], axis=0
    )


def pair_decay(cum, cum_rows, pair, causal):
    parts = []
    for head in (2 * pair, 2 * pair + 1):
        differ = cum[:, head : head + 1] - cum_rows[head : head + 1, :]
        parts.append(jnp.exp(jnp.where(causal, differ, MASKED)))
    return parts


def scan_forward(
    devices, spans,
    z_ref, x_ref, bc_ref, step_ref,
    tap_ref, tapb_ref, row_ref, shard_ref,
    y_ref, gated_ref, square_ref, enter_ref, all_ref,
    state, xbuf, bbuf, *sems,
):
    span, channels = x_ref.shape
    ring = RingGather(devices, shard_ref, all_ref, sems)
    turn = pl.program_id(0)

    @pl.when(turn == 0)
    def _():
        ring.greet()
        ring.begin()


    @pl.when(pl.program_id(0) == 0)
    def _():
        state[...] = jnp.zeros_like(state)
        xbuf[span:, :] = jnp.zeros((EDGE, channels), F32)
        bbuf[span:, :] = jnp.zeros((EDGE, 2 * NS), F32)

    xbuf[:EDGE, :] = xbuf[span:, :]
    bbuf[:EDGE, :] = bbuf[span:, :]
    xbuf[EDGE:, :] = x_ref[...]
    bbuf[EDGE:, :] = bc_ref[...]
    spread = head_spread(channels)
    bias, gain, biasb, stepb, decay, skip = unpack_rows(row_ref, spread)
    inputs = jax.nn.silu(conv_window(xbuf, tap_ref, bias, span))
    shared = jax.nn.silu(conv_window(bbuf, tapb_ref, biasb, span))
    raw, step, cum, step_w, tails_w, grown_w = span_rates(step_ref, stepb, decay, spread, span)
    cum_rows = cum.T
    b_low = shared[:, :NS].astype(BF16)
    c_low = shared[:, NS:].astype(BF16)
    scaled = inputs * step_w
    scaled_low = scaled.astype(BF16)
    enter_ref[0] = state[...]
    outer = dot(c_low, state[...].astype(BF16)) * grown_w
    fresh = dot(b_low, (scaled * tails_w).astype(BF16), TN)
    state[...] = state[...] * grown_w[span - 1 : span, :] + fresh
    cross = dot(c_low, b_low, NT)
    causal = iota((span, span), 1) <= iota((span, span), 0)
    low_lanes = iota((span, LANES), 1) < MP
    for pair in range(channels // LANES):
        lanes = slice(pair * LANES, (pair + 1) * LANES)
        first, second = pair_decay(cum, cum_rows, pair, causal)
        weights = jnp.concatenate(
            [(cross * first).astype(BF16), (cross * second).astype(BF16)], axis=1
        )
        y_ref[:, lanes] = dot(weights, pair_split(scaled_low[:, lanes], low_lanes))
    y = y_ref[...] + outer + skip * inputs
    y_ref[...] = y
    gated = y * jax.nn.silu(z_ref[...])
    gated_ref[...] = gated
    square_ref[...] = row_sums(gated * gated)

    count = spans
    for step in range(1, ring.ahead + 1):
        pl.when(turn == min(count - 1, count * step // ring.ahead))(
            functools.partial(ring.hop, step)
        )
    pl.when(turn == count - 1)(ring.finish)


def scan_backward(
    devices, spans, windows, pieces, outs_count, count,
    z_ref, x_ref, xp_ref, bc_ref, bp_ref, step_ref, y_ref, enter_ref,
    dyg_ref, scale_ref, inner_ref, dqkv_ref,
    tap_ref, tapb_ref, row_ref,
    *refs,
):
    sent, refs = refs[:count], refs[count:]
    (grad_ref, gx_ref, gb_ref, gh_ref), refs = refs[:4], refs[4:]
    outs, refs = refs[:outs_count], refs[outs_count:]
    (dstate, xbuf, bbuf, dxbuf, dbbuf, du_buf, col_buf), scratch = refs[:7], refs[7:]
    ring = RingScatter(devices, windows, pieces, sent, outs, scratch)
    span, channels = x_ref.shape
    turn = pl.program_id(0)

    @pl.when(turn == 0)
    def _():
        ring.greet()
        ring.begin()
        dstate[...] = jnp.zeros_like(dstate)
        dxbuf[...] = jnp.zeros_like(dxbuf)
        dbbuf[...] = jnp.zeros_like(dbbuf)
        col_buf[...] = jnp.zeros_like(col_buf)
        gx_ref[...] = jnp.zeros_like(gx_ref)
        gb_ref[...] = jnp.zeros_like(gb_ref)
        gh_ref[...] = jnp.zeros_like(gh_ref)

    inside = (turn < spans - 1).astype(F32)
    xbuf[:EDGE, :] = xp_ref[...] * inside
    bbuf[:EDGE, :] = bp_ref[...] * inside
    xbuf[EDGE:, :] = x_ref[...]
    bbuf[EDGE:, :] = bc_ref[...]
    spread = head_spread(channels)
    bias, gain, biasb, stepb, decay, skip = unpack_rows(row_ref, spread)
    conv = conv_window(xbuf, tap_ref, bias, span)
    sig = jax.nn.sigmoid(conv)
    inputs = conv * sig
    convb = conv_window(bbuf, tapb_ref, biasb, span)
    sigb = jax.nn.sigmoid(convb)
    shared = convb * sigb
    b_low = shared[:, :NS].astype(BF16)
    c_low = shared[:, NS:].astype(BF16)
    raw, step, cum, step_w, tails_w, grown_w = span_rates(step_ref, stepb, decay, spread, span)
    cum_rows = cum.T
    scaled = inputs * step_w
    scaled_low = scaled.astype(BF16)

    z = z_ref[...]
    sig_z = jax.nn.sigmoid(z)
    swish = z * sig_z
    y = y_ref[...]
    scale = scale_ref[...].T[:, :1]
    normed = y * swish * scale
    dyg = dyg_ref[...]
    gain_grad = jnp.sum(dyg * normed, axis=0, keepdims=True)
    dgated = scale * (dyg * gain - normed * inner_ref[...].T[:, :1])
    dy = dgated * swish
    grad_ref[:, :channels] = (dgated * y * (sig_z * (1.0 + z * (1.0 - sig_z)))).astype(BF16)

    state_low = enter_ref[0].astype(BF16)
    dstate_low = dstate[...].astype(BF16)
    grown_low = (dy * grown_w).astype(BF16)
    dy_low = dy.astype(BF16)
    tailed = scaled * tails_w
    outer = dot(c_low, state_low) * grown_w
    from_state = dot(b_low, dstate_low)
    dc = dot(grown_low, state_low, NT)
    db = dot(tailed.astype(BF16), dstate_low, NT)
    leak = from_state * tailed
    last_w = grown_w[span - 1 : span, :]
    ends = (
        jnp.sum(leak, axis=0, keepdims=True)
        + jnp.sum(enter_ref[0] * dstate[...], axis=0, keepdims=True) * last_w
    )
    skips = jnp.sum(dy * inputs, axis=0, keepdims=True)
    dstate[...] = dstate[...] * last_w + dot(c_low, grown_low, TN)

    cross = dot(c_low, b_low, NT)
    causal = iota((span, span), 1) <= iota((span, span), 0)
    low_lanes = iota((span, LANES), 1) < MP
    lane = iota((span, LANES), 1)
    dcross = jnp.zeros((span, span), F32)
    row_part = jnp.zeros((span, LANES), F32)
    for pair in range(channels // LANES):
        lanes = slice(pair * LANES, (pair + 1) * LANES)
        decays = pair_decay(cum, cum_rows, pair, causal)
        dy_pair = pair_split(dy_low[:, lanes], low_lanes)
        dweights = dot(dy_pair, scaled_low[:, lanes], NT)
        both = []
        for part in range(2):
            head = 2 * pair + part
            dterm = dweights[part * span : (part + 1) * span] * decays[part]
            dcross = dcross + dterm
            flow = dterm * cross
            row_part = row_part + jnp.where(
                lane == head, jnp.sum(flow, axis=1, keepdims=True), 0.0
            )
            col_buf[head : head + 1, :] = jnp.sum(flow, axis=0, keepdims=True)
            both.append((cross * decays[part]).astype(BF16))
        du_buf[:, lanes] = dot(jnp.concatenate(both, axis=0), dy_pair, TN)
    du = du_buf[...] + from_state * tails_w
    dcross_low = dcross.astype(BF16)
    dc = dc + dot(dcross_low, b_low)
    db = db + dot(dcross_low, c_low, TN)

    sums = gather_heads(
        jnp.concatenate(
            [dy * outer - leak, du * inputs, ends, skips, jnp.zeros((EDGE - 2, channels), F32)],
            axis=0,
        ),
        spread,
    )
    at_end = sums[2 * span : 2 * span + 1, :]
    dcum = sums[:span] + row_part - col_buf[...].T
    upper = (iota((span, span), 1) >= iota((span, span), 0)).astype(BF16)
    drate = pick_left(upper, dcum, 3) + at_end
    dstep = drate * decay + sums[span : 2 * span]
    draw = dstep * jax.nn.sigmoid(raw)
    gh_ref[0:1, :] += jnp.sum(draw, axis=0, keepdims=True)
    gh_ref[1:2, :] += jnp.sum(drate * step, axis=0, keepdims=True) * decay
    gh_ref[2:3, :] += sums[2 * span + 1 : 2 * span + 2, :]

    dinputs = du * step_w + skip * dy
    dxbuf[span:, :] = dxbuf[:EDGE, :]
    dbbuf[span:, :] = dbbuf[:EDGE, :]
    dconv = dinputs * (sig * (1.0 + conv * (1.0 - sig)))
    dconvb = jnp.concatenate([db, dc], axis=1) * (sigb * (1.0 + convb * (1.0 - sigb)))
    dxbuf[:span, :] = dconv
    dbbuf[:span, :] = dconvb
    dx = jnp.zeros_like(dconv)
    dbc = jnp.zeros_like(dconvb)
    for tap in range(KCONV):
        back = KCONV - 1 - tap
        start = EDGE - 3 + tap
        dx = dx + tap_ref[tap : tap + 1, :] * dxbuf[back : back + span, :]
        dbc = dbc + tapb_ref[tap : tap + 1, :] * dbbuf[back : back + span, :]
        gx_ref[tap : tap + 1, :] += jnp.sum(
            dconv * xbuf[start : start + span, :], axis=0, keepdims=True
        )
        gb_ref[tap : tap + 1, :] += jnp.sum(
            dconvb * bbuf[start : start + span, :], axis=0, keepdims=True
        )
    gx_ref[KCONV : KCONV + 1, :] += jnp.sum(dconv, axis=0, keepdims=True)
    gb_ref[KCONV : KCONV + 1, :] += jnp.sum(dconvb, axis=0, keepdims=True)
    gx_ref[KCONV + 1 : KCONV + 2, :] += gain_grad
    width = 2 * channels + 2 * NS
    grad_ref[:, channels : 2 * channels] = dx.astype(BF16)
    grad_ref[:, 2 * channels : width] = dbc.astype(BF16)
    grad_ref[:, width : width + dqkv_ref.shape[1]] = dqkv_ref[...]
    grad_ref[:, width + dqkv_ref.shape[1] :] = draw.astype(BF16)
    for step in range(ring.ahead):
        pl.when(turn == spans * step // ring.ahead)(functools.partial(ring.hop, step))
    pl.when(turn == spans - 1)(ring.finish)


def scan_params(conv_x, conv_xb, conv_bc, conv_bcb, dt_bias, a_log, d_skip, w_mnorm):
    heads = dt_bias.shape[0]
    fill = jnp.zeros((LANES - heads,), BF16)
    flat = [conv_xb, w_mnorm, conv_bcb, dt_bias, fill, a_log, fill, d_skip, fill]
    size = sum(item.shape[0] for item in flat) // LANES
    flat.append(jnp.zeros((-size % EDGE * LANES,), BF16))
    rows = jnp.concatenate(flat).astype(F32).reshape(-1, LANES)
    return (conv_x.astype(F32), conv_bc.astype(F32), rows)


def unpack_rows(row_ref, spread):
    channels = spread.shape[1]
    count = channels // LANES
    at = 2 * count + 2 * NS // LANES

    def join_rows(first, number):
        return jnp.concatenate(
            [row_ref[i : i + 1, :] for i in range(first, first + number)], axis=1
        )

    skip = jnp.broadcast_to(row_ref[at + 2 : at + 3, :], (EDGE, LANES)).astype(BF16)
    return (
        join_rows(0, count),
        join_rows(count, count),
        join_rows(2 * count, 2 * NS // LANES),
        row_ref[at : at + 1, :],
        -jnp.exp(row_ref[at + 1 : at + 2, :]),
        dot(skip, spread)[:1],
    )


def whole_spec(array):
    return pl.BlockSpec(array.shape, lambda turn: (0,) * array.ndim)


def run_scan_forward(proj, qkv_width, params, shard, devices):
    tokens = proj.shape[0]
    channels = params[0].shape[1]
    step_at = (2 * channels + 2 * NS + qkv_width) // LANES
    spans = tokens // SPAN
    bc_at = 2 * channels // (2 * NS)
    rows = lambda width, at: pl.BlockSpec((SPAN, width), lambda turn: (turn, at))
    anywhere = pl.BlockSpec(memory_space=pl.ANY)
    return pl.pallas_call(
        functools.partial(scan_forward, devices, spans),
        grid=(spans,),
        out_shape=(
            jax.ShapeDtypeStruct((tokens, channels), F32),
            jax.ShapeDtypeStruct((tokens, channels), F32),
            jax.ShapeDtypeStruct((EDGE, tokens), F32),
            jax.ShapeDtypeStruct((spans, NS, channels), F32),
            gather_shape(shard, devices),
        ),
        in_specs=[rows(channels, 0), rows(channels, 1), rows(2 * NS, bc_at), rows(LANES, step_at)]
        + [whole_spec(item) for item in params]
        + [anywhere],
        out_specs=(
            rows(channels, 0),
            rows(channels, 0),
            pl.BlockSpec((EDGE, SPAN), lambda turn: (0, turn)),
            pl.BlockSpec((1, NS, channels), lambda turn: (turn, 0, 0)),
            anywhere,
        ),
        scratch_shapes=[
            pltpu.VMEM((NS, channels), F32),
            pltpu.VMEM((SPAN + EDGE, channels), F32),
            pltpu.VMEM((SPAN + EDGE, 2 * NS), F32),
        ]
        + gather_sems(devices),
        compiler_params=pltpu.CompilerParams(collective_id=2, has_side_effects=True),
        cost_estimate=cost(20),
        name="scan_forward",
    )(proj, proj, proj, proj, *params, shard)


def run_scan_backward(
    proj, y, entering, dyg, scale, inner, dqkv, params, sent, windows, pieces, shapes,
    devices,
):
    tokens, width = proj.shape
    channels = params[0].shape[1]
    qkv_width = dqkv.shape[1]
    step_at = (2 * channels + 2 * NS + qkv_width) // LANES
    spans = tokens // SPAN
    bc_at = 2 * channels // (2 * NS)
    edges = SPAN // EDGE
    rows = lambda size, at: pl.BlockSpec((SPAN, size), lambda turn: (spans - 1 - turn, at))
    edge = lambda size, at: pl.BlockSpec(
        (EDGE, size), lambda turn: (jnp.maximum((spans - 1 - turn) * edges - 1, 0), at)
    )
    keep = lambda shape: pl.BlockSpec(shape, lambda turn: (0, 0))
    shapes = tuple(jax.ShapeDtypeStruct(shape, F32) for shape in shapes)
    return pl.pallas_call(
        functools.partial(
            scan_backward, devices, spans, windows, pieces, len(shapes), len(sent)
        ),
        grid=(spans,),
        out_shape=(
            jax.ShapeDtypeStruct((tokens, width), BF16),
            jax.ShapeDtypeStruct((EDGE, channels), F32),
            jax.ShapeDtypeStruct((EDGE, 2 * NS), F32),
            jax.ShapeDtypeStruct((EDGE, LANES), F32),
        )
        + shapes,
        in_specs=[
            rows(channels, 0),
            rows(channels, 1),
            edge(channels, 1),
            rows(2 * NS, bc_at),
            edge(2 * NS, bc_at),
            rows(LANES, step_at),
            rows(channels, 0),
            pl.BlockSpec((1, NS, channels), lambda turn: (spans - 1 - turn, 0, 0)),
            rows(channels, 0),
            pl.BlockSpec((EDGE, SPAN), lambda turn: (0, spans - 1 - turn)),
            pl.BlockSpec((EDGE, SPAN), lambda turn: (0, spans - 1 - turn)),
            rows(qkv_width, 0),
        ]
        + [whole_spec(item) for item in params]
        + [pl.BlockSpec(memory_space=pl.ANY)] * len(sent),
        out_specs=(
            rows(width, 0),
            keep((EDGE, channels)),
            keep((EDGE, 2 * NS)),
            keep((EDGE, LANES)),
        )
        + tuple(keep(item.shape) for item in shapes),
        scratch_shapes=[
            pltpu.VMEM((NS, channels), F32),
            pltpu.VMEM((SPAN + EDGE, channels), F32),
            pltpu.VMEM((SPAN + EDGE, 2 * NS), F32),
            pltpu.VMEM((SPAN + EDGE, channels), F32),
            pltpu.VMEM((SPAN + EDGE, 2 * NS), F32),
            pltpu.VMEM((SPAN, channels), F32),
            pltpu.VMEM((LANES, SPAN), F32),
        ]
        + scatter_scratch(windows, sent[0].shape[0] // devices, devices),
        compiler_params=pltpu.CompilerParams(collective_id=6, has_side_effects=True),
        cost_estimate=cost(47),
        name="scan_backward",
    )(
        proj, proj, proj, proj, proj, proj, y, entering, dyg, scale, inner, dqkv, *params, *sent,
    )


def rotary_tables(tokens):
    half = HEAD_SIZE // 2
    exponent = np.arange(half, dtype=np.float64) * (-2.0 * LOG_BASE / HEAD_SIZE)
    rates = np.tile(np.exp(exponent.astype(np.float32)).astype(np.float64), LANES // half)
    tables = []
    for places in (np.arange(FINE), np.arange(0, tokens, FINE)):
        angles = places[:, None] * rates[None, :]
        tables += [np.cos(angles).astype(np.float32), np.sin(angles).astype(np.float32)]
    return tables


def fill_rotary(fine_cos, fine_sin, coarse_cos, coarse_sin, cosine, sine):
    small_cos, small_sin = fine_cos[...], fine_sin[...]
    for turn in range(coarse_cos.shape[0]):
        big_cos, big_sin = coarse_cos[turn : turn + 1, :], coarse_sin[turn : turn + 1, :]
        rows = slice(turn * FINE, (turn + 1) * FINE)
        cosine[rows, :] = small_cos * big_cos - small_sin * big_sin
        sine[rows, :] = small_sin * big_cos + small_cos * big_sin


def head_masks():
    half = HEAD_SIZE // 2
    row, col = iota((LANES, LANES), 0), iota((LANES, LANES), 1)
    place = col % HEAD_SIZE
    ahead = jnp.where(place < half, -1.0, 0.0)
    behind = jnp.where(place < half, 0.0, 1.0)

    def turn(start):
        return jnp.where(row == start + half, ahead, jnp.where(row == start - half, behind, 0.0))

    first = row < HEAD_SIZE
    left = col < HEAD_SIZE
    low = lambda mask: mask.astype(BF16)
    within = low(turn(col))
    copy = low(jnp.where(row == place, 1.0, 0.0))
    copy_turn = low(jnp.where(first, turn(place), 0.0))
    value = low(jnp.where(row == place + HEAD_SIZE, 1.0, 0.0))
    fold = low(jnp.where(left & (row % HEAD_SIZE == place), 1.0, 0.0))
    other = row % HEAD_SIZE
    fold_turn = low(
        jnp.where(
            left,
            jnp.where(other == place + half, ahead, jnp.where(other == place - half, behind, 0.0)),
            0.0,
        )
    )
    fold_value = low(jnp.where(left, 0.0, jnp.where(other == place, 1.0, 0.0)))
    return within, copy, copy_turn, value, fold, fold_turn, fold_value


def attend_forward(
    q_ref, kv_ref, fine_cos, fine_sin, coarse_cos, coarse_sin,
    qkv_ref, lse_ref, o_ref, vt, cos_ref, sin_ref,
):
    fill_rotary(fine_cos, fine_sin, coarse_cos, coarse_sin, cos_ref, sin_ref)
    tokens, query_width = q_ref.shape
    pairs = query_width // LANES
    within, copy, copy_turn, value = head_masks()[:4]

    def turn_rows(i, carry):
        rows = pl.ds(pl.multiple_of(i * QBLK, QBLK), QBLK)
        cosine, sine = cos_ref[rows, :], sin_ref[rows, :]
        for pair in range(pairs):
            lanes = slice(pair * LANES, (pair + 1) * LANES)
            query = q_ref[rows, lanes]
            turned = query * cosine + pick(query, within) * sine
            qkv_ref[rows, lanes] = (turned * HEAD_SIZE**-0.5).astype(BF16)
        kv = kv_ref[rows, :]
        keys = pick(kv, copy) * cosine + pick(kv, copy_turn) * sine
        qkv_ref[rows, query_width : query_width + LANES] = keys.astype(BF16)
        qkv_ref[rows, query_width + LANES :] = dot(kv.astype(BF16), value).astype(BF16)
        vt[:, rows] = kv.T[HEAD_SIZE:, :].astype(BF16)
        return carry

    lax.fori_loop(0, tokens // QBLK, turn_rows, 0)
    low_lanes = iota((QBLK, LANES), 1) < HEAD_SIZE
    wide = (QBLK, 2 * QBLK)
    visible = iota(wide, 0) <= iota(wide, 1) % QBLK

    def block(i, carry):
        here = pl.ds(pl.multiple_of(i * QBLK, QBLK), QBLK)
        queries = [
            pair_split(qkv_ref[here, pair * LANES : (pair + 1) * LANES], low_lanes)
            for pair in range(pairs)
        ]

        def tile(there, state, edge):
            keys = qkv_ref[there, query_width : query_width + LANES]
            result = []
            for pair in range(pairs):
                top, total, out = state[3 * pair : 3 * pair + 3]
                scores = dot(keys, queries[pair], NT)
                if edge:
                    scores = jnp.where(visible, scores, MASKED)
                higher = jnp.maximum(top, jnp.max(scores, axis=0, keepdims=True))
                probs = jnp.exp(scores - higher)
                fade = jnp.exp(top - higher)
                total = total * fade + jnp.sum(probs, axis=0, keepdims=True)
                out = out * fade + dot(vt[:, there], probs.astype(BF16))
                result += [higher, total, out]
            return tuple(result)

        state = (
            jnp.full((1, 2 * QBLK), MASKED, F32),
            jnp.zeros((1, 2 * QBLK), F32),
            jnp.zeros((HEAD_SIZE, 2 * QBLK), F32),
        ) * pairs
        state = lax.fori_loop(
            0,
            i,
            lambda j, state: tile(pl.ds(pl.multiple_of(j * QBLK, QBLK), QBLK), state, False),
            state,
        )
        state = tile(here, state, True)
        for pair in range(pairs):
            top, total, out = state[3 * pair : 3 * pair + 3]
            out = out / total
            lse = top + jnp.log(total)
            lse_ref[2 * pair : 2 * pair + 1, here] = lse[:, :QBLK]
            lse_ref[2 * pair + 1 : 2 * pair + 2, here] = lse[:, QBLK:]
            both = jnp.concatenate([out[:, :QBLK], out[:, QBLK:]], axis=0)
            o_ref[here, pair * LANES : (pair + 1) * LANES] = both.T.astype(BF16)
        return carry

    lax.fori_loop(0, tokens // QBLK, block, 0)


def attend_backward(
    qkv_ref, lse_ref, o_ref, do_ref, fine_cos, fine_sin, coarse_cos, coarse_sin,
    dqkv_ref,
    dq, kt, dk, dv, cos_ref, sin_ref,
):
    fill_rotary(fine_cos, fine_sin, coarse_cos, coarse_sin, cos_ref, sin_ref)
    tokens, query_width = o_ref.shape
    pairs = query_width // LANES
    key_lanes = slice(query_width, query_width + LANES)
    value_lanes = slice(query_width + LANES, query_width + 2 * LANES)

    def turn_keys(i, carry):
        rows = pl.ds(pl.multiple_of(i * QBLK, QBLK), QBLK)
        kt[:, rows] = qkv_ref[rows, key_lanes].astype(F32).T[:HEAD_SIZE, :].astype(BF16)
        return carry

    lax.fori_loop(0, tokens // QBLK, turn_keys, 0)
    dk[...] = jnp.zeros_like(dk)
    dv[...] = jnp.zeros_like(dv)
    low_lanes = iota((QBLK, LANES), 1) < HEAD_SIZE
    wide = (QBLK, 2 * QBLK)
    visible = iota(wide, 0) <= iota(wide, 1) % QBLK
    ones = jnp.ones((EDGE, LANES), BF16)

    def block(i, carry):
        here = pl.ds(pl.multiple_of(i * QBLK, QBLK), QBLK)
        queries, grads, inners, lses = [], [], [], []
        for pair in range(pairs):
            lanes = slice(pair * LANES, (pair + 1) * LANES)
            queries.append(pair_split(qkv_ref[here, lanes], low_lanes))
            grad = do_ref[here, lanes]
            grads.append(pair_split(grad, low_lanes))
            both = pair_split(grad.astype(F32) * o_ref[here, lanes].astype(F32), low_lanes)
            high, low = parts(both, 2)
            inners.append((dot(ones, high, NT) + dot(ones, low, NT))[:1])
            lses.append(
                jnp.concatenate(
                    [
                        lse_ref[2 * pair : 2 * pair + 1, here],
                        lse_ref[2 * pair + 1 : 2 * pair + 2, here],
                    ],
                    axis=1,
                )
            )
        query_all = jnp.concatenate(queries, axis=0)
        grad_all = jnp.concatenate(grads, axis=0)

        def tile(there, state, edge):
            keys = qkv_ref[there, key_lanes]
            values = qkv_ref[there, value_lanes]
            all_probs, all_dscores, result = [], [], []
            for pair in range(pairs):
                probs = dot(keys, queries[pair], NT) - lses[pair]
                if edge:
                    probs = jnp.where(visible, probs, MASKED)
                probs = jnp.exp(probs)
                dprobs = dot(values, grads[pair], NT)
                dscores = (probs * (dprobs - inners[pair])).astype(BF16)
                all_probs.append(probs.astype(BF16))
                all_dscores.append(dscores)
                result.append(state[pair] + dot(kt[:, there], dscores))
            dv[there, :] += dot(jnp.concatenate(all_probs, axis=1), grad_all)
            dk[there, :] += dot(jnp.concatenate(all_dscores, axis=1), query_all)
            return tuple(result)

        state = (jnp.zeros((HEAD_SIZE, 2 * QBLK), F32),) * pairs
        state = lax.fori_loop(
            0,
            i,
            lambda j, state: tile(pl.ds(pl.multiple_of(j * QBLK, QBLK), QBLK), state, False),
            state,
        )
        state = tile(here, state, True)
        for pair in range(pairs):
            both = jnp.concatenate([state[pair][:, :QBLK], state[pair][:, QBLK:]], axis=0)
            dq[here, pair * LANES : (pair + 1) * LANES] = both.T
        return carry

    lax.fori_loop(0, tokens // QBLK, block, 0)
    masks = head_masks()
    within, (fold, fold_turn, fold_value) = masks[0], masks[4:]

    def turn_back(i, carry):
        rows = pl.ds(pl.multiple_of(i * QBLK, QBLK), QBLK)
        cosine, sine = cos_ref[rows, :], sin_ref[rows, :]
        for pair in range(pairs):
            lanes = slice(pair * LANES, (pair + 1) * LANES)
            grad = dq[rows, lanes]
            grad = grad * cosine - pick(grad, within) * sine
            dqkv_ref[rows, lanes] = (grad * HEAD_SIZE**-0.5).astype(BF16)
        grad = dk[rows, :]
        grad = pick(grad, fold) * cosine - pick(grad, fold_turn) * sine
        grad = grad + pick(dv[rows, :], fold_value)
        dqkv_ref[rows, query_width:] = grad.astype(BF16)
        return carry

    lax.fori_loop(0, tokens // QBLK, turn_back, 0)


def run_attend_forward(proj, query_at, query_width, tables):
    tokens = proj.shape[0]
    cols = lambda size, at: pl.BlockSpec((tokens, size), lambda turn: (0, at // size))
    return pl.pallas_call(
        attend_forward,
        grid=(1,),
        out_shape=(
            jax.ShapeDtypeStruct((tokens, query_width + 2 * LANES), BF16),
            jax.ShapeDtypeStruct((EDGE, tokens), F32),
            jax.ShapeDtypeStruct((tokens, query_width), BF16),
        ),
        in_specs=[
            cols(query_width, query_at),
            cols(2 * HEAD_SIZE, query_at + query_width),
        ]
        + [whole_spec(table) for table in tables],
        out_specs=(
            cols(query_width + 2 * LANES, 0),
            pl.BlockSpec((EDGE, tokens), lambda turn: (0, 0)),
            cols(query_width, 0),
        ),
        scratch_shapes=[
            pltpu.VMEM((HEAD_SIZE, tokens), BF16),
            pltpu.VMEM((tokens, LANES), F32),
            pltpu.VMEM((tokens, LANES), F32),
        ],
        cost_estimate=cost(15),
        name="attend_forward",
    )(proj, proj, *tables)


def run_attend_backward(qkv, lse, attended, grads, grad_at, tables):
    tokens, query_width = attended.shape
    vmem = pl.BlockSpec(memory_space=pltpu.VMEM)
    cols = lambda size, at: pl.BlockSpec((tokens, size), lambda turn: (0, at // size))
    return pl.pallas_call(
        attend_backward,
        grid=(1,),
        out_shape=jax.ShapeDtypeStruct((tokens, query_width + 2 * HEAD_SIZE), BF16),
        in_specs=[
            whole_spec(qkv),
            whole_spec(lse),
            whole_spec(attended),
            cols(query_width, grad_at),
        ]
        + [whole_spec(table) for table in tables],
        out_specs=cols(query_width + 2 * HEAD_SIZE, 0),
        scratch_shapes=[
            pltpu.VMEM((tokens, query_width), F32),
            pltpu.VMEM((HEAD_SIZE, tokens), BF16),
            pltpu.VMEM((tokens, LANES), F32),
            pltpu.VMEM((tokens, LANES), F32),
            pltpu.VMEM((tokens, LANES), F32),
            pltpu.VMEM((tokens, LANES), F32),
        ],
        cost_estimate=cost(16),
        name="attend_backward",
    )(qkv, lse, attended, grads, *tables)


def feed_forward(
    x_ref, mixed_ref, other_ref, top_ref, gain_ref, gu_ref, down_ref,
    after_ref, scale_ref, hidden_ref, act_ref, dgu_ref, part_ref, back_ref,
):
    units = down_ref.shape[1]
    after = x_ref[...].astype(F32) + (mixed_ref[...].astype(F32) + other_ref[...].astype(F32))
    after_ref[...] = after
    scale = lax.rsqrt(jnp.mean(after * after, axis=-1, keepdims=True) + EPSILON)
    scale_ref[...] = scale
    hidden = (after * scale * gain_ref[...]).astype(BF16)
    hidden_ref[...] = hidden
    top = top_ref[...]
    for start in range(0, units, UBLK):
        cols = slice(start, start + UBLK)
        up_cols = slice(units + start, units + start + UBLK)
        gate = dot(hidden, gu_ref[:, cols])
        upward = dot(hidden, gu_ref[:, up_cols])
        grad = dot(top, down_ref[:, cols])
        sigma = jax.nn.sigmoid(gate)
        swish = gate * sigma
        act_ref[:, cols] = (swish * upward).astype(BF16)
        slope = sigma * (1.0 + gate * (1.0 - sigma))
        dgu_ref[:, cols] = (grad * upward * slope).astype(BF16)
        dgu_ref[:, up_cols] = (grad * swish).astype(BF16)
    back_ref[...] = dot(dgu_ref[...], gu_ref[...], NT).astype(BF16)
    part_ref[...] = dot(act_ref[...], down_ref[...], NT).astype(BF16)


def once(item):
    return pl.BlockSpec(item.shape, lambda turn: (0,) * item.ndim, pipeline_mode=pl.Buffered(1))


def run_feed_forward(x, mixed, other, top, gain, w_gate_up, w_down_t):
    tokens, width = x.shape
    units = w_down_t.shape[1]
    rows = lambda size: pl.BlockSpec((TBLK, size), lambda turn: (turn, 0))
    shape = jax.ShapeDtypeStruct
    return pl.pallas_call(
        feed_forward,
        grid=(tokens // TBLK,),
        out_shape=(
            shape((tokens, width), F32),
            shape((tokens, 1), F32),
            shape((tokens, width), BF16),
            shape((tokens, units), BF16),
            shape((tokens, 2 * units), BF16),
            shape((tokens, width), BF16),
            shape((tokens, width), BF16),
        ),
        in_specs=[rows(width)] * 4 + [once(gain), once(w_gate_up), once(w_down_t)],
        out_specs=(
            rows(width), rows(1), rows(width), rows(units), rows(2 * units), rows(width),
            rows(width),
        ),
        cost_estimate=cost(20),
        name="feed_forward",
    )(x, mixed, other, top, gain, w_gate_up, w_down_t)


def mixer_forward(gated_ref, scale_ref, gain_ref, attended_ref, w_ref, low_ref, mixed_ref):
    channels = gated_ref.shape[1]
    scale = scale_ref[...].T[:, :1]
    low_ref[:, :channels] = (gated_ref[...] * scale * gain_ref[...]).astype(BF16)
    low_ref[:, channels:] = attended_ref[...]
    mixed_ref[...] = dot(low_ref[...], w_ref[...], NT).astype(BF16)


def run_mixer_forward(gated, scale, gain, attended, w_out):
    tokens, channels = gated.shape
    width, inner = w_out.shape
    rows = lambda size: pl.BlockSpec((TBLK, size), lambda turn: (turn, 0))
    return pl.pallas_call(
        mixer_forward,
        grid=(tokens // TBLK,),
        out_shape=(
            jax.ShapeDtypeStruct((tokens, inner), BF16),
            jax.ShapeDtypeStruct((tokens, width), BF16),
        ),
        in_specs=[
            rows(channels),
            pl.BlockSpec((EDGE, TBLK), lambda turn: (0, turn)),
            once(gain),
            rows(attended.shape[1]),
            once(w_out),
        ],
        out_specs=(rows(inner), rows(width)),
        cost_estimate=cost(5),
        name="mixer_forward",
    )(gated, scale, gain, attended, w_out)


def mixer_backward(
    part_ref, other_ref, after_ref, scale_ref, top_ref, gain_ref,
    w_ref, gated_ref, scale_m_ref, gain_m_ref,
    grad_ref, low_ref, mamba_ref, attended_ref, inner_ref, gain_grad_ref,
):
    channels = gated_ref.shape[1]

    @pl.when(pl.program_id(0) == 0)
    def _():
        gain_grad_ref[...] = jnp.zeros_like(gain_grad_ref)

    grad = part_ref[...].astype(F32) + other_ref[...].astype(F32)
    scale = scale_ref[...]
    normed = after_ref[...] * scale
    gain_grad_ref[:1, :] += jnp.sum(grad * normed, axis=0, keepdims=True)
    weighted = grad * gain_ref[...]
    mean = jnp.mean(weighted * normed, axis=-1, keepdims=True)
    total = top_ref[...].astype(F32) + scale * (weighted - normed * mean)
    grad_ref[...] = total
    low_ref[...] = total.astype(BF16)
    back = dot(low_ref[...], w_ref[...])
    mamba = back[:, :channels]
    mamba_ref[...] = mamba
    attended_ref[...] = back[:, channels:].astype(BF16)
    inner_ref[...] = row_sums(mamba * gain_m_ref[...] * gated_ref[...]) * scale_m_ref[...]


def run_mixer_backward(part, other, after, scale, top, gain, w_out, gated, scale_m, gain_m):
    tokens, width = after.shape
    channels = gated.shape[1]
    inner = w_out.shape[1]
    shape = jax.ShapeDtypeStruct
    rows = lambda size: pl.BlockSpec((NBLK, size), lambda turn: (turn, 0))
    lanes = pl.BlockSpec((EDGE, NBLK), lambda turn: (0, turn))
    return pl.pallas_call(
        mixer_backward,
        grid=(tokens // NBLK,),
        out_shape=(
            shape((tokens, width), F32),
            shape((tokens, width), BF16),
            shape((tokens, channels), F32),
            shape((tokens, inner - channels), BF16),
            shape((EDGE, tokens), F32),
            shape((EDGE, width), F32),
        ),
        in_specs=[rows(width)] * 3
        + [rows(1), rows(width), once(gain), once(w_out), rows(channels), lanes, once(gain_m)],
        out_specs=(
            rows(width), rows(width), rows(channels), rows(inner - channels), lanes,
            pl.BlockSpec((EDGE, width), lambda turn: (0, 0)),
        ),
        cost_estimate=cost(8),
        name="mixer_backward",
    )(part, other, after, scale, top, gain, w_out, gated, scale_m, gain_m)


def finish_layer(
    x_ref, gain_ref, part_ref, other_ref, grad_ref, after_ref, ffn_ref, ffn_other_ref, *refs,
):
    count = len(refs) // 2 - 1
    passed, out_ref, result_ref, handed = refs[:count], refs[count], refs[count + 1], refs[count + 2 :]

    @pl.when(pl.program_id(0) == 0)
    def _():
        for source, target in zip(passed, handed):
            target[...] = source[...]

    x = x_ref[...].astype(F32)
    scale = lax.rsqrt(jnp.mean(x * x, axis=-1, keepdims=True) + EPSILON)
    normed = x * scale
    weighted = (part_ref[...].astype(F32) + other_ref[...].astype(F32)) * gain_ref[...]
    mean = jnp.mean(weighted * normed, axis=-1, keepdims=True)
    out_ref[...] = grad_ref[...] + scale * (weighted - normed * mean)
    ffn = ffn_ref[...].astype(F32) + ffn_other_ref[...].astype(F32)
    result_ref[...] = (after_ref[...] + ffn).astype(BF16)


def run_finish(x, gain, part, other, grad, after, ffn, ffn_other, passed):
    tokens, width = x.shape
    rows = pl.BlockSpec((TBLK, width), lambda turn: (turn, 0))
    return pl.pallas_call(
        finish_layer,
        grid=(tokens // TBLK,),
        out_shape=(
            jax.ShapeDtypeStruct((tokens, width), F32),
            jax.ShapeDtypeStruct((tokens, width), BF16),
        )
        + tuple(jax.ShapeDtypeStruct(item.shape, F32) for item in passed),
        in_specs=[rows, once(gain)] + [rows] * 6 + [once(item) for item in passed],
        out_specs=(rows, rows) + tuple(once(item) for item in passed),
        cost_estimate=cost(8),
        name="finish_layer",
    )(x, gain, part, other, grad, after, ffn, ffn_other, *passed)


def swap(partial):
    return lax.ppermute(partial, "tensor", [(0, 1), (1, 0)])


def join(mine, other):
    return mine.astype(F32) + other.astype(F32)


def tensor_sum(partial):
    return join(partial, swap(partial))


def thirds(size):
    part = size // 3
    return [(0, part), (part, 2 * part), (2 * part, size)]


def local(
    layer_input, w_norm1, w_zx, w_bc, w_dt, conv_x, conv_xb, conv_bc, conv_bcb, dt_bias, a_log,
    d_skip, w_mnorm, w_mout, query_key_value_weight, output_weight, w_norm2, w_gu, w_down,
    grad_output,
):
    devices = lax.axis_size("dp")
    tokens, width = layer_input.shape
    shard = w_zx.shape[0]
    channels = conv_xb.shape[0]
    heads = dt_bias.shape[0]
    qkv_width = query_key_value_weight.shape[2]
    units = w_down.shape[0]
    attn_width = output_weight.shape[1]
    tail = jnp.concatenate(
        [w_dt, w_norm1[:, None], w_norm2[:, None], jnp.zeros((shard, LANES - heads - 2), BF16)],
        axis=1,
    )
    mixer_in = jnp.concatenate(
        [w_zx.reshape(shard, -1), w_bc, query_key_value_weight.reshape(shard, -1), tail], axis=1
    )
    in_width = mixer_in.shape[1]
    (w_in,) = gather_rows([mixer_in], devices, 0, [(0, *window) for window in thirds(in_width)])
    norm1 = w_in[:, in_width - LANES + heads].astype(F32)
    norm2 = w_in[:, in_width - LANES + heads + 1].astype(F32)

    source = layer_input.astype(F32)
    scale_one = lax.rsqrt(jnp.mean(source * source, axis=-1, keepdims=True) + EPSILON)
    normed_one = source * scale_one
    hidden_one = lax.optimization_barrier((normed_one * norm1).astype(BF16))
    proj = dot(hidden_one, w_in)
    params = scan_params(
        conv_x, conv_xb, conv_bc, conv_bcb, dt_bias, a_log, d_skip, w_mnorm
    )
    out_shard = jnp.concatenate([w_mout.T, output_weight.reshape(attn_width, -1).T], axis=1)
    y, gated, square_sum, entering, w_out = run_scan_forward(
        proj, qkv_width, params, out_shard, devices
    )
    channels_all = channels * lax.axis_size("tensor")
    scale_m = lax.rsqrt(tensor_sum(square_sum) / channels_all + EPSILON)
    tables = rotary_tables(tokens)
    qkv_at = 2 * channels + 2 * NS
    qkv, lse, attended = run_attend_forward(proj, qkv_at, attn_width, tables)
    gain_m = w_mnorm.astype(F32)[None, :]
    mixer_out, mixed = run_mixer_forward(gated, scale_m, gain_m, attended, w_out)
    mixed, gate_up_shard, down_shard = lax.optimization_barrier(
        (mixed, w_gu.reshape(shard, -1), w_down.T)
    )
    other = swap(mixed)
    w_gate_up, w_down_t = gather_rows(
        [gate_up_shard, down_shard],
        devices,
        3,
        [(0, 0, units), (0, units, 2 * units), (1, 0, units)],
    )
    other, w_gate_up, w_down_t = lax.optimization_barrier((other, w_gate_up, w_down_t))
    after, scale_two, hidden_two, activated, grad_gu_low, ffn_part, partial_two = run_feed_forward(
        layer_input, mixed, other, grad_output, norm2[None, :], w_gate_up, w_down_t
    )
    other = swap(partial_two)
    grad_down = dot(grad_output, activated, TN).astype(BF16)
    (mine_gu,) = scatter_product(
        hidden_two,
        grad_gu_low,
        [
            ([(0, 1, 0, units)], [(0, 0, units, 0, 0)]),
            ([(0, 1, units, 2 * units)], [(0, 0, units, 0, 1)]),
        ],
        [(shard, 2, units)],
        devices,
        1,
    )
    other, mine_gu, grad_down, ffn_part = lax.optimization_barrier(
        (other, mine_gu, grad_down, ffn_part)
    )
    ffn_other = swap(ffn_part)
    grad_after, grad_mix_low, grad_mamba, grad_attended, inner_m, grad_norm2 = run_mixer_backward(
        partial_two, other, after, scale_two, grad_output, norm2[None, :], w_out, gated, scale_m,
        gain_m,
    )
    inner_m = tensor_sum(inner_m) / channels_all
    dqkv = run_attend_backward(qkv, lse, attended, grad_attended, 0, tables)
    grad_out = dot(grad_mix_low, mixer_out, TN).astype(BF16)
    windows = [(0, None, 0, channels + attn_width), (1, None, 0, units)]
    pieces = [
        (0, 0, channels, 0, None),
        (0, channels, channels + attn_width, 1, None),
        (1, 0, units, 2, None),
    ]
    shapes = [(shard, channels), (shard, attn_width), (shard, units)]
    grad_proj, small_x, small_b, small_h, mine_mout, mine_o, mine_down = run_scan_backward(
        proj, y, entering, grad_mamba, scale_m, inner_m, dqkv, params,
        [grad_out, grad_down], windows, pieces, shapes, devices,
    )
    ffn_other, grad_proj = lax.optimization_barrier((ffn_other, grad_proj))
    partial_one, grad_proj = lax.optimization_barrier(
        (dot(grad_proj, w_in, NT).astype(BF16), grad_proj)
    )
    other = swap(partial_one)
    grad_norm1 = jnp.sum(partial_one.astype(F32) * normed_one, axis=0)
    small = jnp.concatenate(
        [
            small_x[: KCONV + 2].reshape(-1, LANES),
            small_h[:3],
            grad_norm2[0].reshape(-1, LANES),
            small_b[: KCONV + 1].reshape(-1, LANES),
            grad_norm1.reshape(-1, LANES),
        ],
        axis=0,
    )
    small_rows = small.shape[0]
    cross_rows = (KCONV + 1) * 2 * NS // LANES + width // LANES
    cross_at = small_rows - cross_rows
    small = jnp.pad(small, ((0, -small_rows % EDGE), (0, 0)))
    shared_at = 2 * channels
    step_at = qkv_at + qkv_width
    mine_zx, mine_bc, mine_qkv, mine_step, small = scatter_product(
        hidden_one,
        grad_proj,
        [
            ([(0, 1, 0, channels)], [(0, 0, channels, 0, 0)]),
            ([(0, 1, channels, shared_at)], [(0, 0, channels, 0, 1)]),
            (
                [(0, 1, shared_at, in_width)],
                [
                    (0, 0, 2 * NS, 1, None),
                    (0, 2 * NS, 2 * NS + qkv_width, 2, 0),
                    (0, 2 * NS + qkv_width, in_width - shared_at, 3, "turned"),
                ],
            ),
        ],
        [
            (shard, 2, channels),
            (shard, 2 * NS),
            (shard, 1, qkv_width),
            (heads, shard),
        ],
        devices,
        5,
        (small,),
    )
    other, mine_bc = lax.optimization_barrier((other, mine_bc))
    crossing = tensor_sum(small[cross_at : cross_at + cross_rows])
    shared_cols = tensor_sum(mine_bc)
    passed = (mine_zx, mine_qkv, mine_step, mine_mout, mine_o, mine_gu, mine_down)
    grad_source, result, *passed = run_finish(
        layer_input, norm1[None, :], partial_one, other, grad_after, after, ffn_part, ffn_other,
        passed,
    )
    mine_zx, mine_qkv, mine_step, mine_mout, mine_o, mine_gu, mine_down = passed

    half = NS * 2 // lax.axis_size("tensor")
    begin = lax.axis_index("tensor") * half
    grad_bc = lax.dynamic_slice_in_dim(shared_cols, begin, half, 1)
    x_rows = (KCONV + 2) * channels // LANES
    norm_rows = width // LANES
    total_x = small[:x_rows].reshape(KCONV + 2, channels)
    total_h = small[x_rows : x_rows + 3]
    norm2_total = small[x_rows + 3 : cross_at].reshape(width)
    total_b = crossing[: cross_rows - norm_rows].reshape(KCONV + 1, 2 * NS)
    total_b = lax.dynamic_slice_in_dim(total_b, begin, half, 1)
    norm1_total = crossing[cross_rows - norm_rows :].reshape(width)
    norms = [
        lax.dynamic_slice_in_dim(item, lax.axis_index("dp") * shard, shard, 0)
        for item in (norm1_total, norm2_total)
    ]
    return (
        result,
        grad_source,
        norms[0],
        mine_zx,
        grad_bc,
        mine_step.T,
        total_x[:KCONV],
        total_x[KCONV],
        total_b[:KCONV],
        total_b[KCONV],
        total_h[0, :heads],
        total_h[1, :heads],
        total_h[2, :heads],
        total_x[KCONV + 1],
        mine_mout.T,
        mine_qkv,
        mine_o.T.reshape(output_weight.shape),
        norms[1],
        mine_gu,
        mine_down.T,
    )


def solution(mesh):
    return jax.shard_map(
        local,
        mesh=mesh,
        in_specs=(
            P("dp", None),
            P("dp"),
            P("dp", None, "tensor"),
            P("dp", None),
            P("dp", "tensor"),
            P(None, "tensor"),
            P("tensor"),
            P(),
            P(),
            P("tensor"),
            P("tensor"),
            P("tensor"),
            P("tensor"),
            P("tensor", "dp"),
            P("dp", "tensor", None),
            P("tensor", None, "dp"),
            P("dp"),
            P("dp", None, "tensor"),
            P("tensor", "dp"),
            P("dp", None),
        ),
        out_specs=(
            P("dp", None),
            P("dp", None),
            P("dp"),
            P("dp", None, "tensor"),
            P("dp", "tensor"),
            P("dp", "tensor"),
            P(None, "tensor"),
            P("tensor"),
            P(None, "tensor"),
            P("tensor"),
            P("tensor"),
            P("tensor"),
            P("tensor"),
            P("tensor"),
            P("tensor", "dp"),
            P("dp", "tensor", None),
            P("tensor", None, "dp"),
            P("dp"),
            P("dp", None, "tensor"),
            P("tensor", "dp"),
        ),
        check_vma=False,
    )
```

```python
import functools
import math

import jax
import jax.numpy as jnp
import numpy as np
from jax import lax
from jax.experimental import pallas as pl
from jax.experimental.pallas import tpu as pltpu
from jax.sharding import PartitionSpec as P

HEAD_SIZE = 64
MP = 64
NS = 128
KCONV = 4
SPAN = 128
QBLK = 256
FINE = 32
TBLK = 256
NBLK = 128
UBLK = 256
LANES = 128
EDGE = 8

EPSILON = 1e-05
HIGHEST = lax.Precision.HIGHEST
LOG_BASE = math.log(100000000000.0)
MASKED = -1e30
MESH = pl.DeviceIdType.MESH
F32 = jnp.float32
BF16 = jnp.bfloat16

NN = ((1,), (0,))
NT = ((1,), (1,))
TN = ((0,), (0,))


def dot(left, right, dims=NN, precision=None):
    return lax.dot_general(
        left, right, (dims, ((), ())), preferred_element_type=F32, precision=precision
    )


def iota(shape, dim):
    return lax.broadcasted_iota(jnp.int32, shape, dim)


def ring_place(chip, chips):
    odd = lax.rem(chip, 2)
    half = lax.div(chip, 2)
    return (1 - odd) * half + odd * (chips - 1 - half)


def ring_chip(place, chips):
    place = lax.rem(place + 4 * chips, chips)
    back = lax.div(place, chips // 2)
    return (1 - back) * (2 * place) + back * (2 * (chips - 1 - place) + 1)


def ring_setup(chips):
    me = lax.axis_index("dp")
    group = lax.axis_index("tensor")
    chip = lax.div(me, 2)
    core = lax.rem(me, 2)
    place = ring_place(chip, chips)
    right = ring_chip(place + 1, chips) * 2 + core
    left = ring_chip(place - 1, chips) * 2 + core
    mate = chip * 2 + (1 - core)
    barrier = pltpu.get_barrier_semaphore()
    for other in (right, left, mate):
        pl.semaphore_signal(barrier, inc=1, device_id=(other, group), device_id_type=MESH)
    pl.semaphore_wait(barrier, 3)
    return me, group, core, place, right, left, mate


class RingGather:
    def __init__(self, devices, x_ref, o_ref, sems, cols=slice(None)):
        self.cols = cols
        self.chips = devices // 2
        self.ahead = self.chips // 2
        self.behind = self.chips - 1 - self.ahead
        self.x_ref, self.o_ref, self.rows = x_ref, o_ref, x_ref.shape[0]
        self.fs, self.fr, self.bs, self.br, self.cs, self.cr, self.own_sem = sems

    def locate(self):
        me = lax.axis_index("dp")
        self.group = lax.axis_index("tensor")
        self.core = lax.rem(me, 2)
        chip = lax.div(me, 2)
        self.place = ring_place(chip, self.chips)
        self.right = ring_chip(self.place + 1, self.chips) * 2 + self.core
        self.left = ring_chip(self.place - 1, self.chips) * 2 + self.core
        self.mate = chip * 2 + (1 - self.core)
        self.me = me

    def slot(self, index):
        rows = pl.ds(pl.multiple_of(index * self.rows, self.rows), self.rows)
        return self.o_ref.at[rows, self.cols]

    def copy(self, shift, ssem, rsem, target):
        if shift == 0:
            index, source = self.me, self.x_ref.at[:, self.cols]
        else:
            index = ring_chip(self.place + shift, self.chips) * 2 + self.core
            source = self.slot(index)
        return pltpu.make_async_remote_copy(
            src_ref=source,
            dst_ref=self.slot(index),
            send_sem=ssem,
            recv_sem=rsem,
            device_id=(target, self.group),
            device_id_type=MESH,
        )

    def fore(self, step):
        return self.copy(-step, self.fs.at[step], self.fr.at[step], self.right)

    def back(self, step):
        return self.copy(step, self.bs.at[step], self.br.at[step], self.left)

    def across(self, shift):
        number = 0 if shift == 0 else 2 * abs(shift) - (1 if shift < 0 else 0)
        return self.copy(shift, self.cs.at[number], self.cr.at[number], self.mate)

    def own(self):
        return pltpu.make_async_copy(
            self.x_ref.at[:, self.cols], self.slot(self.me), self.own_sem
        )

    def greet(self):
        self.locate()
        barrier = pltpu.get_barrier_semaphore()
        for other in (self.right, self.left, self.mate):
            pl.semaphore_signal(
                barrier, inc=1, device_id=(other, self.group), device_id_type=MESH
            )
        pl.semaphore_wait(barrier, 3)

    def begin(self):
        self.locate()
        self.fore(0).start()
        self.back(0).start()
        self.across(0).start()
        self.own().start()

    def hop(self, step):
        self.locate()
        self.fore(step - 1).wait_recv()
        if step < self.ahead:
            self.fore(step).start()
        self.across(-step).start()
        if step <= self.behind:
            self.back(step - 1).wait_recv()
            if step < self.behind:
                self.back(step).start()
            self.across(step).start()

    def finish(self):
        self.locate()
        self.own().wait()
        for step in range(self.ahead):
            self.fore(step).wait_send()
        for step in range(self.behind):
            self.back(step).wait_send()
        for shift in range(-self.ahead, self.behind + 1):
            self.across(shift).wait()


def gather_sems(devices):
    dma = pltpu.SemaphoreType.DMA
    return [dma((devices // 2,))] * 6 + [dma(())]


def gather_shape(shard, devices):
    return jax.ShapeDtypeStruct((shard.shape[0] * devices, shard.shape[1]), shard.dtype)


def gather_kernel(devices, count, windows, *refs):
    shards, outs, sems = refs[:count], refs[count : 2 * count], refs[2 * count :]
    each = len(sems) // len(windows)
    rings = [
        RingGather(
            devices, shards[i], outs[i], sems[place * each : (place + 1) * each], slice(first, last)
        )
        for place, (i, first, last) in enumerate(windows)
    ]
    rings[0].greet()
    for ring in rings:
        ring.begin()
    for step in range(1, rings[0].ahead + 1):
        for ring in rings:
            ring.hop(step)
    for ring in rings:
        ring.finish()


def cost(micros):
    return pl.CostEstimate(flops=int(micros * 1e9), bytes_accessed=0, transcendentals=0)


def gather_rows(shards, devices, collective, windows):
    count = len(shards)
    anywhere = pl.BlockSpec(memory_space=pl.ANY)
    return pl.pallas_call(
        functools.partial(gather_kernel, devices, count, windows),
        out_shape=tuple(gather_shape(shard, devices) for shard in shards),
        in_specs=[anywhere] * count,
        out_specs=(anywhere,) * count,
        scratch_shapes=gather_sems(devices) * len(windows),
        compiler_params=pltpu.CompilerParams(collective_id=collective, has_side_effects=True),
        cost_estimate=cost(3),
        name="gather_rows",
    )(*shards)


def scatter_order(chips):
    ahead = chips // 2
    behind = chips - 1 - ahead
    order = []
    for step in range(ahead):
        order.append(-(ahead - step))
        if step < behind:
            order.append(behind - step)
    order.append(0)
    return order


class RingScatter:
    def __init__(self, devices, windows, pieces, operands, outs, scratch):
        self.chips = devices // 2
        self.ahead = self.chips // 2
        self.behind = self.chips - 1 - self.ahead
        self.windows, self.pieces, self.operands, self.outs = windows, pieces, operands, outs
        count = len(windows)
        self.mine, self.boxes, rest = scratch[:count], scratch[count : 2 * count], scratch[2 * count :]
        self.fbox, self.bbox, self.fout, self.bout = rest[:4]
        self.os, self.ms, self.mr, self.fs, self.fr, self.bs, self.br = rest[4:]
        self.rows = self.fbox.shape[1]
        widths = [item.shape[2] for item in self.mine]
        self.cols = [slice(sum(widths[:i]), sum(widths[: i + 1])) for i in range(count)]

    def locate(self):
        me = lax.axis_index("dp")
        self.group = lax.axis_index("tensor")
        self.core = lax.rem(me, 2)
        chip = lax.div(me, 2)
        self.place = ring_place(chip, self.chips)
        self.right = ring_chip(self.place + 1, self.chips) * 2 + self.core
        self.left = ring_chip(self.place - 1, self.chips) * 2 + self.core
        self.mate = chip * 2 + (1 - self.core)

    def greet(self):
        self.locate()
        barrier = pltpu.get_barrier_semaphore()
        for other in (self.right, self.left, self.mate):
            pl.semaphore_signal(
                barrier, inc=1, device_id=(other, self.group), device_id_type=MESH
            )
        pl.semaphore_wait(barrier, 3)

    def product(self, i):
        return self.windows[i][1] is not None

    def shift_of(self, slot):
        step = slot // 2
        odd = slot % 2
        return (1 - odd) * (step - self.ahead) + odd * (self.behind - step)

    def half(self, which):
        return pl.ds(pl.multiple_of(which * self.rows, self.rows), self.rows)

    def block(self, i, slot, which):
        index = ring_chip(self.place + self.shift_of(slot), self.chips) * 2 + which
        left, right, first, last = self.windows[i]
        return self.operands[left].at[self.half(index), first:last]

    def remote(self, source, target_ref, ssem, rsem, target):
        return pltpu.make_async_remote_copy(
            src_ref=source,
            dst_ref=target_ref,
            send_sem=ssem,
            recv_sem=rsem,
            device_id=(target, self.group),
            device_id_type=MESH,
        )

    def across(self, i, slot):
        if self.product(i):
            source = self.mine[i].at[slot, self.half(1 - self.core)]
        else:
            source = self.block(i, slot, 1 - self.core)
        return self.remote(
            source, self.boxes[i].at[slot], self.ms.at[i, slot], self.mr.at[i, slot], self.mate
        )

    def own(self, i, slot):
        return pltpu.make_async_copy(
            self.block(i, slot, self.core), self.mine[i].at[slot], self.os.at[i, slot]
        )

    def fore(self, step):
        return self.remote(
            self.fout.at[step], self.fbox.at[step], self.fs.at[step], self.fr.at[step], self.right
        )

    def back(self, step):
        return self.remote(
            self.bout.at[step], self.bbox.at[step], self.bs.at[step], self.br.at[step], self.left
        )

    def begin(self):
        self.locate()
        for i in range(len(self.windows)):
            if not self.product(i):
                for slot in range(self.chips):
                    self.across(i, slot).start()
                    self.own(i, slot).start()

    def produce(self, slot):
        chip = ring_chip(self.place + self.shift_of(slot), self.chips)
        size = 2 * self.rows
        for i, (left, right, first, last) in enumerate(self.windows):
            if right is None:
                continue
            at = pl.multiple_of(chip * size, size)
            terms = dot(self.operands[left][pl.ds(at, size), :], self.operands[right][:, first:last])
            self.mine[i][slot] = terms.astype(BF16)
            self.across(i, slot).start()

    def local_sum(self, i, slot, cols, others):
        rows = self.half(self.core) if self.product(i) else slice(None)
        total = self.mine[i][slot, rows, cols].astype(F32) + self.boxes[i][slot, :, cols].astype(F32)
        whole = slice(self.cols[i].start + cols.start, self.cols[i].start + cols.stop)
        for ref in others:
            total = total + ref[:, whole].astype(F32)
        return total

    def arrive(self, slot):
        for i in range(len(self.windows)):
            if not self.product(i):
                self.own(i, slot).wait()
            self.across(i, slot).wait_recv()

    def put(self, target, slot, others):
        self.arrive(slot)
        for i, cols in enumerate(self.cols):
            total = self.local_sum(i, slot, slice(0, cols.stop - cols.start), others)
            target[:, cols] = total.astype(BF16)

    def hop_back(self, step, later):
        if later:
            self.back(step - 1).wait_recv()
        self.put(self.bout.at[step], 2 * step, [self.bbox.at[step - 1]] if later else [])
        self.back(step).start()

    def hop_fore(self, step, later):
        if later:
            self.fore(step - 1).wait_recv()
        self.put(self.fout.at[step], 2 * step + 1, [self.fbox.at[step - 1]] if later else [])
        self.fore(step).start()

    def hop(self, step):
        self.locate()
        self.hop_back(step, step > 0)
        if step < self.behind:
            self.hop_fore(step, step > 0)

    def finish(self):
        self.locate()
        slot = self.chips - 1
        self.arrive(slot)
        self.fore(self.behind - 1).wait_recv()
        self.back(self.ahead - 1).wait_recv()
        others = [self.fbox.at[self.behind - 1], self.bbox.at[self.ahead - 1]]
        for i, first, last, out, form in self.pieces:
            total = self.local_sum(i, slot, slice(first, last), others)
            if form == "turned":
                self.outs[out][...] = total.T[: self.outs[out].shape[0]]
            elif form is None:
                self.outs[out][...] = total
            else:
                self.outs[out][:, form, :] = total
        for step in range(self.ahead):
            self.back(step).wait_send()
        for step in range(self.behind):
            self.fore(step).wait_send()
        for slot in range(self.chips):
            for i in range(len(self.windows)):
                self.across(i, slot).wait_send()


def run_rings(rings, after_first=None):
    ahead, behind = rings[0].ahead, rings[0].behind

    def turn(step, carry):
        def part(odd, kept):
            for ring in rings:
                ring.produce(2 * step + odd)
            return kept

        lax.fori_loop(0, 2, part, 0)

        @pl.when(step == 0)
        def _():
            for ring in rings:
                ring.hop_back(0, False)
                ring.hop_fore(0, False)
            if after_first is not None:
                after_first()

        @pl.when(step > 0)
        def _():
            for ring in rings:
                ring.hop_back(step, True)
                pl.when(step < behind)(functools.partial(ring.hop_fore, step, True))

        return carry

    lax.fori_loop(0, ahead, turn, 0)


def scatter_scratch(windows, rows, devices):
    chips = devices // 2
    count = len(windows)
    dma = pltpu.SemaphoreType.DMA
    widths = [last - first for left, right, first, last in windows]
    mine = [
        pltpu.VMEM((chips, rows if right is None else 2 * rows, last - first), BF16)
        for left, right, first, last in windows
    ]
    boxes = [pltpu.VMEM((chips, rows, width), BF16) for width in widths]
    box = pltpu.VMEM((chips // 2, rows, sum(widths)), BF16)
    return mine + boxes + [box] * 4 + [dma((count, chips))] * 3 + [dma((chips,))] * 4


class Total:
    def __init__(self, devices, x_ref, o_ref, scratch):
        self.chips = devices // 2
        self.x_ref, self.o_ref = x_ref, o_ref
        self.mate_box, self.joined, self.boxes, self.ms, self.mr, self.ss, self.sr = scratch
        me = lax.axis_index("dp")
        self.group = lax.axis_index("tensor")
        self.chip = lax.div(me, 2)
        core = lax.rem(me, 2)
        self.mate = self.chip * 2 + (1 - core)
        self.peers = [
            lax.rem(self.chip + shift, self.chips) * 2 + core for shift in range(self.chips)
        ]

    def greet(self):
        barrier = pltpu.get_barrier_semaphore()
        for other in [self.mate] + self.peers[1:]:
            pl.semaphore_signal(
                barrier, inc=1, device_id=(other, self.group), device_id_type=MESH
            )
        pl.semaphore_wait(barrier, self.chips)

    def remote(self, source, target_ref, ssem, rsem, target):
        return pltpu.make_async_remote_copy(
            src_ref=source,
            dst_ref=target_ref,
            send_sem=ssem,
            recv_sem=rsem,
            device_id=(target, self.group),
            device_id_type=MESH,
        )

    def across(self):
        return self.remote(self.x_ref, self.mate_box, self.ms, self.mr, self.mate)

    def copies(self):
        return [
            self.remote(
                self.joined,
                self.boxes.at[self.chip],
                self.ss.at[shift],
                self.sr.at[shift],
                self.peers[shift],
            )
            for shift in range(1, self.chips)
        ]

    def begin(self):
        self.across().start()

    def spread(self):
        self.across().wait_recv()
        self.joined[...] = self.x_ref[...] + self.mate_box[...]
        for copy in self.copies():
            copy.start()
        self.boxes[self.chip] = self.joined[...]

    def finish(self):
        for copy in self.copies():
            copy.wait_recv()
        result = self.boxes[0]
        for other in range(1, self.chips):
            result = result + self.boxes[other]
        self.o_ref[...] = result
        self.across().wait_send()
        for copy in self.copies():
            copy.wait_send()


def total_scratch(values, devices):
    chips = devices // 2
    dma = pltpu.SemaphoreType.DMA
    return [
        pltpu.VMEM(values.shape, F32),
        pltpu.VMEM(values.shape, F32),
        pltpu.VMEM((chips,) + values.shape, F32),
        dma(()),
        dma(()),
        dma((chips,)),
        dma((chips,)),
    ]


def turned_copy(source, target):
    for start in range(0, source.shape[1], LANES):
        target[start : start + LANES, :] = source[:, start : start + LANES].T


def product_kernel(devices, groups, outs, summed, left_ref, right_ref, *refs):
    values = refs[:summed]
    refs = refs[summed:]
    pieces_out, refs = refs[:outs], refs[outs:]
    totals_out, refs = refs[:summed], refs[summed:]
    turned, scratch = refs[0], refs[1:]
    total = None
    if summed:
        scratch, rest = scratch[:-7], scratch[-7:]
        total = Total(devices, values[0], totals_out[0], rest)
    each = len(scratch) // len(groups)
    rings = [
        RingScatter(
            devices, windows, pieces, (turned, right_ref), pieces_out,
            scratch[place * each : (place + 1) * each],
        )
        for place, (windows, pieces) in enumerate(groups)
    ]
    if total is None:
        rings[0].greet()
    else:
        total.greet()
        total.begin()
    for ring in rings:
        ring.locate()
    turned_copy(left_ref, turned)
    run_rings(rings, total.spread if total is not None else None)
    for ring in rings:
        ring.finish()
    if total is not None:
        total.finish()


def scatter_product(left, right, groups, shapes, devices, collective, values=()):
    vmem = pl.BlockSpec(memory_space=pltpu.VMEM)
    rows = left.shape[1] // devices
    scratch = [pltpu.VMEM(left.shape[::-1], BF16)]
    for windows, pieces in groups:
        scratch += scatter_scratch(windows, rows, devices)
    for item in values:
        scratch += total_scratch(item, devices)
    return pl.pallas_call(
        functools.partial(
            product_kernel, devices, groups, len(shapes), len(values)
        ),
        out_shape=tuple(jax.ShapeDtypeStruct(shape, F32) for shape in shapes)
        + tuple(jax.ShapeDtypeStruct(item.shape, F32) for item in values),
        in_specs=[vmem] * (2 + len(values)),
        out_specs=(vmem,) * (len(shapes) + len(values)),
        scratch_shapes=scratch,
        compiler_params=pltpu.CompilerParams(collective_id=collective, has_side_effects=True),
        cost_estimate=cost(3),
        name="scatter_product",
    )(left, right, *values)


def head_spread(channels):
    return (iota((LANES, channels), 1) // MP == iota((LANES, channels), 0)).astype(BF16)


def parts(values, count):
    terms = []
    for _ in range(count):
        term = values.astype(BF16)
        terms.append(term)
        values = values - term.astype(F32)
    return terms


def pick(values, mask, count=2):
    return dot(jnp.concatenate(parts(values, count), axis=1), jnp.concatenate([mask] * count, axis=0))


def pick_left(mask, values, count):
    return dot(jnp.concatenate([mask] * count, axis=1), jnp.concatenate(parts(values, count), axis=0))


def gather_heads(values, spread):
    high, low = parts(values, 2)
    return dot(high, spread, NT) + dot(low, spread, NT)


def row_sums(values):
    high, low = parts(values, 2)
    ones = jnp.ones((EDGE, values.shape[1]), BF16)
    return dot(ones, high, NT) + dot(ones, low, NT)


def soft_step(raw):
    return jnp.maximum(raw, 0.0) + jnp.log1p(jnp.exp(-jnp.abs(raw)))


def conv_window(buffer, taps, bias, span):
    total = bias + taps[0:1, :] * buffer[EDGE - 3 : EDGE - 3 + span, :]
    for tap in range(1, KCONV):
        start = EDGE - 3 + tap
        total = total + taps[tap : tap + 1, :] * buffer[start : start + span, :]
    return total


def span_rates(step_ref, bias, decay, spread, span):
    raw = step_ref[...] + bias
    step = soft_step(raw)
    lower = (iota((span, span), 1) <= iota((span, span), 0)).astype(BF16)
    cum = pick_left(lower, step * decay, 3)
    tails = jnp.exp(cum[span - 1 : span, :] - cum)
    wide = pick(jnp.concatenate([step, tails, jnp.exp(cum)], axis=0), spread)
    return raw, step, cum, wide[:span], wide[span : 2 * span], wide[2 * span :]


def pair_split(values, low_lanes):
    zero = jnp.zeros_like(values)
    return jnp.concatenate(
        [jnp.where(low_lanes, values, zero), jnp.where(low_lanes, zero, values)], axis=0
    )


def pair_decay(cum, cum_rows, pair, causal):
    parts = []
    for head in (2 * pair, 2 * pair + 1):
        differ = cum[:, head : head + 1] - cum_rows[head : head + 1, :]
        parts.append(jnp.exp(jnp.where(causal, differ, MASKED)))
    return parts


def scan_forward(
    devices, spans,
    z_ref, x_ref, bc_ref, step_ref,
    tap_ref, tapb_ref, row_ref, shard_ref,
    y_ref, gated_ref, square_ref, enter_ref, all_ref,
    state, xbuf, bbuf, *sems,
):
    span, channels = x_ref.shape
    ring = RingGather(devices, shard_ref, all_ref, sems)
    turn = pl.program_id(0)

    @pl.when(turn == 0)
    def _():
        ring.greet()
        ring.begin()


    @pl.when(pl.program_id(0) == 0)
    def _():
        state[...] = jnp.zeros_like(state)
        xbuf[span:, :] = jnp.zeros((EDGE, channels), F32)
        bbuf[span:, :] = jnp.zeros((EDGE, 2 * NS), F32)

    xbuf[:EDGE, :] = xbuf[span:, :]
    bbuf[:EDGE, :] = bbuf[span:, :]
    xbuf[EDGE:, :] = x_ref[...]
    bbuf[EDGE:, :] = bc_ref[...]
    spread = head_spread(channels)
    bias, gain, biasb, stepb, decay, skip = unpack_rows(row_ref, spread)
    taps, tapsb = tap_ref[...].astype(F32), tapb_ref[...].astype(F32)
    inputs = jax.nn.silu(conv_window(xbuf, taps, bias, span))
    shared = jax.nn.silu(conv_window(bbuf, tapsb, biasb, span))
    raw, step, cum, step_w, tails_w, grown_w = span_rates(step_ref, stepb, decay, spread, span)
    cum_rows = cum.T
    b_low = shared[:, :NS].astype(BF16)
    c_low = shared[:, NS:].astype(BF16)
    scaled = inputs * step_w
    scaled_low = scaled.astype(BF16)
    enter_ref[0] = state[...]
    outer = dot(c_low, state[...].astype(BF16)) * grown_w
    fresh = dot(b_low, (scaled * tails_w).astype(BF16), TN)
    state[...] = state[...] * grown_w[span - 1 : span, :] + fresh
    cross = dot(c_low, b_low, NT)
    causal = iota((span, span), 1) <= iota((span, span), 0)
    low_lanes = iota((span, LANES), 1) < MP
    for pair in range(channels // LANES):
        lanes = slice(pair * LANES, (pair + 1) * LANES)
        first, second = pair_decay(cum, cum_rows, pair, causal)
        weights = jnp.concatenate(
            [(cross * first).astype(BF16), (cross * second).astype(BF16)], axis=1
        )
        y_ref[:, lanes] = dot(weights, pair_split(scaled_low[:, lanes], low_lanes))
    y = y_ref[...] + outer + skip * inputs
    y_ref[...] = y
    gated = y * jax.nn.silu(z_ref[...])
    gated_ref[...] = gated.astype(BF16)
    square_ref[...] = row_sums(gated * gated)

    count = spans
    for step in range(1, ring.ahead + 1):
        pl.when(turn == min(count - 1, count * step // ring.ahead))(
            functools.partial(ring.hop, step)
        )
    pl.when(turn == count - 1)(ring.finish)


def scan_backward(
    devices, spans, windows, pieces, outs_count, count,
    z_ref, x_ref, xp_ref, bc_ref, bp_ref, step_ref, y_ref, enter_ref,
    dyg_ref, scale_ref, inner_ref, dqkv_ref,
    tap_ref, tapb_ref, row_ref,
    *refs,
):
    sent, refs = refs[:count], refs[count:]
    (grad_ref, gx_ref, gb_ref, gh_ref), refs = refs[:4], refs[4:]
    outs, refs = refs[:outs_count], refs[outs_count:]
    (dstate, xbuf, bbuf, dxbuf, dbbuf, du_buf, col_buf), scratch = refs[:7], refs[7:]
    ring = RingScatter(devices, windows, pieces, sent, outs, scratch)
    span, channels = x_ref.shape
    turn = pl.program_id(0)

    @pl.when(turn == 0)
    def _():
        ring.greet()
        ring.begin()
        dstate[...] = jnp.zeros_like(dstate)
        dxbuf[...] = jnp.zeros_like(dxbuf)
        dbbuf[...] = jnp.zeros_like(dbbuf)
        col_buf[...] = jnp.zeros_like(col_buf)
        gx_ref[...] = jnp.zeros_like(gx_ref)
        gb_ref[...] = jnp.zeros_like(gb_ref)
        gh_ref[...] = jnp.zeros_like(gh_ref)

    inside = (turn < spans - 1).astype(F32)
    xbuf[:EDGE, :] = xp_ref[...] * inside
    bbuf[:EDGE, :] = bp_ref[...] * inside
    xbuf[EDGE:, :] = x_ref[...]
    bbuf[EDGE:, :] = bc_ref[...]
    spread = head_spread(channels)
    bias, gain, biasb, stepb, decay, skip = unpack_rows(row_ref, spread)
    taps, tapsb = tap_ref[...].astype(F32), tapb_ref[...].astype(F32)
    conv = conv_window(xbuf, taps, bias, span)
    sig = jax.nn.sigmoid(conv)
    inputs = conv * sig
    convb = conv_window(bbuf, tapsb, biasb, span)
    sigb = jax.nn.sigmoid(convb)
    shared = convb * sigb
    b_low = shared[:, :NS].astype(BF16)
    c_low = shared[:, NS:].astype(BF16)
    raw, step, cum, step_w, tails_w, grown_w = span_rates(step_ref, stepb, decay, spread, span)
    cum_rows = cum.T
    scaled = inputs * step_w
    scaled_low = scaled.astype(BF16)

    z = z_ref[...]
    sig_z = jax.nn.sigmoid(z)
    swish = z * sig_z
    y = y_ref[...]
    scale = scale_ref[...].T[:, :1]
    normed = y * swish * scale
    dyg = dyg_ref[...].astype(F32)
    gain_grad = jnp.sum(dyg * normed, axis=0, keepdims=True)
    dgated = scale * (dyg * gain - normed * inner_ref[...].T[:, :1])
    dy = dgated * swish
    grad_ref[:, :channels] = (dgated * y * (sig_z * (1.0 + z * (1.0 - sig_z)))).astype(BF16)

    state_low = enter_ref[0].astype(BF16)
    dstate_low = dstate[...].astype(BF16)
    grown_low = (dy * grown_w).astype(BF16)
    dy_low = dy.astype(BF16)
    tailed = scaled * tails_w
    outer = dot(c_low, state_low) * grown_w
    from_state = dot(b_low, dstate_low)
    dc = dot(grown_low, state_low, NT)
    db = dot(tailed.astype(BF16), dstate_low, NT)
    leak = from_state * tailed
    last_w = grown_w[span - 1 : span, :]
    ends = (
        jnp.sum(leak, axis=0, keepdims=True)
        + jnp.sum(enter_ref[0] * dstate[...], axis=0, keepdims=True) * last_w
    )
    skips = jnp.sum(dy * inputs, axis=0, keepdims=True)
    dstate[...] = dstate[...] * last_w + dot(c_low, grown_low, TN)

    cross = dot(c_low, b_low, NT)
    causal = iota((span, span), 1) <= iota((span, span), 0)
    low_lanes = iota((span, LANES), 1) < MP
    lane = iota((span, LANES), 1)
    dcross = jnp.zeros((span, span), F32)
    row_part = jnp.zeros((span, LANES), F32)
    for pair in range(channels // LANES):
        lanes = slice(pair * LANES, (pair + 1) * LANES)
        decays = pair_decay(cum, cum_rows, pair, causal)
        dy_pair = pair_split(dy_low[:, lanes], low_lanes)
        dweights = dot(dy_pair, scaled_low[:, lanes], NT)
        both = []
        for part in range(2):
            head = 2 * pair + part
            dterm = dweights[part * span : (part + 1) * span] * decays[part]
            dcross = dcross + dterm
            flow = dterm * cross
            row_part = row_part + jnp.where(
                lane == head, jnp.sum(flow, axis=1, keepdims=True), 0.0
            )
            col_buf[head : head + 1, :] = jnp.sum(flow, axis=0, keepdims=True)
            both.append((cross * decays[part]).astype(BF16))
        du_buf[:, lanes] = dot(jnp.concatenate(both, axis=0), dy_pair, TN)
    du = du_buf[...] + from_state * tails_w
    dcross_low = dcross.astype(BF16)
    dc = dc + dot(dcross_low, b_low)
    db = db + dot(dcross_low, c_low, TN)

    sums = gather_heads(
        jnp.concatenate(
            [dy * outer - leak, du * inputs, ends, skips, jnp.zeros((EDGE - 2, channels), F32)],
            axis=0,
        ),
        spread,
    )
    at_end = sums[2 * span : 2 * span + 1, :]
    dcum = sums[:span] + row_part - col_buf[...].T
    upper = (iota((span, span), 1) >= iota((span, span), 0)).astype(BF16)
    drate = pick_left(upper, dcum, 3) + at_end
    dstep = drate * decay + sums[span : 2 * span]
    draw = dstep * jax.nn.sigmoid(raw)
    gh_ref[0:1, :] += jnp.sum(draw, axis=0, keepdims=True)
    gh_ref[1:2, :] += jnp.sum(drate * step, axis=0, keepdims=True) * decay
    gh_ref[2:3, :] += sums[2 * span + 1 : 2 * span + 2, :]

    dinputs = du * step_w + skip * dy
    dxbuf[span:, :] = dxbuf[:EDGE, :]
    dbbuf[span:, :] = dbbuf[:EDGE, :]
    dconv = dinputs * (sig * (1.0 + conv * (1.0 - sig)))
    dconvb = jnp.concatenate([db, dc], axis=1) * (sigb * (1.0 + convb * (1.0 - sigb)))
    dxbuf[:span, :] = dconv
    dbbuf[:span, :] = dconvb
    dx = jnp.zeros_like(dconv)
    dbc = jnp.zeros_like(dconvb)
    for tap in range(KCONV):
        back = KCONV - 1 - tap
        start = EDGE - 3 + tap
        dx = dx + taps[tap : tap + 1, :] * dxbuf[back : back + span, :]
        dbc = dbc + tapsb[tap : tap + 1, :] * dbbuf[back : back + span, :]
        gx_ref[tap : tap + 1, :] += jnp.sum(
            dconv * xbuf[start : start + span, :], axis=0, keepdims=True
        )
        gb_ref[tap : tap + 1, :] += jnp.sum(
            dconvb * bbuf[start : start + span, :], axis=0, keepdims=True
        )
    gx_ref[KCONV : KCONV + 1, :] += jnp.sum(dconv, axis=0, keepdims=True)
    gb_ref[KCONV : KCONV + 1, :] += jnp.sum(dconvb, axis=0, keepdims=True)
    gx_ref[KCONV + 1 : KCONV + 2, :] += gain_grad
    width = 2 * channels + 2 * NS
    grad_ref[:, channels : 2 * channels] = dx.astype(BF16)
    grad_ref[:, 2 * channels : width] = dbc.astype(BF16)
    grad_ref[:, width : width + dqkv_ref.shape[1]] = dqkv_ref[...]
    grad_ref[:, width + dqkv_ref.shape[1] :] = draw.astype(BF16)
    for step in range(ring.ahead):
        pl.when(turn == spans * step // ring.ahead)(functools.partial(ring.hop, step))
    pl.when(turn == spans - 1)(ring.finish)


def scan_params(conv_x, conv_xb, conv_bc, conv_bcb, dt_bias, a_log, d_skip, w_mnorm):
    heads = dt_bias.shape[0]
    fill = jnp.zeros((LANES - heads,), BF16)
    flat = [conv_xb, w_mnorm, conv_bcb, dt_bias, fill, a_log, fill, d_skip, fill]
    size = sum(item.shape[0] for item in flat) // LANES
    flat.append(jnp.zeros((-size % EDGE * LANES,), BF16))
    rows = jnp.concatenate(flat).astype(F32).reshape(-1, LANES)
    return (conv_x, conv_bc, rows)


def unpack_rows(row_ref, spread):
    channels = spread.shape[1]
    count = channels // LANES
    at = 2 * count + 2 * NS // LANES

    def join_rows(first, number):
        return jnp.concatenate(
            [row_ref[i : i + 1, :] for i in range(first, first + number)], axis=1
        )

    skip = jnp.broadcast_to(row_ref[at + 2 : at + 3, :], (EDGE, LANES)).astype(BF16)
    return (
        join_rows(0, count),
        join_rows(count, count),
        join_rows(2 * count, 2 * NS // LANES),
        row_ref[at : at + 1, :],
        -jnp.exp(row_ref[at + 1 : at + 2, :]),
        dot(skip, spread)[:1],
    )


def whole_spec(array):
    return pl.BlockSpec(array.shape, lambda turn: (0,) * array.ndim)


def run_scan_forward(proj, qkv_width, params, shard, devices):
    tokens = proj.shape[0]
    channels = params[0].shape[1]
    step_at = (2 * channels + 2 * NS + qkv_width) // LANES
    spans = tokens // SPAN
    bc_at = 2 * channels // (2 * NS)
    rows = lambda width, at: pl.BlockSpec((SPAN, width), lambda turn: (turn, at))
    anywhere = pl.BlockSpec(memory_space=pl.ANY)
    return pl.pallas_call(
        functools.partial(scan_forward, devices, spans),
        grid=(spans,),
        out_shape=(
            jax.ShapeDtypeStruct((tokens, channels), F32),
            jax.ShapeDtypeStruct((tokens, channels), BF16),
            jax.ShapeDtypeStruct((EDGE, tokens), F32),
            jax.ShapeDtypeStruct((spans, NS, channels), F32),
            gather_shape(shard, devices),
        ),
        in_specs=[rows(channels, 0), rows(channels, 1), rows(2 * NS, bc_at), rows(LANES, step_at)]
        + [whole_spec(item) for item in params]
        + [anywhere],
        out_specs=(
            rows(channels, 0),
            rows(channels, 0),
            pl.BlockSpec((EDGE, SPAN), lambda turn: (0, turn)),
            pl.BlockSpec((1, NS, channels), lambda turn: (turn, 0, 0)),
            anywhere,
        ),
        scratch_shapes=[
            pltpu.VMEM((NS, channels), F32),
            pltpu.VMEM((SPAN + EDGE, channels), F32),
            pltpu.VMEM((SPAN + EDGE, 2 * NS), F32),
        ]
        + gather_sems(devices),
        compiler_params=pltpu.CompilerParams(collective_id=2, has_side_effects=True),
        cost_estimate=cost(20),
        name="scan_forward",
    )(proj, proj, proj, proj, *params, shard)


def run_scan_backward(
    proj, y, entering, dyg, scale, inner, dqkv, params, sent, windows, pieces, shapes,
    devices,
):
    tokens, width = proj.shape
    channels = params[0].shape[1]
    qkv_width = dqkv.shape[1]
    step_at = (2 * channels + 2 * NS + qkv_width) // LANES
    spans = tokens // SPAN
    bc_at = 2 * channels // (2 * NS)
    edges = SPAN // EDGE
    rows = lambda size, at: pl.BlockSpec((SPAN, size), lambda turn: (spans - 1 - turn, at))
    edge = lambda size, at: pl.BlockSpec(
        (EDGE, size), lambda turn: (jnp.maximum((spans - 1 - turn) * edges - 1, 0), at)
    )
    keep = lambda shape: pl.BlockSpec(shape, lambda turn: (0, 0))
    shapes = tuple(jax.ShapeDtypeStruct(shape, F32) for shape in shapes)
    return pl.pallas_call(
        functools.partial(
            scan_backward, devices, spans, windows, pieces, len(shapes), len(sent)
        ),
        grid=(spans,),
        out_shape=(
            jax.ShapeDtypeStruct((tokens, width), BF16),
            jax.ShapeDtypeStruct((EDGE, channels), F32),
            jax.ShapeDtypeStruct((EDGE, 2 * NS), F32),
            jax.ShapeDtypeStruct((EDGE, LANES), F32),
        )
        + shapes,
        in_specs=[
            rows(channels, 0),
            rows(channels, 1),
            edge(channels, 1),
            rows(2 * NS, bc_at),
            edge(2 * NS, bc_at),
            rows(LANES, step_at),
            rows(channels, 0),
            pl.BlockSpec((1, NS, channels), lambda turn: (spans - 1 - turn, 0, 0)),
            rows(channels, 0),
            pl.BlockSpec((EDGE, SPAN), lambda turn: (0, spans - 1 - turn)),
            pl.BlockSpec((EDGE, SPAN), lambda turn: (0, spans - 1 - turn)),
            rows(qkv_width, 0),
        ]
        + [whole_spec(item) for item in params]
        + [pl.BlockSpec(memory_space=pl.ANY)] * len(sent),
        out_specs=(
            rows(width, 0),
            keep((EDGE, channels)),
            keep((EDGE, 2 * NS)),
            keep((EDGE, LANES)),
        )
        + tuple(keep(item.shape) for item in shapes),
        scratch_shapes=[
            pltpu.VMEM((NS, channels), F32),
            pltpu.VMEM((SPAN + EDGE, channels), F32),
            pltpu.VMEM((SPAN + EDGE, 2 * NS), F32),
            pltpu.VMEM((SPAN + EDGE, channels), F32),
            pltpu.VMEM((SPAN + EDGE, 2 * NS), F32),
            pltpu.VMEM((SPAN, channels), F32),
            pltpu.VMEM((LANES, SPAN), F32),
        ]
        + scatter_scratch(windows, sent[0].shape[0] // devices, devices),
        compiler_params=pltpu.CompilerParams(collective_id=6, has_side_effects=True),
        cost_estimate=cost(47),
        name="scan_backward",
    )(
        proj, proj, proj, proj, proj, proj, y, entering, dyg, scale, inner, dqkv, *params, *sent,
    )


def rotary_tables(tokens):
    half = HEAD_SIZE // 2
    exponent = np.arange(half, dtype=np.float64) * (-2.0 * LOG_BASE / HEAD_SIZE)
    rates = np.tile(np.exp(exponent.astype(np.float32)).astype(np.float64), LANES // half)
    tables = []
    for places in (np.arange(FINE), np.arange(0, tokens, FINE)):
        angles = places[:, None] * rates[None, :]
        tables += [np.cos(angles).astype(np.float32), np.sin(angles).astype(np.float32)]
    return tables


def fill_rotary(fine_cos, fine_sin, coarse_cos, coarse_sin, cosine, sine):
    small_cos, small_sin = fine_cos[...], fine_sin[...]
    for turn in range(coarse_cos.shape[0]):
        big_cos, big_sin = coarse_cos[turn : turn + 1, :], coarse_sin[turn : turn + 1, :]
        rows = slice(turn * FINE, (turn + 1) * FINE)
        cosine[rows, :] = small_cos * big_cos - small_sin * big_sin
        sine[rows, :] = small_sin * big_cos + small_cos * big_sin


def head_masks():
    half = HEAD_SIZE // 2
    row, col = iota((LANES, LANES), 0), iota((LANES, LANES), 1)
    place = col % HEAD_SIZE
    ahead = jnp.where(place < half, -1.0, 0.0)
    behind = jnp.where(place < half, 0.0, 1.0)

    def turn(start):
        return jnp.where(row == start + half, ahead, jnp.where(row == start - half, behind, 0.0))

    first = row < HEAD_SIZE
    left = col < HEAD_SIZE
    low = lambda mask: mask.astype(BF16)
    within = low(turn(col))
    copy = low(jnp.where(row == place, 1.0, 0.0))
    copy_turn = low(jnp.where(first, turn(place), 0.0))
    value = low(jnp.where(row == place + HEAD_SIZE, 1.0, 0.0))
    fold = low(jnp.where(left & (row % HEAD_SIZE == place), 1.0, 0.0))
    other = row % HEAD_SIZE
    fold_turn = low(
        jnp.where(
            left,
            jnp.where(other == place + half, ahead, jnp.where(other == place - half, behind, 0.0)),
            0.0,
        )
    )
    fold_value = low(jnp.where(left, 0.0, jnp.where(other == place, 1.0, 0.0)))
    return within, copy, copy_turn, value, fold, fold_turn, fold_value


def attend_forward(
    q_ref, kv_ref, fine_cos, fine_sin, coarse_cos, coarse_sin,
    qkv_ref, lse_ref, o_ref, vt, cos_ref, sin_ref,
):
    fill_rotary(fine_cos, fine_sin, coarse_cos, coarse_sin, cos_ref, sin_ref)
    tokens, query_width = q_ref.shape
    pairs = query_width // LANES
    within, copy, copy_turn, value = head_masks()[:4]

    def turn_rows(i, carry):
        rows = pl.ds(pl.multiple_of(i * QBLK, QBLK), QBLK)
        cosine, sine = cos_ref[rows, :], sin_ref[rows, :]
        for pair in range(pairs):
            lanes = slice(pair * LANES, (pair + 1) * LANES)
            query = q_ref[rows, lanes]
            turned = query * cosine + pick(query, within) * sine
            qkv_ref[rows, lanes] = (turned * HEAD_SIZE**-0.5).astype(BF16)
        kv = kv_ref[rows, :]
        keys = pick(kv, copy) * cosine + pick(kv, copy_turn) * sine
        qkv_ref[rows, query_width : query_width + LANES] = keys.astype(BF16)
        qkv_ref[rows, query_width + LANES :] = dot(kv.astype(BF16), value).astype(BF16)
        vt[:, rows] = kv.T[HEAD_SIZE:, :].astype(BF16)
        return carry

    lax.fori_loop(0, tokens // QBLK, turn_rows, 0)
    low_lanes = iota((QBLK, LANES), 1) < HEAD_SIZE
    wide = (QBLK, 2 * QBLK)
    visible = iota(wide, 0) <= iota(wide, 1) % QBLK

    def block(i, carry):
        here = pl.ds(pl.multiple_of(i * QBLK, QBLK), QBLK)
        queries = [
            pair_split(qkv_ref[here, pair * LANES : (pair + 1) * LANES], low_lanes)
            for pair in range(pairs)
        ]

        def tile(there, state, edge):
            keys = qkv_ref[there, query_width : query_width + LANES]
            result = []
            for pair in range(pairs):
                top, total, out = state[3 * pair : 3 * pair + 3]
                scores = dot(keys, queries[pair], NT)
                if edge:
                    scores = jnp.where(visible, scores, MASKED)
                higher = jnp.maximum(top, jnp.max(scores, axis=0, keepdims=True))
                probs = jnp.exp(scores - higher)
                fade = jnp.exp(top - higher)
                total = total * fade + jnp.sum(probs, axis=0, keepdims=True)
                out = out * fade + dot(vt[:, there], probs.astype(BF16))
                result += [higher, total, out]
            return tuple(result)

        state = (
            jnp.full((1, 2 * QBLK), MASKED, F32),
            jnp.zeros((1, 2 * QBLK), F32),
            jnp.zeros((HEAD_SIZE, 2 * QBLK), F32),
        ) * pairs
        state = lax.fori_loop(
            0,
            i,
            lambda j, state: tile(pl.ds(pl.multiple_of(j * QBLK, QBLK), QBLK), state, False),
            state,
        )
        state = tile(here, state, True)
        for pair in range(pairs):
            top, total, out = state[3 * pair : 3 * pair + 3]
            out = out / total
            lse = top + jnp.log(total)
            lse_ref[2 * pair : 2 * pair + 1, here] = lse[:, :QBLK]
            lse_ref[2 * pair + 1 : 2 * pair + 2, here] = lse[:, QBLK:]
            both = jnp.concatenate([out[:, :QBLK], out[:, QBLK:]], axis=0)
            o_ref[here, pair * LANES : (pair + 1) * LANES] = both.T.astype(BF16)
        return carry

    lax.fori_loop(0, tokens // QBLK, block, 0)


def attend_backward(
    qkv_ref, lse_ref, o_ref, do_ref, fine_cos, fine_sin, coarse_cos, coarse_sin,
    dqkv_ref,
    dq, kt, dk, dv, cos_ref, sin_ref,
):
    fill_rotary(fine_cos, fine_sin, coarse_cos, coarse_sin, cos_ref, sin_ref)
    tokens, query_width = o_ref.shape
    pairs = query_width // LANES
    key_lanes = slice(query_width, query_width + LANES)
    value_lanes = slice(query_width + LANES, query_width + 2 * LANES)

    def turn_keys(i, carry):
        rows = pl.ds(pl.multiple_of(i * QBLK, QBLK), QBLK)
        kt[:, rows] = qkv_ref[rows, key_lanes].astype(F32).T[:HEAD_SIZE, :].astype(BF16)
        return carry

    lax.fori_loop(0, tokens // QBLK, turn_keys, 0)
    dk[...] = jnp.zeros_like(dk)
    dv[...] = jnp.zeros_like(dv)
    low_lanes = iota((QBLK, LANES), 1) < HEAD_SIZE
    wide = (QBLK, 2 * QBLK)
    visible = iota(wide, 0) <= iota(wide, 1) % QBLK
    ones = jnp.ones((EDGE, LANES), BF16)

    def block(i, carry):
        here = pl.ds(pl.multiple_of(i * QBLK, QBLK), QBLK)
        queries, grads, inners, lses = [], [], [], []
        for pair in range(pairs):
            lanes = slice(pair * LANES, (pair + 1) * LANES)
            queries.append(pair_split(qkv_ref[here, lanes], low_lanes))
            grad = do_ref[here, lanes]
            grads.append(pair_split(grad, low_lanes))
            both = pair_split(grad.astype(F32) * o_ref[here, lanes].astype(F32), low_lanes)
            high, low = parts(both, 2)
            inners.append((dot(ones, high, NT) + dot(ones, low, NT))[:1])
            lses.append(
                jnp.concatenate(
                    [
                        lse_ref[2 * pair : 2 * pair + 1, here],
                        lse_ref[2 * pair + 1 : 2 * pair + 2, here],
                    ],
                    axis=1,
                )
            )
        query_all = jnp.concatenate(queries, axis=0)
        grad_all = jnp.concatenate(grads, axis=0)

        def tile(there, state, edge):
            keys = qkv_ref[there, key_lanes]
            values = qkv_ref[there, value_lanes]
            all_probs, all_dscores, result = [], [], []
            for pair in range(pairs):
                probs = dot(keys, queries[pair], NT) - lses[pair]
                if edge:
                    probs = jnp.where(visible, probs, MASKED)
                probs = jnp.exp(probs)
                dprobs = dot(values, grads[pair], NT)
                dscores = (probs * (dprobs - inners[pair])).astype(BF16)
                all_probs.append(probs.astype(BF16))
                all_dscores.append(dscores)
                result.append(state[pair] + dot(kt[:, there], dscores))
            dv[there, :] += dot(jnp.concatenate(all_probs, axis=1), grad_all)
            dk[there, :] += dot(jnp.concatenate(all_dscores, axis=1), query_all)
            return tuple(result)

        state = (jnp.zeros((HEAD_SIZE, 2 * QBLK), F32),) * pairs
        state = lax.fori_loop(
            0,
            i,
            lambda j, state: tile(pl.ds(pl.multiple_of(j * QBLK, QBLK), QBLK), state, False),
            state,
        )
        state = tile(here, state, True)
        for pair in range(pairs):
            both = jnp.concatenate([state[pair][:, :QBLK], state[pair][:, QBLK:]], axis=0)
            dq[here, pair * LANES : (pair + 1) * LANES] = both.T
        return carry

    lax.fori_loop(0, tokens // QBLK, block, 0)
    masks = head_masks()
    within, (fold, fold_turn, fold_value) = masks[0], masks[4:]

    def turn_back(i, carry):
        rows = pl.ds(pl.multiple_of(i * QBLK, QBLK), QBLK)
        cosine, sine = cos_ref[rows, :], sin_ref[rows, :]
        for pair in range(pairs):
            lanes = slice(pair * LANES, (pair + 1) * LANES)
            grad = dq[rows, lanes]
            grad = grad * cosine - pick(grad, within) * sine
            dqkv_ref[rows, lanes] = (grad * HEAD_SIZE**-0.5).astype(BF16)
        grad = dk[rows, :]
        grad = pick(grad, fold) * cosine - pick(grad, fold_turn) * sine
        grad = grad + pick(dv[rows, :], fold_value)
        dqkv_ref[rows, query_width:] = grad.astype(BF16)
        return carry

    lax.fori_loop(0, tokens // QBLK, turn_back, 0)


def run_attend_forward(proj, query_at, query_width, tables):
    tokens = proj.shape[0]
    cols = lambda size, at: pl.BlockSpec((tokens, size), lambda turn: (0, at // size))
    return pl.pallas_call(
        attend_forward,
        grid=(1,),
        out_shape=(
            jax.ShapeDtypeStruct((tokens, query_width + 2 * LANES), BF16),
            jax.ShapeDtypeStruct((EDGE, tokens), F32),
            jax.ShapeDtypeStruct((tokens, query_width), BF16),
        ),
        in_specs=[
            cols(query_width, query_at),
            cols(2 * HEAD_SIZE, query_at + query_width),
        ]
        + [whole_spec(table) for table in tables],
        out_specs=(
            cols(query_width + 2 * LANES, 0),
            pl.BlockSpec((EDGE, tokens), lambda turn: (0, 0)),
            cols(query_width, 0),
        ),
        scratch_shapes=[
            pltpu.VMEM((HEAD_SIZE, tokens), BF16),
            pltpu.VMEM((tokens, LANES), F32),
            pltpu.VMEM((tokens, LANES), F32),
        ],
        cost_estimate=cost(15),
        name="attend_forward",
    )(proj, proj, *tables)


def run_attend_backward(qkv, lse, attended, grads, grad_at, tables):
    tokens, query_width = attended.shape
    vmem = pl.BlockSpec(memory_space=pltpu.VMEM)
    cols = lambda size, at: pl.BlockSpec((tokens, size), lambda turn: (0, at // size))
    return pl.pallas_call(
        attend_backward,
        grid=(1,),
        out_shape=jax.ShapeDtypeStruct((tokens, query_width + 2 * HEAD_SIZE), BF16),
        in_specs=[
            whole_spec(qkv),
            whole_spec(lse),
            whole_spec(attended),
            cols(query_width, grad_at),
        ]
        + [whole_spec(table) for table in tables],
        out_specs=cols(query_width + 2 * HEAD_SIZE, 0),
        scratch_shapes=[
            pltpu.VMEM((tokens, query_width), F32),
            pltpu.VMEM((HEAD_SIZE, tokens), BF16),
            pltpu.VMEM((tokens, LANES), F32),
            pltpu.VMEM((tokens, LANES), F32),
            pltpu.VMEM((tokens, LANES), F32),
            pltpu.VMEM((tokens, LANES), F32),
        ],
        cost_estimate=cost(16),
        name="attend_backward",
    )(qkv, lse, attended, grads, *tables)


def feed_forward(
    x_ref, mixed_ref, other_ref, act_grad_ref, norms_ref, gu_ref,
    after_ref, scale_ref, hidden_ref, act_ref, dgu_ref, back_ref,
):
    units = act_grad_ref.shape[1]
    after = x_ref[...].astype(F32) + (mixed_ref[...].astype(F32) + other_ref[...].astype(F32))
    after_ref[...] = after.astype(BF16)
    scale = lax.rsqrt(jnp.mean(after * after, axis=-1, keepdims=True) + EPSILON)
    scale_ref[...] = scale
    hidden = (after * scale * norms_ref[1:2, :]).astype(BF16)
    hidden_ref[...] = hidden
    for start in range(0, units, UBLK):
        cols = slice(start, start + UBLK)
        up_cols = slice(units + start, units + start + UBLK)
        gate = dot(hidden, gu_ref[:, cols])
        upward = dot(hidden, gu_ref[:, up_cols])
        grad = act_grad_ref[:, cols]
        sigma = jax.nn.sigmoid(gate)
        swish = gate * sigma
        act_ref[:, cols] = (swish * upward).astype(BF16)
        slope = sigma * (1.0 + gate * (1.0 - sigma))
        dgu_ref[:, cols] = (grad * upward * slope).astype(BF16)
        dgu_ref[:, up_cols] = (grad * swish).astype(BF16)
    back_ref[...] = dot(dgu_ref[...], gu_ref[...], NT).astype(BF16)


def product_rows(dims, left_ref, right_ref, out_ref):
    out_ref[...] = dot(left_ref[...], right_ref[...], dims).astype(out_ref.dtype)


def run_product(left, right, dims, dtype):
    tokens, depth = left.shape
    cols = right.shape[1 - dims[1][0]]
    return pl.pallas_call(
        functools.partial(product_rows, dims),
        grid=(tokens // TBLK,),
        out_shape=jax.ShapeDtypeStruct((tokens, cols), dtype),
        in_specs=[pl.BlockSpec((TBLK, depth), lambda turn: (turn, 0)), once(right)],
        out_specs=pl.BlockSpec((TBLK, cols), lambda turn: (turn, 0)),
        cost_estimate=cost(4),
        name="product_rows",
    )(left, right)


def project(heads, x_ref, w_ref, hidden_ref, proj_ref, norms_ref):
    @pl.when(pl.program_id(0) == 0)
    def _():
        gains = w_ref[:, w_ref.shape[1] - LANES :].astype(F32).T
        norms_ref[...] = jnp.zeros_like(norms_ref)
        norms_ref[0:2, :] = gains[heads : heads + 2, :]

    x = x_ref[...].astype(F32)
    scale = lax.rsqrt(jnp.mean(x * x, axis=-1, keepdims=True) + EPSILON)
    hidden = (x * scale * norms_ref[0:1, :]).astype(BF16)
    hidden_ref[...] = hidden
    proj_ref[...] = dot(hidden, w_ref[...])


def run_project(x, w_in, heads):
    tokens, width = x.shape
    cols = w_in.shape[1]
    rows = lambda size: pl.BlockSpec((TBLK, size), lambda turn: (turn, 0))
    return pl.pallas_call(
        functools.partial(project, heads),
        grid=(tokens // TBLK,),
        out_shape=(
            jax.ShapeDtypeStruct((tokens, width), BF16),
            jax.ShapeDtypeStruct((tokens, cols), F32),
            jax.ShapeDtypeStruct((EDGE, width), F32),
        ),
        in_specs=[rows(width), once(w_in)],
        out_specs=(
            rows(width), rows(cols), pl.BlockSpec((EDGE, width), lambda turn: (0, 0)),
        ),
        cost_estimate=cost(8),
        name="project",
    )(x, w_in)


def project_back(grad_ref, w_ref, x_ref, part_ref, gain_grad_ref):
    @pl.when(pl.program_id(0) == 0)
    def _():
        gain_grad_ref[...] = jnp.zeros_like(gain_grad_ref)

    x = x_ref[...].astype(F32)
    normed = x * lax.rsqrt(jnp.mean(x * x, axis=-1, keepdims=True) + EPSILON)
    part = dot(grad_ref[...], w_ref[...], NT).astype(BF16)
    part_ref[...] = part
    gain_grad_ref[:1, :] += jnp.sum(part.astype(F32) * normed, axis=0, keepdims=True)


def run_project_back(grads, w_in, x):
    tokens, width = x.shape
    cols = w_in.shape[1]
    rows = lambda size: pl.BlockSpec((TBLK, size), lambda turn: (turn, 0))
    return pl.pallas_call(
        project_back,
        grid=(tokens // TBLK,),
        out_shape=(
            jax.ShapeDtypeStruct((tokens, width), BF16),
            jax.ShapeDtypeStruct((EDGE, width), F32),
        ),
        in_specs=[rows(cols), once(w_in), rows(width)],
        out_specs=(rows(width), pl.BlockSpec((EDGE, width), lambda turn: (0, 0))),
        cost_estimate=cost(8),
        name="project_back",
    )(grads, w_in, x)


def once(item):
    return pl.BlockSpec(item.shape, lambda turn: (0,) * item.ndim, pipeline_mode=pl.Buffered(1))


def run_feed_forward(x, mixed, other, act_grad, norms, w_gate_up):
    tokens, width = x.shape
    units = act_grad.shape[1]
    rows = lambda size: pl.BlockSpec((TBLK, size), lambda turn: (turn, 0))
    shape = jax.ShapeDtypeStruct
    return pl.pallas_call(
        feed_forward,
        grid=(tokens // TBLK,),
        out_shape=(
            shape((tokens, width), BF16),
            shape((tokens, 1), F32),
            shape((tokens, width), BF16),
            shape((tokens, units), BF16),
            shape((tokens, 2 * units), BF16),
            shape((tokens, width), BF16),
        ),
        in_specs=[rows(width)] * 3 + [rows(units), once(norms), once(w_gate_up)],
        out_specs=(rows(width), rows(1), rows(width), rows(units), rows(2 * units), rows(width)),
        cost_estimate=cost(14),
        name="feed_forward",
    )(x, mixed, other, act_grad, norms, w_gate_up)


def mixer_forward(gated_ref, scale_ref, gain_ref, attended_ref, w_ref, low_ref, mixed_ref):
    channels = gated_ref.shape[1]
    scale = scale_ref[...].T[:, :1]
    low_ref[:, :channels] = (gated_ref[...].astype(F32) * scale * gain_ref[...]).astype(BF16)
    low_ref[:, channels:] = attended_ref[...]
    mixed_ref[...] = dot(low_ref[...], w_ref[...], NT).astype(BF16)


def run_mixer_forward(gated, scale, gain, attended, w_out):
    tokens, channels = gated.shape
    width, inner = w_out.shape
    rows = lambda size: pl.BlockSpec((TBLK, size), lambda turn: (turn, 0))
    return pl.pallas_call(
        mixer_forward,
        grid=(tokens // TBLK,),
        out_shape=(
            jax.ShapeDtypeStruct((tokens, inner), BF16),
            jax.ShapeDtypeStruct((tokens, width), BF16),
        ),
        in_specs=[
            rows(channels),
            pl.BlockSpec((EDGE, TBLK), lambda turn: (0, turn)),
            once(gain),
            rows(attended.shape[1]),
            once(w_out),
        ],
        out_specs=(rows(inner), rows(width)),
        cost_estimate=cost(5),
        name="mixer_forward",
    )(gated, scale, gain, attended, w_out)


def mixer_backward(
    part_ref, other_ref, after_ref, scale_ref, top_ref, norms_ref,
    w_ref, gated_ref, scale_m_ref, gain_m_ref,
    low_ref, mamba_ref, attended_ref, inner_ref, gain_grad_ref,
):
    channels = gated_ref.shape[1]

    @pl.when(pl.program_id(0) == 0)
    def _():
        gain_grad_ref[...] = jnp.zeros_like(gain_grad_ref)

    grad = part_ref[...].astype(F32) + other_ref[...].astype(F32)
    scale = scale_ref[...]
    normed = after_ref[...].astype(F32) * scale
    gain_grad_ref[:1, :] += jnp.sum(grad * normed, axis=0, keepdims=True)
    weighted = grad * norms_ref[1:2, :]
    mean = jnp.mean(weighted * normed, axis=-1, keepdims=True)
    total = top_ref[...].astype(F32) + scale * (weighted - normed * mean)
    low_ref[...] = total.astype(BF16)
    back = dot(low_ref[...], w_ref[...])
    mamba = back[:, :channels]
    mamba_ref[...] = mamba.astype(BF16)
    attended_ref[...] = back[:, channels:].astype(BF16)
    inner_ref[...] = row_sums(mamba * gain_m_ref[...] * gated_ref[...].astype(F32)) * scale_m_ref[...]


def run_mixer_backward(part, other, after, scale, top, norms, w_out, gated, scale_m, gain_m):
    tokens, width = after.shape
    channels = gated.shape[1]
    inner = w_out.shape[1]
    shape = jax.ShapeDtypeStruct
    rows = lambda size: pl.BlockSpec((NBLK, size), lambda turn: (turn, 0))
    lanes = pl.BlockSpec((EDGE, NBLK), lambda turn: (0, turn))
    return pl.pallas_call(
        mixer_backward,
        grid=(tokens // NBLK,),
        out_shape=(
            shape((tokens, width), BF16),
            shape((tokens, channels), BF16),
            shape((tokens, inner - channels), BF16),
            shape((EDGE, tokens), F32),
            shape((EDGE, width), F32),
        ),
        in_specs=[rows(width)] * 3
        + [rows(1), rows(width), once(norms), once(w_out), rows(channels), lanes, once(gain_m)],
        out_specs=(
            rows(width), rows(channels), rows(inner - channels), lanes,
            pl.BlockSpec((EDGE, width), lambda turn: (0, 0)),
        ),
        cost_estimate=cost(8),
        name="mixer_backward",
    )(part, other, after, scale, top, norms, w_out, gated, scale_m, gain_m)


def finish_layer(
    x_ref, norms_ref, part_ref, other_ref, grad_ref, after_ref, ffn_ref, ffn_other_ref, *refs,
):
    count = len(refs) // 2 - 1
    passed, out_ref, result_ref, handed = refs[:count], refs[count], refs[count + 1], refs[count + 2 :]

    @pl.when(pl.program_id(0) == 0)
    def _():
        for source, target in zip(passed, handed):
            target[...] = source[...]

    x = x_ref[...].astype(F32)
    scale = lax.rsqrt(jnp.mean(x * x, axis=-1, keepdims=True) + EPSILON)
    normed = x * scale
    weighted = (part_ref[...].astype(F32) + other_ref[...].astype(F32)) * norms_ref[0:1, :]
    mean = jnp.mean(weighted * normed, axis=-1, keepdims=True)
    out_ref[...] = grad_ref[...].astype(F32) + scale * (weighted - normed * mean)
    ffn = ffn_ref[...].astype(F32) + ffn_other_ref[...].astype(F32)
    result_ref[...] = (after_ref[...].astype(F32) + ffn).astype(BF16)


def run_finish(x, norms, part, other, grad, after, ffn, ffn_other, passed):
    tokens, width = x.shape
    rows = pl.BlockSpec((TBLK, width), lambda turn: (turn, 0))
    return pl.pallas_call(
        finish_layer,
        grid=(tokens // TBLK,),
        out_shape=(
            jax.ShapeDtypeStruct((tokens, width), F32),
            jax.ShapeDtypeStruct((tokens, width), BF16),
        )
        + tuple(jax.ShapeDtypeStruct(item.shape, F32) for item in passed),
        in_specs=[rows, once(norms)] + [rows] * 6 + [once(item) for item in passed],
        out_specs=(rows, rows) + tuple(once(item) for item in passed),
        cost_estimate=cost(8),
        name="finish_layer",
    )(x, norms, part, other, grad, after, ffn, ffn_other, *passed)


def swap(partial):
    return lax.ppermute(partial, "tensor", [(0, 1), (1, 0)])


def join(mine, other):
    return mine.astype(F32) + other.astype(F32)


def tensor_sum(partial):
    return join(partial, swap(partial))


def thirds(size):
    part = size // 3
    return [(0, part), (part, 2 * part), (2 * part, size)]


def local(
    layer_input, w_norm1, w_zx, w_bc, w_dt, conv_x, conv_xb, conv_bc, conv_bcb, dt_bias, a_log,
    d_skip, w_mnorm, w_mout, query_key_value_weight, output_weight, w_norm2, w_gu, w_down,
    grad_output,
):
    devices = lax.axis_size("dp")
    tokens, width = layer_input.shape
    shard = w_zx.shape[0]
    channels = conv_xb.shape[0]
    heads = dt_bias.shape[0]
    qkv_width = query_key_value_weight.shape[2]
    units = w_down.shape[0]
    attn_width = output_weight.shape[1]
    tail = jnp.concatenate(
        [w_dt, w_norm1[:, None], w_norm2[:, None], jnp.zeros((shard, LANES - heads - 2), BF16)],
        axis=1,
    )
    mixer_in = jnp.concatenate(
        [w_zx.reshape(shard, -1), w_bc, query_key_value_weight.reshape(shard, -1), tail], axis=1
    )
    in_width = mixer_in.shape[1]
    (w_in,) = gather_rows([mixer_in], devices, 0, [(0, *window) for window in thirds(in_width)])
    hidden_one, proj, norms = run_project(layer_input, w_in, heads)
    params = scan_params(
        conv_x, conv_xb, conv_bc, conv_bcb, dt_bias, a_log, d_skip, w_mnorm
    )
    out_shard = jnp.concatenate([w_mout.T, output_weight.reshape(attn_width, -1).T], axis=1)
    y, gated, square_sum, entering, w_out = run_scan_forward(
        proj, qkv_width, params, out_shard, devices
    )
    channels_all = channels * lax.axis_size("tensor")
    scale_m = lax.rsqrt(tensor_sum(square_sum) / channels_all + EPSILON)
    tables = rotary_tables(tokens)
    qkv_at = 2 * channels + 2 * NS
    qkv, lse, attended = run_attend_forward(proj, qkv_at, attn_width, tables)
    gain_m = w_mnorm.astype(F32)[None, :]
    mixer_out, mixed = run_mixer_forward(gated, scale_m, gain_m, attended, w_out)
    mixed, gate_up_shard, down_shard = lax.optimization_barrier(
        (mixed, w_gu.reshape(shard, -1), w_down.T)
    )
    other = swap(mixed)
    w_gate_up, w_down_t = gather_rows(
        [gate_up_shard, down_shard],
        devices,
        3,
        [(0, 0, units), (0, units, 2 * units), (1, 0, units)],
    )
    act_grad = run_product(grad_output, w_down_t, NN, F32)
    other, w_gate_up, w_down_t, act_grad = lax.optimization_barrier(
        (other, w_gate_up, w_down_t, act_grad)
    )
    after, scale_two, hidden_two, activated, grad_gu_low, partial_two = run_feed_forward(
        layer_input, mixed, other, act_grad, norms, w_gate_up
    )
    other = swap(partial_two)
    grad_down = dot(grad_output, activated, TN).astype(BF16)
    (mine_gu,) = scatter_product(
        hidden_two,
        grad_gu_low,
        [
            ([(0, 1, 0, units)], [(0, 0, units, 0, 0)]),
            ([(0, 1, units, 2 * units)], [(0, 0, units, 0, 1)]),
        ],
        [(shard, 2, units)],
        devices,
        1,
    )
    ffn_part = run_product(activated, w_down_t, NT, BF16)
    other, mine_gu, grad_down, ffn_part = lax.optimization_barrier(
        (other, mine_gu, grad_down, ffn_part)
    )
    ffn_other = swap(ffn_part)
    grad_mix_low, grad_mamba, grad_attended, inner_m, grad_norm2 = run_mixer_backward(
        partial_two, other, after, scale_two, grad_output, norms, w_out, gated, scale_m, gain_m
    )
    inner_m = tensor_sum(inner_m) / channels_all
    dqkv = run_attend_backward(qkv, lse, attended, grad_attended, 0, tables)
    grad_out = dot(grad_mix_low, mixer_out, TN).astype(BF16)
    windows = [(0, None, 0, channels + attn_width), (1, None, 0, units)]
    pieces = [
        (0, 0, channels, 0, None),
        (0, channels, channels + attn_width, 1, None),
        (1, 0, units, 2, None),
    ]
    shapes = [(shard, channels), (shard, attn_width), (shard, units)]
    grad_proj, small_x, small_b, small_h, mine_mout, mine_o, mine_down = run_scan_backward(
        proj, y, entering, grad_mamba, scale_m, inner_m, dqkv, params,
        [grad_out, grad_down], windows, pieces, shapes, devices,
    )
    ffn_other, grad_proj = lax.optimization_barrier((ffn_other, grad_proj))
    partial_one, grad_norm1 = run_project_back(grad_proj, w_in, layer_input)
    partial_one, grad_proj = lax.optimization_barrier((partial_one, grad_proj))
    other = swap(partial_one)
    small = jnp.concatenate(
        [
            small_x[: KCONV + 2].reshape(-1, LANES),
            small_h[:3],
            grad_norm2[0].reshape(-1, LANES),
            small_b[: KCONV + 1].reshape(-1, LANES),
            grad_norm1[0].reshape(-1, LANES),
        ],
        axis=0,
    )
    small_rows = small.shape[0]
    cross_rows = (KCONV + 1) * 2 * NS // LANES + width // LANES
    cross_at = small_rows - cross_rows
    small = jnp.pad(small, ((0, -small_rows % EDGE), (0, 0)))
    shared_at = 2 * channels
    step_at = qkv_at + qkv_width
    mine_zx, mine_bc, mine_qkv, mine_step, small = scatter_product(
        hidden_one,
        grad_proj,
        [
            ([(0, 1, 0, channels)], [(0, 0, channels, 0, 0)]),
            ([(0, 1, channels, shared_at)], [(0, 0, channels, 0, 1)]),
            (
                [(0, 1, shared_at, in_width)],
                [
                    (0, 0, 2 * NS, 1, None),
                    (0, 2 * NS, 2 * NS + qkv_width, 2, 0),
                    (0, 2 * NS + qkv_width, in_width - shared_at, 3, "turned"),
                ],
            ),
        ],
        [
            (shard, 2, channels),
            (shard, 2 * NS),
            (shard, 1, qkv_width),
            (heads, shard),
        ],
        devices,
        5,
        (small,),
    )
    other, mine_bc = lax.optimization_barrier((other, mine_bc))
    crossing = tensor_sum(small[cross_at : cross_at + cross_rows])
    shared_cols = tensor_sum(mine_bc)
    passed = (mine_zx, mine_qkv, mine_step, mine_mout, mine_o, mine_gu, mine_down)
    grad_source, result, *passed = run_finish(
        layer_input, norms, partial_one, other, grad_mix_low, after, ffn_part, ffn_other,
        passed,
    )
    mine_zx, mine_qkv, mine_step, mine_mout, mine_o, mine_gu, mine_down = passed

    half = NS * 2 // lax.axis_size("tensor")
    begin = lax.axis_index("tensor") * half
    grad_bc = lax.dynamic_slice_in_dim(shared_cols, begin, half, 1)
    x_rows = (KCONV + 2) * channels // LANES
    norm_rows = width // LANES
    total_x = small[:x_rows].reshape(KCONV + 2, channels)
    total_h = small[x_rows : x_rows + 3]
    norm2_total = small[x_rows + 3 : cross_at].reshape(width)
    total_b = crossing[: cross_rows - norm_rows].reshape(KCONV + 1, 2 * NS)
    total_b = lax.dynamic_slice_in_dim(total_b, begin, half, 1)
    norm1_total = crossing[cross_rows - norm_rows :].reshape(width)
    norms = [
        lax.dynamic_slice_in_dim(item, lax.axis_index("dp") * shard, shard, 0)
        for item in (norm1_total, norm2_total)
    ]
    return (
        result,
        grad_source,
        norms[0],
        mine_zx,
        grad_bc,
        mine_step.T,
        total_x[:KCONV],
        total_x[KCONV],
        total_b[:KCONV],
        total_b[KCONV],
        total_h[0, :heads],
        total_h[1, :heads],
        total_h[2, :heads],
        total_x[KCONV + 1],
        mine_mout.T,
        mine_qkv,
        mine_o.T.reshape(output_weight.shape),
        norms[1],
        mine_gu,
        mine_down.T,
    )


def solution(mesh):
    return jax.shard_map(
        local,
        mesh=mesh,
        in_specs=(
            P("dp", None),
            P("dp"),
            P("dp", None, "tensor"),
            P("dp", None),
            P("dp", "tensor"),
            P(None, "tensor"),
            P("tensor"),
            P(),
            P(),
            P("tensor"),
            P("tensor"),
            P("tensor"),
            P("tensor"),
            P("tensor", "dp"),
            P("dp", "tensor", None),
            P("tensor", None, "dp"),
            P("dp"),
            P("dp", None, "tensor"),
            P("tensor", "dp"),
            P("dp", None),
        ),
        out_specs=(
            P("dp", None),
            P("dp", None),
            P("dp"),
            P("dp", None, "tensor"),
            P("dp", "tensor"),
            P("dp", "tensor"),
            P(None, "tensor"),
            P("tensor"),
            P(None, "tensor"),
            P("tensor"),
            P("tensor"),
            P("tensor"),
            P("tensor"),
            P("tensor"),
            P("tensor", "dp"),
            P("dp", "tensor", None),
            P("tensor", None, "dp"),
            P("dp"),
            P("dp", None, "tensor"),
            P("tensor", "dp"),
        ),
        check_vma=False,
    )
```

```python
import functools
import math

import jax
import jax.numpy as jnp
import numpy as np
from jax import lax
from jax.experimental import pallas as pl
from jax.experimental.pallas import tpu as pltpu
from jax.sharding import PartitionSpec as P

HEAD_SIZE = 64
MP = 64
NS = 128
KCONV = 4
SPAN = 128
QBLK = 256
FINE = 32
TBLK = 256
NBLK = 128
UBLK = 256
LANES = 128
EDGE = 8

EPSILON = 1e-05
HIGHEST = lax.Precision.HIGHEST
LOG_BASE = math.log(100000000000.0)
MASKED = -1e30
MESH = pl.DeviceIdType.MESH
F32 = jnp.float32
BF16 = jnp.bfloat16

NN = ((1,), (0,))
NT = ((1,), (1,))
TN = ((0,), (0,))


def dot(left, right, dims=NN, precision=None):
    return lax.dot_general(
        left, right, (dims, ((), ())), preferred_element_type=F32, precision=precision
    )


def iota(shape, dim):
    return lax.broadcasted_iota(jnp.int32, shape, dim)


def ring_place(chip, chips):
    odd = lax.rem(chip, 2)
    half = lax.div(chip, 2)
    return (1 - odd) * half + odd * (chips - 1 - half)


def ring_chip(place, chips):
    place = lax.rem(place + 4 * chips, chips)
    back = lax.div(place, chips // 2)
    return (1 - back) * (2 * place) + back * (2 * (chips - 1 - place) + 1)


def ring_setup(chips):
    me = lax.axis_index("dp")
    group = lax.axis_index("tensor")
    chip = lax.div(me, 2)
    core = lax.rem(me, 2)
    place = ring_place(chip, chips)
    right = ring_chip(place + 1, chips) * 2 + core
    left = ring_chip(place - 1, chips) * 2 + core
    mate = chip * 2 + (1 - core)
    barrier = pltpu.get_barrier_semaphore()
    for other in (right, left, mate):
        pl.semaphore_signal(barrier, inc=1, device_id=(other, group), device_id_type=MESH)
    pl.semaphore_wait(barrier, 3)
    return me, group, core, place, right, left, mate


class RingGather:
    def __init__(self, devices, x_ref, o_ref, sems, cols=slice(None)):
        self.cols = cols
        self.chips = devices // 2
        self.ahead = self.chips // 2
        self.behind = self.chips - 1 - self.ahead
        self.x_ref, self.o_ref, self.rows = x_ref, o_ref, x_ref.shape[0]
        self.fs, self.fr, self.bs, self.br, self.cs, self.cr, self.own_sem = sems

    def locate(self):
        me = lax.axis_index("dp")
        self.group = lax.axis_index("tensor")
        self.core = lax.rem(me, 2)
        chip = lax.div(me, 2)
        self.place = ring_place(chip, self.chips)
        self.right = ring_chip(self.place + 1, self.chips) * 2 + self.core
        self.left = ring_chip(self.place - 1, self.chips) * 2 + self.core
        self.mate = chip * 2 + (1 - self.core)
        self.me = me

    def slot(self, index):
        rows = pl.ds(pl.multiple_of(index * self.rows, self.rows), self.rows)
        return self.o_ref.at[rows, self.cols]

    def copy(self, shift, ssem, rsem, target):
        if shift == 0:
            index, source = self.me, self.x_ref.at[:, self.cols]
        else:
            index = ring_chip(self.place + shift, self.chips) * 2 + self.core
            source = self.slot(index)
        return pltpu.make_async_remote_copy(
            src_ref=source,
            dst_ref=self.slot(index),
            send_sem=ssem,
            recv_sem=rsem,
            device_id=(target, self.group),
            device_id_type=MESH,
        )

    def fore(self, step):
        return self.copy(-step, self.fs.at[step], self.fr.at[step], self.right)

    def back(self, step):
        return self.copy(step, self.bs.at[step], self.br.at[step], self.left)

    def across(self, shift):
        number = 0 if shift == 0 else 2 * abs(shift) - (1 if shift < 0 else 0)
        return self.copy(shift, self.cs.at[number], self.cr.at[number], self.mate)

    def own(self):
        return pltpu.make_async_copy(
            self.x_ref.at[:, self.cols], self.slot(self.me), self.own_sem
        )

    def greet(self):
        self.locate()
        barrier = pltpu.get_barrier_semaphore()
        for other in (self.right, self.left, self.mate):
            pl.semaphore_signal(
                barrier, inc=1, device_id=(other, self.group), device_id_type=MESH
            )
        pl.semaphore_wait(barrier, 3)

    def begin(self):
        self.locate()
        self.fore(0).start()
        self.back(0).start()
        self.across(0).start()
        self.own().start()

    def hop(self, step):
        self.locate()
        self.fore(step - 1).wait_recv()
        if step < self.ahead:
            self.fore(step).start()
        self.across(-step).start()
        if step <= self.behind:
            self.back(step - 1).wait_recv()
            if step < self.behind:
                self.back(step).start()
            self.across(step).start()

    def finish(self):
        self.locate()
        self.own().wait()
        for step in range(self.ahead):
            self.fore(step).wait_send()
        for step in range(self.behind):
            self.back(step).wait_send()
        for shift in range(-self.ahead, self.behind + 1):
            self.across(shift).wait()


def gather_sems(devices):
    dma = pltpu.SemaphoreType.DMA
    return [dma((devices // 2,))] * 6 + [dma(())]


def gather_shape(shard, devices):
    return jax.ShapeDtypeStruct((shard.shape[0] * devices, shard.shape[1]), shard.dtype)


def gather_kernel(devices, count, windows, *refs):
    shards, outs, sems = refs[:count], refs[count : 2 * count], refs[2 * count :]
    each = len(sems) // len(windows)
    rings = [
        RingGather(
            devices, shards[i], outs[i], sems[place * each : (place + 1) * each], slice(first, last)
        )
        for place, (i, first, last) in enumerate(windows)
    ]
    rings[0].greet()
    for ring in rings:
        ring.begin()
    for step in range(1, rings[0].ahead + 1):
        for ring in rings:
            ring.hop(step)
    for ring in rings:
        ring.finish()


def cost(micros):
    return pl.CostEstimate(flops=int(micros * 1e9), bytes_accessed=0, transcendentals=0)


def gather_rows(shards, devices, collective, windows):
    count = len(shards)
    anywhere = pl.BlockSpec(memory_space=pl.ANY)
    return pl.pallas_call(
        functools.partial(gather_kernel, devices, count, windows),
        out_shape=tuple(gather_shape(shard, devices) for shard in shards),
        in_specs=[anywhere] * count,
        out_specs=(anywhere,) * count,
        scratch_shapes=gather_sems(devices) * len(windows),
        compiler_params=pltpu.CompilerParams(collective_id=collective, has_side_effects=True),
        cost_estimate=cost(3),
        name="gather_rows",
    )(*shards)


def scatter_order(chips):
    ahead = chips // 2
    behind = chips - 1 - ahead
    order = []
    for step in range(ahead):
        order.append(-(ahead - step))
        if step < behind:
            order.append(behind - step)
    order.append(0)
    return order


class RingScatter:
    def __init__(self, devices, windows, pieces, operands, outs, scratch):
        self.chips = devices // 2
        self.ahead = self.chips // 2
        self.behind = self.chips - 1 - self.ahead
        self.windows, self.pieces, self.operands, self.outs = windows, pieces, operands, outs
        count = len(windows)
        self.mine, self.boxes, rest = scratch[:count], scratch[count : 2 * count], scratch[2 * count :]
        self.fbox, self.bbox, self.fout, self.bout = rest[:4]
        self.os, self.ms, self.mr, self.fs, self.fr, self.bs, self.br = rest[4:]
        self.rows = self.fbox.shape[1]
        widths = [item.shape[2] for item in self.mine]
        self.cols = [slice(sum(widths[:i]), sum(widths[: i + 1])) for i in range(count)]

    def locate(self):
        me = lax.axis_index("dp")
        self.group = lax.axis_index("tensor")
        self.core = lax.rem(me, 2)
        chip = lax.div(me, 2)
        self.place = ring_place(chip, self.chips)
        self.right = ring_chip(self.place + 1, self.chips) * 2 + self.core
        self.left = ring_chip(self.place - 1, self.chips) * 2 + self.core
        self.mate = chip * 2 + (1 - self.core)

    def greet(self):
        self.locate()
        barrier = pltpu.get_barrier_semaphore()
        for other in (self.right, self.left, self.mate):
            pl.semaphore_signal(
                barrier, inc=1, device_id=(other, self.group), device_id_type=MESH
            )
        pl.semaphore_wait(barrier, 3)

    def product(self, i):
        return self.windows[i][1] is not None

    def shift_of(self, slot):
        step = slot // 2
        odd = slot % 2
        return (1 - odd) * (step - self.ahead) + odd * (self.behind - step)

    def half(self, which):
        return pl.ds(pl.multiple_of(which * self.rows, self.rows), self.rows)

    def block(self, i, slot, which):
        index = ring_chip(self.place + self.shift_of(slot), self.chips) * 2 + which
        left, right, first, last = self.windows[i]
        return self.operands[left].at[self.half(index), first:last]

    def remote(self, source, target_ref, ssem, rsem, target):
        return pltpu.make_async_remote_copy(
            src_ref=source,
            dst_ref=target_ref,
            send_sem=ssem,
            recv_sem=rsem,
            device_id=(target, self.group),
            device_id_type=MESH,
        )

    def across(self, i, slot):
        if self.product(i):
            source = self.mine[i].at[slot, self.half(1 - self.core)]
        else:
            source = self.block(i, slot, 1 - self.core)
        return self.remote(
            source, self.boxes[i].at[slot], self.ms.at[i, slot], self.mr.at[i, slot], self.mate
        )

    def own(self, i, slot):
        return pltpu.make_async_copy(
            self.block(i, slot, self.core), self.mine[i].at[slot], self.os.at[i, slot]
        )

    def fore(self, step):
        return self.remote(
            self.fout.at[step], self.fbox.at[step], self.fs.at[step], self.fr.at[step], self.right
        )

    def back(self, step):
        return self.remote(
            self.bout.at[step], self.bbox.at[step], self.bs.at[step], self.br.at[step], self.left
        )

    def begin(self):
        self.locate()
        for i in range(len(self.windows)):
            if not self.product(i):
                for slot in range(self.chips):
                    self.across(i, slot).start()
                    self.own(i, slot).start()

    def produce(self, slot):
        chip = ring_chip(self.place + self.shift_of(slot), self.chips)
        size = 2 * self.rows
        for i, (left, right, first, last) in enumerate(self.windows):
            if right is None:
                continue
            at = pl.multiple_of(chip * size, size)
            terms = dot(self.operands[left][pl.ds(at, size), :], self.operands[right][:, first:last])
            self.mine[i][slot] = terms.astype(BF16)
            self.across(i, slot).start()

    def local_sum(self, i, slot, cols, others):
        rows = self.half(self.core) if self.product(i) else slice(None)
        total = self.mine[i][slot, rows, cols].astype(F32) + self.boxes[i][slot, :, cols].astype(F32)
        whole = slice(self.cols[i].start + cols.start, self.cols[i].start + cols.stop)
        for ref in others:
            total = total + ref[:, whole].astype(F32)
        return total

    def arrive(self, slot):
        for i in range(len(self.windows)):
            if not self.product(i):
                self.own(i, slot).wait()
            self.across(i, slot).wait_recv()

    def put(self, target, slot, others):
        self.arrive(slot)
        for i, cols in enumerate(self.cols):
            total = self.local_sum(i, slot, slice(0, cols.stop - cols.start), others)
            target[:, cols] = total.astype(BF16)

    def hop_back(self, step, later):
        if later:
            self.back(step - 1).wait_recv()
        self.put(self.bout.at[step], 2 * step, [self.bbox.at[step - 1]] if later else [])
        self.back(step).start()

    def hop_fore(self, step, later):
        if later:
            self.fore(step - 1).wait_recv()
        self.put(self.fout.at[step], 2 * step + 1, [self.fbox.at[step - 1]] if later else [])
        self.fore(step).start()

    def hop(self, step):
        self.locate()
        self.hop_back(step, step > 0)
        if step < self.behind:
            self.hop_fore(step, step > 0)

    def finish(self):
        self.locate()
        slot = self.chips - 1
        self.arrive(slot)
        self.fore(self.behind - 1).wait_recv()
        self.back(self.ahead - 1).wait_recv()
        others = [self.fbox.at[self.behind - 1], self.bbox.at[self.ahead - 1]]
        for i, first, last, out, form in self.pieces:
            total = self.local_sum(i, slot, slice(first, last), others)
            if form == "turned":
                self.outs[out][...] = total.T[: self.outs[out].shape[0]]
            elif form is None:
                self.outs[out][...] = total
            else:
                self.outs[out][:, form, :] = total
        for step in range(self.ahead):
            self.back(step).wait_send()
        for step in range(self.behind):
            self.fore(step).wait_send()
        for slot in range(self.chips):
            for i in range(len(self.windows)):
                self.across(i, slot).wait_send()


def run_rings(rings, after_first=None):
    ahead, behind = rings[0].ahead, rings[0].behind

    def turn(step, carry):
        def part(odd, kept):
            for ring in rings:
                ring.produce(2 * step + odd)
            return kept

        lax.fori_loop(0, 2, part, 0)

        @pl.when(step == 0)
        def _():
            for ring in rings:
                ring.hop_back(0, False)
                ring.hop_fore(0, False)
            if after_first is not None:
                after_first()

        @pl.when(step > 0)
        def _():
            for ring in rings:
                ring.hop_back(step, True)
                pl.when(step < behind)(functools.partial(ring.hop_fore, step, True))

        return carry

    lax.fori_loop(0, ahead, turn, 0)


def scatter_scratch(windows, rows, devices):
    chips = devices // 2
    count = len(windows)
    dma = pltpu.SemaphoreType.DMA
    widths = [last - first for left, right, first, last in windows]
    mine = [
        pltpu.VMEM((chips, rows if right is None else 2 * rows, last - first), BF16)
        for left, right, first, last in windows
    ]
    boxes = [pltpu.VMEM((chips, rows, width), BF16) for width in widths]
    box = pltpu.VMEM((chips // 2, rows, sum(widths)), BF16)
    return mine + boxes + [box] * 4 + [dma((count, chips))] * 3 + [dma((chips,))] * 4


class Total:
    def __init__(self, devices, x_ref, o_ref, scratch):
        self.chips = devices // 2
        self.x_ref, self.o_ref = x_ref, o_ref
        self.mate_box, self.joined, self.boxes, self.ms, self.mr, self.ss, self.sr = scratch
        me = lax.axis_index("dp")
        self.group = lax.axis_index("tensor")
        self.chip = lax.div(me, 2)
        core = lax.rem(me, 2)
        self.mate = self.chip * 2 + (1 - core)
        self.peers = [
            lax.rem(self.chip + shift, self.chips) * 2 + core for shift in range(self.chips)
        ]

    def greet(self):
        barrier = pltpu.get_barrier_semaphore()
        for other in [self.mate] + self.peers[1:]:
            pl.semaphore_signal(
                barrier, inc=1, device_id=(other, self.group), device_id_type=MESH
            )
        pl.semaphore_wait(barrier, self.chips)

    def remote(self, source, target_ref, ssem, rsem, target):
        return pltpu.make_async_remote_copy(
            src_ref=source,
            dst_ref=target_ref,
            send_sem=ssem,
            recv_sem=rsem,
            device_id=(target, self.group),
            device_id_type=MESH,
        )

    def across(self):
        return self.remote(self.x_ref, self.mate_box, self.ms, self.mr, self.mate)

    def copies(self):
        return [
            self.remote(
                self.joined,
                self.boxes.at[self.chip],
                self.ss.at[shift],
                self.sr.at[shift],
                self.peers[shift],
            )
            for shift in range(1, self.chips)
        ]

    def begin(self):
        self.across().start()

    def spread(self):
        self.across().wait_recv()
        self.joined[...] = self.x_ref[...] + self.mate_box[...]
        for copy in self.copies():
            copy.start()
        self.boxes[self.chip] = self.joined[...]

    def finish(self):
        for copy in self.copies():
            copy.wait_recv()
        result = self.boxes[0]
        for other in range(1, self.chips):
            result = result + self.boxes[other]
        self.o_ref[...] = result
        self.across().wait_send()
        for copy in self.copies():
            copy.wait_send()


def total_scratch(values, devices):
    chips = devices // 2
    dma = pltpu.SemaphoreType.DMA
    return [
        pltpu.VMEM(values.shape, F32),
        pltpu.VMEM(values.shape, F32),
        pltpu.VMEM((chips,) + values.shape, F32),
        dma(()),
        dma(()),
        dma((chips,)),
        dma((chips,)),
    ]


def turned_copy(source, target):
    for start in range(0, source.shape[1], LANES):
        target[start : start + LANES, :] = source[:, start : start + LANES].T


def product_kernel(devices, groups, outs, places, summed, left_ref, right_ref, *refs):
    values = refs[:summed]
    refs = refs[summed:]
    pieces_out, refs = refs[:outs], refs[outs:]
    total = None
    if summed:
        total_out, refs = refs[0], refs[1:]
    turned, scratch = refs[0], refs[1:]
    if summed:
        scratch, rest = scratch[:-8], scratch[-8:]
        together = rest[0]
        together[...] = jnp.zeros_like(together)
        for at, (which, row, lane) in enumerate(places):
            together[at : at + 1, :] = values[which][row : row + 1, lane : lane + LANES]
        total = Total(devices, together, total_out, rest[1:])
    each = len(scratch) // len(groups)
    rings = [
        RingScatter(
            devices, windows, pieces, (turned, right_ref), pieces_out,
            scratch[place * each : (place + 1) * each],
        )
        for place, (windows, pieces) in enumerate(groups)
    ]
    if total is None:
        rings[0].greet()
    else:
        total.greet()
        total.begin()
    for ring in rings:
        ring.locate()
    turned_copy(left_ref, turned)
    run_rings(rings, total.spread if total is not None else None)
    for ring in rings:
        ring.finish()
    if total is not None:
        total.finish()


def scatter_product(left, right, groups, shapes, devices, collective, values=(), places=()):
    vmem = pl.BlockSpec(memory_space=pltpu.VMEM)
    rows = left.shape[1] // devices
    scratch = [pltpu.VMEM(left.shape[::-1], BF16)]
    for windows, pieces in groups:
        scratch += scatter_scratch(windows, rows, devices)
    totals = ()
    if values:
        total = jax.ShapeDtypeStruct((len(places) + -len(places) % EDGE, LANES), F32)
        totals = (total,)
        scratch += [pltpu.VMEM(total.shape, F32)] + total_scratch(total, devices)
    return pl.pallas_call(
        functools.partial(
            product_kernel, devices, groups, len(shapes), places, len(values)
        ),
        out_shape=tuple(jax.ShapeDtypeStruct(shape, F32) for shape in shapes) + totals,
        in_specs=[vmem] * (2 + len(values)),
        out_specs=(vmem,) * (len(shapes) + len(totals)),
        scratch_shapes=scratch,
        compiler_params=pltpu.CompilerParams(collective_id=collective, has_side_effects=True),
        cost_estimate=cost(3),
        name="scatter_product",
    )(left, right, *values)


def head_spread(channels):
    return (iota((LANES, channels), 1) // MP == iota((LANES, channels), 0)).astype(BF16)


def parts(values, count):
    terms = []
    for _ in range(count):
        term = values.astype(BF16)
        terms.append(term)
        values = values - term.astype(F32)
    return terms


def pick(values, mask, count=2):
    return dot(jnp.concatenate(parts(values, count), axis=1), jnp.concatenate([mask] * count, axis=0))


def pick_left(mask, values, count):
    return dot(jnp.concatenate([mask] * count, axis=1), jnp.concatenate(parts(values, count), axis=0))


def gather_heads(values, spread):
    high, low = parts(values, 2)
    return dot(high, spread, NT) + dot(low, spread, NT)


def row_sums(values):
    high, low = parts(values, 2)
    ones = jnp.ones((EDGE, values.shape[1]), BF16)
    return dot(ones, high, NT) + dot(ones, low, NT)


def soft_step(raw):
    return jnp.maximum(raw, 0.0) + jnp.log1p(jnp.exp(-jnp.abs(raw)))


def shifted(values, edge, ahead):
    span = values.shape[0]
    moves = range(1, KCONV)
    row, col = iota((span, span), 0), iota((span, span), 1)
    mask = jnp.concatenate(
        [(col == (row + move if ahead else row - move)).astype(BF16) for move in moves], axis=0
    )
    moved = pick_left(mask, values, 2)
    place = iota(edge.shape, 0)
    result = []
    for move in moves:
        part = moved[(move - 1) * span : move * span]
        if ahead:
            into = jnp.where(place >= EDGE - move, pltpu.roll(edge, EDGE - move, 0), 0.0)
            part = jnp.concatenate([part[:-EDGE], part[-EDGE:] + into], axis=0)
        else:
            into = jnp.where(place < move, pltpu.roll(edge, move, 0), 0.0)
            part = jnp.concatenate([part[:EDGE] + into, part[EDGE:]], axis=0)
        result.append(part)
    return result


def apply_taps(values, moved, taps):
    total = taps[KCONV - 1 : KCONV, :] * values
    for move, part in enumerate(moved, 1):
        total = total + taps[KCONV - 1 - move : KCONV - move, :] * part
    return total


def span_rates(step_ref, bias, decay, spread, span):
    raw = step_ref[...] + bias
    step = soft_step(raw)
    lower = (iota((span, span), 1) <= iota((span, span), 0)).astype(BF16)
    cum = pick_left(lower, step * decay, 3)
    tails = jnp.exp(cum[span - 1 : span, :] - cum)
    wide = pick(jnp.concatenate([step, tails, jnp.exp(cum)], axis=0), spread)
    return raw, step, cum, wide[:span], wide[span : 2 * span], wide[2 * span :]


def pair_split(values, low_lanes):
    zero = jnp.zeros_like(values)
    return jnp.concatenate(
        [jnp.where(low_lanes, values, zero), jnp.where(low_lanes, zero, values)], axis=0
    )


def pair_decay(cum, cum_rows, pair, causal):
    parts = []
    for head in (2 * pair, 2 * pair + 1):
        differ = cum[:, head : head + 1] - cum_rows[head : head + 1, :]
        parts.append(jnp.exp(jnp.where(causal, differ, MASKED)))
    return parts


def scan_forward(
    devices, spans,
    z_ref, x_ref, bc_ref, step_ref,
    tap_ref, tapb_ref, row_ref, shard_ref,
    y_ref, gated_ref, square_ref, enter_ref, all_ref,
    state, edge, *sems,
):
    span, channels = x_ref.shape
    ring = RingGather(devices, shard_ref, all_ref, sems)
    turn = pl.program_id(0)

    @pl.when(turn == 0)
    def _():
        ring.greet()
        ring.begin()


    @pl.when(pl.program_id(0) == 0)
    def _():
        state[...] = jnp.zeros_like(state)
        edge[...] = jnp.zeros_like(edge)

    spread = head_spread(channels)
    bias, gain, biasb, stepb, decay, skip = unpack_rows(row_ref, spread)
    taps = jnp.concatenate([tap_ref[...], tapb_ref[...]], axis=1).astype(F32)
    before = jnp.concatenate([x_ref[...], bc_ref[...]], axis=1)
    conv = apply_taps(before, shifted(before, edge[...], False), taps)
    edge[...] = before[-EDGE:]
    conv = jax.nn.silu(conv + jnp.concatenate([bias, biasb], axis=1))
    inputs, shared = conv[:, :channels], conv[:, channels:]
    raw, step, cum, step_w, tails_w, grown_w = span_rates(step_ref, stepb, decay, spread, span)
    cum_rows = cum.T
    b_low = shared[:, :NS].astype(BF16)
    c_low = shared[:, NS:].astype(BF16)
    scaled = inputs * step_w
    scaled_low = scaled.astype(BF16)
    enter_ref[0] = state[...]
    outer = dot(c_low, state[...].astype(BF16)) * grown_w
    fresh = dot(b_low, (scaled * tails_w).astype(BF16), TN)
    state[...] = state[...] * grown_w[span - 1 : span, :] + fresh
    cross = dot(c_low, b_low, NT)
    causal = iota((span, span), 1) <= iota((span, span), 0)
    low_lanes = iota((span, LANES), 1) < MP
    for pair in range(channels // LANES):
        lanes = slice(pair * LANES, (pair + 1) * LANES)
        first, second = pair_decay(cum, cum_rows, pair, causal)
        weights = jnp.concatenate(
            [(cross * first).astype(BF16), (cross * second).astype(BF16)], axis=1
        )
        y_ref[:, lanes] = dot(weights, pair_split(scaled_low[:, lanes], low_lanes))
    y = y_ref[...] + outer + skip * inputs
    y_ref[...] = y
    gated = y * jax.nn.silu(z_ref[...])
    gated_ref[...] = gated.astype(BF16)
    square_ref[...] = row_sums(gated * gated)

    count = spans
    for step in range(1, ring.ahead + 1):
        pl.when(turn == min(count - 1, count * step // ring.ahead))(
            functools.partial(ring.hop, step)
        )
    pl.when(turn == count - 1)(ring.finish)


def scan_backward(
    devices, spans, windows, pieces, outs_count, count,
    z_ref, x_ref, xp_ref, bc_ref, bp_ref, step_ref, y_ref, enter_ref,
    dyg_ref, scale_ref, inner_ref, dqkv_ref,
    tap_ref, tapb_ref, row_ref,
    *refs,
):
    sent, refs = refs[:count], refs[count:]
    (grad_ref, gx_ref, gh_ref), refs = refs[:3], refs[3:]
    outs, refs = refs[:outs_count], refs[outs_count:]
    (dstate, dedge, du_buf, col_buf), scratch = refs[:4], refs[4:]
    ring = RingScatter(devices, windows, pieces, sent, outs, scratch)
    span, channels = x_ref.shape
    turn = pl.program_id(0)

    @pl.when(turn == 0)
    def _():
        ring.greet()
        ring.begin()
        dstate[...] = jnp.zeros_like(dstate)
        dedge[...] = jnp.zeros_like(dedge)
        col_buf[...] = jnp.zeros_like(col_buf)
        gx_ref[...] = jnp.zeros_like(gx_ref)
        gh_ref[...] = jnp.zeros_like(gh_ref)

    inside = (turn < spans - 1).astype(F32)
    before = jnp.concatenate([x_ref[...], bc_ref[...]], axis=1)
    edge = jnp.concatenate([xp_ref[...], bp_ref[...]], axis=1) * inside
    spread = head_spread(channels)
    bias, gain, biasb, stepb, decay, skip = unpack_rows(row_ref, spread)
    taps = jnp.concatenate([tap_ref[...], tapb_ref[...]], axis=1).astype(F32)
    moved = shifted(before, edge, False)
    conv = apply_taps(before, moved, taps) + jnp.concatenate([bias, biasb], axis=1)
    sig = jax.nn.sigmoid(conv)
    swished = conv * sig
    inputs, shared = swished[:, :channels], swished[:, channels:]
    b_low = shared[:, :NS].astype(BF16)
    c_low = shared[:, NS:].astype(BF16)
    raw, step, cum, step_w, tails_w, grown_w = span_rates(step_ref, stepb, decay, spread, span)
    cum_rows = cum.T
    scaled = inputs * step_w
    scaled_low = scaled.astype(BF16)

    z = z_ref[...]
    sig_z = jax.nn.sigmoid(z)
    swish = z * sig_z
    y = y_ref[...]
    scale = scale_ref[...].T[:, :1]
    normed = y * swish * scale
    dyg = dyg_ref[...].astype(F32)
    gain_grad = jnp.sum(dyg * normed, axis=0, keepdims=True)
    dgated = scale * (dyg * gain - normed * inner_ref[...].T[:, :1])
    dy = dgated * swish
    grad_ref[:, :channels] = (dgated * y * (sig_z * (1.0 + z * (1.0 - sig_z)))).astype(BF16)

    state_low = enter_ref[0].astype(BF16)
    dstate_low = dstate[...].astype(BF16)
    grown_low = (dy * grown_w).astype(BF16)
    dy_low = dy.astype(BF16)
    tailed = scaled * tails_w
    outer = dot(c_low, state_low) * grown_w
    from_state = dot(b_low, dstate_low)
    dc = dot(grown_low, state_low, NT)
    db = dot(tailed.astype(BF16), dstate_low, NT)
    leak = from_state * tailed
    last_w = grown_w[span - 1 : span, :]
    ends = (
        jnp.sum(leak, axis=0, keepdims=True)
        + jnp.sum(enter_ref[0] * dstate[...], axis=0, keepdims=True) * last_w
    )
    skips = jnp.sum(dy * inputs, axis=0, keepdims=True)
    dstate[...] = dstate[...] * last_w + dot(c_low, grown_low, TN)

    cross = dot(c_low, b_low, NT)
    causal = iota((span, span), 1) <= iota((span, span), 0)
    low_lanes = iota((span, LANES), 1) < MP
    lane = iota((span, LANES), 1)
    dcross = jnp.zeros((span, span), F32)
    row_part = jnp.zeros((span, LANES), F32)
    for pair in range(channels // LANES):
        lanes = slice(pair * LANES, (pair + 1) * LANES)
        decays = pair_decay(cum, cum_rows, pair, causal)
        dy_pair = pair_split(dy_low[:, lanes], low_lanes)
        dweights = dot(dy_pair, scaled_low[:, lanes], NT)
        both = []
        for part in range(2):
            head = 2 * pair + part
            dterm = dweights[part * span : (part + 1) * span] * decays[part]
            dcross = dcross + dterm
            flow = dterm * cross
            row_part = row_part + jnp.where(
                lane == head, jnp.sum(flow, axis=1, keepdims=True), 0.0
            )
            col_buf[head : head + 1, :] = jnp.sum(flow, axis=0, keepdims=True)
            both.append((cross * decays[part]).astype(BF16))
        du_buf[:, lanes] = dot(jnp.concatenate(both, axis=0), dy_pair, TN)
    du = du_buf[...] + from_state * tails_w
    dcross_low = dcross.astype(BF16)
    dc = dc + dot(dcross_low, b_low)
    db = db + dot(dcross_low, c_low, TN)

    sums = gather_heads(
        jnp.concatenate(
            [dy * outer - leak, du * inputs, ends, skips, jnp.zeros((EDGE - 2, channels), F32)],
            axis=0,
        ),
        spread,
    )
    at_end = sums[2 * span : 2 * span + 1, :]
    dcum = sums[:span] + row_part - col_buf[...].T
    upper = (iota((span, span), 1) >= iota((span, span), 0)).astype(BF16)
    drate = pick_left(upper, dcum, 3) + at_end
    dstep = drate * decay + sums[span : 2 * span]
    draw = dstep * jax.nn.sigmoid(raw)
    gh_ref[0:1, :] += jnp.sum(draw, axis=0, keepdims=True)
    gh_ref[1:2, :] += jnp.sum(drate * step, axis=0, keepdims=True) * decay
    gh_ref[2:3, :] += sums[2 * span + 1 : 2 * span + 2, :]

    dinputs = du * step_w + skip * dy
    dconv = jnp.concatenate([dinputs, db, dc], axis=1) * (sig * (1.0 + conv * (1.0 - sig)))
    dbefore = apply_taps(dconv, shifted(dconv, dedge[...], True), taps)
    dedge[...] = dconv[:EDGE]
    gx_ref[KCONV - 1 : KCONV, :] += jnp.sum(dconv * before, axis=0, keepdims=True)
    for move, part in enumerate(moved, 1):
        tap = KCONV - 1 - move
        gx_ref[tap : tap + 1, :] += jnp.sum(dconv * part, axis=0, keepdims=True)
    gx_ref[KCONV : KCONV + 1, :] += jnp.sum(dconv, axis=0, keepdims=True)
    gx_ref[KCONV + 1 : KCONV + 2, :channels] += gain_grad
    width = 2 * channels + 2 * NS
    grad_ref[:, channels:width] = dbefore.astype(BF16)
    grad_ref[:, width : width + dqkv_ref.shape[1]] = dqkv_ref[...]
    grad_ref[:, width + dqkv_ref.shape[1] :] = draw.astype(BF16)
    for step in range(ring.ahead):
        pl.when(turn == spans * step // ring.ahead)(functools.partial(ring.hop, step))
    pl.when(turn == spans - 1)(ring.finish)


def scan_params(conv_x, conv_xb, conv_bc, conv_bcb, dt_bias, a_log, d_skip, w_mnorm):
    heads = dt_bias.shape[0]
    fill = jnp.zeros((LANES - heads,), BF16)
    flat = [conv_xb, w_mnorm, conv_bcb, dt_bias, fill, a_log, fill, d_skip, fill]
    size = sum(item.shape[0] for item in flat) // LANES
    flat.append(jnp.zeros((-size % EDGE * LANES,), BF16))
    rows = jnp.concatenate(flat).astype(F32).reshape(-1, LANES)
    return (conv_x, conv_bc, rows)


def unpack_rows(row_ref, spread):
    channels = spread.shape[1]
    count = channels // LANES
    at = 2 * count + 2 * NS // LANES

    def join_rows(first, number):
        return jnp.concatenate(
            [row_ref[i : i + 1, :] for i in range(first, first + number)], axis=1
        )

    skip = jnp.broadcast_to(row_ref[at + 2 : at + 3, :], (EDGE, LANES)).astype(BF16)
    return (
        join_rows(0, count),
        join_rows(count, count),
        join_rows(2 * count, 2 * NS // LANES),
        row_ref[at : at + 1, :],
        -jnp.exp(row_ref[at + 1 : at + 2, :]),
        dot(skip, spread)[:1],
    )


def whole_spec(array):
    return pl.BlockSpec(array.shape, lambda turn: (0,) * array.ndim)


def run_scan_forward(proj, qkv_width, params, shard, devices):
    tokens = proj.shape[0]
    channels = params[0].shape[1]
    step_at = (2 * channels + 2 * NS + qkv_width) // LANES
    spans = tokens // SPAN
    bc_at = 2 * channels // (2 * NS)
    rows = lambda width, at: pl.BlockSpec((SPAN, width), lambda turn: (turn, at))
    anywhere = pl.BlockSpec(memory_space=pl.ANY)
    return pl.pallas_call(
        functools.partial(scan_forward, devices, spans),
        grid=(spans,),
        out_shape=(
            jax.ShapeDtypeStruct((tokens, channels), F32),
            jax.ShapeDtypeStruct((tokens, channels), BF16),
            jax.ShapeDtypeStruct((EDGE, tokens), F32),
            jax.ShapeDtypeStruct((spans, NS, channels), F32),
            gather_shape(shard, devices),
        ),
        in_specs=[rows(channels, 0), rows(channels, 1), rows(2 * NS, bc_at), rows(LANES, step_at)]
        + [whole_spec(item) for item in params]
        + [anywhere],
        out_specs=(
            rows(channels, 0),
            rows(channels, 0),
            pl.BlockSpec((EDGE, SPAN), lambda turn: (0, turn)),
            pl.BlockSpec((1, NS, channels), lambda turn: (turn, 0, 0)),
            anywhere,
        ),
        scratch_shapes=[
            pltpu.VMEM((NS, channels), F32),
            pltpu.VMEM((EDGE, channels + 2 * NS), F32),
        ]
        + gather_sems(devices),
        compiler_params=pltpu.CompilerParams(collective_id=2, has_side_effects=True),
        cost_estimate=cost(20),
        name="scan_forward",
    )(proj, proj, proj, proj, *params, shard)


def run_scan_backward(
    proj, y, entering, dyg, scale, inner, dqkv, params, sent, windows, pieces, shapes,
    devices,
):
    tokens, width = proj.shape
    channels = params[0].shape[1]
    qkv_width = dqkv.shape[1]
    step_at = (2 * channels + 2 * NS + qkv_width) // LANES
    spans = tokens // SPAN
    bc_at = 2 * channels // (2 * NS)
    edges = SPAN // EDGE
    rows = lambda size, at: pl.BlockSpec((SPAN, size), lambda turn: (spans - 1 - turn, at))
    edge = lambda size, at: pl.BlockSpec(
        (EDGE, size), lambda turn: (jnp.maximum((spans - 1 - turn) * edges - 1, 0), at)
    )
    keep = lambda shape: pl.BlockSpec(shape, lambda turn: (0, 0))
    shapes = tuple(jax.ShapeDtypeStruct(shape, F32) for shape in shapes)
    return pl.pallas_call(
        functools.partial(
            scan_backward, devices, spans, windows, pieces, len(shapes), len(sent)
        ),
        grid=(spans,),
        out_shape=(
            jax.ShapeDtypeStruct((tokens, width), BF16),
            jax.ShapeDtypeStruct((EDGE, channels + 2 * NS), F32),
            jax.ShapeDtypeStruct((EDGE, LANES), F32),
        )
        + shapes,
        in_specs=[
            rows(channels, 0),
            rows(channels, 1),
            edge(channels, 1),
            rows(2 * NS, bc_at),
            edge(2 * NS, bc_at),
            rows(LANES, step_at),
            rows(channels, 0),
            pl.BlockSpec((1, NS, channels), lambda turn: (spans - 1 - turn, 0, 0)),
            rows(channels, 0),
            pl.BlockSpec((EDGE, SPAN), lambda turn: (0, spans - 1 - turn)),
            pl.BlockSpec((EDGE, SPAN), lambda turn: (0, spans - 1 - turn)),
            rows(qkv_width, 0),
        ]
        + [whole_spec(item) for item in params]
        + [pl.BlockSpec(memory_space=pl.ANY)] * len(sent),
        out_specs=(
            rows(width, 0),
            keep((EDGE, channels + 2 * NS)),
            keep((EDGE, LANES)),
        )
        + tuple(keep(item.shape) for item in shapes),
        scratch_shapes=[
            pltpu.VMEM((NS, channels), F32),
            pltpu.VMEM((EDGE, channels + 2 * NS), F32),
            pltpu.VMEM((SPAN, channels), F32),
            pltpu.VMEM((LANES, SPAN), F32),
        ]
        + scatter_scratch(windows, sent[0].shape[0] // devices, devices),
        compiler_params=pltpu.CompilerParams(collective_id=6, has_side_effects=True),
        cost_estimate=cost(47),
        name="scan_backward",
    )(
        proj, proj, proj, proj, proj, proj, y, entering, dyg, scale, inner, dqkv, *params, *sent,
    )


def rotary_tables(tokens):
    half = HEAD_SIZE // 2
    exponent = np.arange(half, dtype=np.float64) * (-2.0 * LOG_BASE / HEAD_SIZE)
    rates = np.tile(np.exp(exponent.astype(np.float32)).astype(np.float64), LANES // half)
    tables = []
    for places in (np.arange(FINE), np.arange(0, tokens, FINE)):
        angles = places[:, None] * rates[None, :]
        tables += [np.cos(angles).astype(np.float32), np.sin(angles).astype(np.float32)]
    return tables


def fill_rotary(fine_cos, fine_sin, coarse_cos, coarse_sin, cosine, sine):
    small_cos, small_sin = fine_cos[...], fine_sin[...]
    for turn in range(coarse_cos.shape[0]):
        big_cos, big_sin = coarse_cos[turn : turn + 1, :], coarse_sin[turn : turn + 1, :]
        rows = slice(turn * FINE, (turn + 1) * FINE)
        cosine[rows, :] = small_cos * big_cos - small_sin * big_sin
        sine[rows, :] = small_sin * big_cos + small_cos * big_sin


def head_masks():
    half = HEAD_SIZE // 2
    row, col = iota((LANES, LANES), 0), iota((LANES, LANES), 1)
    place = col % HEAD_SIZE
    ahead = jnp.where(place < half, -1.0, 0.0)
    behind = jnp.where(place < half, 0.0, 1.0)

    def turn(start):
        return jnp.where(row == start + half, ahead, jnp.where(row == start - half, behind, 0.0))

    first = row < HEAD_SIZE
    left = col < HEAD_SIZE
    low = lambda mask: mask.astype(BF16)
    within = low(turn(col))
    copy = low(jnp.where(row == place, 1.0, 0.0))
    copy_turn = low(jnp.where(first, turn(place), 0.0))
    value = low(jnp.where(row == place + HEAD_SIZE, 1.0, 0.0))
    fold = low(jnp.where(left & (row % HEAD_SIZE == place), 1.0, 0.0))
    other = row % HEAD_SIZE
    fold_turn = low(
        jnp.where(
            left,
            jnp.where(other == place + half, ahead, jnp.where(other == place - half, behind, 0.0)),
            0.0,
        )
    )
    fold_value = low(jnp.where(left, 0.0, jnp.where(other == place, 1.0, 0.0)))
    return within, copy, copy_turn, value, fold, fold_turn, fold_value


def attend_forward(
    q_ref, kv_ref, fine_cos, fine_sin, coarse_cos, coarse_sin,
    qkv_ref, lse_ref, o_ref, vt, cos_ref, sin_ref,
):
    fill_rotary(fine_cos, fine_sin, coarse_cos, coarse_sin, cos_ref, sin_ref)
    tokens, query_width = q_ref.shape
    pairs = query_width // LANES
    within, copy, copy_turn, value = head_masks()[:4]

    def turn_rows(i, carry):
        rows = pl.ds(pl.multiple_of(i * QBLK, QBLK), QBLK)
        cosine, sine = cos_ref[rows, :], sin_ref[rows, :]
        for pair in range(pairs):
            lanes = slice(pair * LANES, (pair + 1) * LANES)
            query = q_ref[rows, lanes]
            turned = query * cosine + pick(query, within) * sine
            qkv_ref[rows, lanes] = (turned * HEAD_SIZE**-0.5).astype(BF16)
        kv = kv_ref[rows, :]
        keys = pick(kv, copy) * cosine + pick(kv, copy_turn) * sine
        qkv_ref[rows, query_width : query_width + LANES] = keys.astype(BF16)
        qkv_ref[rows, query_width + LANES :] = dot(kv.astype(BF16), value).astype(BF16)
        vt[:, rows] = kv.T[HEAD_SIZE:, :].astype(BF16)
        return carry

    lax.fori_loop(0, tokens // QBLK, turn_rows, 0)
    low_lanes = iota((QBLK, LANES), 1) < HEAD_SIZE
    wide = (QBLK, 2 * QBLK)
    visible = iota(wide, 0) <= iota(wide, 1) % QBLK

    def block(i, carry):
        here = pl.ds(pl.multiple_of(i * QBLK, QBLK), QBLK)
        queries = [
            pair_split(qkv_ref[here, pair * LANES : (pair + 1) * LANES], low_lanes)
            for pair in range(pairs)
        ]

        def tile(there, state, edge):
            keys = qkv_ref[there, query_width : query_width + LANES]
            result = []
            for pair in range(pairs):
                top, total, out = state[3 * pair : 3 * pair + 3]
                scores = dot(keys, queries[pair], NT)
                if edge:
                    scores = jnp.where(visible, scores, MASKED)
                higher = jnp.maximum(top, jnp.max(scores, axis=0, keepdims=True))
                probs = jnp.exp(scores - higher)
                fade = jnp.exp(top - higher)
                total = total * fade + jnp.sum(probs, axis=0, keepdims=True)
                out = out * fade + dot(vt[:, there], probs.astype(BF16))
                result += [higher, total, out]
            return tuple(result)

        state = (
            jnp.full((1, 2 * QBLK), MASKED, F32),
            jnp.zeros((1, 2 * QBLK), F32),
            jnp.zeros((HEAD_SIZE, 2 * QBLK), F32),
        ) * pairs
        state = lax.fori_loop(
            0,
            i,
            lambda j, state: tile(pl.ds(pl.multiple_of(j * QBLK, QBLK), QBLK), state, False),
            state,
        )
        state = tile(here, state, True)
        for pair in range(pairs):
            top, total, out = state[3 * pair : 3 * pair + 3]
            out = out / total
            lse = top + jnp.log(total)
            lse_ref[2 * pair : 2 * pair + 1, here] = lse[:, :QBLK]
            lse_ref[2 * pair + 1 : 2 * pair + 2, here] = lse[:, QBLK:]
            both = jnp.concatenate([out[:, :QBLK], out[:, QBLK:]], axis=0)
            o_ref[here, pair * LANES : (pair + 1) * LANES] = both.T.astype(BF16)
        return carry

    lax.fori_loop(0, tokens // QBLK, block, 0)


def attend_backward(
    qkv_ref, lse_ref, o_ref, do_ref, fine_cos, fine_sin, coarse_cos, coarse_sin,
    dqkv_ref,
    dq, kt, dk, dv, cos_ref, sin_ref,
):
    fill_rotary(fine_cos, fine_sin, coarse_cos, coarse_sin, cos_ref, sin_ref)
    tokens, query_width = o_ref.shape
    pairs = query_width // LANES
    key_lanes = slice(query_width, query_width + LANES)
    value_lanes = slice(query_width + LANES, query_width + 2 * LANES)

    def turn_keys(i, carry):
        rows = pl.ds(pl.multiple_of(i * QBLK, QBLK), QBLK)
        kt[:, rows] = qkv_ref[rows, key_lanes].astype(F32).T[:HEAD_SIZE, :].astype(BF16)
        return carry

    lax.fori_loop(0, tokens // QBLK, turn_keys, 0)
    dk[...] = jnp.zeros_like(dk)
    dv[...] = jnp.zeros_like(dv)
    low_lanes = iota((QBLK, LANES), 1) < HEAD_SIZE
    wide = (QBLK, 2 * QBLK)
    visible = iota(wide, 0) <= iota(wide, 1) % QBLK
    ones = jnp.ones((EDGE, LANES), BF16)

    def block(i, carry):
        here = pl.ds(pl.multiple_of(i * QBLK, QBLK), QBLK)
        queries, grads, inners, lses = [], [], [], []
        for pair in range(pairs):
            lanes = slice(pair * LANES, (pair + 1) * LANES)
            queries.append(pair_split(qkv_ref[here, lanes], low_lanes))
            grad = do_ref[here, lanes]
            grads.append(pair_split(grad, low_lanes))
            both = pair_split(grad.astype(F32) * o_ref[here, lanes].astype(F32), low_lanes)
            high, low = parts(both, 2)
            inners.append((dot(ones, high, NT) + dot(ones, low, NT))[:1])
            lses.append(
                jnp.concatenate(
                    [
                        lse_ref[2 * pair : 2 * pair + 1, here],
                        lse_ref[2 * pair + 1 : 2 * pair + 2, here],
                    ],
                    axis=1,
                )
            )
        query_all = jnp.concatenate(queries, axis=0)
        grad_all = jnp.concatenate(grads, axis=0)

        def tile(there, state, edge):
            keys = qkv_ref[there, key_lanes]
            values = qkv_ref[there, value_lanes]
            all_probs, all_dscores, result = [], [], []
            for pair in range(pairs):
                probs = dot(keys, queries[pair], NT) - lses[pair]
                if edge:
                    probs = jnp.where(visible, probs, MASKED)
                probs = jnp.exp(probs)
                dprobs = dot(values, grads[pair], NT)
                dscores = (probs * (dprobs - inners[pair])).astype(BF16)
                all_probs.append(probs.astype(BF16))
                all_dscores.append(dscores)
                result.append(state[pair] + dot(kt[:, there], dscores))
            dv[there, :] += dot(jnp.concatenate(all_probs, axis=1), grad_all)
            dk[there, :] += dot(jnp.concatenate(all_dscores, axis=1), query_all)
            return tuple(result)

        state = (jnp.zeros((HEAD_SIZE, 2 * QBLK), F32),) * pairs
        state = lax.fori_loop(
            0,
            i,
            lambda j, state: tile(pl.ds(pl.multiple_of(j * QBLK, QBLK), QBLK), state, False),
            state,
        )
        state = tile(here, state, True)
        for pair in range(pairs):
            both = jnp.concatenate([state[pair][:, :QBLK], state[pair][:, QBLK:]], axis=0)
            dq[here, pair * LANES : (pair + 1) * LANES] = both.T
        return carry

    lax.fori_loop(0, tokens // QBLK, block, 0)
    masks = head_masks()
    within, (fold, fold_turn, fold_value) = masks[0], masks[4:]

    def turn_back(i, carry):
        rows = pl.ds(pl.multiple_of(i * QBLK, QBLK), QBLK)
        cosine, sine = cos_ref[rows, :], sin_ref[rows, :]
        for pair in range(pairs):
            lanes = slice(pair * LANES, (pair + 1) * LANES)
            grad = dq[rows, lanes]
            grad = grad * cosine - pick(grad, within) * sine
            dqkv_ref[rows, lanes] = (grad * HEAD_SIZE**-0.5).astype(BF16)
        grad = dk[rows, :]
        grad = pick(grad, fold) * cosine - pick(grad, fold_turn) * sine
        grad = grad + pick(dv[rows, :], fold_value)
        dqkv_ref[rows, query_width:] = grad.astype(BF16)
        return carry

    lax.fori_loop(0, tokens // QBLK, turn_back, 0)


def run_attend_forward(proj, query_at, query_width, tables):
    tokens = proj.shape[0]
    cols = lambda size, at: pl.BlockSpec((tokens, size), lambda turn: (0, at // size))
    return pl.pallas_call(
        attend_forward,
        grid=(1,),
        out_shape=(
            jax.ShapeDtypeStruct((tokens, query_width + 2 * LANES), BF16),
            jax.ShapeDtypeStruct((EDGE, tokens), F32),
            jax.ShapeDtypeStruct((tokens, query_width), BF16),
        ),
        in_specs=[
            cols(query_width, query_at),
            cols(2 * HEAD_SIZE, query_at + query_width),
        ]
        + [whole_spec(table) for table in tables],
        out_specs=(
            cols(query_width + 2 * LANES, 0),
            pl.BlockSpec((EDGE, tokens), lambda turn: (0, 0)),
            cols(query_width, 0),
        ),
        scratch_shapes=[
            pltpu.VMEM((HEAD_SIZE, tokens), BF16),
            pltpu.VMEM((tokens, LANES), F32),
            pltpu.VMEM((tokens, LANES), F32),
        ],
        cost_estimate=cost(15),
        name="attend_forward",
    )(proj, proj, *tables)


def run_attend_backward(qkv, lse, attended, grads, grad_at, tables):
    tokens, query_width = attended.shape
    vmem = pl.BlockSpec(memory_space=pltpu.VMEM)
    cols = lambda size, at: pl.BlockSpec((tokens, size), lambda turn: (0, at // size))
    return pl.pallas_call(
        attend_backward,
        grid=(1,),
        out_shape=jax.ShapeDtypeStruct((tokens, query_width + 2 * HEAD_SIZE), BF16),
        in_specs=[
            whole_spec(qkv),
            whole_spec(lse),
            whole_spec(attended),
            cols(query_width, grad_at),
        ]
        + [whole_spec(table) for table in tables],
        out_specs=cols(query_width + 2 * HEAD_SIZE, 0),
        scratch_shapes=[
            pltpu.VMEM((tokens, query_width), F32),
            pltpu.VMEM((HEAD_SIZE, tokens), BF16),
            pltpu.VMEM((tokens, LANES), F32),
            pltpu.VMEM((tokens, LANES), F32),
            pltpu.VMEM((tokens, LANES), F32),
            pltpu.VMEM((tokens, LANES), F32),
        ],
        cost_estimate=cost(16),
        name="attend_backward",
    )(qkv, lse, attended, grads, *tables)


def feed_forward(
    x_ref, mixed_ref, other_ref, act_grad_ref, norms_ref, gu_ref,
    after_ref, scale_ref, hidden_ref, act_ref, dgu_ref, back_ref,
):
    units = act_grad_ref.shape[1]
    after = x_ref[...].astype(F32) + (mixed_ref[...].astype(F32) + other_ref[...].astype(F32))
    after_ref[...] = after.astype(BF16)
    scale = lax.rsqrt(jnp.mean(after * after, axis=-1, keepdims=True) + EPSILON)
    scale_ref[...] = scale
    hidden = (after * scale * norms_ref[1:2, :]).astype(BF16)
    hidden_ref[...] = hidden
    for start in range(0, units, UBLK):
        cols = slice(start, start + UBLK)
        up_cols = slice(units + start, units + start + UBLK)
        gate = dot(hidden, gu_ref[:, cols])
        upward = dot(hidden, gu_ref[:, up_cols])
        grad = act_grad_ref[:, cols]
        sigma = jax.nn.sigmoid(gate)
        swish = gate * sigma
        act_ref[:, cols] = (swish * upward).astype(BF16)
        slope = sigma * (1.0 + gate * (1.0 - sigma))
        dgu_ref[:, cols] = (grad * upward * slope).astype(BF16)
        dgu_ref[:, up_cols] = (grad * swish).astype(BF16)
    back_ref[...] = dot(dgu_ref[...], gu_ref[...], NT).astype(BF16)


def product_rows(dims, left_ref, right_ref, out_ref):
    out_ref[...] = dot(left_ref[...], right_ref[...], dims).astype(out_ref.dtype)


def run_product(left, right, dims, dtype):
    tokens, depth = left.shape
    cols = right.shape[1 - dims[1][0]]
    return pl.pallas_call(
        functools.partial(product_rows, dims),
        grid=(tokens // TBLK,),
        out_shape=jax.ShapeDtypeStruct((tokens, cols), dtype),
        in_specs=[pl.BlockSpec((TBLK, depth), lambda turn: (turn, 0)), once(right)],
        out_specs=pl.BlockSpec((TBLK, cols), lambda turn: (turn, 0)),
        cost_estimate=cost(4),
        name="product_rows",
    )(left, right)


def project(heads, x_ref, w_ref, hidden_ref, proj_ref, norms_ref):
    @pl.when(pl.program_id(0) == 0)
    def _():
        gains = w_ref[:, w_ref.shape[1] - LANES :].astype(F32).T
        norms_ref[...] = jnp.zeros_like(norms_ref)
        norms_ref[0:2, :] = gains[heads : heads + 2, :]

    x = x_ref[...].astype(F32)
    scale = lax.rsqrt(jnp.mean(x * x, axis=-1, keepdims=True) + EPSILON)
    hidden = (x * scale * norms_ref[0:1, :]).astype(BF16)
    hidden_ref[...] = hidden
    proj_ref[...] = dot(hidden, w_ref[...])


def run_project(x, w_in, heads):
    tokens, width = x.shape
    cols = w_in.shape[1]
    rows = lambda size: pl.BlockSpec((TBLK, size), lambda turn: (turn, 0))
    return pl.pallas_call(
        functools.partial(project, heads),
        grid=(tokens // TBLK,),
        out_shape=(
            jax.ShapeDtypeStruct((tokens, width), BF16),
            jax.ShapeDtypeStruct((tokens, cols), F32),
            jax.ShapeDtypeStruct((EDGE, width), F32),
        ),
        in_specs=[rows(width), once(w_in)],
        out_specs=(
            rows(width), rows(cols), pl.BlockSpec((EDGE, width), lambda turn: (0, 0)),
        ),
        cost_estimate=cost(8),
        name="project",
    )(x, w_in)


def project_back(grad_ref, w_ref, x_ref, part_ref, gain_grad_ref):
    @pl.when(pl.program_id(0) == 0)
    def _():
        gain_grad_ref[...] = jnp.zeros_like(gain_grad_ref)

    x = x_ref[...].astype(F32)
    normed = x * lax.rsqrt(jnp.mean(x * x, axis=-1, keepdims=True) + EPSILON)
    part = dot(grad_ref[...], w_ref[...], NT).astype(BF16)
    part_ref[...] = part
    gain_grad_ref[:1, :] += jnp.sum(part.astype(F32) * normed, axis=0, keepdims=True)


def run_project_back(grads, w_in, x):
    tokens, width = x.shape
    cols = w_in.shape[1]
    rows = lambda size: pl.BlockSpec((TBLK, size), lambda turn: (turn, 0))
    return pl.pallas_call(
        project_back,
        grid=(tokens // TBLK,),
        out_shape=(
            jax.ShapeDtypeStruct((tokens, width), BF16),
            jax.ShapeDtypeStruct((EDGE, width), F32),
        ),
        in_specs=[rows(cols), once(w_in), rows(width)],
        out_specs=(rows(width), pl.BlockSpec((EDGE, width), lambda turn: (0, 0))),
        cost_estimate=cost(8),
        name="project_back",
    )(grads, w_in, x)


def once(item):
    return pl.BlockSpec(item.shape, lambda turn: (0,) * item.ndim, pipeline_mode=pl.Buffered(1))


def run_feed_forward(x, mixed, other, act_grad, norms, w_gate_up):
    tokens, width = x.shape
    units = act_grad.shape[1]
    rows = lambda size: pl.BlockSpec((TBLK, size), lambda turn: (turn, 0))
    shape = jax.ShapeDtypeStruct
    return pl.pallas_call(
        feed_forward,
        grid=(tokens // TBLK,),
        out_shape=(
            shape((tokens, width), BF16),
            shape((tokens, 1), F32),
            shape((tokens, width), BF16),
            shape((tokens, units), BF16),
            shape((tokens, 2 * units), BF16),
            shape((tokens, width), BF16),
        ),
        in_specs=[rows(width)] * 3 + [rows(units), once(norms), once(w_gate_up)],
        out_specs=(rows(width), rows(1), rows(width), rows(units), rows(2 * units), rows(width)),
        cost_estimate=cost(14),
        name="feed_forward",
    )(x, mixed, other, act_grad, norms, w_gate_up)


def mixer_forward(gated_ref, scale_ref, gain_ref, attended_ref, w_ref, low_ref, mixed_ref):
    channels = gated_ref.shape[1]
    scale = scale_ref[...].T[:, :1]
    low_ref[:, :channels] = (gated_ref[...].astype(F32) * scale * gain_ref[...]).astype(BF16)
    low_ref[:, channels:] = attended_ref[...]
    mixed_ref[...] = dot(low_ref[...], w_ref[...], NT).astype(BF16)


def run_mixer_forward(gated, scale, gain, attended, w_out):
    tokens, channels = gated.shape
    width, inner = w_out.shape
    rows = lambda size: pl.BlockSpec((TBLK, size), lambda turn: (turn, 0))
    return pl.pallas_call(
        mixer_forward,
        grid=(tokens // TBLK,),
        out_shape=(
            jax.ShapeDtypeStruct((tokens, inner), BF16),
            jax.ShapeDtypeStruct((tokens, width), BF16),
        ),
        in_specs=[
            rows(channels),
            pl.BlockSpec((EDGE, TBLK), lambda turn: (0, turn)),
            once(gain),
            rows(attended.shape[1]),
            once(w_out),
        ],
        out_specs=(rows(inner), rows(width)),
        cost_estimate=cost(5),
        name="mixer_forward",
    )(gated, scale, gain, attended, w_out)


def mixer_backward(
    part_ref, other_ref, after_ref, scale_ref, top_ref, norms_ref,
    w_ref, gated_ref, scale_m_ref, gain_m_ref,
    low_ref, mamba_ref, attended_ref, inner_ref, gain_grad_ref,
):
    channels = gated_ref.shape[1]

    @pl.when(pl.program_id(0) == 0)
    def _():
        gain_grad_ref[...] = jnp.zeros_like(gain_grad_ref)

    grad = part_ref[...].astype(F32) + other_ref[...].astype(F32)
    scale = scale_ref[...]
    normed = after_ref[...].astype(F32) * scale
    gain_grad_ref[:1, :] += jnp.sum(grad * normed, axis=0, keepdims=True)
    weighted = grad * norms_ref[1:2, :]
    mean = jnp.mean(weighted * normed, axis=-1, keepdims=True)
    total = top_ref[...].astype(F32) + scale * (weighted - normed * mean)
    low_ref[...] = total.astype(BF16)
    back = dot(low_ref[...], w_ref[...])
    mamba = back[:, :channels]
    mamba_ref[...] = mamba.astype(BF16)
    attended_ref[...] = back[:, channels:].astype(BF16)
    inner_ref[...] = row_sums(mamba * gain_m_ref[...] * gated_ref[...].astype(F32)) * scale_m_ref[...]


def run_mixer_backward(part, other, after, scale, top, norms, w_out, gated, scale_m, gain_m):
    tokens, width = after.shape
    channels = gated.shape[1]
    inner = w_out.shape[1]
    shape = jax.ShapeDtypeStruct
    rows = lambda size: pl.BlockSpec((NBLK, size), lambda turn: (turn, 0))
    lanes = pl.BlockSpec((EDGE, NBLK), lambda turn: (0, turn))
    return pl.pallas_call(
        mixer_backward,
        grid=(tokens // NBLK,),
        out_shape=(
            shape((tokens, width), BF16),
            shape((tokens, channels), BF16),
            shape((tokens, inner - channels), BF16),
            shape((EDGE, tokens), F32),
            shape((EDGE, width), F32),
        ),
        in_specs=[rows(width)] * 3
        + [rows(1), rows(width), once(norms), once(w_out), rows(channels), lanes, once(gain_m)],
        out_specs=(
            rows(width), rows(channels), rows(inner - channels), lanes,
            pl.BlockSpec((EDGE, width), lambda turn: (0, 0)),
        ),
        cost_estimate=cost(8),
        name="mixer_backward",
    )(part, other, after, scale, top, norms, w_out, gated, scale_m, gain_m)


def lane_row(ref, first, count):
    return jnp.concatenate([ref[i : i + 1, :] for i in range(first, first + count)], axis=1)


def own_lanes(ref, first, size):
    start = lax.axis_index("dp") * size
    row = ref[pl.ds(first + lax.div(start, LANES), 1), :]
    row = jnp.broadcast_to(row, (EDGE, LANES))
    return pltpu.roll(row, lax.rem(LANES - lax.rem(start, LANES), LANES), 1)[0, :size]


def finish_layer(
    norm_at, x_ref, norms_ref, part_ref, other_ref, grad_ref, after_ref, ffn_ref, ffn_other_ref,
    total_ref, *refs,
):
    count = (len(refs) - 9) // 2
    passed, out_ref, result_ref, handed = refs[:count], refs[count], refs[count + 1], refs[count + 2 :]
    tap_ref, bias_ref, gain_ref, step_ref, log_ref, skip_ref, norm_ref = handed[count:]

    @pl.when(pl.program_id(0) == 0)
    def _():
        for source, target in zip(passed, handed):
            target[...] = source[...]
        rows = tap_ref.shape[1] // LANES
        for tap in range(KCONV):
            tap_ref[tap : tap + 1, :] = lane_row(total_ref, tap * rows, rows)
        bias_ref[...] = lane_row(total_ref, KCONV * rows, rows)[0]
        gain_ref[...] = lane_row(total_ref, (KCONV + 1) * rows, rows)[0]
        at = (KCONV + 2) * rows
        for place, ref in enumerate((step_ref, log_ref, skip_ref)):
            ref[...] = total_ref[at + place : at + place + 1, :][0, : ref.shape[0]]
        norm_ref[...] = own_lanes(total_ref, norm_at, norm_ref.shape[0])

    x = x_ref[...].astype(F32)
    scale = lax.rsqrt(jnp.mean(x * x, axis=-1, keepdims=True) + EPSILON)
    normed = x * scale
    weighted = (part_ref[...].astype(F32) + other_ref[...].astype(F32)) * norms_ref[0:1, :]
    mean = jnp.mean(weighted * normed, axis=-1, keepdims=True)
    out_ref[...] = grad_ref[...].astype(F32) + scale * (weighted - normed * mean)
    ffn = ffn_ref[...].astype(F32) + ffn_other_ref[...].astype(F32)
    result_ref[...] = (after_ref[...].astype(F32) + ffn).astype(BF16)


def run_finish(
    x, norms, part, other, grad, after, ffn, ffn_other, total, passed, channels, heads, shard,
    norm_at,
):
    tokens, width = x.shape
    rows = pl.BlockSpec((TBLK, width), lambda turn: (turn, 0))
    shape = lambda *sizes: jax.ShapeDtypeStruct(sizes, F32)
    small = (
        shape(KCONV, channels), shape(channels), shape(channels), shape(heads), shape(heads),
        shape(heads), shape(shard),
    )
    return pl.pallas_call(
        functools.partial(finish_layer, norm_at),
        grid=(tokens // TBLK,),
        out_shape=(shape(tokens, width), jax.ShapeDtypeStruct((tokens, width), BF16))
        + tuple(shape(*item.shape) for item in passed)
        + small,
        in_specs=[rows, once(norms)] + [rows] * 6 + [once(total)] + [once(item) for item in passed],
        out_specs=(rows, rows) + tuple(once(item) for item in passed + small),
        cost_estimate=cost(8),
        name="finish_layer",
    )(x, norms, part, other, grad, after, ffn, ffn_other, total, *passed)


def finish_shared(at, total_ref, cross_ref, mine_ref, other_ref, bc_ref, tap_ref, bias_ref, norm_ref, both):
    half = lax.axis_index("tensor")
    cols = pl.ds(pl.multiple_of(half * LANES, LANES), LANES)
    bc_ref[...] = mine_ref[:, cols] + other_ref[:, cols]
    both[...] = total_ref[...] + cross_ref[...]
    for tap in range(KCONV):
        tap_ref[tap : tap + 1, :] = both[pl.ds(at + 2 * tap + half, 1), :]
    bias_ref[...] = both[pl.ds(at + 2 * KCONV + half, 1), :][0]
    norm_ref[...] = own_lanes(both, at + 2 * KCONV + 2, norm_ref.shape[0])


def run_finish_shared(total, cross, mine, other, shard, at):
    vmem = pl.BlockSpec(memory_space=pltpu.VMEM)
    shape = lambda *sizes: jax.ShapeDtypeStruct(sizes, F32)
    return pl.pallas_call(
        functools.partial(finish_shared, at),
        out_shape=(shape(mine.shape[0], LANES), shape(KCONV, LANES), shape(LANES), shape(shard)),
        in_specs=[vmem] * 4,
        out_specs=(vmem,) * 4,
        scratch_shapes=[pltpu.VMEM(total.shape, F32)],
        name="finish_shared",
    )(total, cross, mine, other)


def swap(partial):
    return lax.ppermute(partial, "tensor", [(0, 1), (1, 0)])


def join(mine, other):
    return mine.astype(F32) + other.astype(F32)


def tensor_sum(partial):
    return join(partial, swap(partial))


def thirds(size):
    part = size // 3
    return [(0, part), (part, 2 * part), (2 * part, size)]


def local(
    layer_input, w_norm1, w_zx, w_bc, w_dt, conv_x, conv_xb, conv_bc, conv_bcb, dt_bias, a_log,
    d_skip, w_mnorm, w_mout, query_key_value_weight, output_weight, w_norm2, w_gu, w_down,
    grad_output,
):
    devices = lax.axis_size("dp")
    tokens, width = layer_input.shape
    shard = w_zx.shape[0]
    channels = conv_xb.shape[0]
    heads = dt_bias.shape[0]
    qkv_width = query_key_value_weight.shape[2]
    units = w_down.shape[0]
    attn_width = output_weight.shape[1]
    tail = jnp.concatenate(
        [w_dt, w_norm1[:, None], w_norm2[:, None], jnp.zeros((shard, LANES - heads - 2), BF16)],
        axis=1,
    )
    mixer_in = jnp.concatenate(
        [w_zx.reshape(shard, -1), w_bc, query_key_value_weight.reshape(shard, -1), tail], axis=1
    )
    in_width = mixer_in.shape[1]
    (w_in,) = gather_rows([mixer_in], devices, 0, [(0, *window) for window in thirds(in_width)])
    hidden_one, proj, norms = run_project(layer_input, w_in, heads)
    params = scan_params(
        conv_x, conv_xb, conv_bc, conv_bcb, dt_bias, a_log, d_skip, w_mnorm
    )
    out_shard = jnp.concatenate([w_mout.T, output_weight.reshape(attn_width, -1).T], axis=1)
    y, gated, square_sum, entering, w_out = run_scan_forward(
        proj, qkv_width, params, out_shard, devices
    )
    channels_all = channels * lax.axis_size("tensor")
    scale_m = lax.rsqrt(tensor_sum(square_sum) / channels_all + EPSILON)
    tables = rotary_tables(tokens)
    qkv_at = 2 * channels + 2 * NS
    qkv, lse, attended = run_attend_forward(proj, qkv_at, attn_width, tables)
    gain_m = w_mnorm.astype(F32)[None, :]
    mixer_out, mixed = run_mixer_forward(gated, scale_m, gain_m, attended, w_out)
    mixed, gate_up_shard, down_shard = lax.optimization_barrier(
        (mixed, w_gu.reshape(shard, -1), w_down.T)
    )
    other = swap(mixed)
    w_gate_up, w_down_t = gather_rows(
        [gate_up_shard, down_shard],
        devices,
        3,
        [(0, 0, units), (0, units, 2 * units), (1, 0, units)],
    )
    act_grad = run_product(grad_output, w_down_t, NN, F32)
    other, w_gate_up, w_down_t, act_grad = lax.optimization_barrier(
        (other, w_gate_up, w_down_t, act_grad)
    )
    after, scale_two, hidden_two, activated, grad_gu_low, partial_two = run_feed_forward(
        layer_input, mixed, other, act_grad, norms, w_gate_up
    )
    other = swap(partial_two)
    grad_down = dot(grad_output, activated, TN).astype(BF16)
    (mine_gu,) = scatter_product(
        hidden_two,
        grad_gu_low,
        [
            ([(0, 1, 0, units)], [(0, 0, units, 0, 0)]),
            ([(0, 1, units, 2 * units)], [(0, 0, units, 0, 1)]),
        ],
        [(shard, 2, units)],
        devices,
        1,
    )
    ffn_part = run_product(activated, w_down_t, NT, BF16)
    other, mine_gu, grad_down, ffn_part = lax.optimization_barrier(
        (other, mine_gu, grad_down, ffn_part)
    )
    ffn_other = swap(ffn_part)
    grad_mix_low, grad_mamba, grad_attended, inner_m, grad_norm2 = run_mixer_backward(
        partial_two, other, after, scale_two, grad_output, norms, w_out, gated, scale_m, gain_m
    )
    inner_m = tensor_sum(inner_m) / channels_all
    dqkv = run_attend_backward(qkv, lse, attended, grad_attended, 0, tables)
    grad_out = dot(grad_mix_low, mixer_out, TN).astype(BF16)
    windows = [(0, None, 0, channels + attn_width), (1, None, 0, units)]
    pieces = [
        (0, 0, channels, 0, None),
        (0, channels, channels + attn_width, 1, None),
        (1, 0, units, 2, None),
    ]
    shapes = [(shard, channels), (shard, attn_width), (shard, units)]
    grad_proj, small_x, small_h, mine_mout, mine_o, mine_down = run_scan_backward(
        proj, y, entering, grad_mamba, scale_m, inner_m, dqkv, params,
        [grad_out, grad_down], windows, pieces, shapes, devices,
    )
    ffn_other, grad_proj = lax.optimization_barrier((ffn_other, grad_proj))
    partial_one, grad_norm1 = run_project_back(grad_proj, w_in, layer_input)
    partial_one, grad_proj = lax.optimization_barrier((partial_one, grad_proj))
    other = swap(partial_one)
    lanes_of = lambda size, start=0: range(start, start + size, LANES)
    places = [(0, row, lane) for row in range(KCONV + 2) for lane in lanes_of(channels)]
    places += [(1, row, 0) for row in range(3)]
    norm_at = len(places)
    places += [(2, 0, lane) for lane in lanes_of(width)]
    cross_at = len(places)
    places += [(0, row, lane) for row in range(KCONV + 1) for lane in lanes_of(2 * NS, channels)]
    places += [(3, 0, lane) for lane in lanes_of(width)]
    shared_at = 2 * channels
    step_at = qkv_at + qkv_width
    mine_zx, mine_bc, mine_qkv, mine_step, small = scatter_product(
        hidden_one,
        grad_proj,
        [
            ([(0, 1, 0, channels)], [(0, 0, channels, 0, 0)]),
            ([(0, 1, channels, shared_at)], [(0, 0, channels, 0, 1)]),
            (
                [(0, 1, shared_at, in_width)],
                [
                    (0, 0, 2 * NS, 1, None),
                    (0, 2 * NS, 2 * NS + qkv_width, 2, 0),
                    (0, 2 * NS + qkv_width, in_width - shared_at, 3, "turned"),
                ],
            ),
        ],
        [
            (shard, 2, channels),
            (shard, 2 * NS),
            (shard, 1, qkv_width),
            (heads, shard),
        ],
        devices,
        5,
        (small_x, small_h, grad_norm2, grad_norm1),
        places,
    )
    other, mine_bc = lax.optimization_barrier((other, mine_bc))
    passed = (mine_zx, mine_qkv, mine_step, mine_mout, mine_o, mine_gu, mine_down)
    cross, other_bc = swap(small), swap(mine_bc)
    grad_source, result, *rest = run_finish(
        layer_input, norms, partial_one, other, grad_mix_low, after, ffn_part, ffn_other, small,
        passed, channels, heads, shard, norm_at,
    )
    mine_zx, mine_qkv, mine_step, mine_mout, mine_o, mine_gu, mine_down = rest[: len(passed)]
    grad_taps, grad_bias, grad_gain, grad_steps, grad_log, grad_skip, own_norm2 = rest[len(passed) :]
    grad_bc, grad_tapsb, grad_biasb, own_norm1 = run_finish_shared(
        small, cross, mine_bc, other_bc, shard, cross_at
    )
    return (
        result,
        grad_source,
        own_norm1,
        mine_zx,
        grad_bc,
        mine_step.T,
        grad_taps,
        grad_bias,
        grad_tapsb,
        grad_biasb,
        grad_steps,
        grad_log,
        grad_skip,
        grad_gain,
        mine_mout.T,
        mine_qkv,
        mine_o.T.reshape(output_weight.shape),
        own_norm2,
        mine_gu,
        mine_down.T,
    )


def solution(mesh):
    return jax.shard_map(
        local,
        mesh=mesh,
        in_specs=(
            P("dp", None),
            P("dp"),
            P("dp", None, "tensor"),
            P("dp", None),
            P("dp", "tensor"),
            P(None, "tensor"),
            P("tensor"),
            P(),
            P(),
            P("tensor"),
            P("tensor"),
            P("tensor"),
            P("tensor"),
            P("tensor", "dp"),
            P("dp", "tensor", None),
            P("tensor", None, "dp"),
            P("dp"),
            P("dp", None, "tensor"),
            P("tensor", "dp"),
            P("dp", None),
        ),
        out_specs=(
            P("dp", None),
            P("dp", None),
            P("dp"),
            P("dp", None, "tensor"),
            P("dp", "tensor"),
            P("dp", "tensor"),
            P(None, "tensor"),
            P("tensor"),
            P(None, "tensor"),
            P("tensor"),
            P("tensor"),
            P("tensor"),
            P("tensor"),
            P("tensor"),
            P("tensor", "dp"),
            P("dp", "tensor", None),
            P("tensor", None, "dp"),
            P("dp"),
            P("dp", None, "tensor"),
            P("tensor", "dp"),
        ),
        check_vma=False,
    )
```

```python
import functools
import math

import jax
import jax.numpy as jnp
import numpy as np
from jax import lax
from jax.experimental import pallas as pl
from jax.experimental.pallas import tpu as pltpu
from jax.sharding import PartitionSpec as P

HEAD_SIZE = 64
MP = 64
NS = 128
KCONV = 4
SPAN = 128
QBLK = 256
FINE = 32
TBLK = 256
NBLK = 128
UBLK = 256
LANES = 128
EDGE = 8

EPSILON = 1e-05
HIGHEST = lax.Precision.HIGHEST
LOG_BASE = math.log(100000000000.0)
MASKED = -1e30
MESH = pl.DeviceIdType.MESH
F32 = jnp.float32
BF16 = jnp.bfloat16

NN = ((1,), (0,))
NT = ((1,), (1,))
TN = ((0,), (0,))


def dot(left, right, dims=NN, precision=None):
    return lax.dot_general(
        left, right, (dims, ((), ())), preferred_element_type=F32, precision=precision
    )


def iota(shape, dim):
    return lax.broadcasted_iota(jnp.int32, shape, dim)


def ring_place(chip, chips):
    odd = lax.rem(chip, 2)
    half = lax.div(chip, 2)
    return (1 - odd) * half + odd * (chips - 1 - half)


def ring_chip(place, chips):
    place = lax.rem(place + 4 * chips, chips)
    back = lax.div(place, chips // 2)
    return (1 - back) * (2 * place) + back * (2 * (chips - 1 - place) + 1)


def ring_setup(chips):
    me = lax.axis_index("dp")
    group = lax.axis_index("tensor")
    chip = lax.div(me, 2)
    core = lax.rem(me, 2)
    place = ring_place(chip, chips)
    right = ring_chip(place + 1, chips) * 2 + core
    left = ring_chip(place - 1, chips) * 2 + core
    mate = chip * 2 + (1 - core)
    barrier = pltpu.get_barrier_semaphore()
    for other in (right, left, mate):
        pl.semaphore_signal(barrier, inc=1, device_id=(other, group), device_id_type=MESH)
    pl.semaphore_wait(barrier, 3)
    return me, group, core, place, right, left, mate


class RingGather:
    def __init__(self, devices, x_ref, o_ref, sems, cols=slice(None)):
        self.cols = cols
        self.chips = devices // 2
        self.ahead = self.chips // 2
        self.behind = self.chips - 1 - self.ahead
        self.x_ref, self.o_ref, self.rows = x_ref, o_ref, x_ref.shape[0]
        self.fs, self.fr, self.bs, self.br, self.cs, self.cr, self.own_sem = sems

    def locate(self):
        me = lax.axis_index("dp")
        self.group = lax.axis_index("tensor")
        self.core = lax.rem(me, 2)
        chip = lax.div(me, 2)
        self.place = ring_place(chip, self.chips)
        self.right = ring_chip(self.place + 1, self.chips) * 2 + self.core
        self.left = ring_chip(self.place - 1, self.chips) * 2 + self.core
        self.mate = chip * 2 + (1 - self.core)
        self.me = me

    def slot(self, index):
        rows = pl.ds(pl.multiple_of(index * self.rows, self.rows), self.rows)
        return self.o_ref.at[rows, self.cols]

    def copy(self, shift, ssem, rsem, target):
        if shift == 0:
            index, source = self.me, self.x_ref.at[:, self.cols]
        else:
            index = ring_chip(self.place + shift, self.chips) * 2 + self.core
            source = self.slot(index)
        return pltpu.make_async_remote_copy(
            src_ref=source,
            dst_ref=self.slot(index),
            send_sem=ssem,
            recv_sem=rsem,
            device_id=(target, self.group),
            device_id_type=MESH,
        )

    def fore(self, step):
        return self.copy(-step, self.fs.at[step], self.fr.at[step], self.right)

    def back(self, step):
        return self.copy(step, self.bs.at[step], self.br.at[step], self.left)

    def across(self, shift):
        number = 0 if shift == 0 else 2 * abs(shift) - (1 if shift < 0 else 0)
        return self.copy(shift, self.cs.at[number], self.cr.at[number], self.mate)

    def own(self):
        return pltpu.make_async_copy(
            self.x_ref.at[:, self.cols], self.slot(self.me), self.own_sem
        )

    def greet(self):
        self.locate()
        barrier = pltpu.get_barrier_semaphore()
        for other in (self.right, self.left, self.mate):
            pl.semaphore_signal(
                barrier, inc=1, device_id=(other, self.group), device_id_type=MESH
            )
        pl.semaphore_wait(barrier, 3)

    def begin(self):
        self.locate()
        self.fore(0).start()
        self.back(0).start()
        self.across(0).start()
        self.own().start()

    def hop(self, step):
        self.locate()
        self.fore(step - 1).wait_recv()
        if step < self.ahead:
            self.fore(step).start()
        self.across(-step).start()
        if step <= self.behind:
            self.back(step - 1).wait_recv()
            if step < self.behind:
                self.back(step).start()
            self.across(step).start()

    def finish(self):
        self.locate()
        self.own().wait()
        for step in range(self.ahead):
            self.fore(step).wait_send()
        for step in range(self.behind):
            self.back(step).wait_send()
        for shift in range(-self.ahead, self.behind + 1):
            self.across(shift).wait()


def gather_sems(devices):
    dma = pltpu.SemaphoreType.DMA
    return [dma((devices // 2,))] * 6 + [dma(())]


def gather_shape(shard, devices):
    return jax.ShapeDtypeStruct((shard.shape[0] * devices, shard.shape[1]), shard.dtype)


def gather_kernel(devices, count, windows, *refs):
    shards, outs, sems = refs[:count], refs[count : 2 * count], refs[2 * count :]
    each = len(sems) // len(windows)
    rings = [
        RingGather(
            devices, shards[i], outs[i], sems[place * each : (place + 1) * each], slice(first, last)
        )
        for place, (i, first, last) in enumerate(windows)
    ]
    rings[0].greet()
    for ring in rings:
        ring.begin()
    for step in range(1, rings[0].ahead + 1):
        for ring in rings:
            ring.hop(step)
    for ring in rings:
        ring.finish()


def cost(micros):
    return pl.CostEstimate(flops=int(micros * 1e9), bytes_accessed=0, transcendentals=0)


def gather_rows(shards, devices, collective, windows):
    count = len(shards)
    anywhere = pl.BlockSpec(memory_space=pl.ANY)
    return pl.pallas_call(
        functools.partial(gather_kernel, devices, count, windows),
        out_shape=tuple(gather_shape(shard, devices) for shard in shards),
        in_specs=[anywhere] * count,
        out_specs=(anywhere,) * count,
        scratch_shapes=gather_sems(devices) * len(windows),
        compiler_params=pltpu.CompilerParams(collective_id=collective, has_side_effects=True),
        cost_estimate=cost(3),
        name="gather_rows",
    )(*shards)


def scatter_order(chips):
    ahead = chips // 2
    behind = chips - 1 - ahead
    order = []
    for step in range(ahead):
        order.append(-(ahead - step))
        if step < behind:
            order.append(behind - step)
    order.append(0)
    return order


class RingScatter:
    def __init__(self, devices, windows, pieces, operands, outs, scratch):
        self.chips = devices // 2
        self.ahead = self.chips // 2
        self.behind = self.chips - 1 - self.ahead
        self.windows, self.pieces, self.operands, self.outs = windows, pieces, operands, outs
        count = len(windows)
        self.mine, self.boxes, rest = scratch[:count], scratch[count : 2 * count], scratch[2 * count :]
        self.fbox, self.bbox, self.fout, self.bout = rest[:4]
        self.os, self.ms, self.mr, self.fs, self.fr, self.bs, self.br = rest[4:]
        self.rows = self.fbox.shape[1]
        widths = [item.shape[2] for item in self.mine]
        self.cols = [slice(sum(widths[:i]), sum(widths[: i + 1])) for i in range(count)]

    def locate(self):
        me = lax.axis_index("dp")
        self.group = lax.axis_index("tensor")
        self.core = lax.rem(me, 2)
        chip = lax.div(me, 2)
        self.place = ring_place(chip, self.chips)
        self.right = ring_chip(self.place + 1, self.chips) * 2 + self.core
        self.left = ring_chip(self.place - 1, self.chips) * 2 + self.core
        self.mate = chip * 2 + (1 - self.core)

    def greet(self):
        self.locate()
        barrier = pltpu.get_barrier_semaphore()
        for other in (self.right, self.left, self.mate):
            pl.semaphore_signal(
                barrier, inc=1, device_id=(other, self.group), device_id_type=MESH
            )
        pl.semaphore_wait(barrier, 3)

    def product(self, i):
        return self.windows[i][1] is not None

    def shift_of(self, slot):
        step = slot // 2
        odd = slot % 2
        return (1 - odd) * (step - self.ahead) + odd * (self.behind - step)

    def half(self, which):
        return pl.ds(pl.multiple_of(which * self.rows, self.rows), self.rows)

    def block(self, i, slot, which):
        index = ring_chip(self.place + self.shift_of(slot), self.chips) * 2 + which
        left, right, first, last = self.windows[i]
        return self.operands[left].at[self.half(index), first:last]

    def remote(self, source, target_ref, ssem, rsem, target):
        return pltpu.make_async_remote_copy(
            src_ref=source,
            dst_ref=target_ref,
            send_sem=ssem,
            recv_sem=rsem,
            device_id=(target, self.group),
            device_id_type=MESH,
        )

    def across(self, i, slot):
        if self.product(i):
            source = self.mine[i].at[slot, self.half(1 - self.core)]
        else:
            source = self.block(i, slot, 1 - self.core)
        return self.remote(
            source, self.boxes[i].at[slot], self.ms.at[i, slot], self.mr.at[i, slot], self.mate
        )

    def own(self, i, slot):
        return pltpu.make_async_copy(
            self.block(i, slot, self.core), self.mine[i].at[slot], self.os.at[i, slot]
        )

    def fore(self, step):
        return self.remote(
            self.fout.at[step], self.fbox.at[step], self.fs.at[step], self.fr.at[step], self.right
        )

    def back(self, step):
        return self.remote(
            self.bout.at[step], self.bbox.at[step], self.bs.at[step], self.br.at[step], self.left
        )

    def begin(self):
        self.locate()
        for i in range(len(self.windows)):
            if not self.product(i):
                for slot in range(self.chips):
                    self.across(i, slot).start()
                    self.own(i, slot).start()

    def produce(self, slot):
        chip = ring_chip(self.place + self.shift_of(slot), self.chips)
        size = 2 * self.rows
        for i, (left, right, first, last) in enumerate(self.windows):
            if right is None:
                continue
            at = pl.multiple_of(chip * size, size)
            terms = dot(self.operands[left][pl.ds(at, size), :], self.operands[right][:, first:last])
            self.mine[i][slot] = terms.astype(BF16)
            self.across(i, slot).start()

    def local_sum(self, i, slot, cols, others):
        rows = self.half(self.core) if self.product(i) else slice(None)
        total = self.mine[i][slot, rows, cols].astype(F32) + self.boxes[i][slot, :, cols].astype(F32)
        whole = slice(self.cols[i].start + cols.start, self.cols[i].start + cols.stop)
        for ref in others:
            total = total + ref[:, whole].astype(F32)
        return total

    def arrive(self, slot):
        for i in range(len(self.windows)):
            if not self.product(i):
                self.own(i, slot).wait()
            self.across(i, slot).wait_recv()

    def put(self, target, slot, others):
        self.arrive(slot)
        for i, cols in enumerate(self.cols):
            total = self.local_sum(i, slot, slice(0, cols.stop - cols.start), others)
            target[:, cols] = total.astype(BF16)

    def hop_back(self, step, later):
        if later:
            self.back(step - 1).wait_recv()
        self.put(self.bout.at[step], 2 * step, [self.bbox.at[step - 1]] if later else [])
        self.back(step).start()

    def hop_fore(self, step, later):
        if later:
            self.fore(step - 1).wait_recv()
        self.put(self.fout.at[step], 2 * step + 1, [self.fbox.at[step - 1]] if later else [])
        self.fore(step).start()

    def hop(self, step):
        self.locate()
        self.hop_back(step, step > 0)
        if step < self.behind:
            self.hop_fore(step, step > 0)

    def finish(self):
        self.locate()
        slot = self.chips - 1
        self.arrive(slot)
        self.fore(self.behind - 1).wait_recv()
        self.back(self.ahead - 1).wait_recv()
        others = [self.fbox.at[self.behind - 1], self.bbox.at[self.ahead - 1]]
        for i, first, last, out, form in self.pieces:
            total = self.local_sum(i, slot, slice(first, last), others)
            if form == "turned":
                self.outs[out][...] = total.T[: self.outs[out].shape[0]]
            elif form is None:
                self.outs[out][...] = total
            else:
                self.outs[out][:, form, :] = total
        for step in range(self.ahead):
            self.back(step).wait_send()
        for step in range(self.behind):
            self.fore(step).wait_send()
        for slot in range(self.chips):
            for i in range(len(self.windows)):
                self.across(i, slot).wait_send()


def run_rings(rings, after_first=None):
    ahead, behind = rings[0].ahead, rings[0].behind

    def turn(step, carry):
        def part(odd, kept):
            for ring in rings:
                ring.produce(2 * step + odd)
            return kept

        lax.fori_loop(0, 2, part, 0)

        @pl.when(step == 0)
        def _():
            for ring in rings:
                ring.hop_back(0, False)
                ring.hop_fore(0, False)
            if after_first is not None:
                after_first()

        @pl.when(step > 0)
        def _():
            for ring in rings:
                ring.hop_back(step, True)
                pl.when(step < behind)(functools.partial(ring.hop_fore, step, True))

        return carry

    lax.fori_loop(0, ahead, turn, 0)


def scatter_scratch(windows, rows, devices):
    chips = devices // 2
    count = len(windows)
    dma = pltpu.SemaphoreType.DMA
    widths = [last - first for left, right, first, last in windows]
    mine = [
        pltpu.VMEM((chips, rows if right is None else 2 * rows, last - first), BF16)
        for left, right, first, last in windows
    ]
    boxes = [pltpu.VMEM((chips, rows, width), BF16) for width in widths]
    box = pltpu.VMEM((chips // 2, rows, sum(widths)), BF16)
    return mine + boxes + [box] * 4 + [dma((count, chips))] * 3 + [dma((chips,))] * 4


class Total:
    def __init__(self, devices, x_ref, o_ref, scratch):
        self.chips = devices // 2
        self.x_ref, self.o_ref = x_ref, o_ref
        self.mate_box, self.joined, self.boxes, self.ms, self.mr, self.ss, self.sr = scratch
        me = lax.axis_index("dp")
        self.group = lax.axis_index("tensor")
        self.chip = lax.div(me, 2)
        core = lax.rem(me, 2)
        self.mate = self.chip * 2 + (1 - core)
        self.peers = [
            lax.rem(self.chip + shift, self.chips) * 2 + core for shift in range(self.chips)
        ]

    def greet(self):
        barrier = pltpu.get_barrier_semaphore()
        for other in [self.mate] + self.peers[1:]:
            pl.semaphore_signal(
                barrier, inc=1, device_id=(other, self.group), device_id_type=MESH
            )
        pl.semaphore_wait(barrier, self.chips)

    def remote(self, source, target_ref, ssem, rsem, target):
        return pltpu.make_async_remote_copy(
            src_ref=source,
            dst_ref=target_ref,
            send_sem=ssem,
            recv_sem=rsem,
            device_id=(target, self.group),
            device_id_type=MESH,
        )

    def across(self):
        return self.remote(self.x_ref, self.mate_box, self.ms, self.mr, self.mate)

    def copies(self):
        return [
            self.remote(
                self.joined,
                self.boxes.at[self.chip],
                self.ss.at[shift],
                self.sr.at[shift],
                self.peers[shift],
            )
            for shift in range(1, self.chips)
        ]

    def begin(self):
        self.across().start()

    def spread(self):
        self.across().wait_recv()
        self.joined[...] = self.x_ref[...] + self.mate_box[...]
        for copy in self.copies():
            copy.start()
        self.boxes[self.chip] = self.joined[...]

    def finish(self):
        for copy in self.copies():
            copy.wait_recv()
        result = self.boxes[0]
        for other in range(1, self.chips):
            result = result + self.boxes[other]
        self.o_ref[...] = result
        self.across().wait_send()
        for copy in self.copies():
            copy.wait_send()


def total_scratch(values, devices):
    chips = devices // 2
    dma = pltpu.SemaphoreType.DMA
    return [
        pltpu.VMEM(values.shape, F32),
        pltpu.VMEM(values.shape, F32),
        pltpu.VMEM((chips,) + values.shape, F32),
        dma(()),
        dma(()),
        dma((chips,)),
        dma((chips,)),
    ]


def turned_copy(source, target):
    for start in range(0, source.shape[1], LANES):
        target[start : start + LANES, :] = source[:, start : start + LANES].T


def product_kernel(devices, groups, outs, places, summed, left_ref, right_ref, *refs):
    values = refs[:summed]
    refs = refs[summed:]
    pieces_out, refs = refs[:outs], refs[outs:]
    total = None
    if summed:
        total_out, refs = refs[0], refs[1:]
    turned, scratch = refs[0], refs[1:]
    if summed:
        scratch, rest = scratch[:-8], scratch[-8:]
        together = rest[0]
        together[...] = jnp.zeros_like(together)
        for at, (which, row, lane) in enumerate(places):
            together[at : at + 1, :] = values[which][row : row + 1, lane : lane + LANES]
        total = Total(devices, together, total_out, rest[1:])
    each = len(scratch) // len(groups)
    rings = [
        RingScatter(
            devices, windows, pieces, (turned, right_ref), pieces_out,
            scratch[place * each : (place + 1) * each],
        )
        for place, (windows, pieces) in enumerate(groups)
    ]
    if total is None:
        rings[0].greet()
    else:
        total.greet()
        total.begin()
    for ring in rings:
        ring.locate()
    turned_copy(left_ref, turned)
    run_rings(rings, total.spread if total is not None else None)
    for ring in rings:
        ring.finish()
    if total is not None:
        total.finish()


def scatter_product(left, right, groups, shapes, devices, collective, values=(), places=()):
    vmem = pl.BlockSpec(memory_space=pltpu.VMEM)
    rows = left.shape[1] // devices
    scratch = [pltpu.VMEM(left.shape[::-1], BF16)]
    for windows, pieces in groups:
        scratch += scatter_scratch(windows, rows, devices)
    totals = ()
    if values:
        total = jax.ShapeDtypeStruct((len(places) + -len(places) % EDGE, LANES), F32)
        totals = (total,)
        scratch += [pltpu.VMEM(total.shape, F32)] + total_scratch(total, devices)
    return pl.pallas_call(
        functools.partial(
            product_kernel, devices, groups, len(shapes), places, len(values)
        ),
        out_shape=tuple(jax.ShapeDtypeStruct(shape, F32) for shape in shapes) + totals,
        in_specs=[vmem] * (2 + len(values)),
        out_specs=(vmem,) * (len(shapes) + len(totals)),
        scratch_shapes=scratch,
        compiler_params=pltpu.CompilerParams(collective_id=collective, has_side_effects=True),
        cost_estimate=cost(3),
        name="scatter_product",
    )(left, right, *values)


def head_spread(channels):
    return (iota((LANES, channels), 1) // MP == iota((LANES, channels), 0)).astype(BF16)


def parts(values, count):
    terms = []
    for _ in range(count):
        term = values.astype(BF16)
        terms.append(term)
        values = values - term.astype(F32)
    return terms


def pick(values, mask, count=2):
    return dot(jnp.concatenate(parts(values, count), axis=1), jnp.concatenate([mask] * count, axis=0))


def pick_left(mask, values, count):
    return dot(jnp.concatenate([mask] * count, axis=1), jnp.concatenate(parts(values, count), axis=0))


def gather_heads(values, spread):
    high, low = parts(values, 2)
    return dot(high, spread, NT) + dot(low, spread, NT)


def row_sums(values):
    high, low = parts(values, 2)
    ones = jnp.ones((EDGE, values.shape[1]), BF16)
    return dot(ones, high, NT) + dot(ones, low, NT)


def soft_step(raw):
    return jnp.maximum(raw, 0.0) + jnp.log1p(jnp.exp(-jnp.abs(raw)))


def window(buffer, start, span):
    return buffer[start : start + span, :]


def causal_taps(buffer, taps, span):
    total = taps[0:1, :] * window(buffer, EDGE - KCONV + 1, span)
    for tap in range(1, KCONV):
        total = total + taps[tap : tap + 1, :] * window(buffer, EDGE - KCONV + 1 + tap, span)
    return total


def span_rates(step_ref, bias, decay, spread, span):
    raw = step_ref[...] + bias
    step = soft_step(raw)
    lower = (iota((span, span), 1) <= iota((span, span), 0)).astype(BF16)
    cum = pick_left(lower, step * decay, 3)
    tails = jnp.exp(cum[span - 1 : span, :] - cum)
    wide = pick(jnp.concatenate([step, tails, jnp.exp(cum)], axis=0), spread)
    return raw, step, cum, wide[:span], wide[span : 2 * span], wide[2 * span :]


def pair_split(values, low_lanes):
    zero = jnp.zeros_like(values)
    return jnp.concatenate(
        [jnp.where(low_lanes, values, zero), jnp.where(low_lanes, zero, values)], axis=0
    )


def pair_decay(cum, cum_rows, pair, causal):
    parts = []
    for head in (2 * pair, 2 * pair + 1):
        differ = cum[:, head : head + 1] - cum_rows[head : head + 1, :]
        parts.append(jnp.exp(jnp.where(causal, differ, MASKED)))
    return parts


def scan_forward(
    devices, spans,
    z_ref, x_ref, bc_ref, step_ref,
    tap_ref, tapb_ref, row_ref, shard_ref,
    y_ref, gated_ref, square_ref, enter_ref, all_ref,
    state, buffer, *sems,
):
    span, channels = x_ref.shape
    ring = RingGather(devices, shard_ref, all_ref, sems)
    turn = pl.program_id(0)

    @pl.when(turn == 0)
    def _():
        ring.greet()
        ring.begin()


    @pl.when(pl.program_id(0) == 0)
    def _():
        state[...] = jnp.zeros_like(state)
        buffer[span:, :] = jnp.zeros((EDGE, buffer.shape[1]), F32)

    buffer[:EDGE, :] = buffer[span:, :]
    buffer[EDGE:, :channels] = x_ref[...]
    buffer[EDGE:, channels:] = bc_ref[...]
    spread = head_spread(channels)
    bias, gain, biasb, stepb, decay, skip = unpack_rows(row_ref, spread)
    taps = jnp.concatenate([tap_ref[...], tapb_ref[...]], axis=1).astype(F32)
    conv = causal_taps(buffer, taps, span)
    conv = jax.nn.silu(conv + jnp.concatenate([bias, biasb], axis=1))
    inputs, shared = conv[:, :channels], conv[:, channels:]
    raw, step, cum, step_w, tails_w, grown_w = span_rates(step_ref, stepb, decay, spread, span)
    cum_rows = cum.T
    b_low = shared[:, :NS].astype(BF16)
    c_low = shared[:, NS:].astype(BF16)
    scaled = inputs * step_w
    scaled_low = scaled.astype(BF16)
    enter_ref[0] = state[...]
    outer = dot(c_low, state[...].astype(BF16)) * grown_w
    fresh = dot(b_low, (scaled * tails_w).astype(BF16), TN)
    state[...] = state[...] * grown_w[span - 1 : span, :] + fresh
    cross = dot(c_low, b_low, NT)
    causal = iota((span, span), 1) <= iota((span, span), 0)
    low_lanes = iota((span, LANES), 1) < MP
    for pair in range(channels // LANES):
        lanes = slice(pair * LANES, (pair + 1) * LANES)
        first, second = pair_decay(cum, cum_rows, pair, causal)
        weights = jnp.concatenate(
            [(cross * first).astype(BF16), (cross * second).astype(BF16)], axis=1
        )
        y_ref[:, lanes] = dot(weights, pair_split(scaled_low[:, lanes], low_lanes))
    y = y_ref[...] + outer + skip * inputs
    y_ref[...] = y
    gated = y * jax.nn.silu(z_ref[...])
    gated_ref[...] = gated.astype(BF16)
    square_ref[...] = row_sums(gated * gated)

    count = spans
    for step in range(1, ring.ahead + 1):
        pl.when(turn == min(count - 1, count * step // ring.ahead))(
            functools.partial(ring.hop, step)
        )
    pl.when(turn == count - 1)(ring.finish)


def scan_backward(
    devices, spans, windows, pieces, outs_count, count,
    z_ref, x_ref, xp_ref, bc_ref, bp_ref, step_ref, y_ref, enter_ref,
    dyg_ref, scale_ref, inner_ref, dqkv_ref,
    tap_ref, tapb_ref, row_ref,
    *refs,
):
    sent, refs = refs[:count], refs[count:]
    (grad_ref, gx_ref, gh_ref), refs = refs[:3], refs[3:]
    outs, refs = refs[:outs_count], refs[outs_count:]
    (dstate, buffer, dbuffer, du_buf, col_buf), scratch = refs[:5], refs[5:]
    ring = RingScatter(devices, windows, pieces, sent, outs, scratch)
    span, channels = x_ref.shape
    turn = pl.program_id(0)

    @pl.when(turn == 0)
    def _():
        ring.greet()
        ring.begin()
        dstate[...] = jnp.zeros_like(dstate)
        dbuffer[...] = jnp.zeros_like(dbuffer)
        col_buf[...] = jnp.zeros_like(col_buf)
        gx_ref[...] = jnp.zeros_like(gx_ref)
        gh_ref[...] = jnp.zeros_like(gh_ref)

    inside = (turn < spans - 1).astype(F32)
    buffer[:EDGE, :channels] = xp_ref[...] * inside
    buffer[:EDGE, channels:] = bp_ref[...] * inside
    buffer[EDGE:, :channels] = x_ref[...]
    buffer[EDGE:, channels:] = bc_ref[...]
    spread = head_spread(channels)
    bias, gain, biasb, stepb, decay, skip = unpack_rows(row_ref, spread)
    taps = jnp.concatenate([tap_ref[...], tapb_ref[...]], axis=1).astype(F32)
    conv = causal_taps(buffer, taps, span) + jnp.concatenate([bias, biasb], axis=1)
    sig = jax.nn.sigmoid(conv)
    swished = conv * sig
    inputs, shared = swished[:, :channels], swished[:, channels:]
    b_low = shared[:, :NS].astype(BF16)
    c_low = shared[:, NS:].astype(BF16)
    raw, step, cum, step_w, tails_w, grown_w = span_rates(step_ref, stepb, decay, spread, span)
    cum_rows = cum.T
    scaled = inputs * step_w
    scaled_low = scaled.astype(BF16)

    z = z_ref[...]
    sig_z = jax.nn.sigmoid(z)
    swish = z * sig_z
    y = y_ref[...]
    scale = scale_ref[...].T[:, :1]
    normed = y * swish * scale
    dyg = dyg_ref[...]
    gain_grad = jnp.sum(dyg * normed, axis=0, keepdims=True)
    dgated = scale * (dyg * gain - normed * inner_ref[...].T[:, :1])
    dy = dgated * swish
    grad_ref[:, :channels] = (dgated * y * (sig_z * (1.0 + z * (1.0 - sig_z)))).astype(BF16)

    state_low = enter_ref[0].astype(BF16)
    dstate_low = dstate[...].astype(BF16)
    grown_low = (dy * grown_w).astype(BF16)
    dy_low = dy.astype(BF16)
    tailed = scaled * tails_w
    outer = dot(c_low, state_low) * grown_w
    from_state = dot(b_low, dstate_low)
    dc = dot(grown_low, state_low, NT)
    db = dot(tailed.astype(BF16), dstate_low, NT)
    leak = from_state * tailed
    last_w = grown_w[span - 1 : span, :]
    ends = (
        jnp.sum(leak, axis=0, keepdims=True)
        + jnp.sum(enter_ref[0] * dstate[...], axis=0, keepdims=True) * last_w
    )
    skips = jnp.sum(dy * inputs, axis=0, keepdims=True)
    dstate[...] = dstate[...] * last_w + dot(c_low, grown_low, TN)

    cross = dot(c_low, b_low, NT)
    causal = iota((span, span), 1) <= iota((span, span), 0)
    low_lanes = iota((span, LANES), 1) < MP
    lane = iota((span, LANES), 1)
    dcross = jnp.zeros((span, span), F32)
    row_part = jnp.zeros((span, LANES), F32)
    for pair in range(channels // LANES):
        lanes = slice(pair * LANES, (pair + 1) * LANES)
        decays = pair_decay(cum, cum_rows, pair, causal)
        dy_pair = pair_split(dy_low[:, lanes], low_lanes)
        dweights = dot(dy_pair, scaled_low[:, lanes], NT)
        both = []
        for part in range(2):
            head = 2 * pair + part
            dterm = dweights[part * span : (part + 1) * span] * decays[part]
            dcross = dcross + dterm
            flow = dterm * cross
            row_part = row_part + jnp.where(
                lane == head, jnp.sum(flow, axis=1, keepdims=True), 0.0
            )
            col_buf[head : head + 1, :] = jnp.sum(flow, axis=0, keepdims=True)
            both.append((cross * decays[part]).astype(BF16))
        du_buf[:, lanes] = dot(jnp.concatenate(both, axis=0), dy_pair, TN)
    du = du_buf[...] + from_state * tails_w
    dcross_low = dcross.astype(BF16)
    dc = dc + dot(dcross_low, b_low)
    db = db + dot(dcross_low, c_low, TN)

    sums = gather_heads(
        jnp.concatenate(
            [dy * outer - leak, du * inputs, ends, skips, jnp.zeros((EDGE - 2, channels), F32)],
            axis=0,
        ),
        spread,
    )
    at_end = sums[2 * span : 2 * span + 1, :]
    dcum = sums[:span] + row_part - col_buf[...].T
    upper = (iota((span, span), 1) >= iota((span, span), 0)).astype(BF16)
    drate = pick_left(upper, dcum, 3) + at_end
    dstep = drate * decay + sums[span : 2 * span]
    draw = dstep * jax.nn.sigmoid(raw)
    gh_ref[0:1, :] += jnp.sum(draw, axis=0, keepdims=True)
    gh_ref[1:2, :] += jnp.sum(drate * step, axis=0, keepdims=True) * decay
    gh_ref[2:3, :] += sums[2 * span + 1 : 2 * span + 2, :]

    dinputs = du * step_w + skip * dy
    dconv = jnp.concatenate([dinputs, db, dc], axis=1) * (sig * (1.0 + conv * (1.0 - sig)))
    dbuffer[span:, :] = dbuffer[:EDGE, :]
    dbuffer[:span, :] = dconv
    dbefore = jnp.zeros_like(dconv)
    for tap in range(KCONV):
        dbefore = dbefore + taps[tap : tap + 1, :] * window(dbuffer, KCONV - 1 - tap, span)
        gx_ref[tap : tap + 1, :] += jnp.sum(
            dconv * window(buffer, EDGE - KCONV + 1 + tap, span), axis=0, keepdims=True
        )
    gx_ref[KCONV : KCONV + 1, :] += jnp.sum(dconv, axis=0, keepdims=True)
    gx_ref[KCONV + 1 : KCONV + 2, :channels] += gain_grad
    width = 2 * channels + 2 * NS
    grad_ref[:, channels:width] = dbefore.astype(BF16)
    grad_ref[:, width : width + dqkv_ref.shape[1]] = dqkv_ref[...]
    grad_ref[:, width + dqkv_ref.shape[1] :] = draw.astype(BF16)
    for step in range(ring.ahead):
        pl.when(turn == spans * step // ring.ahead)(functools.partial(ring.hop, step))
    pl.when(turn == spans - 1)(ring.finish)


def scan_params(conv_x, conv_xb, conv_bc, conv_bcb, dt_bias, a_log, d_skip, w_mnorm):
    heads = dt_bias.shape[0]
    fill = jnp.zeros((LANES - heads,), BF16)
    flat = [conv_xb, w_mnorm, conv_bcb, dt_bias, fill, a_log, fill, d_skip, fill]
    size = sum(item.shape[0] for item in flat) // LANES
    flat.append(jnp.zeros((-size % EDGE * LANES,), BF16))
    rows = jnp.concatenate(flat).astype(F32).reshape(-1, LANES)
    return (conv_x, conv_bc, rows)


def unpack_rows(row_ref, spread):
    channels = spread.shape[1]
    count = channels // LANES
    at = 2 * count + 2 * NS // LANES

    def join_rows(first, number):
        return jnp.concatenate(
            [row_ref[i : i + 1, :] for i in range(first, first + number)], axis=1
        )

    skip = jnp.broadcast_to(row_ref[at + 2 : at + 3, :], (EDGE, LANES)).astype(BF16)
    return (
        join_rows(0, count),
        join_rows(count, count),
        join_rows(2 * count, 2 * NS // LANES),
        row_ref[at : at + 1, :],
        -jnp.exp(row_ref[at + 1 : at + 2, :]),
        dot(skip, spread)[:1],
    )


def whole_spec(array):
    return pl.BlockSpec(array.shape, lambda turn: (0,) * array.ndim)


def run_scan_forward(proj, qkv_width, params, shard, devices):
    tokens = proj.shape[0]
    channels = params[0].shape[1]
    step_at = (2 * channels + 2 * NS + qkv_width) // LANES
    spans = tokens // SPAN
    bc_at = 2 * channels // (2 * NS)
    rows = lambda width, at: pl.BlockSpec((SPAN, width), lambda turn: (turn, at))
    anywhere = pl.BlockSpec(memory_space=pl.ANY)
    return pl.pallas_call(
        functools.partial(scan_forward, devices, spans),
        grid=(spans,),
        out_shape=(
            jax.ShapeDtypeStruct((tokens, channels), F32),
            jax.ShapeDtypeStruct((tokens, channels), BF16),
            jax.ShapeDtypeStruct((EDGE, tokens), F32),
            jax.ShapeDtypeStruct((spans, NS, channels), F32),
            gather_shape(shard, devices),
        ),
        in_specs=[rows(channels, 0), rows(channels, 1), rows(2 * NS, bc_at), rows(LANES, step_at)]
        + [whole_spec(item) for item in params]
        + [anywhere],
        out_specs=(
            rows(channels, 0),
            rows(channels, 0),
            pl.BlockSpec((EDGE, SPAN), lambda turn: (0, turn)),
            pl.BlockSpec((1, NS, channels), lambda turn: (turn, 0, 0)),
            anywhere,
        ),
        scratch_shapes=[
            pltpu.VMEM((NS, channels), F32),
            pltpu.VMEM((SPAN + EDGE, channels + 2 * NS), F32),
        ]
        + gather_sems(devices),
        compiler_params=pltpu.CompilerParams(collective_id=2, has_side_effects=True),
        cost_estimate=cost(20),
        name="scan_forward",
    )(proj, proj, proj, proj, *params, shard)


def run_scan_backward(
    proj, y, entering, dyg, scale, inner, dqkv, params, sent, windows, pieces, shapes,
    devices,
):
    tokens, width = proj.shape
    channels = params[0].shape[1]
    qkv_width = dqkv.shape[1]
    step_at = (2 * channels + 2 * NS + qkv_width) // LANES
    spans = tokens // SPAN
    bc_at = 2 * channels // (2 * NS)
    edges = SPAN // EDGE
    rows = lambda size, at: pl.BlockSpec((SPAN, size), lambda turn: (spans - 1 - turn, at))
    edge = lambda size, at: pl.BlockSpec(
        (EDGE, size), lambda turn: (jnp.maximum((spans - 1 - turn) * edges - 1, 0), at)
    )
    keep = lambda shape: pl.BlockSpec(shape, lambda turn: (0, 0))
    shapes = tuple(jax.ShapeDtypeStruct(shape, F32) for shape in shapes)
    return pl.pallas_call(
        functools.partial(
            scan_backward, devices, spans, windows, pieces, len(shapes), len(sent)
        ),
        grid=(spans,),
        out_shape=(
            jax.ShapeDtypeStruct((tokens, width), BF16),
            jax.ShapeDtypeStruct((EDGE, channels + 2 * NS), F32),
            jax.ShapeDtypeStruct((EDGE, LANES), F32),
        )
        + shapes,
        in_specs=[
            rows(channels, 0),
            rows(channels, 1),
            edge(channels, 1),
            rows(2 * NS, bc_at),
            edge(2 * NS, bc_at),
            rows(LANES, step_at),
            rows(channels, 0),
            pl.BlockSpec((1, NS, channels), lambda turn: (spans - 1 - turn, 0, 0)),
            rows(channels, 0),
            pl.BlockSpec((EDGE, SPAN), lambda turn: (0, spans - 1 - turn)),
            pl.BlockSpec((EDGE, SPAN), lambda turn: (0, spans - 1 - turn)),
            rows(qkv_width, 0),
        ]
        + [whole_spec(item) for item in params]
        + [pl.BlockSpec(memory_space=pl.ANY)] * len(sent),
        out_specs=(
            rows(width, 0),
            keep((EDGE, channels + 2 * NS)),
            keep((EDGE, LANES)),
        )
        + tuple(keep(item.shape) for item in shapes),
        scratch_shapes=[
            pltpu.VMEM((NS, channels), F32),
            pltpu.VMEM((SPAN + EDGE, channels + 2 * NS), F32),
            pltpu.VMEM((SPAN + EDGE, channels + 2 * NS), F32),
            pltpu.VMEM((SPAN, channels), F32),
            pltpu.VMEM((LANES, SPAN), F32),
        ]
        + scatter_scratch(windows, sent[0].shape[0] // devices, devices),
        compiler_params=pltpu.CompilerParams(collective_id=6, has_side_effects=True),
        cost_estimate=cost(47),
        name="scan_backward",
    )(
        proj, proj, proj, proj, proj, proj, y, entering, dyg, scale, inner, dqkv, *params, *sent,
    )


def rotary_tables(tokens):
    half = HEAD_SIZE // 2
    exponent = np.arange(half, dtype=np.float64) * (-2.0 * LOG_BASE / HEAD_SIZE)
    rates = np.tile(np.exp(exponent.astype(np.float32)).astype(np.float64), LANES // half)
    tables = []
    for places in (np.arange(FINE), np.arange(0, tokens, FINE)):
        angles = places[:, None] * rates[None, :]
        tables += [np.cos(angles).astype(np.float32), np.sin(angles).astype(np.float32)]
    return tables


def fill_rotary(fine_cos, fine_sin, coarse_cos, coarse_sin, cosine, sine):
    small_cos, small_sin = fine_cos[...], fine_sin[...]
    for turn in range(coarse_cos.shape[0]):
        big_cos, big_sin = coarse_cos[turn : turn + 1, :], coarse_sin[turn : turn + 1, :]
        rows = slice(turn * FINE, (turn + 1) * FINE)
        cosine[rows, :] = small_cos * big_cos - small_sin * big_sin
        sine[rows, :] = small_sin * big_cos + small_cos * big_sin


def head_masks():
    half = HEAD_SIZE // 2
    row, col = iota((LANES, LANES), 0), iota((LANES, LANES), 1)
    place = col % HEAD_SIZE
    ahead = jnp.where(place < half, -1.0, 0.0)
    behind = jnp.where(place < half, 0.0, 1.0)

    def turn(start):
        return jnp.where(row == start + half, ahead, jnp.where(row == start - half, behind, 0.0))

    first = row < HEAD_SIZE
    left = col < HEAD_SIZE
    low = lambda mask: mask.astype(BF16)
    within = low(turn(col))
    copy = low(jnp.where(row == place, 1.0, 0.0))
    copy_turn = low(jnp.where(first, turn(place), 0.0))
    value = low(jnp.where(row == place + HEAD_SIZE, 1.0, 0.0))
    fold = low(jnp.where(left & (row % HEAD_SIZE == place), 1.0, 0.0))
    other = row % HEAD_SIZE
    fold_turn = low(
        jnp.where(
            left,
            jnp.where(other == place + half, ahead, jnp.where(other == place - half, behind, 0.0)),
            0.0,
        )
    )
    fold_value = low(jnp.where(left, 0.0, jnp.where(other == place, 1.0, 0.0)))
    return within, copy, copy_turn, value, fold, fold_turn, fold_value


def attend_forward(
    q_ref, kv_ref, fine_cos, fine_sin, coarse_cos, coarse_sin,
    qkv_ref, lse_ref, o_ref, vt, cos_ref, sin_ref,
):
    fill_rotary(fine_cos, fine_sin, coarse_cos, coarse_sin, cos_ref, sin_ref)
    tokens, query_width = q_ref.shape
    pairs = query_width // LANES
    within, copy, copy_turn, value = head_masks()[:4]

    def turn_rows(i, carry):
        rows = pl.ds(pl.multiple_of(i * QBLK, QBLK), QBLK)
        cosine, sine = cos_ref[rows, :], sin_ref[rows, :]
        for pair in range(pairs):
            lanes = slice(pair * LANES, (pair + 1) * LANES)
            query = q_ref[rows, lanes]
            turned = query * cosine + pick(query, within) * sine
            qkv_ref[rows, lanes] = (turned * HEAD_SIZE**-0.5).astype(BF16)
        kv = kv_ref[rows, :]
        keys = pick(kv, copy) * cosine + pick(kv, copy_turn) * sine
        qkv_ref[rows, query_width : query_width + LANES] = keys.astype(BF16)
        qkv_ref[rows, query_width + LANES :] = dot(kv.astype(BF16), value).astype(BF16)
        vt[:, rows] = kv.T[HEAD_SIZE:, :].astype(BF16)
        return carry

    lax.fori_loop(0, tokens // QBLK, turn_rows, 0)
    low_lanes = iota((QBLK, LANES), 1) < HEAD_SIZE
    wide = (QBLK, 2 * QBLK)
    visible = iota(wide, 0) <= iota(wide, 1) % QBLK

    def block(i, carry):
        here = pl.ds(pl.multiple_of(i * QBLK, QBLK), QBLK)
        queries = [
            pair_split(qkv_ref[here, pair * LANES : (pair + 1) * LANES], low_lanes)
            for pair in range(pairs)
        ]

        def tile(there, state, edge):
            keys = qkv_ref[there, query_width : query_width + LANES]
            result = []
            for pair in range(pairs):
                top, total, out = state[3 * pair : 3 * pair + 3]
                scores = dot(keys, queries[pair], NT)
                if edge:
                    scores = jnp.where(visible, scores, MASKED)
                higher = jnp.maximum(top, jnp.max(scores, axis=0, keepdims=True))
                probs = jnp.exp(scores - higher)
                fade = jnp.exp(top - higher)
                total = total * fade + jnp.sum(probs, axis=0, keepdims=True)
                out = out * fade + dot(vt[:, there], probs.astype(BF16))
                result += [higher, total, out]
            return tuple(result)

        state = (
            jnp.full((1, 2 * QBLK), MASKED, F32),
            jnp.zeros((1, 2 * QBLK), F32),
            jnp.zeros((HEAD_SIZE, 2 * QBLK), F32),
        ) * pairs
        state = lax.fori_loop(
            0,
            i,
            lambda j, state: tile(pl.ds(pl.multiple_of(j * QBLK, QBLK), QBLK), state, False),
            state,
        )
        state = tile(here, state, True)
        for pair in range(pairs):
            top, total, out = state[3 * pair : 3 * pair + 3]
            out = out / total
            lse = top + jnp.log(total)
            lse_ref[2 * pair : 2 * pair + 1, here] = lse[:, :QBLK]
            lse_ref[2 * pair + 1 : 2 * pair + 2, here] = lse[:, QBLK:]
            both = jnp.concatenate([out[:, :QBLK], out[:, QBLK:]], axis=0)
            o_ref[here, pair * LANES : (pair + 1) * LANES] = both.T.astype(BF16)
        return carry

    lax.fori_loop(0, tokens // QBLK, block, 0)


def attend_backward(
    qkv_ref, lse_ref, o_ref, do_ref, fine_cos, fine_sin, coarse_cos, coarse_sin,
    dqkv_ref,
    dq, kt, dk, dv, cos_ref, sin_ref,
):
    fill_rotary(fine_cos, fine_sin, coarse_cos, coarse_sin, cos_ref, sin_ref)
    tokens, query_width = o_ref.shape
    pairs = query_width // LANES
    key_lanes = slice(query_width, query_width + LANES)
    value_lanes = slice(query_width + LANES, query_width + 2 * LANES)

    def turn_keys(i, carry):
        rows = pl.ds(pl.multiple_of(i * QBLK, QBLK), QBLK)
        kt[:, rows] = qkv_ref[rows, key_lanes].astype(F32).T[:HEAD_SIZE, :].astype(BF16)
        return carry

    lax.fori_loop(0, tokens // QBLK, turn_keys, 0)
    dk[...] = jnp.zeros_like(dk)
    dv[...] = jnp.zeros_like(dv)
    low_lanes = iota((QBLK, LANES), 1) < HEAD_SIZE
    wide = (QBLK, 2 * QBLK)
    visible = iota(wide, 0) <= iota(wide, 1) % QBLK
    ones = jnp.ones((EDGE, LANES), BF16)

    def block(i, carry):
        here = pl.ds(pl.multiple_of(i * QBLK, QBLK), QBLK)
        queries, grads, inners, lses = [], [], [], []
        for pair in range(pairs):
            lanes = slice(pair * LANES, (pair + 1) * LANES)
            queries.append(pair_split(qkv_ref[here, lanes], low_lanes))
            grad = do_ref[here, lanes]
            grads.append(pair_split(grad, low_lanes))
            both = pair_split(grad.astype(F32) * o_ref[here, lanes].astype(F32), low_lanes)
            high, low = parts(both, 2)
            inners.append((dot(ones, high, NT) + dot(ones, low, NT))[:1])
            lses.append(
                jnp.concatenate(
                    [
                        lse_ref[2 * pair : 2 * pair + 1, here],
                        lse_ref[2 * pair + 1 : 2 * pair + 2, here],
                    ],
                    axis=1,
                )
            )
        query_all = jnp.concatenate(queries, axis=0)
        grad_all = jnp.concatenate(grads, axis=0)

        def tile(there, state, edge):
            keys = qkv_ref[there, key_lanes]
            values = qkv_ref[there, value_lanes]
            all_probs, all_dscores, result = [], [], []
            for pair in range(pairs):
                probs = dot(keys, queries[pair], NT) - lses[pair]
                if edge:
                    probs = jnp.where(visible, probs, MASKED)
                probs = jnp.exp(probs)
                dprobs = dot(values, grads[pair], NT)
                dscores = (probs * (dprobs - inners[pair])).astype(BF16)
                all_probs.append(probs.astype(BF16))
                all_dscores.append(dscores)
                result.append(state[pair] + dot(kt[:, there], dscores))
            dv[there, :] += dot(jnp.concatenate(all_probs, axis=1), grad_all)
            dk[there, :] += dot(jnp.concatenate(all_dscores, axis=1), query_all)
            return tuple(result)

        state = (jnp.zeros((HEAD_SIZE, 2 * QBLK), F32),) * pairs
        state = lax.fori_loop(
            0,
            i,
            lambda j, state: tile(pl.ds(pl.multiple_of(j * QBLK, QBLK), QBLK), state, False),
            state,
        )
        state = tile(here, state, True)
        for pair in range(pairs):
            both = jnp.concatenate([state[pair][:, :QBLK], state[pair][:, QBLK:]], axis=0)
            dq[here, pair * LANES : (pair + 1) * LANES] = both.T
        return carry

    lax.fori_loop(0, tokens // QBLK, block, 0)
    masks = head_masks()
    within, (fold, fold_turn, fold_value) = masks[0], masks[4:]

    def turn_back(i, carry):
        rows = pl.ds(pl.multiple_of(i * QBLK, QBLK), QBLK)
        cosine, sine = cos_ref[rows, :], sin_ref[rows, :]
        for pair in range(pairs):
            lanes = slice(pair * LANES, (pair + 1) * LANES)
            grad = dq[rows, lanes]
            grad = grad * cosine - pick(grad, within) * sine
            dqkv_ref[rows, lanes] = (grad * HEAD_SIZE**-0.5).astype(BF16)
        grad = dk[rows, :]
        grad = pick(grad, fold) * cosine - pick(grad, fold_turn) * sine
        grad = grad + pick(dv[rows, :], fold_value)
        dqkv_ref[rows, query_width:] = grad.astype(BF16)
        return carry

    lax.fori_loop(0, tokens // QBLK, turn_back, 0)


def run_attend_forward(proj, query_at, query_width, tables):
    tokens = proj.shape[0]
    cols = lambda size, at: pl.BlockSpec((tokens, size), lambda turn: (0, at // size))
    return pl.pallas_call(
        attend_forward,
        grid=(1,),
        out_shape=(
            jax.ShapeDtypeStruct((tokens, query_width + 2 * LANES), BF16),
            jax.ShapeDtypeStruct((EDGE, tokens), F32),
            jax.ShapeDtypeStruct((tokens, query_width), BF16),
        ),
        in_specs=[
            cols(query_width, query_at),
            cols(2 * HEAD_SIZE, query_at + query_width),
        ]
        + [whole_spec(table) for table in tables],
        out_specs=(
            cols(query_width + 2 * LANES, 0),
            pl.BlockSpec((EDGE, tokens), lambda turn: (0, 0)),
            cols(query_width, 0),
        ),
        scratch_shapes=[
            pltpu.VMEM((HEAD_SIZE, tokens), BF16),
            pltpu.VMEM((tokens, LANES), F32),
            pltpu.VMEM((tokens, LANES), F32),
        ],
        cost_estimate=cost(15),
        name="attend_forward",
    )(proj, proj, *tables)


def run_attend_backward(qkv, lse, attended, grads, grad_at, tables):
    tokens, query_width = attended.shape
    vmem = pl.BlockSpec(memory_space=pltpu.VMEM)
    cols = lambda size, at: pl.BlockSpec((tokens, size), lambda turn: (0, at // size))
    return pl.pallas_call(
        attend_backward,
        grid=(1,),
        out_shape=jax.ShapeDtypeStruct((tokens, query_width + 2 * HEAD_SIZE), BF16),
        in_specs=[
            whole_spec(qkv),
            whole_spec(lse),
            whole_spec(attended),
            cols(query_width, grad_at),
        ]
        + [whole_spec(table) for table in tables],
        out_specs=cols(query_width + 2 * HEAD_SIZE, 0),
        scratch_shapes=[
            pltpu.VMEM((tokens, query_width), F32),
            pltpu.VMEM((HEAD_SIZE, tokens), BF16),
            pltpu.VMEM((tokens, LANES), F32),
            pltpu.VMEM((tokens, LANES), F32),
            pltpu.VMEM((tokens, LANES), F32),
            pltpu.VMEM((tokens, LANES), F32),
        ],
        cost_estimate=cost(16),
        name="attend_backward",
    )(qkv, lse, attended, grads, *tables)


def feed_forward(
    x_ref, mixed_ref, other_ref, act_grad_ref, norms_ref, gu_ref,
    after_ref, scale_ref, hidden_ref, act_ref, dgu_ref, back_ref,
):
    units = act_grad_ref.shape[1]
    after = x_ref[...].astype(F32) + (mixed_ref[...].astype(F32) + other_ref[...].astype(F32))
    after_ref[...] = after.astype(BF16)
    scale = lax.rsqrt(jnp.mean(after * after, axis=-1, keepdims=True) + EPSILON)
    scale_ref[...] = scale
    hidden = (after * scale * norms_ref[1:2, :]).astype(BF16)
    hidden_ref[...] = hidden
    for start in range(0, units, UBLK):
        cols = slice(start, start + UBLK)
        up_cols = slice(units + start, units + start + UBLK)
        gate = dot(hidden, gu_ref[:, cols])
        upward = dot(hidden, gu_ref[:, up_cols])
        grad = act_grad_ref[:, cols]
        sigma = jax.nn.sigmoid(gate)
        swish = gate * sigma
        act_ref[:, cols] = (swish * upward).astype(BF16)
        slope = sigma * (1.0 + gate * (1.0 - sigma))
        dgu_ref[:, cols] = (grad * upward * slope).astype(BF16)
        dgu_ref[:, up_cols] = (grad * swish).astype(BF16)
    back_ref[...] = dot(dgu_ref[...], gu_ref[...], NT).astype(BF16)


def product_rows(dims, left_ref, right_ref, out_ref):
    out_ref[...] = dot(left_ref[...], right_ref[...], dims).astype(out_ref.dtype)


def run_product(left, right, dims, dtype):
    tokens, depth = left.shape
    cols = right.shape[1 - dims[1][0]]
    return pl.pallas_call(
        functools.partial(product_rows, dims),
        grid=(tokens // TBLK,),
        out_shape=jax.ShapeDtypeStruct((tokens, cols), dtype),
        in_specs=[pl.BlockSpec((TBLK, depth), lambda turn: (turn, 0)), once(right)],
        out_specs=pl.BlockSpec((TBLK, cols), lambda turn: (turn, 0)),
        cost_estimate=cost(4),
        name="product_rows",
    )(left, right)


def project(heads, x_ref, w_ref, hidden_ref, proj_ref, norms_ref):
    @pl.when(pl.program_id(0) == 0)
    def _():
        gains = w_ref[:, w_ref.shape[1] - LANES :].astype(F32).T
        norms_ref[...] = jnp.zeros_like(norms_ref)
        norms_ref[0:2, :] = gains[heads : heads + 2, :]

    x = x_ref[...].astype(F32)
    scale = lax.rsqrt(jnp.mean(x * x, axis=-1, keepdims=True) + EPSILON)
    hidden = (x * scale * norms_ref[0:1, :]).astype(BF16)
    hidden_ref[...] = hidden
    proj_ref[...] = dot(hidden, w_ref[...])


def run_project(x, w_in, heads):
    tokens, width = x.shape
    cols = w_in.shape[1]
    rows = lambda size: pl.BlockSpec((TBLK, size), lambda turn: (turn, 0))
    return pl.pallas_call(
        functools.partial(project, heads),
        grid=(tokens // TBLK,),
        out_shape=(
            jax.ShapeDtypeStruct((tokens, width), BF16),
            jax.ShapeDtypeStruct((tokens, cols), F32),
            jax.ShapeDtypeStruct((EDGE, width), F32),
        ),
        in_specs=[rows(width), once(w_in)],
        out_specs=(
            rows(width), rows(cols), pl.BlockSpec((EDGE, width), lambda turn: (0, 0)),
        ),
        cost_estimate=cost(8),
        name="project",
    )(x, w_in)


def project_back(grad_ref, w_ref, x_ref, part_ref, gain_grad_ref):
    @pl.when(pl.program_id(0) == 0)
    def _():
        gain_grad_ref[...] = jnp.zeros_like(gain_grad_ref)

    x = x_ref[...].astype(F32)
    normed = x * lax.rsqrt(jnp.mean(x * x, axis=-1, keepdims=True) + EPSILON)
    part = dot(grad_ref[...], w_ref[...], NT).astype(BF16)
    part_ref[...] = part
    gain_grad_ref[:1, :] += jnp.sum(part.astype(F32) * normed, axis=0, keepdims=True)


def run_project_back(grads, w_in, x):
    tokens, width = x.shape
    cols = w_in.shape[1]
    rows = lambda size: pl.BlockSpec((TBLK, size), lambda turn: (turn, 0))
    return pl.pallas_call(
        project_back,
        grid=(tokens // TBLK,),
        out_shape=(
            jax.ShapeDtypeStruct((tokens, width), BF16),
            jax.ShapeDtypeStruct((EDGE, width), F32),
        ),
        in_specs=[rows(cols), once(w_in), rows(width)],
        out_specs=(rows(width), pl.BlockSpec((EDGE, width), lambda turn: (0, 0))),
        cost_estimate=cost(8),
        name="project_back",
    )(grads, w_in, x)


def once(item):
    return pl.BlockSpec(item.shape, lambda turn: (0,) * item.ndim, pipeline_mode=pl.Buffered(1))


def run_feed_forward(x, mixed, other, act_grad, norms, w_gate_up):
    tokens, width = x.shape
    units = act_grad.shape[1]
    rows = lambda size: pl.BlockSpec((TBLK, size), lambda turn: (turn, 0))
    shape = jax.ShapeDtypeStruct
    return pl.pallas_call(
        feed_forward,
        grid=(tokens // TBLK,),
        out_shape=(
            shape((tokens, width), BF16),
            shape((tokens, 1), F32),
            shape((tokens, width), BF16),
            shape((tokens, units), BF16),
            shape((tokens, 2 * units), BF16),
            shape((tokens, width), BF16),
        ),
        in_specs=[rows(width)] * 3 + [rows(units), once(norms), once(w_gate_up)],
        out_specs=(rows(width), rows(1), rows(width), rows(units), rows(2 * units), rows(width)),
        cost_estimate=cost(14),
        name="feed_forward",
    )(x, mixed, other, act_grad, norms, w_gate_up)


def mixer_forward(gated_ref, scale_ref, gain_ref, attended_ref, w_ref, low_ref, mixed_ref):
    channels = gated_ref.shape[1]
    scale = scale_ref[...].T[:, :1]
    low_ref[:, :channels] = (gated_ref[...].astype(F32) * scale * gain_ref[...]).astype(BF16)
    low_ref[:, channels:] = attended_ref[...]
    mixed_ref[...] = dot(low_ref[...], w_ref[...], NT).astype(BF16)


def run_mixer_forward(gated, scale, gain, attended, w_out):
    tokens, channels = gated.shape
    width, inner = w_out.shape
    rows = lambda size: pl.BlockSpec((TBLK, size), lambda turn: (turn, 0))
    return pl.pallas_call(
        mixer_forward,
        grid=(tokens // TBLK,),
        out_shape=(
            jax.ShapeDtypeStruct((tokens, inner), BF16),
            jax.ShapeDtypeStruct((tokens, width), BF16),
        ),
        in_specs=[
            rows(channels),
            pl.BlockSpec((EDGE, TBLK), lambda turn: (0, turn)),
            once(gain),
            rows(attended.shape[1]),
            once(w_out),
        ],
        out_specs=(rows(inner), rows(width)),
        cost_estimate=cost(5),
        name="mixer_forward",
    )(gated, scale, gain, attended, w_out)


def mixer_backward(
    part_ref, other_ref, after_ref, scale_ref, top_ref, norms_ref,
    w_ref, gated_ref, scale_m_ref, gain_m_ref,
    low_ref, mamba_ref, attended_ref, inner_ref, gain_grad_ref,
):
    channels = gated_ref.shape[1]

    @pl.when(pl.program_id(0) == 0)
    def _():
        gain_grad_ref[...] = jnp.zeros_like(gain_grad_ref)

    grad = part_ref[...].astype(F32) + other_ref[...].astype(F32)
    scale = scale_ref[...]
    normed = after_ref[...].astype(F32) * scale
    gain_grad_ref[:1, :] += jnp.sum(grad * normed, axis=0, keepdims=True)
    weighted = grad * norms_ref[1:2, :]
    mean = jnp.mean(weighted * normed, axis=-1, keepdims=True)
    total = top_ref[...].astype(F32) + scale * (weighted - normed * mean)
    low_ref[...] = total.astype(BF16)
    back = dot(low_ref[...], w_ref[...])
    mamba = back[:, :channels]
    mamba_ref[...] = mamba
    attended_ref[...] = back[:, channels:].astype(BF16)
    inner_ref[...] = row_sums(mamba * gain_m_ref[...] * gated_ref[...].astype(F32)) * scale_m_ref[...]


def run_mixer_backward(part, other, after, scale, top, norms, w_out, gated, scale_m, gain_m):
    tokens, width = after.shape
    channels = gated.shape[1]
    inner = w_out.shape[1]
    shape = jax.ShapeDtypeStruct
    rows = lambda size: pl.BlockSpec((NBLK, size), lambda turn: (turn, 0))
    lanes = pl.BlockSpec((EDGE, NBLK), lambda turn: (0, turn))
    return pl.pallas_call(
        mixer_backward,
        grid=(tokens // NBLK,),
        out_shape=(
            shape((tokens, width), BF16),
            shape((tokens, channels), F32),
            shape((tokens, inner - channels), BF16),
            shape((EDGE, tokens), F32),
            shape((EDGE, width), F32),
        ),
        in_specs=[rows(width)] * 3
        + [rows(1), rows(width), once(norms), once(w_out), rows(channels), lanes, once(gain_m)],
        out_specs=(
            rows(width), rows(channels), rows(inner - channels), lanes,
            pl.BlockSpec((EDGE, width), lambda turn: (0, 0)),
        ),
        cost_estimate=cost(8),
        name="mixer_backward",
    )(part, other, after, scale, top, norms, w_out, gated, scale_m, gain_m)


def lane_row(ref, first, count):
    return jnp.concatenate([ref[i : i + 1, :] for i in range(first, first + count)], axis=1)


def own_lanes(ref, first, size):
    start = lax.axis_index("dp") * size
    row = ref[pl.ds(first + lax.div(start, LANES), 1), :]
    row = jnp.broadcast_to(row, (EDGE, LANES))
    return pltpu.roll(row, lax.rem(LANES - lax.rem(start, LANES), LANES), 1)[0, :size]


def finish_layer(
    norm_at, x_ref, norms_ref, part_ref, other_ref, grad_ref, after_ref, ffn_ref, ffn_other_ref,
    total_ref, *refs,
):
    count = (len(refs) - 9) // 2
    passed, out_ref, result_ref, handed = refs[:count], refs[count], refs[count + 1], refs[count + 2 :]
    tap_ref, bias_ref, gain_ref, step_ref, log_ref, skip_ref, norm_ref = handed[count:]

    @pl.when(pl.program_id(0) == 0)
    def _():
        for source, target in zip(passed, handed):
            target[...] = source[...]
        rows = tap_ref.shape[1] // LANES
        for tap in range(KCONV):
            tap_ref[tap : tap + 1, :] = lane_row(total_ref, tap * rows, rows)
        bias_ref[...] = lane_row(total_ref, KCONV * rows, rows)[0]
        gain_ref[...] = lane_row(total_ref, (KCONV + 1) * rows, rows)[0]
        at = (KCONV + 2) * rows
        for place, ref in enumerate((step_ref, log_ref, skip_ref)):
            ref[...] = total_ref[at + place : at + place + 1, :][0, : ref.shape[0]]
        norm_ref[...] = own_lanes(total_ref, norm_at, norm_ref.shape[0])

    x = x_ref[...].astype(F32)
    scale = lax.rsqrt(jnp.mean(x * x, axis=-1, keepdims=True) + EPSILON)
    normed = x * scale
    weighted = (part_ref[...].astype(F32) + other_ref[...].astype(F32)) * norms_ref[0:1, :]
    mean = jnp.mean(weighted * normed, axis=-1, keepdims=True)
    out_ref[...] = grad_ref[...].astype(F32) + scale * (weighted - normed * mean)
    ffn = ffn_ref[...].astype(F32) + ffn_other_ref[...].astype(F32)
    result_ref[...] = (after_ref[...].astype(F32) + ffn).astype(BF16)


def run_finish(
    x, norms, part, other, grad, after, ffn, ffn_other, total, passed, channels, heads, shard,
    norm_at,
):
    tokens, width = x.shape
    rows = pl.BlockSpec((TBLK, width), lambda turn: (turn, 0))
    shape = lambda *sizes: jax.ShapeDtypeStruct(sizes, F32)
    small = (
        shape(KCONV, channels), shape(channels), shape(channels), shape(heads), shape(heads),
        shape(heads), shape(shard),
    )
    return pl.pallas_call(
        functools.partial(finish_layer, norm_at),
        grid=(tokens // TBLK,),
        out_shape=(shape(tokens, width), jax.ShapeDtypeStruct((tokens, width), BF16))
        + tuple(shape(*item.shape) for item in passed)
        + small,
        in_specs=[rows, once(norms)] + [rows] * 6 + [once(total)] + [once(item) for item in passed],
        out_specs=(rows, rows) + tuple(once(item) for item in passed + small),
        cost_estimate=cost(8),
        name="finish_layer",
    )(x, norms, part, other, grad, after, ffn, ffn_other, total, *passed)


def finish_shared(at, total_ref, cross_ref, mine_ref, other_ref, bc_ref, tap_ref, bias_ref, norm_ref, both):
    half = lax.axis_index("tensor")
    cols = pl.ds(pl.multiple_of(half * LANES, LANES), LANES)
    bc_ref[...] = mine_ref[:, cols] + other_ref[:, cols]
    both[...] = total_ref[...] + cross_ref[...]
    for tap in range(KCONV):
        tap_ref[tap : tap + 1, :] = both[pl.ds(at + 2 * tap + half, 1), :]
    bias_ref[...] = both[pl.ds(at + 2 * KCONV + half, 1), :][0]
    norm_ref[...] = own_lanes(both, at + 2 * KCONV + 2, norm_ref.shape[0])


def run_finish_shared(total, cross, mine, other, shard, at):
    vmem = pl.BlockSpec(memory_space=pltpu.VMEM)
    shape = lambda *sizes: jax.ShapeDtypeStruct(sizes, F32)
    return pl.pallas_call(
        functools.partial(finish_shared, at),
        out_shape=(shape(mine.shape[0], LANES), shape(KCONV, LANES), shape(LANES), shape(shard)),
        in_specs=[vmem] * 4,
        out_specs=(vmem,) * 4,
        scratch_shapes=[pltpu.VMEM(total.shape, F32)],
        name="finish_shared",
    )(total, cross, mine, other)


def swap(partial):
    return lax.ppermute(partial, "tensor", [(0, 1), (1, 0)])


def join(mine, other):
    return mine.astype(F32) + other.astype(F32)


def tensor_sum(partial):
    return join(partial, swap(partial))


def thirds(size):
    part = size // 3
    return [(0, part), (part, 2 * part), (2 * part, size)]


def local(
    layer_input, w_norm1, w_zx, w_bc, w_dt, conv_x, conv_xb, conv_bc, conv_bcb, dt_bias, a_log,
    d_skip, w_mnorm, w_mout, query_key_value_weight, output_weight, w_norm2, w_gu, w_down,
    grad_output,
):
    devices = lax.axis_size("dp")
    tokens, width = layer_input.shape
    shard = w_zx.shape[0]
    channels = conv_xb.shape[0]
    heads = dt_bias.shape[0]
    qkv_width = query_key_value_weight.shape[2]
    units = w_down.shape[0]
    attn_width = output_weight.shape[1]
    tail = jnp.concatenate(
        [w_dt, w_norm1[:, None], w_norm2[:, None], jnp.zeros((shard, LANES - heads - 2), BF16)],
        axis=1,
    )
    mixer_in = jnp.concatenate(
        [w_zx.reshape(shard, -1), w_bc, query_key_value_weight.reshape(shard, -1), tail], axis=1
    )
    in_width = mixer_in.shape[1]
    (w_in,) = gather_rows([mixer_in], devices, 0, [(0, *window) for window in thirds(in_width)])
    w_in, *small_params = lax.optimization_barrier(
        (w_in, conv_x, conv_xb, conv_bc, conv_bcb, dt_bias, a_log, d_skip, w_mnorm)
    )
    params = scan_params(*small_params)
    hidden_one, proj, norms = run_project(layer_input, w_in, heads)
    out_shard = jnp.concatenate([w_mout.T, output_weight.reshape(attn_width, -1).T], axis=1)
    y, gated, square_sum, entering, w_out = run_scan_forward(
        proj, qkv_width, params, out_shard, devices
    )
    channels_all = channels * lax.axis_size("tensor")
    scale_m = lax.rsqrt(tensor_sum(square_sum) / channels_all + EPSILON)
    tables = rotary_tables(tokens)
    qkv_at = 2 * channels + 2 * NS
    qkv, lse, attended = run_attend_forward(proj, qkv_at, attn_width, tables)
    gain_m = w_mnorm.astype(F32)[None, :]
    mixer_out, mixed = run_mixer_forward(gated, scale_m, gain_m, attended, w_out)
    mixed, gate_up_shard, down_shard = lax.optimization_barrier(
        (mixed, w_gu.reshape(shard, -1), w_down.T)
    )
    other = swap(mixed)
    w_gate_up, w_down_t = gather_rows(
        [gate_up_shard, down_shard],
        devices,
        3,
        [(0, 0, units), (0, units, 2 * units), (1, 0, units)],
    )
    act_grad = run_product(grad_output, w_down_t, NN, F32)
    other, w_gate_up, w_down_t, act_grad = lax.optimization_barrier(
        (other, w_gate_up, w_down_t, act_grad)
    )
    after, scale_two, hidden_two, activated, grad_gu_low, partial_two = run_feed_forward(
        layer_input, mixed, other, act_grad, norms, w_gate_up
    )
    other = swap(partial_two)
    grad_down = dot(grad_output, activated, TN).astype(BF16)
    (mine_gu,) = scatter_product(
        hidden_two,
        grad_gu_low,
        [
            ([(0, 1, 0, units)], [(0, 0, units, 0, 0)]),
            ([(0, 1, units, 2 * units)], [(0, 0, units, 0, 1)]),
        ],
        [(shard, 2, units)],
        devices,
        1,
    )
    ffn_part = run_product(activated, w_down_t, NT, BF16)
    other, mine_gu, grad_down, ffn_part = lax.optimization_barrier(
        (other, mine_gu, grad_down, ffn_part)
    )
    ffn_other = swap(ffn_part)
    grad_mix_low, grad_mamba, grad_attended, inner_m, grad_norm2 = run_mixer_backward(
        partial_two, other, after, scale_two, grad_output, norms, w_out, gated, scale_m, gain_m
    )
    inner_m = tensor_sum(inner_m) / channels_all
    dqkv = run_attend_backward(qkv, lse, attended, grad_attended, 0, tables)
    grad_out = dot(grad_mix_low, mixer_out, TN).astype(BF16)
    windows = [(0, None, 0, channels + attn_width), (1, None, 0, units)]
    pieces = [
        (0, 0, channels, 0, None),
        (0, channels, channels + attn_width, 1, None),
        (1, 0, units, 2, None),
    ]
    shapes = [(shard, channels), (shard, attn_width), (shard, units)]
    grad_proj, small_x, small_h, mine_mout, mine_o, mine_down = run_scan_backward(
        proj, y, entering, grad_mamba, scale_m, inner_m, dqkv, params,
        [grad_out, grad_down], windows, pieces, shapes, devices,
    )
    ffn_other, grad_proj = lax.optimization_barrier((ffn_other, grad_proj))
    partial_one, grad_norm1 = run_project_back(grad_proj, w_in, layer_input)
    partial_one, grad_proj = lax.optimization_barrier((partial_one, grad_proj))
    other = swap(partial_one)
    lanes_of = lambda size, start=0: range(start, start + size, LANES)
    places = [(0, row, lane) for row in range(KCONV + 2) for lane in lanes_of(channels)]
    places += [(1, row, 0) for row in range(3)]
    norm_at = len(places)
    places += [(2, 0, lane) for lane in lanes_of(width)]
    cross_at = len(places)
    places += [(0, row, lane) for row in range(KCONV + 1) for lane in lanes_of(2 * NS, channels)]
    places += [(3, 0, lane) for lane in lanes_of(width)]
    shared_at = 2 * channels
    step_at = qkv_at + qkv_width
    mine_zx, mine_bc, mine_qkv, mine_step, small = scatter_product(
        hidden_one,
        grad_proj,
        [
            ([(0, 1, 0, channels)], [(0, 0, channels, 0, 0)]),
            ([(0, 1, channels, shared_at)], [(0, 0, channels, 0, 1)]),
            (
                [(0, 1, shared_at, in_width)],
                [
                    (0, 0, 2 * NS, 1, None),
                    (0, 2 * NS, 2 * NS + qkv_width, 2, 0),
                    (0, 2 * NS + qkv_width, in_width - shared_at, 3, "turned"),
                ],
            ),
        ],
        [
            (shard, 2, channels),
            (shard, 2 * NS),
            (shard, 1, qkv_width),
            (heads, shard),
        ],
        devices,
        5,
        (small_x, small_h, grad_norm2, grad_norm1),
        places,
    )
    other, mine_bc = lax.optimization_barrier((other, mine_bc))
    passed = (mine_zx, mine_qkv, mine_step, mine_mout, mine_o, mine_gu, mine_down)
    cross, other_bc = swap(small), swap(mine_bc)
    grad_source, result, *rest = run_finish(
        layer_input, norms, partial_one, other, grad_mix_low, after, ffn_part, ffn_other, small,
        passed, channels, heads, shard, norm_at,
    )
    mine_zx, mine_qkv, mine_step, mine_mout, mine_o, mine_gu, mine_down = rest[: len(passed)]
    grad_taps, grad_bias, grad_gain, grad_steps, grad_log, grad_skip, own_norm2 = rest[len(passed) :]
    grad_bc, grad_tapsb, grad_biasb, own_norm1 = run_finish_shared(
        small, cross, mine_bc, other_bc, shard, cross_at
    )
    return (
        result,
        grad_source,
        own_norm1,
        mine_zx,
        grad_bc,
        mine_step.T,
        grad_taps,
        grad_bias,
        grad_tapsb,
        grad_biasb,
        grad_steps,
        grad_log,
        grad_skip,
        grad_gain,
        mine_mout.T,
        mine_qkv,
        mine_o.T.reshape(output_weight.shape),
        own_norm2,
        mine_gu,
        mine_down.T,
    )


def solution(mesh):
    return jax.shard_map(
        local,
        mesh=mesh,
        in_specs=(
            P("dp", None),
            P("dp"),
            P("dp", None, "tensor"),
            P("dp", None),
            P("dp", "tensor"),
            P(None, "tensor"),
            P("tensor"),
            P(),
            P(),
            P("tensor"),
            P("tensor"),
            P("tensor"),
            P("tensor"),
            P("tensor", "dp"),
            P("dp", "tensor", None),
            P("tensor", None, "dp"),
            P("dp"),
            P("dp", None, "tensor"),
            P("tensor", "dp"),
            P("dp", None),
        ),
        out_specs=(
            P("dp", None),
            P("dp", None),
            P("dp"),
            P("dp", None, "tensor"),
            P("dp", "tensor"),
            P("dp", "tensor"),
            P(None, "tensor"),
            P("tensor"),
            P(None, "tensor"),
            P("tensor"),
            P("tensor"),
            P("tensor"),
            P("tensor"),
            P("tensor"),
            P("tensor", "dp"),
            P("dp", "tensor", None),
            P("tensor", None, "dp"),
            P("dp"),
            P("dp", None, "tensor"),
            P("tensor", "dp"),
        ),
        check_vma=False,
    )
```

```python
import functools
import math

import jax
import jax.numpy as jnp
import numpy as np
from jax import lax
from jax.experimental import pallas as pl
from jax.experimental.pallas import tpu as pltpu
from jax.sharding import PartitionSpec as P


HEAD_SIZE = 64
MP = 64
NS = 128
KCONV = 4
SPAN = 128
QBLK = 256
FINE = 32
TBLK = 256
NBLK = 128
UBLK = 256
LANES = 128
EDGE = 8

EPSILON = 1e-05
LOG_BASE = math.log(100000000000.0)
MASKED = -1e30
MESH = pl.DeviceIdType.MESH
F32 = jnp.float32
BF16 = jnp.bfloat16

NN = ((1,), (0,))
NT = ((1,), (1,))
TN = ((0,), (0,))


def dot(left, right, dims=NN, precision=None):
    return lax.dot_general(
        left, right, (dims, ((), ())), preferred_element_type=F32, precision=precision
    )


def iota(shape, dim):
    return lax.broadcasted_iota(jnp.int32, shape, dim)


def ring_place(chip, chips):
    odd = lax.rem(chip, 2)
    half = lax.div(chip, 2)
    return (1 - odd) * half + odd * (chips - 1 - half)


def ring_chip(place, chips):
    place = lax.rem(place + 4 * chips, chips)
    back = lax.div(place, chips // 2)
    return (1 - back) * (2 * place) + back * (2 * (chips - 1 - place) + 1)


class RingGather:
    def __init__(self, devices, x_ref, o_ref, sems, cols=slice(None)):
        self.cols = cols
        self.chips = devices // 2
        self.ahead = self.chips // 2
        self.behind = self.chips - 1 - self.ahead
        self.x_ref, self.o_ref, self.rows = x_ref, o_ref, x_ref.shape[0]
        self.fs, self.fr, self.bs, self.br, self.cs, self.cr, self.own_sem = sems

    def locate(self):
        me = lax.axis_index("dp")
        self.group = lax.axis_index("tensor")
        self.core = lax.rem(me, 2)
        chip = lax.div(me, 2)
        self.place = ring_place(chip, self.chips)
        self.right = ring_chip(self.place + 1, self.chips) * 2 + self.core
        self.left = ring_chip(self.place - 1, self.chips) * 2 + self.core
        self.mate = chip * 2 + (1 - self.core)
        self.me = me

    def slot(self, index):
        rows = pl.ds(pl.multiple_of(index * self.rows, self.rows), self.rows)
        return self.o_ref.at[rows, self.cols]

    def copy(self, shift, ssem, rsem, target):
        if shift == 0:
            index, source = self.me, self.x_ref.at[:, self.cols]
        else:
            index = ring_chip(self.place + shift, self.chips) * 2 + self.core
            source = self.slot(index)
        return pltpu.make_async_remote_copy(
            src_ref=source,
            dst_ref=self.slot(index),
            send_sem=ssem,
            recv_sem=rsem,
            device_id=(target, self.group),
            device_id_type=MESH,
        )

    def fore(self, step):
        return self.copy(-step, self.fs.at[step], self.fr.at[step], self.right)

    def back(self, step):
        return self.copy(step, self.bs.at[step], self.br.at[step], self.left)

    def across(self, shift):
        number = 0 if shift == 0 else 2 * abs(shift) - (1 if shift < 0 else 0)
        return self.copy(shift, self.cs.at[number], self.cr.at[number], self.mate)

    def own(self):
        return pltpu.make_async_copy(
            self.x_ref.at[:, self.cols], self.slot(self.me), self.own_sem
        )

    def greet(self):
        self.locate()
        barrier = pltpu.get_barrier_semaphore()
        for other in (self.right, self.left, self.mate):
            pl.semaphore_signal(
                barrier, inc=1, device_id=(other, self.group), device_id_type=MESH
            )
        pl.semaphore_wait(barrier, 3)

    def begin(self):
        self.locate()
        self.fore(0).start()
        self.back(0).start()
        self.across(0).start()
        self.own().start()

    def hop(self, step):
        self.locate()
        self.fore(step - 1).wait_recv()
        if step < self.ahead:
            self.fore(step).start()
        self.across(-step).start()
        if step <= self.behind:
            self.back(step - 1).wait_recv()
            if step < self.behind:
                self.back(step).start()
            self.across(step).start()

    def finish(self):
        self.locate()
        self.own().wait()
        for step in range(self.ahead):
            self.fore(step).wait_send()
        for step in range(self.behind):
            self.back(step).wait_send()
        for shift in range(-self.ahead, self.behind + 1):
            self.across(shift).wait()


def gather_sems(devices):
    dma = pltpu.SemaphoreType.DMA
    return [dma((devices // 2,))] * 6 + [dma(())]


def gather_shape(shard, devices):
    return jax.ShapeDtypeStruct((shard.shape[0] * devices, shard.shape[1]), shard.dtype)


def gather_kernel(devices, count, windows, *refs):
    shards, outs, sems = refs[:count], refs[count : 2 * count], refs[2 * count :]
    each = len(sems) // len(windows)
    rings = [
        RingGather(
            devices, shards[i], outs[i], sems[place * each : (place + 1) * each], slice(first, last)
        )
        for place, (i, first, last) in enumerate(windows)
    ]
    rings[0].greet()
    for ring in rings:
        ring.begin()
    for step in range(1, rings[0].ahead + 1):
        for ring in rings:
            ring.hop(step)
    for ring in rings:
        ring.finish()


def cost(micros):
    return pl.CostEstimate(flops=int(micros * 1e9), bytes_accessed=0, transcendentals=0)


def gather_rows(shards, devices, collective, windows):
    count = len(shards)
    anywhere = pl.BlockSpec(memory_space=pl.ANY)
    return pl.pallas_call(
        functools.partial(gather_kernel, devices, count, windows),
        out_shape=tuple(gather_shape(shard, devices) for shard in shards),
        in_specs=[anywhere] * count,
        out_specs=(anywhere,) * count,
        scratch_shapes=gather_sems(devices) * len(windows),
        compiler_params=pltpu.CompilerParams(collective_id=collective, has_side_effects=True),
        cost_estimate=cost(3),
        name="gather_rows",
    )(*shards)


class RingScatter:
    def __init__(self, devices, windows, pieces, operands, outs, scratch):
        self.chips = devices // 2
        self.ahead = self.chips // 2
        self.behind = self.chips - 1 - self.ahead
        self.windows, self.pieces, self.operands, self.outs = windows, pieces, operands, outs
        count = len(windows)
        self.mine, self.boxes, rest = scratch[:count], scratch[count : 2 * count], scratch[2 * count :]
        self.fbox, self.bbox, self.fout, self.bout = rest[:4]
        self.os, self.ms, self.mr, self.fs, self.fr, self.bs, self.br = rest[4:]
        self.rows = self.fbox.shape[1]
        widths = [item.shape[2] for item in self.mine]
        self.cols = [slice(sum(widths[:i]), sum(widths[: i + 1])) for i in range(count)]

    def locate(self):
        me = lax.axis_index("dp")
        self.group = lax.axis_index("tensor")
        self.core = lax.rem(me, 2)
        chip = lax.div(me, 2)
        self.place = ring_place(chip, self.chips)
        self.right = ring_chip(self.place + 1, self.chips) * 2 + self.core
        self.left = ring_chip(self.place - 1, self.chips) * 2 + self.core
        self.mate = chip * 2 + (1 - self.core)

    def greet(self):
        self.locate()
        barrier = pltpu.get_barrier_semaphore()
        for other in (self.right, self.left, self.mate):
            pl.semaphore_signal(
                barrier, inc=1, device_id=(other, self.group), device_id_type=MESH
            )
        pl.semaphore_wait(barrier, 3)

    def product(self, i):
        return self.windows[i][1] is not None

    def shift_of(self, slot):
        step = slot // 2
        odd = slot % 2
        return (1 - odd) * (step - self.ahead) + odd * (self.behind - step)

    def half(self, which):
        return pl.ds(pl.multiple_of(which * self.rows, self.rows), self.rows)

    def block(self, i, slot, which):
        index = ring_chip(self.place + self.shift_of(slot), self.chips) * 2 + which
        left, _, first, last = self.windows[i]
        return self.operands[left].at[self.half(index), first:last]

    def remote(self, source, target_ref, ssem, rsem, target):
        return pltpu.make_async_remote_copy(
            src_ref=source,
            dst_ref=target_ref,
            send_sem=ssem,
            recv_sem=rsem,
            device_id=(target, self.group),
            device_id_type=MESH,
        )

    def across(self, i, slot):
        if self.product(i):
            source = self.mine[i].at[slot, self.half(1 - self.core)]
        else:
            source = self.block(i, slot, 1 - self.core)
        return self.remote(
            source, self.boxes[i].at[slot], self.ms.at[i, slot], self.mr.at[i, slot], self.mate
        )

    def own(self, i, slot):
        return pltpu.make_async_copy(
            self.block(i, slot, self.core), self.mine[i].at[slot], self.os.at[i, slot]
        )

    def fore(self, step):
        return self.remote(
            self.fout.at[step], self.fbox.at[step], self.fs.at[step], self.fr.at[step], self.right
        )

    def back(self, step):
        return self.remote(
            self.bout.at[step], self.bbox.at[step], self.bs.at[step], self.br.at[step], self.left
        )

    def begin(self):
        self.locate()
        for i in range(len(self.windows)):
            if not self.product(i):
                for slot in range(self.chips):
                    self.across(i, slot).start()
                    self.own(i, slot).start()

    def produce(self, slot):
        chip = ring_chip(self.place + self.shift_of(slot), self.chips)
        size = 2 * self.rows
        for i, (left, right, first, last) in enumerate(self.windows):
            if right is None:
                continue
            at = pl.multiple_of(chip * size, size)
            terms = dot(self.operands[left][pl.ds(at, size), :], self.operands[right][:, first:last])
            self.mine[i][slot] = terms.astype(BF16)
            self.across(i, slot).start()

    def local_sum(self, i, slot, cols, others):
        rows = self.half(self.core) if self.product(i) else slice(None)
        total = self.mine[i][slot, rows, cols].astype(F32) + self.boxes[i][slot, :, cols].astype(F32)
        whole = slice(self.cols[i].start + cols.start, self.cols[i].start + cols.stop)
        for ref in others:
            total = total + ref[:, whole].astype(F32)
        return total

    def arrive(self, slot):
        for i in range(len(self.windows)):
            if not self.product(i):
                self.own(i, slot).wait()
            self.across(i, slot).wait_recv()

    def put(self, target, slot, others):
        self.arrive(slot)
        for i, cols in enumerate(self.cols):
            total = self.local_sum(i, slot, slice(0, cols.stop - cols.start), others)
            target[:, cols] = total.astype(BF16)

    def hop_back(self, step, later):
        if later:
            self.back(step - 1).wait_recv()
        self.put(self.bout.at[step], 2 * step, [self.bbox.at[step - 1]] if later else [])
        self.back(step).start()

    def hop_fore(self, step, later):
        if later:
            self.fore(step - 1).wait_recv()
        self.put(self.fout.at[step], 2 * step + 1, [self.fbox.at[step - 1]] if later else [])
        self.fore(step).start()

    def hop(self, step):
        self.locate()
        self.hop_back(step, step > 0)
        if step < self.behind:
            self.hop_fore(step, step > 0)

    def finish(self):
        self.locate()
        slot = self.chips - 1
        self.arrive(slot)
        self.fore(self.behind - 1).wait_recv()
        self.back(self.ahead - 1).wait_recv()
        others = [self.fbox.at[self.behind - 1], self.bbox.at[self.ahead - 1]]
        for i, first, last, out, form in self.pieces:
            total = self.local_sum(i, slot, slice(first, last), others)
            if form == "turned":
                self.outs[out][...] = total.T[: self.outs[out].shape[0]]
            elif form is None:
                self.outs[out][...] = total
            else:
                self.outs[out][:, form, :] = total
        for step in range(self.ahead):
            self.back(step).wait_send()
        for step in range(self.behind):
            self.fore(step).wait_send()
        for slot in range(self.chips):
            for i in range(len(self.windows)):
                self.across(i, slot).wait_send()


def run_rings(rings, after_first=None):
    ahead, behind = rings[0].ahead, rings[0].behind

    def turn(step, carry):
        def part(odd, kept):
            for ring in rings:
                ring.produce(2 * step + odd)
            return kept

        lax.fori_loop(0, 2, part, 0)

        @pl.when(step == 0)
        def _():
            for ring in rings:
                ring.hop_back(0, False)
                ring.hop_fore(0, False)
            if after_first is not None:
                after_first()

        @pl.when(step > 0)
        def _():
            for ring in rings:
                ring.hop_back(step, True)
                pl.when(step < behind)(functools.partial(ring.hop_fore, step, True))

        return carry

    lax.fori_loop(0, ahead, turn, 0)


def scatter_scratch(windows, rows, devices):
    chips = devices // 2
    count = len(windows)
    dma = pltpu.SemaphoreType.DMA
    widths = [last - first for left, right, first, last in windows]
    mine = [
        pltpu.VMEM((chips, rows if right is None else 2 * rows, last - first), BF16)
        for left, right, first, last in windows
    ]
    boxes = [pltpu.VMEM((chips, rows, width), BF16) for width in widths]
    box = pltpu.VMEM((chips // 2, rows, sum(widths)), BF16)
    return mine + boxes + [box] * 4 + [dma((count, chips))] * 3 + [dma((chips,))] * 4


class Total:
    def __init__(self, devices, x_ref, o_ref, scratch):
        self.chips = devices // 2
        self.x_ref, self.o_ref = x_ref, o_ref
        self.mate_box, self.joined, self.boxes, self.ms, self.mr, self.ss, self.sr = scratch
        me = lax.axis_index("dp")
        self.group = lax.axis_index("tensor")
        self.chip = lax.div(me, 2)
        core = lax.rem(me, 2)
        self.mate = self.chip * 2 + (1 - core)
        self.peers = [
            lax.rem(self.chip + shift, self.chips) * 2 + core for shift in range(self.chips)
        ]

    def greet(self):
        barrier = pltpu.get_barrier_semaphore()
        for other in [self.mate] + self.peers[1:]:
            pl.semaphore_signal(
                barrier, inc=1, device_id=(other, self.group), device_id_type=MESH
            )
        pl.semaphore_wait(barrier, self.chips)

    def remote(self, source, target_ref, ssem, rsem, target):
        return pltpu.make_async_remote_copy(
            src_ref=source,
            dst_ref=target_ref,
            send_sem=ssem,
            recv_sem=rsem,
            device_id=(target, self.group),
            device_id_type=MESH,
        )

    def across(self):
        return self.remote(self.x_ref, self.mate_box, self.ms, self.mr, self.mate)

    def copies(self):
        return [
            self.remote(
                self.joined,
                self.boxes.at[self.chip],
                self.ss.at[shift],
                self.sr.at[shift],
                self.peers[shift],
            )
            for shift in range(1, self.chips)
        ]

    def begin(self):
        self.across().start()

    def spread(self):
        self.across().wait_recv()
        self.joined[...] = self.x_ref[...] + self.mate_box[...]
        for copy in self.copies():
            copy.start()
        self.boxes[self.chip] = self.joined[...]

    def finish(self):
        for copy in self.copies():
            copy.wait_recv()
        result = self.boxes[0]
        for other in range(1, self.chips):
            result = result + self.boxes[other]
        self.o_ref[...] = result
        self.across().wait_send()
        for copy in self.copies():
            copy.wait_send()


def total_scratch(values, devices):
    chips = devices // 2
    dma = pltpu.SemaphoreType.DMA
    return [
        pltpu.VMEM(values.shape, F32),
        pltpu.VMEM(values.shape, F32),
        pltpu.VMEM((chips,) + values.shape, F32),
        dma(()),
        dma(()),
        dma((chips,)),
        dma((chips,)),
    ]


def turned_copy(source, target):
    for start in range(0, source.shape[1], LANES):
        target[start : start + LANES, :] = source[:, start : start + LANES].T


def product_kernel(devices, groups, outs, places, summed, left_ref, right_ref, *refs):
    values = refs[:summed]
    refs = refs[summed:]
    pieces_out, refs = refs[:outs], refs[outs:]
    total = None
    if summed:
        total_out, refs = refs[0], refs[1:]
    turned, scratch = refs[0], refs[1:]
    if summed:
        scratch, rest = scratch[:-8], scratch[-8:]
        together = rest[0]
        together[...] = jnp.zeros_like(together)
        for at, (which, row, lane) in enumerate(places):
            together[at : at + 1, :] = values[which][row : row + 1, lane : lane + LANES]
        total = Total(devices, together, total_out, rest[1:])
    each = len(scratch) // len(groups)
    rings = [
        RingScatter(
            devices, windows, pieces, (turned, right_ref), pieces_out,
            scratch[place * each : (place + 1) * each],
        )
        for place, (windows, pieces) in enumerate(groups)
    ]
    if total is None:
        rings[0].greet()
    else:
        total.greet()
        total.begin()
    for ring in rings:
        ring.locate()
    turned_copy(left_ref, turned)
    run_rings(rings, total.spread if total is not None else None)
    for ring in rings:
        ring.finish()
    if total is not None:
        total.finish()


def scatter_product(left, right, groups, shapes, devices, collective, values=(), places=()):
    vmem = pl.BlockSpec(memory_space=pltpu.VMEM)
    rows = left.shape[1] // devices
    scratch = [pltpu.VMEM(left.shape[::-1], BF16)]
    for windows, pieces in groups:
        scratch += scatter_scratch(windows, rows, devices)
    totals = ()
    if values:
        total = jax.ShapeDtypeStruct((len(places) + -len(places) % EDGE, LANES), F32)
        totals = (total,)
        scratch += [pltpu.VMEM(total.shape, F32)] + total_scratch(total, devices)
    return pl.pallas_call(
        functools.partial(
            product_kernel, devices, groups, len(shapes), places, len(values)
        ),
        out_shape=tuple(jax.ShapeDtypeStruct(shape, F32) for shape in shapes) + totals,
        in_specs=[vmem] * (2 + len(values)),
        out_specs=(vmem,) * (len(shapes) + len(totals)),
        scratch_shapes=scratch,
        compiler_params=pltpu.CompilerParams(collective_id=collective, has_side_effects=True),
        cost_estimate=cost(3),
        name="scatter_product",
    )(left, right, *values)


def head_spread(channels):
    return (iota((LANES, channels), 1) // MP == iota((LANES, channels), 0)).astype(BF16)


def parts(values, count):
    terms = []
    for _ in range(count):
        term = values.astype(BF16)
        terms.append(term)
        values = values - term.astype(F32)
    return terms


def pick(values, mask, count=2):
    return dot(jnp.concatenate(parts(values, count), axis=1), jnp.concatenate([mask] * count, axis=0))


def pick_left(mask, values, count):
    return dot(jnp.concatenate([mask] * count, axis=1), jnp.concatenate(parts(values, count), axis=0))


def gather_heads(values, spread):
    high, low = parts(values, 2)
    return dot(high, spread, NT) + dot(low, spread, NT)


def row_sums(values):
    high, low = parts(values, 2)
    ones = jnp.ones((EDGE, values.shape[1]), BF16)
    return dot(ones, high, NT) + dot(ones, low, NT)


def soft_step(raw):
    return jnp.maximum(raw, 0.0) + jnp.log1p(jnp.exp(-jnp.abs(raw)))


def window(buffer, start, span):
    return buffer[start : start + span, :]


def causal_taps(buffer, taps, span):
    total = taps[0:1, :] * window(buffer, EDGE - KCONV + 1, span)
    for tap in range(1, KCONV):
        total = total + taps[tap : tap + 1, :] * window(buffer, EDGE - KCONV + 1 + tap, span)
    return total


def span_rates(step_ref, bias, decay, spread, span):
    raw = step_ref[...] + bias
    step = soft_step(raw)
    lower = (iota((span, span), 1) <= iota((span, span), 0)).astype(BF16)
    cum = pick_left(lower, step * decay, 3)
    tails = jnp.exp(cum[span - 1 : span, :] - cum)
    wide = pick(jnp.concatenate([step, tails, jnp.exp(cum)], axis=0), spread)
    return raw, step, cum, wide[:span], wide[span : 2 * span], wide[2 * span :]


def pair_split(values, low_lanes):
    zero = jnp.zeros_like(values)
    return jnp.concatenate(
        [jnp.where(low_lanes, values, zero), jnp.where(low_lanes, zero, values)], axis=0
    )


def pair_decay(cum, cum_rows, pair, causal):
    parts = []
    for head in (2 * pair, 2 * pair + 1):
        differ = cum[:, head : head + 1] - cum_rows[head : head + 1, :]
        parts.append(jnp.exp(jnp.where(causal, differ, MASKED)))
    return parts


def scan_forward(
    devices, spans,
    z_ref, x_ref, bc_ref, step_ref,
    tap_ref, tapb_ref, row_ref, shard_ref,
    y_ref, gated_ref, square_ref, enter_ref, all_ref,
    state, buffer, *sems,
):
    span, channels = x_ref.shape
    ring = RingGather(devices, shard_ref, all_ref, sems)
    turn = pl.program_id(0)

    @pl.when(turn == 0)
    def _():
        ring.greet()
        ring.begin()


    @pl.when(pl.program_id(0) == 0)
    def _():
        state[...] = jnp.zeros_like(state)
        buffer[span:, :] = jnp.zeros((EDGE, buffer.shape[1]), F32)

    buffer[:EDGE, :] = buffer[span:, :]
    buffer[EDGE:, :channels] = x_ref[...]
    buffer[EDGE:, channels:] = bc_ref[...]
    spread = head_spread(channels)
    bias, _, biasb, stepb, decay, skip = unpack_rows(row_ref, spread)
    taps = jnp.concatenate([tap_ref[...], tapb_ref[...]], axis=1).astype(F32)
    conv = causal_taps(buffer, taps, span)
    conv = jax.nn.silu(conv + jnp.concatenate([bias, biasb], axis=1))
    inputs, shared = conv[:, :channels], conv[:, channels:]
    _, step, cum, step_w, tails_w, grown_w = span_rates(step_ref, stepb, decay, spread, span)
    cum_rows = cum.T
    b_low = shared[:, :NS].astype(BF16)
    c_low = shared[:, NS:].astype(BF16)
    scaled = inputs * step_w
    scaled_low = scaled.astype(BF16)
    enter_ref[0] = state[...]
    outer = dot(c_low, state[...].astype(BF16)) * grown_w
    fresh = dot(b_low, (scaled * tails_w).astype(BF16), TN)
    state[...] = state[...] * grown_w[span - 1 : span, :] + fresh
    cross = dot(c_low, b_low, NT)
    causal = iota((span, span), 1) <= iota((span, span), 0)
    low_lanes = iota((span, LANES), 1) < MP
    for pair in range(channels // LANES):
        lanes = slice(pair * LANES, (pair + 1) * LANES)
        first, second = pair_decay(cum, cum_rows, pair, causal)
        weights = jnp.concatenate(
            [(cross * first).astype(BF16), (cross * second).astype(BF16)], axis=1
        )
        y_ref[:, lanes] = dot(weights, pair_split(scaled_low[:, lanes], low_lanes))
    y = y_ref[...] + outer + skip * inputs
    y_ref[...] = y
    gated = y * jax.nn.silu(z_ref[...])
    gated_ref[...] = gated.astype(BF16)
    square_ref[...] = row_sums(gated * gated)

    for step in range(1, ring.ahead + 1):
        after = spans * step // ring.ahead - (2 if step == ring.ahead else 1)
        pl.when(turn == max(0, after))(functools.partial(ring.hop, step))
    pl.when(turn == spans - 1)(ring.finish)


def scan_backward(
    devices, spans, windows, pieces, outs_count, count,
    z_ref, x_ref, xp_ref, bc_ref, bp_ref, step_ref, y_ref, enter_ref,
    dyg_ref, scale_ref, inner_ref, dqkv_ref,
    tap_ref, tapb_ref, row_ref,
    *refs,
):
    sent, refs = refs[:count], refs[count:]
    (grad_ref, gx_ref, gh_ref), refs = refs[:3], refs[3:]
    outs, refs = refs[:outs_count], refs[outs_count:]
    (dstate, buffer, dbuffer, du_buf, col_buf), scratch = refs[:5], refs[5:]
    ring = RingScatter(devices, windows, pieces, sent, outs, scratch)
    span, channels = x_ref.shape
    turn = pl.program_id(0)

    @pl.when(turn == 0)
    def _():
        ring.greet()
        ring.begin()
        dstate[...] = jnp.zeros_like(dstate)
        dbuffer[...] = jnp.zeros_like(dbuffer)
        col_buf[...] = jnp.zeros_like(col_buf)
        gx_ref[...] = jnp.zeros_like(gx_ref)
        gh_ref[...] = jnp.zeros_like(gh_ref)

    inside = (turn < spans - 1).astype(F32)
    buffer[:EDGE, :channels] = xp_ref[...] * inside
    buffer[:EDGE, channels:] = bp_ref[...] * inside
    buffer[EDGE:, :channels] = x_ref[...]
    buffer[EDGE:, channels:] = bc_ref[...]
    spread = head_spread(channels)
    bias, gain, biasb, stepb, decay, skip = unpack_rows(row_ref, spread)
    taps = jnp.concatenate([tap_ref[...], tapb_ref[...]], axis=1).astype(F32)
    conv = causal_taps(buffer, taps, span) + jnp.concatenate([bias, biasb], axis=1)
    sig = jax.nn.sigmoid(conv)
    swished = conv * sig
    inputs, shared = swished[:, :channels], swished[:, channels:]
    b_low = shared[:, :NS].astype(BF16)
    c_low = shared[:, NS:].astype(BF16)
    raw, step, cum, step_w, tails_w, grown_w = span_rates(step_ref, stepb, decay, spread, span)
    cum_rows = cum.T
    scaled = inputs * step_w
    scaled_low = scaled.astype(BF16)

    z = z_ref[...]
    sig_z = jax.nn.sigmoid(z)
    swish = z * sig_z
    y = y_ref[...]
    scale = scale_ref[...].T[:, :1]
    normed = y * swish * scale
    dyg = dyg_ref[...]
    gain_grad = jnp.sum(dyg * normed, axis=0, keepdims=True)
    dgated = scale * (dyg * gain - normed * inner_ref[...].T[:, :1])
    dy = dgated * swish
    grad_ref[:, :channels] = (dgated * y * (sig_z * (1.0 + z * (1.0 - sig_z)))).astype(BF16)

    state_low = enter_ref[0].astype(BF16)
    dstate_low = dstate[...].astype(BF16)
    grown_low = (dy * grown_w).astype(BF16)
    dy_low = dy.astype(BF16)
    tailed = scaled * tails_w
    outer = dot(c_low, state_low) * grown_w
    from_state = dot(b_low, dstate_low)
    dc = dot(grown_low, state_low, NT)
    db = dot(tailed.astype(BF16), dstate_low, NT)
    leak = from_state * tailed
    last_w = grown_w[span - 1 : span, :]
    ends = (
        jnp.sum(leak, axis=0, keepdims=True)
        + jnp.sum(enter_ref[0] * dstate[...], axis=0, keepdims=True) * last_w
    )
    skips = jnp.sum(dy * inputs, axis=0, keepdims=True)
    dstate[...] = dstate[...] * last_w + dot(c_low, grown_low, TN)

    cross = dot(c_low, b_low, NT)
    causal = iota((span, span), 1) <= iota((span, span), 0)
    low_lanes = iota((span, LANES), 1) < MP
    lane = iota((span, LANES), 1)
    dcross = jnp.zeros((span, span), F32)
    row_part = jnp.zeros((span, LANES), F32)
    for pair in range(channels // LANES):
        lanes = slice(pair * LANES, (pair + 1) * LANES)
        decays = pair_decay(cum, cum_rows, pair, causal)
        dy_pair = pair_split(dy_low[:, lanes], low_lanes)
        dweights = dot(dy_pair, scaled_low[:, lanes], NT)
        both = []
        for part in range(2):
            head = 2 * pair + part
            dterm = dweights[part * span : (part + 1) * span] * decays[part]
            dcross = dcross + dterm
            flow = dterm * cross
            row_part = row_part + jnp.where(
                lane == head, jnp.sum(flow, axis=1, keepdims=True), 0.0
            )
            col_buf[head : head + 1, :] = jnp.sum(flow, axis=0, keepdims=True)
            both.append((cross * decays[part]).astype(BF16))
        du_buf[:, lanes] = dot(jnp.concatenate(both, axis=0), dy_pair, TN)
    du = du_buf[...] + from_state * tails_w
    dcross_low = dcross.astype(BF16)
    dc = dc + dot(dcross_low, b_low)
    db = db + dot(dcross_low, c_low, TN)

    sums = gather_heads(
        jnp.concatenate(
            [dy * outer - leak, du * inputs, ends, skips, jnp.zeros((EDGE - 2, channels), F32)],
            axis=0,
        ),
        spread,
    )
    at_end = sums[2 * span : 2 * span + 1, :]
    dcum = sums[:span] + row_part - col_buf[...].T
    upper = (iota((span, span), 1) >= iota((span, span), 0)).astype(BF16)
    drate = pick_left(upper, dcum, 3) + at_end
    dstep = drate * decay + sums[span : 2 * span]
    draw = dstep * jax.nn.sigmoid(raw)
    gh_ref[0:1, :] += jnp.sum(draw, axis=0, keepdims=True)
    gh_ref[1:2, :] += jnp.sum(drate * step, axis=0, keepdims=True) * decay
    gh_ref[2:3, :] += sums[2 * span + 1 : 2 * span + 2, :]

    dinputs = du * step_w + skip * dy
    dconv = jnp.concatenate([dinputs, db, dc], axis=1) * (sig * (1.0 + conv * (1.0 - sig)))
    dbuffer[span:, :] = dbuffer[:EDGE, :]
    dbuffer[:span, :] = dconv
    dbefore = jnp.zeros_like(dconv)
    for tap in range(KCONV):
        dbefore = dbefore + taps[tap : tap + 1, :] * window(dbuffer, KCONV - 1 - tap, span)
        gx_ref[tap : tap + 1, :] += jnp.sum(
            dconv * window(buffer, EDGE - KCONV + 1 + tap, span), axis=0, keepdims=True
        )
    gx_ref[KCONV : KCONV + 1, :] += jnp.sum(dconv, axis=0, keepdims=True)
    gx_ref[KCONV + 1 : KCONV + 2, :channels] += gain_grad
    width = 2 * channels + 2 * NS
    grad_ref[:, channels:width] = dbefore.astype(BF16)
    grad_ref[:, width : width + dqkv_ref.shape[1]] = dqkv_ref[...]
    grad_ref[:, width + dqkv_ref.shape[1] :] = draw.astype(BF16)
    for step in range(ring.ahead):
        pl.when(turn == spans * step // ring.ahead)(functools.partial(ring.hop, step))
    pl.when(turn == spans - 1)(ring.finish)


def scan_params(conv_x, conv_xb, conv_bc, conv_bcb, dt_bias, a_log, d_skip, w_mnorm):
    heads = dt_bias.shape[0]
    fill = jnp.zeros((LANES - heads,), BF16)
    flat = [conv_xb, w_mnorm, conv_bcb, dt_bias, fill, a_log, fill, d_skip, fill]
    size = sum(item.shape[0] for item in flat) // LANES
    flat.append(jnp.zeros((-size % EDGE * LANES,), BF16))
    rows = jnp.concatenate(flat).astype(F32).reshape(-1, LANES)
    return (conv_x, conv_bc, rows)


def unpack_rows(row_ref, spread):
    channels = spread.shape[1]
    count = channels // LANES
    at = 2 * count + 2 * NS // LANES

    def join_rows(first, number):
        return jnp.concatenate(
            [row_ref[i : i + 1, :] for i in range(first, first + number)], axis=1
        )

    skip = jnp.broadcast_to(row_ref[at + 2 : at + 3, :], (EDGE, LANES)).astype(BF16)
    return (
        join_rows(0, count),
        join_rows(count, count),
        join_rows(2 * count, 2 * NS // LANES),
        row_ref[at : at + 1, :],
        -jnp.exp(row_ref[at + 1 : at + 2, :]),
        dot(skip, spread)[:1],
    )


def whole_spec(array):
    return pl.BlockSpec(array.shape, lambda turn: (0,) * array.ndim)


def run_scan_forward(proj, qkv_width, params, shard, devices):
    tokens = proj.shape[0]
    channels = params[0].shape[1]
    step_at = (2 * channels + 2 * NS + qkv_width) // LANES
    spans = tokens // SPAN
    bc_at = 2 * channels // (2 * NS)
    rows = lambda width, at: pl.BlockSpec((SPAN, width), lambda turn: (turn, at))
    anywhere = pl.BlockSpec(memory_space=pl.ANY)
    return pl.pallas_call(
        functools.partial(scan_forward, devices, spans),
        grid=(spans,),
        out_shape=(
            jax.ShapeDtypeStruct((tokens, channels), F32),
            jax.ShapeDtypeStruct((tokens, channels), BF16),
            jax.ShapeDtypeStruct((EDGE, tokens), F32),
            jax.ShapeDtypeStruct((spans, NS, channels), F32),
            gather_shape(shard, devices),
        ),
        in_specs=[rows(channels, 0), rows(channels, 1), rows(2 * NS, bc_at), rows(LANES, step_at)]
        + [whole_spec(item) for item in params]
        + [anywhere],
        out_specs=(
            rows(channels, 0),
            rows(channels, 0),
            pl.BlockSpec((EDGE, SPAN), lambda turn: (0, turn)),
            pl.BlockSpec((1, NS, channels), lambda turn: (turn, 0, 0)),
            anywhere,
        ),
        scratch_shapes=[
            pltpu.VMEM((NS, channels), F32),
            pltpu.VMEM((SPAN + EDGE, channels + 2 * NS), F32),
        ]
        + gather_sems(devices),
        compiler_params=pltpu.CompilerParams(collective_id=2, has_side_effects=True),
        cost_estimate=cost(20),
        name="scan_forward",
    )(proj, proj, proj, proj, *params, shard)


def run_scan_backward(
    proj, y, entering, dyg, scale, inner, dqkv, params, sent, windows, pieces, shapes,
    devices,
):
    tokens, width = proj.shape
    channels = params[0].shape[1]
    qkv_width = dqkv.shape[1]
    step_at = (2 * channels + 2 * NS + qkv_width) // LANES
    spans = tokens // SPAN
    bc_at = 2 * channels // (2 * NS)
    edges = SPAN // EDGE
    rows = lambda size, at: pl.BlockSpec((SPAN, size), lambda turn: (spans - 1 - turn, at))
    edge = lambda size, at: pl.BlockSpec(
        (EDGE, size), lambda turn: (jnp.maximum((spans - 1 - turn) * edges - 1, 0), at)
    )
    keep = lambda shape: pl.BlockSpec(shape, lambda turn: (0, 0))
    shapes = tuple(jax.ShapeDtypeStruct(shape, F32) for shape in shapes)
    return pl.pallas_call(
        functools.partial(
            scan_backward, devices, spans, windows, pieces, len(shapes), len(sent)
        ),
        grid=(spans,),
        out_shape=(
            jax.ShapeDtypeStruct((tokens, width), BF16),
            jax.ShapeDtypeStruct((EDGE, channels + 2 * NS), F32),
            jax.ShapeDtypeStruct((EDGE, LANES), F32),
        )
        + shapes,
        in_specs=[
            rows(channels, 0),
            rows(channels, 1),
            edge(channels, 1),
            rows(2 * NS, bc_at),
            edge(2 * NS, bc_at),
            rows(LANES, step_at),
            rows(channels, 0),
            pl.BlockSpec((1, NS, channels), lambda turn: (spans - 1 - turn, 0, 0)),
            rows(channels, 0),
            pl.BlockSpec((EDGE, SPAN), lambda turn: (0, spans - 1 - turn)),
            pl.BlockSpec((EDGE, SPAN), lambda turn: (0, spans - 1 - turn)),
            rows(qkv_width, 0),
        ]
        + [whole_spec(item) for item in params]
        + [pl.BlockSpec(memory_space=pl.ANY)] * len(sent),
        out_specs=(
            rows(width, 0),
            keep((EDGE, channels + 2 * NS)),
            keep((EDGE, LANES)),
        )
        + tuple(keep(item.shape) for item in shapes),
        scratch_shapes=[
            pltpu.VMEM((NS, channels), F32),
            pltpu.VMEM((SPAN + EDGE, channels + 2 * NS), F32),
            pltpu.VMEM((SPAN + EDGE, channels + 2 * NS), F32),
            pltpu.VMEM((SPAN, channels), F32),
            pltpu.VMEM((LANES, SPAN), F32),
        ]
        + scatter_scratch(windows, sent[0].shape[0] // devices, devices),
        compiler_params=pltpu.CompilerParams(collective_id=6, has_side_effects=True),
        cost_estimate=cost(47),
        name="scan_backward",
    )(
        proj, proj, proj, proj, proj, proj, y, entering, dyg, scale, inner, dqkv, *params, *sent,
    )


def rotary_tables(tokens):
    half = HEAD_SIZE // 2
    exponent = np.arange(half, dtype=np.float64) * (-2.0 * LOG_BASE / HEAD_SIZE)
    rates = np.tile(np.exp(exponent.astype(np.float32)).astype(np.float64), LANES // half)
    tables = []
    for places in (np.arange(FINE), np.arange(0, tokens, FINE)):
        angles = places[:, None] * rates[None, :]
        tables += [np.cos(angles).astype(np.float32), np.sin(angles).astype(np.float32)]
    return tables


def fill_rotary(fine_cos, fine_sin, coarse_cos, coarse_sin, cosine, sine):
    small_cos, small_sin = fine_cos[...], fine_sin[...]
    for turn in range(coarse_cos.shape[0]):
        big_cos, big_sin = coarse_cos[turn : turn + 1, :], coarse_sin[turn : turn + 1, :]
        rows = slice(turn * FINE, (turn + 1) * FINE)
        cosine[rows, :] = small_cos * big_cos - small_sin * big_sin
        sine[rows, :] = small_sin * big_cos + small_cos * big_sin


def head_masks():
    half = HEAD_SIZE // 2
    row, col = iota((LANES, LANES), 0), iota((LANES, LANES), 1)
    place = col % HEAD_SIZE
    ahead = jnp.where(place < half, -1.0, 0.0)
    behind = jnp.where(place < half, 0.0, 1.0)

    def turn(start):
        return jnp.where(row == start + half, ahead, jnp.where(row == start - half, behind, 0.0))

    first = row < HEAD_SIZE
    left = col < HEAD_SIZE
    low = lambda mask: mask.astype(BF16)
    within = low(turn(col))
    copy = low(jnp.where(row == place, 1.0, 0.0))
    copy_turn = low(jnp.where(first, turn(place), 0.0))
    value = low(jnp.where(row == place + HEAD_SIZE, 1.0, 0.0))
    fold = low(jnp.where(left & (row % HEAD_SIZE == place), 1.0, 0.0))
    other = row % HEAD_SIZE
    fold_turn = low(
        jnp.where(
            left,
            jnp.where(other == place + half, ahead, jnp.where(other == place - half, behind, 0.0)),
            0.0,
        )
    )
    fold_value = low(jnp.where(left, 0.0, jnp.where(other == place, 1.0, 0.0)))
    return within, copy, copy_turn, value, fold, fold_turn, fold_value


def attend_forward(
    q_ref, kv_ref, fine_cos, fine_sin, coarse_cos, coarse_sin,
    qkv_ref, lse_ref, o_ref, vt, cos_ref, sin_ref,
):
    fill_rotary(fine_cos, fine_sin, coarse_cos, coarse_sin, cos_ref, sin_ref)
    tokens, query_width = q_ref.shape
    pairs = query_width // LANES
    within, copy, copy_turn, value = head_masks()[:4]

    def turn_rows(i, carry):
        rows = pl.ds(pl.multiple_of(i * QBLK, QBLK), QBLK)
        cosine, sine = cos_ref[rows, :], sin_ref[rows, :]
        for pair in range(pairs):
            lanes = slice(pair * LANES, (pair + 1) * LANES)
            query = q_ref[rows, lanes]
            turned = query * cosine + pick(query, within) * sine
            qkv_ref[rows, lanes] = (turned * HEAD_SIZE**-0.5).astype(BF16)
        kv = kv_ref[rows, :]
        keys = pick(kv, copy) * cosine + pick(kv, copy_turn) * sine
        qkv_ref[rows, query_width : query_width + LANES] = keys.astype(BF16)
        qkv_ref[rows, query_width + LANES :] = dot(kv.astype(BF16), value).astype(BF16)
        vt[:, rows] = kv.T[HEAD_SIZE:, :].astype(BF16)
        return carry

    lax.fori_loop(0, tokens // QBLK, turn_rows, 0)
    low_lanes = iota((QBLK, LANES), 1) < HEAD_SIZE
    wide = (QBLK, 2 * QBLK)
    visible = iota(wide, 0) <= iota(wide, 1) % QBLK

    def block(i, carry):
        here = pl.ds(pl.multiple_of(i * QBLK, QBLK), QBLK)
        queries = [
            pair_split(qkv_ref[here, pair * LANES : (pair + 1) * LANES], low_lanes)
            for pair in range(pairs)
        ]

        def tile(there, state, edge):
            keys = qkv_ref[there, query_width : query_width + LANES]
            result = []
            for pair in range(pairs):
                top, total, out = state[3 * pair : 3 * pair + 3]
                scores = dot(keys, queries[pair], NT)
                if edge:
                    scores = jnp.where(visible, scores, MASKED)
                higher = jnp.maximum(top, jnp.max(scores, axis=0, keepdims=True))
                probs = jnp.exp(scores - higher)
                fade = jnp.exp(top - higher)
                total = total * fade + jnp.sum(probs, axis=0, keepdims=True)
                out = out * fade + dot(vt[:, there], probs.astype(BF16))
                result += [higher, total, out]
            return tuple(result)

        state = (
            jnp.full((1, 2 * QBLK), MASKED, F32),
            jnp.zeros((1, 2 * QBLK), F32),
            jnp.zeros((HEAD_SIZE, 2 * QBLK), F32),
        ) * pairs
        state = lax.fori_loop(
            0,
            i,
            lambda j, state: tile(pl.ds(pl.multiple_of(j * QBLK, QBLK), QBLK), state, False),
            state,
        )
        state = tile(here, state, True)
        for pair in range(pairs):
            top, total, out = state[3 * pair : 3 * pair + 3]
            out = out / total
            lse = top + jnp.log(total)
            lse_ref[2 * pair : 2 * pair + 1, here] = lse[:, :QBLK]
            lse_ref[2 * pair + 1 : 2 * pair + 2, here] = lse[:, QBLK:]
            both = jnp.concatenate([out[:, :QBLK], out[:, QBLK:]], axis=0)
            o_ref[here, pair * LANES : (pair + 1) * LANES] = both.T.astype(BF16)
        return carry

    lax.fori_loop(0, tokens // QBLK, block, 0)


def attend_backward(
    qkv_ref, lse_ref, o_ref, do_ref, fine_cos, fine_sin, coarse_cos, coarse_sin,
    dqkv_ref,
    dq, kt, dk, dv, cos_ref, sin_ref,
):
    fill_rotary(fine_cos, fine_sin, coarse_cos, coarse_sin, cos_ref, sin_ref)
    tokens, query_width = o_ref.shape
    pairs = query_width // LANES
    key_lanes = slice(query_width, query_width + LANES)
    value_lanes = slice(query_width + LANES, query_width + 2 * LANES)

    def turn_keys(i, carry):
        rows = pl.ds(pl.multiple_of(i * QBLK, QBLK), QBLK)
        kt[:, rows] = qkv_ref[rows, key_lanes].astype(F32).T[:HEAD_SIZE, :].astype(BF16)
        return carry

    lax.fori_loop(0, tokens // QBLK, turn_keys, 0)
    dk[...] = jnp.zeros_like(dk)
    dv[...] = jnp.zeros_like(dv)
    low_lanes = iota((QBLK, LANES), 1) < HEAD_SIZE
    wide = (QBLK, 2 * QBLK)
    visible = iota(wide, 0) <= iota(wide, 1) % QBLK
    ones = jnp.ones((EDGE, LANES), BF16)

    def block(i, carry):
        here = pl.ds(pl.multiple_of(i * QBLK, QBLK), QBLK)
        queries, grads, inners, lses = [], [], [], []
        for pair in range(pairs):
            lanes = slice(pair * LANES, (pair + 1) * LANES)
            queries.append(pair_split(qkv_ref[here, lanes], low_lanes))
            grad = do_ref[here, lanes]
            grads.append(pair_split(grad, low_lanes))
            both = pair_split(grad.astype(F32) * o_ref[here, lanes].astype(F32), low_lanes)
            high, low = parts(both, 2)
            inners.append((dot(ones, high, NT) + dot(ones, low, NT))[:1])
            lses.append(
                jnp.concatenate(
                    [
                        lse_ref[2 * pair : 2 * pair + 1, here],
                        lse_ref[2 * pair + 1 : 2 * pair + 2, here],
                    ],
                    axis=1,
                )
            )
        query_all = jnp.concatenate(queries, axis=0)
        grad_all = jnp.concatenate(grads, axis=0)

        def tile(there, state, edge):
            keys = qkv_ref[there, key_lanes]
            values = qkv_ref[there, value_lanes]
            all_probs, all_dscores, result = [], [], []
            for pair in range(pairs):
                probs = dot(keys, queries[pair], NT) - lses[pair]
                if edge:
                    probs = jnp.where(visible, probs, MASKED)
                probs = jnp.exp(probs)
                dprobs = dot(values, grads[pair], NT)
                dscores = (probs * (dprobs - inners[pair])).astype(BF16)
                all_probs.append(probs.astype(BF16))
                all_dscores.append(dscores)
                result.append(state[pair] + dot(kt[:, there], dscores))
            dv[there, :] += dot(jnp.concatenate(all_probs, axis=1), grad_all)
            dk[there, :] += dot(jnp.concatenate(all_dscores, axis=1), query_all)
            return tuple(result)

        state = (jnp.zeros((HEAD_SIZE, 2 * QBLK), F32),) * pairs
        state = lax.fori_loop(
            0,
            i,
            lambda j, state: tile(pl.ds(pl.multiple_of(j * QBLK, QBLK), QBLK), state, False),
            state,
        )
        state = tile(here, state, True)
        for pair in range(pairs):
            both = jnp.concatenate([state[pair][:, :QBLK], state[pair][:, QBLK:]], axis=0)
            dq[here, pair * LANES : (pair + 1) * LANES] = both.T
        return carry

    lax.fori_loop(0, tokens // QBLK, block, 0)
    masks = head_masks()
    within, (fold, fold_turn, fold_value) = masks[0], masks[4:]

    def turn_back(i, carry):
        rows = pl.ds(pl.multiple_of(i * QBLK, QBLK), QBLK)
        cosine, sine = cos_ref[rows, :], sin_ref[rows, :]
        for pair in range(pairs):
            lanes = slice(pair * LANES, (pair + 1) * LANES)
            grad = dq[rows, lanes]
            grad = grad * cosine - pick(grad, within) * sine
            dqkv_ref[rows, lanes] = (grad * HEAD_SIZE**-0.5).astype(BF16)
        grad = dk[rows, :]
        grad = pick(grad, fold) * cosine - pick(grad, fold_turn) * sine
        grad = grad + pick(dv[rows, :], fold_value)
        dqkv_ref[rows, query_width:] = grad.astype(BF16)
        return carry

    lax.fori_loop(0, tokens // QBLK, turn_back, 0)


def run_attend_forward(proj, query_at, query_width, tables):
    tokens = proj.shape[0]
    cols = lambda size, at: pl.BlockSpec((tokens, size), lambda turn: (0, at // size))
    return pl.pallas_call(
        attend_forward,
        grid=(1,),
        out_shape=(
            jax.ShapeDtypeStruct((tokens, query_width + 2 * LANES), BF16),
            jax.ShapeDtypeStruct((EDGE, tokens), F32),
            jax.ShapeDtypeStruct((tokens, query_width), BF16),
        ),
        in_specs=[
            cols(query_width, query_at),
            cols(2 * HEAD_SIZE, query_at + query_width),
        ]
        + [whole_spec(table) for table in tables],
        out_specs=(
            cols(query_width + 2 * LANES, 0),
            pl.BlockSpec((EDGE, tokens), lambda turn: (0, 0)),
            cols(query_width, 0),
        ),
        scratch_shapes=[
            pltpu.VMEM((HEAD_SIZE, tokens), BF16),
            pltpu.VMEM((tokens, LANES), F32),
            pltpu.VMEM((tokens, LANES), F32),
        ],
        cost_estimate=cost(15),
        name="attend_forward",
    )(proj, proj, *tables)


def run_attend_backward(qkv, lse, attended, grads, grad_at, tables):
    tokens, query_width = attended.shape
    vmem = pl.BlockSpec(memory_space=pltpu.VMEM)
    cols = lambda size, at: pl.BlockSpec((tokens, size), lambda turn: (0, at // size))
    return pl.pallas_call(
        attend_backward,
        grid=(1,),
        out_shape=jax.ShapeDtypeStruct((tokens, query_width + 2 * HEAD_SIZE), BF16),
        in_specs=[
            whole_spec(qkv),
            whole_spec(lse),
            whole_spec(attended),
            cols(query_width, grad_at),
        ]
        + [whole_spec(table) for table in tables],
        out_specs=cols(query_width + 2 * HEAD_SIZE, 0),
        scratch_shapes=[
            pltpu.VMEM((tokens, query_width), F32),
            pltpu.VMEM((HEAD_SIZE, tokens), BF16),
            pltpu.VMEM((tokens, LANES), F32),
            pltpu.VMEM((tokens, LANES), F32),
            pltpu.VMEM((tokens, LANES), F32),
            pltpu.VMEM((tokens, LANES), F32),
        ],
        cost_estimate=cost(16),
        name="attend_backward",
    )(qkv, lse, attended, grads, *tables)


def feed_forward(
    x_ref, mixed_ref, other_ref, act_grad_ref, norms_ref, gu_ref,
    after_ref, scale_ref, hidden_ref, act_ref, dgu_ref, back_ref,
):
    units = act_grad_ref.shape[1]
    after = x_ref[...].astype(F32) + (mixed_ref[...].astype(F32) + other_ref[...].astype(F32))
    after_ref[...] = after.astype(BF16)
    scale = lax.rsqrt(jnp.mean(after * after, axis=-1, keepdims=True) + EPSILON)
    scale_ref[...] = scale
    hidden = (after * scale * norms_ref[1:2, :]).astype(BF16)
    hidden_ref[...] = hidden
    for start in range(0, units, UBLK):
        cols = slice(start, start + UBLK)
        up_cols = slice(units + start, units + start + UBLK)
        gate = dot(hidden, gu_ref[:, cols])
        upward = dot(hidden, gu_ref[:, up_cols])
        grad = act_grad_ref[:, cols]
        sigma = jax.nn.sigmoid(gate)
        swish = gate * sigma
        act_ref[:, cols] = (swish * upward).astype(BF16)
        slope = sigma * (1.0 + gate * (1.0 - sigma))
        dgu_ref[:, cols] = (grad * upward * slope).astype(BF16)
        dgu_ref[:, up_cols] = (grad * swish).astype(BF16)
    back_ref[...] = dot(dgu_ref[...], gu_ref[...], NT).astype(BF16)


def product_rows(dims, left_ref, right_ref, out_ref):
    out_ref[...] = dot(left_ref[...], right_ref[...], dims).astype(out_ref.dtype)


def run_product(left, right, dims, dtype):
    tokens, depth = left.shape
    cols = right.shape[1 - dims[1][0]]
    return pl.pallas_call(
        functools.partial(product_rows, dims),
        grid=(tokens // TBLK,),
        out_shape=jax.ShapeDtypeStruct((tokens, cols), dtype),
        in_specs=[pl.BlockSpec((TBLK, depth), lambda turn: (turn, 0)), once(right)],
        out_specs=pl.BlockSpec((TBLK, cols), lambda turn: (turn, 0)),
        cost_estimate=cost(4),
        name="product_rows",
    )(left, right)


def project(heads, x_ref, w_ref, hidden_ref, proj_ref, norms_ref):
    @pl.when(pl.program_id(0) == 0)
    def _():
        gains = w_ref[:, w_ref.shape[1] - LANES :].astype(F32).T
        norms_ref[...] = jnp.zeros_like(norms_ref)
        norms_ref[0:2, :] = gains[heads : heads + 2, :]

    x = x_ref[...].astype(F32)
    scale = lax.rsqrt(jnp.mean(x * x, axis=-1, keepdims=True) + EPSILON)
    hidden = (x * scale * norms_ref[0:1, :]).astype(BF16)
    hidden_ref[...] = hidden
    proj_ref[...] = dot(hidden, w_ref[...])


def run_project(x, w_in, heads):
    tokens, width = x.shape
    cols = w_in.shape[1]
    rows = lambda size: pl.BlockSpec((TBLK, size), lambda turn: (turn, 0))
    return pl.pallas_call(
        functools.partial(project, heads),
        grid=(tokens // TBLK,),
        out_shape=(
            jax.ShapeDtypeStruct((tokens, width), BF16),
            jax.ShapeDtypeStruct((tokens, cols), F32),
            jax.ShapeDtypeStruct((EDGE, width), F32),
        ),
        in_specs=[rows(width), once(w_in)],
        out_specs=(
            rows(width), rows(cols), pl.BlockSpec((EDGE, width), lambda turn: (0, 0)),
        ),
        cost_estimate=cost(8),
        name="project",
    )(x, w_in)


def project_back(grad_ref, w_ref, x_ref, before_ref, part_ref, gain_grad_ref):
    @pl.when(pl.program_id(0) == 0)
    def _():
        gain_grad_ref[...] = before_ref[...]

    x = x_ref[...].astype(F32)
    normed = x * lax.rsqrt(jnp.mean(x * x, axis=-1, keepdims=True) + EPSILON)
    part = dot(grad_ref[...], w_ref[...], NT).astype(BF16)
    part_ref[...] = part
    gain_grad_ref[:1, :] += jnp.sum(part.astype(F32) * normed, axis=0, keepdims=True)


def once(item):
    return pl.BlockSpec(item.shape, lambda turn: (0,) * item.ndim, pipeline_mode=pl.Buffered(1))


def run_project_back(half, grads, w_in, x, before):
    tokens, width = x.shape
    cols = w_in.shape[1]
    turns = tokens // TBLK // 2
    rows = lambda size: pl.BlockSpec((TBLK, size), lambda turn: (turn + half * turns, 0))
    return pl.pallas_call(
        project_back,
        grid=(turns,),
        out_shape=(
            jax.ShapeDtypeStruct((tokens // 2, width), BF16),
            jax.ShapeDtypeStruct((EDGE, width), F32),
        ),
        in_specs=[rows(cols), once(w_in), rows(width), once(before)],
        out_specs=(
            pl.BlockSpec((TBLK, width), lambda turn: (turn, 0)),
            pl.BlockSpec((EDGE, width), lambda turn: (0, 0)),
        ),
        cost_estimate=cost(5),
        name="project_back",
    )(grads, w_in, x, before)


def run_feed_forward(x, mixed, other, act_grad, norms, w_gate_up):
    tokens, width = x.shape
    units = act_grad.shape[1]
    rows = lambda size: pl.BlockSpec((TBLK, size), lambda turn: (turn, 0))
    shape = jax.ShapeDtypeStruct
    return pl.pallas_call(
        feed_forward,
        grid=(tokens // TBLK,),
        out_shape=(
            shape((tokens, width), BF16),
            shape((tokens, 1), F32),
            shape((tokens, width), BF16),
            shape((tokens, units), BF16),
            shape((tokens, 2 * units), BF16),
            shape((tokens, width), BF16),
        ),
        in_specs=[rows(width)] * 3 + [rows(units), once(norms), once(w_gate_up)],
        out_specs=(rows(width), rows(1), rows(width), rows(units), rows(2 * units), rows(width)),
        cost_estimate=cost(14),
        name="feed_forward",
    )(x, mixed, other, act_grad, norms, w_gate_up)


def mixer_forward(gated_ref, scale_ref, gain_ref, attended_ref, w_ref, low_ref, mixed_ref):
    channels = gated_ref.shape[1]
    scale = scale_ref[...].T[:, :1]
    low_ref[:, :channels] = (gated_ref[...].astype(F32) * scale * gain_ref[...]).astype(BF16)
    low_ref[:, channels:] = attended_ref[...]
    mixed_ref[...] = dot(low_ref[...], w_ref[...], NT).astype(BF16)


def run_mixer_forward(gated, scale, gain, attended, w_out):
    tokens, channels = gated.shape
    width, inner = w_out.shape
    rows = lambda size: pl.BlockSpec((TBLK, size), lambda turn: (turn, 0))
    return pl.pallas_call(
        mixer_forward,
        grid=(tokens // TBLK,),
        out_shape=(
            jax.ShapeDtypeStruct((tokens, inner), BF16),
            jax.ShapeDtypeStruct((tokens, width), BF16),
        ),
        in_specs=[
            rows(channels),
            pl.BlockSpec((EDGE, TBLK), lambda turn: (0, turn)),
            once(gain),
            rows(attended.shape[1]),
            once(w_out),
        ],
        out_specs=(rows(inner), rows(width)),
        cost_estimate=cost(5),
        name="mixer_forward",
    )(gated, scale, gain, attended, w_out)


def mixer_backward(
    part_ref, other_ref, after_ref, scale_ref, top_ref, norms_ref,
    w_ref, gated_ref, scale_m_ref, gain_m_ref,
    low_ref, mamba_ref, attended_ref, inner_ref, gain_grad_ref,
):
    channels = gated_ref.shape[1]

    @pl.when(pl.program_id(0) == 0)
    def _():
        gain_grad_ref[...] = jnp.zeros_like(gain_grad_ref)

    grad = part_ref[...].astype(F32) + other_ref[...].astype(F32)
    scale = scale_ref[...]
    normed = after_ref[...].astype(F32) * scale
    gain_grad_ref[:1, :] += jnp.sum(grad * normed, axis=0, keepdims=True)
    weighted = grad * norms_ref[1:2, :]
    mean = jnp.mean(weighted * normed, axis=-1, keepdims=True)
    total = top_ref[...].astype(F32) + scale * (weighted - normed * mean)
    low_ref[...] = total.astype(BF16)
    back = dot(low_ref[...], w_ref[...])
    mamba = back[:, :channels]
    mamba_ref[...] = mamba
    attended_ref[...] = back[:, channels:].astype(BF16)
    inner_ref[...] = row_sums(mamba * gain_m_ref[...] * gated_ref[...].astype(F32)) * scale_m_ref[...]


def run_mixer_backward(part, other, after, scale, top, norms, w_out, gated, scale_m, gain_m):
    tokens, width = after.shape
    channels = gated.shape[1]
    inner = w_out.shape[1]
    shape = jax.ShapeDtypeStruct
    rows = lambda size: pl.BlockSpec((NBLK, size), lambda turn: (turn, 0))
    lanes = pl.BlockSpec((EDGE, NBLK), lambda turn: (0, turn))
    return pl.pallas_call(
        mixer_backward,
        grid=(tokens // NBLK,),
        out_shape=(
            shape((tokens, width), BF16),
            shape((tokens, channels), F32),
            shape((tokens, inner - channels), BF16),
            shape((EDGE, tokens), F32),
            shape((EDGE, width), F32),
        ),
        in_specs=[rows(width)] * 3
        + [rows(1), rows(width), once(norms), once(w_out), rows(channels), lanes, once(gain_m)],
        out_specs=(
            rows(width), rows(channels), rows(inner - channels), lanes,
            pl.BlockSpec((EDGE, width), lambda turn: (0, 0)),
        ),
        cost_estimate=cost(8),
        name="mixer_backward",
    )(part, other, after, scale, top, norms, w_out, gated, scale_m, gain_m)


def lane_row(ref, first, count):
    return jnp.concatenate([ref[i : i + 1, :] for i in range(first, first + count)], axis=1)


def own_lanes(ref, first, size):
    start = lax.axis_index("dp") * size
    row = ref[pl.ds(first + lax.div(start, LANES), 1), :]
    row = jnp.broadcast_to(row, (EDGE, LANES))
    return pltpu.roll(row, lax.rem(LANES - lax.rem(start, LANES), LANES), 1)[0, :size]


def finish_layer(
    norm_at, x_ref, norms_ref, pa_ref, oa_ref, pb_ref, ob_ref, grad_ref, after_ref, ffn_ref, ffn_other_ref,
    total_ref, *refs,
):
    count = (len(refs) - 9) // 2
    passed, out_ref, result_ref, handed = refs[:count], refs[count], refs[count + 1], refs[count + 2 :]
    tap_ref, bias_ref, gain_ref, step_ref, log_ref, skip_ref, norm_ref = handed[count:]

    @pl.when(pl.program_id(0) == 0)
    def _():
        for source, target in zip(passed, handed):
            target[...] = source[...]
        rows = tap_ref.shape[1] // LANES
        for tap in range(KCONV):
            tap_ref[tap : tap + 1, :] = lane_row(total_ref, tap * rows, rows)
        bias_ref[...] = lane_row(total_ref, KCONV * rows, rows)[0]
        gain_ref[...] = lane_row(total_ref, (KCONV + 1) * rows, rows)[0]
        at = (KCONV + 2) * rows
        for place, ref in enumerate((step_ref, log_ref, skip_ref)):
            ref[...] = total_ref[at + place : at + place + 1, :][0, : ref.shape[0]]
        norm_ref[...] = own_lanes(total_ref, norm_at, norm_ref.shape[0])

    x = x_ref[...].astype(F32)
    scale = lax.rsqrt(jnp.mean(x * x, axis=-1, keepdims=True) + EPSILON)
    normed = x * scale
    grad = jnp.where(
        pl.program_id(0) < pl.num_programs(0) // 2,
        pa_ref[...].astype(F32) + oa_ref[...].astype(F32),
        pb_ref[...].astype(F32) + ob_ref[...].astype(F32),
    )
    weighted = grad * norms_ref[0:1, :]
    mean = jnp.mean(weighted * normed, axis=-1, keepdims=True)
    out_ref[...] = grad_ref[...].astype(F32) + scale * (weighted - normed * mean)
    ffn = ffn_ref[...].astype(F32) + ffn_other_ref[...].astype(F32)
    result_ref[...] = (after_ref[...].astype(F32) + ffn).astype(BF16)


def run_finish(
    x, norms, halves, grad, after, ffn, ffn_other, total, passed, channels, heads, shard, norm_at
):
    tokens, width = x.shape
    rows = pl.BlockSpec((TBLK, width), lambda turn: (turn, 0))
    turns = tokens // TBLK // 2
    low_half = pl.BlockSpec((TBLK, width), lambda turn: (jnp.minimum(turn, turns - 1), 0))
    high_half = pl.BlockSpec((TBLK, width), lambda turn: (jnp.maximum(turn - turns, 0), 0))
    shape = lambda *sizes: jax.ShapeDtypeStruct(sizes, F32)
    small = (
        shape(KCONV, channels), shape(channels), shape(channels), shape(heads), shape(heads),
        shape(heads), shape(shard),
    )
    return pl.pallas_call(
        functools.partial(finish_layer, norm_at),
        grid=(tokens // TBLK,),
        out_shape=(shape(tokens, width), jax.ShapeDtypeStruct((tokens, width), BF16))
        + tuple(shape(*item.shape) for item in passed)
        + small,
        in_specs=[rows, once(norms)]
        + [low_half] * 2
        + [high_half] * 2
        + [rows] * 4
        + [once(total)] + [once(item) for item in passed],
        out_specs=(rows, rows) + tuple(once(item) for item in passed + small),
        cost_estimate=cost(8),
        name="finish_layer",
    )(x, norms, *halves, grad, after, ffn, ffn_other, total, *passed)


def finish_shared(at, total_ref, cross_ref, mine_ref, other_ref, bc_ref, tap_ref, bias_ref, norm_ref, both):
    half = lax.axis_index("tensor")
    cols = pl.ds(pl.multiple_of(half * LANES, LANES), LANES)
    bc_ref[...] = mine_ref[:, cols] + other_ref[:, cols]
    both[...] = total_ref[...] + cross_ref[...]
    for tap in range(KCONV):
        tap_ref[tap : tap + 1, :] = both[pl.ds(at + 2 * tap + half, 1), :]
    bias_ref[...] = both[pl.ds(at + 2 * KCONV + half, 1), :][0]
    norm_ref[...] = own_lanes(both, at + 2 * KCONV + 2, norm_ref.shape[0])


def run_finish_shared(total, cross, mine, other, shard, at):
    vmem = pl.BlockSpec(memory_space=pltpu.VMEM)
    shape = lambda *sizes: jax.ShapeDtypeStruct(sizes, F32)
    return pl.pallas_call(
        functools.partial(finish_shared, at),
        out_shape=(shape(mine.shape[0], LANES), shape(KCONV, LANES), shape(LANES), shape(shard)),
        in_specs=[vmem] * 4,
        out_specs=(vmem,) * 4,
        scratch_shapes=[pltpu.VMEM(total.shape, F32)],
        name="finish_shared",
    )(total, cross, mine, other)


def swap(partial):
    return lax.ppermute(partial, "tensor", [(0, 1), (1, 0)])


def join(mine, other):
    return mine.astype(F32) + other.astype(F32)


def tensor_sum(partial):
    return join(partial, swap(partial))


def thirds(size):
    part = size // 3
    return [(0, part), (part, 2 * part), (2 * part, size)]


def local(
    layer_input, w_norm1, w_zx, w_bc, w_dt, conv_x, conv_xb, conv_bc, conv_bcb, dt_bias, a_log,
    d_skip, w_mnorm, w_mout, query_key_value_weight, output_weight, w_norm2, w_gu, w_down,
    grad_output,
):
    devices = lax.axis_size("dp")
    tokens, width = layer_input.shape
    shard = w_zx.shape[0]
    channels = conv_xb.shape[0]
    heads = dt_bias.shape[0]
    qkv_width = query_key_value_weight.shape[2]
    units = w_down.shape[0]
    attn_width = output_weight.shape[1]
    tail = jnp.concatenate(
        [w_dt, w_norm1[:, None], w_norm2[:, None], jnp.zeros((shard, LANES - heads - 2), BF16)],
        axis=1,
    )
    mixer_in = jnp.concatenate(
        [w_zx.reshape(shard, -1), w_bc, query_key_value_weight.reshape(shard, -1), tail], axis=1
    )
    in_width = mixer_in.shape[1]
    (w_in,) = gather_rows([mixer_in], devices, 0, [(0, *window) for window in thirds(in_width)])
    w_in, *small_params = lax.optimization_barrier(
        (w_in, conv_x, conv_xb, conv_bc, conv_bcb, dt_bias, a_log, d_skip, w_mnorm)
    )
    params = scan_params(*small_params)
    hidden_one, proj, norms = run_project(layer_input, w_in, heads)
    out_shard = jnp.concatenate([w_mout.T, output_weight.reshape(attn_width, -1).T], axis=1)
    y, gated, square_sum, entering, w_out = run_scan_forward(
        proj, qkv_width, params, out_shard, devices
    )
    channels_all = channels * lax.axis_size("tensor")
    scale_m = lax.rsqrt(tensor_sum(square_sum) / channels_all + EPSILON)
    tables = rotary_tables(tokens)
    qkv_at = 2 * channels + 2 * NS
    qkv, lse, attended = run_attend_forward(proj, qkv_at, attn_width, tables)
    gain_m = w_mnorm.astype(F32)[None, :]
    mixer_out, mixed = run_mixer_forward(gated, scale_m, gain_m, attended, w_out)
    mixed, gate_up_shard, down_shard = lax.optimization_barrier(
        (mixed, w_gu.reshape(shard, -1), w_down.T)
    )
    other = swap(mixed)
    w_gate_up, w_down_t = gather_rows(
        [gate_up_shard, down_shard],
        devices,
        3,
        [(0, 0, units), (0, units, 2 * units), (1, 0, units)],
    )
    act_grad = run_product(grad_output, w_down_t, NN, F32)
    other, w_gate_up, w_down_t, act_grad = lax.optimization_barrier(
        (other, w_gate_up, w_down_t, act_grad)
    )
    after, scale_two, hidden_two, activated, grad_gu_low, partial_two = run_feed_forward(
        layer_input, mixed, other, act_grad, norms, w_gate_up
    )
    other = swap(partial_two)
    grad_down = dot(grad_output, activated, TN).astype(BF16)
    (mine_gu,) = scatter_product(
        hidden_two,
        grad_gu_low,
        [
            ([(0, 1, 0, units)], [(0, 0, units, 0, 0)]),
            ([(0, 1, units, 2 * units)], [(0, 0, units, 0, 1)]),
        ],
        [(shard, 2, units)],
        devices,
        1,
    )
    ffn_part = run_product(activated, w_down_t, NT, BF16)
    other, mine_gu, grad_down, ffn_part = lax.optimization_barrier(
        (other, mine_gu, grad_down, ffn_part)
    )
    ffn_other = swap(ffn_part)
    grad_mix_low, grad_mamba, grad_attended, inner_m, grad_norm2 = run_mixer_backward(
        partial_two, other, after, scale_two, grad_output, norms, w_out, gated, scale_m, gain_m
    )
    inner_m = tensor_sum(inner_m) / channels_all
    dqkv = run_attend_backward(qkv, lse, attended, grad_attended, 0, tables)
    grad_out = dot(grad_mix_low, mixer_out, TN).astype(BF16)
    windows = [(0, None, 0, channels + attn_width), (1, None, 0, units)]
    pieces = [
        (0, 0, channels, 0, None),
        (0, channels, channels + attn_width, 1, None),
        (1, 0, units, 2, None),
    ]
    shapes = [(shard, channels), (shard, attn_width), (shard, units)]
    grad_proj, small_x, small_h, mine_mout, mine_o, mine_down = run_scan_backward(
        proj, y, entering, grad_mamba, scale_m, inner_m, dqkv, params,
        [grad_out, grad_down], windows, pieces, shapes, devices,
    )
    ffn_other, grad_proj = lax.optimization_barrier((ffn_other, grad_proj))
    part_a, grad_norm1 = run_project_back(
        0, grad_proj, w_in, layer_input, jnp.zeros((EDGE, width), F32)
    )
    other_a = swap(part_a)
    part_b, grad_norm1 = run_project_back(1, grad_proj, w_in, layer_input, grad_norm1)
    part_b, grad_proj = lax.optimization_barrier((part_b, grad_proj))
    other_b = swap(part_b)
    lanes_of = lambda size, start=0: range(start, start + size, LANES)
    places = [(0, row, lane) for row in range(KCONV + 2) for lane in lanes_of(channels)]
    places += [(1, row, 0) for row in range(3)]
    norm_at = len(places)
    places += [(2, 0, lane) for lane in lanes_of(width)]
    cross_at = len(places)
    places += [(0, row, lane) for row in range(KCONV + 1) for lane in lanes_of(2 * NS, channels)]
    places += [(3, 0, lane) for lane in lanes_of(width)]
    shared_at = 2 * channels
    mine_zx, mine_bc, mine_qkv, mine_step, small = scatter_product(
        hidden_one,
        grad_proj,
        [
            ([(0, 1, 0, channels)], [(0, 0, channels, 0, 0)]),
            ([(0, 1, channels, shared_at)], [(0, 0, channels, 0, 1)]),
            (
                [(0, 1, shared_at, in_width)],
                [
                    (0, 0, 2 * NS, 1, None),
                    (0, 2 * NS, 2 * NS + qkv_width, 2, 0),
                    (0, 2 * NS + qkv_width, in_width - shared_at, 3, "turned"),
                ],
            ),
        ],
        [
            (shard, 2, channels),
            (shard, 2 * NS),
            (shard, 1, qkv_width),
            (heads, shard),
        ],
        devices,
        5,
        (small_x, small_h, grad_norm2, grad_norm1),
        places,
    )
    other_a, other_b, mine_bc = lax.optimization_barrier((other_a, other_b, mine_bc))
    passed = (mine_zx, mine_qkv, mine_step, mine_mout, mine_o, mine_gu, mine_down)
    cross, other_bc = swap(small), swap(mine_bc)
    grad_source, result, *rest = run_finish(
        layer_input, norms, (part_a, other_a, part_b, other_b), grad_mix_low, after, ffn_part,
        ffn_other, small, passed, channels, heads, shard, norm_at,
    )
    mine_zx, mine_qkv, mine_step, mine_mout, mine_o, mine_gu, mine_down = rest[: len(passed)]
    grad_taps, grad_bias, grad_gain, grad_steps, grad_log, grad_skip, own_norm2 = rest[len(passed) :]
    grad_bc, grad_tapsb, grad_biasb, own_norm1 = run_finish_shared(
        small, cross, mine_bc, other_bc, shard, cross_at
    )
    return (
        result,
        grad_source,
        own_norm1,
        mine_zx,
        grad_bc,
        mine_step.T,
        grad_taps,
        grad_bias,
        grad_tapsb,
        grad_biasb,
        grad_steps,
        grad_log,
        grad_skip,
        grad_gain,
        mine_mout.T,
        mine_qkv,
        mine_o.T.reshape(output_weight.shape),
        own_norm2,
        mine_gu,
        mine_down.T,
    )


def solution(mesh):
    return jax.shard_map(
        local,
        mesh=mesh,
        in_specs=(
            P("dp", None),
            P("dp"),
            P("dp", None, "tensor"),
            P("dp", None),
            P("dp", "tensor"),
            P(None, "tensor"),
            P("tensor"),
            P(),
            P(),
            P("tensor"),
            P("tensor"),
            P("tensor"),
            P("tensor"),
            P("tensor", "dp"),
            P("dp", "tensor", None),
            P("tensor", None, "dp"),
            P("dp"),
            P("dp", None, "tensor"),
            P("tensor", "dp"),
            P("dp", None),
        ),
        out_specs=(
            P("dp", None),
            P("dp", None),
            P("dp"),
            P("dp", None, "tensor"),
            P("dp", "tensor"),
            P("dp", "tensor"),
            P(None, "tensor"),
            P("tensor"),
            P(None, "tensor"),
            P("tensor"),
            P("tensor"),
            P("tensor"),
            P("tensor"),
            P("tensor"),
            P("tensor", "dp"),
            P("dp", "tensor", None),
            P("tensor", None, "dp"),
            P("dp"),
            P("dp", None, "tensor"),
            P("tensor", "dp"),
        ),
        check_vma=False,
    )
```

```python
import functools
import math

import jax
import jax.numpy as jnp
import numpy as np
from jax import lax
from jax.experimental import pallas as pl
from jax.experimental.pallas import tpu as pltpu
from jax.sharding import PartitionSpec as P

HEAD_SIZE = 64
MP = 64
NS = 128
KCONV = 4
SPAN = 128
QBLK = 256
FINE = 32
TBLK = 256
NBLK = 128
UBLK = 256
LANES = 128
EDGE = 8

EPSILON = 1e-05
HIGHEST = lax.Precision.HIGHEST
LOG_BASE = math.log(100000000000.0)
MASKED = -1e30
MESH = pl.DeviceIdType.MESH
F32 = jnp.float32
BF16 = jnp.bfloat16

NN = ((1,), (0,))
NT = ((1,), (1,))
TN = ((0,), (0,))


def dot(left, right, dims=NN, precision=None):
    return lax.dot_general(
        left, right, (dims, ((), ())), preferred_element_type=F32, precision=precision
    )


def iota(shape, dim):
    return lax.broadcasted_iota(jnp.int32, shape, dim)


def ring_place(chip, chips):
    odd = lax.rem(chip, 2)
    half = lax.div(chip, 2)
    return (1 - odd) * half + odd * (chips - 1 - half)


def ring_chip(place, chips):
    place = lax.rem(place + 4 * chips, chips)
    back = lax.div(place, chips // 2)
    return (1 - back) * (2 * place) + back * (2 * (chips - 1 - place) + 1)


def ring_setup(chips):
    me = lax.axis_index("dp")
    group = lax.axis_index("tensor")
    chip = lax.div(me, 2)
    core = lax.rem(me, 2)
    place = ring_place(chip, chips)
    right = ring_chip(place + 1, chips) * 2 + core
    left = ring_chip(place - 1, chips) * 2 + core
    mate = chip * 2 + (1 - core)
    barrier = pltpu.get_barrier_semaphore()
    for other in (right, left, mate):
        pl.semaphore_signal(barrier, inc=1, device_id=(other, group), device_id_type=MESH)
    pl.semaphore_wait(barrier, 3)
    return me, group, core, place, right, left, mate


class RingGather:
    def __init__(self, devices, x_ref, o_ref, sems, cols=slice(None)):
        self.cols = cols
        self.chips = devices // 2
        self.ahead = self.chips // 2
        self.behind = self.chips - 1 - self.ahead
        self.x_ref, self.o_ref, self.rows = x_ref, o_ref, x_ref.shape[0]
        self.fs, self.fr, self.bs, self.br, self.cs, self.cr, self.own_sem = sems

    def locate(self):
        me = lax.axis_index("dp")
        self.group = lax.axis_index("tensor")
        self.core = lax.rem(me, 2)
        chip = lax.div(me, 2)
        self.place = ring_place(chip, self.chips)
        self.right = ring_chip(self.place + 1, self.chips) * 2 + self.core
        self.left = ring_chip(self.place - 1, self.chips) * 2 + self.core
        self.mate = chip * 2 + (1 - self.core)
        self.me = me

    def slot(self, index):
        rows = pl.ds(pl.multiple_of(index * self.rows, self.rows), self.rows)
        return self.o_ref.at[rows, self.cols]

    def copy(self, shift, ssem, rsem, target):
        if shift == 0:
            index, source = self.me, self.x_ref.at[:, self.cols]
        else:
            index = ring_chip(self.place + shift, self.chips) * 2 + self.core
            source = self.slot(index)
        return pltpu.make_async_remote_copy(
            src_ref=source,
            dst_ref=self.slot(index),
            send_sem=ssem,
            recv_sem=rsem,
            device_id=(target, self.group),
            device_id_type=MESH,
        )

    def fore(self, step):
        return self.copy(-step, self.fs.at[step], self.fr.at[step], self.right)

    def back(self, step):
        return self.copy(step, self.bs.at[step], self.br.at[step], self.left)

    def across(self, shift):
        number = 0 if shift == 0 else 2 * abs(shift) - (1 if shift < 0 else 0)
        return self.copy(shift, self.cs.at[number], self.cr.at[number], self.mate)

    def own(self):
        return pltpu.make_async_copy(
            self.x_ref.at[:, self.cols], self.slot(self.me), self.own_sem
        )

    def greet(self):
        self.locate()
        barrier = pltpu.get_barrier_semaphore()
        for other in (self.right, self.left, self.mate):
            pl.semaphore_signal(
                barrier, inc=1, device_id=(other, self.group), device_id_type=MESH
            )
        pl.semaphore_wait(barrier, 3)

    def begin(self):
        self.locate()
        self.fore(0).start()
        self.back(0).start()
        self.across(0).start()
        self.own().start()

    def hop(self, step):
        self.locate()
        self.fore(step - 1).wait_recv()
        if step < self.ahead:
            self.fore(step).start()
        self.across(-step).start()
        if step <= self.behind:
            self.back(step - 1).wait_recv()
            if step < self.behind:
                self.back(step).start()
            self.across(step).start()

    def finish(self):
        self.locate()
        self.own().wait()
        for step in range(self.ahead):
            self.fore(step).wait_send()
        for step in range(self.behind):
            self.back(step).wait_send()
        for shift in range(-self.ahead, self.behind + 1):
            self.across(shift).wait()


def gather_sems(devices):
    dma = pltpu.SemaphoreType.DMA
    return [dma((devices // 2,))] * 6 + [dma(())]


def gather_shape(shard, devices):
    return jax.ShapeDtypeStruct((shard.shape[0] * devices, shard.shape[1]), shard.dtype)


def gather_kernel(devices, count, windows, *refs):
    shards, outs, sems = refs[:count], refs[count : 2 * count], refs[2 * count :]
    each = len(sems) // len(windows)
    rings = [
        RingGather(
            devices, shards[i], outs[i], sems[place * each : (place + 1) * each], slice(first, last)
        )
        for place, (i, first, last) in enumerate(windows)
    ]
    rings[0].greet()
    for ring in rings:
        ring.begin()
    for step in range(1, rings[0].ahead + 1):
        for ring in rings:
            ring.hop(step)
    for ring in rings:
        ring.finish()


def cost(micros):
    return pl.CostEstimate(flops=int(micros * 1e9), bytes_accessed=0, transcendentals=0)


def gather_rows(shards, devices, collective, windows):
    count = len(shards)
    anywhere = pl.BlockSpec(memory_space=pl.ANY)
    return pl.pallas_call(
        functools.partial(gather_kernel, devices, count, windows),
        out_shape=tuple(gather_shape(shard, devices) for shard in shards),
        in_specs=[anywhere] * count,
        out_specs=(anywhere,) * count,
        scratch_shapes=gather_sems(devices) * len(windows),
        compiler_params=pltpu.CompilerParams(collective_id=collective, has_side_effects=True),
        cost_estimate=cost(3),
        name="gather_rows",
    )(*shards)


def scatter_order(chips):
    ahead = chips // 2
    behind = chips - 1 - ahead
    order = []
    for step in range(ahead):
        order.append(-(ahead - step))
        if step < behind:
            order.append(behind - step)
    order.append(0)
    return order


class RingScatter:
    def __init__(self, devices, windows, pieces, operands, outs, scratch):
        self.chips = devices // 2
        self.ahead = self.chips // 2
        self.behind = self.chips - 1 - self.ahead
        self.windows, self.pieces, self.operands, self.outs = windows, pieces, operands, outs
        count = len(windows)
        self.mine, self.boxes, rest = scratch[:count], scratch[count : 2 * count], scratch[2 * count :]
        self.fbox, self.bbox, self.fout, self.bout = rest[:4]
        self.os, self.ms, self.mr, self.fs, self.fr, self.bs, self.br = rest[4:]
        self.rows = self.fbox.shape[1]
        widths = [item.shape[2] for item in self.mine]
        self.cols = [slice(sum(widths[:i]), sum(widths[: i + 1])) for i in range(count)]

    def locate(self):
        me = lax.axis_index("dp")
        self.group = lax.axis_index("tensor")
        self.core = lax.rem(me, 2)
        chip = lax.div(me, 2)
        self.place = ring_place(chip, self.chips)
        self.right = ring_chip(self.place + 1, self.chips) * 2 + self.core
        self.left = ring_chip(self.place - 1, self.chips) * 2 + self.core
        self.mate = chip * 2 + (1 - self.core)

    def greet(self):
        self.locate()
        barrier = pltpu.get_barrier_semaphore()
        for other in (self.right, self.left, self.mate):
            pl.semaphore_signal(
                barrier, inc=1, device_id=(other, self.group), device_id_type=MESH
            )
        pl.semaphore_wait(barrier, 3)

    def product(self, i):
        return self.windows[i][1] is not None

    def shift_of(self, slot):
        step = slot // 2
        odd = slot % 2
        return (1 - odd) * (step - self.ahead) + odd * (self.behind - step)

    def half(self, which):
        return pl.ds(pl.multiple_of(which * self.rows, self.rows), self.rows)

    def block(self, i, slot, which):
        index = ring_chip(self.place + self.shift_of(slot), self.chips) * 2 + which
        left, right, first, last = self.windows[i]
        return self.operands[left].at[self.half(index), first:last]

    def remote(self, source, target_ref, ssem, rsem, target):
        return pltpu.make_async_remote_copy(
            src_ref=source,
            dst_ref=target_ref,
            send_sem=ssem,
            recv_sem=rsem,
            device_id=(target, self.group),
            device_id_type=MESH,
        )

    def across(self, i, slot):
        if self.product(i):
            source = self.mine[i].at[slot, self.half(1 - self.core)]
        else:
            source = self.block(i, slot, 1 - self.core)
        return self.remote(
            source, self.boxes[i].at[slot], self.ms.at[i, slot], self.mr.at[i, slot], self.mate
        )

    def own(self, i, slot):
        return pltpu.make_async_copy(
            self.block(i, slot, self.core), self.mine[i].at[slot], self.os.at[i, slot]
        )

    def fore(self, step):
        return self.remote(
            self.fout.at[step], self.fbox.at[step], self.fs.at[step], self.fr.at[step], self.right
        )

    def back(self, step):
        return self.remote(
            self.bout.at[step], self.bbox.at[step], self.bs.at[step], self.br.at[step], self.left
        )

    def begin(self):
        self.locate()
        for i in range(len(self.windows)):
            if not self.product(i):
                for slot in range(self.chips):
                    self.across(i, slot).start()
                    self.own(i, slot).start()

    def produce(self, slot):
        chip = ring_chip(self.place + self.shift_of(slot), self.chips)
        size = 2 * self.rows
        for i, (left, right, first, last) in enumerate(self.windows):
            if right is None:
                continue
            at = pl.multiple_of(chip * size, size)
            terms = dot(self.operands[left][pl.ds(at, size), :], self.operands[right][:, first:last])
            self.mine[i][slot] = terms.astype(BF16)
            self.across(i, slot).start()

    def local_sum(self, i, slot, cols, others):
        rows = self.half(self.core) if self.product(i) else slice(None)
        total = self.mine[i][slot, rows, cols].astype(F32) + self.boxes[i][slot, :, cols].astype(F32)
        whole = slice(self.cols[i].start + cols.start, self.cols[i].start + cols.stop)
        for ref in others:
            total = total + ref[:, whole].astype(F32)
        return total

    def arrive(self, slot):
        for i in range(len(self.windows)):
            if not self.product(i):
                self.own(i, slot).wait()
            self.across(i, slot).wait_recv()

    def put(self, target, slot, others):
        self.arrive(slot)
        for i, cols in enumerate(self.cols):
            total = self.local_sum(i, slot, slice(0, cols.stop - cols.start), others)
            target[:, cols] = total.astype(BF16)

    def hop_back(self, step, later):
        if later:
            self.back(step - 1).wait_recv()
        self.put(self.bout.at[step], 2 * step, [self.bbox.at[step - 1]] if later else [])
        self.back(step).start()

    def hop_fore(self, step, later):
        if later:
            self.fore(step - 1).wait_recv()
        self.put(self.fout.at[step], 2 * step + 1, [self.fbox.at[step - 1]] if later else [])
        self.fore(step).start()

    def hop(self, step):
        self.locate()
        self.hop_back(step, step > 0)
        if step < self.behind:
            self.hop_fore(step, step > 0)

    def finish(self):
        self.locate()
        slot = self.chips - 1
        self.arrive(slot)
        self.fore(self.behind - 1).wait_recv()
        self.back(self.ahead - 1).wait_recv()
        others = [self.fbox.at[self.behind - 1], self.bbox.at[self.ahead - 1]]
        for i, first, last, out, form in self.pieces:
            total = self.local_sum(i, slot, slice(first, last), others)
            if form == "turned":
                self.outs[out][...] = total.T[: self.outs[out].shape[0]]
            elif form is None:
                self.outs[out][...] = total
            else:
                self.outs[out][:, form, :] = total
        for step in range(self.ahead):
            self.back(step).wait_send()
        for step in range(self.behind):
            self.fore(step).wait_send()
        for slot in range(self.chips):
            for i in range(len(self.windows)):
                self.across(i, slot).wait_send()


def run_rings(rings, after_first=None):
    ahead, behind = rings[0].ahead, rings[0].behind

    def turn(step, carry):
        def part(odd, kept):
            for ring in rings:
                ring.produce(2 * step + odd)
            return kept

        lax.fori_loop(0, 2, part, 0)

        @pl.when(step == 0)
        def _():
            for ring in rings:
                ring.hop_back(0, False)
                ring.hop_fore(0, False)
            if after_first is not None:
                after_first()

        @pl.when(step > 0)
        def _():
            for ring in rings:
                ring.hop_back(step, True)
                pl.when(step < behind)(functools.partial(ring.hop_fore, step, True))

        return carry

    lax.fori_loop(0, ahead, turn, 0)


def scatter_scratch(windows, rows, devices):
    chips = devices // 2
    count = len(windows)
    dma = pltpu.SemaphoreType.DMA
    widths = [last - first for left, right, first, last in windows]
    mine = [
        pltpu.VMEM((chips, rows if right is None else 2 * rows, last - first), BF16)
        for left, right, first, last in windows
    ]
    boxes = [pltpu.VMEM((chips, rows, width), BF16) for width in widths]
    box = pltpu.VMEM((chips // 2, rows, sum(widths)), BF16)
    return mine + boxes + [box] * 4 + [dma((count, chips))] * 3 + [dma((chips,))] * 4


class Total:
    def __init__(self, devices, x_ref, o_ref, scratch):
        self.chips = devices // 2
        self.x_ref, self.o_ref = x_ref, o_ref
        self.mate_box, self.joined, self.boxes, self.ms, self.mr, self.ss, self.sr = scratch
        me = lax.axis_index("dp")
        self.group = lax.axis_index("tensor")
        self.chip = lax.div(me, 2)
        core = lax.rem(me, 2)
        self.mate = self.chip * 2 + (1 - core)
        self.peers = [
            lax.rem(self.chip + shift, self.chips) * 2 + core for shift in range(self.chips)
        ]

    def greet(self):
        barrier = pltpu.get_barrier_semaphore()
        for other in [self.mate] + self.peers[1:]:
            pl.semaphore_signal(
                barrier, inc=1, device_id=(other, self.group), device_id_type=MESH
            )
        pl.semaphore_wait(barrier, self.chips)

    def remote(self, source, target_ref, ssem, rsem, target):
        return pltpu.make_async_remote_copy(
            src_ref=source,
            dst_ref=target_ref,
            send_sem=ssem,
            recv_sem=rsem,
            device_id=(target, self.group),
            device_id_type=MESH,
        )

    def across(self):
        return self.remote(self.x_ref, self.mate_box, self.ms, self.mr, self.mate)

    def copies(self):
        return [
            self.remote(
                self.joined,
                self.boxes.at[self.chip],
                self.ss.at[shift],
                self.sr.at[shift],
                self.peers[shift],
            )
            for shift in range(1, self.chips)
        ]

    def begin(self):
        self.across().start()

    def spread(self):
        self.across().wait_recv()
        self.joined[...] = self.x_ref[...] + self.mate_box[...]
        for copy in self.copies():
            copy.start()
        self.boxes[self.chip] = self.joined[...]

    def finish(self):
        for copy in self.copies():
            copy.wait_recv()
        result = self.boxes[0]
        for other in range(1, self.chips):
            result = result + self.boxes[other]
        self.o_ref[...] = result
        self.across().wait_send()
        for copy in self.copies():
            copy.wait_send()


def total_scratch(values, devices):
    chips = devices // 2
    dma = pltpu.SemaphoreType.DMA
    return [
        pltpu.VMEM(values.shape, F32),
        pltpu.VMEM(values.shape, F32),
        pltpu.VMEM((chips,) + values.shape, F32),
        dma(()),
        dma(()),
        dma((chips,)),
        dma((chips,)),
    ]


def product_kernel(devices, groups, outs, places, summed, left_ref, right_ref, *refs):
    values = refs[:summed]
    refs = refs[summed:]
    pieces_out, refs = refs[:outs], refs[outs:]
    total = None
    if summed:
        total_out, refs = refs[0], refs[1:]
    scratch = refs
    if summed:
        scratch, rest = scratch[:-8], scratch[-8:]
        together = rest[0]
        together[...] = jnp.zeros_like(together)
        for at, (which, row, lane) in enumerate(places):
            together[at : at + 1, :] = values[which][row : row + 1, lane : lane + LANES]
        total = Total(devices, together, total_out, rest[1:])
    each = len(scratch) // len(groups)
    rings = [
        RingScatter(
            devices, windows, pieces, (left_ref, right_ref), pieces_out,
            scratch[place * each : (place + 1) * each],
        )
        for place, (windows, pieces) in enumerate(groups)
    ]
    if total is None:
        rings[0].greet()
    else:
        total.greet()
        total.begin()
    for ring in rings:
        ring.locate()
    run_rings(rings, total.spread if total is not None else None)
    for ring in rings:
        ring.finish()
    if total is not None:
        total.finish()


def scatter_product(left, right, groups, shapes, devices, collective, values=(), places=()):
    vmem = pl.BlockSpec(memory_space=pltpu.VMEM)
    rows = left.shape[0] // devices
    scratch = []
    for windows, pieces in groups:
        scratch += scatter_scratch(windows, rows, devices)
    totals = ()
    if values:
        total = jax.ShapeDtypeStruct((len(places) + -len(places) % EDGE, LANES), F32)
        totals = (total,)
        scratch += [pltpu.VMEM(total.shape, F32)] + total_scratch(total, devices)
    return pl.pallas_call(
        functools.partial(
            product_kernel, devices, groups, len(shapes), places, len(values)
        ),
        out_shape=tuple(jax.ShapeDtypeStruct(shape, F32) for shape in shapes) + totals,
        in_specs=[vmem] * (2 + len(values)),
        out_specs=(vmem,) * (len(shapes) + len(totals)),
        scratch_shapes=scratch,
        compiler_params=pltpu.CompilerParams(collective_id=collective, has_side_effects=True),
        cost_estimate=cost(3),
        name="scatter_product",
    )(left, right, *values)


def head_spread(channels):
    return (iota((LANES, channels), 1) // MP == iota((LANES, channels), 0)).astype(BF16)


def parts(values, count):
    terms = []
    for _ in range(count):
        term = values.astype(BF16)
        terms.append(term)
        values = values - term.astype(F32)
    return terms


def pick(values, mask, count=2):
    return dot(jnp.concatenate(parts(values, count), axis=1), jnp.concatenate([mask] * count, axis=0))


def pick_left(mask, values, count):
    return dot(jnp.concatenate([mask] * count, axis=1), jnp.concatenate(parts(values, count), axis=0))


def gather_heads(values, spread):
    high, low = parts(values, 2)
    return dot(high, spread, NT) + dot(low, spread, NT)


def row_sums(values):
    high, low = parts(values, 2)
    ones = jnp.ones((EDGE, values.shape[1]), BF16)
    return dot(ones, high, NT) + dot(ones, low, NT)


def soft_step(raw):
    return jnp.maximum(raw, 0.0) + jnp.log1p(jnp.exp(-jnp.abs(raw)))


def window(buffer, start, span):
    return buffer[start : start + span, :]


def causal_taps(buffer, taps, span):
    total = taps[0:1, :] * window(buffer, EDGE - KCONV + 1, span)
    for tap in range(1, KCONV):
        total = total + taps[tap : tap + 1, :] * window(buffer, EDGE - KCONV + 1 + tap, span)
    return total


def span_rates(step_ref, bias, decay, spread, span):
    raw = step_ref[...] + bias
    step = soft_step(raw)
    lower = (iota((span, span), 1) <= iota((span, span), 0)).astype(BF16)
    cum = pick_left(lower, step * decay, 3)
    tails = jnp.exp(cum[span - 1 : span, :] - cum)
    wide = pick(jnp.concatenate([step, tails, jnp.exp(cum)], axis=0), spread)
    return raw, step, cum, wide[:span], wide[span : 2 * span], wide[2 * span :]


def pair_split(values, low_lanes):
    zero = jnp.zeros_like(values)
    return jnp.concatenate(
        [jnp.where(low_lanes, values, zero), jnp.where(low_lanes, zero, values)], axis=0
    )


def pair_decay(cum, cum_rows, pair, causal):
    parts = []
    for head in (2 * pair, 2 * pair + 1):
        differ = cum[:, head : head + 1] - cum_rows[head : head + 1, :]
        parts.append(jnp.exp(jnp.where(causal, differ, MASKED)))
    return parts


def scan_forward(
    devices, spans,
    z_ref, x_ref, bc_ref, step_ref,
    tap_ref, tapb_ref, row_ref, shard_ref,
    y_ref, gated_ref, square_ref, enter_ref, all_ref,
    state, buffer, *sems,
):
    span, channels = x_ref.shape
    ring = RingGather(devices, shard_ref, all_ref, sems)
    turn = pl.program_id(0)

    @pl.when(turn == 0)
    def _():
        ring.greet()
        ring.begin()


    @pl.when(pl.program_id(0) == 0)
    def _():
        state[...] = jnp.zeros_like(state)
        buffer[span:, :] = jnp.zeros((EDGE, buffer.shape[1]), F32)

    buffer[:EDGE, :] = buffer[span:, :]
    buffer[EDGE:, :channels] = x_ref[...]
    buffer[EDGE:, channels:] = bc_ref[...]
    spread = head_spread(channels)
    bias, gain, biasb, stepb, decay, skip = unpack_rows(row_ref, spread)
    taps = jnp.concatenate([tap_ref[...], tapb_ref[...]], axis=1).astype(F32)
    conv = causal_taps(buffer, taps, span)
    conv = jax.nn.silu(conv + jnp.concatenate([bias, biasb], axis=1))
    inputs, shared = conv[:, :channels], conv[:, channels:]
    raw, step, cum, step_w, tails_w, grown_w = span_rates(step_ref, stepb, decay, spread, span)
    cum_rows = cum.T
    b_low = shared[:, :NS].astype(BF16)
    c_low = shared[:, NS:].astype(BF16)
    scaled = inputs * step_w
    scaled_low = scaled.astype(BF16)
    enter_ref[0] = state[...]
    outer = dot(c_low, state[...].astype(BF16)) * grown_w
    fresh = dot(b_low, (scaled * tails_w).astype(BF16), TN)
    state[...] = state[...] * grown_w[span - 1 : span, :] + fresh
    cross = dot(c_low, b_low, NT)
    causal = iota((span, span), 1) <= iota((span, span), 0)
    low_lanes = iota((span, LANES), 1) < MP
    for pair in range(channels // LANES):
        lanes = slice(pair * LANES, (pair + 1) * LANES)
        first, second = pair_decay(cum, cum_rows, pair, causal)
        weights = jnp.concatenate(
            [(cross * first).astype(BF16), (cross * second).astype(BF16)], axis=1
        )
        y_ref[:, lanes] = dot(weights, pair_split(scaled_low[:, lanes], low_lanes))
    y = y_ref[...] + outer + skip * inputs
    y_ref[...] = y
    gated = y * jax.nn.silu(z_ref[...])
    gated_ref[...] = gated.astype(BF16)
    square_ref[...] = row_sums(gated * gated)

    count = spans
    for step in range(1, ring.ahead + 1):
        pl.when(turn == min(count - 1, count * step // ring.ahead))(
            functools.partial(ring.hop, step)
        )
    pl.when(turn == count - 1)(ring.finish)


def scan_backward(
    devices, spans, windows, pieces, outs_count, count,
    z_ref, x_ref, xp_ref, bc_ref, bp_ref, step_ref, y_ref, enter_ref,
    dyg_ref, scale_ref, inner_ref, dqkv_ref,
    tap_ref, tapb_ref, row_ref,
    *refs,
):
    sent, refs = refs[:count], refs[count:]
    (grad_ref, gx_ref, gh_ref), refs = refs[:3], refs[3:]
    outs, refs = refs[:outs_count], refs[outs_count:]
    (dstate, buffer, dbuffer, du_buf, col_buf), scratch = refs[:5], refs[5:]
    ring = RingScatter(devices, windows, pieces, sent, outs, scratch)
    span, channels = x_ref.shape
    turn = pl.program_id(0)

    @pl.when(turn == 0)
    def _():
        ring.greet()
        ring.begin()
        dstate[...] = jnp.zeros_like(dstate)
        dbuffer[...] = jnp.zeros_like(dbuffer)
        col_buf[...] = jnp.zeros_like(col_buf)
        gx_ref[...] = jnp.zeros_like(gx_ref)
        gh_ref[...] = jnp.zeros_like(gh_ref)

    inside = (turn < spans - 1).astype(F32)
    buffer[:EDGE, :channels] = xp_ref[...] * inside
    buffer[:EDGE, channels:] = bp_ref[...] * inside
    buffer[EDGE:, :channels] = x_ref[...]
    buffer[EDGE:, channels:] = bc_ref[...]
    spread = head_spread(channels)
    bias, gain, biasb, stepb, decay, skip = unpack_rows(row_ref, spread)
    taps = jnp.concatenate([tap_ref[...], tapb_ref[...]], axis=1).astype(F32)
    conv = causal_taps(buffer, taps, span) + jnp.concatenate([bias, biasb], axis=1)
    sig = jax.nn.sigmoid(conv)
    swished = conv * sig
    inputs, shared = swished[:, :channels], swished[:, channels:]
    b_low = shared[:, :NS].astype(BF16)
    c_low = shared[:, NS:].astype(BF16)
    raw, step, cum, step_w, tails_w, grown_w = span_rates(step_ref, stepb, decay, spread, span)
    cum_rows = cum.T
    scaled = inputs * step_w
    scaled_low = scaled.astype(BF16)

    z = z_ref[...]
    sig_z = jax.nn.sigmoid(z)
    swish = z * sig_z
    y = y_ref[...]
    scale = scale_ref[...].T[:, :1]
    normed = y * swish * scale
    dyg = dyg_ref[...]
    gain_grad = jnp.sum(dyg * normed, axis=0, keepdims=True)
    dgated = scale * (dyg * gain - normed * inner_ref[...].T[:, :1])
    dy = dgated * swish
    grad_ref[:, :channels] = (dgated * y * (sig_z * (1.0 + z * (1.0 - sig_z)))).astype(BF16)

    state_low = enter_ref[0].astype(BF16)
    dstate_low = dstate[...].astype(BF16)
    grown_low = (dy * grown_w).astype(BF16)
    dy_low = dy.astype(BF16)
    tailed = scaled * tails_w
    outer = dot(c_low, state_low) * grown_w
    from_state = dot(b_low, dstate_low)
    dc = dot(grown_low, state_low, NT)
    db = dot(tailed.astype(BF16), dstate_low, NT)
    leak = from_state * tailed
    last_w = grown_w[span - 1 : span, :]
    ends = (
        jnp.sum(leak, axis=0, keepdims=True)
        + jnp.sum(enter_ref[0] * dstate[...], axis=0, keepdims=True) * last_w
    )
    skips = jnp.sum(dy * inputs, axis=0, keepdims=True)
    dstate[...] = dstate[...] * last_w + dot(c_low, grown_low, TN)

    cross = dot(c_low, b_low, NT)
    causal = iota((span, span), 1) <= iota((span, span), 0)
    low_lanes = iota((span, LANES), 1) < MP
    lane = iota((span, LANES), 1)
    dcross = jnp.zeros((span, span), F32)
    row_part = jnp.zeros((span, LANES), F32)
    for pair in range(channels // LANES):
        lanes = slice(pair * LANES, (pair + 1) * LANES)
        decays = pair_decay(cum, cum_rows, pair, causal)
        dy_pair = pair_split(dy_low[:, lanes], low_lanes)
        dweights = dot(dy_pair, scaled_low[:, lanes], NT)
        both = []
        for part in range(2):
            head = 2 * pair + part
            dterm = dweights[part * span : (part + 1) * span] * decays[part]
            dcross = dcross + dterm
            flow = dterm * cross
            row_part = row_part + jnp.where(
                lane == head, jnp.sum(flow, axis=1, keepdims=True), 0.0
            )
            col_buf[head : head + 1, :] = jnp.sum(flow, axis=0, keepdims=True)
            both.append((cross * decays[part]).astype(BF16))
        du_buf[:, lanes] = dot(jnp.concatenate(both, axis=0), dy_pair, TN)
    du = du_buf[...] + from_state * tails_w
    dcross_low = dcross.astype(BF16)
    dc = dc + dot(dcross_low, b_low)
    db = db + dot(dcross_low, c_low, TN)

    sums = gather_heads(
        jnp.concatenate(
            [dy * outer - leak, du * inputs, ends, skips, jnp.zeros((EDGE - 2, channels), F32)],
            axis=0,
        ),
        spread,
    )
    at_end = sums[2 * span : 2 * span + 1, :]
    dcum = sums[:span] + row_part - col_buf[...].T
    upper = (iota((span, span), 1) >= iota((span, span), 0)).astype(BF16)
    drate = pick_left(upper, dcum, 3) + at_end
    dstep = drate * decay + sums[span : 2 * span]
    draw = dstep * jax.nn.sigmoid(raw)
    gh_ref[0:1, :] += jnp.sum(draw, axis=0, keepdims=True)
    gh_ref[1:2, :] += jnp.sum(drate * step, axis=0, keepdims=True) * decay
    gh_ref[2:3, :] += sums[2 * span + 1 : 2 * span + 2, :]

    dinputs = du * step_w + skip * dy
    dconv = jnp.concatenate([dinputs, db, dc], axis=1) * (sig * (1.0 + conv * (1.0 - sig)))
    dbuffer[span:, :] = dbuffer[:EDGE, :]
    dbuffer[:span, :] = dconv
    dbefore = jnp.zeros_like(dconv)
    for tap in range(KCONV):
        dbefore = dbefore + taps[tap : tap + 1, :] * window(dbuffer, KCONV - 1 - tap, span)
        gx_ref[tap : tap + 1, :] += jnp.sum(
            dconv * window(buffer, EDGE - KCONV + 1 + tap, span), axis=0, keepdims=True
        )
    gx_ref[KCONV : KCONV + 1, :] += jnp.sum(dconv, axis=0, keepdims=True)
    gx_ref[KCONV + 1 : KCONV + 2, :channels] += gain_grad
    width = 2 * channels + 2 * NS
    grad_ref[:, channels:width] = dbefore.astype(BF16)
    grad_ref[:, width : width + dqkv_ref.shape[1]] = dqkv_ref[...]
    grad_ref[:, width + dqkv_ref.shape[1] :] = draw.astype(BF16)
    for step in range(ring.ahead):
        pl.when(turn == spans * step // ring.ahead)(functools.partial(ring.hop, step))
    pl.when(turn == spans - 1)(ring.finish)


def scan_params(conv_x, conv_xb, conv_bc, conv_bcb, dt_bias, a_log, d_skip, w_mnorm):
    heads = dt_bias.shape[0]
    fill = jnp.zeros((LANES - heads,), BF16)
    flat = [conv_xb, w_mnorm, conv_bcb, dt_bias, fill, a_log, fill, d_skip, fill]
    size = sum(item.shape[0] for item in flat) // LANES
    flat.append(jnp.zeros((-size % EDGE * LANES,), BF16))
    rows = jnp.concatenate(flat).astype(F32).reshape(-1, LANES)
    return (conv_x, conv_bc, rows)


def unpack_rows(row_ref, spread):
    channels = spread.shape[1]
    count = channels // LANES
    at = 2 * count + 2 * NS // LANES

    def join_rows(first, number):
        return jnp.concatenate(
            [row_ref[i : i + 1, :] for i in range(first, first + number)], axis=1
        )

    skip = jnp.broadcast_to(row_ref[at + 2 : at + 3, :], (EDGE, LANES)).astype(BF16)
    return (
        join_rows(0, count),
        join_rows(count, count),
        join_rows(2 * count, 2 * NS // LANES),
        row_ref[at : at + 1, :],
        -jnp.exp(row_ref[at + 1 : at + 2, :]),
        dot(skip, spread)[:1],
    )


def whole_spec(array):
    return pl.BlockSpec(array.shape, lambda turn: (0,) * array.ndim)


def run_scan_forward(proj, qkv_width, params, shard, devices):
    tokens = proj.shape[0]
    channels = params[0].shape[1]
    step_at = (2 * channels + 2 * NS + qkv_width) // LANES
    spans = tokens // SPAN
    bc_at = 2 * channels // (2 * NS)
    rows = lambda width, at: pl.BlockSpec((SPAN, width), lambda turn: (turn, at))
    anywhere = pl.BlockSpec(memory_space=pl.ANY)
    return pl.pallas_call(
        functools.partial(scan_forward, devices, spans),
        grid=(spans,),
        out_shape=(
            jax.ShapeDtypeStruct((tokens, channels), F32),
            jax.ShapeDtypeStruct((tokens, channels), BF16),
            jax.ShapeDtypeStruct((EDGE, tokens), F32),
            jax.ShapeDtypeStruct((spans, NS, channels), F32),
            gather_shape(shard, devices),
        ),
        in_specs=[rows(channels, 0), rows(channels, 1), rows(2 * NS, bc_at), rows(LANES, step_at)]
        + [whole_spec(item) for item in params]
        + [anywhere],
        out_specs=(
            rows(channels, 0),
            rows(channels, 0),
            pl.BlockSpec((EDGE, SPAN), lambda turn: (0, turn)),
            pl.BlockSpec((1, NS, channels), lambda turn: (turn, 0, 0)),
            anywhere,
        ),
        scratch_shapes=[
            pltpu.VMEM((NS, channels), F32),
            pltpu.VMEM((SPAN + EDGE, channels + 2 * NS), F32),
        ]
        + gather_sems(devices),
        compiler_params=pltpu.CompilerParams(collective_id=2, has_side_effects=True),
        cost_estimate=cost(20),
        name="scan_forward",
    )(proj, proj, proj, proj, *params, shard)


def run_scan_backward(
    proj, y, entering, dyg, scale, inner, dqkv, params, sent, windows, pieces, shapes,
    devices,
):
    tokens, width = proj.shape
    channels = params[0].shape[1]
    qkv_width = dqkv.shape[1]
    step_at = (2 * channels + 2 * NS + qkv_width) // LANES
    spans = tokens // SPAN
    bc_at = 2 * channels // (2 * NS)
    edges = SPAN // EDGE
    rows = lambda size, at: pl.BlockSpec((SPAN, size), lambda turn: (spans - 1 - turn, at))
    edge = lambda size, at: pl.BlockSpec(
        (EDGE, size), lambda turn: (jnp.maximum((spans - 1 - turn) * edges - 1, 0), at)
    )
    keep = lambda shape: pl.BlockSpec(shape, lambda turn: (0, 0))
    shapes = tuple(jax.ShapeDtypeStruct(shape, F32) for shape in shapes)
    return pl.pallas_call(
        functools.partial(
            scan_backward, devices, spans, windows, pieces, len(shapes), len(sent)
        ),
        grid=(spans,),
        out_shape=(
            jax.ShapeDtypeStruct((tokens, width), BF16),
            jax.ShapeDtypeStruct((EDGE, channels + 2 * NS), F32),
            jax.ShapeDtypeStruct((EDGE, LANES), F32),
        )
        + shapes,
        in_specs=[
            rows(channels, 0),
            rows(channels, 1),
            edge(channels, 1),
            rows(2 * NS, bc_at),
            edge(2 * NS, bc_at),
            rows(LANES, step_at),
            rows(channels, 0),
            pl.BlockSpec((1, NS, channels), lambda turn: (spans - 1 - turn, 0, 0)),
            rows(channels, 0),
            pl.BlockSpec((EDGE, SPAN), lambda turn: (0, spans - 1 - turn)),
            pl.BlockSpec((EDGE, SPAN), lambda turn: (0, spans - 1 - turn)),
            rows(qkv_width, 0),
        ]
        + [whole_spec(item) for item in params]
        + [pl.BlockSpec(memory_space=pl.ANY)] * len(sent),
        out_specs=(
            rows(width, 0),
            keep((EDGE, channels + 2 * NS)),
            keep((EDGE, LANES)),
        )
        + tuple(keep(item.shape) for item in shapes),
        scratch_shapes=[
            pltpu.VMEM((NS, channels), F32),
            pltpu.VMEM((SPAN + EDGE, channels + 2 * NS), F32),
            pltpu.VMEM((SPAN + EDGE, channels + 2 * NS), F32),
            pltpu.VMEM((SPAN, channels), F32),
            pltpu.VMEM((LANES, SPAN), F32),
        ]
        + scatter_scratch(windows, sent[0].shape[0] // devices, devices),
        compiler_params=pltpu.CompilerParams(collective_id=6, has_side_effects=True),
        cost_estimate=cost(47),
        name="scan_backward",
    )(
        proj, proj, proj, proj, proj, proj, y, entering, dyg, scale, inner, dqkv, *params, *sent,
    )


def rotary_tables(tokens):
    half = HEAD_SIZE // 2
    exponent = np.arange(half, dtype=np.float64) * (-2.0 * LOG_BASE / HEAD_SIZE)
    rates = np.tile(np.exp(exponent.astype(np.float32)).astype(np.float64), LANES // half)
    tables = []
    for places in (np.arange(FINE), np.arange(0, tokens, FINE)):
        angles = places[:, None] * rates[None, :]
        tables += [np.cos(angles).astype(np.float32), np.sin(angles).astype(np.float32)]
    return tables


def fill_rotary(fine_cos, fine_sin, coarse_cos, coarse_sin, cosine, sine):
    small_cos, small_sin = fine_cos[...], fine_sin[...]
    for turn in range(coarse_cos.shape[0]):
        big_cos, big_sin = coarse_cos[turn : turn + 1, :], coarse_sin[turn : turn + 1, :]
        rows = slice(turn * FINE, (turn + 1) * FINE)
        cosine[rows, :] = small_cos * big_cos - small_sin * big_sin
        sine[rows, :] = small_sin * big_cos + small_cos * big_sin


def head_masks():
    half = HEAD_SIZE // 2
    row, col = iota((LANES, LANES), 0), iota((LANES, LANES), 1)
    place = col % HEAD_SIZE
    ahead = jnp.where(place < half, -1.0, 0.0)
    behind = jnp.where(place < half, 0.0, 1.0)

    def turn(start):
        return jnp.where(row == start + half, ahead, jnp.where(row == start - half, behind, 0.0))

    first = row < HEAD_SIZE
    left = col < HEAD_SIZE
    low = lambda mask: mask.astype(BF16)
    within = low(turn(col))
    copy = low(jnp.where(row == place, 1.0, 0.0))
    copy_turn = low(jnp.where(first, turn(place), 0.0))
    value = low(jnp.where(row == place + HEAD_SIZE, 1.0, 0.0))
    fold = low(jnp.where(left & (row % HEAD_SIZE == place), 1.0, 0.0))
    other = row % HEAD_SIZE
    fold_turn = low(
        jnp.where(
            left,
            jnp.where(other == place + half, ahead, jnp.where(other == place - half, behind, 0.0)),
            0.0,
        )
    )
    fold_value = low(jnp.where(left, 0.0, jnp.where(other == place, 1.0, 0.0)))
    return within, copy, copy_turn, value, fold, fold_turn, fold_value


def attend_forward(
    q_ref, kv_ref, fine_cos, fine_sin, coarse_cos, coarse_sin,
    qkv_ref, lse_ref, o_ref, vt, cos_ref, sin_ref,
):
    fill_rotary(fine_cos, fine_sin, coarse_cos, coarse_sin, cos_ref, sin_ref)
    tokens, query_width = q_ref.shape
    pairs = query_width // LANES
    within, copy, copy_turn, value = head_masks()[:4]

    def turn_rows(i, carry):
        rows = pl.ds(pl.multiple_of(i * QBLK, QBLK), QBLK)
        cosine, sine = cos_ref[rows, :], sin_ref[rows, :]
        for pair in range(pairs):
            lanes = slice(pair * LANES, (pair + 1) * LANES)
            query = q_ref[rows, lanes]
            turned = query * cosine + pick(query, within) * sine
            qkv_ref[rows, lanes] = (turned * HEAD_SIZE**-0.5).astype(BF16)
        kv = kv_ref[rows, :]
        keys = pick(kv, copy) * cosine + pick(kv, copy_turn) * sine
        qkv_ref[rows, query_width : query_width + LANES] = keys.astype(BF16)
        qkv_ref[rows, query_width + LANES :] = dot(kv.astype(BF16), value).astype(BF16)
        vt[:, rows] = kv.T[HEAD_SIZE:, :].astype(BF16)
        return carry

    lax.fori_loop(0, tokens // QBLK, turn_rows, 0)
    low_lanes = iota((QBLK, LANES), 1) < HEAD_SIZE
    wide = (QBLK, 2 * QBLK)
    visible = iota(wide, 0) <= iota(wide, 1) % QBLK

    def block(i, carry):
        here = pl.ds(pl.multiple_of(i * QBLK, QBLK), QBLK)
        queries = [
            pair_split(qkv_ref[here, pair * LANES : (pair + 1) * LANES], low_lanes)
            for pair in range(pairs)
        ]

        def tile(there, state, edge):
            keys = qkv_ref[there, query_width : query_width + LANES]
            result = []
            for pair in range(pairs):
                top, total, out = state[3 * pair : 3 * pair + 3]
                scores = dot(keys, queries[pair], NT)
                if edge:
                    scores = jnp.where(visible, scores, MASKED)
                higher = jnp.maximum(top, jnp.max(scores, axis=0, keepdims=True))
                probs = jnp.exp(scores - higher)
                fade = jnp.exp(top - higher)
                total = total * fade + jnp.sum(probs, axis=0, keepdims=True)
                out = out * fade + dot(vt[:, there], probs.astype(BF16))
                result += [higher, total, out]
            return tuple(result)

        state = (
            jnp.full((1, 2 * QBLK), MASKED, F32),
            jnp.zeros((1, 2 * QBLK), F32),
            jnp.zeros((HEAD_SIZE, 2 * QBLK), F32),
        ) * pairs
        state = lax.fori_loop(
            0,
            i,
            lambda j, state: tile(pl.ds(pl.multiple_of(j * QBLK, QBLK), QBLK), state, False),
            state,
        )
        state = tile(here, state, True)
        for pair in range(pairs):
            top, total, out = state[3 * pair : 3 * pair + 3]
            out = out / total
            lse = top + jnp.log(total)
            lse_ref[2 * pair : 2 * pair + 1, here] = lse[:, :QBLK]
            lse_ref[2 * pair + 1 : 2 * pair + 2, here] = lse[:, QBLK:]
            both = jnp.concatenate([out[:, :QBLK], out[:, QBLK:]], axis=0)
            o_ref[here, pair * LANES : (pair + 1) * LANES] = both.T.astype(BF16)
        return carry

    lax.fori_loop(0, tokens // QBLK, block, 0)


def attend_backward(
    qkv_ref, lse_ref, o_ref, do_ref, fine_cos, fine_sin, coarse_cos, coarse_sin,
    dqkv_ref,
    dq, kt, dk, dv, cos_ref, sin_ref,
):
    fill_rotary(fine_cos, fine_sin, coarse_cos, coarse_sin, cos_ref, sin_ref)
    tokens, query_width = o_ref.shape
    pairs = query_width // LANES
    key_lanes = slice(query_width, query_width + LANES)
    value_lanes = slice(query_width + LANES, query_width + 2 * LANES)

    def turn_keys(i, carry):
        rows = pl.ds(pl.multiple_of(i * QBLK, QBLK), QBLK)
        kt[:, rows] = qkv_ref[rows, key_lanes].astype(F32).T[:HEAD_SIZE, :].astype(BF16)
        return carry

    lax.fori_loop(0, tokens // QBLK, turn_keys, 0)
    dk[...] = jnp.zeros_like(dk)
    dv[...] = jnp.zeros_like(dv)
    low_lanes = iota((QBLK, LANES), 1) < HEAD_SIZE
    wide = (QBLK, 2 * QBLK)
    visible = iota(wide, 0) <= iota(wide, 1) % QBLK
    ones = jnp.ones((EDGE, LANES), BF16)

    def block(i, carry):
        here = pl.ds(pl.multiple_of(i * QBLK, QBLK), QBLK)
        queries, grads, inners, lses = [], [], [], []
        for pair in range(pairs):
            lanes = slice(pair * LANES, (pair + 1) * LANES)
            queries.append(pair_split(qkv_ref[here, lanes], low_lanes))
            grad = do_ref[here, lanes]
            grads.append(pair_split(grad, low_lanes))
            both = pair_split(grad.astype(F32) * o_ref[here, lanes].astype(F32), low_lanes)
            high, low = parts(both, 2)
            inners.append((dot(ones, high, NT) + dot(ones, low, NT))[:1])
            lses.append(
                jnp.concatenate(
                    [
                        lse_ref[2 * pair : 2 * pair + 1, here],
                        lse_ref[2 * pair + 1 : 2 * pair + 2, here],
                    ],
                    axis=1,
                )
            )
        query_all = jnp.concatenate(queries, axis=0)
        grad_all = jnp.concatenate(grads, axis=0)

        def tile(there, state, edge):
            keys = qkv_ref[there, key_lanes]
            values = qkv_ref[there, value_lanes]
            all_probs, all_dscores, result = [], [], []
            for pair in range(pairs):
                probs = dot(keys, queries[pair], NT) - lses[pair]
                if edge:
                    probs = jnp.where(visible, probs, MASKED)
                probs = jnp.exp(probs)
                dprobs = dot(values, grads[pair], NT)
                dscores = (probs * (dprobs - inners[pair])).astype(BF16)
                all_probs.append(probs.astype(BF16))
                all_dscores.append(dscores)
                result.append(state[pair] + dot(kt[:, there], dscores))
            dv[there, :] += dot(jnp.concatenate(all_probs, axis=1), grad_all)
            dk[there, :] += dot(jnp.concatenate(all_dscores, axis=1), query_all)
            return tuple(result)

        state = (jnp.zeros((HEAD_SIZE, 2 * QBLK), F32),) * pairs
        state = lax.fori_loop(
            0,
            i,
            lambda j, state: tile(pl.ds(pl.multiple_of(j * QBLK, QBLK), QBLK), state, False),
            state,
        )
        state = tile(here, state, True)
        for pair in range(pairs):
            both = jnp.concatenate([state[pair][:, :QBLK], state[pair][:, QBLK:]], axis=0)
            dq[here, pair * LANES : (pair + 1) * LANES] = both.T
        return carry

    lax.fori_loop(0, tokens // QBLK, block, 0)
    masks = head_masks()
    within, (fold, fold_turn, fold_value) = masks[0], masks[4:]

    def turn_back(i, carry):
        rows = pl.ds(pl.multiple_of(i * QBLK, QBLK), QBLK)
        cosine, sine = cos_ref[rows, :], sin_ref[rows, :]
        for pair in range(pairs):
            lanes = slice(pair * LANES, (pair + 1) * LANES)
            grad = dq[rows, lanes]
            grad = grad * cosine - pick(grad, within) * sine
            dqkv_ref[rows, lanes] = (grad * HEAD_SIZE**-0.5).astype(BF16)
        grad = dk[rows, :]
        grad = pick(grad, fold) * cosine - pick(grad, fold_turn) * sine
        grad = grad + pick(dv[rows, :], fold_value)
        dqkv_ref[rows, query_width:] = grad.astype(BF16)
        return carry

    lax.fori_loop(0, tokens // QBLK, turn_back, 0)


def run_attend_forward(proj, query_at, query_width, tables):
    tokens = proj.shape[0]
    cols = lambda size, at: pl.BlockSpec((tokens, size), lambda turn: (0, at // size))
    return pl.pallas_call(
        attend_forward,
        grid=(1,),
        out_shape=(
            jax.ShapeDtypeStruct((tokens, query_width + 2 * LANES), BF16),
            jax.ShapeDtypeStruct((EDGE, tokens), F32),
            jax.ShapeDtypeStruct((tokens, query_width), BF16),
        ),
        in_specs=[
            cols(query_width, query_at),
            cols(2 * HEAD_SIZE, query_at + query_width),
        ]
        + [whole_spec(table) for table in tables],
        out_specs=(
            cols(query_width + 2 * LANES, 0),
            pl.BlockSpec((EDGE, tokens), lambda turn: (0, 0)),
            cols(query_width, 0),
        ),
        scratch_shapes=[
            pltpu.VMEM((HEAD_SIZE, tokens), BF16),
            pltpu.VMEM((tokens, LANES), F32),
            pltpu.VMEM((tokens, LANES), F32),
        ],
        cost_estimate=cost(15),
        name="attend_forward",
    )(proj, proj, *tables)


def run_attend_backward(qkv, lse, attended, grads, grad_at, tables):
    tokens, query_width = attended.shape
    vmem = pl.BlockSpec(memory_space=pltpu.VMEM)
    cols = lambda size, at: pl.BlockSpec((tokens, size), lambda turn: (0, at // size))
    return pl.pallas_call(
        attend_backward,
        grid=(1,),
        out_shape=jax.ShapeDtypeStruct((tokens, query_width + 2 * HEAD_SIZE), BF16),
        in_specs=[
            whole_spec(qkv),
            whole_spec(lse),
            whole_spec(attended),
            cols(query_width, grad_at),
        ]
        + [whole_spec(table) for table in tables],
        out_specs=cols(query_width + 2 * HEAD_SIZE, 0),
        scratch_shapes=[
            pltpu.VMEM((tokens, query_width), F32),
            pltpu.VMEM((HEAD_SIZE, tokens), BF16),
            pltpu.VMEM((tokens, LANES), F32),
            pltpu.VMEM((tokens, LANES), F32),
            pltpu.VMEM((tokens, LANES), F32),
            pltpu.VMEM((tokens, LANES), F32),
        ],
        cost_estimate=cost(16),
        name="attend_backward",
    )(qkv, lse, attended, grads, *tables)


def feed_forward(
    x_ref, mixed_ref, other_ref, act_grad_ref, norms_ref, gu_ref,
    after_ref, scale_ref, turned_ref, act_ref, dgu_ref, back_ref,
):
    units = act_grad_ref.shape[1]
    after = x_ref[...].astype(F32) + (mixed_ref[...].astype(F32) + other_ref[...].astype(F32))
    after_ref[...] = after.astype(BF16)
    scale = lax.rsqrt(jnp.mean(after * after, axis=-1, keepdims=True) + EPSILON)
    scale_ref[...] = scale
    hidden = (after * scale * norms_ref[1:2, :]).astype(BF16)
    turned_ref[...] = hidden.T
    for start in range(0, units, UBLK):
        cols = slice(start, start + UBLK)
        up_cols = slice(units + start, units + start + UBLK)
        gate = dot(hidden, gu_ref[:, cols])
        upward = dot(hidden, gu_ref[:, up_cols])
        grad = act_grad_ref[:, cols]
        sigma = jax.nn.sigmoid(gate)
        swish = gate * sigma
        act_ref[:, cols] = (swish * upward).astype(BF16)
        slope = sigma * (1.0 + gate * (1.0 - sigma))
        dgu_ref[:, cols] = (grad * upward * slope).astype(BF16)
        dgu_ref[:, up_cols] = (grad * swish).astype(BF16)
    back_ref[...] = dot(dgu_ref[...], gu_ref[...], NT).astype(BF16)


def product_rows(dims, left_ref, right_ref, out_ref):
    out_ref[...] = dot(left_ref[...], right_ref[...], dims).astype(out_ref.dtype)


def run_product(left, right, dims, dtype):
    tokens, depth = left.shape
    cols = right.shape[1 - dims[1][0]]
    return pl.pallas_call(
        functools.partial(product_rows, dims),
        grid=(tokens // TBLK,),
        out_shape=jax.ShapeDtypeStruct((tokens, cols), dtype),
        in_specs=[pl.BlockSpec((TBLK, depth), lambda turn: (turn, 0)), once(right)],
        out_specs=pl.BlockSpec((TBLK, cols), lambda turn: (turn, 0)),
        cost_estimate=cost(4),
        name="product_rows",
    )(left, right)


def project(heads, x_ref, w_ref, turned_ref, proj_ref, norms_ref):
    @pl.when(pl.program_id(0) == 0)
    def _():
        gains = w_ref[:, w_ref.shape[1] - LANES :].astype(F32).T
        norms_ref[...] = jnp.zeros_like(norms_ref)
        norms_ref[0:2, :] = gains[heads : heads + 2, :]

    x = x_ref[...].astype(F32)
    scale = lax.rsqrt(jnp.mean(x * x, axis=-1, keepdims=True) + EPSILON)
    hidden = (x * scale * norms_ref[0:1, :]).astype(BF16)
    turned_ref[...] = hidden.T
    proj_ref[...] = dot(hidden, w_ref[...])


def run_project(x, w_in, heads):
    tokens, width = x.shape
    cols = w_in.shape[1]
    rows = lambda size: pl.BlockSpec((TBLK, size), lambda turn: (turn, 0))
    return pl.pallas_call(
        functools.partial(project, heads),
        grid=(tokens // TBLK,),
        out_shape=(
            jax.ShapeDtypeStruct((width, tokens), BF16),
            jax.ShapeDtypeStruct((tokens, cols), F32),
            jax.ShapeDtypeStruct((EDGE, width), F32),
        ),
        in_specs=[rows(width), once(w_in)],
        out_specs=(
            pl.BlockSpec((width, TBLK), lambda turn: (0, turn)),
            rows(cols),
            pl.BlockSpec((EDGE, width), lambda turn: (0, 0)),
        ),
        cost_estimate=cost(8),
        name="project",
    )(x, w_in)


def project_back(grad_ref, w_ref, x_ref, part_ref, gain_grad_ref):
    @pl.when(pl.program_id(0) == 0)
    def _():
        gain_grad_ref[...] = jnp.zeros_like(gain_grad_ref)

    x = x_ref[...].astype(F32)
    normed = x * lax.rsqrt(jnp.mean(x * x, axis=-1, keepdims=True) + EPSILON)
    part = dot(grad_ref[...], w_ref[...], NT).astype(BF16)
    part_ref[...] = part
    gain_grad_ref[:1, :] += jnp.sum(part.astype(F32) * normed, axis=0, keepdims=True)


def run_project_back(grads, w_in, x):
    tokens, width = x.shape
    cols = w_in.shape[1]
    rows = lambda size: pl.BlockSpec((TBLK, size), lambda turn: (turn, 0))
    return pl.pallas_call(
        project_back,
        grid=(tokens // TBLK,),
        out_shape=(
            jax.ShapeDtypeStruct((tokens, width), BF16),
            jax.ShapeDtypeStruct((EDGE, width), F32),
        ),
        in_specs=[rows(cols), once(w_in), rows(width)],
        out_specs=(rows(width), pl.BlockSpec((EDGE, width), lambda turn: (0, 0))),
        cost_estimate=cost(8),
        name="project_back",
    )(grads, w_in, x)


def once(item):
    return pl.BlockSpec(item.shape, lambda turn: (0,) * item.ndim, pipeline_mode=pl.Buffered(1))


def run_feed_forward(x, mixed, other, act_grad, norms, w_gate_up):
    tokens, width = x.shape
    units = act_grad.shape[1]
    rows = lambda size: pl.BlockSpec((TBLK, size), lambda turn: (turn, 0))
    shape = jax.ShapeDtypeStruct
    return pl.pallas_call(
        feed_forward,
        grid=(tokens // TBLK,),
        out_shape=(
            shape((tokens, width), BF16),
            shape((tokens, 1), F32),
            shape((width, tokens), BF16),
            shape((tokens, units), BF16),
            shape((tokens, 2 * units), BF16),
            shape((tokens, width), BF16),
        ),
        in_specs=[rows(width)] * 3 + [rows(units), once(norms), once(w_gate_up)],
        out_specs=(
            rows(width), rows(1), pl.BlockSpec((width, TBLK), lambda turn: (0, turn)), rows(units),
            rows(2 * units), rows(width),
        ),
        cost_estimate=cost(14),
        name="feed_forward",
    )(x, mixed, other, act_grad, norms, w_gate_up)


def mixer_forward(gated_ref, scale_ref, gain_ref, attended_ref, w_ref, low_ref, mixed_ref):
    channels = gated_ref.shape[1]
    scale = scale_ref[...].T[:, :1]
    low_ref[:, :channels] = (gated_ref[...].astype(F32) * scale * gain_ref[...]).astype(BF16)
    low_ref[:, channels:] = attended_ref[...]
    mixed_ref[...] = dot(low_ref[...], w_ref[...], NT).astype(BF16)


def run_mixer_forward(gated, scale, gain, attended, w_out):
    tokens, channels = gated.shape
    width, inner = w_out.shape
    rows = lambda size: pl.BlockSpec((TBLK, size), lambda turn: (turn, 0))
    return pl.pallas_call(
        mixer_forward,
        grid=(tokens // TBLK,),
        out_shape=(
            jax.ShapeDtypeStruct((tokens, inner), BF16),
            jax.ShapeDtypeStruct((tokens, width), BF16),
        ),
        in_specs=[
            rows(channels),
            pl.BlockSpec((EDGE, TBLK), lambda turn: (0, turn)),
            once(gain),
            rows(attended.shape[1]),
            once(w_out),
        ],
        out_specs=(rows(inner), rows(width)),
        cost_estimate=cost(5),
        name="mixer_forward",
    )(gated, scale, gain, attended, w_out)


def mixer_backward(
    part_ref, other_ref, after_ref, scale_ref, top_ref, norms_ref,
    w_ref, gated_ref, scale_m_ref, gain_m_ref,
    low_ref, turned_ref, mamba_ref, attended_ref, inner_ref, gain_grad_ref,
):
    channels = gated_ref.shape[1]

    @pl.when(pl.program_id(0) == 0)
    def _():
        gain_grad_ref[...] = jnp.zeros_like(gain_grad_ref)

    grad = part_ref[...].astype(F32) + other_ref[...].astype(F32)
    scale = scale_ref[...]
    normed = after_ref[...].astype(F32) * scale
    gain_grad_ref[:1, :] += jnp.sum(grad * normed, axis=0, keepdims=True)
    weighted = grad * norms_ref[1:2, :]
    mean = jnp.mean(weighted * normed, axis=-1, keepdims=True)
    total = top_ref[...].astype(F32) + scale * (weighted - normed * mean)
    low = total.astype(BF16)
    low_ref[...] = low
    turned_ref[...] = low.T
    back = dot(low, w_ref[...])
    mamba = back[:, :channels]
    mamba_ref[...] = mamba
    attended_ref[...] = back[:, channels:].astype(BF16)
    inner_ref[...] = row_sums(mamba * gain_m_ref[...] * gated_ref[...].astype(F32)) * scale_m_ref[...]


def run_mixer_backward(part, other, after, scale, top, norms, w_out, gated, scale_m, gain_m):
    tokens, width = after.shape
    channels = gated.shape[1]
    inner = w_out.shape[1]
    shape = jax.ShapeDtypeStruct
    rows = lambda size: pl.BlockSpec((NBLK, size), lambda turn: (turn, 0))
    lanes = pl.BlockSpec((EDGE, NBLK), lambda turn: (0, turn))
    return pl.pallas_call(
        mixer_backward,
        grid=(tokens // NBLK,),
        out_shape=(
            shape((tokens, width), BF16),
            shape((width, tokens), BF16),
            shape((tokens, channels), F32),
            shape((tokens, inner - channels), BF16),
            shape((EDGE, tokens), F32),
            shape((EDGE, width), F32),
        ),
        in_specs=[rows(width)] * 3
        + [rows(1), rows(width), once(norms), once(w_out), rows(channels), lanes, once(gain_m)],
        out_specs=(
            rows(width), pl.BlockSpec((width, NBLK), lambda turn: (0, turn)), rows(channels),
            rows(inner - channels), lanes,
            pl.BlockSpec((EDGE, width), lambda turn: (0, 0)),
        ),
        cost_estimate=cost(8),
        name="mixer_backward",
    )(part, other, after, scale, top, norms, w_out, gated, scale_m, gain_m)


def lane_row(ref, first, count):
    return jnp.concatenate([ref[i : i + 1, :] for i in range(first, first + count)], axis=1)


def own_lanes(ref, first, size):
    start = lax.axis_index("dp") * size
    row = ref[pl.ds(first + lax.div(start, LANES), 1), :]
    row = jnp.broadcast_to(row, (EDGE, LANES))
    return pltpu.roll(row, lax.rem(LANES - lax.rem(start, LANES), LANES), 1)[0, :size]


def finish_layer(
    norm_at, x_ref, norms_ref, part_ref, other_ref, grad_ref, after_ref, ffn_ref, ffn_other_ref,
    total_ref, *refs,
):
    count = (len(refs) - 9) // 2
    passed, out_ref, result_ref, handed = refs[:count], refs[count], refs[count + 1], refs[count + 2 :]
    tap_ref, bias_ref, gain_ref, step_ref, log_ref, skip_ref, norm_ref = handed[count:]

    @pl.when(pl.program_id(0) == 0)
    def _():
        for source, target in zip(passed, handed):
            target[...] = source[...]
        rows = tap_ref.shape[1] // LANES
        for tap in range(KCONV):
            tap_ref[tap : tap + 1, :] = lane_row(total_ref, tap * rows, rows)
        bias_ref[...] = lane_row(total_ref, KCONV * rows, rows)[0]
        gain_ref[...] = lane_row(total_ref, (KCONV + 1) * rows, rows)[0]
        at = (KCONV + 2) * rows
        for place, ref in enumerate((step_ref, log_ref, skip_ref)):
            ref[...] = total_ref[at + place : at + place + 1, :][0, : ref.shape[0]]
        norm_ref[...] = own_lanes(total_ref, norm_at, norm_ref.shape[0])

    x = x_ref[...].astype(F32)
    scale = lax.rsqrt(jnp.mean(x * x, axis=-1, keepdims=True) + EPSILON)
    normed = x * scale
    weighted = (part_ref[...].astype(F32) + other_ref[...].astype(F32)) * norms_ref[0:1, :]
    mean = jnp.mean(weighted * normed, axis=-1, keepdims=True)
    out_ref[...] = grad_ref[...].astype(F32) + scale * (weighted - normed * mean)
    ffn = ffn_ref[...].astype(F32) + ffn_other_ref[...].astype(F32)
    result_ref[...] = (after_ref[...].astype(F32) + ffn).astype(BF16)


def run_finish(
    x, norms, part, other, grad, after, ffn, ffn_other, total, passed, channels, heads, shard,
    norm_at,
):
    tokens, width = x.shape
    rows = pl.BlockSpec((TBLK, width), lambda turn: (turn, 0))
    shape = lambda *sizes: jax.ShapeDtypeStruct(sizes, F32)
    small = (
        shape(KCONV, channels), shape(channels), shape(channels), shape(heads), shape(heads),
        shape(heads), shape(shard),
    )
    return pl.pallas_call(
        functools.partial(finish_layer, norm_at),
        grid=(tokens // TBLK,),
        out_shape=(shape(tokens, width), jax.ShapeDtypeStruct((tokens, width), BF16))
        + tuple(shape(*item.shape) for item in passed)
        + small,
        in_specs=[rows, once(norms)] + [rows] * 6 + [once(total)] + [once(item) for item in passed],
        out_specs=(rows, rows) + tuple(once(item) for item in passed + small),
        cost_estimate=cost(8),
        name="finish_layer",
    )(x, norms, part, other, grad, after, ffn, ffn_other, total, *passed)


def finish_shared(at, total_ref, cross_ref, mine_ref, other_ref, bc_ref, tap_ref, bias_ref, norm_ref, both):
    half = lax.axis_index("tensor")
    cols = pl.ds(pl.multiple_of(half * LANES, LANES), LANES)
    bc_ref[...] = mine_ref[:, cols] + other_ref[:, cols]
    both[...] = total_ref[...] + cross_ref[...]
    for tap in range(KCONV):
        tap_ref[tap : tap + 1, :] = both[pl.ds(at + 2 * tap + half, 1), :]
    bias_ref[...] = both[pl.ds(at + 2 * KCONV + half, 1), :][0]
    norm_ref[...] = own_lanes(both, at + 2 * KCONV + 2, norm_ref.shape[0])


def run_finish_shared(total, cross, mine, other, shard, at):
    vmem = pl.BlockSpec(memory_space=pltpu.VMEM)
    shape = lambda *sizes: jax.ShapeDtypeStruct(sizes, F32)
    return pl.pallas_call(
        functools.partial(finish_shared, at),
        out_shape=(shape(mine.shape[0], LANES), shape(KCONV, LANES), shape(LANES), shape(shard)),
        in_specs=[vmem] * 4,
        out_specs=(vmem,) * 4,
        scratch_shapes=[pltpu.VMEM(total.shape, F32)],
        name="finish_shared",
    )(total, cross, mine, other)


def swap(partial):
    return lax.ppermute(partial, "tensor", [(0, 1), (1, 0)])


def join(mine, other):
    return mine.astype(F32) + other.astype(F32)


def tensor_sum(partial):
    return join(partial, swap(partial))


def thirds(size):
    part = size // 3
    return [(0, part), (part, 2 * part), (2 * part, size)]


def local(
    layer_input, w_norm1, w_zx, w_bc, w_dt, conv_x, conv_xb, conv_bc, conv_bcb, dt_bias, a_log,
    d_skip, w_mnorm, w_mout, query_key_value_weight, output_weight, w_norm2, w_gu, w_down,
    grad_output,
):
    devices = lax.axis_size("dp")
    tokens, width = layer_input.shape
    shard = w_zx.shape[0]
    channels = conv_xb.shape[0]
    heads = dt_bias.shape[0]
    qkv_width = query_key_value_weight.shape[2]
    units = w_down.shape[0]
    attn_width = output_weight.shape[1]
    tail = jnp.concatenate(
        [w_dt, w_norm1[:, None], w_norm2[:, None], jnp.zeros((shard, LANES - heads - 2), BF16)],
        axis=1,
    )
    mixer_in = jnp.concatenate(
        [w_zx.reshape(shard, -1), w_bc, query_key_value_weight.reshape(shard, -1), tail], axis=1
    )
    in_width = mixer_in.shape[1]
    (w_in,) = gather_rows([mixer_in], devices, 0, [(0, *window) for window in thirds(in_width)])
    w_in, *small_params = lax.optimization_barrier(
        (w_in, conv_x, conv_xb, conv_bc, conv_bcb, dt_bias, a_log, d_skip, w_mnorm)
    )
    params = scan_params(*small_params)
    turned_one, proj, norms = run_project(layer_input, w_in, heads)
    out_shard = jnp.concatenate([w_mout.T, output_weight.reshape(attn_width, -1).T], axis=1)
    y, gated, square_sum, entering, w_out = run_scan_forward(
        proj, qkv_width, params, out_shard, devices
    )
    channels_all = channels * lax.axis_size("tensor")
    scale_m = lax.rsqrt(tensor_sum(square_sum) / channels_all + EPSILON)
    tables = rotary_tables(tokens)
    qkv_at = 2 * channels + 2 * NS
    qkv, lse, attended = run_attend_forward(proj, qkv_at, attn_width, tables)
    gain_m = w_mnorm.astype(F32)[None, :]
    mixer_out, mixed = run_mixer_forward(gated, scale_m, gain_m, attended, w_out)
    mixed, gate_up_shard, down_shard = lax.optimization_barrier(
        (mixed, w_gu.reshape(shard, -1), w_down.T)
    )
    other = swap(mixed)
    w_gate_up, w_down_t = gather_rows(
        [gate_up_shard, down_shard],
        devices,
        3,
        [(0, 0, units), (0, units, 2 * units), (1, 0, units)],
    )
    act_grad = run_product(grad_output, w_down_t, NN, F32)
    other, w_gate_up, w_down_t, act_grad = lax.optimization_barrier(
        (other, w_gate_up, w_down_t, act_grad)
    )
    after, scale_two, turned_two, activated, grad_gu_low, partial_two = run_feed_forward(
        layer_input, mixed, other, act_grad, norms, w_gate_up
    )
    other = swap(partial_two)
    grad_down = dot(grad_output, activated, TN).astype(BF16)
    (mine_gu,) = scatter_product(
        turned_two,
        grad_gu_low,
        [
            ([(0, 1, 0, units)], [(0, 0, units, 0, 0)]),
            ([(0, 1, units, 2 * units)], [(0, 0, units, 0, 1)]),
        ],
        [(shard, 2, units)],
        devices,
        1,
    )
    ffn_part = run_product(activated, w_down_t, NT, BF16)
    other, mine_gu, grad_down, ffn_part = lax.optimization_barrier(
        (other, mine_gu, grad_down, ffn_part)
    )
    ffn_other = swap(ffn_part)
    grad_mix_low, turned_mix, grad_mamba, grad_attended, inner_m, grad_norm2 = run_mixer_backward(
        partial_two, other, after, scale_two, grad_output, norms, w_out, gated, scale_m, gain_m
    )
    inner_m = tensor_sum(inner_m) / channels_all
    dqkv = run_attend_backward(qkv, lse, attended, grad_attended, 0, tables)
    grad_out = dot(turned_mix, mixer_out).astype(BF16)
    windows = [(0, None, 0, channels + attn_width), (1, None, 0, units)]
    pieces = [
        (0, 0, channels, 0, None),
        (0, channels, channels + attn_width, 1, None),
        (1, 0, units, 2, None),
    ]
    shapes = [(shard, channels), (shard, attn_width), (shard, units)]
    grad_proj, small_x, small_h, mine_mout, mine_o, mine_down = run_scan_backward(
        proj, y, entering, grad_mamba, scale_m, inner_m, dqkv, params,
        [grad_out, grad_down], windows, pieces, shapes, devices,
    )
    ffn_other, grad_proj = lax.optimization_barrier((ffn_other, grad_proj))
    partial_one, grad_norm1 = run_project_back(grad_proj, w_in, layer_input)
    partial_one, grad_proj = lax.optimization_barrier((partial_one, grad_proj))
    other = swap(partial_one)
    lanes_of = lambda size, start=0: range(start, start + size, LANES)
    places = [(0, row, lane) for row in range(KCONV + 2) for lane in lanes_of(channels)]
    places += [(1, row, 0) for row in range(3)]
    norm_at = len(places)
    places += [(2, 0, lane) for lane in lanes_of(width)]
    cross_at = len(places)
    places += [(0, row, lane) for row in range(KCONV + 1) for lane in lanes_of(2 * NS, channels)]
    places += [(3, 0, lane) for lane in lanes_of(width)]
    shared_at = 2 * channels
    step_at = qkv_at + qkv_width
    mine_zx, mine_bc, mine_qkv, mine_step, small = scatter_product(
        turned_one,
        grad_proj,
        [
            ([(0, 1, 0, channels)], [(0, 0, channels, 0, 0)]),
            ([(0, 1, channels, shared_at)], [(0, 0, channels, 0, 1)]),
            (
                [(0, 1, shared_at, in_width)],
                [
                    (0, 0, 2 * NS, 1, None),
                    (0, 2 * NS, 2 * NS + qkv_width, 2, 0),
                    (0, 2 * NS + qkv_width, in_width - shared_at, 3, "turned"),
                ],
            ),
        ],
        [
            (shard, 2, channels),
            (shard, 2 * NS),
            (shard, 1, qkv_width),
            (heads, shard),
        ],
        devices,
        5,
        (small_x, small_h, grad_norm2, grad_norm1),
        places,
    )
    other, mine_bc = lax.optimization_barrier((other, mine_bc))
    passed = (mine_zx, mine_qkv, mine_step, mine_mout, mine_o, mine_gu, mine_down)
    cross, other_bc = swap(small), swap(mine_bc)
    grad_source, result, *rest = run_finish(
        layer_input, norms, partial_one, other, grad_mix_low, after, ffn_part, ffn_other, small,
        passed, channels, heads, shard, norm_at,
    )
    mine_zx, mine_qkv, mine_step, mine_mout, mine_o, mine_gu, mine_down = rest[: len(passed)]
    grad_taps, grad_bias, grad_gain, grad_steps, grad_log, grad_skip, own_norm2 = rest[len(passed) :]
    grad_bc, grad_tapsb, grad_biasb, own_norm1 = run_finish_shared(
        small, cross, mine_bc, other_bc, shard, cross_at
    )
    return (
        result,
        grad_source,
        own_norm1,
        mine_zx,
        grad_bc,
        mine_step.T,
        grad_taps,
        grad_bias,
        grad_tapsb,
        grad_biasb,
        grad_steps,
        grad_log,
        grad_skip,
        grad_gain,
        mine_mout.T,
        mine_qkv,
        mine_o.T.reshape(output_weight.shape),
        own_norm2,
        mine_gu,
        mine_down.T,
    )


def solution(mesh):
    return jax.shard_map(
        local,
        mesh=mesh,
        in_specs=(
            P("dp", None),
            P("dp"),
            P("dp", None, "tensor"),
            P("dp", None),
            P("dp", "tensor"),
            P(None, "tensor"),
            P("tensor"),
            P(),
            P(),
            P("tensor"),
            P("tensor"),
            P("tensor"),
            P("tensor"),
            P("tensor", "dp"),
            P("dp", "tensor", None),
            P("tensor", None, "dp"),
            P("dp"),
            P("dp", None, "tensor"),
            P("tensor", "dp"),
            P("dp", None),
        ),
        out_specs=(
            P("dp", None),
            P("dp", None),
            P("dp"),
            P("dp", None, "tensor"),
            P("dp", "tensor"),
            P("dp", "tensor"),
            P(None, "tensor"),
            P("tensor"),
            P(None, "tensor"),
            P("tensor"),
            P("tensor"),
            P("tensor"),
            P("tensor"),
            P("tensor"),
            P("tensor", "dp"),
            P("dp", "tensor", None),
            P("tensor", None, "dp"),
            P("dp"),
            P("dp", None, "tensor"),
            P("tensor", "dp"),
        ),
        check_vma=False,
    )
```

```python
import functools
import math

import jax
import jax.numpy as jnp
import numpy as np
from jax import lax
from jax.experimental import pallas as pl
from jax.experimental.pallas import tpu as pltpu
from jax.sharding import PartitionSpec as P

HEAD_SIZE = 64
MP = 64
NS = 128
KCONV = 4
SPAN = 128
QBLK = 256
FINE = 32
TBLK = 256
NBLK = 128
UBLK = 256
LANES = 128
EDGE = 8

EPSILON = 1e-05
HIGHEST = lax.Precision.HIGHEST
LOG_BASE = math.log(100000000000.0)
MASKED = -1e30
MESH = pl.DeviceIdType.MESH
F32 = jnp.float32
BF16 = jnp.bfloat16

NN = ((1,), (0,))
NT = ((1,), (1,))
TN = ((0,), (0,))


def dot(left, right, dims=NN, precision=None):
    return lax.dot_general(
        left, right, (dims, ((), ())), preferred_element_type=F32, precision=precision
    )


def iota(shape, dim):
    return lax.broadcasted_iota(jnp.int32, shape, dim)


def ring_place(chip, chips):
    odd = lax.rem(chip, 2)
    half = lax.div(chip, 2)
    return (1 - odd) * half + odd * (chips - 1 - half)


def ring_chip(place, chips):
    place = lax.rem(place + 4 * chips, chips)
    back = lax.div(place, chips // 2)
    return (1 - back) * (2 * place) + back * (2 * (chips - 1 - place) + 1)


def ring_setup(chips):
    me = lax.axis_index("dp")
    group = lax.axis_index("tensor")
    chip = lax.div(me, 2)
    core = lax.rem(me, 2)
    place = ring_place(chip, chips)
    right = ring_chip(place + 1, chips) * 2 + core
    left = ring_chip(place - 1, chips) * 2 + core
    mate = chip * 2 + (1 - core)
    barrier = pltpu.get_barrier_semaphore()
    for other in (right, left, mate):
        pl.semaphore_signal(barrier, inc=1, device_id=(other, group), device_id_type=MESH)
    pl.semaphore_wait(barrier, 3)
    return me, group, core, place, right, left, mate


class RingGather:
    def __init__(self, devices, x_ref, o_ref, sems, cols=slice(None)):
        self.cols = cols
        self.chips = devices // 2
        self.ahead = self.chips // 2
        self.behind = self.chips - 1 - self.ahead
        self.x_ref, self.o_ref, self.rows = x_ref, o_ref, x_ref.shape[0]
        self.fs, self.fr, self.bs, self.br, self.cs, self.cr, self.own_sem = sems

    def locate(self):
        me = lax.axis_index("dp")
        self.group = lax.axis_index("tensor")
        self.core = lax.rem(me, 2)
        chip = lax.div(me, 2)
        self.place = ring_place(chip, self.chips)
        self.right = ring_chip(self.place + 1, self.chips) * 2 + self.core
        self.left = ring_chip(self.place - 1, self.chips) * 2 + self.core
        self.mate = chip * 2 + (1 - self.core)
        self.me = me

    def slot(self, index):
        rows = pl.ds(pl.multiple_of(index * self.rows, self.rows), self.rows)
        return self.o_ref.at[rows, self.cols]

    def copy(self, shift, ssem, rsem, target):
        if shift == 0:
            index, source = self.me, self.x_ref.at[:, self.cols]
        else:
            index = ring_chip(self.place + shift, self.chips) * 2 + self.core
            source = self.slot(index)
        return pltpu.make_async_remote_copy(
            src_ref=source,
            dst_ref=self.slot(index),
            send_sem=ssem,
            recv_sem=rsem,
            device_id=(target, self.group),
            device_id_type=MESH,
        )

    def fore(self, step):
        return self.copy(-step, self.fs.at[step], self.fr.at[step], self.right)

    def back(self, step):
        return self.copy(step, self.bs.at[step], self.br.at[step], self.left)

    def across(self, shift):
        number = 0 if shift == 0 else 2 * abs(shift) - (1 if shift < 0 else 0)
        return self.copy(shift, self.cs.at[number], self.cr.at[number], self.mate)

    def own(self):
        return pltpu.make_async_copy(
            self.x_ref.at[:, self.cols], self.slot(self.me), self.own_sem
        )

    def greet(self):
        self.locate()
        barrier = pltpu.get_barrier_semaphore()
        for other in (self.right, self.left, self.mate):
            pl.semaphore_signal(
                barrier, inc=1, device_id=(other, self.group), device_id_type=MESH
            )
        pl.semaphore_wait(barrier, 3)

    def begin(self):
        self.locate()
        self.fore(0).start()
        self.back(0).start()
        self.across(0).start()
        self.own().start()

    def hop(self, step):
        self.locate()
        self.fore(step - 1).wait_recv()
        if step < self.ahead:
            self.fore(step).start()
        self.across(-step).start()
        if step <= self.behind:
            self.back(step - 1).wait_recv()
            if step < self.behind:
                self.back(step).start()
            self.across(step).start()

    def finish(self):
        self.locate()
        self.own().wait()
        for step in range(self.ahead):
            self.fore(step).wait_send()
        for step in range(self.behind):
            self.back(step).wait_send()
        for shift in range(-self.ahead, self.behind + 1):
            self.across(shift).wait()


def gather_sems(devices):
    dma = pltpu.SemaphoreType.DMA
    return [dma((devices // 2,))] * 6 + [dma(())]


def gather_shape(shard, devices):
    return jax.ShapeDtypeStruct((shard.shape[0] * devices, shard.shape[1]), shard.dtype)


def gather_kernel(devices, count, windows, *refs):
    shards, outs, sems = refs[:count], refs[count : 2 * count], refs[2 * count :]
    each = len(sems) // len(windows)
    rings = [
        RingGather(
            devices, shards[i], outs[i], sems[place * each : (place + 1) * each], slice(first, last)
        )
        for place, (i, first, last) in enumerate(windows)
    ]
    rings[0].greet()
    for ring in rings:
        ring.begin()
    for step in range(1, rings[0].ahead + 1):
        for ring in rings:
            ring.hop(step)
    for ring in rings:
        ring.finish()


def cost(micros):
    return pl.CostEstimate(flops=int(micros * 1e9), bytes_accessed=0, transcendentals=0)


def gather_rows(shards, devices, collective, windows):
    count = len(shards)
    anywhere = pl.BlockSpec(memory_space=pl.ANY)
    return pl.pallas_call(
        functools.partial(gather_kernel, devices, count, windows),
        out_shape=tuple(gather_shape(shard, devices) for shard in shards),
        in_specs=[anywhere] * count,
        out_specs=(anywhere,) * count,
        scratch_shapes=gather_sems(devices) * len(windows),
        compiler_params=pltpu.CompilerParams(collective_id=collective, has_side_effects=True),
        cost_estimate=cost(3),
        name="gather_rows",
    )(*shards)


def scatter_order(chips):
    ahead = chips // 2
    behind = chips - 1 - ahead
    order = []
    for step in range(ahead):
        order.append(-(ahead - step))
        if step < behind:
            order.append(behind - step)
    order.append(0)
    return order


class RingScatter:
    def __init__(self, devices, windows, pieces, operands, outs, scratch):
        self.chips = devices // 2
        self.ahead = self.chips // 2
        self.behind = self.chips - 1 - self.ahead
        self.windows, self.pieces, self.operands, self.outs = windows, pieces, operands, outs
        count = len(windows)
        self.mine, self.boxes, rest = scratch[:count], scratch[count : 2 * count], scratch[2 * count :]
        self.fbox, self.bbox, self.fout, self.bout = rest[:4]
        self.os, self.ms, self.mr, self.fs, self.fr, self.bs, self.br = rest[4:]
        self.rows = self.fbox.shape[1]
        widths = [item.shape[2] for item in self.mine]
        self.cols = [slice(sum(widths[:i]), sum(widths[: i + 1])) for i in range(count)]

    def locate(self):
        me = lax.axis_index("dp")
        self.group = lax.axis_index("tensor")
        self.core = lax.rem(me, 2)
        chip = lax.div(me, 2)
        self.place = ring_place(chip, self.chips)
        self.right = ring_chip(self.place + 1, self.chips) * 2 + self.core
        self.left = ring_chip(self.place - 1, self.chips) * 2 + self.core
        self.mate = chip * 2 + (1 - self.core)

    def greet(self):
        self.locate()
        barrier = pltpu.get_barrier_semaphore()
        for other in (self.right, self.left, self.mate):
            pl.semaphore_signal(
                barrier, inc=1, device_id=(other, self.group), device_id_type=MESH
            )
        pl.semaphore_wait(barrier, 3)

    def product(self, i):
        return self.windows[i][1] is not None

    def shift_of(self, slot):
        step = slot // 2
        odd = slot % 2
        return (1 - odd) * (step - self.ahead) + odd * (self.behind - step)

    def half(self, which):
        return pl.ds(pl.multiple_of(which * self.rows, self.rows), self.rows)

    def block(self, i, slot, which):
        index = ring_chip(self.place + self.shift_of(slot), self.chips) * 2 + which
        left, right, first, last = self.windows[i]
        return self.operands[left].at[self.half(index), first:last]

    def remote(self, source, target_ref, ssem, rsem, target):
        return pltpu.make_async_remote_copy(
            src_ref=source,
            dst_ref=target_ref,
            send_sem=ssem,
            recv_sem=rsem,
            device_id=(target, self.group),
            device_id_type=MESH,
        )

    def across(self, i, slot):
        if self.product(i):
            source = self.mine[i].at[slot, self.half(1 - self.core)]
        else:
            source = self.block(i, slot, 1 - self.core)
        return self.remote(
            source, self.boxes[i].at[slot], self.ms.at[i, slot], self.mr.at[i, slot], self.mate
        )

    def own(self, i, slot):
        return pltpu.make_async_copy(
            self.block(i, slot, self.core), self.mine[i].at[slot], self.os.at[i, slot]
        )

    def fore(self, step):
        return self.remote(
            self.fout.at[step], self.fbox.at[step], self.fs.at[step], self.fr.at[step], self.right
        )

    def back(self, step):
        return self.remote(
            self.bout.at[step], self.bbox.at[step], self.bs.at[step], self.br.at[step], self.left
        )

    def begin(self):
        self.locate()
        for i in range(len(self.windows)):
            if not self.product(i):
                for slot in range(self.chips):
                    self.across(i, slot).start()
                    self.own(i, slot).start()

    def produce(self, slot):
        chip = ring_chip(self.place + self.shift_of(slot), self.chips)
        size = 2 * self.rows
        for i, (left, right, first, last) in enumerate(self.windows):
            if right is None:
                continue
            at = pl.multiple_of(chip * size, size)
            terms = dot(self.operands[left][pl.ds(at, size), :], self.operands[right][:, first:last])
            self.mine[i][slot] = terms.astype(BF16)
            self.across(i, slot).start()

    def local_sum(self, i, slot, cols, others):
        rows = self.half(self.core) if self.product(i) else slice(None)
        total = self.mine[i][slot, rows, cols].astype(F32) + self.boxes[i][slot, :, cols].astype(F32)
        whole = slice(self.cols[i].start + cols.start, self.cols[i].start + cols.stop)
        for ref in others:
            total = total + ref[:, whole].astype(F32)
        return total

    def arrive(self, slot):
        for i in range(len(self.windows)):
            if not self.product(i):
                self.own(i, slot).wait()
            self.across(i, slot).wait_recv()

    def put(self, target, slot, others):
        self.arrive(slot)
        for i, cols in enumerate(self.cols):
            total = self.local_sum(i, slot, slice(0, cols.stop - cols.start), others)
            target[:, cols] = total.astype(BF16)

    def hop_back(self, step, later):
        if later:
            self.back(step - 1).wait_recv()
        self.put(self.bout.at[step], 2 * step, [self.bbox.at[step - 1]] if later else [])
        self.back(step).start()

    def hop_fore(self, step, later):
        if later:
            self.fore(step - 1).wait_recv()
        self.put(self.fout.at[step], 2 * step + 1, [self.fbox.at[step - 1]] if later else [])
        self.fore(step).start()

    def hop(self, step):
        self.locate()
        self.hop_back(step, step > 0)
        if step < self.behind:
            self.hop_fore(step, step > 0)

    def finish(self):
        self.locate()
        slot = self.chips - 1
        self.arrive(slot)
        self.fore(self.behind - 1).wait_recv()
        self.back(self.ahead - 1).wait_recv()
        others = [self.fbox.at[self.behind - 1], self.bbox.at[self.ahead - 1]]
        for i, first, last, out, form in self.pieces:
            total = self.local_sum(i, slot, slice(first, last), others)
            if form == "turned":
                self.outs[out][...] = total.T[: self.outs[out].shape[0]]
            elif form is None:
                self.outs[out][...] = total
            else:
                self.outs[out][:, form, :] = total
        for step in range(self.ahead):
            self.back(step).wait_send()
        for step in range(self.behind):
            self.fore(step).wait_send()
        for slot in range(self.chips):
            for i in range(len(self.windows)):
                self.across(i, slot).wait_send()


def run_rings(rings, after_first=None):
    ahead, behind = rings[0].ahead, rings[0].behind

    def turn(step, carry):
        def part(odd, kept):
            for ring in rings:
                ring.produce(2 * step + odd)
            return kept

        lax.fori_loop(0, 2, part, 0)

        @pl.when(step == 0)
        def _():
            for ring in rings:
                ring.hop_back(0, False)
                ring.hop_fore(0, False)
            if after_first is not None:
                after_first()

        @pl.when(step > 0)
        def _():
            for ring in rings:
                ring.hop_back(step, True)
                pl.when(step < behind)(functools.partial(ring.hop_fore, step, True))

        return carry

    lax.fori_loop(0, ahead, turn, 0)


def scatter_scratch(windows, rows, devices):
    chips = devices // 2
    count = len(windows)
    dma = pltpu.SemaphoreType.DMA
    widths = [last - first for left, right, first, last in windows]
    mine = [
        pltpu.VMEM((chips, rows if right is None else 2 * rows, last - first), BF16)
        for left, right, first, last in windows
    ]
    boxes = [pltpu.VMEM((chips, rows, width), BF16) for width in widths]
    box = pltpu.VMEM((chips // 2, rows, sum(widths)), BF16)
    return mine + boxes + [box] * 4 + [dma((count, chips))] * 3 + [dma((chips,))] * 4


class Total:
    def __init__(self, devices, x_ref, o_ref, scratch):
        self.chips = devices // 2
        self.x_ref, self.o_ref = x_ref, o_ref
        self.mate_box, self.joined, self.boxes, self.ms, self.mr, self.ss, self.sr = scratch
        me = lax.axis_index("dp")
        self.group = lax.axis_index("tensor")
        self.chip = lax.div(me, 2)
        core = lax.rem(me, 2)
        self.mate = self.chip * 2 + (1 - core)
        self.peers = [
            lax.rem(self.chip + shift, self.chips) * 2 + core for shift in range(self.chips)
        ]

    def greet(self):
        barrier = pltpu.get_barrier_semaphore()
        for other in [self.mate] + self.peers[1:]:
            pl.semaphore_signal(
                barrier, inc=1, device_id=(other, self.group), device_id_type=MESH
            )
        pl.semaphore_wait(barrier, self.chips)

    def remote(self, source, target_ref, ssem, rsem, target):
        return pltpu.make_async_remote_copy(
            src_ref=source,
            dst_ref=target_ref,
            send_sem=ssem,
            recv_sem=rsem,
            device_id=(target, self.group),
            device_id_type=MESH,
        )

    def across(self):
        return self.remote(self.x_ref, self.mate_box, self.ms, self.mr, self.mate)

    def copies(self):
        return [
            self.remote(
                self.joined,
                self.boxes.at[self.chip],
                self.ss.at[shift],
                self.sr.at[shift],
                self.peers[shift],
            )
            for shift in range(1, self.chips)
        ]

    def begin(self):
        self.across().start()

    def spread(self):
        self.across().wait_recv()
        self.joined[...] = self.x_ref[...] + self.mate_box[...]
        for copy in self.copies():
            copy.start()
        self.boxes[self.chip] = self.joined[...]

    def finish(self):
        for copy in self.copies():
            copy.wait_recv()
        result = self.boxes[0]
        for other in range(1, self.chips):
            result = result + self.boxes[other]
        self.o_ref[...] = result
        self.across().wait_send()
        for copy in self.copies():
            copy.wait_send()


def total_scratch(values, devices):
    chips = devices // 2
    dma = pltpu.SemaphoreType.DMA
    return [
        pltpu.VMEM(values.shape, F32),
        pltpu.VMEM(values.shape, F32),
        pltpu.VMEM((chips,) + values.shape, F32),
        dma(()),
        dma(()),
        dma((chips,)),
        dma((chips,)),
    ]


def turned_copy(source, target):
    for start in range(0, source.shape[1], LANES):
        target[start : start + LANES, :] = source[:, start : start + LANES].T


def product_kernel(devices, groups, outs, places, summed, left_ref, right_ref, *refs):
    values = refs[:summed]
    refs = refs[summed:]
    pieces_out, refs = refs[:outs], refs[outs:]
    total = None
    if summed:
        total_out, refs = refs[0], refs[1:]
    turned, scratch = refs[0], refs[1:]
    if summed:
        scratch, rest = scratch[:-8], scratch[-8:]
        together = rest[0]
        together[...] = jnp.zeros_like(together)
        for at, (which, row, lane) in enumerate(places):
            together[at : at + 1, :] = values[which][row : row + 1, lane : lane + LANES]
        total = Total(devices, together, total_out, rest[1:])
    each = len(scratch) // len(groups)
    rings = [
        RingScatter(
            devices, windows, pieces, (turned, right_ref), pieces_out,
            scratch[place * each : (place + 1) * each],
        )
        for place, (windows, pieces) in enumerate(groups)
    ]
    if total is None:
        rings[0].greet()
    else:
        total.greet()
        total.begin()
    for ring in rings:
        ring.locate()
    turned_copy(left_ref, turned)
    run_rings(rings, total.spread if total is not None else None)
    for ring in rings:
        ring.finish()
    if total is not None:
        total.finish()


def scatter_product(left, right, groups, shapes, devices, collective, values=(), places=()):
    vmem = pl.BlockSpec(memory_space=pltpu.VMEM)
    rows = left.shape[1] // devices
    scratch = [pltpu.VMEM(left.shape[::-1], BF16)]
    for windows, pieces in groups:
        scratch += scatter_scratch(windows, rows, devices)
    totals = ()
    if values:
        total = jax.ShapeDtypeStruct((len(places) + -len(places) % EDGE, LANES), F32)
        totals = (total,)
        scratch += [pltpu.VMEM(total.shape, F32)] + total_scratch(total, devices)
    return pl.pallas_call(
        functools.partial(
            product_kernel, devices, groups, len(shapes), places, len(values)
        ),
        out_shape=tuple(jax.ShapeDtypeStruct(shape, F32) for shape in shapes) + totals,
        in_specs=[vmem] * (2 + len(values)),
        out_specs=(vmem,) * (len(shapes) + len(totals)),
        scratch_shapes=scratch,
        compiler_params=pltpu.CompilerParams(collective_id=collective, has_side_effects=True),
        cost_estimate=cost(3),
        name="scatter_product",
    )(left, right, *values)


def head_spread(channels):
    return (iota((LANES, channels), 1) // MP == iota((LANES, channels), 0)).astype(BF16)


def parts(values, count):
    terms = []
    for _ in range(count):
        term = values.astype(BF16)
        terms.append(term)
        values = values - term.astype(F32)
    return terms


def pick(values, mask, count=2):
    return dot(jnp.concatenate(parts(values, count), axis=1), jnp.concatenate([mask] * count, axis=0))


def pick_left(mask, values, count):
    return dot(jnp.concatenate([mask] * count, axis=1), jnp.concatenate(parts(values, count), axis=0))


def gather_heads(values, spread):
    high, low = parts(values, 2)
    return dot(high, spread, NT) + dot(low, spread, NT)


def row_sums(values):
    high, low = parts(values, 2)
    ones = jnp.ones((EDGE, values.shape[1]), BF16)
    return dot(ones, high, NT) + dot(ones, low, NT)


def soft_step(raw):
    return jnp.maximum(raw, 0.0) + jnp.log1p(jnp.exp(-jnp.abs(raw)))


def window(buffer, start, span):
    return buffer[start : start + span, :]


def causal_taps(buffer, taps, span):
    total = taps[0:1, :] * window(buffer, EDGE - KCONV + 1, span)
    for tap in range(1, KCONV):
        total = total + taps[tap : tap + 1, :] * window(buffer, EDGE - KCONV + 1 + tap, span)
    return total


def span_rates(step_ref, bias, decay, spread, span):
    raw = step_ref[...] + bias
    step = soft_step(raw)
    lower = (iota((span, span), 1) <= iota((span, span), 0)).astype(BF16)
    cum = pick_left(lower, step * decay, 3)
    tails = jnp.exp(cum[span - 1 : span, :] - cum)
    wide = pick(jnp.concatenate([step, tails, jnp.exp(cum)], axis=0), spread)
    return raw, step, cum, wide[:span], wide[span : 2 * span], wide[2 * span :]


def pair_split(values, low_lanes):
    zero = jnp.zeros_like(values)
    return jnp.concatenate(
        [jnp.where(low_lanes, values, zero), jnp.where(low_lanes, zero, values)], axis=0
    )


def pair_decay(cum, cum_rows, pair, causal):
    parts = []
    for head in (2 * pair, 2 * pair + 1):
        differ = cum[:, head : head + 1] - cum_rows[head : head + 1, :]
        parts.append(jnp.exp(jnp.where(causal, differ, MASKED)))
    return parts


def scan_forward(
    devices, spans,
    z_ref, x_ref, bc_ref, step_ref,
    tap_ref, tapb_ref, row_ref, shard_ref,
    y_ref, gated_ref, square_ref, enter_ref, all_ref,
    state, buffer, *sems,
):
    span, channels = x_ref.shape
    width = shard_ref.shape[1]
    each = len(sems) // 2
    rings = [
        RingGather(devices, shard_ref, all_ref, sems[:each], slice(0, width // 2)),
        RingGather(devices, shard_ref, all_ref, sems[each:], slice(width // 2, width)),
    ]
    turn = pl.program_id(0)

    @pl.when(turn == 0)
    def _():
        rings[0].greet()
        for ring in rings:
            ring.begin()


    @pl.when(pl.program_id(0) == 0)
    def _():
        state[...] = jnp.zeros_like(state)
        buffer[span:, :] = jnp.zeros((EDGE, buffer.shape[1]), F32)

    buffer[:EDGE, :] = buffer[span:, :]
    buffer[EDGE:, :channels] = x_ref[...]
    buffer[EDGE:, channels:] = bc_ref[...]
    spread = head_spread(channels)
    bias, gain, biasb, stepb, decay, skip = unpack_rows(row_ref, spread)
    taps = jnp.concatenate([tap_ref[...], tapb_ref[...]], axis=1).astype(F32)
    conv = causal_taps(buffer, taps, span)
    conv = jax.nn.silu(conv + jnp.concatenate([bias, biasb], axis=1))
    inputs, shared = conv[:, :channels], conv[:, channels:]
    raw, step, cum, step_w, tails_w, grown_w = span_rates(step_ref, stepb, decay, spread, span)
    cum_rows = cum.T
    b_low = shared[:, :NS].astype(BF16)
    c_low = shared[:, NS:].astype(BF16)
    scaled = inputs * step_w
    scaled_low = scaled.astype(BF16)
    enter_ref[0] = state[...]
    outer = dot(c_low, state[...].astype(BF16)) * grown_w
    fresh = dot(b_low, (scaled * tails_w).astype(BF16), TN)
    state[...] = state[...] * grown_w[span - 1 : span, :] + fresh
    cross = dot(c_low, b_low, NT)
    causal = iota((span, span), 1) <= iota((span, span), 0)
    low_lanes = iota((span, LANES), 1) < MP
    for pair in range(channels // LANES):
        lanes = slice(pair * LANES, (pair + 1) * LANES)
        first, second = pair_decay(cum, cum_rows, pair, causal)
        weights = jnp.concatenate(
            [(cross * first).astype(BF16), (cross * second).astype(BF16)], axis=1
        )
        y_ref[:, lanes] = dot(weights, pair_split(scaled_low[:, lanes], low_lanes))
    y = y_ref[...] + outer + skip * inputs
    y_ref[...] = y
    gated = y * jax.nn.silu(z_ref[...])
    gated_ref[...] = gated.astype(BF16)
    square_ref[...] = row_sums(gated * gated)

    ahead = rings[0].ahead
    for step in range(1, ahead + 1):
        after = max(0, spans * step // ahead - (2 if step == ahead else 1))
        for ring in rings:
            pl.when(turn == after)(functools.partial(ring.hop, step))
    for ring in rings:
        pl.when(turn == spans - 1)(ring.finish)


def scan_backward(
    devices, spans, windows, pieces, outs_count, count,
    z_ref, x_ref, xp_ref, bc_ref, bp_ref, step_ref, y_ref, enter_ref,
    dyg_ref, scale_ref, inner_ref, dqkv_ref,
    tap_ref, tapb_ref, row_ref,
    *refs,
):
    sent, refs = refs[:count], refs[count:]
    (grad_ref, gx_ref, gh_ref), refs = refs[:3], refs[3:]
    outs, refs = refs[:outs_count], refs[outs_count:]
    (dstate, buffer, dbuffer, du_buf, col_buf), scratch = refs[:5], refs[5:]
    ring = RingScatter(devices, windows, pieces, sent, outs, scratch)
    span, channels = x_ref.shape
    turn = pl.program_id(0)

    @pl.when(turn == 0)
    def _():
        ring.greet()
        ring.begin()
        dstate[...] = jnp.zeros_like(dstate)
        dbuffer[...] = jnp.zeros_like(dbuffer)
        col_buf[...] = jnp.zeros_like(col_buf)
        gx_ref[...] = jnp.zeros_like(gx_ref)
        gh_ref[...] = jnp.zeros_like(gh_ref)

    inside = (turn < spans - 1).astype(F32)
    buffer[:EDGE, :channels] = xp_ref[...] * inside
    buffer[:EDGE, channels:] = bp_ref[...] * inside
    buffer[EDGE:, :channels] = x_ref[...]
    buffer[EDGE:, channels:] = bc_ref[...]
    spread = head_spread(channels)
    bias, gain, biasb, stepb, decay, skip = unpack_rows(row_ref, spread)
    taps = jnp.concatenate([tap_ref[...], tapb_ref[...]], axis=1).astype(F32)
    conv = causal_taps(buffer, taps, span) + jnp.concatenate([bias, biasb], axis=1)
    sig = jax.nn.sigmoid(conv)
    swished = conv * sig
    inputs, shared = swished[:, :channels], swished[:, channels:]
    b_low = shared[:, :NS].astype(BF16)
    c_low = shared[:, NS:].astype(BF16)
    raw, step, cum, step_w, tails_w, grown_w = span_rates(step_ref, stepb, decay, spread, span)
    cum_rows = cum.T
    scaled = inputs * step_w
    scaled_low = scaled.astype(BF16)

    z = z_ref[...]
    sig_z = jax.nn.sigmoid(z)
    swish = z * sig_z
    y = y_ref[...]
    scale = scale_ref[...].T[:, :1]
    normed = y * swish * scale
    dyg = dyg_ref[...]
    gain_grad = jnp.sum(dyg * normed, axis=0, keepdims=True)
    dgated = scale * (dyg * gain - normed * inner_ref[...].T[:, :1])
    dy = dgated * swish
    grad_ref[:, :channels] = (dgated * y * (sig_z * (1.0 + z * (1.0 - sig_z)))).astype(BF16)

    state_low = enter_ref[0].astype(BF16)
    dstate_low = dstate[...].astype(BF16)
    grown_low = (dy * grown_w).astype(BF16)
    dy_low = dy.astype(BF16)
    tailed = scaled * tails_w
    outer = dot(c_low, state_low) * grown_w
    from_state = dot(b_low, dstate_low)
    dc = dot(grown_low, state_low, NT)
    db = dot(tailed.astype(BF16), dstate_low, NT)
    leak = from_state * tailed
    last_w = grown_w[span - 1 : span, :]
    ends = (
        jnp.sum(leak, axis=0, keepdims=True)
        + jnp.sum(enter_ref[0] * dstate[...], axis=0, keepdims=True) * last_w
    )
    skips = jnp.sum(dy * inputs, axis=0, keepdims=True)
    dstate[...] = dstate[...] * last_w + dot(c_low, grown_low, TN)

    cross = dot(c_low, b_low, NT)
    causal = iota((span, span), 1) <= iota((span, span), 0)
    low_lanes = iota((span, LANES), 1) < MP
    lane = iota((span, LANES), 1)
    dcross = jnp.zeros((span, span), F32)
    row_part = jnp.zeros((span, LANES), F32)
    for pair in range(channels // LANES):
        lanes = slice(pair * LANES, (pair + 1) * LANES)
        decays = pair_decay(cum, cum_rows, pair, causal)
        dy_pair = pair_split(dy_low[:, lanes], low_lanes)
        dweights = dot(dy_pair, scaled_low[:, lanes], NT)
        both = []
        for part in range(2):
            head = 2 * pair + part
            dterm = dweights[part * span : (part + 1) * span] * decays[part]
            dcross = dcross + dterm
            flow = dterm * cross
            row_part = row_part + jnp.where(
                lane == head, jnp.sum(flow, axis=1, keepdims=True), 0.0
            )
            col_buf[head : head + 1, :] = jnp.sum(flow, axis=0, keepdims=True)
            both.append((cross * decays[part]).astype(BF16))
        du_buf[:, lanes] = dot(jnp.concatenate(both, axis=0), dy_pair, TN)
    du = du_buf[...] + from_state * tails_w
    dcross_low = dcross.astype(BF16)
    dc = dc + dot(dcross_low, b_low)
    db = db + dot(dcross_low, c_low, TN)

    sums = gather_heads(
        jnp.concatenate(
            [dy * outer - leak, du * inputs, ends, skips, jnp.zeros((EDGE - 2, channels), F32)],
            axis=0,
        ),
        spread,
    )
    at_end = sums[2 * span : 2 * span + 1, :]
    dcum = sums[:span] + row_part - col_buf[...].T
    upper = (iota((span, span), 1) >= iota((span, span), 0)).astype(BF16)
    drate = pick_left(upper, dcum, 3) + at_end
    dstep = drate * decay + sums[span : 2 * span]
    draw = dstep * jax.nn.sigmoid(raw)
    gh_ref[0:1, :] += jnp.sum(draw, axis=0, keepdims=True)
    gh_ref[1:2, :] += jnp.sum(drate * step, axis=0, keepdims=True) * decay
    gh_ref[2:3, :] += sums[2 * span + 1 : 2 * span + 2, :]

    dinputs = du * step_w + skip * dy
    dconv = jnp.concatenate([dinputs, db, dc], axis=1) * (sig * (1.0 + conv * (1.0 - sig)))
    dbuffer[span:, :] = dbuffer[:EDGE, :]
    dbuffer[:span, :] = dconv
    dbefore = jnp.zeros_like(dconv)
    for tap in range(KCONV):
        dbefore = dbefore + taps[tap : tap + 1, :] * window(dbuffer, KCONV - 1 - tap, span)
        gx_ref[tap : tap + 1, :] += jnp.sum(
            dconv * window(buffer, EDGE - KCONV + 1 + tap, span), axis=0, keepdims=True
        )
    gx_ref[KCONV : KCONV + 1, :] += jnp.sum(dconv, axis=0, keepdims=True)
    gx_ref[KCONV + 1 : KCONV + 2, :channels] += gain_grad
    width = 2 * channels + 2 * NS
    grad_ref[:, channels:width] = dbefore.astype(BF16)
    grad_ref[:, width : width + dqkv_ref.shape[1]] = dqkv_ref[...]
    grad_ref[:, width + dqkv_ref.shape[1] :] = draw.astype(BF16)
    for step in range(ring.ahead):
        pl.when(turn == spans * step // ring.ahead)(functools.partial(ring.hop, step))
    pl.when(turn == spans - 1)(ring.finish)


def scan_params(conv_x, conv_xb, conv_bc, conv_bcb, dt_bias, a_log, d_skip, w_mnorm):
    heads = dt_bias.shape[0]
    fill = jnp.zeros((LANES - heads,), BF16)
    flat = [conv_xb, w_mnorm, conv_bcb, dt_bias, fill, a_log, fill, d_skip, fill]
    size = sum(item.shape[0] for item in flat) // LANES
    flat.append(jnp.zeros((-size % EDGE * LANES,), BF16))
    rows = jnp.concatenate(flat).astype(F32).reshape(-1, LANES)
    return (conv_x, conv_bc, rows)


def unpack_rows(row_ref, spread):
    channels = spread.shape[1]
    count = channels // LANES
    at = 2 * count + 2 * NS // LANES

    def join_rows(first, number):
        return jnp.concatenate(
            [row_ref[i : i + 1, :] for i in range(first, first + number)], axis=1
        )

    skip = jnp.broadcast_to(row_ref[at + 2 : at + 3, :], (EDGE, LANES)).astype(BF16)
    return (
        join_rows(0, count),
        join_rows(count, count),
        join_rows(2 * count, 2 * NS // LANES),
        row_ref[at : at + 1, :],
        -jnp.exp(row_ref[at + 1 : at + 2, :]),
        dot(skip, spread)[:1],
    )


def whole_spec(array):
    return pl.BlockSpec(array.shape, lambda turn: (0,) * array.ndim)


def run_scan_forward(proj, qkv_width, params, shard, devices):
    tokens = proj.shape[0]
    channels = params[0].shape[1]
    step_at = (2 * channels + 2 * NS + qkv_width) // LANES
    spans = tokens // SPAN
    bc_at = 2 * channels // (2 * NS)
    rows = lambda width, at: pl.BlockSpec((SPAN, width), lambda turn: (turn, at))
    anywhere = pl.BlockSpec(memory_space=pl.ANY)
    return pl.pallas_call(
        functools.partial(scan_forward, devices, spans),
        grid=(spans,),
        out_shape=(
            jax.ShapeDtypeStruct((tokens, channels), F32),
            jax.ShapeDtypeStruct((tokens, channels), BF16),
            jax.ShapeDtypeStruct((EDGE, tokens), F32),
            jax.ShapeDtypeStruct((spans, NS, channels), F32),
            gather_shape(shard, devices),
        ),
        in_specs=[rows(channels, 0), rows(channels, 1), rows(2 * NS, bc_at), rows(LANES, step_at)]
        + [whole_spec(item) for item in params]
        + [anywhere],
        out_specs=(
            rows(channels, 0),
            rows(channels, 0),
            pl.BlockSpec((EDGE, SPAN), lambda turn: (0, turn)),
            pl.BlockSpec((1, NS, channels), lambda turn: (turn, 0, 0)),
            anywhere,
        ),
        scratch_shapes=[
            pltpu.VMEM((NS, channels), F32),
            pltpu.VMEM((SPAN + EDGE, channels + 2 * NS), F32),
        ]
        + gather_sems(devices) * 2,
        compiler_params=pltpu.CompilerParams(collective_id=2, has_side_effects=True),
        cost_estimate=cost(20),
        name="scan_forward",
    )(proj, proj, proj, proj, *params, shard)


def run_scan_backward(
    proj, y, entering, dyg, scale, inner, dqkv, params, sent, windows, pieces, shapes,
    devices,
):
    tokens, width = proj.shape
    channels = params[0].shape[1]
    qkv_width = dqkv.shape[1]
    step_at = (2 * channels + 2 * NS + qkv_width) // LANES
    spans = tokens // SPAN
    bc_at = 2 * channels // (2 * NS)
    edges = SPAN // EDGE
    rows = lambda size, at: pl.BlockSpec((SPAN, size), lambda turn: (spans - 1 - turn, at))
    edge = lambda size, at: pl.BlockSpec(
        (EDGE, size), lambda turn: (jnp.maximum((spans - 1 - turn) * edges - 1, 0), at)
    )
    keep = lambda shape: pl.BlockSpec(shape, lambda turn: (0, 0))
    shapes = tuple(jax.ShapeDtypeStruct(shape, F32) for shape in shapes)
    return pl.pallas_call(
        functools.partial(
            scan_backward, devices, spans, windows, pieces, len(shapes), len(sent)
        ),
        grid=(spans,),
        out_shape=(
            jax.ShapeDtypeStruct((tokens, width), BF16),
            jax.ShapeDtypeStruct((EDGE, channels + 2 * NS), F32),
            jax.ShapeDtypeStruct((EDGE, LANES), F32),
        )
        + shapes,
        in_specs=[
            rows(channels, 0),
            rows(channels, 1),
            edge(channels, 1),
            rows(2 * NS, bc_at),
            edge(2 * NS, bc_at),
            rows(LANES, step_at),
            rows(channels, 0),
            pl.BlockSpec((1, NS, channels), lambda turn: (spans - 1 - turn, 0, 0)),
            rows(channels, 0),
            pl.BlockSpec((EDGE, SPAN), lambda turn: (0, spans - 1 - turn)),
            pl.BlockSpec((EDGE, SPAN), lambda turn: (0, spans - 1 - turn)),
            rows(qkv_width, 0),
        ]
        + [whole_spec(item) for item in params]
        + [pl.BlockSpec(memory_space=pl.ANY)] * len(sent),
        out_specs=(
            rows(width, 0),
            keep((EDGE, channels + 2 * NS)),
            keep((EDGE, LANES)),
        )
        + tuple(keep(item.shape) for item in shapes),
        scratch_shapes=[
            pltpu.VMEM((NS, channels), F32),
            pltpu.VMEM((SPAN + EDGE, channels + 2 * NS), F32),
            pltpu.VMEM((SPAN + EDGE, channels + 2 * NS), F32),
            pltpu.VMEM((SPAN, channels), F32),
            pltpu.VMEM((LANES, SPAN), F32),
        ]
        + scatter_scratch(windows, sent[0].shape[0] // devices, devices),
        compiler_params=pltpu.CompilerParams(collective_id=6, has_side_effects=True),
        cost_estimate=cost(47),
        name="scan_backward",
    )(
        proj, proj, proj, proj, proj, proj, y, entering, dyg, scale, inner, dqkv, *params, *sent,
    )


def rotary_tables(tokens):
    half = HEAD_SIZE // 2
    exponent = np.arange(half, dtype=np.float64) * (-2.0 * LOG_BASE / HEAD_SIZE)
    rates = np.tile(np.exp(exponent.astype(np.float32)).astype(np.float64), LANES // half)
    tables = []
    for places in (np.arange(FINE), np.arange(0, tokens, FINE)):
        angles = places[:, None] * rates[None, :]
        tables += [np.cos(angles).astype(np.float32), np.sin(angles).astype(np.float32)]
    return tables


def fill_rotary(fine_cos, fine_sin, coarse_cos, coarse_sin, cosine, sine):
    small_cos, small_sin = fine_cos[...], fine_sin[...]
    for turn in range(coarse_cos.shape[0]):
        big_cos, big_sin = coarse_cos[turn : turn + 1, :], coarse_sin[turn : turn + 1, :]
        rows = slice(turn * FINE, (turn + 1) * FINE)
        cosine[rows, :] = small_cos * big_cos - small_sin * big_sin
        sine[rows, :] = small_sin * big_cos + small_cos * big_sin


def head_masks():
    half = HEAD_SIZE // 2
    row, col = iota((LANES, LANES), 0), iota((LANES, LANES), 1)
    place = col % HEAD_SIZE
    ahead = jnp.where(place < half, -1.0, 0.0)
    behind = jnp.where(place < half, 0.0, 1.0)

    def turn(start):
        return jnp.where(row == start + half, ahead, jnp.where(row == start - half, behind, 0.0))

    first = row < HEAD_SIZE
    left = col < HEAD_SIZE
    low = lambda mask: mask.astype(BF16)
    within = low(turn(col))
    copy = low(jnp.where(row == place, 1.0, 0.0))
    copy_turn = low(jnp.where(first, turn(place), 0.0))
    value = low(jnp.where(row == place + HEAD_SIZE, 1.0, 0.0))
    fold = low(jnp.where(left & (row % HEAD_SIZE == place), 1.0, 0.0))
    other = row % HEAD_SIZE
    fold_turn = low(
        jnp.where(
            left,
            jnp.where(other == place + half, ahead, jnp.where(other == place - half, behind, 0.0)),
            0.0,
        )
    )
    fold_value = low(jnp.where(left, 0.0, jnp.where(other == place, 1.0, 0.0)))
    return within, copy, copy_turn, value, fold, fold_turn, fold_value


def attend_forward(
    q_ref, kv_ref, fine_cos, fine_sin, coarse_cos, coarse_sin,
    qkv_ref, lse_ref, o_ref, vt, cos_ref, sin_ref,
):
    fill_rotary(fine_cos, fine_sin, coarse_cos, coarse_sin, cos_ref, sin_ref)
    tokens, query_width = q_ref.shape
    pairs = query_width // LANES
    within, copy, copy_turn, value = head_masks()[:4]

    def turn_rows(i, carry):
        rows = pl.ds(pl.multiple_of(i * QBLK, QBLK), QBLK)
        cosine, sine = cos_ref[rows, :], sin_ref[rows, :]
        for pair in range(pairs):
            lanes = slice(pair * LANES, (pair + 1) * LANES)
            query = q_ref[rows, lanes]
            turned = query * cosine + pick(query, within) * sine
            qkv_ref[rows, lanes] = (turned * HEAD_SIZE**-0.5).astype(BF16)
        kv = kv_ref[rows, :]
        keys = pick(kv, copy) * cosine + pick(kv, copy_turn) * sine
        qkv_ref[rows, query_width : query_width + LANES] = keys.astype(BF16)
        qkv_ref[rows, query_width + LANES :] = dot(kv.astype(BF16), value).astype(BF16)
        vt[:, rows] = kv.T[HEAD_SIZE:, :].astype(BF16)
        return carry

    lax.fori_loop(0, tokens // QBLK, turn_rows, 0)
    low_lanes = iota((QBLK, LANES), 1) < HEAD_SIZE
    wide = (QBLK, 2 * QBLK)
    visible = iota(wide, 0) <= iota(wide, 1) % QBLK

    def block(i, carry):
        here = pl.ds(pl.multiple_of(i * QBLK, QBLK), QBLK)
        queries = [
            pair_split(qkv_ref[here, pair * LANES : (pair + 1) * LANES], low_lanes)
            for pair in range(pairs)
        ]

        def tile(there, state, edge):
            keys = qkv_ref[there, query_width : query_width + LANES]
            result = []
            for pair in range(pairs):
                top, total, out = state[3 * pair : 3 * pair + 3]
                scores = dot(keys, queries[pair], NT)
                if edge:
                    scores = jnp.where(visible, scores, MASKED)
                higher = jnp.maximum(top, jnp.max(scores, axis=0, keepdims=True))
                probs = jnp.exp(scores - higher)
                fade = jnp.exp(top - higher)
                total = total * fade + jnp.sum(probs, axis=0, keepdims=True)
                out = out * fade + dot(vt[:, there], probs.astype(BF16))
                result += [higher, total, out]
            return tuple(result)

        state = (
            jnp.full((1, 2 * QBLK), MASKED, F32),
            jnp.zeros((1, 2 * QBLK), F32),
            jnp.zeros((HEAD_SIZE, 2 * QBLK), F32),
        ) * pairs
        state = lax.fori_loop(
            0,
            i,
            lambda j, state: tile(pl.ds(pl.multiple_of(j * QBLK, QBLK), QBLK), state, False),
            state,
        )
        state = tile(here, state, True)
        for pair in range(pairs):
            top, total, out = state[3 * pair : 3 * pair + 3]
            out = out / total
            lse = top + jnp.log(total)
            lse_ref[2 * pair : 2 * pair + 1, here] = lse[:, :QBLK]
            lse_ref[2 * pair + 1 : 2 * pair + 2, here] = lse[:, QBLK:]
            both = jnp.concatenate([out[:, :QBLK], out[:, QBLK:]], axis=0)
            o_ref[here, pair * LANES : (pair + 1) * LANES] = both.T.astype(BF16)
        return carry

    lax.fori_loop(0, tokens // QBLK, block, 0)


def attend_backward(
    qkv_ref, lse_ref, o_ref, do_ref, fine_cos, fine_sin, coarse_cos, coarse_sin,
    dqkv_ref,
    dq, kt, dk, dv, cos_ref, sin_ref,
):
    fill_rotary(fine_cos, fine_sin, coarse_cos, coarse_sin, cos_ref, sin_ref)
    tokens, query_width = o_ref.shape
    pairs = query_width // LANES
    key_lanes = slice(query_width, query_width + LANES)
    value_lanes = slice(query_width + LANES, query_width + 2 * LANES)

    def turn_keys(i, carry):
        rows = pl.ds(pl.multiple_of(i * QBLK, QBLK), QBLK)
        kt[:, rows] = qkv_ref[rows, key_lanes].astype(F32).T[:HEAD_SIZE, :].astype(BF16)
        return carry

    lax.fori_loop(0, tokens // QBLK, turn_keys, 0)
    dk[...] = jnp.zeros_like(dk)
    dv[...] = jnp.zeros_like(dv)
    low_lanes = iota((QBLK, LANES), 1) < HEAD_SIZE
    wide = (QBLK, 2 * QBLK)
    visible = iota(wide, 0) <= iota(wide, 1) % QBLK
    ones = jnp.ones((EDGE, LANES), BF16)

    def block(i, carry):
        here = pl.ds(pl.multiple_of(i * QBLK, QBLK), QBLK)
        queries, grads, inners, lses = [], [], [], []
        for pair in range(pairs):
            lanes = slice(pair * LANES, (pair + 1) * LANES)
            queries.append(pair_split(qkv_ref[here, lanes], low_lanes))
            grad = do_ref[here, lanes]
            grads.append(pair_split(grad, low_lanes))
            both = pair_split(grad.astype(F32) * o_ref[here, lanes].astype(F32), low_lanes)
            high, low = parts(both, 2)
            inners.append((dot(ones, high, NT) + dot(ones, low, NT))[:1])
            lses.append(
                jnp.concatenate(
                    [
                        lse_ref[2 * pair : 2 * pair + 1, here],
                        lse_ref[2 * pair + 1 : 2 * pair + 2, here],
                    ],
                    axis=1,
                )
            )
        query_all = jnp.concatenate(queries, axis=0)
        grad_all = jnp.concatenate(grads, axis=0)

        def tile(there, state, edge):
            keys = qkv_ref[there, key_lanes]
            values = qkv_ref[there, value_lanes]
            all_probs, all_dscores, result = [], [], []
            for pair in range(pairs):
                probs = dot(keys, queries[pair], NT) - lses[pair]
                if edge:
                    probs = jnp.where(visible, probs, MASKED)
                probs = jnp.exp(probs)
                dprobs = dot(values, grads[pair], NT)
                dscores = (probs * (dprobs - inners[pair])).astype(BF16)
                all_probs.append(probs.astype(BF16))
                all_dscores.append(dscores)
                result.append(state[pair] + dot(kt[:, there], dscores))
            dv[there, :] += dot(jnp.concatenate(all_probs, axis=1), grad_all)
            dk[there, :] += dot(jnp.concatenate(all_dscores, axis=1), query_all)
            return tuple(result)

        state = (jnp.zeros((HEAD_SIZE, 2 * QBLK), F32),) * pairs
        state = lax.fori_loop(
            0,
            i,
            lambda j, state: tile(pl.ds(pl.multiple_of(j * QBLK, QBLK), QBLK), state, False),
            state,
        )
        state = tile(here, state, True)
        for pair in range(pairs):
            both = jnp.concatenate([state[pair][:, :QBLK], state[pair][:, QBLK:]], axis=0)
            dq[here, pair * LANES : (pair + 1) * LANES] = both.T
        return carry

    lax.fori_loop(0, tokens // QBLK, block, 0)
    masks = head_masks()
    within, (fold, fold_turn, fold_value) = masks[0], masks[4:]

    def turn_back(i, carry):
        rows = pl.ds(pl.multiple_of(i * QBLK, QBLK), QBLK)
        cosine, sine = cos_ref[rows, :], sin_ref[rows, :]
        for pair in range(pairs):
            lanes = slice(pair * LANES, (pair + 1) * LANES)
            grad = dq[rows, lanes]
            grad = grad * cosine - pick(grad, within) * sine
            dqkv_ref[rows, lanes] = (grad * HEAD_SIZE**-0.5).astype(BF16)
        grad = dk[rows, :]
        grad = pick(grad, fold) * cosine - pick(grad, fold_turn) * sine
        grad = grad + pick(dv[rows, :], fold_value)
        dqkv_ref[rows, query_width:] = grad.astype(BF16)
        return carry

    lax.fori_loop(0, tokens // QBLK, turn_back, 0)


def run_attend_forward(proj, query_at, query_width, tables):
    tokens = proj.shape[0]
    cols = lambda size, at: pl.BlockSpec((tokens, size), lambda turn: (0, at // size))
    return pl.pallas_call(
        attend_forward,
        grid=(1,),
        out_shape=(
            jax.ShapeDtypeStruct((tokens, query_width + 2 * LANES), BF16),
            jax.ShapeDtypeStruct((EDGE, tokens), F32),
            jax.ShapeDtypeStruct((tokens, query_width), BF16),
        ),
        in_specs=[
            cols(query_width, query_at),
            cols(2 * HEAD_SIZE, query_at + query_width),
        ]
        + [whole_spec(table) for table in tables],
        out_specs=(
            cols(query_width + 2 * LANES, 0),
            pl.BlockSpec((EDGE, tokens), lambda turn: (0, 0)),
            cols(query_width, 0),
        ),
        scratch_shapes=[
            pltpu.VMEM((HEAD_SIZE, tokens), BF16),
            pltpu.VMEM((tokens, LANES), F32),
            pltpu.VMEM((tokens, LANES), F32),
        ],
        cost_estimate=cost(15),
        name="attend_forward",
    )(proj, proj, *tables)


def run_attend_backward(qkv, lse, attended, grads, grad_at, tables):
    tokens, query_width = attended.shape
    vmem = pl.BlockSpec(memory_space=pltpu.VMEM)
    cols = lambda size, at: pl.BlockSpec((tokens, size), lambda turn: (0, at // size))
    return pl.pallas_call(
        attend_backward,
        grid=(1,),
        out_shape=jax.ShapeDtypeStruct((tokens, query_width + 2 * HEAD_SIZE), BF16),
        in_specs=[
            whole_spec(qkv),
            whole_spec(lse),
            whole_spec(attended),
            cols(query_width, grad_at),
        ]
        + [whole_spec(table) for table in tables],
        out_specs=cols(query_width + 2 * HEAD_SIZE, 0),
        scratch_shapes=[
            pltpu.VMEM((tokens, query_width), F32),
            pltpu.VMEM((HEAD_SIZE, tokens), BF16),
            pltpu.VMEM((tokens, LANES), F32),
            pltpu.VMEM((tokens, LANES), F32),
            pltpu.VMEM((tokens, LANES), F32),
            pltpu.VMEM((tokens, LANES), F32),
        ],
        cost_estimate=cost(16),
        name="attend_backward",
    )(qkv, lse, attended, grads, *tables)


def feed_forward(
    x_ref, mixed_ref, other_ref, act_grad_ref, norms_ref, gu_ref,
    after_ref, scale_ref, hidden_ref, act_ref, dgu_ref, back_ref,
):
    units = act_grad_ref.shape[1]
    after = x_ref[...].astype(F32) + (mixed_ref[...].astype(F32) + other_ref[...].astype(F32))
    after_ref[...] = after.astype(BF16)
    scale = lax.rsqrt(jnp.mean(after * after, axis=-1, keepdims=True) + EPSILON)
    scale_ref[...] = scale
    hidden = (after * scale * norms_ref[1:2, :]).astype(BF16)
    hidden_ref[...] = hidden
    for start in range(0, units, UBLK):
        cols = slice(start, start + UBLK)
        up_cols = slice(units + start, units + start + UBLK)
        gate = dot(hidden, gu_ref[:, cols])
        upward = dot(hidden, gu_ref[:, up_cols])
        grad = act_grad_ref[:, cols]
        sigma = jax.nn.sigmoid(gate)
        swish = gate * sigma
        act_ref[:, cols] = (swish * upward).astype(BF16)
        slope = sigma * (1.0 + gate * (1.0 - sigma))
        dgu_ref[:, cols] = (grad * upward * slope).astype(BF16)
        dgu_ref[:, up_cols] = (grad * swish).astype(BF16)
    back_ref[...] = dot(dgu_ref[...], gu_ref[...], NT).astype(BF16)


def product_rows(dims, left_ref, right_ref, out_ref):
    out_ref[...] = dot(left_ref[...], right_ref[...], dims).astype(out_ref.dtype)


def run_product(left, right, dims, dtype):
    tokens, depth = left.shape
    cols = right.shape[1 - dims[1][0]]
    return pl.pallas_call(
        functools.partial(product_rows, dims),
        grid=(tokens // TBLK,),
        out_shape=jax.ShapeDtypeStruct((tokens, cols), dtype),
        in_specs=[pl.BlockSpec((TBLK, depth), lambda turn: (turn, 0)), once(right)],
        out_specs=pl.BlockSpec((TBLK, cols), lambda turn: (turn, 0)),
        cost_estimate=cost(4),
        name="product_rows",
    )(left, right)


def project(heads, x_ref, w_ref, hidden_ref, proj_ref, norms_ref):
    @pl.when(pl.program_id(0) == 0)
    def _():
        gains = w_ref[:, w_ref.shape[1] - LANES :].astype(F32).T
        norms_ref[...] = jnp.zeros_like(norms_ref)
        norms_ref[0:2, :] = gains[heads : heads + 2, :]

    x = x_ref[...].astype(F32)
    scale = lax.rsqrt(jnp.mean(x * x, axis=-1, keepdims=True) + EPSILON)
    hidden = (x * scale * norms_ref[0:1, :]).astype(BF16)
    hidden_ref[...] = hidden
    proj_ref[...] = dot(hidden, w_ref[...])


def run_project(x, w_in, heads):
    tokens, width = x.shape
    cols = w_in.shape[1]
    rows = lambda size: pl.BlockSpec((TBLK, size), lambda turn: (turn, 0))
    return pl.pallas_call(
        functools.partial(project, heads),
        grid=(tokens // TBLK,),
        out_shape=(
            jax.ShapeDtypeStruct((tokens, width), BF16),
            jax.ShapeDtypeStruct((tokens, cols), F32),
            jax.ShapeDtypeStruct((EDGE, width), F32),
        ),
        in_specs=[rows(width), once(w_in)],
        out_specs=(
            rows(width), rows(cols), pl.BlockSpec((EDGE, width), lambda turn: (0, 0)),
        ),
        cost_estimate=cost(8),
        name="project",
    )(x, w_in)


def project_back(grad_ref, w_ref, x_ref, part_ref, gain_grad_ref):
    @pl.when(pl.program_id(0) == 0)
    def _():
        gain_grad_ref[...] = jnp.zeros_like(gain_grad_ref)

    x = x_ref[...].astype(F32)
    normed = x * lax.rsqrt(jnp.mean(x * x, axis=-1, keepdims=True) + EPSILON)
    part = dot(grad_ref[...], w_ref[...], NT).astype(BF16)
    part_ref[...] = part
    gain_grad_ref[:1, :] += jnp.sum(part.astype(F32) * normed, axis=0, keepdims=True)


def run_project_back(grads, w_in, x):
    tokens, width = x.shape
    cols = w_in.shape[1]
    rows = lambda size: pl.BlockSpec((TBLK, size), lambda turn: (turn, 0))
    return pl.pallas_call(
        project_back,
        grid=(tokens // TBLK,),
        out_shape=(
            jax.ShapeDtypeStruct((tokens, width), BF16),
            jax.ShapeDtypeStruct((EDGE, width), F32),
        ),
        in_specs=[rows(cols), once(w_in), rows(width)],
        out_specs=(rows(width), pl.BlockSpec((EDGE, width), lambda turn: (0, 0))),
        cost_estimate=cost(8),
        name="project_back",
    )(grads, w_in, x)


def once(item):
    return pl.BlockSpec(item.shape, lambda turn: (0,) * item.ndim, pipeline_mode=pl.Buffered(1))


def run_feed_forward(x, mixed, other, act_grad, norms, w_gate_up):
    tokens, width = x.shape
    units = act_grad.shape[1]
    rows = lambda size: pl.BlockSpec((TBLK, size), lambda turn: (turn, 0))
    shape = jax.ShapeDtypeStruct
    return pl.pallas_call(
        feed_forward,
        grid=(tokens // TBLK,),
        out_shape=(
            shape((tokens, width), BF16),
            shape((tokens, 1), F32),
            shape((tokens, width), BF16),
            shape((tokens, units), BF16),
            shape((tokens, 2 * units), BF16),
            shape((tokens, width), BF16),
        ),
        in_specs=[rows(width)] * 3 + [rows(units), once(norms), once(w_gate_up)],
        out_specs=(rows(width), rows(1), rows(width), rows(units), rows(2 * units), rows(width)),
        cost_estimate=cost(14),
        name="feed_forward",
    )(x, mixed, other, act_grad, norms, w_gate_up)


def mixer_forward(gated_ref, scale_ref, gain_ref, attended_ref, w_ref, low_ref, mixed_ref):
    channels = gated_ref.shape[1]
    scale = scale_ref[...].T[:, :1]
    low_ref[:, :channels] = (gated_ref[...].astype(F32) * scale * gain_ref[...]).astype(BF16)
    low_ref[:, channels:] = attended_ref[...]
    mixed_ref[...] = dot(low_ref[...], w_ref[...], NT).astype(BF16)


def run_mixer_forward(gated, scale, gain, attended, w_out):
    tokens, channels = gated.shape
    width, inner = w_out.shape
    rows = lambda size: pl.BlockSpec((TBLK, size), lambda turn: (turn, 0))
    return pl.pallas_call(
        mixer_forward,
        grid=(tokens // TBLK,),
        out_shape=(
            jax.ShapeDtypeStruct((tokens, inner), BF16),
            jax.ShapeDtypeStruct((tokens, width), BF16),
        ),
        in_specs=[
            rows(channels),
            pl.BlockSpec((EDGE, TBLK), lambda turn: (0, turn)),
            once(gain),
            rows(attended.shape[1]),
            once(w_out),
        ],
        out_specs=(rows(inner), rows(width)),
        cost_estimate=cost(5),
        name="mixer_forward",
    )(gated, scale, gain, attended, w_out)


def mixer_backward(
    part_ref, other_ref, after_ref, scale_ref, top_ref, norms_ref,
    w_ref, gated_ref, scale_m_ref, gain_m_ref,
    low_ref, mamba_ref, attended_ref, inner_ref, gain_grad_ref,
):
    channels = gated_ref.shape[1]

    @pl.when(pl.program_id(0) == 0)
    def _():
        gain_grad_ref[...] = jnp.zeros_like(gain_grad_ref)

    grad = part_ref[...].astype(F32) + other_ref[...].astype(F32)
    scale = scale_ref[...]
    normed = after_ref[...].astype(F32) * scale
    gain_grad_ref[:1, :] += jnp.sum(grad * normed, axis=0, keepdims=True)
    weighted = grad * norms_ref[1:2, :]
    mean = jnp.mean(weighted * normed, axis=-1, keepdims=True)
    total = top_ref[...].astype(F32) + scale * (weighted - normed * mean)
    low_ref[...] = total.astype(BF16)
    back = dot(low_ref[...], w_ref[...])
    mamba = back[:, :channels]
    mamba_ref[...] = mamba
    attended_ref[...] = back[:, channels:].astype(BF16)
    inner_ref[...] = row_sums(mamba * gain_m_ref[...] * gated_ref[...].astype(F32)) * scale_m_ref[...]


def run_mixer_backward(part, other, after, scale, top, norms, w_out, gated, scale_m, gain_m):
    tokens, width = after.shape
    channels = gated.shape[1]
    inner = w_out.shape[1]
    shape = jax.ShapeDtypeStruct
    rows = lambda size: pl.BlockSpec((NBLK, size), lambda turn: (turn, 0))
    lanes = pl.BlockSpec((EDGE, NBLK), lambda turn: (0, turn))
    return pl.pallas_call(
        mixer_backward,
        grid=(tokens // NBLK,),
        out_shape=(
            shape((tokens, width), BF16),
            shape((tokens, channels), F32),
            shape((tokens, inner - channels), BF16),
            shape((EDGE, tokens), F32),
            shape((EDGE, width), F32),
        ),
        in_specs=[rows(width)] * 3
        + [rows(1), rows(width), once(norms), once(w_out), rows(channels), lanes, once(gain_m)],
        out_specs=(
            rows(width), rows(channels), rows(inner - channels), lanes,
            pl.BlockSpec((EDGE, width), lambda turn: (0, 0)),
        ),
        cost_estimate=cost(8),
        name="mixer_backward",
    )(part, other, after, scale, top, norms, w_out, gated, scale_m, gain_m)


def lane_row(ref, first, count):
    return jnp.concatenate([ref[i : i + 1, :] for i in range(first, first + count)], axis=1)


def own_lanes(ref, first, size):
    start = lax.axis_index("dp") * size
    row = ref[pl.ds(first + lax.div(start, LANES), 1), :]
    row = jnp.broadcast_to(row, (EDGE, LANES))
    return pltpu.roll(row, lax.rem(LANES - lax.rem(start, LANES), LANES), 1)[0, :size]


def finish_layer(
    norm_at, x_ref, norms_ref, part_ref, other_ref, grad_ref, after_ref, ffn_ref, ffn_other_ref,
    total_ref, *refs,
):
    count = (len(refs) - 9) // 2
    passed, out_ref, result_ref, handed = refs[:count], refs[count], refs[count + 1], refs[count + 2 :]
    tap_ref, bias_ref, gain_ref, step_ref, log_ref, skip_ref, norm_ref = handed[count:]

    @pl.when(pl.program_id(0) == 0)
    def _():
        for source, target in zip(passed, handed):
            target[...] = source[...]
        rows = tap_ref.shape[1] // LANES
        for tap in range(KCONV):
            tap_ref[tap : tap + 1, :] = lane_row(total_ref, tap * rows, rows)
        bias_ref[...] = lane_row(total_ref, KCONV * rows, rows)[0]
        gain_ref[...] = lane_row(total_ref, (KCONV + 1) * rows, rows)[0]
        at = (KCONV + 2) * rows
        for place, ref in enumerate((step_ref, log_ref, skip_ref)):
            ref[...] = total_ref[at + place : at + place + 1, :][0, : ref.shape[0]]
        norm_ref[...] = own_lanes(total_ref, norm_at, norm_ref.shape[0])

    x = x_ref[...].astype(F32)
    scale = lax.rsqrt(jnp.mean(x * x, axis=-1, keepdims=True) + EPSILON)
    normed = x * scale
    weighted = (part_ref[...].astype(F32) + other_ref[...].astype(F32)) * norms_ref[0:1, :]
    mean = jnp.mean(weighted * normed, axis=-1, keepdims=True)
    out_ref[...] = grad_ref[...].astype(F32) + scale * (weighted - normed * mean)
    ffn = ffn_ref[...].astype(F32) + ffn_other_ref[...].astype(F32)
    result_ref[...] = (after_ref[...].astype(F32) + ffn).astype(BF16)


def run_finish(
    x, norms, part, other, grad, after, ffn, ffn_other, total, passed, channels, heads, shard,
    norm_at,
):
    tokens, width = x.shape
    rows = pl.BlockSpec((TBLK, width), lambda turn: (turn, 0))
    shape = lambda *sizes: jax.ShapeDtypeStruct(sizes, F32)
    small = (
        shape(KCONV, channels), shape(channels), shape(channels), shape(heads), shape(heads),
        shape(heads), shape(shard),
    )
    return pl.pallas_call(
        functools.partial(finish_layer, norm_at),
        grid=(tokens // TBLK,),
        out_shape=(shape(tokens, width), jax.ShapeDtypeStruct((tokens, width), BF16))
        + tuple(shape(*item.shape) for item in passed)
        + small,
        in_specs=[rows, once(norms)] + [rows] * 6 + [once(total)] + [once(item) for item in passed],
        out_specs=(rows, rows) + tuple(once(item) for item in passed + small),
        cost_estimate=cost(8),
        name="finish_layer",
    )(x, norms, part, other, grad, after, ffn, ffn_other, total, *passed)


def finish_shared(at, total_ref, cross_ref, mine_ref, other_ref, bc_ref, tap_ref, bias_ref, norm_ref, both):
    half = lax.axis_index("tensor")
    cols = pl.ds(pl.multiple_of(half * LANES, LANES), LANES)
    bc_ref[...] = mine_ref[:, cols] + other_ref[:, cols]
    both[...] = total_ref[...] + cross_ref[...]
    for tap in range(KCONV):
        tap_ref[tap : tap + 1, :] = both[pl.ds(at + 2 * tap + half, 1), :]
    bias_ref[...] = both[pl.ds(at + 2 * KCONV + half, 1), :][0]
    norm_ref[...] = own_lanes(both, at + 2 * KCONV + 2, norm_ref.shape[0])


def run_finish_shared(total, cross, mine, other, shard, at):
    vmem = pl.BlockSpec(memory_space=pltpu.VMEM)
    shape = lambda *sizes: jax.ShapeDtypeStruct(sizes, F32)
    return pl.pallas_call(
        functools.partial(finish_shared, at),
        out_shape=(shape(mine.shape[0], LANES), shape(KCONV, LANES), shape(LANES), shape(shard)),
        in_specs=[vmem] * 4,
        out_specs=(vmem,) * 4,
        scratch_shapes=[pltpu.VMEM(total.shape, F32)],
        name="finish_shared",
    )(total, cross, mine, other)


def swap(partial):
    return lax.ppermute(partial, "tensor", [(0, 1), (1, 0)])


def join(mine, other):
    return mine.astype(F32) + other.astype(F32)


def tensor_sum(partial):
    return join(partial, swap(partial))


def thirds(size):
    part = size // 3
    return [(0, part), (part, 2 * part), (2 * part, size)]


def local(
    layer_input, w_norm1, w_zx, w_bc, w_dt, conv_x, conv_xb, conv_bc, conv_bcb, dt_bias, a_log,
    d_skip, w_mnorm, w_mout, query_key_value_weight, output_weight, w_norm2, w_gu, w_down,
    grad_output,
):
    devices = lax.axis_size("dp")
    tokens, width = layer_input.shape
    shard = w_zx.shape[0]
    channels = conv_xb.shape[0]
    heads = dt_bias.shape[0]
    qkv_width = query_key_value_weight.shape[2]
    units = w_down.shape[0]
    attn_width = output_weight.shape[1]
    tail = jnp.concatenate(
        [w_dt, w_norm1[:, None], w_norm2[:, None], jnp.zeros((shard, LANES - heads - 2), BF16)],
        axis=1,
    )
    mixer_in = jnp.concatenate(
        [w_zx.reshape(shard, -1), w_bc, query_key_value_weight.reshape(shard, -1), tail], axis=1
    )
    in_width = mixer_in.shape[1]
    (w_in,) = gather_rows([mixer_in], devices, 0, [(0, *window) for window in thirds(in_width)])
    w_in, *small_params = lax.optimization_barrier(
        (w_in, conv_x, conv_xb, conv_bc, conv_bcb, dt_bias, a_log, d_skip, w_mnorm)
    )
    params = scan_params(*small_params)
    hidden_one, proj, norms = run_project(layer_input, w_in, heads)
    out_shard = jnp.concatenate([w_mout.T, output_weight.reshape(attn_width, -1).T], axis=1)
    y, gated, square_sum, entering, w_out = run_scan_forward(
        proj, qkv_width, params, out_shard, devices
    )
    channels_all = channels * lax.axis_size("tensor")
    scale_m = lax.rsqrt(tensor_sum(square_sum) / channels_all + EPSILON)
    tables = rotary_tables(tokens)
    qkv_at = 2 * channels + 2 * NS
    qkv, lse, attended = run_attend_forward(proj, qkv_at, attn_width, tables)
    gain_m = w_mnorm.astype(F32)[None, :]
    mixer_out, mixed = run_mixer_forward(gated, scale_m, gain_m, attended, w_out)
    mixed, gate_up_shard, down_shard = lax.optimization_barrier(
        (mixed, w_gu.reshape(shard, -1), w_down.T)
    )
    other = swap(mixed)
    w_gate_up, w_down_t = gather_rows(
        [gate_up_shard, down_shard],
        devices,
        3,
        [(0, 0, units), (0, units, 2 * units), (1, 0, units)],
    )
    act_grad = run_product(grad_output, w_down_t, NN, F32)
    other, w_gate_up, w_down_t, act_grad = lax.optimization_barrier(
        (other, w_gate_up, w_down_t, act_grad)
    )
    after, scale_two, hidden_two, activated, grad_gu_low, partial_two = run_feed_forward(
        layer_input, mixed, other, act_grad, norms, w_gate_up
    )
    other = swap(partial_two)
    grad_down = dot(grad_output, activated, TN).astype(BF16)
    (mine_gu,) = scatter_product(
        hidden_two,
        grad_gu_low,
        [
            ([(0, 1, 0, units)], [(0, 0, units, 0, 0)]),
            ([(0, 1, units, 2 * units)], [(0, 0, units, 0, 1)]),
        ],
        [(shard, 2, units)],
        devices,
        1,
    )
    ffn_part = run_product(activated, w_down_t, NT, BF16)
    other, mine_gu, grad_down, ffn_part = lax.optimization_barrier(
        (other, mine_gu, grad_down, ffn_part)
    )
    ffn_other = swap(ffn_part)
    grad_mix_low, grad_mamba, grad_attended, inner_m, grad_norm2 = run_mixer_backward(
        partial_two, other, after, scale_two, grad_output, norms, w_out, gated, scale_m, gain_m
    )
    inner_m = tensor_sum(inner_m) / channels_all
    dqkv = run_attend_backward(qkv, lse, attended, grad_attended, 0, tables)
    grad_out = dot(grad_mix_low, mixer_out, TN).astype(BF16)
    windows = [(0, None, 0, channels + attn_width), (1, None, 0, units)]
    pieces = [
        (0, 0, channels, 0, None),
        (0, channels, channels + attn_width, 1, None),
        (1, 0, units, 2, None),
    ]
    shapes = [(shard, channels), (shard, attn_width), (shard, units)]
    grad_proj, small_x, small_h, mine_mout, mine_o, mine_down = run_scan_backward(
        proj, y, entering, grad_mamba, scale_m, inner_m, dqkv, params,
        [grad_out, grad_down], windows, pieces, shapes, devices,
    )
    ffn_other, grad_proj = lax.optimization_barrier((ffn_other, grad_proj))
    partial_one, grad_norm1 = run_project_back(grad_proj, w_in, layer_input)
    partial_one, grad_proj = lax.optimization_barrier((partial_one, grad_proj))
    other = swap(partial_one)
    lanes_of = lambda size, start=0: range(start, start + size, LANES)
    places = [(0, row, lane) for row in range(KCONV + 2) for lane in lanes_of(channels)]
    places += [(1, row, 0) for row in range(3)]
    norm_at = len(places)
    places += [(2, 0, lane) for lane in lanes_of(width)]
    cross_at = len(places)
    places += [(0, row, lane) for row in range(KCONV + 1) for lane in lanes_of(2 * NS, channels)]
    places += [(3, 0, lane) for lane in lanes_of(width)]
    shared_at = 2 * channels
    step_at = qkv_at + qkv_width
    mine_zx, mine_bc, mine_qkv, mine_step, small = scatter_product(
        hidden_one,
        grad_proj,
        [
            ([(0, 1, 0, channels)], [(0, 0, channels, 0, 0)]),
            ([(0, 1, channels, shared_at)], [(0, 0, channels, 0, 1)]),
            (
                [(0, 1, shared_at, in_width)],
                [
                    (0, 0, 2 * NS, 1, None),
                    (0, 2 * NS, 2 * NS + qkv_width, 2, 0),
                    (0, 2 * NS + qkv_width, in_width - shared_at, 3, "turned"),
                ],
            ),
        ],
        [
            (shard, 2, channels),
            (shard, 2 * NS),
            (shard, 1, qkv_width),
            (heads, shard),
        ],
        devices,
        5,
        (small_x, small_h, grad_norm2, grad_norm1),
        places,
    )
    other, mine_bc = lax.optimization_barrier((other, mine_bc))
    passed = (mine_zx, mine_qkv, mine_step, mine_mout, mine_o, mine_gu, mine_down)
    cross, other_bc = swap(small), swap(mine_bc)
    grad_source, result, *rest = run_finish(
        layer_input, norms, partial_one, other, grad_mix_low, after, ffn_part, ffn_other, small,
        passed, channels, heads, shard, norm_at,
    )
    mine_zx, mine_qkv, mine_step, mine_mout, mine_o, mine_gu, mine_down = rest[: len(passed)]
    grad_taps, grad_bias, grad_gain, grad_steps, grad_log, grad_skip, own_norm2 = rest[len(passed) :]
    grad_bc, grad_tapsb, grad_biasb, own_norm1 = run_finish_shared(
        small, cross, mine_bc, other_bc, shard, cross_at
    )
    return (
        result,
        grad_source,
        own_norm1,
        mine_zx,
        grad_bc,
        mine_step.T,
        grad_taps,
        grad_bias,
        grad_tapsb,
        grad_biasb,
        grad_steps,
        grad_log,
        grad_skip,
        grad_gain,
        mine_mout.T,
        mine_qkv,
        mine_o.T.reshape(output_weight.shape),
        own_norm2,
        mine_gu,
        mine_down.T,
    )


def solution(mesh):
    return jax.shard_map(
        local,
        mesh=mesh,
        in_specs=(
            P("dp", None),
            P("dp"),
            P("dp", None, "tensor"),
            P("dp", None),
            P("dp", "tensor"),
            P(None, "tensor"),
            P("tensor"),
            P(),
            P(),
            P("tensor"),
            P("tensor"),
            P("tensor"),
            P("tensor"),
            P("tensor", "dp"),
            P("dp", "tensor", None),
            P("tensor", None, "dp"),
            P("dp"),
            P("dp", None, "tensor"),
            P("tensor", "dp"),
            P("dp", None),
        ),
        out_specs=(
            P("dp", None),
            P("dp", None),
            P("dp"),
            P("dp", None, "tensor"),
            P("dp", "tensor"),
            P("dp", "tensor"),
            P(None, "tensor"),
            P("tensor"),
            P(None, "tensor"),
            P("tensor"),
            P("tensor"),
            P("tensor"),
            P("tensor"),
            P("tensor"),
            P("tensor", "dp"),
            P("dp", "tensor", None),
            P("tensor", None, "dp"),
            P("dp"),
            P("dp", None, "tensor"),
            P("tensor", "dp"),
        ),
        check_vma=False,
    )
```

```python
import functools
import math

import jax
import jax.numpy as jnp
import numpy as np
from jax import lax
from jax.experimental import pallas as pl
from jax.experimental.pallas import tpu as pltpu
from jax.sharding import PartitionSpec as P

HEAD_SIZE = 64
MP = 64
NS = 128
KCONV = 4
SPAN = 128
QBLK = 256
FINE = 32
TBLK = 256
NBLK = 128
UBLK = 256
LANES = 128
EDGE = 8

EPSILON = 1e-05
HIGHEST = lax.Precision.HIGHEST
LOG_BASE = math.log(100000000000.0)
MASKED = -1e30
MESH = pl.DeviceIdType.MESH
F32 = jnp.float32
BF16 = jnp.bfloat16

NN = ((1,), (0,))
NT = ((1,), (1,))
TN = ((0,), (0,))


def dot(left, right, dims=NN, precision=None):
    return lax.dot_general(
        left, right, (dims, ((), ())), preferred_element_type=F32, precision=precision
    )


def iota(shape, dim):
    return lax.broadcasted_iota(jnp.int32, shape, dim)


def ring_place(chip, chips):
    odd = lax.rem(chip, 2)
    half = lax.div(chip, 2)
    return (1 - odd) * half + odd * (chips - 1 - half)


def ring_chip(place, chips):
    place = lax.rem(place + 4 * chips, chips)
    back = lax.div(place, chips // 2)
    return (1 - back) * (2 * place) + back * (2 * (chips - 1 - place) + 1)


def ring_setup(chips):
    me = lax.axis_index("dp")
    group = lax.axis_index("tensor")
    chip = lax.div(me, 2)
    core = lax.rem(me, 2)
    place = ring_place(chip, chips)
    right = ring_chip(place + 1, chips) * 2 + core
    left = ring_chip(place - 1, chips) * 2 + core
    mate = chip * 2 + (1 - core)
    barrier = pltpu.get_barrier_semaphore()
    for other in (right, left, mate):
        pl.semaphore_signal(barrier, inc=1, device_id=(other, group), device_id_type=MESH)
    pl.semaphore_wait(barrier, 3)
    return me, group, core, place, right, left, mate


class RingGather:
    def __init__(self, devices, x_ref, o_ref, sems, cols=slice(None)):
        self.cols = cols
        self.chips = devices // 2
        self.ahead = self.chips // 2
        self.behind = self.chips - 1 - self.ahead
        self.x_ref, self.o_ref, self.rows = x_ref, o_ref, x_ref.shape[0]
        self.fs, self.fr, self.bs, self.br, self.cs, self.cr, self.own_sem = sems

    def locate(self):
        me = lax.axis_index("dp")
        self.group = lax.axis_index("tensor")
        self.core = lax.rem(me, 2)
        chip = lax.div(me, 2)
        self.place = ring_place(chip, self.chips)
        self.right = ring_chip(self.place + 1, self.chips) * 2 + self.core
        self.left = ring_chip(self.place - 1, self.chips) * 2 + self.core
        self.mate = chip * 2 + (1 - self.core)
        self.me = me

    def slot(self, index):
        rows = pl.ds(pl.multiple_of(index * self.rows, self.rows), self.rows)
        return self.o_ref.at[rows, self.cols]

    def copy(self, shift, ssem, rsem, target):
        if shift == 0:
            index, source = self.me, self.x_ref.at[:, self.cols]
        else:
            index = ring_chip(self.place + shift, self.chips) * 2 + self.core
            source = self.slot(index)
        return pltpu.make_async_remote_copy(
            src_ref=source,
            dst_ref=self.slot(index),
            send_sem=ssem,
            recv_sem=rsem,
            device_id=(target, self.group),
            device_id_type=MESH,
        )

    def fore(self, step):
        return self.copy(-step, self.fs.at[step], self.fr.at[step], self.right)

    def back(self, step):
        return self.copy(step, self.bs.at[step], self.br.at[step], self.left)

    def across(self, shift):
        number = 0 if shift == 0 else 2 * abs(shift) - (1 if shift < 0 else 0)
        return self.copy(shift, self.cs.at[number], self.cr.at[number], self.mate)

    def own(self):
        return pltpu.make_async_copy(
            self.x_ref.at[:, self.cols], self.slot(self.me), self.own_sem
        )

    def greet(self):
        self.locate()
        barrier = pltpu.get_barrier_semaphore()
        for other in (self.right, self.left, self.mate):
            pl.semaphore_signal(
                barrier, inc=1, device_id=(other, self.group), device_id_type=MESH
            )
        pl.semaphore_wait(barrier, 3)

    def begin(self):
        self.locate()
        self.fore(0).start()
        self.back(0).start()
        self.across(0).start()
        self.own().start()

    def hop(self, step):
        self.locate()
        self.fore(step - 1).wait_recv()
        if step < self.ahead:
            self.fore(step).start()
        self.across(-step).start()
        if step <= self.behind:
            self.back(step - 1).wait_recv()
            if step < self.behind:
                self.back(step).start()
            self.across(step).start()

    def finish(self):
        self.locate()
        self.own().wait()
        for step in range(self.ahead):
            self.fore(step).wait_send()
        for step in range(self.behind):
            self.back(step).wait_send()
        for shift in range(-self.ahead, self.behind + 1):
            self.across(shift).wait()


def gather_sems(devices):
    dma = pltpu.SemaphoreType.DMA
    return [dma((devices // 2,))] * 6 + [dma(())]


def gather_shape(shard, devices):
    return jax.ShapeDtypeStruct((shard.shape[0] * devices, shard.shape[1]), shard.dtype)


def gather_kernel(devices, count, windows, *refs):
    shards, outs, sems = refs[:count], refs[count : 2 * count], refs[2 * count :]
    each = len(sems) // len(windows)
    rings = [
        RingGather(
            devices, shards[i], outs[i], sems[place * each : (place + 1) * each], slice(first, last)
        )
        for place, (i, first, last) in enumerate(windows)
    ]
    rings[0].greet()
    for ring in rings:
        ring.begin()
    for step in range(1, rings[0].ahead + 1):
        for ring in rings:
            ring.hop(step)
    for ring in rings:
        ring.finish()


def cost(micros):
    return pl.CostEstimate(flops=int(micros * 1e9), bytes_accessed=0, transcendentals=0)


def gather_rows(shards, devices, collective, windows):
    count = len(shards)
    anywhere = pl.BlockSpec(memory_space=pl.ANY)
    return pl.pallas_call(
        functools.partial(gather_kernel, devices, count, windows),
        out_shape=tuple(gather_shape(shard, devices) for shard in shards),
        in_specs=[anywhere] * count,
        out_specs=(anywhere,) * count,
        scratch_shapes=gather_sems(devices) * len(windows),
        compiler_params=pltpu.CompilerParams(collective_id=collective, has_side_effects=True),
        cost_estimate=cost(3),
        name="gather_rows",
    )(*shards)


def scatter_order(chips):
    ahead = chips // 2
    behind = chips - 1 - ahead
    order = []
    for step in range(ahead):
        order.append(-(ahead - step))
        if step < behind:
            order.append(behind - step)
    order.append(0)
    return order


class RingScatter:
    def __init__(self, devices, windows, pieces, operands, outs, scratch):
        self.chips = devices // 2
        self.ahead = self.chips // 2
        self.behind = self.chips - 1 - self.ahead
        self.windows, self.pieces, self.operands, self.outs = windows, pieces, operands, outs
        count = len(windows)
        self.mine, self.boxes, rest = scratch[:count], scratch[count : 2 * count], scratch[2 * count :]
        self.fbox, self.bbox, self.fout, self.bout = rest[:4]
        self.os, self.ms, self.mr, self.fs, self.fr, self.bs, self.br = rest[4:]
        self.rows = self.fbox.shape[1]
        widths = [item.shape[2] for item in self.mine]
        self.cols = [slice(sum(widths[:i]), sum(widths[: i + 1])) for i in range(count)]

    def locate(self):
        me = lax.axis_index("dp")
        self.group = lax.axis_index("tensor")
        self.core = lax.rem(me, 2)
        chip = lax.div(me, 2)
        self.place = ring_place(chip, self.chips)
        self.right = ring_chip(self.place + 1, self.chips) * 2 + self.core
        self.left = ring_chip(self.place - 1, self.chips) * 2 + self.core
        self.mate = chip * 2 + (1 - self.core)

    def greet(self):
        self.locate()
        barrier = pltpu.get_barrier_semaphore()
        for other in (self.right, self.left, self.mate):
            pl.semaphore_signal(
                barrier, inc=1, device_id=(other, self.group), device_id_type=MESH
            )
        pl.semaphore_wait(barrier, 3)

    def product(self, i):
        return self.windows[i][1] is not None

    def shift_of(self, slot):
        step = slot // 2
        odd = slot % 2
        return (1 - odd) * (step - self.ahead) + odd * (self.behind - step)

    def half(self, which):
        return pl.ds(pl.multiple_of(which * self.rows, self.rows), self.rows)

    def block(self, i, slot, which):
        index = ring_chip(self.place + self.shift_of(slot), self.chips) * 2 + which
        left, right, first, last = self.windows[i]
        return self.operands[left].at[self.half(index), first:last]

    def remote(self, source, target_ref, ssem, rsem, target):
        return pltpu.make_async_remote_copy(
            src_ref=source,
            dst_ref=target_ref,
            send_sem=ssem,
            recv_sem=rsem,
            device_id=(target, self.group),
            device_id_type=MESH,
        )

    def across(self, i, slot):
        if self.product(i):
            source = self.mine[i].at[slot, self.half(1 - self.core)]
        else:
            source = self.block(i, slot, 1 - self.core)
        return self.remote(
            source, self.boxes[i].at[slot], self.ms.at[i, slot], self.mr.at[i, slot], self.mate
        )

    def own(self, i, slot):
        return pltpu.make_async_copy(
            self.block(i, slot, self.core), self.mine[i].at[slot], self.os.at[i, slot]
        )

    def fore(self, step):
        return self.remote(
            self.fout.at[step], self.fbox.at[step], self.fs.at[step], self.fr.at[step], self.right
        )

    def back(self, step):
        return self.remote(
            self.bout.at[step], self.bbox.at[step], self.bs.at[step], self.br.at[step], self.left
        )

    def begin(self):
        self.locate()
        for i in range(len(self.windows)):
            if not self.product(i):
                for slot in range(self.chips):
                    self.across(i, slot).start()
                    self.own(i, slot).start()

    def produce(self, slot):
        chip = ring_chip(self.place + self.shift_of(slot), self.chips)
        size = 2 * self.rows
        for i, (left, right, first, last) in enumerate(self.windows):
            if right is None:
                continue
            at = pl.multiple_of(chip * size, size)
            terms = dot(self.operands[left][pl.ds(at, size), :], self.operands[right][:, first:last])
            self.mine[i][slot] = terms.astype(BF16)
            self.across(i, slot).start()

    def local_sum(self, i, slot, cols, others):
        rows = self.half(self.core) if self.product(i) else slice(None)
        total = self.mine[i][slot, rows, cols].astype(F32) + self.boxes[i][slot, :, cols].astype(F32)
        whole = slice(self.cols[i].start + cols.start, self.cols[i].start + cols.stop)
        for ref in others:
            total = total + ref[:, whole].astype(F32)
        return total

    def arrive(self, slot):
        for i in range(len(self.windows)):
            if not self.product(i):
                self.own(i, slot).wait()
            self.across(i, slot).wait_recv()

    def put(self, target, slot, others):
        self.arrive(slot)
        for i, cols in enumerate(self.cols):
            total = self.local_sum(i, slot, slice(0, cols.stop - cols.start), others)
            target[:, cols] = total.astype(BF16)

    def hop_back(self, step, later):
        if later:
            self.back(step - 1).wait_recv()
        self.put(self.bout.at[step], 2 * step, [self.bbox.at[step - 1]] if later else [])
        self.back(step).start()

    def hop_fore(self, step, later):
        if later:
            self.fore(step - 1).wait_recv()
        self.put(self.fout.at[step], 2 * step + 1, [self.fbox.at[step - 1]] if later else [])
        self.fore(step).start()

    def hop(self, step):
        self.locate()
        self.hop_back(step, step > 0)
        if step < self.behind:
            self.hop_fore(step, step > 0)

    def finish(self):
        self.locate()
        slot = self.chips - 1
        self.arrive(slot)
        self.fore(self.behind - 1).wait_recv()
        self.back(self.ahead - 1).wait_recv()
        others = [self.fbox.at[self.behind - 1], self.bbox.at[self.ahead - 1]]
        for i, first, last, out, form in self.pieces:
            total = self.local_sum(i, slot, slice(first, last), others)
            if form == "turned":
                self.outs[out][...] = total.T[: self.outs[out].shape[0]]
            elif form is None:
                self.outs[out][...] = total
            else:
                self.outs[out][:, form, :] = total
        for step in range(self.ahead):
            self.back(step).wait_send()
        for step in range(self.behind):
            self.fore(step).wait_send()
        for slot in range(self.chips):
            for i in range(len(self.windows)):
                self.across(i, slot).wait_send()


def run_rings(rings, after_first=None):
    ahead, behind = rings[0].ahead, rings[0].behind

    def turn(step, carry):
        def part(odd, kept):
            for ring in rings:
                ring.produce(2 * step + odd)
            return kept

        lax.fori_loop(0, 2, part, 0)

        @pl.when(step == 0)
        def _():
            for ring in rings:
                ring.hop_back(0, False)
                ring.hop_fore(0, False)
            if after_first is not None:
                after_first()

        @pl.when(step > 0)
        def _():
            for ring in rings:
                ring.hop_back(step, True)
                pl.when(step < behind)(functools.partial(ring.hop_fore, step, True))

        return carry

    lax.fori_loop(0, ahead, turn, 0)


def scatter_scratch(windows, rows, devices):
    chips = devices // 2
    count = len(windows)
    dma = pltpu.SemaphoreType.DMA
    widths = [last - first for left, right, first, last in windows]
    mine = [
        pltpu.VMEM((chips, rows if right is None else 2 * rows, last - first), BF16)
        for left, right, first, last in windows
    ]
    boxes = [pltpu.VMEM((chips, rows, width), BF16) for width in widths]
    box = pltpu.VMEM((chips // 2, rows, sum(widths)), BF16)
    return mine + boxes + [box] * 4 + [dma((count, chips))] * 3 + [dma((chips,))] * 4


class Total:
    def __init__(self, devices, x_ref, o_ref, scratch):
        self.chips = devices // 2
        self.x_ref, self.o_ref = x_ref, o_ref
        self.mate_box, self.joined, self.boxes, self.ms, self.mr, self.ss, self.sr = scratch
        me = lax.axis_index("dp")
        self.group = lax.axis_index("tensor")
        self.chip = lax.div(me, 2)
        core = lax.rem(me, 2)
        self.mate = self.chip * 2 + (1 - core)
        self.peers = [
            lax.rem(self.chip + shift, self.chips) * 2 + core for shift in range(self.chips)
        ]

    def greet(self):
        barrier = pltpu.get_barrier_semaphore()
        for other in [self.mate] + self.peers[1:]:
            pl.semaphore_signal(
                barrier, inc=1, device_id=(other, self.group), device_id_type=MESH
            )
        pl.semaphore_wait(barrier, self.chips)

    def remote(self, source, target_ref, ssem, rsem, target):
        return pltpu.make_async_remote_copy(
            src_ref=source,
            dst_ref=target_ref,
            send_sem=ssem,
            recv_sem=rsem,
            device_id=(target, self.group),
            device_id_type=MESH,
        )

    def across(self):
        return self.remote(self.x_ref, self.mate_box, self.ms, self.mr, self.mate)

    def copies(self):
        return [
            self.remote(
                self.joined,
                self.boxes.at[self.chip],
                self.ss.at[shift],
                self.sr.at[shift],
                self.peers[shift],
            )
            for shift in range(1, self.chips)
        ]

    def begin(self):
        self.across().start()

    def spread(self):
        self.across().wait_recv()
        self.joined[...] = self.x_ref[...] + self.mate_box[...]
        for copy in self.copies():
            copy.start()
        self.boxes[self.chip] = self.joined[...]

    def finish(self):
        for copy in self.copies():
            copy.wait_recv()
        result = self.boxes[0]
        for other in range(1, self.chips):
            result = result + self.boxes[other]
        self.o_ref[...] = result
        self.across().wait_send()
        for copy in self.copies():
            copy.wait_send()


def total_scratch(values, devices):
    chips = devices // 2
    dma = pltpu.SemaphoreType.DMA
    return [
        pltpu.VMEM(values.shape, F32),
        pltpu.VMEM(values.shape, F32),
        pltpu.VMEM((chips,) + values.shape, F32),
        dma(()),
        dma(()),
        dma((chips,)),
        dma((chips,)),
    ]


def turned_copy(source, target):
    for start in range(0, source.shape[1], LANES):
        target[start : start + LANES, :] = source[:, start : start + LANES].T


def product_kernel(devices, groups, outs, places, summed, left_ref, right_ref, *refs):
    values = refs[:summed]
    refs = refs[summed:]
    pieces_out, refs = refs[:outs], refs[outs:]
    total = None
    if summed:
        total_out, refs = refs[0], refs[1:]
    turned, scratch = refs[0], refs[1:]
    if summed:
        scratch, rest = scratch[:-8], scratch[-8:]
        together = rest[0]
        together[...] = jnp.zeros_like(together)
        for at, (which, row, lane) in enumerate(places):
            together[at : at + 1, :] = values[which][row : row + 1, lane : lane + LANES]
        total = Total(devices, together, total_out, rest[1:])
    each = len(scratch) // len(groups)
    rings = [
        RingScatter(
            devices, windows, pieces, (turned, right_ref), pieces_out,
            scratch[place * each : (place + 1) * each],
        )
        for place, (windows, pieces) in enumerate(groups)
    ]
    if total is None:
        rings[0].greet()
    else:
        total.greet()
        total.begin()
    for ring in rings:
        ring.locate()
    turned_copy(left_ref, turned)
    run_rings(rings, total.spread if total is not None else None)
    for ring in rings:
        ring.finish()
    if total is not None:
        total.finish()


def scatter_product(left, right, groups, shapes, devices, collective, values=(), places=()):
    vmem = pl.BlockSpec(memory_space=pltpu.VMEM)
    rows = left.shape[1] // devices
    scratch = [pltpu.VMEM(left.shape[::-1], BF16)]
    for windows, pieces in groups:
        scratch += scatter_scratch(windows, rows, devices)
    totals = ()
    if values:
        total = jax.ShapeDtypeStruct((len(places) + -len(places) % EDGE, LANES), F32)
        totals = (total,)
        scratch += [pltpu.VMEM(total.shape, F32)] + total_scratch(total, devices)
    return pl.pallas_call(
        functools.partial(
            product_kernel, devices, groups, len(shapes), places, len(values)
        ),
        out_shape=tuple(jax.ShapeDtypeStruct(shape, F32) for shape in shapes) + totals,
        in_specs=[vmem] * (2 + len(values)),
        out_specs=(vmem,) * (len(shapes) + len(totals)),
        scratch_shapes=scratch,
        compiler_params=pltpu.CompilerParams(collective_id=collective, has_side_effects=True),
        cost_estimate=cost(3),
        name="scatter_product",
    )(left, right, *values)


def head_spread(channels):
    return (iota((LANES, channels), 1) // MP == iota((LANES, channels), 0)).astype(BF16)


def parts(values, count):
    terms = []
    for _ in range(count):
        term = values.astype(BF16)
        terms.append(term)
        values = values - term.astype(F32)
    return terms


def pick(values, mask, count=2):
    return dot(jnp.concatenate(parts(values, count), axis=1), jnp.concatenate([mask] * count, axis=0))


def pick_left(mask, values, count):
    return dot(jnp.concatenate([mask] * count, axis=1), jnp.concatenate(parts(values, count), axis=0))


def gather_heads(values, spread):
    high, low = parts(values, 2)
    return dot(high, spread, NT) + dot(low, spread, NT)


def row_sums(values):
    high, low = parts(values, 2)
    ones = jnp.ones((EDGE, values.shape[1]), BF16)
    return dot(ones, high, NT) + dot(ones, low, NT)


def soft_step(raw):
    return jnp.maximum(raw, 0.0) + jnp.log1p(jnp.exp(-jnp.abs(raw)))


def window(buffer, start, span):
    return buffer[start : start + span, :]


def causal_taps(buffer, taps, span):
    total = taps[0:1, :] * window(buffer, EDGE - KCONV + 1, span)
    for tap in range(1, KCONV):
        total = total + taps[tap : tap + 1, :] * window(buffer, EDGE - KCONV + 1 + tap, span)
    return total


def span_rates(step_ref, bias, decay, spread, span):
    raw = step_ref[...] + bias
    step = soft_step(raw)
    lower = (iota((span, span), 1) <= iota((span, span), 0)).astype(BF16)
    cum = pick_left(lower, step * decay, 3)
    tails = jnp.exp(cum[span - 1 : span, :] - cum)
    wide = pick(jnp.concatenate([step, tails, jnp.exp(cum)], axis=0), spread)
    return raw, step, cum, wide[:span], wide[span : 2 * span], wide[2 * span :]


def pair_split(values, low_lanes):
    zero = jnp.zeros_like(values)
    return jnp.concatenate(
        [jnp.where(low_lanes, values, zero), jnp.where(low_lanes, zero, values)], axis=0
    )


def pair_decay(cum, cum_rows, pair, causal):
    parts = []
    for head in (2 * pair, 2 * pair + 1):
        differ = cum[:, head : head + 1] - cum_rows[head : head + 1, :]
        parts.append(jnp.exp(jnp.where(causal, differ, MASKED)))
    return parts


def scan_forward(
    devices, spans,
    z_ref, x_ref, bc_ref, step_ref,
    tap_ref, tapb_ref, row_ref, shard_ref,
    y_ref, gated_ref, square_ref, enter_ref, all_ref,
    state, buffer, *sems,
):
    span, channels = x_ref.shape
    width = shard_ref.shape[1]
    each = len(sems) // 2
    rings = [
        RingGather(devices, shard_ref, all_ref, sems[:each], slice(0, width // 2)),
        RingGather(devices, shard_ref, all_ref, sems[each:], slice(width // 2, width)),
    ]
    turn = pl.program_id(0)

    @pl.when(turn == 0)
    def _():
        rings[0].greet()
        for ring in rings:
            ring.begin()


    @pl.when(pl.program_id(0) == 0)
    def _():
        state[...] = jnp.zeros_like(state)
        buffer[span:, :] = jnp.zeros((EDGE, buffer.shape[1]), F32)

    buffer[:EDGE, :] = buffer[span:, :]
    buffer[EDGE:, :channels] = x_ref[...]
    buffer[EDGE:, channels:] = bc_ref[...]
    spread = head_spread(channels)
    bias, gain, biasb, stepb, decay, skip = unpack_rows(row_ref, spread)
    taps = jnp.concatenate([tap_ref[...], tapb_ref[...]], axis=1).astype(F32)
    conv = causal_taps(buffer, taps, span)
    conv = jax.nn.silu(conv + jnp.concatenate([bias, biasb], axis=1))
    inputs, shared = conv[:, :channels], conv[:, channels:]
    raw, step, cum, step_w, tails_w, grown_w = span_rates(step_ref, stepb, decay, spread, span)
    cum_rows = cum.T
    b_low = shared[:, :NS].astype(BF16)
    c_low = shared[:, NS:].astype(BF16)
    scaled = inputs * step_w
    scaled_low = scaled.astype(BF16)
    enter_ref[0] = state[...]
    outer = dot(c_low, state[...].astype(BF16)) * grown_w
    fresh = dot(b_low, (scaled * tails_w).astype(BF16), TN)
    state[...] = state[...] * grown_w[span - 1 : span, :] + fresh
    cross = dot(c_low, b_low, NT)
    causal = iota((span, span), 1) <= iota((span, span), 0)
    low_lanes = iota((span, LANES), 1) < MP
    for pair in range(channels // LANES):
        lanes = slice(pair * LANES, (pair + 1) * LANES)
        first, second = pair_decay(cum, cum_rows, pair, causal)
        weights = jnp.concatenate(
            [(cross * first).astype(BF16), (cross * second).astype(BF16)], axis=1
        )
        y_ref[:, lanes] = dot(weights, pair_split(scaled_low[:, lanes], low_lanes))
    y = y_ref[...] + outer + skip * inputs
    y_ref[...] = y
    gated = y * jax.nn.silu(z_ref[...])
    gated_ref[...] = gated.astype(BF16)
    square_ref[...] = row_sums(gated * gated)

    ahead = rings[0].ahead
    for step in range(1, ahead + 1):
        after = max(0, spans * step // ahead - (2 if step == ahead else 1))
        for ring in rings:
            pl.when(turn == after)(functools.partial(ring.hop, step))
    for ring in rings:
        pl.when(turn == spans - 1)(ring.finish)


def scan_backward(
    devices, spans, windows, pieces, outs_count, count,
    z_ref, x_ref, xp_ref, bc_ref, bp_ref, step_ref, y_ref, enter_ref,
    dyg_ref, scale_ref, inner_ref, dqkv_ref,
    tap_ref, tapb_ref, row_ref,
    *refs,
):
    sent, refs = refs[:count], refs[count:]
    (grad_ref, gx_ref, gh_ref), refs = refs[:3], refs[3:]
    outs, refs = refs[:outs_count], refs[outs_count:]
    (dstate, buffer, dbuffer, du_buf, col_buf), scratch = refs[:5], refs[5:]
    ring = RingScatter(devices, windows, pieces, sent, outs, scratch)
    span, channels = x_ref.shape
    turn = pl.program_id(0)

    @pl.when(turn == 0)
    def _():
        ring.greet()
        ring.begin()
        dstate[...] = jnp.zeros_like(dstate)
        dbuffer[...] = jnp.zeros_like(dbuffer)
        col_buf[...] = jnp.zeros_like(col_buf)
        gx_ref[...] = jnp.zeros_like(gx_ref)
        gh_ref[...] = jnp.zeros_like(gh_ref)

    inside = (turn < spans - 1).astype(F32)
    buffer[:EDGE, :channels] = xp_ref[...] * inside
    buffer[:EDGE, channels:] = bp_ref[...] * inside
    buffer[EDGE:, :channels] = x_ref[...]
    buffer[EDGE:, channels:] = bc_ref[...]
    spread = head_spread(channels)
    bias, gain, biasb, stepb, decay, skip = unpack_rows(row_ref, spread)
    taps = jnp.concatenate([tap_ref[...], tapb_ref[...]], axis=1).astype(F32)
    conv = causal_taps(buffer, taps, span) + jnp.concatenate([bias, biasb], axis=1)
    sig = jax.nn.sigmoid(conv)
    swished = conv * sig
    inputs, shared = swished[:, :channels], swished[:, channels:]
    b_low = shared[:, :NS].astype(BF16)
    c_low = shared[:, NS:].astype(BF16)
    raw, step, cum, step_w, tails_w, grown_w = span_rates(step_ref, stepb, decay, spread, span)
    cum_rows = cum.T
    scaled = inputs * step_w
    scaled_low = scaled.astype(BF16)

    z = z_ref[...]
    sig_z = jax.nn.sigmoid(z)
    swish = z * sig_z
    y = y_ref[...]
    scale = scale_ref[...].T[:, :1]
    normed = y * swish * scale
    dyg = dyg_ref[...]
    gain_grad = jnp.sum(dyg * normed, axis=0, keepdims=True)
    dgated = scale * (dyg * gain - normed * inner_ref[...].T[:, :1])
    dy = dgated * swish
    grad_ref[:, :channels] = (dgated * y * (sig_z * (1.0 + z * (1.0 - sig_z)))).astype(BF16)

    state_low = enter_ref[0].astype(BF16)
    dstate_low = dstate[...].astype(BF16)
    grown_low = (dy * grown_w).astype(BF16)
    dy_low = dy.astype(BF16)
    tailed = scaled * tails_w
    outer = dot(c_low, state_low) * grown_w
    from_state = dot(b_low, dstate_low)
    dc = dot(grown_low, state_low, NT)
    db = dot(tailed.astype(BF16), dstate_low, NT)
    leak = from_state * tailed
    last_w = grown_w[span - 1 : span, :]
    ends = (
        jnp.sum(leak, axis=0, keepdims=True)
        + jnp.sum(enter_ref[0] * dstate[...], axis=0, keepdims=True) * last_w
    )
    skips = jnp.sum(dy * inputs, axis=0, keepdims=True)
    dstate[...] = dstate[...] * last_w + dot(c_low, grown_low, TN)

    cross = dot(c_low, b_low, NT)
    causal = iota((span, span), 1) <= iota((span, span), 0)
    low_lanes = iota((span, LANES), 1) < MP
    lane = iota((span, LANES), 1)
    dcross = jnp.zeros((span, span), F32)
    row_part = jnp.zeros((span, LANES), F32)
    for pair in range(channels // LANES):
        lanes = slice(pair * LANES, (pair + 1) * LANES)
        decays = pair_decay(cum, cum_rows, pair, causal)
        dy_pair = pair_split(dy_low[:, lanes], low_lanes)
        dweights = dot(dy_pair, scaled_low[:, lanes], NT)
        both = []
        for part in range(2):
            head = 2 * pair + part
            dterm = dweights[part * span : (part + 1) * span] * decays[part]
            dcross = dcross + dterm
            flow = dterm * cross
            row_part = row_part + jnp.where(
                lane == head, jnp.sum(flow, axis=1, keepdims=True), 0.0
            )
            col_buf[head : head + 1, :] = jnp.sum(flow, axis=0, keepdims=True)
            both.append((cross * decays[part]).astype(BF16))
        du_buf[:, lanes] = dot(jnp.concatenate(both, axis=0), dy_pair, TN)
    du = du_buf[...] + from_state * tails_w
    dcross_low = dcross.astype(BF16)
    dc = dc + dot(dcross_low, b_low)
    db = db + dot(dcross_low, c_low, TN)

    sums = gather_heads(
        jnp.concatenate(
            [dy * outer - leak, du * inputs, ends, skips, jnp.zeros((EDGE - 2, channels), F32)],
            axis=0,
        ),
        spread,
    )
    at_end = sums[2 * span : 2 * span + 1, :]
    dcum = sums[:span] + row_part - col_buf[...].T
    upper = (iota((span, span), 1) >= iota((span, span), 0)).astype(BF16)
    drate = pick_left(upper, dcum, 3) + at_end
    dstep = drate * decay + sums[span : 2 * span]
    draw = dstep * jax.nn.sigmoid(raw)
    gh_ref[0:1, :] += jnp.sum(draw, axis=0, keepdims=True)
    gh_ref[1:2, :] += jnp.sum(drate * step, axis=0, keepdims=True) * decay
    gh_ref[2:3, :] += sums[2 * span + 1 : 2 * span + 2, :]

    dinputs = du * step_w + skip * dy
    dconv = jnp.concatenate([dinputs, db, dc], axis=1) * (sig * (1.0 + conv * (1.0 - sig)))
    dbuffer[span:, :] = dbuffer[:EDGE, :]
    dbuffer[:span, :] = dconv
    dbefore = jnp.zeros_like(dconv)
    for tap in range(KCONV):
        dbefore = dbefore + taps[tap : tap + 1, :] * window(dbuffer, KCONV - 1 - tap, span)
        gx_ref[tap : tap + 1, :] += jnp.sum(
            dconv * window(buffer, EDGE - KCONV + 1 + tap, span), axis=0, keepdims=True
        )
    gx_ref[KCONV : KCONV + 1, :] += jnp.sum(dconv, axis=0, keepdims=True)
    gx_ref[KCONV + 1 : KCONV + 2, :channels] += gain_grad
    width = 2 * channels + 2 * NS
    grad_ref[:, channels:width] = dbefore.astype(BF16)
    grad_ref[:, width : width + dqkv_ref.shape[1]] = dqkv_ref[...]
    grad_ref[:, width + dqkv_ref.shape[1] :] = draw.astype(BF16)
    for step in range(ring.ahead):
        pl.when(turn == spans * step // ring.ahead)(functools.partial(ring.hop, step))
    pl.when(turn == spans - 1)(ring.finish)


def scan_params(conv_x, conv_xb, conv_bc, conv_bcb, dt_bias, a_log, d_skip, w_mnorm):
    heads = dt_bias.shape[0]
    fill = jnp.zeros((LANES - heads,), BF16)
    flat = [conv_xb, w_mnorm, conv_bcb, dt_bias, fill, a_log, fill, d_skip, fill]
    size = sum(item.shape[0] for item in flat) // LANES
    flat.append(jnp.zeros((-size % EDGE * LANES,), BF16))
    rows = jnp.concatenate(flat).astype(F32).reshape(-1, LANES)
    return (conv_x, conv_bc, rows)


def unpack_rows(row_ref, spread):
    channels = spread.shape[1]
    count = channels // LANES
    at = 2 * count + 2 * NS // LANES

    def join_rows(first, number):
        return jnp.concatenate(
            [row_ref[i : i + 1, :] for i in range(first, first + number)], axis=1
        )

    skip = jnp.broadcast_to(row_ref[at + 2 : at + 3, :], (EDGE, LANES)).astype(BF16)
    return (
        join_rows(0, count),
        join_rows(count, count),
        join_rows(2 * count, 2 * NS // LANES),
        row_ref[at : at + 1, :],
        -jnp.exp(row_ref[at + 1 : at + 2, :]),
        dot(skip, spread)[:1],
    )


def whole_spec(array):
    return pl.BlockSpec(array.shape, lambda turn: (0,) * array.ndim)


def run_scan_forward(proj, qkv_width, params, shard, devices):
    tokens = proj.shape[0]
    channels = params[0].shape[1]
    step_at = (2 * channels + 2 * NS + qkv_width) // LANES
    spans = tokens // SPAN
    bc_at = 2 * channels // (2 * NS)
    rows = lambda width, at: pl.BlockSpec((SPAN, width), lambda turn: (turn, at))
    anywhere = pl.BlockSpec(memory_space=pl.ANY)
    return pl.pallas_call(
        functools.partial(scan_forward, devices, spans),
        grid=(spans,),
        out_shape=(
            jax.ShapeDtypeStruct((tokens, channels), F32),
            jax.ShapeDtypeStruct((tokens, channels), BF16),
            jax.ShapeDtypeStruct((EDGE, tokens), F32),
            jax.ShapeDtypeStruct((spans, NS, channels), F32),
            gather_shape(shard, devices),
        ),
        in_specs=[rows(channels, 0), rows(channels, 1), rows(2 * NS, bc_at), rows(LANES, step_at)]
        + [whole_spec(item) for item in params]
        + [anywhere],
        out_specs=(
            rows(channels, 0),
            rows(channels, 0),
            pl.BlockSpec((EDGE, SPAN), lambda turn: (0, turn)),
            pl.BlockSpec((1, NS, channels), lambda turn: (turn, 0, 0)),
            anywhere,
        ),
        scratch_shapes=[
            pltpu.VMEM((NS, channels), F32),
            pltpu.VMEM((SPAN + EDGE, channels + 2 * NS), F32),
        ]
        + gather_sems(devices) * 2,
        compiler_params=pltpu.CompilerParams(collective_id=2, has_side_effects=True),
        cost_estimate=cost(20),
        name="scan_forward",
    )(proj, proj, proj, proj, *params, shard)


def run_scan_backward(
    proj, y, entering, dyg, scale, inner, dqkv, params, sent, windows, pieces, shapes,
    devices,
):
    tokens, width = proj.shape
    channels = params[0].shape[1]
    qkv_width = dqkv.shape[1]
    step_at = (2 * channels + 2 * NS + qkv_width) // LANES
    spans = tokens // SPAN
    bc_at = 2 * channels // (2 * NS)
    edges = SPAN // EDGE
    rows = lambda size, at: pl.BlockSpec((SPAN, size), lambda turn: (spans - 1 - turn, at))
    edge = lambda size, at: pl.BlockSpec(
        (EDGE, size), lambda turn: (jnp.maximum((spans - 1 - turn) * edges - 1, 0), at)
    )
    keep = lambda shape: pl.BlockSpec(shape, lambda turn: (0, 0))
    shapes = tuple(jax.ShapeDtypeStruct(shape, F32) for shape in shapes)
    return pl.pallas_call(
        functools.partial(
            scan_backward, devices, spans, windows, pieces, len(shapes), len(sent)
        ),
        grid=(spans,),
        out_shape=(
            jax.ShapeDtypeStruct((tokens, width), BF16),
            jax.ShapeDtypeStruct((EDGE, channels + 2 * NS), F32),
            jax.ShapeDtypeStruct((EDGE, LANES), F32),
        )
        + shapes,
        in_specs=[
            rows(channels, 0),
            rows(channels, 1),
            edge(channels, 1),
            rows(2 * NS, bc_at),
            edge(2 * NS, bc_at),
            rows(LANES, step_at),
            rows(channels, 0),
            pl.BlockSpec((1, NS, channels), lambda turn: (spans - 1 - turn, 0, 0)),
            rows(channels, 0),
            pl.BlockSpec((EDGE, SPAN), lambda turn: (0, spans - 1 - turn)),
            pl.BlockSpec((EDGE, SPAN), lambda turn: (0, spans - 1 - turn)),
            rows(qkv_width, 0),
        ]
        + [whole_spec(item) for item in params]
        + [pl.BlockSpec(memory_space=pl.ANY)] * len(sent),
        out_specs=(
            rows(width, 0),
            keep((EDGE, channels + 2 * NS)),
            keep((EDGE, LANES)),
        )
        + tuple(keep(item.shape) for item in shapes),
        scratch_shapes=[
            pltpu.VMEM((NS, channels), F32),
            pltpu.VMEM((SPAN + EDGE, channels + 2 * NS), F32),
            pltpu.VMEM((SPAN + EDGE, channels + 2 * NS), F32),
            pltpu.VMEM((SPAN, channels), F32),
            pltpu.VMEM((LANES, SPAN), F32),
        ]
        + scatter_scratch(windows, sent[0].shape[0] // devices, devices),
        compiler_params=pltpu.CompilerParams(collective_id=6, has_side_effects=True),
        cost_estimate=cost(47),
        name="scan_backward",
    )(
        proj, proj, proj, proj, proj, proj, y, entering, dyg, scale, inner, dqkv, *params, *sent,
    )


def rotary_tables(tokens):
    half = HEAD_SIZE // 2
    exponent = np.arange(half, dtype=np.float64) * (-2.0 * LOG_BASE / HEAD_SIZE)
    rates = np.tile(np.exp(exponent.astype(np.float32)).astype(np.float64), LANES // half)
    tables = []
    for places in (np.arange(FINE), np.arange(0, tokens, FINE)):
        angles = places[:, None] * rates[None, :]
        tables += [np.cos(angles).astype(np.float32), np.sin(angles).astype(np.float32)]
    return tables


def fill_rotary(fine_cos, fine_sin, coarse_cos, coarse_sin, cosine, sine):
    small_cos, small_sin = fine_cos[...], fine_sin[...]
    for turn in range(coarse_cos.shape[0]):
        big_cos, big_sin = coarse_cos[turn : turn + 1, :], coarse_sin[turn : turn + 1, :]
        rows = slice(turn * FINE, (turn + 1) * FINE)
        cosine[rows, :] = small_cos * big_cos - small_sin * big_sin
        sine[rows, :] = small_sin * big_cos + small_cos * big_sin


def head_masks():
    half = HEAD_SIZE // 2
    row, col = iota((LANES, LANES), 0), iota((LANES, LANES), 1)
    place = col % HEAD_SIZE
    ahead = jnp.where(place < half, -1.0, 0.0)
    behind = jnp.where(place < half, 0.0, 1.0)

    def turn(start):
        return jnp.where(row == start + half, ahead, jnp.where(row == start - half, behind, 0.0))

    first = row < HEAD_SIZE
    left = col < HEAD_SIZE
    low = lambda mask: mask.astype(BF16)
    within = low(turn(col))
    copy = low(jnp.where(row == place, 1.0, 0.0))
    copy_turn = low(jnp.where(first, turn(place), 0.0))
    value = low(jnp.where(row == place + HEAD_SIZE, 1.0, 0.0))
    fold = low(jnp.where(left & (row % HEAD_SIZE == place), 1.0, 0.0))
    other = row % HEAD_SIZE
    fold_turn = low(
        jnp.where(
            left,
            jnp.where(other == place + half, ahead, jnp.where(other == place - half, behind, 0.0)),
            0.0,
        )
    )
    fold_value = low(jnp.where(left, 0.0, jnp.where(other == place, 1.0, 0.0)))
    return within, copy, copy_turn, value, fold, fold_turn, fold_value


def attend_forward(
    q_ref, kv_ref, fine_cos, fine_sin, coarse_cos, coarse_sin,
    qkv_ref, lse_ref, o_ref, vt, cos_ref, sin_ref,
):
    fill_rotary(fine_cos, fine_sin, coarse_cos, coarse_sin, cos_ref, sin_ref)
    tokens, query_width = q_ref.shape
    pairs = query_width // LANES
    within, copy, copy_turn, value = head_masks()[:4]

    def turn_rows(i, carry):
        rows = pl.ds(pl.multiple_of(i * QBLK, QBLK), QBLK)
        cosine, sine = cos_ref[rows, :], sin_ref[rows, :]
        for pair in range(pairs):
            lanes = slice(pair * LANES, (pair + 1) * LANES)
            query = q_ref[rows, lanes]
            turned = query * cosine + pick(query, within) * sine
            qkv_ref[rows, lanes] = (turned * HEAD_SIZE**-0.5).astype(BF16)
        kv = kv_ref[rows, :]
        keys = pick(kv, copy) * cosine + pick(kv, copy_turn) * sine
        qkv_ref[rows, query_width : query_width + LANES] = keys.astype(BF16)
        qkv_ref[rows, query_width + LANES :] = dot(kv.astype(BF16), value).astype(BF16)
        vt[:, rows] = kv.T[HEAD_SIZE:, :].astype(BF16)
        return carry

    lax.fori_loop(0, tokens // QBLK, turn_rows, 0)
    low_lanes = iota((QBLK, LANES), 1) < HEAD_SIZE
    wide = (QBLK, 2 * QBLK)
    visible = iota(wide, 0) <= iota(wide, 1) % QBLK

    def block(i, carry):
        here = pl.ds(pl.multiple_of(i * QBLK, QBLK), QBLK)
        queries = [
            pair_split(qkv_ref[here, pair * LANES : (pair + 1) * LANES], low_lanes)
            for pair in range(pairs)
        ]

        def tile(there, state, edge):
            keys = qkv_ref[there, query_width : query_width + LANES]
            result = []
            for pair in range(pairs):
                top, total, out = state[3 * pair : 3 * pair + 3]
                scores = dot(keys, queries[pair], NT)
                if edge:
                    scores = jnp.where(visible, scores, MASKED)
                higher = jnp.maximum(top, jnp.max(scores, axis=0, keepdims=True))
                probs = jnp.exp(scores - higher)
                fade = jnp.exp(top - higher)
                total = total * fade + jnp.sum(probs, axis=0, keepdims=True)
                out = out * fade + dot(vt[:, there], probs.astype(BF16))
                result += [higher, total, out]
            return tuple(result)

        state = (
            jnp.full((1, 2 * QBLK), MASKED, F32),
            jnp.zeros((1, 2 * QBLK), F32),
            jnp.zeros((HEAD_SIZE, 2 * QBLK), F32),
        ) * pairs
        state = lax.fori_loop(
            0,
            i,
            lambda j, state: tile(pl.ds(pl.multiple_of(j * QBLK, QBLK), QBLK), state, False),
            state,
        )
        state = tile(here, state, True)
        for pair in range(pairs):
            top, total, out = state[3 * pair : 3 * pair + 3]
            out = out / total
            lse = top + jnp.log(total)
            lse_ref[2 * pair : 2 * pair + 1, here] = lse[:, :QBLK]
            lse_ref[2 * pair + 1 : 2 * pair + 2, here] = lse[:, QBLK:]
            both = jnp.concatenate([out[:, :QBLK], out[:, QBLK:]], axis=0)
            o_ref[here, pair * LANES : (pair + 1) * LANES] = both.T.astype(BF16)
        return carry

    lax.fori_loop(0, tokens // QBLK, block, 0)


def attend_backward(
    qkv_ref, lse_ref, o_ref, do_ref, fine_cos, fine_sin, coarse_cos, coarse_sin,
    dqkv_ref,
    dq, kt, dk, dv, cos_ref, sin_ref,
):
    fill_rotary(fine_cos, fine_sin, coarse_cos, coarse_sin, cos_ref, sin_ref)
    tokens, query_width = o_ref.shape
    pairs = query_width // LANES
    key_lanes = slice(query_width, query_width + LANES)
    value_lanes = slice(query_width + LANES, query_width + 2 * LANES)

    def turn_keys(i, carry):
        rows = pl.ds(pl.multiple_of(i * QBLK, QBLK), QBLK)
        kt[:, rows] = qkv_ref[rows, key_lanes].astype(F32).T[:HEAD_SIZE, :].astype(BF16)
        return carry

    lax.fori_loop(0, tokens // QBLK, turn_keys, 0)
    dk[...] = jnp.zeros_like(dk)
    dv[...] = jnp.zeros_like(dv)
    low_lanes = iota((QBLK, LANES), 1) < HEAD_SIZE
    wide = (QBLK, 2 * QBLK)
    visible = iota(wide, 0) <= iota(wide, 1) % QBLK
    ones = jnp.ones((EDGE, LANES), BF16)

    def block(i, carry):
        here = pl.ds(pl.multiple_of(i * QBLK, QBLK), QBLK)
        queries, grads, inners, lses = [], [], [], []
        for pair in range(pairs):
            lanes = slice(pair * LANES, (pair + 1) * LANES)
            queries.append(pair_split(qkv_ref[here, lanes], low_lanes))
            grad = do_ref[here, lanes]
            grads.append(pair_split(grad, low_lanes))
            both = pair_split(grad.astype(F32) * o_ref[here, lanes].astype(F32), low_lanes)
            high, low = parts(both, 2)
            inners.append((dot(ones, high, NT) + dot(ones, low, NT))[:1])
            lses.append(
                jnp.concatenate(
                    [
                        lse_ref[2 * pair : 2 * pair + 1, here],
                        lse_ref[2 * pair + 1 : 2 * pair + 2, here],
                    ],
                    axis=1,
                )
            )
        query_all = jnp.concatenate(queries, axis=0)
        grad_all = jnp.concatenate(grads, axis=0)

        def tile(there, state, edge):
            keys = qkv_ref[there, key_lanes]
            values = qkv_ref[there, value_lanes]
            all_probs, all_dscores, result = [], [], []
            for pair in range(pairs):
                probs = dot(keys, queries[pair], NT) - lses[pair]
                if edge:
                    probs = jnp.where(visible, probs, MASKED)
                probs = jnp.exp(probs)
                dprobs = dot(values, grads[pair], NT)
                dscores = (probs * (dprobs - inners[pair])).astype(BF16)
                all_probs.append(probs.astype(BF16))
                all_dscores.append(dscores)
                result.append(state[pair] + dot(kt[:, there], dscores))
            dv[there, :] += dot(jnp.concatenate(all_probs, axis=1), grad_all)
            dk[there, :] += dot(jnp.concatenate(all_dscores, axis=1), query_all)
            return tuple(result)

        state = (jnp.zeros((HEAD_SIZE, 2 * QBLK), F32),) * pairs
        state = lax.fori_loop(
            0,
            i,
            lambda j, state: tile(pl.ds(pl.multiple_of(j * QBLK, QBLK), QBLK), state, False),
            state,
        )
        state = tile(here, state, True)
        for pair in range(pairs):
            both = jnp.concatenate([state[pair][:, :QBLK], state[pair][:, QBLK:]], axis=0)
            dq[here, pair * LANES : (pair + 1) * LANES] = both.T
        return carry

    lax.fori_loop(0, tokens // QBLK, block, 0)
    masks = head_masks()
    within, (fold, fold_turn, fold_value) = masks[0], masks[4:]

    def turn_back(i, carry):
        rows = pl.ds(pl.multiple_of(i * QBLK, QBLK), QBLK)
        cosine, sine = cos_ref[rows, :], sin_ref[rows, :]
        for pair in range(pairs):
            lanes = slice(pair * LANES, (pair + 1) * LANES)
            grad = dq[rows, lanes]
            grad = grad * cosine - pick(grad, within) * sine
            dqkv_ref[rows, lanes] = (grad * HEAD_SIZE**-0.5).astype(BF16)
        grad = dk[rows, :]
        grad = pick(grad, fold) * cosine - pick(grad, fold_turn) * sine
        grad = grad + pick(dv[rows, :], fold_value)
        dqkv_ref[rows, query_width:] = grad.astype(BF16)
        return carry

    lax.fori_loop(0, tokens // QBLK, turn_back, 0)


def run_attend_forward(proj, query_at, query_width, tables):
    tokens = proj.shape[0]
    cols = lambda size, at: pl.BlockSpec((tokens, size), lambda turn: (0, at // size))
    return pl.pallas_call(
        attend_forward,
        grid=(1,),
        out_shape=(
            jax.ShapeDtypeStruct((tokens, query_width + 2 * LANES), BF16),
            jax.ShapeDtypeStruct((EDGE, tokens), F32),
            jax.ShapeDtypeStruct((tokens, query_width), BF16),
        ),
        in_specs=[
            cols(query_width, query_at),
            cols(2 * HEAD_SIZE, query_at + query_width),
        ]
        + [whole_spec(table) for table in tables],
        out_specs=(
            cols(query_width + 2 * LANES, 0),
            pl.BlockSpec((EDGE, tokens), lambda turn: (0, 0)),
            cols(query_width, 0),
        ),
        scratch_shapes=[
            pltpu.VMEM((HEAD_SIZE, tokens), BF16),
            pltpu.VMEM((tokens, LANES), F32),
            pltpu.VMEM((tokens, LANES), F32),
        ],
        cost_estimate=cost(15),
        name="attend_forward",
    )(proj, proj, *tables)


def run_attend_backward(qkv, lse, attended, grads, grad_at, tables):
    tokens, query_width = attended.shape
    vmem = pl.BlockSpec(memory_space=pltpu.VMEM)
    cols = lambda size, at: pl.BlockSpec((tokens, size), lambda turn: (0, at // size))
    return pl.pallas_call(
        attend_backward,
        grid=(1,),
        out_shape=jax.ShapeDtypeStruct((tokens, query_width + 2 * HEAD_SIZE), BF16),
        in_specs=[
            whole_spec(qkv),
            whole_spec(lse),
            whole_spec(attended),
            cols(query_width, grad_at),
        ]
        + [whole_spec(table) for table in tables],
        out_specs=cols(query_width + 2 * HEAD_SIZE, 0),
        scratch_shapes=[
            pltpu.VMEM((tokens, query_width), F32),
            pltpu.VMEM((HEAD_SIZE, tokens), BF16),
            pltpu.VMEM((tokens, LANES), F32),
            pltpu.VMEM((tokens, LANES), F32),
            pltpu.VMEM((tokens, LANES), F32),
            pltpu.VMEM((tokens, LANES), F32),
        ],
        cost_estimate=cost(16),
        name="attend_backward",
    )(qkv, lse, attended, grads, *tables)


def feed_forward(
    x_ref, mixed_ref, other_ref, act_grad_ref, norms_ref, gu_ref,
    after_ref, scale_ref, hidden_ref, act_ref, dgu_ref, back_ref,
):
    units = act_grad_ref.shape[1]
    after = x_ref[...].astype(F32) + (mixed_ref[...].astype(F32) + other_ref[...].astype(F32))
    after_ref[...] = after.astype(BF16)
    scale = lax.rsqrt(jnp.mean(after * after, axis=-1, keepdims=True) + EPSILON)
    scale_ref[...] = scale
    hidden = (after * scale * norms_ref[1:2, :]).astype(BF16)
    hidden_ref[...] = hidden
    for start in range(0, units, UBLK):
        cols = slice(start, start + UBLK)
        up_cols = slice(units + start, units + start + UBLK)
        gate = dot(hidden, gu_ref[:, cols])
        upward = dot(hidden, gu_ref[:, up_cols])
        grad = act_grad_ref[:, cols]
        sigma = jax.nn.sigmoid(gate)
        swish = gate * sigma
        act_ref[:, cols] = (swish * upward).astype(BF16)
        slope = sigma * (1.0 + gate * (1.0 - sigma))
        dgu_ref[:, cols] = (grad * upward * slope).astype(BF16)
        dgu_ref[:, up_cols] = (grad * swish).astype(BF16)
    back_ref[...] = dot(dgu_ref[...], gu_ref[...], NT).astype(BF16)


def product_rows(dims, left_ref, right_ref, out_ref):
    out_ref[...] = dot(left_ref[...], right_ref[...], dims).astype(out_ref.dtype)


def run_product(left, right, dims, dtype):
    tokens, depth = left.shape
    cols = right.shape[1 - dims[1][0]]
    return pl.pallas_call(
        functools.partial(product_rows, dims),
        grid=(tokens // TBLK,),
        out_shape=jax.ShapeDtypeStruct((tokens, cols), dtype),
        in_specs=[pl.BlockSpec((TBLK, depth), lambda turn: (turn, 0)), once(right)],
        out_specs=pl.BlockSpec((TBLK, cols), lambda turn: (turn, 0)),
        cost_estimate=cost(4),
        name="product_rows",
    )(left, right)


def project(heads, x_ref, w_ref, hidden_ref, proj_ref, norms_ref):
    @pl.when(pl.program_id(0) == 0)
    def _():
        gains = w_ref[:, w_ref.shape[1] - LANES :].astype(F32).T
        norms_ref[...] = jnp.zeros_like(norms_ref)
        norms_ref[0:2, :] = gains[heads : heads + 2, :]

    x = x_ref[...].astype(F32)
    scale = lax.rsqrt(jnp.mean(x * x, axis=-1, keepdims=True) + EPSILON)
    hidden = (x * scale * norms_ref[0:1, :]).astype(BF16)
    hidden_ref[...] = hidden
    proj_ref[...] = dot(hidden, w_ref[...])


def run_project(x, w_in, heads):
    tokens, width = x.shape
    cols = w_in.shape[1]
    rows = lambda size: pl.BlockSpec((TBLK, size), lambda turn: (turn, 0))
    return pl.pallas_call(
        functools.partial(project, heads),
        grid=(tokens // TBLK,),
        out_shape=(
            jax.ShapeDtypeStruct((tokens, width), BF16),
            jax.ShapeDtypeStruct((tokens, cols), F32),
            jax.ShapeDtypeStruct((EDGE, width), F32),
        ),
        in_specs=[rows(width), once(w_in)],
        out_specs=(
            rows(width), rows(cols), pl.BlockSpec((EDGE, width), lambda turn: (0, 0)),
        ),
        cost_estimate=cost(8),
        name="project",
    )(x, w_in)


def project_back(grad_ref, w_ref, x_ref, part_ref, gain_grad_ref):
    @pl.when(pl.program_id(0) == 0)
    def _():
        gain_grad_ref[...] = jnp.zeros_like(gain_grad_ref)

    x = x_ref[...].astype(F32)
    normed = x * lax.rsqrt(jnp.mean(x * x, axis=-1, keepdims=True) + EPSILON)
    part = dot(grad_ref[...], w_ref[...], NT).astype(BF16)
    part_ref[...] = part
    gain_grad_ref[:1, :] += jnp.sum(part.astype(F32) * normed, axis=0, keepdims=True)


def run_project_back(grads, w_in, x):
    tokens, width = x.shape
    cols = w_in.shape[1]
    rows = lambda size: pl.BlockSpec((TBLK, size), lambda turn: (turn, 0))
    return pl.pallas_call(
        project_back,
        grid=(tokens // TBLK,),
        out_shape=(
            jax.ShapeDtypeStruct((tokens, width), BF16),
            jax.ShapeDtypeStruct((EDGE, width), F32),
        ),
        in_specs=[rows(cols), once(w_in), rows(width)],
        out_specs=(rows(width), pl.BlockSpec((EDGE, width), lambda turn: (0, 0))),
        cost_estimate=cost(8),
        name="project_back",
    )(grads, w_in, x)


def once(item):
    return pl.BlockSpec(item.shape, lambda turn: (0,) * item.ndim, pipeline_mode=pl.Buffered(1))


def run_feed_forward(x, mixed, other, act_grad, norms, w_gate_up):
    tokens, width = x.shape
    units = act_grad.shape[1]
    rows = lambda size: pl.BlockSpec((TBLK, size), lambda turn: (turn, 0))
    shape = jax.ShapeDtypeStruct
    return pl.pallas_call(
        feed_forward,
        grid=(tokens // TBLK,),
        out_shape=(
            shape((tokens, width), BF16),
            shape((tokens, 1), F32),
            shape((tokens, width), BF16),
            shape((tokens, units), BF16),
            shape((tokens, 2 * units), BF16),
            shape((tokens, width), BF16),
        ),
        in_specs=[rows(width)] * 3 + [rows(units), once(norms), once(w_gate_up)],
        out_specs=(rows(width), rows(1), rows(width), rows(units), rows(2 * units), rows(width)),
        cost_estimate=cost(14),
        name="feed_forward",
    )(x, mixed, other, act_grad, norms, w_gate_up)


def mixer_forward(gated_ref, scale_ref, gain_ref, attended_ref, w_ref, low_ref, mixed_ref):
    channels = gated_ref.shape[1]
    scale = scale_ref[...].T[:, :1]
    low_ref[:, :channels] = (gated_ref[...].astype(F32) * scale * gain_ref[...]).astype(BF16)
    low_ref[:, channels:] = attended_ref[...]
    mixed_ref[...] = dot(low_ref[...], w_ref[...], NT).astype(BF16)


def run_mixer_forward(gated, scale, gain, attended, w_out):
    tokens, channels = gated.shape
    width, inner = w_out.shape
    rows = lambda size: pl.BlockSpec((TBLK, size), lambda turn: (turn, 0))
    return pl.pallas_call(
        mixer_forward,
        grid=(tokens // TBLK,),
        out_shape=(
            jax.ShapeDtypeStruct((tokens, inner), BF16),
            jax.ShapeDtypeStruct((tokens, width), BF16),
        ),
        in_specs=[
            rows(channels),
            pl.BlockSpec((EDGE, TBLK), lambda turn: (0, turn)),
            once(gain),
            rows(attended.shape[1]),
            once(w_out),
        ],
        out_specs=(rows(inner), rows(width)),
        cost_estimate=cost(5),
        name="mixer_forward",
    )(gated, scale, gain, attended, w_out)


def mixer_backward(
    part_ref, other_ref, after_ref, scale_ref, top_ref, norms_ref,
    w_ref, gated_ref, scale_m_ref, gain_m_ref,
    low_ref, mamba_ref, attended_ref, inner_ref, gain_grad_ref,
):
    channels = gated_ref.shape[1]

    @pl.when(pl.program_id(0) == 0)
    def _():
        gain_grad_ref[...] = jnp.zeros_like(gain_grad_ref)

    grad = part_ref[...].astype(F32) + other_ref[...].astype(F32)
    scale = scale_ref[...]
    normed = after_ref[...].astype(F32) * scale
    gain_grad_ref[:1, :] += jnp.sum(grad * normed, axis=0, keepdims=True)
    weighted = grad * norms_ref[1:2, :]
    mean = jnp.mean(weighted * normed, axis=-1, keepdims=True)
    total = top_ref[...].astype(F32) + scale * (weighted - normed * mean)
    low_ref[...] = total.astype(BF16)
    back = dot(low_ref[...], w_ref[...])
    mamba = back[:, :channels]
    mamba_ref[...] = mamba
    attended_ref[...] = back[:, channels:].astype(BF16)
    inner_ref[...] = row_sums(mamba * gain_m_ref[...] * gated_ref[...].astype(F32)) * scale_m_ref[...]


def run_mixer_backward(part, other, after, scale, top, norms, w_out, gated, scale_m, gain_m):
    tokens, width = after.shape
    channels = gated.shape[1]
    inner = w_out.shape[1]
    shape = jax.ShapeDtypeStruct
    rows = lambda size: pl.BlockSpec((NBLK, size), lambda turn: (turn, 0))
    lanes = pl.BlockSpec((EDGE, NBLK), lambda turn: (0, turn))
    return pl.pallas_call(
        mixer_backward,
        grid=(tokens // NBLK,),
        out_shape=(
            shape((tokens, width), BF16),
            shape((tokens, channels), F32),
            shape((tokens, inner - channels), BF16),
            shape((EDGE, tokens), F32),
            shape((EDGE, width), F32),
        ),
        in_specs=[rows(width)] * 3
        + [rows(1), rows(width), once(norms), once(w_out), rows(channels), lanes, once(gain_m)],
        out_specs=(
            rows(width), rows(channels), rows(inner - channels), lanes,
            pl.BlockSpec((EDGE, width), lambda turn: (0, 0)),
        ),
        cost_estimate=cost(8),
        name="mixer_backward",
    )(part, other, after, scale, top, norms, w_out, gated, scale_m, gain_m)


def lane_row(ref, first, count):
    return jnp.concatenate([ref[i : i + 1, :] for i in range(first, first + count)], axis=1)


def own_lanes(ref, first, size):
    start = lax.axis_index("dp") * size
    row = ref[pl.ds(first + lax.div(start, LANES), 1), :]
    row = jnp.broadcast_to(row, (EDGE, LANES))
    return pltpu.roll(row, lax.rem(LANES - lax.rem(start, LANES), LANES), 1)[0, :size]


def finish_layer(
    norm_at, x_ref, norms_ref, part_ref, other_ref, grad_ref, after_ref, ffn_ref, ffn_other_ref,
    total_ref, *refs,
):
    count = (len(refs) - 9) // 2
    passed, out_ref, result_ref, handed = refs[:count], refs[count], refs[count + 1], refs[count + 2 :]
    tap_ref, bias_ref, gain_ref, step_ref, log_ref, skip_ref, norm_ref = handed[count:]

    @pl.when(pl.program_id(0) == 0)
    def _():
        for source, target in zip(passed, handed):
            target[...] = source[...]
        rows = tap_ref.shape[1] // LANES
        for tap in range(KCONV):
            tap_ref[tap : tap + 1, :] = lane_row(total_ref, tap * rows, rows)
        bias_ref[...] = lane_row(total_ref, KCONV * rows, rows)[0]
        gain_ref[...] = lane_row(total_ref, (KCONV + 1) * rows, rows)[0]
        at = (KCONV + 2) * rows
        for place, ref in enumerate((step_ref, log_ref, skip_ref)):
            ref[...] = total_ref[at + place : at + place + 1, :][0, : ref.shape[0]]
        norm_ref[...] = own_lanes(total_ref, norm_at, norm_ref.shape[0])

    x = x_ref[...].astype(F32)
    scale = lax.rsqrt(jnp.mean(x * x, axis=-1, keepdims=True) + EPSILON)
    normed = x * scale
    weighted = (part_ref[...].astype(F32) + other_ref[...].astype(F32)) * norms_ref[0:1, :]
    mean = jnp.mean(weighted * normed, axis=-1, keepdims=True)
    out_ref[...] = grad_ref[...].astype(F32) + scale * (weighted - normed * mean)
    ffn = ffn_ref[...].astype(F32) + ffn_other_ref[...].astype(F32)
    result_ref[...] = (after_ref[...].astype(F32) + ffn).astype(BF16)


def run_finish(
    x, norms, part, other, grad, after, ffn, ffn_other, total, passed, channels, heads, shard,
    norm_at,
):
    tokens, width = x.shape
    rows = pl.BlockSpec((TBLK, width), lambda turn: (turn, 0))
    shape = lambda *sizes: jax.ShapeDtypeStruct(sizes, F32)
    small = (
        shape(KCONV, channels), shape(channels), shape(channels), shape(heads), shape(heads),
        shape(heads), shape(shard),
    )
    return pl.pallas_call(
        functools.partial(finish_layer, norm_at),
        grid=(tokens // TBLK,),
        out_shape=(shape(tokens, width), jax.ShapeDtypeStruct((tokens, width), BF16))
        + tuple(shape(*item.shape) for item in passed)
        + small,
        in_specs=[rows, once(norms)] + [rows] * 6 + [once(total)] + [once(item) for item in passed],
        out_specs=(rows, rows) + tuple(once(item) for item in passed + small),
        cost_estimate=cost(8),
        name="finish_layer",
    )(x, norms, part, other, grad, after, ffn, ffn_other, total, *passed)


def finish_shared(at, total_ref, cross_ref, mine_ref, other_ref, bc_ref, tap_ref, bias_ref, norm_ref, both):
    half = lax.axis_index("tensor")
    cols = pl.ds(pl.multiple_of(half * LANES, LANES), LANES)
    bc_ref[...] = mine_ref[:, cols] + other_ref[:, cols]
    both[...] = total_ref[...] + cross_ref[...]
    for tap in range(KCONV):
        tap_ref[tap : tap + 1, :] = both[pl.ds(at + 2 * tap + half, 1), :]
    bias_ref[...] = both[pl.ds(at + 2 * KCONV + half, 1), :][0]
    norm_ref[...] = own_lanes(both, at + 2 * KCONV + 2, norm_ref.shape[0])


def run_finish_shared(total, cross, mine, other, shard, at):
    vmem = pl.BlockSpec(memory_space=pltpu.VMEM)
    shape = lambda *sizes: jax.ShapeDtypeStruct(sizes, F32)
    return pl.pallas_call(
        functools.partial(finish_shared, at),
        out_shape=(shape(mine.shape[0], LANES), shape(KCONV, LANES), shape(LANES), shape(shard)),
        in_specs=[vmem] * 4,
        out_specs=(vmem,) * 4,
        scratch_shapes=[pltpu.VMEM(total.shape, F32)],
        name="finish_shared",
    )(total, cross, mine, other)


def swap(partial):
    return lax.ppermute(partial, "tensor", [(0, 1), (1, 0)])


def join(mine, other):
    return mine.astype(F32) + other.astype(F32)


def tensor_sum(partial):
    return join(partial, swap(partial))


def windows_of(size, count):
    part = size // count // LANES * LANES
    return [(i * part, size if i == count - 1 else (i + 1) * part) for i in range(count)]


def local(
    layer_input, w_norm1, w_zx, w_bc, w_dt, conv_x, conv_xb, conv_bc, conv_bcb, dt_bias, a_log,
    d_skip, w_mnorm, w_mout, query_key_value_weight, output_weight, w_norm2, w_gu, w_down,
    grad_output,
):
    devices = lax.axis_size("dp")
    tokens, width = layer_input.shape
    shard = w_zx.shape[0]
    channels = conv_xb.shape[0]
    heads = dt_bias.shape[0]
    qkv_width = query_key_value_weight.shape[2]
    units = w_down.shape[0]
    attn_width = output_weight.shape[1]
    tail = jnp.concatenate(
        [w_dt, w_norm1[:, None], w_norm2[:, None], jnp.zeros((shard, LANES - heads - 2), BF16)],
        axis=1,
    )
    mixer_in = jnp.concatenate(
        [w_zx.reshape(shard, -1), w_bc, query_key_value_weight.reshape(shard, -1), tail], axis=1
    )
    in_width = mixer_in.shape[1]
    (w_in,) = gather_rows([mixer_in], devices, 0, [(0, *window) for window in windows_of(in_width, 6)])
    w_in, *small_params = lax.optimization_barrier(
        (w_in, conv_x, conv_xb, conv_bc, conv_bcb, dt_bias, a_log, d_skip, w_mnorm)
    )
    params = scan_params(*small_params)
    hidden_one, proj, norms = run_project(layer_input, w_in, heads)
    out_shard = jnp.concatenate([w_mout.T, output_weight.reshape(attn_width, -1).T], axis=1)
    y, gated, square_sum, entering, w_out = run_scan_forward(
        proj, qkv_width, params, out_shard, devices
    )
    channels_all = channels * lax.axis_size("tensor")
    scale_m = lax.rsqrt(tensor_sum(square_sum) / channels_all + EPSILON)
    tables = rotary_tables(tokens)
    qkv_at = 2 * channels + 2 * NS
    qkv, lse, attended = run_attend_forward(proj, qkv_at, attn_width, tables)
    gain_m = w_mnorm.astype(F32)[None, :]
    mixer_out, mixed = run_mixer_forward(gated, scale_m, gain_m, attended, w_out)
    mixed, gate_up_shard, down_shard = lax.optimization_barrier(
        (mixed, w_gu.reshape(shard, -1), w_down.T)
    )
    other = swap(mixed)
    w_gate_up, w_down_t = gather_rows(
        [gate_up_shard, down_shard],
        devices,
        3,
        [(0, 0, units), (0, units, 2 * units), (1, 0, units)],
    )
    act_grad = run_product(grad_output, w_down_t, NN, F32)
    other, w_gate_up, w_down_t, act_grad = lax.optimization_barrier(
        (other, w_gate_up, w_down_t, act_grad)
    )
    after, scale_two, hidden_two, activated, grad_gu_low, partial_two = run_feed_forward(
        layer_input, mixed, other, act_grad, norms, w_gate_up
    )
    other = swap(partial_two)
    grad_down = dot(grad_output, activated, TN).astype(BF16)
    (mine_gu,) = scatter_product(
        hidden_two,
        grad_gu_low,
        [
            ([(0, 1, 0, units)], [(0, 0, units, 0, 0)]),
            ([(0, 1, units, 2 * units)], [(0, 0, units, 0, 1)]),
        ],
        [(shard, 2, units)],
        devices,
        1,
    )
    ffn_part = run_product(activated, w_down_t, NT, BF16)
    other, mine_gu, grad_down, ffn_part = lax.optimization_barrier(
        (other, mine_gu, grad_down, ffn_part)
    )
    ffn_other = swap(ffn_part)
    grad_mix_low, grad_mamba, grad_attended, inner_m, grad_norm2 = run_mixer_backward(
        partial_two, other, after, scale_two, grad_output, norms, w_out, gated, scale_m, gain_m
    )
    inner_m = tensor_sum(inner_m) / channels_all
    dqkv = run_attend_backward(qkv, lse, attended, grad_attended, 0, tables)
    grad_out = dot(grad_mix_low, mixer_out, TN).astype(BF16)
    windows = [(0, None, 0, channels + attn_width), (1, None, 0, units)]
    pieces = [
        (0, 0, channels, 0, None),
        (0, channels, channels + attn_width, 1, None),
        (1, 0, units, 2, None),
    ]
    shapes = [(shard, channels), (shard, attn_width), (shard, units)]
    grad_proj, small_x, small_h, mine_mout, mine_o, mine_down = run_scan_backward(
        proj, y, entering, grad_mamba, scale_m, inner_m, dqkv, params,
        [grad_out, grad_down], windows, pieces, shapes, devices,
    )
    ffn_other, grad_proj = lax.optimization_barrier((ffn_other, grad_proj))
    partial_one, grad_norm1 = run_project_back(grad_proj, w_in, layer_input)
    partial_one, grad_proj = lax.optimization_barrier((partial_one, grad_proj))
    other = swap(partial_one)
    lanes_of = lambda size, start=0: range(start, start + size, LANES)
    places = [(0, row, lane) for row in range(KCONV + 2) for lane in lanes_of(channels)]
    places += [(1, row, 0) for row in range(3)]
    norm_at = len(places)
    places += [(2, 0, lane) for lane in lanes_of(width)]
    cross_at = len(places)
    places += [(0, row, lane) for row in range(KCONV + 1) for lane in lanes_of(2 * NS, channels)]
    places += [(3, 0, lane) for lane in lanes_of(width)]
    shared_at = 2 * channels
    step_at = qkv_at + qkv_width
    mine_zx, mine_bc, mine_qkv, mine_step, small = scatter_product(
        hidden_one,
        grad_proj,
        [
            ([(0, 1, 0, channels)], [(0, 0, channels, 0, 0)]),
            ([(0, 1, channels, shared_at)], [(0, 0, channels, 0, 1)]),
            (
                [(0, 1, shared_at, in_width)],
                [
                    (0, 0, 2 * NS, 1, None),
                    (0, 2 * NS, 2 * NS + qkv_width, 2, 0),
                    (0, 2 * NS + qkv_width, in_width - shared_at, 3, "turned"),
                ],
            ),
        ],
        [
            (shard, 2, channels),
            (shard, 2 * NS),
            (shard, 1, qkv_width),
            (heads, shard),
        ],
        devices,
        5,
        (small_x, small_h, grad_norm2, grad_norm1),
        places,
    )
    other, mine_bc = lax.optimization_barrier((other, mine_bc))
    passed = (mine_zx, mine_qkv, mine_step, mine_mout, mine_o, mine_gu, mine_down)
    cross, other_bc = swap(small), swap(mine_bc)
    grad_source, result, *rest = run_finish(
        layer_input, norms, partial_one, other, grad_mix_low, after, ffn_part, ffn_other, small,
        passed, channels, heads, shard, norm_at,
    )
    mine_zx, mine_qkv, mine_step, mine_mout, mine_o, mine_gu, mine_down = rest[: len(passed)]
    grad_taps, grad_bias, grad_gain, grad_steps, grad_log, grad_skip, own_norm2 = rest[len(passed) :]
    grad_bc, grad_tapsb, grad_biasb, own_norm1 = run_finish_shared(
        small, cross, mine_bc, other_bc, shard, cross_at
    )
    return (
        result,
        grad_source,
        own_norm1,
        mine_zx,
        grad_bc,
        mine_step.T,
        grad_taps,
        grad_bias,
        grad_tapsb,
        grad_biasb,
        grad_steps,
        grad_log,
        grad_skip,
        grad_gain,
        mine_mout.T,
        mine_qkv,
        mine_o.T.reshape(output_weight.shape),
        own_norm2,
        mine_gu,
        mine_down.T,
    )


def solution(mesh):
    return jax.shard_map(
        local,
        mesh=mesh,
        in_specs=(
            P("dp", None),
            P("dp"),
            P("dp", None, "tensor"),
            P("dp", None),
            P("dp", "tensor"),
            P(None, "tensor"),
            P("tensor"),
            P(),
            P(),
            P("tensor"),
            P("tensor"),
            P("tensor"),
            P("tensor"),
            P("tensor", "dp"),
            P("dp", "tensor", None),
            P("tensor", None, "dp"),
            P("dp"),
            P("dp", None, "tensor"),
            P("tensor", "dp"),
            P("dp", None),
        ),
        out_specs=(
            P("dp", None),
            P("dp", None),
            P("dp"),
            P("dp", None, "tensor"),
            P("dp", "tensor"),
            P("dp", "tensor"),
            P(None, "tensor"),
            P("tensor"),
            P(None, "tensor"),
            P("tensor"),
            P("tensor"),
            P("tensor"),
            P("tensor"),
            P("tensor"),
            P("tensor", "dp"),
            P("dp", "tensor", None),
            P("tensor", None, "dp"),
            P("dp"),
            P("dp", None, "tensor"),
            P("tensor", "dp"),
        ),
        check_vma=False,
    )
```
